128 devices in a mesh: cp: 2 (over core), fsdp: 64 (over z, y, x).
Axes of the slice: x: 4, y: 4, z: 4, core: 2. Of those that a mesh axis runs over, the one named last changes fastest.
Arguments:
- hidden: bfloat16 [64, 1024, 2048], P('fsdp', 'cp')
- tok_pos: int32 [64, 1024], P('fsdp', 'cp')
- grad_out: bfloat16 [64, 1024, 2048], P('fsdp', 'cp')
- norm_gain: float32 [2048], P(('fsdp', 'cp'))
- w_query: bfloat16 [2048, 2048], P(('fsdp', 'cp'))
- w_key: bfloat16 [2048, 256], P(('fsdp', 'cp'))
- w_value: bfloat16 [2048, 256], P(('fsdp', 'cp'))
- w_out: bfloat16 [2048, 2048], P(('fsdp', 'cp'))
Outputs:
- output 1: bfloat16 [64, 1024, 2048], P('fsdp', 'cp')
- output 2: bfloat16 [64, 1024, 2048], P('fsdp', 'cp')
- output 3: float32 [2048, 2048], P(('fsdp', 'cp'))
- output 4: float32 [2048, 256], P(('fsdp', 'cp'))
- output 5: float32 [2048, 256], P(('fsdp', 'cp'))
- output 6: float32 [2048, 2048], P(('fsdp', 'cp'))
- output 7: float32 [2048], P(('fsdp', 'cp'))
All inputs are finite; a program needn't handle non-finite values.
Results may differ from the reference program's by a relative error of at most 0.00684.
Values are sent between devices in bfloat16 or wider.
A program may use at most 1 GiB of HBM per device.

```python
import jax
import jax.numpy as jnp
from jax import lax

SEQS_TOTAL = 64
SEQ_LEN = 1024
MODEL_DIM = 2048
NUM_HEADS = 16
NUM_KV_HEADS = 2
HEAD_DIM = 128
Q_BLOCK = 32
ROPE_THETA = 1000000.0
RMS_EPS = 1e-5
NEG_BIG = -1e30
SCALE = HEAD_DIM ** -0.5
GROUP_SIZE = NUM_HEADS // NUM_KV_HEADS
N_QBLOCKS = SEQ_LEN // Q_BLOCK


def setup_inputs(seed: int = 0) -> dict:
    rand_keys = jax.random.split(jax.random.key(seed), 8)
    q_cols = NUM_HEADS * HEAD_DIM
    kv_cols = NUM_KV_HEADS * HEAD_DIM
    in_scale = MODEL_DIM ** -0.5
    hidden = jax.random.normal(rand_keys[0], (SEQS_TOTAL, SEQ_LEN, MODEL_DIM), jnp.float32)
    base_pos = jnp.broadcast_to(jnp.arange(SEQ_LEN, dtype=jnp.int32), (SEQS_TOTAL, SEQ_LEN))
    tok_pos = jax.random.permutation(rand_keys[1], base_pos, axis=1, independent=True)
    grad_out = jax.random.normal(rand_keys[2], (SEQS_TOTAL, SEQ_LEN, MODEL_DIM), jnp.float32)
    norm_gain = jax.random.uniform(rand_keys[3], (MODEL_DIM,), jnp.float32, 0.5, 1.5)
    w_query = jax.random.normal(rand_keys[4], (MODEL_DIM, q_cols), jnp.float32) * in_scale
    w_key = jax.random.normal(rand_keys[5], (MODEL_DIM, kv_cols), jnp.float32) * in_scale
    w_value = jax.random.normal(rand_keys[6], (MODEL_DIM, kv_cols), jnp.float32) * in_scale
    w_out = jax.random.normal(rand_keys[7], (q_cols, MODEL_DIM), jnp.float32) * q_cols ** -0.5
    return {'hidden': hidden.astype(jnp.bfloat16), 'tok_pos': tok_pos, 'grad_out': grad_out.astype(jnp.bfloat16), 'norm_gain': norm_gain, 'w_query': w_query.astype(jnp.bfloat16), 'w_key': w_key.astype(jnp.bfloat16), 'w_value': w_value.astype(jnp.bfloat16), 'w_out': w_out.astype(jnp.bfloat16)}


def rope_tables(positions):
    half_dim = HEAD_DIM // 2
    inv_freq = ROPE_THETA ** (-jnp.arange(half_dim, dtype=jnp.float32) / half_dim)
    angles = positions.astype(jnp.float32)[..., None] * inv_freq
    return jnp.cos(angles)[..., None, :], jnp.sin(angles)[..., None, :]


def rope_apply(values, cos_tab, sin_tab):
    half_dim = HEAD_DIM // 2
    first_half = values[..., :half_dim]
    second_half = values[..., half_dim:]
    return jnp.concatenate([first_half * cos_tab - second_half * sin_tab, second_half * cos_tab + first_half * sin_tab], axis=-1)


def rope_transpose(values, cos_tab, sin_tab):
    half_dim = HEAD_DIM // 2
    first_half = values[..., :half_dim]
    second_half = values[..., half_dim:]
    return jnp.concatenate([first_half * cos_tab + second_half * sin_tab, second_half * cos_tab - first_half * sin_tab], axis=-1)


def seq_pass(hidden, tok_pos, grad_out, norm_gain, w_query, w_key, w_value, w_out):
    x_f32 = hidden.astype(jnp.float32)
    inv_rms = lax.rsqrt(jnp.mean(x_f32 * x_f32, axis=-1) + RMS_EPS)
    x_hat = x_f32 * inv_rms[:, None]
    normed = (x_hat * norm_gain).astype(jnp.bfloat16)
    cos_tab, sin_tab = rope_tables(tok_pos)
    q_lin = jnp.dot(normed, w_query, preferred_element_type=jnp.float32).reshape(SEQ_LEN, NUM_HEADS, HEAD_DIM)
    k_lin = jnp.dot(normed, w_key, preferred_element_type=jnp.float32).reshape(SEQ_LEN, NUM_KV_HEADS, HEAD_DIM)
    q_rot = rope_apply(q_lin, cos_tab, sin_tab).astype(jnp.bfloat16)
    k_rot = rope_apply(k_lin, cos_tab, sin_tab).astype(jnp.bfloat16)
    v_val = jnp.dot(normed, w_value, preferred_element_type=jnp.float32).astype(jnp.bfloat16).reshape(SEQ_LEN, NUM_KV_HEADS, HEAD_DIM)
    k_f32 = k_rot.astype(jnp.float32)
    v_f32 = v_val.astype(jnp.float32)
    q_blocks = q_rot.reshape(N_QBLOCKS, Q_BLOCK, NUM_KV_HEADS, GROUP_SIZE, HEAD_DIM)
    pos_blocks = tok_pos.reshape(N_QBLOCKS, Q_BLOCK)

    def block_scores(q_blk, q_pos):
        scores = jnp.einsum('ikgd,jkd->kigj', q_blk.astype(jnp.float32), k_f32) * SCALE
        visible = tok_pos[None, None, None, :] <= q_pos[None, :, None, None]
        return jnp.where(visible, scores, NEG_BIG), visible

    def fwd_block(blk_args):
        q_blk, q_pos = blk_args
        scores, visible = block_scores(q_blk, q_pos)
        row_max = jnp.max(scores, axis=-1)
        att_probs = jnp.where(visible, jnp.exp(scores - row_max[..., None]), 0.0)
        row_sum = jnp.sum(att_probs, axis=-1)
        out_blk = jnp.einsum('kigj,jkd->ikgd', att_probs.astype(jnp.bfloat16).astype(jnp.float32), v_f32)
        out_blk = out_blk / jnp.transpose(row_sum, (1, 0, 2))[..., None]
        return out_blk.astype(jnp.bfloat16), row_max + jnp.log(row_sum)

    attn_out, log_sum = lax.map(fwd_block, (q_blocks, pos_blocks))
    attn_flat = attn_out.reshape(SEQ_LEN, NUM_HEADS * HEAD_DIM)
    result = (x_f32 + jnp.dot(attn_flat, w_out, preferred_element_type=jnp.float32)).astype(jnp.bfloat16)
    grad_w_out = jnp.dot(attn_flat.T, grad_out, preferred_element_type=jnp.float32)
    grad_attn = jnp.dot(grad_out, w_out.T, preferred_element_type=jnp.float32).astype(jnp.bfloat16)
    gout_blocks = grad_attn.reshape(N_QBLOCKS, Q_BLOCK, NUM_KV_HEADS, GROUP_SIZE, HEAD_DIM)
    row_delta = jnp.einsum('nikgd,nikgd->nkig', gout_blocks.astype(jnp.float32), attn_out.astype(jnp.float32))

    def bwd_block(kv_grads, blk_args):
        grad_k, grad_v = kv_grads
        q_blk, q_pos, gout_blk, lse_blk, delta_blk = blk_args
        scores, visible = block_scores(q_blk, q_pos)
        att_probs = jnp.where(visible, jnp.exp(scores - lse_blk[..., None]), 0.0)
        gout_f32 = gout_blk.astype(jnp.float32)
        grad_v = grad_v + jnp.einsum('kigj,ikgd->jkd', att_probs.astype(jnp.bfloat16).astype(jnp.float32), gout_f32)
        grad_probs = jnp.einsum('ikgd,jkd->kigj', gout_f32, v_f32)
        grad_scores = (att_probs * (grad_probs - delta_blk[..., None])).astype(jnp.bfloat16).astype(jnp.float32)
        grad_q = jnp.einsum('kigj,jkd->ikgd', grad_scores, k_f32)
        grad_k = grad_k + jnp.einsum('kigj,ikgd->jkd', grad_scores, q_blk.astype(jnp.float32))
        return (grad_k, grad_v), grad_q

    zero_kv = jnp.zeros((SEQ_LEN, NUM_KV_HEADS, HEAD_DIM), jnp.float32)
    kv_grads, grad_q = lax.scan(bwd_block, (zero_kv, zero_kv), (q_blocks, pos_blocks, gout_blocks, log_sum, row_delta))
    dq_pre = rope_transpose(grad_q.reshape(SEQ_LEN, NUM_HEADS, HEAD_DIM) * SCALE, cos_tab, sin_tab).astype(jnp.bfloat16).reshape(SEQ_LEN, NUM_HEADS * HEAD_DIM)
    dk_pre = rope_transpose(kv_grads[0] * SCALE, cos_tab, sin_tab).astype(jnp.bfloat16).reshape(SEQ_LEN, NUM_KV_HEADS * HEAD_DIM)
    dv_pre = kv_grads[1].astype(jnp.bfloat16).reshape(SEQ_LEN, NUM_KV_HEADS * HEAD_DIM)
    grad_w_query = jnp.dot(normed.T, dq_pre, preferred_element_type=jnp.float32)
    grad_w_key = jnp.dot(normed.T, dk_pre, preferred_element_type=jnp.float32)
    grad_w_value = jnp.dot(normed.T, dv_pre, preferred_element_type=jnp.float32)
    grad_normed = (jnp.dot(dq_pre, w_query.T, preferred_element_type=jnp.float32) + jnp.dot(dk_pre, w_key.T, preferred_element_type=jnp.float32) + jnp.dot(dv_pre, w_value.T, preferred_element_type=jnp.float32))
    grad_xhat = grad_normed * norm_gain
    grad_gain = jnp.sum(grad_normed * x_hat, axis=0)
    grad_x = inv_rms[:, None] * (grad_xhat - x_hat * jnp.mean(grad_xhat * x_hat, axis=-1, keepdims=True))
    grad_hidden = (grad_out.astype(jnp.float32) + grad_x).astype(jnp.bfloat16)
    return result, grad_hidden, (grad_w_query, grad_w_key, grad_w_value, grad_w_out, grad_gain)


def reference(hidden, tok_pos, grad_out, norm_gain, w_query, w_key, w_value, w_out):
    def per_seq(totals, seq_args):
        result, grad_hidden, seq_grads = seq_pass(seq_args[0], seq_args[1], seq_args[2], norm_gain, w_query, w_key, w_value, w_out)
        return jax.tree.map(jnp.add, totals, seq_grads), (result, grad_hidden)

    init_totals = (jnp.zeros(w_query.shape, jnp.float32), jnp.zeros(w_key.shape, jnp.float32), jnp.zeros(w_value.shape, jnp.float32), jnp.zeros(w_out.shape, jnp.float32), jnp.zeros(norm_gain.shape, jnp.float32))
    totals, seq_outs = lax.scan(per_seq, init_totals, (hidden, tok_pos, grad_out))
    return seq_outs[0], seq_outs[1], totals[0], totals[1], totals[2], totals[3], totals[4]
```

```python
import functools
import jax
import jax.numpy as jnp
from jax import lax
from jax.experimental import pallas as pl
from jax.experimental.pallas import tpu as pltpu

from jax.sharding import PartitionSpec as P

HEAD_DIM = 128
ROPE_THETA = 1000000.0
RMS_EPS = 1e-5
SCALE = HEAD_DIM ** -0.5
LOG2E = 1.4426950408889634
COLORS = ((0, 384, 384), (768, 384, 384), (1536, 384, 384))

MESH = pl.DeviceIdType.MESH
AXES = ('x', 'y', 'z')
ORDERS = (('x', 'y', 'z'), ('y', 'z', 'x'), ('z', 'x', 'y'))
ALL = pl.ds(0, 4)


def torus():
    f = lax.axis_index('fsdp')
    return {'x': lax.rem(f, 4), 'y': lax.rem(lax.div(f, 4), 4), 'z': lax.div(f, 16)}


def step(pos, axis, hop):
    return lax.rem(pos[axis] + hop, 4)


class Comm:
    def __init__(self, send_sems, recv_sems, local_sems):
        self.pos = torus()
        self.core = lax.axis_index('cp')
        self.sems = (send_sems, recv_sems, local_sems)
        self.used = self.used_local = 0
        self.sent, self.exchanged, self.stored = [], [], []

    def far(self, axis, hop):
        p = dict(self.pos)
        p[axis] = step(self.pos, axis, hop)
        return {'fsdp': (p['z'] * 4 + p['y']) * 4 + p['x'], 'cp': self.core}

    def peer(self):
        return {'fsdp': lax.axis_index('fsdp'), 'cp': 1 - self.core}

    def barrier(self):
        sem = pltpu.get_barrier_semaphore()
        for axis in AXES:
            for hop in (1, 2, 3):
                pl.semaphore_signal(sem, inc=1, device_id=self.far(axis, hop), device_id_type=MESH)
        pl.semaphore_signal(sem, inc=1, device_id=self.peer(), device_id_type=MESH)
        pl.semaphore_wait(sem, 10)

    def _copy(self, src, dst, device):
        i = self.used
        self.used += 1
        c = pltpu.make_async_remote_copy(src_ref=src, dst_ref=dst, send_sem=self.sems[0].at[i], recv_sem=self.sems[1].at[i], device_id=device, device_id_type=MESH)
        c.start()
        return c

    def send(self, src, dst, device):
        c = self._copy(src, dst, device)
        self.sent.append(c)
        return c

    def trade(self, src, dst):
        self.exchanged.append(self._copy(src, dst, self.peer()))

    def local(self, src, dst):
        i = self.used_local
        self.used_local += 1
        c = pltpu.make_async_copy(src, dst, self.sems[2].at[i])
        c.start()
        return c

    def store(self, src, dst):
        self.stored.append(self.local(src, dst))

    def finish(self):
        for c in self.sent:
            c.wait_send()
        for c in self.exchanged:
            c.wait_send()
            c.wait_recv()
        for c in self.stored:
            c.wait()


def pick(ref, sel, cols):
    return ref.at[sel['z'], sel['y'], sel['x'], :, pl.ds(cols[0], cols[1])]


def gather_kernel(colors, wcat, gtile, w_own, w_peer, g_out, wv, gbuf, gx, gy, gz, *sems):
    comm = Comm(*sems)
    pos, core = comm.pos, comm.core
    rows = pl.ds(pl.multiple_of(core * 16, 16), 16)
    mine = wv.at[pos['z'], pos['y'], pos['x'], rows]
    load = comm.local(wcat.at[core], mine)
    comm.barrier()
    swap = comm.send(wcat.at[1 - core], mine, comm.peer())
    gstage = [comm.send(gtile, gbuf, comm.peer())]
    load.wait()
    gstage[0].wait_recv()
    gx[0] = gtile[...] + gbuf[...]
    gstage = [comm.send(gx.at[0], gx.at[hop], comm.far('x', hop)) for hop in (1, 2, 3)]
    swap.wait_recv()

    held = [dict(pos) for _ in colors]
    for phase in range(3):
        last = phase == 2

        def land(s, cols):
            if last:
                comm.trade(pick(wv, s, cols), pick(w_peer, s, cols))
                comm.store(pick(wv, s, cols), pick(w_own, s, cols))

        first, second = [], []
        for k, (lo, na, nb) in enumerate(colors):
            d = ORDERS[k][phase]
            a, b = (lo, na), (lo + na, nb)
            up, dn, s = comm.far(d, 1), comm.far(d, 3), held[k]
            first.append([comm.send(pick(wv, s, cols), pick(wv, s, cols), to) for cols, to in ((a, up), (b, dn), (b, up), (a, dn))])
        for k, (lo, na, nb) in enumerate(colors):
            land(held[k], (lo, na + nb))
        for k, (lo, na, nb) in enumerate(colors):
            d = ORDERS[k][phase]
            a, b = (lo, na), (lo + na, nb)
            below, above = dict(held[k], **{d: step(pos, d, 3)}), dict(held[k], **{d: step(pos, d, 1)})
            up_a, dn_b, up_b, dn_a = first[k]
            up_a.wait_recv()
            far_a = comm.send(pick(wv, below, a), pick(wv, below, a), comm.far(d, 1))
            dn_b.wait_recv()
            far_b = comm.send(pick(wv, above, b), pick(wv, above, b), comm.far(d, 3))
            land(below, a)
            land(above, b)
            second.append((far_a, far_b))
        for c in gstage:
            c.wait_recv()
        if phase == 0:
            gy[pos['y']] = (gx[0] + gx[1]) + (gx[2] + gx[3])
            gstage = [comm.send(gy.at[pos['y']], gy.at[pos['y']], comm.far('y', hop)) for hop in (1, 2, 3)]
        elif phase == 1:
            for j in range(4):
                gz[pos['z'], j] = gy[j]
            gstage = [comm.send(gz.at[pos['z']], gz.at[pos['z']], comm.far('z', hop)) for hop in (1, 2, 3)]
        else:
            g_out[...] = gz[...]
        for k, (lo, na, nb) in enumerate(colors):
            d = ORDERS[k][phase]
            a, b = (lo, na), (lo + na, nb)
            below, above, across = (dict(held[k], **{d: step(pos, d, hop)}) for hop in (3, 1, 2))
            first[k][2].wait_recv()
            land(below, b)
            first[k][3].wait_recv()
            land(above, a)
            second[k][0].wait_recv()
            land(across, a)
            second[k][1].wait_recv()
            land(across, b)
            held[k] = dict(held[k], **{d: ALL})
    comm.finish()


def sem_scratch(remote, local):
    return [pltpu.SemaphoreType.DMA((remote,)), pltpu.SemaphoreType.DMA((remote,)), pltpu.SemaphoreType.DMA((local,))]


def all_gather(wcat, gtile, colors, collective_id):
    width = wcat.shape[-1]
    whole = (4, 4, 4, 32, width)
    any_ = pl.BlockSpec(memory_space=pl.ANY)
    vmem = pl.BlockSpec(memory_space=pltpu.VMEM)
    return pl.pallas_call(
        functools.partial(gather_kernel, colors),
        out_shape=[jax.ShapeDtypeStruct(whole, jnp.bfloat16), jax.ShapeDtypeStruct(whole, jnp.bfloat16), jax.ShapeDtypeStruct((4, 4, 8, 128), jnp.float32)],
        in_specs=[any_, vmem],
        out_specs=[any_, any_, vmem],
        scratch_shapes=[pltpu.VMEM(whole, jnp.bfloat16), pltpu.VMEM((8, 128), jnp.float32)] + [pltpu.VMEM((4, 8, 128), jnp.float32)] * 2 + [pltpu.VMEM((4, 4, 8, 128), jnp.float32)] + sem_scratch(96, 32),
        compiler_params=pltpu.CompilerParams(collective_id=collective_id, has_side_effects=True, vmem_limit_bytes=60 * 2**20),
        name='gather_weights',
    )(wcat, gtile)


def add_into(dst, *srcs):
    lead = dst.shape[:-2]
    n = 1
    for v in lead:
        n *= v

    def body(i):
        idx, rest = [], i
        for v in reversed(lead):
            idx.append(lax.rem(rest, v))
            rest = lax.div(rest, v)
        idx = tuple(reversed(idx))
        total = dst[idx]
        for s in srcs:
            total = total + s[idx]
        dst[idx] = total

    if n == 1:
        total = dst[...]
        for s in srcs:
            total = total + s[...]
        dst[...] = total
    else:
        pl.loop(0, n)(body)


def scatter_kernel(colors, pieces, *refs):
    n_in = len(pieces)
    grads, gpart = refs[:n_in], refs[n_in]
    out, gout = refs[n_in + 1:n_in + 3]
    part, buf1, buf2, buf3, gpeer, gz, gy, gx, *sems = refs[n_in + 3:]
    comm = Comm(*sems)
    pos, core = comm.pos, comm.core
    loads = [[] for _ in colors]
    for k, (lo, na, nb) in enumerate(colors):
        for ref, start, width in pieces_in(grads, pieces, lo, na + nb):
            src, (at, n) = ref, width
            loads[k].append(comm.local(src.at[:, :, :, :, pl.ds(start, n)], part.at[:, :, :, :, pl.ds(at, n)]))
    comm.barrier()
    gstage = [comm.send(gpart, gpeer, comm.peer())]
    held = [dict(x=ALL, y=ALL, z=ALL) for _ in colors]
    for phase, buf in enumerate((buf1, buf2, buf3)):
        flight = []
        for k, (lo, na, nb) in enumerate(colors):
            d = ORDERS[k][phase]
            a, b = (lo, na), (lo + na, nb)
            if phase == 0:
                for c in loads[k]:
                    c.wait()
            up, dn = comm.far(d, 1), comm.far(d, 3)
            nxt, prv, opp = (dict(held[k], **{d: step(pos, d, hop)}) for hop in (1, 3, 2))
            r2a = comm.send(pick(part, opp, a), buf.at[k, 0], up)
            r2b = comm.send(pick(part, opp, b), buf.at[k, 1], dn)
            n1b = comm.send(pick(part, nxt, b), buf.at[k, 2], up)
            m1a = comm.send(pick(part, prv, a), buf.at[k, 3], dn)
            flight.append([r2a, r2b, n1b, m1a])
        for c in gstage:
            c.wait_recv()
        if phase == 0:
            for j in range(4):
                gz[j] = gpart[j] + gpeer[j]
            gstage = [comm.send(gz.at[step(pos, 'z', hop)], gz.at[3 + hop], comm.far('z', hop)) for hop in (1, 2, 3)]
        elif phase == 1:
            gy[0] = (gz[pos['z']] + gz[4]) + (gz[5] + gz[6])
            gstage = [comm.send(gy.at[0], gy.at[hop], comm.far('y', hop)) for hop in (1, 2, 3)]
        else:
            gx[0] = (gy[0] + gy[1]) + (gy[2] + gy[3])
            gstage = [comm.send(gx.at[0], gx.at[hop], comm.far('x', hop)) for hop in (1, 2, 3)]
        for k, (lo, na, nb) in enumerate(colors):
            d = ORDERS[k][phase]
            a, b = (lo, na), (lo + na, nb)
            nxt, prv = (dict(held[k], **{d: step(pos, d, hop)}) for hop in (1, 3))
            r2a, r2b, n1b, m1a = flight[k]
            r2a.wait_recv()
            add_into(pick(part, nxt, a), buf.at[k, 0])
            n1a = comm.send(pick(part, nxt, a), buf.at[k, 4], comm.far(d, 1))
            r2b.wait_recv()
            add_into(pick(part, prv, b), buf.at[k, 1])
            m1b = comm.send(pick(part, prv, b), buf.at[k, 5], comm.far(d, 3))
            flight[k] += [n1a, m1b]
        for k, (lo, na, nb) in enumerate(colors):
            d = ORDERS[k][phase]
            a, b = (lo, na), (lo + na, nb)
            r2a, r2b, n1b, m1a, n1a, m1b = flight[k]
            held[k] = dict(held[k], **{d: pos[d]})
            m1a.wait_recv()
            n1a.wait_recv()
            add_into(pick(part, held[k], a), buf.at[k, 3], buf.at[k, 4])
            n1b.wait_recv()
            m1b.wait_recv()
            add_into(pick(part, held[k], b), buf.at[k, 2], buf.at[k, 5])
    for c in gstage:
        c.wait_recv()
    gout[...] = (gx[0] + gx[1]) + (gx[2] + gx[3])
    keep = pl.ds(pl.multiple_of(core * 16, 16), 16)
    give = pl.ds(pl.multiple_of((1 - core) * 16, 16), 16)
    chip = part.at[pos['z'], pos['y'], pos['x']]
    comm.trade(chip.at[give], out.at[1])
    comm.store(chip.at[keep], out.at[0])
    comm.finish()


def pieces_in(grads, pieces, lo, n):
    found, at = [], 0
    for ref, width in zip(grads, pieces):
        s, e = max(lo, at), min(lo + n, at + width)
        if s < e:
            found.append((ref, s - at, (s, e - s)))
        at += width
    return found


def reduce_scatter(grads, gpart, colors, collective_id):
    pieces = [g.shape[-1] for g in grads]
    width = sum(pieces)
    half = max(max(a, b) for _, a, b in colors)
    assert all(a == half and b == half for _, a, b in colors)
    any_ = pl.BlockSpec(memory_space=pl.ANY)
    vmem = pl.BlockSpec(memory_space=pltpu.VMEM)
    f32 = jnp.float32
    return pl.pallas_call(
        functools.partial(scatter_kernel, colors, pieces),
        out_shape=[jax.ShapeDtypeStruct((2, 16, width), f32), jax.ShapeDtypeStruct((8, 128), f32)],
        in_specs=[any_] * len(grads) + [vmem],
        out_specs=[any_, vmem],
        scratch_shapes=[pltpu.VMEM((4, 4, 4, 32, width), f32), pltpu.VMEM((3, 6, 4, 4, 32, half), f32), pltpu.VMEM((3, 6, 4, 32, half), f32), pltpu.VMEM((3, 6, 32, half), f32), pltpu.VMEM((4, 8, 128), f32), pltpu.VMEM((7, 8, 128), f32), pltpu.VMEM((4, 8, 128), f32), pltpu.VMEM((4, 8, 128), f32)] + sem_scratch(96, 32),
        compiler_params=pltpu.CompilerParams(collective_id=collective_id, has_side_effects=True, vmem_limit_bytes=60 * 2**20),
        name='scatter_gradients',
    )(*[g.reshape(4, 4, 4, 32, -1) for g in grads], gpart)


NEG_INF = float('-inf')
QB = 256
KC = 256


def attn_kernel(qt, q, k, kt, v, vt, dot_, do, posk, posq, cos, sin, ot, dqt, dk, dv, s_scr, e_scr, p_scr, d_scr):
    head = pl.program_id(0)
    n = qt.shape[1]
    f32, bf16 = jnp.float32, jnp.bfloat16
    half = HEAD_DIM // 2

    @pl.when(head == 0)
    def _():
        dk[...] = jnp.zeros_like(dk)
        dv[...] = jnp.zeros_like(dv)

    def dot(a, b):
        return jnp.dot(a, b, preferred_element_type=f32)

    @pl.loop(0, n // QB)
    def _(j):
        cols = pl.ds(pl.multiple_of(j * QB, QB), QB)
        q_t, do_t = qt[:, cols], dot_[:, cols]
        q_pos = posq[0:1, cols]
        top = jnp.full((8, QB), NEG_INF, f32)
        for c in range(n // KC):
            rows = slice(c * KC, (c + 1) * KC)
            s = dot(k[rows, :], q_t)
            pk = posk[rows, :]
            vis = jnp.concatenate([pk] * (QB // 128), axis=1) <= q_pos
            s = jnp.where(vis, s, NEG_INF)
            s_scr[rows, :] = s
            top = jnp.maximum(top, jnp.max(s.reshape(KC // 8, 8, QB), axis=0))
        m = jnp.max(top, axis=0, keepdims=True)
        tot = jnp.zeros((8, QB), f32)
        for c in range(n // KC):
            rows = slice(c * KC, (c + 1) * KC)
            e = jnp.exp2((s_scr[rows, :] - m) * (SCALE * LOG2E))
            s_scr[rows, :] = e
            e_scr[rows, :] = e.astype(bf16)
            tot = tot + jnp.sum(e.reshape(KC // 8, 8, QB), axis=0)
        den = jnp.sum(tot, axis=0, keepdims=True)
        inv = 1.0 / den
        o = (dot(vt[...], e_scr[...]) / den).astype(bf16)
        ot[:, cols] = o
        delta = jnp.sum(do_t.astype(f32) * o.astype(f32), axis=0, keepdims=True)
        q_n, do_n = q[cols, :], do[cols, :]
        for c in range(n // KC):
            rows = slice(c * KC, (c + 1) * KC)
            p = s_scr[rows, :] * inv
            dp = dot(v[rows, :], do_t)
            p_scr[rows, :] = p.astype(bf16)
            d_scr[rows, :] = (p * (dp - delta)).astype(bf16)
            dv[rows, :] += dot(p_scr[rows, :], do_n)
            dk[rows, :] += dot(d_scr[rows, :], q_n)
        g = dot(kt[...], d_scr[...]) * SCALE
        co, si = cos[:, cols], sin[:, cols]
        a, b = g[:half], g[half:]
        dqt[:half, cols] = (a * co + b * si).astype(bf16)
        dqt[half:, cols] = (b * co - a * si).astype(bf16)


def attention(qt, q, k, kt, v, vt, dot_, do, posk, posq, cos_t, sin_t):
    heads, n = qt.shape[0] // HEAD_DIM, qt.shape[1]
    by_row = pl.BlockSpec((HEAD_DIM, n), lambda h: (h, 0))
    by_col = pl.BlockSpec((n, HEAD_DIM), lambda h: (0, h))
    whole = lambda a: pl.BlockSpec(a.shape, lambda h: (0, 0))
    f32, bf16 = jnp.float32, jnp.bfloat16
    return pl.pallas_call(
        attn_kernel,
        grid=(heads,),
        in_specs=[by_row, by_col, whole(k), whole(kt), whole(v), whole(vt), by_row, by_col, whole(posk), whole(posq), whole(cos_t), whole(sin_t)],
        out_specs=[by_row, by_row, pl.BlockSpec((n, HEAD_DIM), lambda h: (0, 0)), pl.BlockSpec((n, HEAD_DIM), lambda h: (0, 0))],
        out_shape=[jax.ShapeDtypeStruct((heads * HEAD_DIM, n), bf16), jax.ShapeDtypeStruct((heads * HEAD_DIM, n), bf16), jax.ShapeDtypeStruct((n, HEAD_DIM), f32), jax.ShapeDtypeStruct((n, HEAD_DIM), f32)],
        scratch_shapes=[pltpu.VMEM((n, QB), f32), pltpu.VMEM((n, QB), bf16), pltpu.VMEM((n, QB), bf16), pltpu.VMEM((n, QB), bf16)],
        compiler_params=pltpu.CompilerParams(dimension_semantics=('arbitrary',), vmem_limit_bytes=48 * 2**20),
        cost_estimate=pl.CostEstimate(flops=12 * heads * n * n * HEAD_DIM, bytes_accessed=16 * n * n, transcendentals=heads * n * n),
        name='attention',
    )(qt, q, k, kt, v, vt, dot_, do, posk, posq, cos_t, sin_t)


def rope_tables(positions):
    half_dim = HEAD_DIM // 2
    inv_freq = ROPE_THETA ** (-jnp.arange(half_dim, dtype=jnp.float32) / half_dim)
    angles = positions.astype(jnp.float32)[..., None] * inv_freq
    return jnp.cos(angles), jnp.sin(angles)


def rope(x, cos, sin, sign):
    n = x.shape[0]
    x = x.reshape(n, -1, 2, HEAD_DIM // 2)
    a, b = x[:, :, 0], x[:, :, 1]
    co, si = cos[:, None, :], sin[:, None, :] * sign
    return jnp.stack([a * co - b * si, b * co + a * si], axis=2).reshape(n, -1)


NT = (((1,), (1,)), ((), ()))
TN = (((0,), (0,)), ((), ()))


def solution(mesh):
    def swap(a):
        return lax.ppermute(a, 'cp', [(0, 1), (1, 0)])

    def shard_fn(hidden, tok_pos, grad_out, norm_gain, w_query, w_key, w_value, w_out):
        f32, bf16 = jnp.float32, jnp.bfloat16
        f, core = lax.axis_index('fsdp'), lax.axis_index('cp')
        x, y = lax.rem(f, 4), lax.rem(lax.div(f, 4), 4)
        first = core == 0
        dim = hidden.shape[-1]
        half = dim // 2
        hidden, grad_out = hidden[0], grad_out[0]
        rows = hidden.shape[0]

        def order(own, other, axis):
            return jnp.where(first, jnp.concatenate([own, other], axis), jnp.concatenate([other, own], axis))

        lane = jnp.arange(128) // 16
        gtile = jnp.broadcast_to(jnp.where(lane == x * 2 + core, jnp.tile(norm_gain, 8), 0.0), (8, 128))
        wcat = jnp.stack([jnp.concatenate([w_query[:, c * half:(c + 1) * half], w_key[:, c * 128:(c + 1) * 128], w_value[:, c * 128:(c + 1) * 128], w_out[:, c * half:(c + 1) * half]], axis=1) for c in range(2)])
        hid2 = jnp.concatenate([hidden, swap(hidden)])
        dy2 = jnp.concatenate([grad_out, swap(grad_out)])
        pos2 = jnp.concatenate([tok_pos[0], swap(tok_pos)[0]])
        w_own, w_peer, gain = all_gather(wcat, gtile, COLORS, 0)
        w_own, w_peer = w_own.reshape(dim, -1), w_peer.reshape(dim, -1)
        gain = gain[:, :, 0].reshape(dim)

        cos, sin = rope_tables(pos2)
        xf = hid2.astype(f32)
        inv_rms = lax.rsqrt(jnp.mean(xf * xf, axis=-1, keepdims=True) + RMS_EPS)
        normed = (xf * inv_rms * gain).astype(bf16)
        lin = jnp.dot(normed, w_own[:, :half + 256], preferred_element_type=f32)
        qk = rope(lin[:, :half + 128], cos, sin, 1.0).astype(bf16)
        q, k = qk[:, :half], qk[:, half:]
        v = lin[:, half + 128:].astype(bf16)
        wo = order(w_own[:, half + 256:], w_peer[:, half + 256:], 1)
        wo_rows = lax.dynamic_slice(wo, (core * half, 0), (half, dim))
        do = lax.dot_general(dy2, wo_rows, NT, preferred_element_type=f32).astype(bf16)
        posk = jnp.broadcast_to(pos2[:, None], (2 * rows, 128))
        posq = jnp.broadcast_to(pos2[None, :], (8, 2 * rows))
        ot, dqt, dk, dv = attention(q.T, q, k, k.T, v, v.T, do.T, do, posk, posq, cos.T, sin.T)
        dk = rope(dk * SCALE, cos, sin, -1.0).astype(bf16)
        dqkv = jnp.concatenate([dqt.T, dk, dv.astype(bf16)], axis=1)
        ot_peer = swap(jnp.concatenate([ot[:, rows:], ot[:, :rows]], axis=1))
        dqkv_peer = swap(dqkv[rows:])
        o_t = order(ot, ot_peer, 0)
        result = (xf[:rows] + lax.dot_general(o_t[:, :rows], wo, TN, preferred_element_type=f32)).astype(bf16)
        dy_cols = lax.dynamic_slice(dy2, (0, core * half), (2 * rows, half))
        grad_o = jnp.dot(o_t, dy_cols, preferred_element_type=f32)
        grad_qkv = lax.dot_general(normed, dqkv, TN, preferred_element_type=f32)
        dr = lax.dot_general(dqkv[:rows], w_own[:, :half + 256], NT, preferred_element_type=f32) + lax.dot_general(dqkv_peer, w_peer[:, :half + 256], NT, preferred_element_type=f32)
        inv, unit = inv_rms[:rows], xf[:rows] * inv_rms[:rows]
        drg = dr * gain
        grad_hidden = (grad_out.astype(f32) + inv * (drg - unit * jnp.mean(drg * unit, axis=-1, keepdims=True))).astype(bf16)
        gpart = jnp.pad(jnp.sum(dr * unit, axis=0).reshape(4, 4, 128), ((0, 0), (0, 4), (0, 0)))
        out, gout = reduce_scatter([grad_qkv, grad_o], gpart, COLORS, 1)
        own, other = out[0], out[1]
        cut = lambda a, b: order(own[:, a:b], other[:, a:b], 1)
        grad_gain = lax.dynamic_slice(gout, (y, x * 32 + core * 16), (1, 16)).reshape(16)
        return result[None], grad_hidden[None], cut(0, half), cut(half, half + 128), cut(half + 128, half + 256), cut(half + 256, 2 * half + 256), grad_gain

    row_spec, pos_spec = P('fsdp', 'cp', None), P('fsdp', 'cp')
    weight_spec, gain_spec = P(('fsdp', 'cp'), None), P(('fsdp', 'cp'))
    return jax.shard_map(shard_fn, mesh=mesh, in_specs=(row_spec, pos_spec, row_spec, gain_spec, weight_spec, weight_spec, weight_spec, weight_spec), out_specs=(row_spec, row_spec, weight_spec, weight_spec, weight_spec, weight_spec, gain_spec), check_vma=False)
```

```python
import functools
import jax
import jax.numpy as jnp
import numpy as np
from jax import lax
from jax.experimental import pallas as pl
from jax.experimental.pallas import tpu as pltpu
from jax.sharding import PartitionSpec as P

HEAD_DIM = 128
ROPE_THETA = 1000000.0
RMS_EPS = 1e-5
SCALE = HEAD_DIM ** -0.5
LOG2E = 1.4426950408889634
COLORS = ((0, 384, 384), (768, 384, 384), (1536, 384, 384))

MESH = pl.DeviceIdType.MESH
AXES = ('x', 'y', 'z')
ORDERS = (('x', 'y', 'z'), ('y', 'z', 'x'), ('z', 'x', 'y'))
ALL = pl.ds(0, 4)


def torus():
    f = lax.axis_index('fsdp')
    return {'x': lax.rem(f, 4), 'y': lax.rem(lax.div(f, 4), 4), 'z': lax.div(f, 16)}


def step(pos, axis, hop):
    return lax.rem(pos[axis] + hop, 4)


class Comm:
    def __init__(self, send_sems, recv_sems, local_sems):
        self.pos = torus()
        self.core = lax.axis_index('cp')
        self.sems = (send_sems, recv_sems, local_sems)
        self.used = self.used_local = 0
        self.sent, self.exchanged, self.stored = [], [], []

    def far(self, axis, hop):
        p = dict(self.pos)
        p[axis] = step(self.pos, axis, hop)
        return {'fsdp': (p['z'] * 4 + p['y']) * 4 + p['x'], 'cp': self.core}

    def peer(self):
        return {'fsdp': lax.axis_index('fsdp'), 'cp': 1 - self.core}

    def barrier(self):
        sem = pltpu.get_barrier_semaphore()
        for axis in AXES:
            for hop in (1, 2, 3):
                pl.semaphore_signal(sem, inc=1, device_id=self.far(axis, hop), device_id_type=MESH)
        pl.semaphore_signal(sem, inc=1, device_id=self.peer(), device_id_type=MESH)
        pl.semaphore_wait(sem, 10)

    def _copy(self, src, dst, device):
        i = self.used
        self.used += 1
        c = pltpu.make_async_remote_copy(src_ref=src, dst_ref=dst, send_sem=self.sems[0].at[i], recv_sem=self.sems[1].at[i], device_id=device, device_id_type=MESH)
        c.start()
        return c

    def send(self, src, dst, device):
        c = self._copy(src, dst, device)
        self.sent.append(c)
        return c

    def trade(self, src, dst):
        self.exchanged.append(self._copy(src, dst, self.peer()))

    def local(self, src, dst):
        i = self.used_local
        self.used_local += 1
        c = pltpu.make_async_copy(src, dst, self.sems[2].at[i])
        c.start()
        return c

    def store(self, src, dst):
        self.stored.append(self.local(src, dst))

    def finish(self):
        for c in self.sent:
            c.wait_send()
        for c in self.exchanged:
            c.wait_send()
            c.wait_recv()
        for c in self.stored:
            c.wait()


def pick(ref, sel, cols):
    return ref.at[sel['z'], sel['y'], sel['x'], :, pl.ds(cols[0], cols[1])]


def sem_scratch(remote, local):
    return [pltpu.SemaphoreType.DMA((remote,)), pltpu.SemaphoreType.DMA((remote,)), pltpu.SemaphoreType.DMA((local,))]


def add_into(dst, *srcs):
    lead = dst.shape[:-2]
    n = 1
    for v in lead:
        n *= v

    def body(i):
        idx, rest = [], i
        for v in reversed(lead):
            idx.append(lax.rem(rest, v))
            rest = lax.div(rest, v)
        idx = tuple(reversed(idx))
        total = dst[idx]
        for s in srcs:
            total = total + s[idx]
        dst[idx] = total

    if n == 1:
        total = dst[...]
        for s in srcs:
            total = total + s[...]
        dst[...] = total
    else:
        pl.loop(0, n)(body)


def scatter_kernel(colors, pieces, *refs):
    n_in = len(pieces)
    grads, gpart = refs[:n_in], refs[n_in]
    out, gout = refs[n_in + 1:n_in + 3]
    part, buf1, buf2, buf3, gpeer, gz, gy, gx, *sems = refs[n_in + 3:]
    comm = Comm(*sems)
    pos, core = comm.pos, comm.core
    loads = [[] for _ in colors]
    for k, (lo, na, nb) in enumerate(colors):
        for ref, start, width in pieces_in(grads, pieces, lo, na + nb):
            src, (at, n) = ref, width
            loads[k].append(comm.local(src.at[:, :, :, :, pl.ds(start, n)], part.at[:, :, :, :, pl.ds(at, n)]))
    comm.barrier()
    gstage = [comm.send(gpart, gpeer, comm.peer())]
    held = [dict(x=ALL, y=ALL, z=ALL) for _ in colors]
    for phase, buf in enumerate((buf1, buf2, buf3)):
        flight = []
        for k, (lo, na, nb) in enumerate(colors):
            d = ORDERS[k][phase]
            a, b = (lo, na), (lo + na, nb)
            if phase == 0:
                for c in loads[k]:
                    c.wait()
            up, dn = comm.far(d, 1), comm.far(d, 3)
            nxt, prv, opp = (dict(held[k], **{d: step(pos, d, hop)}) for hop in (1, 3, 2))
            r2a = comm.send(pick(part, opp, a), buf.at[k, 0], up)
            r2b = comm.send(pick(part, opp, b), buf.at[k, 1], dn)
            n1b = comm.send(pick(part, nxt, b), buf.at[k, 2], up)
            m1a = comm.send(pick(part, prv, a), buf.at[k, 3], dn)
            flight.append([r2a, r2b, n1b, m1a])
        for c in gstage:
            c.wait_recv()
        if phase == 0:
            for j in range(4):
                gz[j] = gpart[j] + gpeer[j]
            gstage = [comm.send(gz.at[step(pos, 'z', hop)], gz.at[3 + hop], comm.far('z', hop)) for hop in (1, 2, 3)]
        elif phase == 1:
            gy[0] = (gz[pos['z']] + gz[4]) + (gz[5] + gz[6])
            gstage = [comm.send(gy.at[0], gy.at[hop], comm.far('y', hop)) for hop in (1, 2, 3)]
        else:
            gx[0] = (gy[0] + gy[1]) + (gy[2] + gy[3])
            gstage = [comm.send(gx.at[0], gx.at[hop], comm.far('x', hop)) for hop in (1, 2, 3)]
        for k, (lo, na, nb) in enumerate(colors):
            d = ORDERS[k][phase]
            a, b = (lo, na), (lo + na, nb)
            nxt, prv = (dict(held[k], **{d: step(pos, d, hop)}) for hop in (1, 3))
            r2a, r2b, n1b, m1a = flight[k]
            r2a.wait_recv()
            add_into(pick(part, nxt, a), buf.at[k, 0])
            n1a = comm.send(pick(part, nxt, a), buf.at[k, 4], comm.far(d, 1))
            r2b.wait_recv()
            add_into(pick(part, prv, b), buf.at[k, 1])
            m1b = comm.send(pick(part, prv, b), buf.at[k, 5], comm.far(d, 3))
            flight[k] += [n1a, m1b]
        for k, (lo, na, nb) in enumerate(colors):
            d = ORDERS[k][phase]
            a, b = (lo, na), (lo + na, nb)
            r2a, r2b, n1b, m1a, n1a, m1b = flight[k]
            held[k] = dict(held[k], **{d: pos[d]})
            m1a.wait_recv()
            n1a.wait_recv()
            add_into(pick(part, held[k], a), buf.at[k, 3], buf.at[k, 4])
            n1b.wait_recv()
            m1b.wait_recv()
            add_into(pick(part, held[k], b), buf.at[k, 2], buf.at[k, 5])
    for c in gstage:
        c.wait_recv()
    gout[...] = (gx[0] + gx[1]) + (gx[2] + gx[3])
    keep = pl.ds(pl.multiple_of(core * 16, 16), 16)
    give = pl.ds(pl.multiple_of((1 - core) * 16, 16), 16)
    chip = part.at[pos['z'], pos['y'], pos['x']]
    comm.trade(chip.at[give], out.at[1])
    comm.store(chip.at[keep], out.at[0])
    comm.finish()


def pieces_in(grads, pieces, lo, n):
    found, at = [], 0
    for ref, width in zip(grads, pieces):
        s, e = max(lo, at), min(lo + n, at + width)
        if s < e:
            found.append((ref, s - at, (s, e - s)))
        at += width
    return found


def reduce_scatter(grads, gpart, colors, collective_id):
    pieces = [g.shape[-1] for g in grads]
    width = sum(pieces)
    half = max(max(a, b) for _, a, b in colors)
    assert all(a == half and b == half for _, a, b in colors)
    any_ = pl.BlockSpec(memory_space=pl.ANY)
    vmem = pl.BlockSpec(memory_space=pltpu.VMEM)
    f32 = jnp.float32
    return pl.pallas_call(
        functools.partial(scatter_kernel, colors, pieces),
        out_shape=[jax.ShapeDtypeStruct((2, 16, width), f32), jax.ShapeDtypeStruct((8, 128), f32)],
        in_specs=[any_] * len(grads) + [vmem],
        out_specs=[any_, vmem],
        scratch_shapes=[pltpu.VMEM((4, 4, 4, 32, width), f32), pltpu.VMEM((3, 6, 4, 4, 32, half), f32), pltpu.VMEM((3, 6, 4, 32, half), f32), pltpu.VMEM((3, 6, 32, half), f32), pltpu.VMEM((4, 8, 128), f32), pltpu.VMEM((7, 8, 128), f32), pltpu.VMEM((4, 8, 128), f32), pltpu.VMEM((4, 8, 128), f32)] + sem_scratch(96, 32),
        compiler_params=pltpu.CompilerParams(collective_id=collective_id, has_side_effects=True, vmem_limit_bytes=60 * 2**20),
        name='scatter_gradients',
    )(*[g.reshape(4, 4, 4, 32, -1) for g in grads], gpart)


QKV_COLORS = ((0, 256, 256), (512, 256, 128), (896, 128, 256))
WO_COLORS = ((0, 128, 128), (256, 128, 256), (640, 256, 128))
ROWS = 512
TOKENS = 1024
DIM = 2048
HALF = 1024
QKV = 1280


def dot(a, b):
    return jnp.dot(a, b, preferred_element_type=jnp.float32)


def dot_nt(a, b):
    return lax.dot_general(a, b, (((1,), (1,)), ((), ())), preferred_element_type=jnp.float32)


def tile_at(i, n):
    return pl.ds(pl.multiple_of(i * n, n), n)


class Gather:
    def __init__(self, comm, ref, colors, land):
        self.comm, self.ref, self.colors, self.land = comm, ref, colors, land
        self.held = [dict(comm.pos) for _ in colors]

    def parts(self, k):
        lo, na, nb = self.colors[k]
        return (lo, na), (lo + na, nb)

    def move(self, s, cols, to):
        return self.comm.send(pick(self.ref, s, cols), pick(self.ref, s, cols), to)

    def begin(self, phase):
        self.phase, self.first, self.second = phase, [], []
        for k in range(3):
            a, b = self.parts(k)
            d = ORDERS[k][phase]
            up, dn, s = self.comm.far(d, 1), self.comm.far(d, 3), self.held[k]
            self.first.append([self.move(s, cols, to) for cols, to in ((a, up), (b, dn), (b, up), (a, dn))])
        if phase == 2:
            for k in range(3):
                for cols in self.parts(k):
                    self.land(self.ref, self.held[k], cols)

    def at(self, k, hop):
        d = ORDERS[k][self.phase]
        return dict(self.held[k], **{d: step(self.comm.pos, d, hop)})

    def forward(self):
        for k in range(3):
            a, b = self.parts(k)
            d = ORDERS[k][self.phase]
            self.first[k][0].wait_recv()
            c = self.move(self.at(k, 3), a, self.comm.far(d, 1))
            self.first[k][1].wait_recv()
            self.second.append((c, self.move(self.at(k, 1), b, self.comm.far(d, 3))))
            if self.phase == 2:
                self.land(self.ref, self.at(k, 3), a)
                self.land(self.ref, self.at(k, 1), b)

    def end(self):
        for k in range(3):
            a, b = self.parts(k)
            d = ORDERS[k][self.phase]
            for c, hop, cols in ((self.first[k][2], 3, b), (self.first[k][3], 1, a), (self.second[k][0], 2, a), (self.second[k][1], 2, b)):
                c.wait_recv()
                if self.phase == 2:
                    self.land(self.ref, self.at(k, hop), cols)
            self.held[k] = dict(self.held[k], **{d: ALL})


def head_kernel(hidden, dy, wq, wk, wv, wo, pos, gtile, cos_t, sin_t,
                qt_o, dot_o, k_o, kt_o, v_o, vt_o, rt_o, dyc_o, wqkv_o, wqkvp_o, wo_o, wop_o, gain_o,
                hid2, dy2, dys, rs, rt, wqkv, wout, wpeer, pi, pos2, qt, dot_s, kk, kt, vv, vt, gain, gbuf, gx, gy, gz, *sems):
    comm = Comm(*sems)
    pos_c, core = comm.pos, comm.core
    bf16, f32 = jnp.bfloat16, jnp.float32
    peer = comm.peer()
    rows = tile_at(core, 16)
    mine_qkv = wqkv.at[pos_c['z'], pos_c['y'], pos_c['x'], rows]
    mine_wo = wout.at[pos_c['z'], pos_c['y'], pos_c['x'], rows]

    def weight_parts(c):
        return ((wq.at[:, tile_at(c, HALF)], mine_qkv.at[:, pl.ds(0, HALF)]), (wk.at[:, tile_at(c, 128)], mine_qkv.at[:, pl.ds(HALF, 128)]),
                (wv.at[:, tile_at(c, 128)], mine_qkv.at[:, pl.ds(HALF + 128, 128)]), (wo.at[:, tile_at(c, HALF)], mine_wo))

    loads = [comm.local(s, d) for s, d in weight_parts(core)]
    load_x = [comm.local(hidden, hid2.at[0]), comm.local(dy, dy2.at[0])]
    comm.barrier()
    swaps = [comm.send(s, d, peer) for s, d in weight_parts(1 - core)]
    gstage = [comm.send(gtile, gbuf, peer)]
    swap_pos = comm.send(pos, pos2.at[1], peer)
    swap_dy = comm.send(dy, dy2.at[1], peer)
    swap_x = comm.send(hidden, hid2.at[1], peer)
    pos2[0] = pos[...]
    for c in loads:
        c.wait()
    gstage[0].wait_recv()
    gx[0] = gtile[...] + gbuf[...]
    gstage = [comm.send(gx.at[0], gx.at[hop], comm.far('x', hop)) for hop in (1, 2, 3)]
    for c in swaps:
        c.wait_recv()

    def land_qkv(ref, s, cols):
        comm.trade(pick(ref, s, cols), pick(wqkvp_o, s, cols))

    arrived = []

    def land_wo(ref, s, cols):
        arrived.append(comm.send(pick(ref, s, cols), pick(wpeer, s, cols), peer))

    g1 = Gather(comm, wqkv, QKV_COLORS, land_qkv)
    g2 = Gather(comm, wout, WO_COLORS, land_wo)
    g1.begin(0)
    g2.begin(0)

    swap_pos.wait_recv()

    @pl.loop(0, TOKENS // 128)
    def _(i):
        want = lax.broadcasted_iota(jnp.int32, (128, ROWS), 0) + i * 128
        for h in range(2):
            have = pos2[h, 0:1, :]
            pi[tile_at(i, 128), h * ROWS:(h + 1) * ROWS] = jnp.where(want == have, 1.0, 0.0).astype(bf16)

    def gain_x():
        for c in gstage:
            c.wait_recv()
        gy[pos_c['y']] = (gx[0] + gx[1]) + (gx[2] + gx[3])
        return [comm.send(gy.at[pos_c['y']], gy.at[pos_c['y']], comm.far('y', hop)) for hop in (1, 2, 3)]

    g1.forward()
    g2.forward()
    gstage = gain_x()
    g1.end()
    g2.end()
    g1.begin(1)
    g2.begin(1)

    def sort(dst, src2, first, last):
        @pl.loop(first, last)
        def _(i):
            r = tile_at(i, 256)

            @pl.loop(0, DIM // 512)
            def _(j):
                c = tile_at(j, 512)
                acc = dot(pi[r, :ROWS], src2[0, :, c]) + dot(pi[r, ROWS:], src2[1, :, c])
                dst[r, c] = acc.astype(bf16)

    load_x[1].wait()
    swap_dy.wait_recv()
    sort(dys, dy2, 0, 1)
    g1.forward()
    g2.forward()
    for c in gstage:
        c.wait_recv()
    for j in range(4):
        gz[pos_c['z'], j] = gy[j]
    gstage = [comm.send(gz.at[pos_c['z']], gz.at[pos_c['z']], comm.far('z', hop)) for hop in (1, 2, 3)]
    g1.end()
    g1.begin(2)
    g2.end()
    sort(dys, dy2, 1, 3)
    for c in gstage:
        c.wait_recv()
    for i in range(4):
        for j in range(4):
            gain[:, (i * 4 + j) * 128:(i * 4 + j + 1) * 128] = gz[i, j]
    comm.store(gain, gain_o)
    load_x[0].wait()
    swap_x.wait_recv()
    for h in range(2):
        @pl.loop(0, ROWS // 32)
        def _(i):
            r = tile_at(i, 32)
            x = hid2[h, r, :].astype(f32)
            inv = lax.rsqrt(jnp.mean(x * x, axis=-1, keepdims=True) + RMS_EPS)
            hid2[h, r, :] = (x * inv * gain[0:1, :]).astype(bf16)
    g1.forward()
    g2.begin(2)
    sort(dys, dy2, 3, 4)
    comm.store(dys.at[:, tile_at(core, HALF)], dyc_o)
    sort(rs, hid2, 0, 4)
    g1.end()
    comm.store(wqkv, wqkv_o)

    w2 = wqkv.reshape(DIM, QKV)

    def project(t, i):
        r = tile_at(i, 256)
        x = dot(rs[r, :], w2[:, tile_at(t, 256)])
        cos, sin = cos_t[:, r], sin_t[:, r]
        cos = jnp.concatenate([cos, cos], axis=0).T
        sin = jnp.concatenate([-sin, sin], axis=0).T
        return r, x, cos, sin

    def rotate(x, cos, sin):
        return x * cos + pltpu.roll(x, 64, 1) * sin

    @pl.loop(0, 4)
    def _(i):
        r, x, cos, sin = project(4, i)
        key, val = rotate(x[:, :128], cos, sin).astype(bf16), x[:, 128:].astype(bf16)
        kk[r, :] = key
        kt[:, r] = key.T
        vv[r, :] = val
        vt[:, r] = val.T

    def queries(first, last):
        @pl.loop(first, last)
        def _(t):
            @pl.loop(0, 4)
            def _(i):
                r, x, cos, sin = project(t, i)
                for h in range(2):
                    q = rotate(x[:, h * 128:(h + 1) * 128], cos, sin).astype(bf16)
                    qt[tile_at(2 * t + h, 128), r] = q.T

    queries(0, 1)
    g2.forward()
    queries(1, 4)
    for src, dst in ((kk, k_o), (kt, kt_o), (vv, v_o), (vt, vt_o), (qt, qt_o)):
        comm.store(src, dst)

    @pl.loop(0, DIM // 256)
    def _(i):
        c = tile_at(i, 256)

        @pl.loop(0, TOKENS // 256)
        def _(j):
            r = tile_at(j, 256)
            rt[c, r] = rs[r, c].T
    comm.store(rt, rt_o)
    g2.end()
    for c in arrived:
        c.wait_recv()
    comm.store(wout, wo_o)
    comm.store(wpeer, wop_o)
    own, other = wout.reshape(DIM, HALF), wpeer.reshape(DIM, HALF)

    @pl.loop(0, HALF // 256)
    def _(i):
        r = pl.ds(pl.multiple_of(core * HALF + i * 256, 256), 256)

        @pl.loop(0, TOKENS // 256)
        def _(j):
            t = tile_at(j, 256)
            acc = dot_nt(own[r, :], dys[t, tile_at(core, HALF)]) + dot_nt(other[r, :], dys[t, tile_at(1 - core, HALF)])
            dot_s[tile_at(i, 256), t] = acc.astype(bf16)
    comm.store(dot_s, dot_o)
    comm.finish()


def head(hidden, dy, wq, wk, wv, wo, pos, gtile, cos_t, sin_t):
    bf16, f32 = jnp.bfloat16, jnp.float32
    any_ = pl.BlockSpec(memory_space=pl.ANY)
    vmem = pl.BlockSpec(memory_space=pltpu.VMEM)
    S = lambda shape, d=bf16: jax.ShapeDtypeStruct(shape, d)
    V = lambda shape, d=bf16: pltpu.VMEM(shape, d)
    w_qkv, w_out = (4, 4, 4, 32, QKV), (4, 4, 4, 32, HALF)
    sq, tall, wide = (HALF, TOKENS), (TOKENS, 128), (128, TOKENS)
    return pl.pallas_call(
        head_kernel,
        out_shape=[S(sq), S(sq), S(tall), S(wide), S(tall), S(wide), S((DIM, TOKENS)), S((TOKENS, HALF)), S(w_qkv), S(w_qkv), S(w_out), S(w_out), S((8, DIM), f32)],
        in_specs=[any_] * 6 + [vmem] * 4,
        out_specs=[any_] * 13,
        scratch_shapes=[V((2, ROWS, DIM)), V((2, ROWS, DIM)), V((TOKENS, DIM)), V((TOKENS, DIM)), V((DIM, TOKENS)), V(w_qkv), V(w_out), V(w_out), V((TOKENS, TOKENS)), V((2, 8, ROWS), jnp.int32),
                        V(sq), V(sq), V(tall), V(wide), V(tall), V(wide), V((8, DIM), f32), V((8, 128), f32), V((4, 8, 128), f32), V((4, 8, 128), f32), V((4, 4, 8, 128), f32)] + sem_scratch(192, 32),
        compiler_params=pltpu.CompilerParams(collective_id=0, has_side_effects=True, vmem_limit_bytes=60 * 2**20),
        name='head',
    )(hidden, dy, wq, wk, wv, wo, pos, gtile, cos_t, sin_t)


NEG_INF = float('-inf')
QB = 256
KC = 256


def attn_kernel(qt, q, k, kt, v, vt, dot_, do, posk, posq, cos, sin, ot, dqt, dk, dv, s_scr, e_scr, p_scr, d_scr):
    head = pl.program_id(0)
    n = qt.shape[1]
    f32, bf16 = jnp.float32, jnp.bfloat16
    half = HEAD_DIM // 2

    @pl.when(head == 0)
    def _():
        dk[...] = jnp.zeros_like(dk)
        dv[...] = jnp.zeros_like(dv)

    def dot(a, b):
        return jnp.dot(a, b, preferred_element_type=f32)

    @pl.loop(0, n // QB)
    def _(j):
        cols = pl.ds(pl.multiple_of(j * QB, QB), QB)
        q_t, do_t = qt[:, cols], dot_[:, cols]
        q_pos = posq[0:1, cols]
        top = jnp.full((8, QB), NEG_INF, f32)
        for c in range(n // KC):
            rows = slice(c * KC, (c + 1) * KC)
            s = dot(k[rows, :], q_t)
            pk = posk[rows, :]
            vis = jnp.concatenate([pk] * (QB // 128), axis=1) <= q_pos
            s = jnp.where(vis, s, NEG_INF)
            s_scr[rows, :] = s
            top = jnp.maximum(top, jnp.max(s.reshape(KC // 8, 8, QB), axis=0))
        m = jnp.max(top, axis=0, keepdims=True)
        tot = jnp.zeros((8, QB), f32)
        for c in range(n // KC):
            rows = slice(c * KC, (c + 1) * KC)
            e = jnp.exp2((s_scr[rows, :] - m) * (SCALE * LOG2E))
            s_scr[rows, :] = e
            e_scr[rows, :] = e.astype(bf16)
            tot = tot + jnp.sum(e.reshape(KC // 8, 8, QB), axis=0)
        den = jnp.sum(tot, axis=0, keepdims=True)
        inv = 1.0 / den
        o = (dot(vt[...], e_scr[...]) / den).astype(bf16)
        ot[:, cols] = o
        delta = jnp.sum(do_t.astype(f32) * o.astype(f32), axis=0, keepdims=True)
        q_n, do_n = q[cols, :], do[cols, :]
        for c in range(n // KC):
            rows = slice(c * KC, (c + 1) * KC)
            p = s_scr[rows, :] * inv
            dp = dot(v[rows, :], do_t)
            p_scr[rows, :] = p.astype(bf16)
            d_scr[rows, :] = (p * (dp - delta)).astype(bf16)
            dv[rows, :] += dot(p_scr[rows, :], do_n)
            dk[rows, :] += dot(d_scr[rows, :], q_n)
        g = dot(kt[...], d_scr[...]) * SCALE
        co, si = cos[:, cols], sin[:, cols]
        a, b = g[:half], g[half:]
        dqt[:half, cols] = (a * co + b * si).astype(bf16)
        dqt[half:, cols] = (b * co - a * si).astype(bf16)


def attention(qt, q, k, kt, v, vt, dot_, do, posk, posq, cos_t, sin_t):
    heads, n = qt.shape[0] // HEAD_DIM, qt.shape[1]
    by_row = pl.BlockSpec((HEAD_DIM, n), lambda h: (h, 0))
    by_col = pl.BlockSpec((n, HEAD_DIM), lambda h: (0, h))
    whole = lambda a: pl.BlockSpec(a.shape, lambda h: (0, 0))
    f32, bf16 = jnp.float32, jnp.bfloat16
    return pl.pallas_call(
        attn_kernel,
        grid=(heads,),
        in_specs=[by_row, by_col, whole(k), whole(kt), whole(v), whole(vt), by_row, by_col, whole(posk), whole(posq), whole(cos_t), whole(sin_t)],
        out_specs=[by_row, by_row, pl.BlockSpec((n, HEAD_DIM), lambda h: (0, 0)), pl.BlockSpec((n, HEAD_DIM), lambda h: (0, 0))],
        out_shape=[jax.ShapeDtypeStruct((heads * HEAD_DIM, n), bf16), jax.ShapeDtypeStruct((heads * HEAD_DIM, n), bf16), jax.ShapeDtypeStruct((n, HEAD_DIM), f32), jax.ShapeDtypeStruct((n, HEAD_DIM), f32)],
        scratch_shapes=[pltpu.VMEM((n, QB), f32), pltpu.VMEM((n, QB), bf16), pltpu.VMEM((n, QB), bf16), pltpu.VMEM((n, QB), bf16)],
        compiler_params=pltpu.CompilerParams(dimension_semantics=('arbitrary',), vmem_limit_bytes=48 * 2**20),
        cost_estimate=pl.CostEstimate(flops=12 * heads * n * n * HEAD_DIM, bytes_accessed=16 * n * n, transcendentals=heads * n * n),
        name='attention',
    )(qt, q, k, kt, v, vt, dot_, do, posk, posq, cos_t, sin_t)


def rope_tables():
    j = np.arange(HEAD_DIM // 2, dtype=np.float64) / (HEAD_DIM // 2)
    freq = (ROPE_THETA ** -j).astype(np.float32)
    angle = freq[:, None] * np.arange(TOKENS, dtype=np.float32)[None, :]
    return np.cos(angle.astype(np.float64)).astype(np.float32), np.sin(angle.astype(np.float64)).astype(np.float32)


def unrope(x, cos, sin):
    a, b = x[:, :64], x[:, 64:]
    return jnp.concatenate([a * cos + b * sin, b * cos - a * sin], axis=1)


NT = (((1,), (1,)), ((), ()))
TN = (((0,), (0,)), ((), ()))


def solution(mesh):
    def swap(a):
        return lax.ppermute(a, 'cp', [(0, 1), (1, 0)])

    def shard_fn(hidden, tok_pos, grad_out, norm_gain, w_query, w_key, w_value, w_out):
        f32, bf16 = jnp.float32, jnp.bfloat16
        f, core = lax.axis_index('fsdp'), lax.axis_index('cp')
        x, y = lax.rem(f, 4), lax.rem(lax.div(f, 4), 4)
        first = core == 0
        hidden, grad_out = hidden[0], grad_out[0]
        dim, half, rows = DIM, HALF, ROWS

        def order(own, other, axis):
            return jnp.where(first, jnp.concatenate([own, other], axis), jnp.concatenate([other, own], axis))

        cos_t, sin_t = (jnp.asarray(t) for t in rope_tables())
        lane = jnp.arange(128) // 16
        gtile = jnp.broadcast_to(jnp.where(lane == x * 2 + core, jnp.tile(norm_gain, 8), 0.0), (8, 128))
        pos8 = jnp.broadcast_to(tok_pos, (8, rows))
        qt, do_t, k, kt, v, vt, rt, dyc, wqkv, wqkvp, wo_own, wo_peer, gain = head(hidden, grad_out, w_query, w_key, w_value, w_out, pos8, gtile, cos_t, sin_t)
        wqkv, wqkvp = wqkv.reshape(dim, QKV), wqkvp.reshape(dim, QKV)
        gain = gain[0:1]
        ip = jnp.arange(TOKENS)
        posk = jnp.broadcast_to(ip[:, None], (TOKENS, 128))
        posq = jnp.broadcast_to(ip[None, :], (8, TOKENS))
        ot, dqt, dk, dv = attention(qt, qt.T, k, kt, v, vt, do_t, do_t.T, posk, posq, cos_t, sin_t)
        dk = unrope(dk * SCALE, cos_t.T, sin_t.T).astype(bf16)
        dkv = jnp.concatenate([dk, dv.astype(bf16)], axis=1)
        dqkv = jnp.concatenate([dqt.T, dkv], axis=1)
        ot_peer = swap(ot)
        dqkv_peer = swap(dqkv)
        pick_own = (tok_pos[0][:, None] == ip[None, :]).astype(bf16)
        o_t = order(ot, ot_peer, 0)
        o_rows = lax.dot_general(pick_own, o_t, NT, preferred_element_type=f32).astype(bf16)
        wo = order(wo_own.reshape(dim, half), wo_peer.reshape(dim, half), 1)
        xf = hidden.astype(f32)
        result = (xf + jnp.dot(o_rows, wo, preferred_element_type=f32)).astype(bf16)
        grad_o = jnp.dot(o_t, dyc, preferred_element_type=f32)
        grad_qkv = jnp.dot(rt, dqkv, preferred_element_type=f32)
        own_rows = jnp.dot(pick_own, jnp.concatenate([dqkv, dqkv_peer], axis=1), preferred_element_type=f32).astype(bf16)
        dr = lax.dot_general(own_rows[:, :QKV], wqkv, NT, preferred_element_type=f32) + lax.dot_general(own_rows[:, QKV:], wqkvp, NT, preferred_element_type=f32)
        inv = lax.rsqrt(jnp.mean(xf * xf, axis=-1, keepdims=True) + RMS_EPS)
        unit = xf * inv
        drg = dr * gain
        grad_hidden = (grad_out.astype(f32) + inv * (drg - unit * jnp.mean(drg * unit, axis=-1, keepdims=True))).astype(bf16)
        gpart = jnp.pad(jnp.sum(dr * unit, axis=0).reshape(4, 4, 128), ((0, 0), (0, 4), (0, 0)))
        out, gout = reduce_scatter([grad_qkv, grad_o], gpart, COLORS, 1)
        own, other = out[0], out[1]
        cut = lambda a, b: order(own[:, a:b], other[:, a:b], 1)
        grad_gain = lax.dynamic_slice(gout, (y, x * 32 + core * 16), (1, 16)).reshape(16)
        return result[None], grad_hidden[None], cut(0, half), cut(half, half + 128), cut(half + 128, half + 256), cut(half + 256, 2 * half + 256), grad_gain

    row_spec, pos_spec = P('fsdp', 'cp', None), P('fsdp', 'cp')
    weight_spec, gain_spec = P(('fsdp', 'cp'), None), P(('fsdp', 'cp'))
    return jax.shard_map(shard_fn, mesh=mesh, in_specs=(row_spec, pos_spec, row_spec, gain_spec, weight_spec, weight_spec, weight_spec, weight_spec), out_specs=(row_spec, row_spec, weight_spec, weight_spec, weight_spec, weight_spec, gain_spec), check_vma=False)
```

```python
import functools
import jax
import jax.numpy as jnp
import numpy as np
from jax import lax
from jax.experimental import pallas as pl
from jax.experimental.pallas import tpu as pltpu
from jax.sharding import PartitionSpec as P

LANES, SUBS, RING, TRIO = 128, 8, 4, 3
PAIR, ROWS, CHIP, SHARE = 256, 512, 32, 16
HEAD_DIM = LANES
ROPE_THETA = 1000000.0
RMS_EPS = 1e-5
SCALE = HEAD_DIM ** -0.5
LOG2E = 1.4426950408889634

MESH = pl.DeviceIdType.MESH
AXES = ('x', 'y', 'z')
ORDERS = (('x', 'y', 'z'), ('y', 'z', 'x'), ('z', 'x', 'y'))
ALL = pl.ds(0, RING)


def torus():
    f = lax.axis_index('fsdp')
    return {'x': lax.rem(f, RING), 'y': lax.rem(lax.div(f, RING), RING), 'z': lax.div(f, SHARE)}


def step(pos, axis, hop):
    return lax.rem(pos[axis] + hop, RING)


class Comm:
    def __init__(self, send_sems, recv_sems, local_sems):
        self.pos = torus()
        self.core = lax.axis_index('cp')
        self.sems = (send_sems, recv_sems, local_sems)
        self.used = self.used_local = 0
        self.sent, self.exchanged, self.stored = [], [], []

    def far(self, axis, hop):
        p = dict(self.pos)
        p[axis] = step(self.pos, axis, hop)
        return {'fsdp': (p['z'] * RING + p['y']) * RING + p['x'], 'cp': self.core}

    def peer(self):
        return {'fsdp': lax.axis_index('fsdp'), 'cp': 1 - self.core}

    def barrier(self):
        sem = pltpu.get_barrier_semaphore()
        for axis in AXES:
            for hop in (1, 2, TRIO):
                pl.semaphore_signal(sem, inc=1, device_id=self.far(axis, hop), device_id_type=MESH)
        pl.semaphore_signal(sem, inc=1, device_id=self.peer(), device_id_type=MESH)
        pl.semaphore_wait(sem, 10)

    def _copy(self, src, dst, device):
        i = self.used
        self.used += 1
        c = pltpu.make_async_remote_copy(src_ref=src, dst_ref=dst, send_sem=self.sems[0].at[i], recv_sem=self.sems[1].at[i], device_id=device, device_id_type=MESH)
        c.start()
        return c

    def send(self, src, dst, device):
        c = self._copy(src, dst, device)
        self.sent.append(c)
        return c

    def trade(self, src, dst):
        self.exchanged.append(self._copy(src, dst, self.peer()))

    def local(self, src, dst):
        i = self.used_local
        self.used_local += 1
        c = pltpu.make_async_copy(src, dst, self.sems[2].at[i])
        c.start()
        return c

    def store(self, src, dst):
        self.stored.append(self.local(src, dst))

    def finish(self):
        for c in self.sent:
            c.wait_send()
        for c in self.exchanged:
            c.wait_send()
            c.wait_recv()
        for c in self.stored:
            c.wait()


def pick(ref, sel, cols):
    return ref.at[sel['z'], sel['y'], sel['x'], :, pl.ds(cols[0], cols[1])]


def sem_scratch(remote, local):
    return [pltpu.SemaphoreType.DMA((remote,)), pltpu.SemaphoreType.DMA((remote,)), pltpu.SemaphoreType.DMA((local,))]


def add_into(dst, *srcs):
    lead = dst.shape[:-2]
    n = 1
    for v in lead:
        n *= v

    def body(i):
        idx, rest = [], i
        for v in reversed(lead):
            idx.append(lax.rem(rest, v))
            rest = lax.div(rest, v)
        idx = tuple(reversed(idx))
        total = dst[idx]
        for s in srcs:
            total = total + s[idx]
        dst[idx] = total

    if n == 1:
        total = dst[...]
        for s in srcs:
            total = total + s[...]
        dst[...] = total
    else:
        pl.loop(0, n)(body)


QKV_COLORS = ((0, PAIR, PAIR), (ROWS, PAIR, LANES), (896, LANES, PAIR))
WO_COLORS = ((0, LANES, LANES), (PAIR, LANES, PAIR), (640, PAIR, LANES))
TOKENS = 1024
DIM = 2048
HALF = 1024
QKV = 1280


def dot(a, b):
    return jnp.dot(a, b, preferred_element_type=jnp.float32)


def dot_nt(a, b):
    return lax.dot_general(a, b, (((1,), (1,)), ((), ())), preferred_element_type=jnp.float32)


def tile_at(i, n):
    return pl.ds(pl.multiple_of(i * n, n), n)


class Gather:
    def __init__(self, comm, ref, colors, land):
        self.comm, self.ref, self.colors, self.land = comm, ref, colors, land
        self.held = [dict(comm.pos) for _ in colors]

    def parts(self, k):
        lo, na, nb = self.colors[k]
        return (lo, na), (lo + na, nb)

    def move(self, s, cols, to):
        return self.comm.send(pick(self.ref, s, cols), pick(self.ref, s, cols), to)

    def begin(self, phase):
        self.phase, self.first, self.second = phase, [], []
        for k in range(TRIO):
            a, b = self.parts(k)
            d = ORDERS[k][phase]
            up, dn, s = self.comm.far(d, 1), self.comm.far(d, TRIO), self.held[k]
            self.first.append([self.move(s, cols, to) for cols, to in ((a, up), (b, dn), (b, up), (a, dn))])
        if phase == 2:
            for k in range(TRIO):
                for cols in self.parts(k):
                    self.land(self.ref, self.held[k], cols)

    def at(self, k, hop):
        d = ORDERS[k][self.phase]
        return dict(self.held[k], **{d: step(self.comm.pos, d, hop)})

    def forward(self):
        for k in range(TRIO):
            a, b = self.parts(k)
            d = ORDERS[k][self.phase]
            self.first[k][0].wait_recv()
            c = self.move(self.at(k, TRIO), a, self.comm.far(d, 1))
            self.first[k][1].wait_recv()
            self.second.append((c, self.move(self.at(k, 1), b, self.comm.far(d, TRIO))))
            if self.phase == 2:
                self.land(self.ref, self.at(k, TRIO), a)
                self.land(self.ref, self.at(k, 1), b)

    def end(self):
        for k in range(TRIO):
            a, b = self.parts(k)
            d = ORDERS[k][self.phase]
            for c, hop, cols in ((self.first[k][2], TRIO, b), (self.first[k][TRIO], 1, a), (self.second[k][0], 2, a), (self.second[k][1], 2, b)):
                c.wait_recv()
                if self.phase == 2:
                    self.land(self.ref, self.at(k, hop), cols)
            self.held[k] = dict(self.held[k], **{d: ALL})


def head_kernel(hidden, dy, wq, wk, wv, wo, pos, gtile, cos_t, sin_t,
                qt_o, dot_o, k_o, kt_o, v_o, vt_o, rt_o, dyc_o, wqkv_o, wqkvp_o, wo_o, wop_o, gain_o,
                hid2, dy2, dys, rs, rt, wqkv, wout, wpeer, pi, pos2, qt, dot_s, kk, kt, vv, vt, gain, gbuf, gx, gy, gz, *sems):
    comm = Comm(*sems)
    pos_c, core = comm.pos, comm.core
    bf16, f32 = jnp.bfloat16, jnp.float32
    peer = comm.peer()
    rows = tile_at(core, SHARE)
    mine_qkv = wqkv.at[pos_c['z'], pos_c['y'], pos_c['x'], rows]
    mine_wo = wout.at[pos_c['z'], pos_c['y'], pos_c['x'], rows]

    def weight_parts(c):
        return ((wq.at[:, tile_at(c, HALF)], mine_qkv.at[:, pl.ds(0, HALF)]), (wk.at[:, tile_at(c, LANES)], mine_qkv.at[:, pl.ds(HALF, LANES)]),
                (wv.at[:, tile_at(c, LANES)], mine_qkv.at[:, pl.ds(HALF + LANES, LANES)]), (wo.at[:, tile_at(c, HALF)], mine_wo))

    loads = [comm.local(s, d) for s, d in weight_parts(core)]
    load_x = [comm.local(hidden, hid2.at[0]), comm.local(dy, dy2.at[0])]
    comm.barrier()
    swaps = [comm.send(s, d, peer) for s, d in weight_parts(1 - core)]
    gstage = [comm.send(gtile, gbuf, peer)]
    swap_pos = comm.send(pos, pos2.at[1], peer)
    swap_dy = comm.send(dy, dy2.at[1], peer)
    swap_x = comm.send(hidden, hid2.at[1], peer)
    pos2[0] = pos[...]
    for c in loads:
        c.wait()
    gstage[0].wait_recv()
    gx[0] = gtile[...] + gbuf[...]
    gstage = [comm.send(gx.at[0], gx.at[hop], comm.far('x', hop)) for hop in (1, 2, TRIO)]
    for c in swaps:
        c.wait_recv()

    def land_qkv(ref, s, cols):
        comm.trade(pick(ref, s, cols), pick(wqkvp_o, s, cols))

    arrived = []

    def land_wo(ref, s, cols):
        arrived.append(comm.send(pick(ref, s, cols), pick(wpeer, s, cols), peer))

    g1 = Gather(comm, wqkv, QKV_COLORS, land_qkv)
    g2 = Gather(comm, wout, WO_COLORS, land_wo)
    g1.begin(0)
    g2.begin(0)

    swap_pos.wait_recv()

    @pl.loop(0, TOKENS // LANES)
    def _(i):
        want = lax.broadcasted_iota(jnp.int32, (LANES, ROWS), 0) + i * LANES
        for h in range(2):
            have = pos2[h, 0:1, :]
            pi[tile_at(i, LANES), h * ROWS:(h + 1) * ROWS] = jnp.where(want == have, 1.0, 0.0).astype(bf16)

    def gain_x():
        for c in gstage:
            c.wait_recv()
        gy[pos_c['y']] = (gx[0] + gx[1]) + (gx[2] + gx[TRIO])
        return [comm.send(gy.at[pos_c['y']], gy.at[pos_c['y']], comm.far('y', hop)) for hop in (1, 2, TRIO)]

    g1.forward()
    g2.forward()
    gstage = gain_x()
    g1.end()
    g2.end()
    g1.begin(1)
    g2.begin(1)

    def sort(dst, src2, first, last):
        @pl.loop(first, last)
        def _(i):
            r = tile_at(i, PAIR)

            @pl.loop(0, DIM // ROWS)
            def _(j):
                c = tile_at(j, ROWS)
                acc = dot(pi[r, :ROWS], src2[0, :, c]) + dot(pi[r, ROWS:], src2[1, :, c])
                dst[r, c] = acc.astype(bf16)

    load_x[1].wait()
    swap_dy.wait_recv()
    sort(dys, dy2, 0, 1)
    g1.forward()
    g2.forward()
    for c in gstage:
        c.wait_recv()
    for j in range(RING):
        gz[pos_c['z'], j] = gy[j]
    gstage = [comm.send(gz.at[pos_c['z']], gz.at[pos_c['z']], comm.far('z', hop)) for hop in (1, 2, TRIO)]
    g1.end()
    g1.begin(2)
    g2.end()
    sort(dys, dy2, 1, TRIO)
    for c in gstage:
        c.wait_recv()
    for i in range(RING):
        for j in range(RING):
            gain[:, (i * RING + j) * LANES:(i * RING + j + 1) * LANES] = gz[i, j]
    comm.store(gain, gain_o)
    load_x[0].wait()
    swap_x.wait_recv()
    for h in range(2):
        @pl.loop(0, ROWS // CHIP)
        def _(i):
            r = tile_at(i, CHIP)
            x = hid2[h, r, :].astype(f32)
            inv = lax.rsqrt(jnp.mean(x * x, axis=-1, keepdims=True) + RMS_EPS)
            hid2[h, r, :] = (x * inv * gain[0:1, :]).astype(bf16)
    g1.forward()
    g2.begin(2)
    sort(dys, dy2, TRIO, RING)
    comm.store(dys.at[:, tile_at(core, HALF)], dyc_o)
    sort(rs, hid2, 0, RING)
    g1.end()
    comm.store(wqkv, wqkv_o)

    w2 = wqkv.reshape(DIM, QKV)

    def project(t, i):
        r = tile_at(i, PAIR)
        x = dot(rs[r, :], w2[:, tile_at(t, PAIR)])
        cos, sin = cos_t[:, r], sin_t[:, r]
        cos = jnp.concatenate([cos, cos], axis=0).T
        sin = jnp.concatenate([-sin, sin], axis=0).T
        return r, x, cos, sin

    def rotate(x, cos, sin):
        return x * cos + pltpu.roll(x, 64, 1) * sin

    @pl.loop(0, RING)
    def _(i):
        r, x, cos, sin = project(RING, i)
        key, val = rotate(x[:, :LANES], cos, sin).astype(bf16), x[:, LANES:].astype(bf16)
        kk[r, :] = key
        kt[:, r] = key.T
        vv[r, :] = val
        vt[:, r] = val.T

    def queries(first, last):
        @pl.loop(first, last)
        def _(t):
            @pl.loop(0, RING)
            def _(i):
                r, x, cos, sin = project(t, i)
                for h in range(2):
                    q = rotate(x[:, h * LANES:(h + 1) * LANES], cos, sin).astype(bf16)
                    qt[tile_at(2 * t + h, LANES), r] = q.T

    queries(0, 1)
    g2.forward()
    queries(1, RING)
    for src, dst in ((kk, k_o), (kt, kt_o), (vv, v_o), (vt, vt_o), (qt, qt_o)):
        comm.store(src, dst)

    @pl.loop(0, DIM // PAIR)
    def _(i):
        c = tile_at(i, PAIR)

        @pl.loop(0, TOKENS // PAIR)
        def _(j):
            r = tile_at(j, PAIR)
            rt[c, r] = rs[r, c].T
    comm.store(rt, rt_o)
    g2.end()
    for c in arrived:
        c.wait_recv()
    comm.store(wout, wo_o)
    comm.store(wpeer, wop_o)
    own, other = wout.reshape(DIM, HALF), wpeer.reshape(DIM, HALF)

    @pl.loop(0, HALF // PAIR)
    def _(i):
        r = pl.ds(pl.multiple_of(core * HALF + i * PAIR, PAIR), PAIR)

        @pl.loop(0, TOKENS // PAIR)
        def _(j):
            t = tile_at(j, PAIR)
            acc = dot_nt(own[r, :], dys[t, tile_at(core, HALF)]) + dot_nt(other[r, :], dys[t, tile_at(1 - core, HALF)])
            dot_s[tile_at(i, PAIR), t] = acc.astype(bf16)
    comm.store(dot_s, dot_o)
    comm.finish()


def head(hidden, dy, wq, wk, wv, wo, pos, gtile, cos_t, sin_t):
    bf16, f32 = jnp.bfloat16, jnp.float32
    any_ = pl.BlockSpec(memory_space=pl.ANY)
    vmem = pl.BlockSpec(memory_space=pltpu.VMEM)
    S = lambda shape, d=bf16: jax.ShapeDtypeStruct(shape, d)
    V = lambda shape, d=bf16: pltpu.VMEM(shape, d)
    w_qkv, w_out = (RING, RING, RING, CHIP, QKV), (RING, RING, RING, CHIP, HALF)
    sq, tall, wide = (HALF, TOKENS), (TOKENS, LANES), (LANES, TOKENS)
    return pl.pallas_call(
        head_kernel,
        out_shape=[S(sq), S(sq), S(tall), S(wide), S(tall), S(wide), S((DIM, TOKENS)), S((TOKENS, HALF)), S(w_qkv), S(w_qkv), S(w_out), S(w_out), S((SUBS, DIM), f32)],
        in_specs=[any_] * 6 + [vmem] * RING,
        out_specs=[any_] * 13,
        scratch_shapes=[V((2, ROWS, DIM)), V((2, ROWS, DIM)), V((TOKENS, DIM)), V((TOKENS, DIM)), V((DIM, TOKENS)), V(w_qkv), V(w_out), V(w_out), V((TOKENS, TOKENS)), V((2, SUBS, ROWS), jnp.int32),
                        V(sq), V(sq), V(tall), V(wide), V(tall), V(wide), V((SUBS, DIM), f32), V((SUBS, LANES), f32), V((RING, SUBS, LANES), f32), V((RING, SUBS, LANES), f32), V((RING, RING, SUBS, LANES), f32)] + sem_scratch(192, CHIP),
        compiler_params=pltpu.CompilerParams(collective_id=0, has_side_effects=True, vmem_limit_bytes=60 * 2**20),
        name='head',
    )(hidden, dy, wq, wk, wv, wo, pos, gtile, cos_t, sin_t)


HEADS = SUBS
QB = PAIR
NBLK = TOKENS // QB
UNIT_Q = tuple(range(HEADS))
UNIT_K, UNIT_V = SUBS, 9
UNIT_O = tuple(range(10, 18))
N_UNITS = 18
LINES = ((0, TRIO, 6, 9, 12, 15), (1, RING, 7, 10, 13, SHARE), (2, 5, SUBS, 11, 14, 17))
COLOR = {u: k for k, line in enumerate(LINES) for u in line}
SLOT = {u: i % RING for line in LINES for i, u in enumerate(line)}
PLACE = {**{u: u for u in range(12)}, **{u: u - 12 for u in range(12, 18)}}
LAG = (0, RING, SUBS, 10, 12, 13, 14)
HALVES = (pl.ds(0, SHARE), pl.ds(SHARE, SHARE))


class Scatter:
    def __init__(self, comm, part, bufs, fin, out, send_sems, recv_sems, swap_sems):
        self.pos, self.part, self.bufs, self.fin, self.out = comm.pos, part, bufs, fin, out
        self.sems, self.swap_sems = (send_sems, recv_sems), swap_sems
        self.near = {(a, hop): comm.far(a, hop) for a in AXES for hop in (1, TRIO)}
        self.hops = {(a, hop): step(comm.pos, a, hop) for a in AXES for hop in (1, 2, TRIO)}
        self.peer, self.core = comm.peer(), comm.core
        self.keep, self.give = tile_at(comm.core, SHARE), tile_at(1 - comm.core, SHARE)

    def sel(self, u, phase, hop):
        order = ORDERS[COLOR[u]]
        s = {a: ALL for a in AXES}
        for a in order[:phase]:
            s[a] = self.pos[a]
        a = order[phase]
        s[a] = self.hops[a, hop] if hop else self.pos[a]
        return s

    def view(self, u, phase, hop, half):
        s = self.sel(u, phase, hop)
        return self.part.at[PLACE[u], s['z'], s['y'], s['x'], HALVES[half], :]

    def buf(self, u, phase, name):
        return self.bufs[phase].at[COLOR[u], SLOT[u], name]

    def copy(self, u, phase, name):
        hop, half, to = ((2, 0, 1), (2, 1, TRIO), (1, 1, 1), (TRIO, 0, TRIO), (1, 0, 1), (TRIO, 1, TRIO))[name]
        i = (u * TRIO + phase) * 6 + name
        return pltpu.make_async_remote_copy(src_ref=self.view(u, phase, hop, half), dst_ref=self.buf(u, phase, name), send_sem=self.sems[0].at[i], recv_sem=self.sems[1].at[i],
                                            device_id=self.near[ORDERS[COLOR[u]][phase], to], device_id_type=MESH)

    def launch(self, u, phase):
        for name in range(RING):
            self.copy(u, phase, name).start()

    def swap(self, u):
        cols = pl.ds(u * LANES, LANES)
        give = pltpu.make_async_remote_copy(src_ref=self.fin.at[u, self.give], dst_ref=self.out.at[1, :, cols], send_sem=self.swap_sems.at[u], recv_sem=self.swap_sems.at[N_UNITS + u], device_id=self.peer, device_id_type=MESH)
        keep = pltpu.make_async_copy(self.fin.at[u, self.keep], self.out.at[0, :, cols], self.swap_sems.at[2 * N_UNITS + u])
        return give, keep

    def run(self, u, stage):
        if stage == 0:
            return self.launch(u, 0)
        phase = (stage - 1) // 2
        if stage % 2:
            for first, hop, half, then in ((0, 1, 0, RING), (1, TRIO, 1, 5)):
                self.copy(u, phase, first).wait_recv()
                add_into(self.view(u, phase, hop, half), self.buf(u, phase, first))
                self.copy(u, phase, then).start()
            return
        for half, names in ((0, (TRIO, RING)), (1, (2, 5))):
            for name in names:
                self.copy(u, phase, name).wait_recv()
            srcs = [self.buf(u, phase, name) for name in names]
            if phase < 2:
                add_into(self.view(u, phase, 0, half), *srcs)
            else:
                self.fin[u, HALVES[half], :] = self.view(u, phase, 0, half)[...] + (srcs[0][...] + srcs[1][...])
        if phase < 2:
            return self.launch(u, phase + 1)
        for c in self.swap(u):
            c.start()

    def drain_sends(self, u):
        for phase in range(TRIO):
            for name in range(6):
                self.copy(u, phase, name).wait_send()

    def finish(self, u):
        give, keep = self.swap(u)
        give.wait_send()
        give.wait_recv()
        keep.wait()


def attend(head, qt, do_t, k, kt, v, vt, cos, sin, o_rows, ot, dq, dk, dv, s_scr, e_scr, p_scr, d_scr, between):
    f32, bf16 = jnp.float32, jnp.bfloat16
    mine = tile_at(head, LANES)
    below = lax.broadcasted_iota(jnp.int32, (QB, QB), 0) <= lax.broadcasted_iota(jnp.int32, (QB, QB), 1)

    def fold(x, op):
        return op(x.reshape(-1, SUBS, QB), axis=0)

    def scores(j):
        cols, b = slice(j * QB, (j + 1) * QB), j % 2
        q_t = qt[mine, cols]
        top = None
        for c in range(j + 1):
            rows = slice(c * QB, (c + 1) * QB)
            s = dot(k[rows, :], q_t)
            if c == j:
                s = jnp.where(below, s, -jnp.inf)
            s_scr[b, rows, :] = s
            t = fold(s, jnp.max)
            top = t if top is None else jnp.maximum(top, t)
        return jnp.max(top, axis=0, keepdims=True)

    def rest(j, m):
        cols, b, n = slice(j * QB, (j + 1) * QB), j % 2, (j + 1) * QB
        q_t, d_t = qt[mine, cols], do_t[mine, cols]
        tot = None
        for c in range(j + 1):
            rows = slice(c * QB, (c + 1) * QB)
            e = jnp.exp2((s_scr[b, rows, :] - m) * (SCALE * LOG2E))
            s_scr[b, rows, :] = e
            e_scr[b, rows, :] = e.astype(bf16)
            t = fold(e, jnp.sum)
            tot = t if tot is None else tot + t
        den = jnp.sum(tot, axis=0, keepdims=True)
        inv = 1.0 / den
        o = (dot(vt[:, :n], e_scr[b, :n, :]) / den).astype(bf16)
        ot[o_rows, cols] = o
        delta = jnp.sum(d_t.astype(f32) * o.astype(f32), axis=0, keepdims=True)
        for c in range(j + 1):
            rows = slice(c * QB, (c + 1) * QB)
            p = s_scr[b, rows, :] * inv
            p_scr[b, rows, :] = p.astype(bf16)
            d_scr[b, rows, :] = (p * (dot(v[rows, :], d_t) - delta)).astype(bf16)
        dv[:n, :] += dot_nt(p_scr[b, :n, :], d_t)
        dk[:n, :] += dot_nt(d_scr[b, :n, :], q_t)
        g = dot(kt[:, :n], d_scr[b, :n, :]) * SCALE
        co, si = cos[:, cols], sin[:, cols]
        x, y = g[:64], g[64:]
        dq[tile_at(head, LANES), cols] = jnp.concatenate([x * co + y * si, y * co - x * si], axis=0).astype(bf16)

    m = scores(0)
    for j in range(NBLK):
        later = scores(j + 1) if j + 1 < NBLK else None
        rest(j, m)
        m = later
        if j == 2:
            between()


def tail_kernel(qt, do_t, k, kt, v, vt, rt, dyc, wqkv, wqkvp, wo, wop, gain, hidden, dy, pos_col, cos, sin,
                result, grad_x, out, gout,
                a1, a2, ks, kts, vs, vts, rts, ots, dqo, dqp, dkvo, dkvp, dk, dv, s_scr, e_scr, p_scr, d_scr, dycs, part, buf1, buf2, buf3, fin, pick_rows, onat, dnat, xs, wkv, wkvp, drs, gacc, gpart, gpeer, gz, gy, gx,
                send_sems, recv_sems, swap_sems, trade_send, trade_recv, local_sems):
    comm = Comm(trade_send, trade_recv, local_sems)
    comm.used = 2 * HEADS
    f32, bf16 = jnp.float32, jnp.bfloat16
    core, peer = comm.core, comm.peer()
    sc = Scatter(comm, part, (buf1, buf2, buf3), fin, out, send_sems, recv_sems, swap_sems)
    loads = [comm.local(s, d) for s, d in ((qt, a1), (do_t, a2), (k, ks), (kt, kts), (v, vs), (vt, vts))]
    load_r = comm.local(rt, rts)
    later = [comm.local(s, d) for s, d in ((dyc, dycs), (hidden, xs), (wqkv.at[:, pl.ds(HALF, PAIR)], wkv), (wqkvp.at[:, pl.ds(HALF, PAIR)], wkvp))]
    comm.barrier()
    dk[...] = jnp.zeros_like(dk)
    dv[...] = jnp.zeros_like(dv)

    @pl.loop(0, ROWS // LANES)
    def _(i):
        have = pos_col[tile_at(i, LANES), :]
        for c in range(TOKENS // LANES):
            want = lax.broadcasted_iota(jnp.int32, (LANES, LANES), 1) + c * LANES
            pick_rows[tile_at(i, LANES), c * LANES:(c + 1) * LANES] = jnp.where(want == have, 1.0, 0.0).astype(bf16)

    for c in loads:
        c.wait()

    events = {}
    clock = [0]

    def schedule(u, at):
        for stage, lag in enumerate(LAG):
            events.setdefault(at + lag, []).append((stage, u))

    for h in range(HEADS):
        schedule(h, 2 * h + 1)

    def tick(t):
        for stage, u in sorted(events.pop(t, []), reverse=True):
            sc.run(u, stage)

    def head_trades(h):
        row = tile_at(core * HEADS + h, LANES)
        mine = tile_at(h, LANES)
        return [pltpu.make_async_remote_copy(src_ref=s, dst_ref=d, send_sem=trade_send.at[i], recv_sem=trade_recv.at[i], device_id=peer, device_id_type=MESH)
                for s, d, i in ((ots.at[row], ots.at[row], h), (dqo.at[mine], dqp.at[mine], HEADS + h))]

    def gradient(place, left, right, mul):
        @pl.loop(0, RING)
        def _(z):
            g = mul(left[tile_at(z, ROWS), :], right)
            n = g.shape[1] // LANES
            for i in range(n):
                part[place + i, z] = g[:, i * LANES:(i + 1) * LANES].reshape(RING, RING, CHIP, LANES)

    load_r.wait()
    tick(0)

    @pl.loop(0, HEADS)
    def _(h):
        def between():
            for hh in range(1, HEADS):
                if events.get(2 * hh):
                    pl.when(h == hh)(functools.partial(tick, 2 * hh))

        attend(h, a1, a2, ks, kts, vs, vts, cos, sin, tile_at(core * HEADS + h, LANES), ots, dqo, dk, dv, s_scr, e_scr, p_scr, d_scr, between)
        for c in head_trades(h):
            c.start()

        @pl.loop(0, RING)
        def _(z):
            g = dot_nt(rts[tile_at(z, ROWS), :], dqo[tile_at(h, LANES), :])
            part[h, z] = g.reshape(RING, RING, CHIP, LANES)
        for hh in range(HEADS):
            pl.when(h == hh)(functools.partial(tick, 2 * hh + 1))

    t = [2 * HEADS]

    def beat():
        tick(t[0])
        t[0] += 1

    key = dk[...] * SCALE
    co, si = jnp.concatenate([cos[...], cos[...]], axis=0).T, jnp.concatenate([sin[...], -sin[...]], axis=0).T
    dkvo[:, :LANES] = (key * co + pltpu.roll(key, 64, 1) * si).astype(bf16)
    dkvo[:, LANES:] = dv[...].astype(bf16)
    comm.trade(dkvo, dkvp)
    gradient(UNIT_K, rts, dkvo[...], dot)
    schedule(UNIT_K, t[0])
    schedule(UNIT_V, t[0])
    beat()
    wo_loads = [comm.local(wo.at[tile_at(i, HALF)], a) for i, a in ((0, a1), (1, a2))]
    wq_load = comm.local(wqkv.at[:, pl.ds(0, HALF)], rts)
    for c in later:
        c.wait()
    for h in range(HEADS):
        for c in head_trades(h):
            c.wait()

    def output_gradient(i):
        for u in (10 + 2 * i, 11 + 2 * i):
            if PLACE[u] != u:
                sc.drain_sends(PLACE[u])
        gradient(PLACE[10 + 2 * i], ots, dycs[:, i * PAIR:(i + 1) * PAIR], dot)
        for u in (10 + 2 * i, 11 + 2 * i):
            schedule(u, t[0])

    def natural(dst, src_t, n):
        @pl.loop(0, n // PAIR)
        def _(i):
            dst[:, tile_at(i, PAIR)] = dot_nt(pick_rows[...], src_t[tile_at(i, PAIR), :]).astype(bf16)

    def project_out(col, weights):
        @pl.loop(0, HALF // PAIR)
        def _(i):
            c = tile_at(i, PAIR)
            dst = pl.ds(pl.multiple_of(col + i * PAIR, PAIR), PAIR)
            acc = dot(onat[:, :HALF], weights[0][:, c]) + dot(onat[:, HALF:], weights[1][:, c])
            dnat[:, dst] = (xs[:, dst].astype(f32) + acc).astype(bf16)

    output_gradient(0)
    beat()
    natural(onat, ots, DIM)
    beat()
    output_gradient(1)
    beat()
    for c in wo_loads:
        c.wait()
    project_out(core * HALF, (a1, a2))
    beat()
    beat()
    wo_loads = [comm.local(wop.at[tile_at(i, HALF)], a) for i, a in ((0, a1), (1, a2))]
    output_gradient(2)
    beat()
    for c in wo_loads:
        c.wait()
    project_out((1 - core) * HALF, (a1, a2))
    beat()
    beat()
    save = comm.local(dnat.at[:, pl.ds(0, DIM)], result)
    load_dy = comm.local(dy, onat)
    beat()
    output_gradient(TRIO)
    beat()
    wqp_load = comm.local(wqkvp.at[:, pl.ds(0, HALF)], ots)
    save.wait()
    for c in comm.exchanged:
        c.wait_recv()
    natural(dnat, dqo, HALF)
    beat()
    for i, src in ((2 * HALF, dkvo), (2 * HALF + PAIR, dkvp)):
        dnat[:, i:i + PAIR] = dot(pick_rows[...], src[...]).astype(bf16)

    @pl.loop(0, HALF // PAIR)
    def _(i):
        dnat[:, pl.ds(pl.multiple_of(HALF + i * PAIR, PAIR), PAIR)] = dot_nt(pick_rows[...], dqp[tile_at(i, PAIR), :]).astype(bf16)
    beat()
    wq_load.wait()
    wqp_load.wait()
    load_dy.wait()
    gacc[...] = jnp.zeros_like(gacc)

    def back(i):
        r = pl.ds(i * LANES, LANES)

        @pl.loop(0, DIM // PAIR)
        def _(j):
            c = tile_at(j, PAIR)
            acc = dot_nt(dnat[r, :HALF], rts[c, :]) + dot_nt(dnat[r, HALF:2 * HALF], ots[c, :])
            acc = acc + dot_nt(dnat[r, 2 * HALF:2 * HALF + PAIR], wkv[c, :]) + dot_nt(dnat[r, 2 * HALF + PAIR:], wkvp[c, :])
            drs[:, c] = acc

        @pl.loop(0, LANES // SHARE)
        def _(j):
            q = pl.ds(pl.multiple_of(i * LANES + j * SHARE, SHARE), SHARE)
            x, d = xs[q, :].astype(f32), drs[tile_at(j, SHARE), :]
            inv = lax.rsqrt(jnp.mean(x * x, axis=-1, keepdims=True) + RMS_EPS)
            unit = x * inv
            gacc[...] += jnp.sum((d * unit).reshape(2, SUBS, DIM), axis=0)
            dg = d * gain[0:1, :]
            onat[q, :] = (onat[q, :].astype(f32) + inv * (dg - unit * jnp.mean(dg * unit, axis=-1, keepdims=True))).astype(bf16)

    for i in range(RING):
        back(i)
        beat()
    comm.store(onat, grad_x)
    total = jnp.sum(gacc[...], axis=0, keepdims=True)
    gpart[...] = jnp.zeros_like(gpart)
    for i in range(RING):
        for j in range(RING):
            gpart[i, j:j + 1, :] = total[:, (i * RING + j) * LANES:(i * RING + j + 1) * LANES]
    stage = [comm.send(gpart, gpeer, peer)]
    beat()
    for c in stage:
        c.wait_recv()
    for j in range(RING):
        gz[j] = gpart[j] + gpeer[j]
    stage = [comm.send(gz.at[step(comm.pos, 'z', hop)], gz.at[TRIO + hop], comm.far('z', hop)) for hop in (1, 2, TRIO)]
    beat()
    for c in stage:
        c.wait_recv()
    gy[0] = (gz[comm.pos['z']] + gz[RING]) + (gz[5] + gz[6])
    stage = [comm.send(gy.at[0], gy.at[hop], comm.far('y', hop)) for hop in (1, 2, TRIO)]
    beat()
    for c in stage:
        c.wait_recv()
    gx[0] = (gy[0] + gy[1]) + (gy[2] + gy[TRIO])
    stage = [comm.send(gx.at[0], gx.at[hop], comm.far('x', hop)) for hop in (1, 2, TRIO)]
    while events:
        beat()
    for c in stage:
        c.wait_recv()
    gout[...] = (gx[0] + gx[1]) + (gx[2] + gx[TRIO])
    for u in range(N_UNITS):
        sc.finish(u)
    for u in range(6, N_UNITS):
        sc.drain_sends(u)
    for c in comm.sent + comm.exchanged:
        c.wait_send()
    for c in comm.stored:
        c.wait()


def tail(qt, do_t, k, kt, v, vt, rt, dyc, wqkv, wqkvp, wo, wop, gain, hidden, dy, pos_col, cos, sin):
    bf16, f32 = jnp.bfloat16, jnp.float32
    any_ = pl.BlockSpec(memory_space=pl.ANY)
    vmem = pl.BlockSpec(memory_space=pltpu.VMEM)
    S = lambda shape, d=bf16: jax.ShapeDtypeStruct(shape, d)
    V = lambda shape, d=bf16: pltpu.VMEM(shape, d)
    D = lambda n: pltpu.SemaphoreType.DMA((n,))
    sq, tall, wide = (HALF, TOKENS), (TOKENS, LANES), (LANES, TOKENS)
    own = (ROWS, DIM)
    return pl.pallas_call(
        tail_kernel,
        out_shape=[S(own), S(own), S((2, SHARE, N_UNITS * LANES), f32), S((SUBS, LANES), f32)],
        in_specs=[any_] * 12 + [vmem] + [any_] * 2 + [vmem] * TRIO,
        out_specs=[any_] * TRIO + [vmem],
        scratch_shapes=[V(sq), V(sq), V(tall), V(wide), V(tall), V(wide), V((DIM, TOKENS)), V((DIM, TOKENS)), V(sq), V(sq), V((TOKENS, PAIR)), V((TOKENS, PAIR)), V(tall, f32), V(tall, f32),
                        V((2, TOKENS, QB), f32), V((2, TOKENS, QB)), V((2, TOKENS, QB)), V((2, TOKENS, QB)), V(sq), V((12, RING, RING, RING, CHIP, LANES), f32),
                        V((TRIO, RING, 6, RING, RING, SHARE, LANES), f32), V((TRIO, RING, 6, RING, SHARE, LANES), f32), V((TRIO, RING, 6, SHARE, LANES), f32), V((N_UNITS, CHIP, LANES), f32), V((ROWS, TOKENS)), V(own), V((ROWS, 2 * QKV)), V(own),
                        V((DIM, PAIR)), V((DIM, PAIR)), V((LANES, DIM), f32), V((SUBS, DIM), f32), V((RING, SUBS, LANES), f32), V((RING, SUBS, LANES), f32), V((7, SUBS, LANES), f32), V((RING, SUBS, LANES), f32), V((RING, SUBS, LANES), f32),
                        D(N_UNITS * 18), D(N_UNITS * 18), D(TRIO * N_UNITS), D(2 * HEADS + SHARE), D(2 * HEADS + SHARE), D(CHIP)],
        compiler_params=pltpu.CompilerParams(collective_id=1, has_side_effects=True, vmem_limit_bytes=67043328),
        name='tail',
    )(qt, do_t, k, kt, v, vt, rt, dyc, wqkv, wqkvp, wo, wop, gain, hidden, dy, pos_col, cos, sin)


def rope_tables():
    j = np.arange(HEAD_DIM // 2, dtype=np.float64) / (HEAD_DIM // 2)
    freq = (ROPE_THETA ** -j).astype(np.float32)
    angle = freq[:, None] * np.arange(TOKENS, dtype=np.float32)[None, :]
    return np.cos(angle.astype(np.float64)).astype(np.float32), np.sin(angle.astype(np.float64)).astype(np.float32)


def solution(mesh):
    def shard_fn(hidden, tok_pos, grad_out, norm_gain, w_query, w_key, w_value, w_out):
        f, core = lax.axis_index('fsdp'), lax.axis_index('cp')
        x, y = lax.rem(f, RING), lax.rem(lax.div(f, RING), RING)
        hidden, grad_out = hidden[0], grad_out[0]
        cos_t, sin_t = (jnp.asarray(t) for t in rope_tables())
        lane = jnp.arange(LANES) // SHARE
        gtile = jnp.broadcast_to(jnp.where(lane == x * 2 + core, jnp.tile(norm_gain, SUBS), 0.0), (SUBS, LANES))
        pos8 = jnp.broadcast_to(tok_pos, (SUBS, ROWS))
        pos_col = jnp.broadcast_to(tok_pos[0][:, None], (ROWS, LANES))
        *parts, wqkv, wqkvp, wo, wop, gain = head(hidden, grad_out, w_query, w_key, w_value, w_out, pos8, gtile, cos_t, sin_t)
        result, grad_hidden, out, gout = tail(*parts, wqkv.reshape(DIM, QKV), wqkvp.reshape(DIM, QKV), wo.reshape(DIM, HALF), wop.reshape(DIM, HALF), gain, hidden, grad_out, pos_col, cos_t, sin_t)
        own, other = out[0], out[1]

        def cut(a, b):
            a, b = own[:, a:b], other[:, a:b]
            return jnp.where(core == 0, jnp.concatenate([a, b], 1), jnp.concatenate([b, a], 1))

        grad_gain = lax.dynamic_slice(gout, (y, x * CHIP + core * SHARE), (1, SHARE)).reshape(SHARE)
        return result[None], grad_hidden[None], cut(0, HALF), cut(HALF, HALF + LANES), cut(HALF + LANES, QKV), cut(QKV, QKV + HALF), grad_gain

    row_spec, pos_spec = P('fsdp', 'cp', None), P('fsdp', 'cp')
    weight_spec, gain_spec = P(('fsdp', 'cp'), None), P(('fsdp', 'cp'))
    return jax.shard_map(shard_fn, mesh=mesh, in_specs=(row_spec, pos_spec, row_spec, gain_spec, weight_spec, weight_spec, weight_spec, weight_spec), out_specs=(row_spec, row_spec, weight_spec, weight_spec, weight_spec, weight_spec, gain_spec), check_vma=False)
```

```python
import functools
import jax
import jax.numpy as jnp
import numpy as np
from jax import lax
from jax.experimental import pallas as pl
from jax.experimental.pallas import tpu as pltpu
from jax.sharding import PartitionSpec as P

LANES, SUBS, RING, TRIO = 128, 8, 4, 3
PAIR, ROWS, CHIP, SHARE = 256, 512, 32, 16
HEAD_DIM = LANES
ROPE_THETA = 1000000.0
RMS_EPS = 1e-5
SCALE = HEAD_DIM ** -0.5
LOG2E = 1.4426950408889634

MESH = pl.DeviceIdType.MESH
AXES = ('x', 'y', 'z')
ORDERS = (('x', 'y', 'z'), ('y', 'z', 'x'), ('z', 'x', 'y'))
ALL = pl.ds(0, RING)


def torus():
    f = lax.axis_index('fsdp')
    return {'x': lax.rem(f, RING), 'y': lax.rem(lax.div(f, RING), RING), 'z': lax.div(f, SHARE)}


def step(pos, axis, hop):
    return lax.rem(pos[axis] + hop, RING)


class Comm:
    def __init__(self, send_sems, recv_sems, local_sems):
        self.pos = torus()
        self.core = lax.axis_index('cp')
        self.sems = (send_sems, recv_sems, local_sems)
        self.used = self.used_local = 0
        self.sent, self.exchanged, self.stored = [], [], []

    def far(self, axis, hop):
        p = dict(self.pos)
        p[axis] = step(self.pos, axis, hop)
        return {'fsdp': (p['z'] * RING + p['y']) * RING + p['x'], 'cp': self.core}

    def peer(self):
        return {'fsdp': lax.axis_index('fsdp'), 'cp': 1 - self.core}

    def barrier(self):
        sem = pltpu.get_barrier_semaphore()
        for axis in AXES:
            for hop in (1, 2, TRIO):
                pl.semaphore_signal(sem, inc=1, device_id=self.far(axis, hop), device_id_type=MESH)
        pl.semaphore_signal(sem, inc=1, device_id=self.peer(), device_id_type=MESH)
        pl.semaphore_wait(sem, 10)

    def _copy(self, src, dst, device):
        i = self.used
        self.used += 1
        c = pltpu.make_async_remote_copy(src_ref=src, dst_ref=dst, send_sem=self.sems[0].at[i], recv_sem=self.sems[1].at[i], device_id=device, device_id_type=MESH)
        c.start()
        return c

    def send(self, src, dst, device):
        c = self._copy(src, dst, device)
        self.sent.append(c)
        return c

    def trade(self, src, dst):
        self.exchanged.append(self._copy(src, dst, self.peer()))

    def local(self, src, dst):
        i = self.used_local
        self.used_local += 1
        c = pltpu.make_async_copy(src, dst, self.sems[2].at[i])
        c.start()
        return c

    def store(self, src, dst):
        self.stored.append(self.local(src, dst))

    def finish(self):
        for c in self.sent:
            c.wait_send()
        for c in self.exchanged:
            c.wait_send()
            c.wait_recv()
        for c in self.stored:
            c.wait()


def pick(ref, sel, cols):
    return ref.at[sel['z'], sel['y'], sel['x'], :, pl.ds(cols[0], cols[1])]


def sem_scratch(remote, local):
    return [pltpu.SemaphoreType.DMA((remote,)), pltpu.SemaphoreType.DMA((remote,)), pltpu.SemaphoreType.DMA((local,))]


def add_into(dst, *srcs):
    def add(idx):
        total = dst[idx]
        for s in srcs:
            total = total + s[idx]
        dst[idx] = total

    if len(dst.shape) > TRIO:
        @pl.loop(0, dst.shape[0])
        def _(i):
            add((i,))
    else:
        add(Ellipsis)


QKV_COLORS = ((0, PAIR, PAIR), (ROWS, PAIR, LANES), (896, LANES, PAIR))
WO_COLORS = ((0, LANES, LANES), (PAIR, LANES, PAIR), (640, PAIR, LANES))
TOKENS = 1024
DIM = 2048
HALF = 1024
QKV = 1280


def scope(name):
    return jax.named_scope(name)


def dot(a, b):
    return jnp.dot(a, b, preferred_element_type=jnp.float32)


def dot_nt(a, b):
    return lax.dot_general(a, b, (((1,), (1,)), ((), ())), preferred_element_type=jnp.float32)


def tile_at(i, n):
    return pl.ds(pl.multiple_of(i * n, n), n)


class Gather:
    def __init__(self, comm, ref, colors, land):
        self.comm, self.ref, self.colors, self.land = comm, ref, colors, land
        self.held = [dict(comm.pos) for _ in colors]

    def parts(self, k):
        lo, na, nb = self.colors[k]
        return (lo, na), (lo + na, nb)

    def move(self, s, cols, to):
        return self.comm.send(pick(self.ref, s, cols), pick(self.ref, s, cols), to)

    def begin(self, phase):
        self.phase, self.first, self.second = phase, [], []
        for k in range(TRIO):
            a, b = self.parts(k)
            d = ORDERS[k][phase]
            up, dn, s = self.comm.far(d, 1), self.comm.far(d, TRIO), self.held[k]
            self.first.append([self.move(s, cols, to) for cols, to in ((a, up), (b, dn), (b, up), (a, dn))])
        if phase == 2:
            for k in range(TRIO):
                for cols in self.parts(k):
                    self.land(self.ref, self.held[k], cols)

    def at(self, k, hop):
        d = ORDERS[k][self.phase]
        return dict(self.held[k], **{d: step(self.comm.pos, d, hop)})

    def forward(self):
        for k in range(TRIO):
            a, b = self.parts(k)
            d = ORDERS[k][self.phase]
            self.first[k][0].wait_recv()
            c = self.move(self.at(k, TRIO), a, self.comm.far(d, 1))
            self.first[k][1].wait_recv()
            self.second.append((c, self.move(self.at(k, 1), b, self.comm.far(d, TRIO))))
            if self.phase == 2:
                self.land(self.ref, self.at(k, TRIO), a)
                self.land(self.ref, self.at(k, 1), b)

    def end(self):
        for k in range(TRIO):
            a, b = self.parts(k)
            d = ORDERS[k][self.phase]
            for c, hop, cols in ((self.first[k][2], TRIO, b), (self.first[k][TRIO], 1, a), (self.second[k][0], 2, a), (self.second[k][1], 2, b)):
                c.wait_recv()
                if self.phase == 2:
                    self.land(self.ref, self.at(k, hop), cols)
            self.held[k] = dict(self.held[k], **{d: ALL})


def head_kernel(hidden, dy, wq, wk, wv, wo, pos, gtile, cos_t, sin_t,
                qt_o, dot_o, k_o, kt_o, v_o, vt_o, rt_o, dyc_o, wqkv_o, wqkvp_o, wo_o, wop_o, gain_o,
                hid2, dy2, dys, rs, rt, wqkv, wout, wpeer, pi, pos2, qt, dot_s, kk, kt, vv, vt, gain, gbuf, gx, gy, gz, *sems):
    comm = Comm(*sems)
    pos_c, core = comm.pos, comm.core
    bf16, f32 = jnp.bfloat16, jnp.float32
    peer = comm.peer()
    rows = tile_at(core, SHARE)
    mine_qkv = wqkv.at[pos_c['z'], pos_c['y'], pos_c['x'], rows]
    mine_wo = wout.at[pos_c['z'], pos_c['y'], pos_c['x'], rows]

    def weight_parts(c):
        return ((wq.at[:, tile_at(c, HALF)], mine_qkv.at[:, pl.ds(0, HALF)]), (wk.at[:, tile_at(c, LANES)], mine_qkv.at[:, pl.ds(HALF, LANES)]),
                (wv.at[:, tile_at(c, LANES)], mine_qkv.at[:, pl.ds(HALF + LANES, LANES)]), (wo.at[:, tile_at(c, HALF)], mine_wo))

    loads = [comm.local(s, d) for s, d in weight_parts(core)]
    load_x = [comm.local(hidden, hid2.at[0]), comm.local(dy, dy2.at[0])]
    with scope('entry'):
        comm.barrier()
    swaps = [comm.send(s, d, peer) for s, d in weight_parts(1 - core)]
    gstage = [comm.send(gtile, gbuf, peer)]
    swap_pos = comm.send(pos, pos2, peer)
    for c in loads:
        c.wait()
    with scope('wait_w'):
        for c in swaps:
            c.wait_recv()

    def land_qkv(ref, s, cols):
        comm.trade(pick(ref, s, cols), pick(wqkvp_o, s, cols))

    arrived = []

    def land_wo(ref, s, cols):
        arrived.append(comm.send(pick(ref, s, cols), pick(wpeer, s, cols), peer))

    g1 = Gather(comm, wqkv, QKV_COLORS, land_qkv)
    g2 = Gather(comm, wout, WO_COLORS, land_wo)
    g1.begin(0)
    g2.begin(0)
    swap_dy = comm.send(dy, dy2.at[1], peer)
    swap_x = comm.send(hidden, hid2.at[1], peer)
    gstage[0].wait_recv()
    gx[0] = gtile[...] + gbuf[...]
    gstage = [comm.send(gx.at[0], gx.at[hop], comm.far('x', hop)) for hop in (1, 2, TRIO)]

    swap_pos.wait_recv()

    @pl.loop(0, TOKENS // LANES)
    def _(i):
        want = lax.broadcasted_iota(jnp.int32, (LANES, ROWS), 0) + i * LANES
        for h, have in enumerate((pos, pos2)):
            pi[tile_at(i, LANES), h * ROWS:(h + 1) * ROWS] = jnp.where(want == have[...], 1.0, 0.0).astype(bf16)

    def sort(dst, src2, first, last):
        with scope('sort'):
            @pl.loop(first, last)
            def _(j):
                c = tile_at(j, PAIR)

                @pl.loop(0, 2)
                def _(i):
                    r = tile_at(i, ROWS)
                    dst[r, c] = (dot(pi[r, :ROWS], src2[0, :, c]) + dot(pi[r, ROWS:], src2[1, :, c])).astype(bf16)

    with scope('p0_fwd'):
        g1.forward()
        g2.forward()
    with scope('wait_dy'):
        load_x[1].wait()
        swap_dy.wait_recv()
    sort(dys, dy2, 0, RING)
    with scope('p0_gain'):
        for c in gstage:
            c.wait_recv()
    gy[pos_c['y']] = (gx[0] + gx[1]) + (gx[2] + gx[TRIO])
    gstage = [comm.send(gy.at[pos_c['y']], gy.at[pos_c['y']], comm.far('y', hop)) for hop in (1, 2, TRIO)]
    with scope('p0_end'):
        g1.end()
        g2.end()
    g1.begin(1)
    g2.begin(1)
    sort(dys, dy2, RING, SUBS)
    with scope('p1_fwd'):
        g1.forward()
        g2.forward()
    comm.store(dys.at[:, tile_at(core, HALF)], dyc_o)
    for c in gstage:
        c.wait_recv()
    for j in range(RING):
        gz[pos_c['z'], j] = gy[j]
    gstage = [comm.send(gz.at[pos_c['z']], gz.at[pos_c['z']], comm.far('z', hop)) for hop in (1, 2, TRIO)]
    with scope('wait_x'):
        load_x[0].wait()
        swap_x.wait_recv()
    sort(rs, hid2, 0, RING)
    with scope('p1_end'):
        g1.end()
        g1.begin(2)
        g2.end()
    sort(rs, hid2, RING, SUBS)
    with scope('gain'):
        for c in gstage:
            c.wait_recv()
    for i in range(RING):
        for j in range(RING):
            gain[:, (i * RING + j) * LANES:(i * RING + j + 1) * LANES] = gz[i, j]
    comm.store(gain, gain_o)

    def norm(first, last):
        with scope('norm'):
            @pl.loop(first, last)
            def _(i):
                r = tile_at(i, CHIP)
                x = rs[r, :].astype(f32)
                inv = lax.rsqrt(jnp.mean(x * x, axis=-1, keepdims=True) + RMS_EPS)
                rs[r, :] = (x * inv * gain[0:1, :]).astype(bf16)

    norm(0, TOKENS // CHIP)
    with scope('p2q_fwd'):
        g1.forward()
    g2.begin(2)
    with scope('r_t'):
        @pl.loop(0, DIM // PAIR)
        def _(i):
            c = tile_at(i, PAIR)

            @pl.loop(0, TOKENS // PAIR)
            def _(j):
                r = tile_at(j, PAIR)
                rt[c, r] = rs[r, c].T
    comm.store(rt, rt_o)
    with scope('p2q_end'):
        g1.end()
    comm.store(wqkv, wqkv_o)
    w2 = wqkv.reshape(DIM, QKV)

    def project(t, i):
        r = tile_at(i, ROWS)
        x = dot(rs[r, :], w2[:, tile_at(t, PAIR)])
        cos, sin = cos_t[:, r], sin_t[:, r]
        cos = jnp.concatenate([cos, cos], axis=0).T
        sin = jnp.concatenate([-sin, sin], axis=0).T
        return r, x, cos, sin

    def rotate(x, cos, sin):
        return x * cos + pltpu.roll(x, 64, 1) * sin

    with scope('kv'):
        @pl.loop(0, 2)
        def _(i):
            r, x, cos, sin = project(RING, i)
            key, val = rotate(x[:, :LANES], cos, sin).astype(bf16), x[:, LANES:].astype(bf16)
            kk[r, :] = key
            kt[:, r] = key.T
            vv[r, :] = val
            vt[:, r] = val.T

    def queries(first, last):
        with scope('q'):
            @pl.loop(first, last)
            def _(t):
                @pl.loop(0, 2)
                def _(i):
                    r, x, cos, sin = project(t, i)
                    for h in range(2):
                        q = rotate(x[:, h * LANES:(h + 1) * LANES], cos, sin).astype(bf16)
                        qt[tile_at(2 * t + h, LANES), r] = q.T

    queries(0, 1)
    with scope('p2o_fwd'):
        g2.forward()
    queries(1, RING)
    for src, dst in ((kk, k_o), (kt, kt_o), (vv, v_o), (vt, vt_o), (qt, qt_o)):
        comm.store(src, dst)
    with scope('p2o_end'):
        g2.end()
    with scope('wo_peer'):
        for c in arrived:
            c.wait_recv()
    comm.store(wout, wo_o)
    comm.store(wpeer, wop_o)
    own, other = wout.reshape(DIM, HALF), wpeer.reshape(DIM, HALF)

    with scope('do_t'):
        @pl.loop(0, TOKENS // PAIR)
        def _(j):
            t = tile_at(j, PAIR)

            @pl.loop(0, 2)
            def _(i):
                r = pl.ds(pl.multiple_of(core * HALF + i * ROWS, ROWS), ROWS)
                acc = dot_nt(own[r, :], dys[t, tile_at(core, HALF)]) + dot_nt(other[r, :], dys[t, tile_at(1 - core, HALF)])
                dot_s[tile_at(i, ROWS), t] = acc.astype(bf16)
    comm.store(dot_s, dot_o)
    with scope('finish'):
        comm.finish()


def head(hidden, dy, wq, wk, wv, wo, pos, gtile, cos_t, sin_t):
    bf16, f32 = jnp.bfloat16, jnp.float32
    any_ = pl.BlockSpec(memory_space=pl.ANY)
    vmem = pl.BlockSpec(memory_space=pltpu.VMEM)
    S = lambda shape, d=bf16: jax.ShapeDtypeStruct(shape, d)
    V = lambda shape, d=bf16: pltpu.VMEM(shape, d)
    w_qkv, w_out = (RING, RING, RING, CHIP, QKV), (RING, RING, RING, CHIP, HALF)
    sq, tall, wide = (HALF, TOKENS), (TOKENS, LANES), (LANES, TOKENS)
    return pl.pallas_call(
        head_kernel,
        out_shape=[S(sq), S(sq), S(tall), S(wide), S(tall), S(wide), S((DIM, TOKENS)), S((TOKENS, HALF)), S(w_qkv), S(w_qkv), S(w_out), S(w_out), S((SUBS, DIM), f32)],
        in_specs=[any_] * 6 + [vmem] * RING,
        out_specs=[any_] * 13,
        scratch_shapes=[V((2, ROWS, DIM)), V((2, ROWS, DIM)), V((TOKENS, DIM)), V((TOKENS, DIM)), V((DIM, TOKENS)), V(w_qkv), V(w_out), V(w_out), V((TOKENS, TOKENS)), V((1, ROWS), jnp.int32),
                        V(sq), V(sq), V(tall), V(wide), V(tall), V(wide), V((SUBS, DIM), f32), V((SUBS, LANES), f32), V((RING, SUBS, LANES), f32), V((RING, SUBS, LANES), f32), V((RING, RING, SUBS, LANES), f32)] + sem_scratch(192, CHIP),
        compiler_params=pltpu.CompilerParams(collective_id=0, has_side_effects=True, vmem_limit_bytes=60 * 2**20),
        name='head',
    )(hidden, dy, wq, wk, wv, wo, pos, gtile, cos_t, sin_t)


HEADS = SUBS
UNIT_K, UNIT_V = SUBS, 9
N_UNITS = 18
SLOTS = RING
LINES = ((0, TRIO, 6, 9, 12, 15), (1, RING, 7, 10, 13, SHARE), (2, 5, SUBS, 11, 14, 17))
COLOR = {u: k for k, line in enumerate(LINES) for u in line}
RANK = {u: i for line in LINES for i, u in enumerate(line)}
PLACE = {**{u: u for u in range(12)}, **{u: u - 12 for u in range(12, SHARE)}, SHARE: 12, 17: 13}
WIRE = (2.9, 0.75, 0.2)
LATENCY = 2.6
STAGE_COST = 0.3


class Plan:
    def __init__(self):
        self.now, self.stage, self.ready, self.order, self.link = 0.0, {}, {}, [], {}
        self.mark = {}

    def _wire(self, u, phase, count):
        link = ORDERS[COLOR[u]][phase]
        arrivals = []
        t = max(self.link.get(link, 0.0), self.now)
        for _ in range(count):
            t += WIRE[phase]
            arrivals.append(t + LATENCY)
        self.link[link] = t
        return arrivals

    def free(self, u, phase):
        i = RANK[u]
        if i < SLOTS:
            return True
        line = LINES[COLOR[u]]
        done = self.mark.get((line[i - SLOTS], 2 * phase + 2))
        return done is not None and any(self.mark.get((j, 2 * phase + 1), -1) > done and (j, 2 * phase + 2) in self.mark for j in line[:i])

    def run(self, u):
        stage = self.stage[u]
        self.order.append((u, stage))
        self.mark[u, stage] = len(self.order)
        self.now = max(self.now, self.ready[u]) + STAGE_COST
        self.stage[u] = stage + 1
        if stage == 6:
            del self.stage[u]
        elif stage % 2:
            self.ready[u] = self._wire(u, stage // 2, 1)[0]
        else:
            self.ready[u] = self._wire(u, stage // 2, 2)[0]

    def blocked(self, u):
        stage = self.stage[u]
        return stage in (0, 2, RING) and not self.free(u, stage // 2)

    def start(self, u):
        self.stage[u], self.ready[u] = 0, self.now

    def due(self):
        first = len(self.order)
        while True:
            ripe = [(self.ready[u], u) for u in self.stage if self.ready[u] <= self.now and not self.blocked(u)]
            if not ripe:
                return self.order[first:]
            self.run(min(ripe)[1])

    def rush(self, units):
        first = len(self.order)
        while any(u in self.stage for u in units):
            self.run(min((self.ready[u], u) for u in self.stage if not self.blocked(u))[1])
        return self.order[first:]


QB = PAIR
NBLK = TOKENS // QB
HALVES = (pl.ds(0, SHARE), pl.ds(SHARE, SHARE))


class Scatter:
    def __init__(self, comm, part, bufs, fin, outs, send_sems, recv_sems, swap_sems):
        self.pos, self.part, self.bufs, self.fin, self.outs = comm.pos, part, bufs, fin, outs
        self.sems, self.swap_sems = (send_sems, recv_sems), swap_sems
        self.near = {(a, hop): comm.far(a, hop) for a in AXES for hop in (1, TRIO)}
        self.hops = {(a, hop): step(comm.pos, a, hop) for a in AXES for hop in (1, 2, TRIO)}
        self.peer, self.core = comm.peer(), comm.core
        self.keep, self.give = tile_at(comm.core, SHARE), tile_at(1 - comm.core, SHARE)
        self.drained = set()

    def sel(self, u, phase, hop):
        order = ORDERS[COLOR[u]]
        s = {a: ALL for a in AXES}
        for a in order[:phase]:
            s[a] = self.pos[a]
        a = order[phase]
        s[a] = self.hops[a, hop] if hop else self.pos[a]
        return s

    def view(self, u, phase, hop, half):
        s = self.sel(u, phase, hop)
        return self.part.at[PLACE[u], s['z'], s['y'], s['x'], HALVES[half], :]

    def buf(self, u, phase, name):
        return self.bufs[phase].at[COLOR[u], RANK[u] % SLOTS, name]

    def copy(self, u, phase, name):
        hop, half, to = ((2, 0, 1), (2, 1, TRIO), (1, 1, 1), (TRIO, 0, TRIO), (1, 0, 1), (TRIO, 1, TRIO))[name]
        i = (u * TRIO + phase) * 6 + name
        return pltpu.make_async_remote_copy(src_ref=self.view(u, phase, hop, half), dst_ref=self.buf(u, phase, name), send_sem=self.sems[0].at[i], recv_sem=self.sems[1].at[i],
                                            device_id=self.near[ORDERS[COLOR[u]][phase], to], device_id_type=MESH)

    def launch(self, u, phase):
        for name in range(RING):
            self.copy(u, phase, name).start()

    def swap(self, u):
        if u < HEADS:
            out, col = self.outs[0], self.core * HALF + u * LANES
        elif u < 10:
            out, col = self.outs[u - 7], self.core * LANES
        else:
            out, col = self.outs[TRIO], self.core * HALF + (u - 10) * LANES
        dst = out.at[:, pl.ds(pl.multiple_of(col, LANES), LANES)]
        give = pltpu.make_async_remote_copy(src_ref=self.fin.at[u, self.give], dst_ref=dst, send_sem=self.swap_sems.at[u], recv_sem=self.swap_sems.at[N_UNITS + u], device_id=self.peer, device_id_type=MESH)
        keep = pltpu.make_async_copy(self.fin.at[u, self.keep], dst, self.swap_sems.at[2 * N_UNITS + u])
        return give, keep

    def run(self, u, stage):
        if stage == 0:
            return self.launch(u, 0)
        phase = (stage - 1) // 2
        if stage % 2:
            for first, hop, half, then in ((0, 1, 0, RING), (1, TRIO, 1, 5)):
                self.copy(u, phase, first).wait_recv()
                add_into(self.view(u, phase, hop, half), self.buf(u, phase, first))
                self.copy(u, phase, then).start()
            return
        for half, names in ((0, (TRIO, RING)), (1, (2, 5))):
            for name in names:
                self.copy(u, phase, name).wait_recv()
            srcs = [self.buf(u, phase, name) for name in names]
            if phase < 2:
                add_into(self.view(u, phase, 0, half), *srcs)
            else:
                self.fin[u, HALVES[half], :] = self.view(u, phase, 0, half)[...] + (srcs[0][...] + srcs[1][...])
        if phase < 2:
            return self.launch(u, phase + 1)
        for c in self.swap(u):
            c.start()

    def drain_sends(self, u):
        self.drained.add(u)
        for phase in range(TRIO):
            for name in range(6):
                self.copy(u, phase, name).wait_send()

    def finish(self):
        for u in range(N_UNITS):
            if u not in self.drained:
                self.drain_sends(u)
            give, keep = self.swap(u)
            give.wait_send()
            give.wait_recv()
            keep.wait()


def attend(head, qt, do_t, k, kt, v, vt, cos, sin, o_rows, ot, dq, dk, dv, s_scr, e_scr, p_scr, d_scr, between):
    f32, bf16 = jnp.float32, jnp.bfloat16
    mine = tile_at(head, LANES)
    below = lax.broadcasted_iota(jnp.int32, (QB, QB), 0) <= lax.broadcasted_iota(jnp.int32, (QB, QB), 1)

    def fold(x, op):
        return op(x.reshape(-1, SUBS, QB), axis=0)

    def scores(j):
        cols, b = slice(j * QB, (j + 1) * QB), j % 2
        q_t = qt[mine, cols]
        top = None
        for c in range(j + 1):
            rows = slice(c * QB, (c + 1) * QB)
            s = dot(k[rows, :], q_t)
            if c == j:
                s = jnp.where(below, s, -jnp.inf)
            s_scr[b, rows, :] = s
            t = fold(s, jnp.max)
            top = t if top is None else jnp.maximum(top, t)
        return jnp.max(top, axis=0, keepdims=True)

    def rest(j, m):
        cols, b, n = slice(j * QB, (j + 1) * QB), j % 2, (j + 1) * QB
        q_t, d_t = qt[mine, cols], do_t[mine, cols]
        tot = None
        for c in range(j + 1):
            rows = slice(c * QB, (c + 1) * QB)
            e = jnp.exp2((s_scr[b, rows, :] - m) * (SCALE * LOG2E))
            s_scr[b, rows, :] = e
            e_scr[b, rows, :] = e.astype(bf16)
            t = fold(e, jnp.sum)
            tot = t if tot is None else tot + t
        den = jnp.sum(tot, axis=0, keepdims=True)
        inv = 1.0 / den
        o = (dot(vt[:, :n], e_scr[b, :n, :]) / den).astype(bf16)
        ot[o_rows, cols] = o
        delta = jnp.sum(d_t.astype(f32) * o.astype(f32), axis=0, keepdims=True)
        for c in range(j + 1):
            rows = slice(c * QB, (c + 1) * QB)
            p = s_scr[b, rows, :] * inv
            p_scr[b, rows, :] = p.astype(bf16)
            d_scr[b, rows, :] = (p * (dot(v[rows, :], d_t) - delta)).astype(bf16)
        dv[:n, :] += dot_nt(p_scr[b, :n, :], d_t)
        dk[:n, :] += dot_nt(d_scr[b, :n, :], q_t)
        g = dot(kt[:, :n], d_scr[b, :n, :]) * SCALE
        co, si = cos[:, cols], sin[:, cols]
        x, y = g[:64], g[64:]
        dq[tile_at(head, LANES), cols] = jnp.concatenate([x * co + y * si, y * co - x * si], axis=0).astype(bf16)

    m = scores(0)
    for j in range(NBLK):
        later = scores(j + 1) if j + 1 < NBLK else None
        rest(j, m)
        m = later
        if j == 2:
            between()


def tail_kernel(qt, do_t, k, kt, v, vt, rt, dyc, wqkv, wqkvp, wo, wop, gain, hidden, dy, pos, cos, sin,
                result, grad_x, gq, gk, gv, go, gout,
                a1, a2, ks, kts, vs, vts, rts, ots, dqo, dqp, dkvo, dkvp, dk, dv, s_scr, e_scr, p_scr, d_scr, dycs, part, buf1, buf2, buf3, fin, pick_rows, onat, dnat, xs, gacc, gpart, gpeer, gz, gy, gx,
                send_sems, recv_sems, swap_sems, trade_send, trade_recv, local_sems):
    comm = Comm(trade_send, trade_recv, local_sems)
    comm.used = 2 * HEADS
    f32, bf16 = jnp.float32, jnp.bfloat16
    core, peer = comm.core, comm.peer()
    sc = Scatter(comm, part, (buf1, buf2, buf3), fin, (gq, gk, gv, go), send_sems, recv_sems, swap_sems)
    plan = Plan()
    loads = [comm.local(s, d) for s, d in ((qt, a1), (do_t, a2), (k, ks), (kt, kts), (v, vs), (vt, vts))]
    load_r = comm.local(rt, rts)
    later = [comm.local(s, d) for s, d in ((dyc, dycs), (hidden, xs))]
    with scope('entry'):
        comm.barrier()
    dk[...] = jnp.zeros_like(dk)
    dv[...] = jnp.zeros_like(dv)
    with scope('wait_q'):
        for c in loads:
            c.wait()

    def emit(stages):
        for u, stage in stages:
            with scope(f'u{u}_s{stage}'):
                sc.run(u, stage)

    def after(cost):
        plan.now += cost
        return plan.due()

    def head_trades(h):
        row = tile_at(core * HEADS + h, LANES)
        mine = tile_at(h, LANES)
        return [pltpu.make_async_remote_copy(src_ref=s, dst_ref=d, send_sem=trade_send.at[i], recv_sem=trade_recv.at[i], device_id=peer, device_id_type=MESH)
                for s, d, i in ((ots.at[row], ots.at[row], h), (dqo.at[mine], dqp.at[mine], HEADS + h))]

    def gradient(place, left, right, mul):
        with scope('grad'):
            @pl.loop(0, RING)
            def _(z):
                g = mul(left[tile_at(z, ROWS), :], right())
                for i in range(2):
                    part[place + i, z] = g[:, i * LANES:(i + 1) * LANES].reshape(RING, RING, CHIP, LANES)

    mid, end, paired = [], [], []
    for h in range(HEADS):
        mid.append(after(2.0))
        end.append(after(1.2))
        if h % 2:
            plan.now += 2.0
            plan.start(h - 1)
            plan.start(h)
            paired.append(plan.due())
        else:
            paired.append([])
    load_r.wait()

    @pl.loop(0, HEADS)
    def _(h):
        def at(table):
            for hh in range(HEADS):
                if table[hh]:
                    pl.when(h == hh)(functools.partial(emit, table[hh]))

        with scope('attend'):
            attend(h, a1, a2, ks, kts, vs, vts, cos, sin, tile_at(core * HEADS + h, LANES), ots, dqo, dk, dv, s_scr, e_scr, p_scr, d_scr, functools.partial(at, mid))
        for c in head_trades(h):
            c.start()
        at(end)

        @pl.when(lax.rem(h, 2) == 1)
        def _():
            gradient(h - 1, rts, lambda: dqo[pl.ds(pl.multiple_of((h - 1) * LANES, PAIR), PAIR), :], dot_nt)
        at(paired)

    def beat(cost, *starts):
        plan.now += cost
        for u in starts:
            plan.start(u)
        emit(plan.due())

    wkv, wkvp = e_scr.reshape(DIM, PAIR), p_scr.reshape(DIM, PAIR)
    later += [comm.local(src.at[:, pl.ds(HALF, PAIR)], dst) for src, dst in ((wqkv, wkv), (wqkvp, wkvp))]
    wo_loads = [comm.local(wo.at[tile_at(i, HALF)], a) for i, a in ((0, a1), (1, a2))]
    key = dk[...] * SCALE
    co, si = jnp.concatenate([cos[...], cos[...]], axis=0).T, jnp.concatenate([sin[...], -sin[...]], axis=0).T
    dkvo[:, :LANES] = (key * co + pltpu.roll(key, 64, 1) * si).astype(bf16)
    dkvo[:, LANES:] = dv[...].astype(bf16)
    comm.trade(dkvo, dkvp)
    gradient(UNIT_K, rts, lambda: dkvo[...], dot)
    beat(2.6, UNIT_K, UNIT_V)
    wq_load = comm.local(wqkv.at[:, pl.ds(0, HALF)], rts)
    for c in later:
        c.wait()
    with scope('trades'):
        for h in range(HEADS):
            for c in head_trades(h):
                c.wait()
    def output_gradient(i):
        first = 10 + 2 * i
        before = [PLACE[u] for u in (first, first + 1) if PLACE[u] < HEADS]
        emit(plan.rush(before))
        for u in before:
            sc.drain_sends(u)
        gradient(PLACE[first], ots, lambda: dycs[:, i * PAIR:(i + 1) * PAIR], dot)
        beat(2.0, first, first + 1)

    output_gradient(0)
    output_gradient(1)

    @pl.loop(0, ROWS // LANES)
    def _(i):
        have = jnp.broadcast_to(pos[0:1, tile_at(i, LANES)].astype(f32), (LANES, LANES)).T
        for c in range(TOKENS // LANES):
            want = (lax.broadcasted_iota(jnp.int32, (LANES, LANES), 1) + c * LANES).astype(f32)
            pick_rows[tile_at(i, LANES), c * LANES:(c + 1) * LANES] = jnp.where(want == have, 1.0, 0.0).astype(bf16)

    def natural(dst, at, src_t, first, last):
        with scope('natural'):
            @pl.loop(first, last)
            def _(i):
                dst[:, pl.ds(pl.multiple_of(at + i * PAIR, PAIR), PAIR)] = dot_nt(pick_rows[...], src_t[tile_at(i, PAIR), :]).astype(bf16)
        beat(0.5 * (last - first))

    natural(onat, 0, ots, 0, RING)
    output_gradient(2)
    natural(onat, 0, ots, RING, SUBS)
    for c in comm.exchanged:
        c.wait_recv()
    natural(dnat, 0, dqo, 0, RING)
    natural(dnat, HALF, dqp, 0, RING)
    output_gradient(TRIO)
    dy_loads = [comm.local(dy.at[:, tile_at(i, HALF)], dycs.at[tile_at(i, ROWS)]) for i in range(2)]
    wqp_load = comm.local(wqkvp.at[:, pl.ds(0, HALF)], ots)
    for i, src in ((2 * HALF, dkvo), (2 * HALF + PAIR, dkvp)):
        dnat[:, i:i + PAIR] = dot(pick_rows[...], src[...]).astype(bf16)
    beat(1.0)
    wq_load.wait()
    wqp_load.wait()
    for c in dy_loads:
        c.wait()
    gacc[...] = jnp.zeros_like(gacc)

    def dr_tile(j):
        if j < RING:
            return (s_scr.at[j // 2, pl.ds(j % 2 * ROWS, ROWS), :],)
        return tuple(part.at[j // 2 + 2].reshape(DIM, LANES).at[pl.ds((j % 2 * 2 + i) * ROWS, ROWS), :] for i in range(2))

    for j in range(SUBS):
        if j == RING:
            emit(plan.rush((RING, 5)))
            sc.drain_sends(RING)
            sc.drain_sends(5)
        with scope('dr'):
            c = slice(j * PAIR, (j + 1) * PAIR)
            acc = dot_nt(dnat[:, :HALF], rts[c, :]) + dot_nt(dnat[:, HALF:2 * HALF], ots[c, :])
            acc = acc + dot_nt(dnat[:, 2 * HALF:2 * HALF + PAIR], wkv[c, :]) + dot_nt(dnat[:, 2 * HALF + PAIR:], wkvp[c, :])
            wide = PAIR // len(dr_tile(j))
            for i, ref in enumerate(dr_tile(j)):
                ref[...] = acc[:, i * wide:(i + 1) * wide]
        beat(0.9)

    def back(first, last):
        with scope('back'):
            @pl.loop(first, last)
            def _(j):
                q = tile_at(j, SHARE)
                d = jnp.concatenate([ref[q, :] for t in range(SUBS) for ref in dr_tile(t)], axis=1)
                x = xs[q, :].astype(f32)
                inv = lax.rsqrt(jnp.mean(x * x, axis=-1, keepdims=True) + RMS_EPS)
                unit = x * inv
                gacc[...] += jnp.sum((d * unit).reshape(2, SUBS, DIM), axis=0)
                dg = d * gain[0:1, :]
                new = inv * (dg - unit * jnp.mean(dg * unit, axis=-1, keepdims=True))
                for half in range(2):
                    r = pl.ds(pl.multiple_of(half * ROWS + j * SHARE, SHARE), SHARE)
                    dycs[r, :] = (dycs[r, :].astype(f32) + new[:, half * HALF:(half + 1) * HALF]).astype(bf16)
        beat(0.1 * (last - first))

    back(0, SHARE)
    back(SHARE, CHIP)
    for i in range(2):
        comm.store(dycs.at[tile_at(i, ROWS)], grad_x.at[:, tile_at(i, HALF)])
    total = jnp.sum(gacc[...], axis=0, keepdims=True)
    gpart[...] = jnp.zeros_like(gpart)
    for i in range(RING):
        for j in range(RING):
            gpart[i, j:j + 1, :] = total[:, (i * RING + j) * LANES:(i * RING + j + 1) * LANES]
    stage = [comm.send(gpart, gpeer, peer)]

    def project_out(col, weights, first, last):
        with scope('project'):
            @pl.loop(first, last)
            def _(i):
                c = tile_at(i, PAIR)
                dst = pl.ds(pl.multiple_of(col + i * PAIR, PAIR), PAIR)
                acc = dot(onat[:, :HALF], weights[0][:, c]) + dot(onat[:, HALF:], weights[1][:, c])
                dnat[:, dst] = (xs[:, dst].astype(f32) + acc).astype(bf16)
        beat(0.7 * (last - first))

    for c in wo_loads:
        c.wait()
    project_out(core * HALF, (a1, a2), 0, 2)
    for c in stage:
        c.wait_recv()
    for j in range(RING):
        gz[j] = gpart[j] + gpeer[j]
    stage = [comm.send(gz.at[step(comm.pos, 'z', hop)], gz.at[TRIO + hop], comm.far('z', hop)) for hop in (1, 2, TRIO)]
    project_out(core * HALF, (a1, a2), 2, RING)
    wo_loads = [comm.local(wop.at[tile_at(i, HALF)], a) for i, a in ((0, a1), (1, a2))]
    for c in stage:
        c.wait_recv()
    gy[0] = (gz[comm.pos['z']] + gz[RING]) + (gz[5] + gz[6])
    stage = [comm.send(gy.at[0], gy.at[hop], comm.far('y', hop)) for hop in (1, 2, TRIO)]
    beat(1.0)
    for c in wo_loads:
        c.wait()
    project_out((1 - core) * HALF, (a1, a2), 0, 2)
    for c in stage:
        c.wait_recv()
    gx[0] = (gy[0] + gy[1]) + (gy[2] + gy[TRIO])
    stage = [comm.send(gx.at[0], gx.at[hop], comm.far('x', hop)) for hop in (1, 2, TRIO)]
    project_out((1 - core) * HALF, (a1, a2), 2, RING)
    comm.store(dnat.at[:, pl.ds(0, DIM)], result)
    for c in stage:
        c.wait_recv()
    gout[...] = (gx[0] + gx[1]) + (gx[2] + gx[TRIO])
    emit(plan.rush(tuple(range(N_UNITS))))
    with scope('finish'):
        sc.finish()
        for c in comm.sent + comm.exchanged:
            c.wait_send()
        for c in comm.stored:
            c.wait()


def tail(qt, do_t, k, kt, v, vt, rt, dyc, wqkv, wqkvp, wo, wop, gain, hidden, dy, pos, cos, sin):
    bf16, f32 = jnp.bfloat16, jnp.float32
    any_ = pl.BlockSpec(memory_space=pl.ANY)
    vmem = pl.BlockSpec(memory_space=pltpu.VMEM)
    S = lambda shape, d=bf16: jax.ShapeDtypeStruct(shape, d)
    V = lambda shape, d=bf16: pltpu.VMEM(shape, d)
    D = lambda n: pltpu.SemaphoreType.DMA((n,))
    sq, tall, wide = (HALF, TOKENS), (TOKENS, LANES), (LANES, TOKENS)
    own = (ROWS, DIM)
    return pl.pallas_call(
        tail_kernel,
        out_shape=[S(own), S(own), S((SHARE, DIM), f32), S((SHARE, PAIR), f32), S((SHARE, PAIR), f32), S((SHARE, DIM), f32), S((SUBS, LANES), f32)],
        in_specs=[any_] * 12 + [vmem] + [any_] * 2 + [vmem] * TRIO,
        out_specs=[any_] * 6 + [vmem],
        scratch_shapes=[V(sq), V(sq), V(tall), V(wide), V(tall), V(wide), V((DIM, TOKENS)), V((DIM, TOKENS)), V(sq), V(sq), V((TOKENS, PAIR)), V((TOKENS, PAIR)), V(tall, f32), V(tall, f32),
                        V((2, TOKENS, QB), f32), V((2, TOKENS, QB)), V((2, TOKENS, QB)), V((2, TOKENS, QB)), V(sq), V((14, RING, RING, RING, CHIP, LANES), f32),
                        V((TRIO, SLOTS, 6, RING, RING, SHARE, LANES), f32), V((TRIO, SLOTS, 6, RING, SHARE, LANES), f32), V((TRIO, SLOTS, 6, SHARE, LANES), f32), V((N_UNITS, CHIP, LANES), f32), V((ROWS, TOKENS)), V(own), V((ROWS, 2 * QKV)), V(own),
                        V((SUBS, DIM), f32), V((RING, SUBS, LANES), f32), V((RING, SUBS, LANES), f32), V((7, SUBS, LANES), f32), V((RING, SUBS, LANES), f32), V((RING, SUBS, LANES), f32),
                        D(N_UNITS * 18), D(N_UNITS * 18), D(TRIO * N_UNITS), D(2 * HEADS + SHARE), D(2 * HEADS + SHARE), D(CHIP)],
        compiler_params=pltpu.CompilerParams(collective_id=1, has_side_effects=True, vmem_limit_bytes=67043328),
        name='tail',
    )(qt, do_t, k, kt, v, vt, rt, dyc, wqkv, wqkvp, wo, wop, gain, hidden, dy, pos, cos, sin)


def rope_tables():
    j = np.arange(HEAD_DIM // 2, dtype=np.float64) / (HEAD_DIM // 2)
    freq = (ROPE_THETA ** -j).astype(np.float32)
    angle = freq[:, None] * np.arange(TOKENS, dtype=np.float32)[None, :]
    return np.cos(angle.astype(np.float64)).astype(np.float32), np.sin(angle.astype(np.float64)).astype(np.float32)


def solution(mesh):
    def shard_fn(hidden, tok_pos, grad_out, norm_gain, w_query, w_key, w_value, w_out):
        f, core = lax.axis_index('fsdp'), lax.axis_index('cp')
        x, y = lax.rem(f, RING), lax.rem(lax.div(f, RING), RING)
        hidden, grad_out = hidden[0], grad_out[0]
        cos_t, sin_t = (jnp.asarray(t) for t in rope_tables())
        lane = jnp.arange(LANES) // SHARE
        gtile = jnp.broadcast_to(jnp.where(lane == x * 2 + core, jnp.tile(norm_gain, SUBS), 0.0), (SUBS, LANES))
        *parts, wqkv, wqkvp, wo, wop, gain = head(hidden, grad_out, w_query, w_key, w_value, w_out, tok_pos, gtile, cos_t, sin_t)
        result, grad_hidden, gq, gk, gv, go, gout = tail(*parts, wqkv.reshape(DIM, QKV), wqkvp.reshape(DIM, QKV), wo.reshape(DIM, HALF), wop.reshape(DIM, HALF), gain, hidden, grad_out, tok_pos, cos_t, sin_t)
        grad_gain = lax.dynamic_slice(gout, (y, x * CHIP + core * SHARE), (1, SHARE)).reshape(SHARE)
        return result[None], grad_hidden[None], gq, gk, gv, go, grad_gain

    row_spec, pos_spec = P('fsdp', 'cp', None), P('fsdp', 'cp')
    weight_spec, gain_spec = P(('fsdp', 'cp'), None), P(('fsdp', 'cp'))
    return jax.shard_map(shard_fn, mesh=mesh, in_specs=(row_spec, pos_spec, row_spec, gain_spec, weight_spec, weight_spec, weight_spec, weight_spec), out_specs=(row_spec, row_spec, weight_spec, weight_spec, weight_spec, weight_spec, gain_spec), check_vma=False)
```

```python
import functools
import jax
import jax.numpy as jnp
import numpy as np
from jax import lax
from jax.experimental import pallas as pl
from jax.experimental.pallas import tpu as pltpu
from jax.sharding import PartitionSpec as P

LANES, SUBS, RING, TRIO = 128, 8, 4, 3
PAIR, ROWS, CHIP, SHARE = 256, 512, 32, 16
HEAD_DIM = LANES
ROPE_THETA = 1000000.0
RMS_EPS = 1e-5
SCALE = HEAD_DIM ** -0.5
LOG2E = 1.4426950408889634

MESH = pl.DeviceIdType.MESH
AXES = ('x', 'y', 'z')
ORDERS = (('x', 'y', 'z'), ('y', 'z', 'x'), ('z', 'x', 'y'))
ALL = pl.ds(0, RING)


def torus():
    f = lax.axis_index('fsdp')
    return {'x': lax.rem(f, RING), 'y': lax.rem(lax.div(f, RING), RING), 'z': lax.div(f, SHARE)}


def step(pos, axis, hop):
    return lax.rem(pos[axis] + hop, RING)


class Comm:
    def __init__(self, send_sems, recv_sems, local_sems):
        self.pos = torus()
        self.core = lax.axis_index('cp')
        self.sems = (send_sems, recv_sems, local_sems)
        self.used = self.used_local = 0
        self.sent, self.exchanged, self.stored = [], [], []

    def far(self, axis, hop):
        p = dict(self.pos)
        p[axis] = step(self.pos, axis, hop)
        return {'fsdp': (p['z'] * RING + p['y']) * RING + p['x'], 'cp': self.core}

    def peer(self):
        return {'fsdp': lax.axis_index('fsdp'), 'cp': 1 - self.core}

    def announce(self):
        sem = pltpu.get_barrier_semaphore()
        for axis in AXES:
            for hop in (1, 2, TRIO):
                pl.semaphore_signal(sem, inc=1, device_id=self.far(axis, hop), device_id_type=MESH)
        pl.semaphore_signal(sem, inc=1, device_id=self.peer(), device_id_type=MESH)

    def meet(self):
        pl.semaphore_wait(pltpu.get_barrier_semaphore(), 10)

    def barrier(self):
        self.announce()
        self.meet()

    def _copy(self, src, dst, device):
        i = self.used
        self.used += 1
        c = pltpu.make_async_remote_copy(src_ref=src, dst_ref=dst, send_sem=self.sems[0].at[i], recv_sem=self.sems[1].at[i], device_id=device, device_id_type=MESH)
        c.start()
        return c

    def send(self, src, dst, device):
        c = self._copy(src, dst, device)
        self.sent.append(c)
        return c

    def trade(self, src, dst):
        self.exchanged.append(self._copy(src, dst, self.peer()))

    def local(self, src, dst):
        i = self.used_local
        self.used_local += 1
        c = pltpu.make_async_copy(src, dst, self.sems[2].at[i])
        c.start()
        return c

    def store(self, src, dst):
        self.stored.append(self.local(src, dst))

    def finish(self):
        for c in self.sent:
            c.wait_send()
        for c in self.exchanged:
            c.wait_send()
            c.wait_recv()
        for c in self.stored:
            c.wait()


def pick(ref, sel, cols):
    return ref.at[sel['z'], sel['y'], sel['x'], :, pl.ds(cols[0], cols[1])]


def sem_scratch(remote, local):
    return [pltpu.SemaphoreType.DMA((remote,)), pltpu.SemaphoreType.DMA((remote,)), pltpu.SemaphoreType.DMA((local,))]


def add_into(dst, *srcs):
    def add(idx):
        total = dst[idx]
        for s in srcs:
            total = total + s[idx]
        dst[idx] = total

    if len(dst.shape) > TRIO:
        @pl.loop(0, dst.shape[0])
        def _(i):
            add((i,))
    else:
        add(Ellipsis)


QK_COLORS = ((0, PAIR, LANES), (384, LANES, PAIR), (768, PAIR, LANES))
VO_COLORS = ((0, LANES, PAIR), (384, PAIR, LANES), (768, LANES, PAIR))
TOKENS = 1024
DIM = 2048
HALF = 1024
QKV = 1280
GROUP = 1152


def scope(name):
    return jax.named_scope(name)


def dot(a, b):
    return jnp.dot(a, b, preferred_element_type=jnp.float32)


def dot_nt(a, b):
    return lax.dot_general(a, b, (((1,), (1,)), ((), ())), preferred_element_type=jnp.float32)


def tile_at(i, n):
    return pl.ds(pl.multiple_of(i * n, n), n)


class Gather:
    def __init__(self, comm, ref, colors, land):
        self.comm, self.ref, self.colors, self.land = comm, ref, colors, land
        self.held = [dict(comm.pos) for _ in colors]

    def parts(self, k):
        lo, na, nb = self.colors[k]
        return (lo, na), (lo + na, nb)

    def move(self, s, cols, to):
        return self.comm.send(pick(self.ref, s, cols), pick(self.ref, s, cols), to)

    def begin(self, phase):
        self.phase, self.first, self.second = phase, [], []
        for k in range(TRIO):
            a, b = self.parts(k)
            d = ORDERS[k][phase]
            up, dn, s = self.comm.far(d, 1), self.comm.far(d, TRIO), self.held[k]
            self.first.append([self.move(s, cols, to) for cols, to in ((a, up), (b, dn), (b, up), (a, dn))])
            if phase == 0:
                across = self.comm.far(d, 2)
                self.second.append([self.move(s, cols, across) for cols in (a, b)])
        if phase == 2:
            for k in range(TRIO):
                for cols in self.parts(k):
                    self.land(self.ref, self.held[k], cols)

    def at(self, k, hop):
        d = ORDERS[k][self.phase]
        return dict(self.held[k], **{d: step(self.comm.pos, d, hop)})

    def forward(self):
        if self.phase == 0:
            return
        for k in range(TRIO):
            a, b = self.parts(k)
            d = ORDERS[k][self.phase]
            self.first[k][0].wait_recv()
            c = self.move(self.at(k, TRIO), a, self.comm.far(d, 1))
            self.first[k][1].wait_recv()
            self.second.append((c, self.move(self.at(k, 1), b, self.comm.far(d, TRIO))))
            if self.phase == 2:
                self.land(self.ref, self.at(k, TRIO), a)
                self.land(self.ref, self.at(k, 1), b)

    def end(self):
        for k in range(TRIO):
            a, b = self.parts(k)
            d = ORDERS[k][self.phase]
            early = [(self.first[k][0], TRIO, a), (self.first[k][1], 1, b)] if self.phase == 0 else []
            for c, hop, cols in early + [(self.first[k][2], TRIO, b), (self.first[k][TRIO], 1, a), (self.second[k][0], 2, a), (self.second[k][1], 2, b)]:
                c.wait_recv()
                if self.phase == 2:
                    self.land(self.ref, self.at(k, hop), cols)
            self.held[k] = dict(self.held[k], **{d: ALL})


def head_kernel(hidden, dy, wq, wk, wv, wo, pos, gain_in, cos_t, sin_t,
                qt_o, dot_o, k_o, kt_o, v_o, vt_o, rt_o, dyc_o, wqk_o, wqkp_o, wvo_o, wvop_o, gain_o,
                hid2, dy2, dys, rs, rt, wqk, wvo, wpeer, pi, pos2, qt, dot_s, kk, kt, vv, vt, gain, gtile, gbuf, gx, gy, gz, *sems):
    comm = Comm(*sems)
    pos_c, core = comm.pos, comm.core
    bf16, f32 = jnp.bfloat16, jnp.float32
    peer = comm.peer()
    rows = tile_at(core, SHARE)
    mine_qk = wqk.at[pos_c['z'], pos_c['y'], pos_c['x'], rows]
    mine_vo = wvo.at[pos_c['z'], pos_c['y'], pos_c['x'], rows]

    def weight_parts(c):
        return ((wq.at[:, tile_at(c, HALF)], mine_qk.at[:, pl.ds(0, HALF)]), (wk.at[:, tile_at(c, LANES)], mine_qk.at[:, pl.ds(HALF, LANES)]),
                (wv.at[:, tile_at(c, LANES)], mine_vo.at[:, pl.ds(0, LANES)]), (wo.at[:, tile_at(c, HALF)], mine_vo.at[:, pl.ds(LANES, HALF)]))

    loads = [comm.local(s, d) for s, d in weight_parts(core)]
    load_x = [comm.local(hidden, hid2.at[pl.ds(0, ROWS)]), comm.local(dy, dy2.at[pl.ds(0, ROWS)])]
    share = lax.broadcasted_iota(jnp.int32, (SUBS, LANES), 1) // SHARE
    gtile[...] = jnp.where(share == pos_c['x'] * 2 + core, jnp.broadcast_to(jnp.concatenate([gain_in[...]] * SUBS, axis=1), (SUBS, LANES)), 0.0)
    with scope('entry'):
        comm.barrier()
    swaps = [comm.send(s, d, peer) for s, d in weight_parts(1 - core)]
    gstage = [comm.send(gtile, gbuf, peer)]
    swap_pos = comm.send(pos, pos2, peer)
    for c in loads:
        c.wait()
    with scope('wait_w'):
        for c in swaps:
            c.wait_recv()

    def land_qk(ref, s, cols):
        comm.trade(pick(ref, s, cols), pick(wqkp_o, s, cols))

    arrived = []

    def land_vo(ref, s, cols):
        arrived.append(comm.send(pick(ref, s, cols), pick(wpeer, s, cols), peer))

    g1 = Gather(comm, wqk, QK_COLORS, land_qk)
    g2 = Gather(comm, wvo, VO_COLORS, land_vo)
    g1.begin(0)
    g2.begin(0)
    swap_dy = comm.send(dy, dy2.at[pl.ds(ROWS, ROWS)], peer)
    gstage[0].wait_recv()
    gx[0] = gtile[...] + gbuf[...]
    gstage = [comm.send(gx.at[0], gx.at[hop], comm.far('x', hop)) for hop in (1, 2, TRIO)]

    swap_pos.wait_recv()

    @pl.loop(0, TOKENS // LANES)
    def _(i):
        want = lax.broadcasted_iota(jnp.int32, (LANES, ROWS), 0) + i * LANES
        for h, have in enumerate((pos, pos2)):
            pi[tile_at(i, LANES), h * ROWS:(h + 1) * ROWS] = jnp.where(want == have[...], 1.0, 0.0).astype(bf16)

    def sort(dst, src, first, last):
        with scope('sort'):
            @pl.loop(first, last)
            def _(j):
                c = tile_at(j, PAIR)
                dst[:, c] = dot(pi[...], src[:, c]).astype(bf16)

    with scope('p0_end'):
        g1.end()
        g2.end()
    g1.begin(1)
    g2.begin(1)
    swap_x = comm.send(hidden, hid2.at[pl.ds(ROWS, ROWS)], peer)
    with scope('p0_gain'):
        for c in gstage:
            c.wait_recv()
    gy[pos_c['y']] = (gx[0] + gx[1]) + (gx[2] + gx[TRIO])
    gstage = [comm.send(gy.at[pos_c['y']], gy.at[pos_c['y']], comm.far('y', hop)) for hop in (1, 2, TRIO)]
    with scope('wait_dy'):
        load_x[1].wait()
        swap_dy.wait_recv()
    sort(dys, dy2, 0, 5)
    with scope('p1_fwd'):
        g1.forward()
        g2.forward()
    for c in gstage:
        c.wait_recv()
    for j in range(RING):
        gz[pos_c['z'], j] = gy[j]
    gstage = [comm.send(gz.at[pos_c['z']], gz.at[pos_c['z']], comm.far('z', hop)) for hop in (1, 2, TRIO)]
    sort(dys, dy2, 5, SUBS)
    comm.store(dys.at[:, tile_at(core, HALF)], dyc_o)
    with scope('p1_end'):
        g1.end()
        g1.begin(2)
        g2.end()
    with scope('wait_x'):
        load_x[0].wait()
        swap_x.wait_recv()
    sort(rs, hid2, 0, SUBS)
    with scope('gain'):
        for c in gstage:
            c.wait_recv()
    for i in range(RING):
        for j in range(RING):
            gain[:, (i * RING + j) * LANES:(i * RING + j + 1) * LANES] = gz[i, j]
    comm.store(gain, gain_o)

    def norm(first, last):
        with scope('norm'):
            @pl.loop(first, last)
            def _(i):
                r = tile_at(i, CHIP)
                x = rs[r, :].astype(f32)
                inv = lax.rsqrt(jnp.mean(x * x, axis=-1, keepdims=True) + RMS_EPS)
                rs[r, :] = (x * inv * gain[0:1, :]).astype(bf16)

    with scope('p2q_fwd'):
        g1.forward()
    g2.begin(2)
    norm(0, TOKENS // CHIP)
    with scope('r_t'):
        @pl.loop(0, DIM // PAIR)
        def _(i):
            c = tile_at(i, PAIR)

            @pl.loop(0, TOKENS // PAIR)
            def _(j):
                r = tile_at(j, PAIR)
                rt[c, r] = rs[r, c].T
    comm.store(rt, rt_o)
    with scope('p2q_end'):
        g1.end()
    comm.store(wqk, wqk_o)
    w_qk, w_vo, w_peer = wqk.reshape(DIM, GROUP), wvo.reshape(DIM, GROUP), wpeer.reshape(DIM, GROUP)

    def rotated(x, r):
        cos, sin = cos_t[:, r], sin_t[:, r]
        cos = jnp.concatenate([cos, cos], axis=0).T
        sin = jnp.concatenate([-sin, sin], axis=0).T
        return (x * cos + pltpu.roll(x, 64, 1) * sin).astype(bf16)

    def queries(first, last):
        with scope('q'):
            @pl.loop(first, last)
            def _(t):
                x = dot(rs[...], w_qk[:, tile_at(t, PAIR)])
                for i in range(RING):
                    r = slice(i * PAIR, (i + 1) * PAIR)
                    for h in range(2):
                        qt[tile_at(2 * t + h, LANES), r] = rotated(x[r, h * LANES:(h + 1) * LANES], r).T

    queries(0, 2)
    with scope('p2o_fwd'):
        g2.forward()
    queries(2, RING)

    @pl.loop(0, 2)
    def _(i):
        r = tile_at(i, ROWS)
        key = rotated(dot(rs[r, :], w_qk[:, HALF:]), r)
        kk[r, :] = key
        kt[:, r] = key.T
    for src, dst in ((kk, k_o), (kt, kt_o), (qt, qt_o)):
        comm.store(src, dst)
    with scope('p2o_end'):
        g2.end()
    with scope('vals'):
        @pl.loop(0, 2)
        def _(i):
            r = tile_at(i, ROWS)
            val = dot(rs[r, :], w_vo[:, :LANES]).astype(bf16)
            vv[r, :] = val
            vt[:, r] = val.T
    for src, dst in ((vv, v_o), (vt, vt_o)):
        comm.store(src, dst)
    with scope('wo_peer'):
        for c in arrived:
            c.wait_recv()
    comm.store(wvo, wvo_o)
    comm.store(wpeer, wvop_o)

    with scope('do_t'):
        r = tile_at(core, HALF)

        @pl.loop(0, TOKENS // PAIR)
        def _(j):
            t = tile_at(j, PAIR)
            w_rows = jnp.concatenate([w_vo[r, LANES:], w_peer[r, LANES:]], axis=1)
            d_rows = jnp.concatenate([dys[t, tile_at(core, HALF)], dys[t, tile_at(1 - core, HALF)]], axis=1)
            dot_s[:, t] = dot_nt(w_rows, d_rows).astype(bf16)
    comm.store(dot_s, dot_o)
    with scope('finish'):
        comm.finish()


def head(hidden, dy, wq, wk, wv, wo, pos, gain, cos_t, sin_t):
    bf16, f32 = jnp.bfloat16, jnp.float32
    any_ = pl.BlockSpec(memory_space=pl.ANY)
    vmem = pl.BlockSpec(memory_space=pltpu.VMEM)
    S = lambda shape, d=bf16: jax.ShapeDtypeStruct(shape, d)
    V = lambda shape, d=bf16: pltpu.VMEM(shape, d)
    group = (RING, RING, RING, CHIP, GROUP)
    sq, tall, wide = (HALF, TOKENS), (TOKENS, LANES), (LANES, TOKENS)
    full = (TOKENS, DIM)
    return pl.pallas_call(
        head_kernel,
        out_shape=[S(sq), S(sq), S(tall), S(wide), S(tall), S(wide), S((DIM, TOKENS)), S((TOKENS, HALF)), S(group), S(group), S(group), S(group), S((SUBS, DIM), f32)],
        in_specs=[any_] * 6 + [vmem] * RING,
        out_specs=[any_] * 13,
        scratch_shapes=[V(full), V(full), V(full), V(full), V((DIM, TOKENS)), V(group), V(group), V(group), V((TOKENS, TOKENS)), V((1, ROWS), jnp.int32),
                        V(sq), V(sq), V(tall), V(wide), V(tall), V(wide), V((SUBS, DIM), f32), V((SUBS, LANES), f32), V((SUBS, LANES), f32), V((RING, SUBS, LANES), f32), V((RING, SUBS, LANES), f32), V((RING, RING, SUBS, LANES), f32)] + sem_scratch(192, CHIP),
        compiler_params=pltpu.CompilerParams(collective_id=0, has_side_effects=True, vmem_limit_bytes=60 * 2**20),
        name='head',
    )(hidden, dy, wq, wk, wv, wo, pos, gain, cos_t, sin_t)


HEADS = SUBS
UNIT_K, UNIT_V = SUBS, 9
N_UNITS = 18
SLOTS = RING
ABREAST = 2
LINES = ((0, TRIO, 6, 9, 12, 15), (1, RING, 7, 10, 13, SHARE), (2, 5, SUBS, 11, 14, 17))
COLOR = {u: k for k, line in enumerate(LINES) for u in line}
RANK = {u: i for line in LINES for i, u in enumerate(line)}
PLACE = {**{u: u for u in range(14)}, **{u: u - 14 for u in range(14, 18)}}
WIRE = (3.2, 0.85, 0.25)
LATENCY = 2.6
STAGE_COST = 0.1


class Plan:
    def __init__(self):
        self.now, self.stage, self.ready, self.order, self.link = 0.0, {}, {}, [], {}
        self.mark = {}

    def _wire(self, u, phase, count):
        link = ORDERS[COLOR[u]][phase]
        arrivals = []
        t = max(self.link.get(link, 0.0), self.now)
        for _ in range(count):
            t += WIRE[phase]
            arrivals.append(t + LATENCY)
        self.link[link] = t
        return arrivals

    def free(self, u, phase):
        i = RANK[u]
        if i < SLOTS:
            return True
        line = LINES[COLOR[u]]
        done = self.mark.get((line[i - SLOTS], 2 * phase + 2))
        return done is not None and any(self.mark.get((j, 2 * phase + 1), -1) > done and (j, 2 * phase + 2) in self.mark for j in line[:i])

    def run(self, u):
        stage = self.stage[u]
        self.order.append((u, stage))
        self.mark[u, stage] = len(self.order)
        self.now = max(self.now, self.ready[u]) + STAGE_COST
        self.stage[u] = stage + 1
        if stage == 6:
            del self.stage[u]
        elif stage % 2:
            self.ready[u] = self._wire(u, stage // 2, 1)[0]
        else:
            self.ready[u] = self._wire(u, stage // 2, 2)[0]

    def blocked(self, u):
        stage = self.stage[u]
        if stage == 0 and sum(0 < self.stage.get(j, 0) <= 2 for j in LINES[COLOR[u]]) >= ABREAST:
            return True
        return stage in (0, 2, RING) and not self.free(u, stage // 2)

    def start(self, u):
        self.stage[u], self.ready[u] = 0, self.now

    def due(self):
        first = len(self.order)
        while True:
            ripe = [(self.ready[u], u) for u in self.stage if self.ready[u] <= self.now and not self.blocked(u)]
            if not ripe:
                return self.order[first:]
            self.run(min(ripe)[1])

    def rush(self, units):
        first = len(self.order)
        while any(u in self.stage for u in units):
            self.run(min((self.ready[u], u) for u in self.stage if not self.blocked(u))[1])
        return self.order[first:]


QB = PAIR
NBLK = TOKENS // QB
HALVES = (pl.ds(0, SHARE), pl.ds(SHARE, SHARE))


class Scatter:
    def __init__(self, comm, part, bufs, fin, outs, send_sems, recv_sems, swap_sems):
        self.pos, self.part, self.bufs, self.fin, self.outs = comm.pos, part, bufs, fin, outs
        self.sems, self.swap_sems = (send_sems, recv_sems), swap_sems
        self.near = {(a, hop): comm.far(a, hop) for a in AXES for hop in (1, TRIO)}
        self.hops = {(a, hop): step(comm.pos, a, hop) for a in AXES for hop in (1, 2, TRIO)}
        self.peer, self.core = comm.peer(), comm.core
        self.keep, self.give = tile_at(comm.core, SHARE), tile_at(1 - comm.core, SHARE)
        self.drained = set()

    def sel(self, u, phase, hop):
        order = ORDERS[COLOR[u]]
        s = {a: ALL for a in AXES}
        for a in order[:phase]:
            s[a] = self.pos[a]
        a = order[phase]
        s[a] = self.hops[a, hop] if hop else self.pos[a]
        return s

    def view(self, u, phase, hop, half):
        s = self.sel(u, phase, hop)
        return self.part.at[PLACE[u], s['z'], s['y'], s['x'], HALVES[half], :]

    def buf(self, u, phase, name):
        return self.bufs[phase].at[COLOR[u], RANK[u] % SLOTS, name]

    def copy(self, u, phase, name):
        hop, half, to = ((2, 0, 1), (2, 1, TRIO), (1, 1, 1), (TRIO, 0, TRIO), (1, 0, 1), (TRIO, 1, TRIO))[name]
        i = (u * TRIO + phase) * 6 + name
        return pltpu.make_async_remote_copy(src_ref=self.view(u, phase, hop, half), dst_ref=self.buf(u, phase, name), send_sem=self.sems[0].at[i], recv_sem=self.sems[1].at[i],
                                            device_id=self.near[ORDERS[COLOR[u]][phase], to], device_id_type=MESH)

    def launch(self, u, phase):
        for name in range(RING):
            self.copy(u, phase, name).start()

    def swap(self, u):
        if u < HEADS:
            out, col = self.outs[0], self.core * HALF + u * LANES
        elif u < 10:
            out, col = self.outs[u - 7], self.core * LANES
        else:
            out, col = self.outs[TRIO], self.core * HALF + (u - 10) * LANES
        dst = out.at[:, pl.ds(pl.multiple_of(col, LANES), LANES)]
        give = pltpu.make_async_remote_copy(src_ref=self.fin.at[u, self.give], dst_ref=dst, send_sem=self.swap_sems.at[u], recv_sem=self.swap_sems.at[N_UNITS + u], device_id=self.peer, device_id_type=MESH)
        keep = pltpu.make_async_copy(self.fin.at[u, self.keep], dst, self.swap_sems.at[2 * N_UNITS + u])
        return give, keep

    def run(self, u, stage):
        if stage == 0:
            return self.launch(u, 0)
        phase = (stage - 1) // 2
        if stage % 2:
            for first, hop, half, then in ((0, 1, 0, RING), (1, TRIO, 1, 5)):
                self.copy(u, phase, first).wait_recv()
                add_into(self.view(u, phase, hop, half), self.buf(u, phase, first))
                self.copy(u, phase, then).start()
            return
        for half, names in ((0, (TRIO, RING)), (1, (2, 5))):
            for name in names:
                self.copy(u, phase, name).wait_recv()
            srcs = [self.buf(u, phase, name) for name in names]
            if phase < 2:
                add_into(self.view(u, phase, 0, half), *srcs)
            else:
                self.fin[u, HALVES[half], :] = self.view(u, phase, 0, half)[...] + (srcs[0][...] + srcs[1][...])
        if phase < 2:
            return self.launch(u, phase + 1)
        for c in self.swap(u):
            c.start()

    def drain_sends(self, u):
        self.drained.add(u)
        for phase in range(TRIO):
            for name in range(6):
                self.copy(u, phase, name).wait_send()

    def finish(self):
        for u in range(N_UNITS):
            if u not in self.drained:
                self.drain_sends(u)
            give, keep = self.swap(u)
            give.wait_send()
            give.wait_recv()
            keep.wait()


def attend(heads, qt, do_t, k, kt, v, vt, cos, sin, o_row, ot, dq, dkt, dvt, s_scr, e_scr, p_scr, d_scr):
    f32, bf16 = jnp.float32, jnp.bfloat16
    strip = 64
    work = [(h, j) for j in range(NBLK) for h in range(len(heads))]

    def strips(c):
        return [(i * strip, slice(c * QB + i * strip, c * QB + (i + 1) * strip)) for i in range(QB // strip)]

    def fold(x, op):
        return op(x.reshape(strip // SUBS, SUBS, QB), axis=0)

    def scores(i):
        (h, j), b = work[i], i % 2
        q_t = qt[heads[h], j * QB:(j + 1) * QB]
        top = jnp.full((SUBS, QB), -jnp.inf, f32)
        for c in range(j + 1):
            tile = dot(k[c * QB:(c + 1) * QB, :], q_t)
            for at, rows in strips(c):
                s = tile[at:at + strip]
                if c == j:
                    seen = lax.broadcasted_iota(jnp.int32, (strip, QB), 0) + at <= lax.broadcasted_iota(jnp.int32, (strip, QB), 1)
                    s = jnp.where(seen, s, -jnp.inf)
                s_scr[b, rows, :] = s
                top = jnp.maximum(top, fold(s, jnp.max))
        return jnp.max(top, axis=0, keepdims=True)

    def rest(i, m):
        (h, j), b = work[i], i % 2
        cols, n = slice(j * QB, (j + 1) * QB), (j + 1) * QB
        q_t, d_t = qt[heads[h], cols], do_t[heads[h], cols]
        tot = jnp.zeros((SUBS, QB), f32)
        for c in range(j + 1):
            for at, rows in strips(c):
                e = jnp.exp2((s_scr[b, rows, :] - m) * (SCALE * LOG2E))
                s_scr[b, rows, :] = e
                e_scr[b, rows, :] = e.astype(bf16)
                tot = tot + fold(e, jnp.sum)
        den = jnp.sum(tot, axis=0, keepdims=True)
        inv = 1.0 / den
        o = (dot(vt[:, :n], e_scr[b, :n, :]) / den).astype(bf16)
        ot[o_row(h), cols] = o
        delta = jnp.sum(d_t.astype(f32) * o.astype(f32), axis=0, keepdims=True)
        for c in range(j + 1):
            dp = dot(v[c * QB:(c + 1) * QB, :], d_t)
            for at, rows in strips(c):
                p = s_scr[b, rows, :] * inv
                p_scr[b, rows, :] = p.astype(bf16)
                d_scr[b, rows, :] = (p * (dp[at:at + strip] - delta)).astype(bf16)
        dvt[:, :n] += dot_nt(d_t, p_scr[b, :n, :])
        dkt[:, :n] += dot_nt(q_t, d_scr[b, :n, :])
        g = dot(kt[:, :n], d_scr[b, :n, :]) * SCALE
        co, si = cos[:, cols], sin[:, cols]
        x, y = g[:64], g[64:]
        dq[heads[h], cols] = jnp.concatenate([x * co + y * si, y * co - x * si], axis=0).astype(bf16)

    m = scores(0)
    for i in range(len(work)):
        later = scores(i + 1) if i + 1 < len(work) else None
        rest(i, m)
        m = later


def tail_kernel(qt, do_t, k, kt, v, vt, rt, dyc, wqk, wqkp, wvo, wvop, gain, hidden, dy, pos, cos, sin,
                result, grad_x, gq, gk, gv, go, gout,
                two, ks, kts, vs, vts, rts, ots, dqo, dqp, dkvo, dkvp, dkt, dvt, s_scr, e_scr, p_scr, d_scr, dycs, part, buf1, buf2, buf3, fin, own, onat, dnat, xs, gacc, gpart, gpeer, gz, gy, gx,
                send_sems, recv_sems, swap_sems, trade_send, trade_recv, local_sems):
    comm = Comm(trade_send, trade_recv, local_sems)
    comm.used = 2 * HEADS
    f32, bf16 = jnp.float32, jnp.bfloat16
    core, peer = comm.core, comm.peer()
    a1, a2 = two.at[0], two.at[1]
    comm.announce()
    sc = Scatter(comm, part, (buf1, buf2, buf3), fin, (gq, gk, gv, go), send_sems, recv_sems, swap_sems)
    plan = Plan()
    loads = [comm.local(s, d) for s, d in ((qt, a1), (do_t, a2), (k, ks), (kt, kts), (v, vs), (vt, vts))]
    load_r = comm.local(rt, rts)
    later = [comm.local(s, d) for s, d in ((dyc, dycs), (hidden, xs))]
    dkt[...] = jnp.zeros_like(dkt)
    dvt[...] = jnp.zeros_like(dvt)

    @pl.loop(0, TOKENS // LANES)
    def _(i):
        want = lax.broadcasted_iota(jnp.int32, (LANES, ROWS), 0) + i * LANES
        own[tile_at(i, LANES), :] = jnp.where(want == pos[...], 1.0, 0.0).astype(bf16)

    with scope('wait_q'):
        for c in loads:
            c.wait()

    def emit(stages):
        for u, stage in stages:
            with scope(f'u{u}_s{stage}'):
                sc.run(u, stage)

    def after(cost):
        plan.now += cost
        return plan.due()

    def head_trades(h):
        row = tile_at(core * HEADS + h, LANES)
        mine = tile_at(h, LANES)
        return [pltpu.make_async_remote_copy(src_ref=s, dst_ref=d, send_sem=trade_send.at[i], recv_sem=trade_recv.at[i], device_id=peer, device_id_type=MESH)
                for s, d, i in ((ots.at[row], ots.at[row], h), (dqo.at[mine], dqp.at[mine], HEADS + h))]

    def gradient(place, left, right, mul):
        with scope('grad'):
            @pl.loop(0, 2)
            def _(z):
                g = mul(left[tile_at(z, HALF), :], right())
                for i in range(2):
                    part[place + i, tile_at(z, 2)] = g[:, i * LANES:(i + 1) * LANES].reshape(2, RING, RING, CHIP, LANES)

    PAIRS = HEADS // 2
    attended, paired = [], []
    for g in range(PAIRS):
        attended.append(after(5.2))
        plan.now += 1.6
        plan.start(2 * g)
        plan.start(2 * g + 1)
        paired.append(plan.due())
    load_r.wait()

    @pl.loop(0, PAIRS)
    def _(g):
        def at(table):
            for i in range(PAIRS):
                if table[i]:
                    pl.when(g == i)(functools.partial(emit, table[i]))

        heads = [tile_at(2 * g + i, LANES) for i in range(2)]
        with scope('attend'):
            attend(heads, a1, a2, ks, kts, vs, vts, cos, sin, lambda i: tile_at(core * HEADS + 2 * g + i, LANES), ots, dqo, dkt, dvt, s_scr, e_scr, p_scr, d_scr)

        @pl.when(g == 0)
        def _():
            with scope('entry'):
                comm.meet()
        for i in range(2):
            for c in head_trades(2 * g + i):
                c.start()
        at(attended)
        gradient(2 * g, rts, lambda: dqo[tile_at(g, PAIR), :], dot_nt)
        at(paired)

    def beat(cost, *starts):
        plan.now += cost
        for u in starts:
            plan.start(u)
        emit(plan.due())

    wkv, wkvp = e_scr.reshape(DIM, PAIR), p_scr.reshape(DIM, PAIR)
    later += [comm.local(src.at[:, pl.ds(at, LANES)], dst.at[:, pl.ds(to, LANES)]) for srcs, dst in (((wqk, wvo), wkv), ((wqkp, wvop), wkvp)) for src, at, to in ((srcs[0], HALF, 0), (srcs[1], 0, LANES))]
    wqp_loads = [comm.local(wqkp.at[tile_at(i, HALF), pl.ds(0, HALF)], two.at[i]) for i in range(2)]
    key = dkt[...] * SCALE
    co, si, x, y = cos[...], sin[...], key[:64], key[64:]
    dkvo[:LANES, :] = jnp.concatenate([x * co + y * si, y * co - x * si], axis=0).astype(bf16)
    dkvo[LANES:, :] = dvt[...].astype(bf16)
    comm.trade(dkvo, dkvp)
    gradient(UNIT_K, rts, lambda: dkvo[...], dot_nt)
    beat(2.0, UNIT_K, UNIT_V)
    wq_load = comm.local(wqk.at[:, pl.ds(0, HALF)], rts)
    for c in later:
        c.wait()
    with scope('trades'):
        for h in range(HEADS):
            for c in head_trades(h):
                c.wait()

    waiting = list(range(RING))

    def output_gradients(force=False):
        while waiting:
            first = 10 + 2 * waiting[0]
            before = [PLACE[u] for u in (first, first + 1) if PLACE[u] < HEADS]
            if force:
                emit(plan.rush(before))
            if any(u in plan.stage for u in before):
                return
            for u in before:
                sc.drain_sends(u)
            i = waiting.pop(0)
            gradient(PLACE[first], ots, lambda: dycs[:, i * PAIR:(i + 1) * PAIR], dot)
            plan.start(first)
            plan.start(first + 1)
            beat(1.5)

    def piece(cost):
        beat(cost)
        output_gradients()

    def unsort(at, src_t, n):
        with scope('unsort'):
            dnat[at:at + n, :] = dot(src_t[:n, :], own[...]).astype(bf16)

    output_gradients()
    for i in range(2):
        with scope('unsort_o'):
            @pl.loop(0, 2)
            def _(j):
                r = pl.ds(pl.multiple_of(i * HALF + j * ROWS, ROWS), ROWS)
                onat[:, r] = dot(ots[r, :], own[...]).astype(bf16).T
        piece(1.4)
    for c in comm.exchanged:
        c.wait_recv()
    unsort(0, dqo, HALF)
    dy_loads = [comm.local(dy.at[:, tile_at(i, HALF)], dqo.at[tile_at(i, ROWS)]) for i in range(2)]
    piece(1.2)
    unsort(HALF, dqp, HALF)
    piece(1.2)
    unsort(2 * HALF, dkvo, PAIR)
    unsort(2 * HALF + PAIR, dkvp, PAIR)
    piece(0.7)
    wq_load.wait()
    for c in wqp_loads + dy_loads:
        c.wait()
    gacc[...] = jnp.zeros_like(gacc)

    def dr_parts(half, r):
        return [s_scr.at[half, r(i * PAIR), :] for i in range(RING)]

    def back(block):
        with scope('dr'):
            @pl.loop(0, 2)
            def _(half):
                c = tile_at(half, HALF)
                left = jnp.concatenate([rts[c, :], two[half], wkv[c, :], wkvp[c, :]], axis=1)
                acc = dot(left, dnat[:, block * PAIR:(block + 1) * PAIR])
                for i, ref in enumerate(dr_parts(half, lambda at: pl.ds(at, PAIR))):
                    ref[...] = acc[i * PAIR:(i + 1) * PAIR, :].T
        piece(3.4)
        with scope('back'):
            @pl.loop(0, SHARE)
            def _(j):
                q = pl.ds(pl.multiple_of(block * PAIR + j * SHARE, SHARE), SHARE)
                d = jnp.concatenate([ref[...] for half in range(2) for ref in dr_parts(half, lambda at: pl.ds(pl.multiple_of(at + j * SHARE, SHARE), SHARE))], axis=1)
                x = xs[q, :].astype(f32)
                inv = lax.rsqrt(jnp.mean(x * x, axis=-1, keepdims=True) + RMS_EPS)
                unit = x * inv
                gacc[...] += jnp.sum((d * unit).reshape(2, SUBS, DIM), axis=0)
                dg = d * gain[0:1, :]
                new = inv * (dg - unit * jnp.mean(dg * unit, axis=-1, keepdims=True))
                for half in range(2):
                    r = pl.ds(pl.multiple_of(half * ROWS + block * PAIR + j * SHARE, SHARE), SHARE)
                    dqo[r, :] = (dqo[r, :].astype(f32) + new[:, half * HALF:(half + 1) * HALF]).astype(bf16)
        piece(3.6)

    back(0)
    back(1)
    wo_loads = [comm.local(wvo.at[:, pl.ds(LANES, HALF)], rts)] + [comm.local(wvop.at[tile_at(i, HALF), pl.ds(LANES, HALF)], two.at[i]) for i in range(2)]
    for i in range(2):
        comm.store(dqo.at[tile_at(i, ROWS)], grad_x.at[:, tile_at(i, HALF)])
    total = jnp.sum(gacc[...], axis=0, keepdims=True)
    gpart[...] = jnp.zeros_like(gpart)
    for i in range(RING):
        for j in range(RING):
            gpart[i, j:j + 1, :] = total[:, (i * RING + j) * LANES:(i * RING + j + 1) * LANES]
    stage = [comm.send(gpart, gpeer, peer)]
    output_gradients(True)

    def project_out(col, weights, i):
        with scope('project'):
            @pl.loop(2 * i, 2 * i + 2)
            def _(j):
                c = tile_at(j, PAIR)
                dst = pl.ds(pl.multiple_of(col + j * PAIR, PAIR), PAIR)
                xs[:, dst] = (xs[:, dst].astype(f32) + dot(onat[...], weights(c))).astype(bf16)
        beat(1.3)

    def own_half(c):
        return rts[:, c]

    def other_half(c):
        return jnp.concatenate([a1[:, c], a2[:, c]], axis=0)

    for c in wo_loads:
        c.wait()
    project_out(core * HALF, own_half, 0)
    for c in stage:
        c.wait_recv()
    for j in range(RING):
        gz[j] = gpart[j] + gpeer[j]
    stage = [comm.send(gz.at[step(comm.pos, 'z', hop)], gz.at[TRIO + hop], comm.far('z', hop)) for hop in (1, 2, TRIO)]
    project_out(core * HALF, own_half, 1)
    for c in stage:
        c.wait_recv()
    gy[0] = (gz[comm.pos['z']] + gz[RING]) + (gz[5] + gz[6])
    stage = [comm.send(gy.at[0], gy.at[hop], comm.far('y', hop)) for hop in (1, 2, TRIO)]
    project_out((1 - core) * HALF, other_half, 0)
    for c in stage:
        c.wait_recv()
    gx[0] = (gy[0] + gy[1]) + (gy[2] + gy[TRIO])
    stage = [comm.send(gx.at[0], gx.at[hop], comm.far('x', hop)) for hop in (1, 2, TRIO)]
    project_out((1 - core) * HALF, other_half, 1)
    comm.store(xs, result)
    for c in stage:
        c.wait_recv()
    gpeer[0] = (gx[0] + gx[1]) + (gx[2] + gx[TRIO])
    mine = jnp.broadcast_to(gpeer[0, pl.ds(comm.pos['y'], 1), :], (SUBS, LANES))
    gout[...] = pltpu.roll(mine, LANES - (comm.pos['x'] * CHIP + core * SHARE), 1)
    emit(plan.rush(tuple(range(N_UNITS))))
    with scope('finish'):
        sc.finish()
        for c in comm.sent + comm.exchanged:
            c.wait_send()
        for c in comm.stored:
            c.wait()


def tail(qt, do_t, k, kt, v, vt, rt, dyc, wqk, wqkp, wvo, wvop, gain, hidden, dy, pos, cos, sin):
    bf16, f32 = jnp.bfloat16, jnp.float32
    any_ = pl.BlockSpec(memory_space=pl.ANY)
    vmem = pl.BlockSpec(memory_space=pltpu.VMEM)
    S = lambda shape, d=bf16: jax.ShapeDtypeStruct(shape, d)
    V = lambda shape, d=bf16: pltpu.VMEM(shape, d)
    D = lambda n: pltpu.SemaphoreType.DMA((n,))
    sq, tall, wide = (HALF, TOKENS), (TOKENS, LANES), (LANES, TOKENS)
    mine, kv = (ROWS, DIM), (PAIR, TOKENS)
    return pl.pallas_call(
        tail_kernel,
        out_shape=[S(mine), S(mine), S((SHARE, DIM), f32), S((SHARE, PAIR), f32), S((SHARE, PAIR), f32), S((SHARE, DIM), f32), S((SUBS, LANES), f32)],
        in_specs=[any_] * 12 + [vmem] + [any_] * 2 + [vmem] * TRIO,
        out_specs=[any_] * 6 + [vmem],
        scratch_shapes=[V((2,) + sq), V(tall), V(wide), V(tall), V(wide), V((DIM, TOKENS)), V((DIM, TOKENS)), V(sq), V(sq), V(kv), V(kv), V(wide, f32), V(wide, f32),
                        V((2, TOKENS, QB), f32), V((2, TOKENS, QB)), V((2, TOKENS, QB)), V((2, TOKENS, QB)), V(sq), V((14, RING, RING, RING, CHIP, LANES), f32),
                        V((TRIO, SLOTS, 6, RING, RING, SHARE, LANES), f32), V((TRIO, SLOTS, 6, RING, SHARE, LANES), f32), V((TRIO, SLOTS, 6, SHARE, LANES), f32), V((N_UNITS, CHIP, LANES), f32), V((TOKENS, ROWS)), V(mine), V((2 * QKV, ROWS)), V(mine),
                        V((SUBS, DIM), f32), V((RING, SUBS, LANES), f32), V((RING, SUBS, LANES), f32), V((7, SUBS, LANES), f32), V((RING, SUBS, LANES), f32), V((RING, SUBS, LANES), f32),
                        D(N_UNITS * 18), D(N_UNITS * 18), D(TRIO * N_UNITS), D(2 * HEADS + SHARE), D(2 * HEADS + SHARE), D(CHIP)],
        compiler_params=pltpu.CompilerParams(collective_id=1, has_side_effects=True, vmem_limit_bytes=67043328),
        name='tail',
    )(qt, do_t, k, kt, v, vt, rt, dyc, wqk, wqkp, wvo, wvop, gain, hidden, dy, pos, cos, sin)


def settle_kernel(*refs):
    n = 7
    ins, outs, bufs, sems = refs[:n], refs[n:2 * n], refs[2 * n:TRIO * n], refs[TRIO * n]
    jobs = []
    for a, o, b in zip(ins, outs, bufs):
        size = a.shape[0] // RING if a.shape[0] == ROWS else a.shape[0]
        jobs += [tuple(r.at[pl.ds(i, size)] for r in (a, b, o)) for i in range(0, a.shape[0], size)]
    takes = [pltpu.make_async_copy(a, b, sems.at[0, i]) for i, (a, b, _) in enumerate(jobs)]
    puts = [pltpu.make_async_copy(b, o, sems.at[1, i]) for i, (_, b, o) in enumerate(jobs)]
    for c in takes:
        c.start()
    for take, put in zip(takes, puts):
        take.wait()
        put.start()
    for c in puts:
        c.wait()


def settle(arrays):
    any_ = pl.BlockSpec(memory_space=pl.ANY)
    return pl.pallas_call(
        settle_kernel,
        out_shape=[jax.ShapeDtypeStruct(a.shape, a.dtype) for a in arrays],
        in_specs=[any_] * len(arrays),
        out_specs=[any_] * len(arrays),
        scratch_shapes=[pltpu.VMEM(a.shape, a.dtype) for a in arrays] + [pltpu.SemaphoreType.DMA((2, SHARE))],
        name='settle',
    )(*arrays)


def rope_tables():
    j = np.arange(HEAD_DIM // 2, dtype=np.float64) / (HEAD_DIM // 2)
    freq = (ROPE_THETA ** -j).astype(np.float32)
    angle = freq[:, None] * np.arange(TOKENS, dtype=np.float32)[None, :]
    return np.cos(angle.astype(np.float64)).astype(np.float32), np.sin(angle.astype(np.float64)).astype(np.float32)


def solution(mesh):
    def shard_fn(hidden, tok_pos, grad_out, norm_gain, w_query, w_key, w_value, w_out):
        hidden, grad_out = hidden[0], grad_out[0]
        cos_t, sin_t = (jnp.asarray(t) for t in rope_tables())
        *parts, gain = head(hidden, grad_out, w_query, w_key, w_value, w_out, tok_pos, norm_gain.reshape(1, SHARE), cos_t, sin_t)
        parts = [p.reshape(DIM, GROUP) if p.ndim > 2 else p for p in parts]
        result, grad_hidden, gq, gk, gv, go, gout = settle(tail(*parts, gain, hidden, grad_out, tok_pos, cos_t, sin_t))
        return result[None], grad_hidden[None], gq, gk, gv, go, gout[0, :SHARE]

    row_spec, pos_spec = P('fsdp', 'cp', None), P('fsdp', 'cp')
    weight_spec, gain_spec = P(('fsdp', 'cp'), None), P(('fsdp', 'cp'))
    return jax.shard_map(shard_fn, mesh=mesh, in_specs=(row_spec, pos_spec, row_spec, gain_spec, weight_spec, weight_spec, weight_spec, weight_spec), out_specs=(row_spec, row_spec, weight_spec, weight_spec, weight_spec, weight_spec, gain_spec), check_vma=False)
```

```python
import functools
import jax
import jax.numpy as jnp
import numpy as np
from jax import lax
from jax.experimental import pallas as pl
from jax.experimental.pallas import tpu as pltpu
from jax.sharding import PartitionSpec as P

LANES, SUBS, RING, TRIO, DUO = 128, 8, 4, 3, 2
PAIR, ROWS, CHIP, SHARE, TURN = 256, 512, 32, 16, 64
HEAD_DIM = LANES
ROPE_THETA = 1000000.0
RMS_EPS = 1e-5
SCALE = HEAD_DIM ** -0.5
LOG2E = 1.4426950408889634

MESH = pl.DeviceIdType.MESH
AXES = ('x', 'y', 'z')
ORDERS = (('x', 'y', 'z'), ('y', 'z', 'x'), ('z', 'x', 'y'))
ALL = pl.ds(0, RING)


def torus():
    f = lax.axis_index('fsdp')
    return {'x': lax.rem(f, RING), 'y': lax.rem(lax.div(f, RING), RING), 'z': lax.div(f, SHARE)}


def step(pos, axis, hop):
    return lax.rem(pos[axis] + hop, RING)


class Batch:
    def __init__(self, comm):
        self.comm, self.index = comm, comm.used
        comm.used += 1

    def _copy(self, src, dst, device):
        send, recv, _ = self.comm.sems
        return pltpu.make_async_remote_copy(src_ref=src, dst_ref=dst, send_sem=send.at[self.index], recv_sem=recv.at[self.index], device_id=device, device_id_type=MESH)

    def send(self, src, dst, device):
        self._copy(src, dst, device).start()
        return self

    def arrived(self, whole):
        self._copy(whole, whole, self.comm.peer()).wait_recv()

    def sent(self, whole):
        self._copy(whole, whole, self.comm.peer()).wait_send()


class Comm:
    def __init__(self, send_sems, recv_sems, local_sems):
        self.pos = torus()
        self.core = lax.axis_index('cp')
        self.sems = (send_sems, recv_sems, local_sems)
        self.used = self.used_local = 0
        self.stored = []

    def far(self, axis, hop):
        p = dict(self.pos)
        p[axis] = step(self.pos, axis, hop)
        return {'fsdp': (p['z'] * RING + p['y']) * RING + p['x'], 'cp': self.core}

    def peer(self):
        return {'fsdp': lax.axis_index('fsdp'), 'cp': 1 - self.core}

    def announce(self):
        sem = pltpu.get_barrier_semaphore()
        for axis in AXES:
            for hop in (1, DUO, TRIO):
                pl.semaphore_signal(sem, inc=1, device_id=self.far(axis, hop), device_id_type=MESH)
        pl.semaphore_signal(sem, inc=1, device_id=self.peer(), device_id_type=MESH)

    def meet(self):
        pl.semaphore_wait(pltpu.get_barrier_semaphore(), 10)

    def ring(self, batch, src, slots, axis):
        for hop in (1, DUO, TRIO):
            batch.send(src, slots.at[hop], self.far(axis, hop))

    def local(self, src, dst):
        i = self.used_local
        self.used_local += 1
        c = pltpu.make_async_copy(src, dst, self.sems[DUO].at[i])
        c.start()
        return c

    def store(self, src, dst):
        self.stored.append(self.local(src, dst))


class OldComm:
    def __init__(self, send_sems, recv_sems, local_sems):
        self.pos = torus()
        self.core = lax.axis_index('cp')
        self.sems = (send_sems, recv_sems, local_sems)
        self.used = self.used_local = 0
        self.sent, self.exchanged, self.stored = [], [], []

    def far(self, axis, hop):
        p = dict(self.pos)
        p[axis] = step(self.pos, axis, hop)
        return {'fsdp': (p['z'] * RING + p['y']) * RING + p['x'], 'cp': self.core}

    def peer(self):
        return {'fsdp': lax.axis_index('fsdp'), 'cp': 1 - self.core}

    def announce(self):
        sem = pltpu.get_barrier_semaphore()
        for axis in AXES:
            for hop in (1, DUO, TRIO):
                pl.semaphore_signal(sem, inc=1, device_id=self.far(axis, hop), device_id_type=MESH)
        pl.semaphore_signal(sem, inc=1, device_id=self.peer(), device_id_type=MESH)

    def meet(self):
        pl.semaphore_wait(pltpu.get_barrier_semaphore(), 10)

    def barrier(self):
        self.announce()
        self.meet()

    def _copy(self, src, dst, device):
        i = self.used
        self.used += 1
        c = pltpu.make_async_remote_copy(src_ref=src, dst_ref=dst, send_sem=self.sems[0].at[i], recv_sem=self.sems[1].at[i], device_id=device, device_id_type=MESH)
        c.start()
        return c

    def send(self, src, dst, device):
        c = self._copy(src, dst, device)
        self.sent.append(c)
        return c

    def trade(self, src, dst):
        self.exchanged.append(self._copy(src, dst, self.peer()))

    def local(self, src, dst):
        i = self.used_local
        self.used_local += 1
        c = pltpu.make_async_copy(src, dst, self.sems[DUO].at[i])
        c.start()
        return c

    def store(self, src, dst):
        self.stored.append(self.local(src, dst))

    def finish(self):
        for c in self.sent:
            c.wait_send()
        for c in self.exchanged:
            c.wait_send()
            c.wait_recv()
        for c in self.stored:
            c.wait()


def pick(ref, sel, cols):
    return ref.at[sel['z'], sel['y'], sel['x'], :, pl.ds(cols[0], cols[1])]


def sem_scratch(remote, local):
    return [pltpu.SemaphoreType.DMA((remote,)), pltpu.SemaphoreType.DMA((remote,)), pltpu.SemaphoreType.DMA((local,))]


def add_into(dst, *srcs, fresh=False):
    def add(idx):
        total, *rest = [s[idx] for s in (srcs if fresh else (dst,) + srcs)]
        for more in rest:
            total = total + more
        dst[idx] = total

    if len(dst.shape) > TRIO:
        @pl.loop(0, dst.shape[0])
        def _(i):
            add((i,))
    else:
        add(Ellipsis)


QK_COLORS = ((0, PAIR, LANES), (384, LANES, PAIR), (768, PAIR, LANES))
VO_COLORS = ((0, LANES, PAIR), (384, PAIR, LANES), (768, LANES, PAIR))
TOKENS = 1024
DIM = 2048
HALF = 1024
QKV = 1280
GROUP = 1152


def scope(name):
    return jax.named_scope(name)


def dot(a, b):
    return jnp.dot(a, b, preferred_element_type=jnp.float32)


def dot_nt(a, b):
    return lax.dot_general(a, b, (((1,), (1,)), ((), ())), preferred_element_type=jnp.float32)


def tile_at(i, n):
    return pl.ds(pl.multiple_of(i * n, n), n)


class Gather:
    def __init__(self, comm, ref, colors, land):
        self.comm, self.ref, self.colors, self.land = comm, ref, colors, land
        self.held = [dict(comm.pos) for _ in colors]
        self.batches = []

    def parts(self, k):
        lo, na, nb = self.colors[k]
        return (lo, na), (lo + na, nb)

    def move(self, batch, s, cols, to):
        batch.send(pick(self.ref, s, cols), pick(self.ref, s, cols), to)

    def at(self, k, hop):
        d = ORDERS[k][self.phase]
        return dict(self.held[k], **{d: step(self.comm.pos, d, hop)})

    def begin(self, phase):
        self.phase = phase
        self.up, self.dn, self.rest = ([Batch(self.comm) for _ in range(TRIO)] for _ in range(TRIO))
        self.batches += self.up + self.dn + self.rest
        for k in range(TRIO):
            a, b = self.parts(k)
            d = ORDERS[k][phase]
            up, dn, s = self.comm.far(d, 1), self.comm.far(d, TRIO), self.held[k]
            self.move(self.up[k], s, a, up)
            self.move(self.dn[k], s, b, dn)
            self.move(self.rest[k], s, b, up)
            self.move(self.rest[k], s, a, dn)
            if phase == 0:
                for cols in (a, b):
                    self.move(self.rest[k], s, cols, self.comm.far(d, DUO))
        if phase == DUO:
            for k in range(TRIO):
                for cols in self.parts(k):
                    self.land(self.ref, self.held[k], cols)

    def forward(self):
        for k in range(TRIO):
            a, b = self.parts(k)
            d = ORDERS[k][self.phase]
            for batch, hop, cols, to in ((self.up[k], TRIO, a, 1), (self.dn[k], 1, b, TRIO)):
                s = self.at(k, hop)
                batch.arrived(pick(self.ref, s, cols))
                if self.phase:
                    self.move(self.rest[k], s, cols, self.comm.far(d, to))
                if self.phase == DUO:
                    self.land(self.ref, s, cols)

    def end(self):
        for k in range(TRIO):
            a, b = self.parts(k)
            d = ORDERS[k][self.phase]
            two = dict(self.held[k], **{d: pl.ds(0, DUO)})
            self.rest[k].arrived(pick(self.ref, two, (a[0], a[1] + b[1])))
            if self.phase == DUO:
                for hop, cols in ((TRIO, b), (1, a), (DUO, a), (DUO, b)):
                    self.land(self.ref, self.at(k, hop), cols)
            for batch, s, cols in ((self.up[k], self.held[k], a), (self.dn[k], self.held[k], b), (self.rest[k], two, (a[0], a[1] + b[1]))):
                batch.spent = pick(self.ref, s, cols)
            self.held[k] = dict(self.held[k], **{d: ALL})

    def finish(self):
        for batch in self.batches:
            batch.sent(batch.spent)


def head_kernel(hidden, dy, wq, wk, wv, wo, pos, gain_in, cos_t, sin_t,
                qt_o, dot_o, k_o, kt_o, v_o, vt_o, rt_o, dyc_o, wqk_o, wqkp_o, wvo_o, wvop_o, gain_o,
                hid2, dy2, dys, rs, rt, wqk, wvo, wpeer, pi, pos2, qt, dot_s, kk, kt, vv, vt, gain, gtile, gbuf, gx, gy, gz, *sems):
    comm = Comm(*sems)
    pos_c, core = comm.pos, comm.core
    bf16, f32 = jnp.bfloat16, jnp.float32
    peer = comm.peer()
    rows = tile_at(core, SHARE)
    mine_qk = wqk.at[pos_c['z'], pos_c['y'], pos_c['x'], rows]
    mine_vo = wvo.at[pos_c['z'], pos_c['y'], pos_c['x'], rows]

    def weight_parts(c):
        return ((wq.at[:, tile_at(c, HALF)], mine_qk.at[:, pl.ds(0, HALF)]), (wk.at[:, tile_at(c, LANES)], mine_qk.at[:, pl.ds(HALF, LANES)]),
                (wv.at[:, tile_at(c, LANES)], mine_vo.at[:, pl.ds(0, LANES)]), (wo.at[:, tile_at(c, HALF)], mine_vo.at[:, pl.ds(LANES, HALF)]))

    loads = [comm.local(s, d) for s, d in weight_parts(core)]
    load_x = [comm.local(hidden, hid2.at[pl.ds(0, ROWS)]), comm.local(dy, dy2.at[pl.ds(0, ROWS)])]
    share = lax.broadcasted_iota(jnp.int32, (SUBS, LANES), 1) // SHARE
    gtile[...] = jnp.where(share == pos_c['x'] * DUO + core, jnp.broadcast_to(jnp.concatenate([gain_in[...]] * SUBS, axis=1), (SUBS, LANES)), 0.0)
    comm.announce()
    with scope('entry'):
        comm.meet()
    swap_w, swap_pos, swap_dy, swap_x, peers_qk, peers_vo = (Batch(comm) for _ in range(6))
    gain_c, gain_x, gain_y, gain_z = (Batch(comm) for _ in range(RING))
    for s, d in weight_parts(1 - core):
        swap_w.send(s, d, peer)
    gain_c.send(gtile, gbuf, peer)
    swap_pos.send(pos, pos2, peer)
    for c in loads:
        c.wait()
    with scope('wait_w'):
        swapped = wqk.at[pos_c['z'], pos_c['y'], pos_c['x']]
        swap_w.arrived(swapped)

    def land_qk(ref, s, cols):
        peers_qk.send(pick(ref, s, cols), pick(wqkp_o, s, cols), peer)

    def land_vo(ref, s, cols):
        peers_vo.send(pick(ref, s, cols), pick(wpeer, s, cols), peer)

    g1 = Gather(comm, wqk, QK_COLORS, land_qk)
    g2 = Gather(comm, wvo, VO_COLORS, land_vo)
    g1.begin(0)
    g2.begin(0)
    swap_dy.send(dy, dy2.at[pl.ds(ROWS, ROWS)], peer)
    gain_c.arrived(gbuf)
    gx[0] = gtile[...] + gbuf[...]
    comm.ring(gain_x, gx.at[0], gx, 'x')

    swap_pos.arrived(pos2)

    @pl.loop(0, TOKENS // LANES)
    def _(i):
        want = lax.broadcasted_iota(jnp.int32, (LANES, ROWS), 0) + i * LANES
        for h, have in enumerate((pos, pos2)):
            pi[tile_at(i, LANES), h * ROWS:(h + 1) * ROWS] = jnp.where(want == have[...], 1.0, 0.0).astype(bf16)

    def sort(dst, src, first, last):
        with scope('sort'):
            @pl.loop(first, last)
            def _(j):
                c = tile_at(j, PAIR)
                dst[:, c] = dot(pi[...], src[:, c]).astype(bf16)

    with scope('p0_end'):
        for g in (g1, g2):
            g.forward()
            g.end()
    g1.begin(1)
    g2.begin(1)
    swap_x.send(hidden, hid2.at[pl.ds(ROWS, ROWS)], peer)
    with scope('p0_gain'):
        gain_x.arrived(gx.at[pl.ds(1, TRIO)])
    gy[pos_c['y']] = (gx[0] + gx[1]) + (gx[DUO] + gx[TRIO])
    for hop in (1, DUO, TRIO):
        gain_y.send(gy.at[pos_c['y']], gy.at[pos_c['y']], comm.far('y', hop))
    with scope('wait_dy'):
        load_x[1].wait()
        swap_dy.arrived(dy2.at[pl.ds(ROWS, ROWS)])
    sort(dys, dy2, 0, 5)
    with scope('p1_fwd'):
        g1.forward()
        g2.forward()
    gain_y.arrived(gy.at[pl.ds(1, TRIO)])
    for j in range(RING):
        gz[pos_c['z'], j] = gy[j]
    for hop in (1, DUO, TRIO):
        gain_z.send(gz.at[pos_c['z']], gz.at[pos_c['z']], comm.far('z', hop))
    sort(dys, dy2, 5, SUBS)
    comm.store(dys.at[:, tile_at(core, HALF)], dyc_o)
    with scope('p1_end'):
        g1.end()
        g1.begin(DUO)
        g2.end()
    with scope('wait_x'):
        load_x[0].wait()
        swap_x.arrived(hid2.at[pl.ds(ROWS, ROWS)])
    sort(rs, hid2, 0, SUBS)
    with scope('gain'):
        gain_z.arrived(gz.at[pl.ds(1, TRIO)])
    for i in range(RING):
        for j in range(RING):
            gain[:, (i * RING + j) * LANES:(i * RING + j + 1) * LANES] = gz[i, j]
    comm.store(gain, gain_o)

    def norm(first, last):
        with scope('norm'):
            @pl.loop(first, last)
            def _(i):
                r = tile_at(i, CHIP)
                x = rs[r, :].astype(f32)
                inv = lax.rsqrt(jnp.mean(x * x, axis=-1, keepdims=True) + RMS_EPS)
                rs[r, :] = (x * inv * gain[0:1, :]).astype(bf16)

    with scope('p2q_fwd'):
        g1.forward()
    g2.begin(DUO)
    norm(0, TOKENS // CHIP)
    with scope('r_t'):
        @pl.loop(0, DIM // PAIR)
        def _(i):
            c = tile_at(i, PAIR)

            @pl.loop(0, TOKENS // PAIR)
            def _(j):
                r = tile_at(j, PAIR)
                rt[c, r] = rs[r, c].T
    comm.store(rt, rt_o)
    with scope('p2q_end'):
        g1.end()
    comm.store(wqk, wqk_o)
    w_qk, w_vo, w_peer = wqk.reshape(DIM, GROUP), wvo.reshape(DIM, GROUP), wpeer.reshape(DIM, GROUP)

    def rotated(x, r):
        cos, sin = cos_t[:, r], sin_t[:, r]
        cos = jnp.concatenate([cos, cos], axis=0).T
        sin = jnp.concatenate([-sin, sin], axis=0).T
        return (x * cos + pltpu.roll(x, TURN, 1) * sin).astype(bf16)

    def queries(first, last):
        with scope('q'):
            @pl.loop(first, last)
            def _(t):
                x = dot(rs[...], w_qk[:, tile_at(t, PAIR)])
                for i in range(RING):
                    r = slice(i * PAIR, (i + 1) * PAIR)
                    for h in range(DUO):
                        qt[tile_at(DUO * t + h, LANES), r] = rotated(x[r, h * LANES:(h + 1) * LANES], r).T

    queries(0, DUO)
    with scope('p2o_fwd'):
        g2.forward()
    queries(DUO, RING)

    @pl.loop(0, DUO)
    def _(i):
        r = tile_at(i, ROWS)
        key = rotated(dot(rs[r, :], w_qk[:, HALF:]), r)
        kk[r, :] = key
        kt[:, r] = key.T
    for src, dst in ((kk, k_o), (kt, kt_o), (qt, qt_o)):
        comm.store(src, dst)
    with scope('p2o_end'):
        g2.end()
    with scope('vals'):
        @pl.loop(0, DUO)
        def _(i):
            r = tile_at(i, ROWS)
            val = dot(rs[r, :], w_vo[:, :LANES]).astype(bf16)
            vv[r, :] = val
            vt[:, r] = val.T
    for src, dst in ((vv, v_o), (vt, vt_o)):
        comm.store(src, dst)
    with scope('wo_peer'):
        peers_vo.arrived(wpeer)
    comm.store(wvo, wvo_o)
    comm.store(wpeer, wvop_o)

    with scope('do_t'):
        r = tile_at(core, HALF)

        @pl.loop(0, TOKENS // PAIR)
        def _(j):
            t = tile_at(j, PAIR)
            w_rows = jnp.concatenate([w_vo[r, LANES:], w_peer[r, LANES:]], axis=1)
            d_rows = jnp.concatenate([dys[t, tile_at(core, HALF)], dys[t, tile_at(1 - core, HALF)]], axis=1)
            dot_s[:, t] = dot_nt(w_rows, d_rows).astype(bf16)
    comm.store(dot_s, dot_o)
    with scope('finish'):
        peers_qk.arrived(wqk)
        for batch, whole in ((swap_w, swapped), (swap_pos, pos2), (swap_dy, dy2.at[pl.ds(ROWS, ROWS)]), (swap_x, hid2.at[pl.ds(ROWS, ROWS)]), (peers_qk, wqk), (peers_vo, wvo),
                             (gain_c, gbuf), (gain_x, gx.at[pl.ds(1, TRIO)]), (gain_y, gy.at[pl.ds(1, TRIO)]), (gain_z, gz.at[pl.ds(1, TRIO)])):
            batch.sent(whole)
        g1.finish()
        g2.finish()
        for c in comm.stored:
            c.wait()


def head(hidden, dy, wq, wk, wv, wo, pos, gain, cos_t, sin_t):
    bf16, f32 = jnp.bfloat16, jnp.float32
    any_ = pl.BlockSpec(memory_space=pl.ANY)
    vmem = pl.BlockSpec(memory_space=pltpu.VMEM)
    S = lambda shape, d=bf16: jax.ShapeDtypeStruct(shape, d)
    V = lambda shape, d=bf16: pltpu.VMEM(shape, d)
    group = (RING, RING, RING, CHIP, GROUP)
    sq, tall, wide = (HALF, TOKENS), (TOKENS, LANES), (LANES, TOKENS)
    full = (TOKENS, DIM)
    return pl.pallas_call(
        head_kernel,
        out_shape=[S(sq), S(sq), S(tall), S(wide), S(tall), S(wide), S((DIM, TOKENS)), S((TOKENS, HALF)), S(group), S(group), S(group), S(group), S((SUBS, DIM), f32)],
        in_specs=[any_] * 6 + [vmem] * RING,
        out_specs=[any_] * 13,
        scratch_shapes=[V(full), V(full), V(full), V(full), V((DIM, TOKENS)), V(group), V(group), V(group), V((TOKENS, TOKENS)), V((1, ROWS), jnp.int32),
                        V(sq), V(sq), V(tall), V(wide), V(tall), V(wide), V((SUBS, DIM), f32), V((SUBS, LANES), f32), V((SUBS, LANES), f32), V((RING, SUBS, LANES), f32), V((RING, SUBS, LANES), f32), V((RING, RING, SUBS, LANES), f32)] + sem_scratch(TURN, 18),
        compiler_params=pltpu.CompilerParams(collective_id=0, has_side_effects=True, vmem_limit_bytes=60 * DUO**20),
        name='head',
    )(hidden, dy, wq, wk, wv, wo, pos, gain, cos_t, sin_t)


HEADS = SUBS
UNIT_K, UNIT_V = SUBS, 9
N_UNITS = 18
SLOTS = RING
ABREAST = DUO
LINES = ((0, TRIO, 6, 9, 12, 15), (1, RING, 7, 10, 13, SHARE), (DUO, 5, SUBS, 11, 14, 17))
COLOR = {u: k for k, line in enumerate(LINES) for u in line}
RANK = {u: i for line in LINES for i, u in enumerate(line)}
PLACE = {**{u: u for u in range(14)}, **{u: u - 14 for u in range(14, 18)}}
WIRE = (3.2, 0.85, 0.25)
LATENCY = 2.6
STAGE_COST = 0.1


class Plan:
    def __init__(self):
        self.now, self.stage, self.ready, self.order, self.link = 0.0, {}, {}, [], {}
        self.mark = {}

    def _wire(self, u, phase, count):
        link = ORDERS[COLOR[u]][phase]
        arrivals = []
        t = max(self.link.get(link, 0.0), self.now)
        for _ in range(count):
            t += WIRE[phase]
            arrivals.append(t + LATENCY)
        self.link[link] = t
        return arrivals

    def free(self, u, phase):
        i = RANK[u]
        if i < SLOTS:
            return True
        line = LINES[COLOR[u]]
        done = self.mark.get((line[i - SLOTS], DUO * phase + DUO))
        return done is not None and any(self.mark.get((j, DUO * phase + 1), -1) > done and (j, DUO * phase + DUO) in self.mark for j in line[:i])

    def run(self, u):
        stage = self.stage[u]
        self.order.append((u, stage))
        self.mark[u, stage] = len(self.order)
        self.now = max(self.now, self.ready[u]) + STAGE_COST
        self.stage[u] = stage + 1
        if stage == 6:
            del self.stage[u]
        elif stage % DUO:
            self.ready[u] = self._wire(u, stage // DUO, 1)[0]
        else:
            self.ready[u] = self._wire(u, stage // DUO, DUO)[0]

    def blocked(self, u):
        stage = self.stage[u]
        if stage == 0 and sum(0 < self.stage.get(j, 0) <= DUO for j in LINES[COLOR[u]]) >= ABREAST:
            return True
        return stage in (0, DUO, RING) and not self.free(u, stage // DUO)

    def start(self, u):
        self.stage[u], self.ready[u] = 0, self.now

    def due(self):
        first = len(self.order)
        while True:
            ripe = [(self.ready[u], u) for u in self.stage if self.ready[u] <= self.now and not self.blocked(u)]
            if not ripe:
                return self.order[first:]
            self.run(min(ripe)[1])

    def rush(self, units):
        first = len(self.order)
        while any(u in self.stage for u in units):
            self.run(min((self.ready[u], u) for u in self.stage if not self.blocked(u))[1])
        return self.order[first:]


QB = PAIR
NBLK = TOKENS // QB
HALVES = (pl.ds(0, SHARE), pl.ds(SHARE, SHARE))


class Scatter:
    def __init__(self, comm, part, bufs, fin, outs, send_sems, recv_sems, swap_sems):
        self.pos, self.part, self.bufs, self.fin, self.outs = comm.pos, part, bufs, fin, outs
        self.sems, self.swap_sems = (send_sems, recv_sems), swap_sems
        self.near = {(a, hop): comm.far(a, hop) for a in AXES for hop in (1, TRIO)}
        self.hops = {(a, hop): step(comm.pos, a, hop) for a in AXES for hop in (1, DUO, TRIO)}
        self.peer, self.core = comm.peer(), comm.core
        self.keep, self.give = tile_at(comm.core, SHARE), tile_at(1 - comm.core, SHARE)
        self.drained = set()

    def sel(self, u, phase, hop):
        order = ORDERS[COLOR[u]]
        s = {a: ALL for a in AXES}
        for a in order[:phase]:
            s[a] = self.pos[a]
        a = order[phase]
        s[a] = self.hops[a, hop] if hop else self.pos[a]
        return s

    def view(self, u, phase, hop, half):
        s = self.sel(u, phase, hop)
        return self.part.at[PLACE[u], s['z'], s['y'], s['x'], HALVES[half], :]

    def buf(self, u, phase, name):
        return self.bufs[phase].at[COLOR[u], RANK[u] % SLOTS, name]

    def copy(self, u, phase, name):
        hop, half, to = ((DUO, 0, 1), (DUO, 1, TRIO), (1, 1, 1), (TRIO, 0, TRIO), (1, 0, 1), (TRIO, 1, TRIO))[name]
        i = (u * TRIO + phase) * 6 + name
        return pltpu.make_async_remote_copy(src_ref=self.view(u, phase, hop, half), dst_ref=self.buf(u, phase, name), send_sem=self.sems[0].at[i], recv_sem=self.sems[1].at[i],
                                            device_id=self.near[ORDERS[COLOR[u]][phase], to], device_id_type=MESH)

    def launch(self, u, phase):
        for name in range(RING):
            self.copy(u, phase, name).start()

    def swap(self, u):
        if u < HEADS:
            out, col = self.outs[0], self.core * HALF + u * LANES
        elif u < 10:
            out, col = self.outs[u - 7], self.core * LANES
        else:
            out, col = self.outs[TRIO], self.core * HALF + (u - 10) * LANES
        dst = out.at[:, pl.ds(pl.multiple_of(col, LANES), LANES)]
        give = pltpu.make_async_remote_copy(src_ref=self.fin.at[u, self.give], dst_ref=dst, send_sem=self.swap_sems.at[u], recv_sem=self.swap_sems.at[N_UNITS + u], device_id=self.peer, device_id_type=MESH)
        keep = pltpu.make_async_copy(self.fin.at[u, self.keep], dst, self.swap_sems.at[DUO * N_UNITS + u])
        return give, keep

    def run(self, u, stage):
        if stage == 0:
            return self.launch(u, 0)
        phase = (stage - 1) // DUO
        if stage % DUO:
            for first, hop, half, then in ((0, 1, 0, RING), (1, TRIO, 1, 5)):
                self.copy(u, phase, first).wait_recv()
                add_into(self.view(u, phase, hop, half), self.buf(u, phase, first))
                self.copy(u, phase, then).start()
            return
        for half, names in ((0, (TRIO, RING)), (1, (DUO, 5))):
            for name in names:
                self.copy(u, phase, name).wait_recv()
            srcs = [self.buf(u, phase, name) for name in names]
            if phase < DUO:
                add_into(self.view(u, phase, 0, half), *srcs)
            else:
                self.fin[u, HALVES[half], :] = self.view(u, phase, 0, half)[...] + (srcs[0][...] + srcs[1][...])
        if phase < DUO:
            return self.launch(u, phase + 1)
        for c in self.swap(u):
            c.start()

    def drain_sends(self, u):
        self.drained.add(u)
        for phase in range(TRIO):
            for name in range(6):
                self.copy(u, phase, name).wait_send()

    def finish(self):
        for u in range(N_UNITS):
            if u not in self.drained:
                self.drain_sends(u)
            give, keep = self.swap(u)
            give.wait_send()
            give.wait_recv()
            keep.wait()


def attend(heads, qt, do_t, k, kt, v, vt, cos, sin, o_row, ot, dq, dkt, dvt, s_scr, e_scr, p_scr, d_scr):
    f32, bf16 = jnp.float32, jnp.bfloat16
    strip = TURN
    work = [(h, j) for j in range(NBLK) for h in range(len(heads))]

    def strips(c):
        return [(i * strip, slice(c * QB + i * strip, c * QB + (i + 1) * strip)) for i in range(QB // strip)]

    def fold(x, op):
        return op(x.reshape(strip // SUBS, SUBS, QB), axis=0)

    def scores(i):
        (h, j), b = work[i], i % DUO
        q_t = qt[heads[h], j * QB:(j + 1) * QB]
        top = jnp.full((SUBS, QB), -jnp.inf, f32)
        for c in range(j + 1):
            tile = dot(k[c * QB:(c + 1) * QB, :], q_t)
            for at, rows in strips(c):
                s = tile[at:at + strip]
                if c == j:
                    seen = lax.broadcasted_iota(jnp.int32, (strip, QB), 0) + at <= lax.broadcasted_iota(jnp.int32, (strip, QB), 1)
                    s = jnp.where(seen, s, -jnp.inf)
                s_scr[b, rows, :] = s
                top = jnp.maximum(top, fold(s, jnp.max))
        return jnp.max(top, axis=0, keepdims=True)

    def rest(i, m):
        (h, j), b = work[i], i % DUO
        cols, n = slice(j * QB, (j + 1) * QB), (j + 1) * QB
        q_t, d_t = qt[heads[h], cols], do_t[heads[h], cols]
        tot = jnp.zeros((SUBS, QB), f32)
        for c in range(j + 1):
            for at, rows in strips(c):
                e = jnp.exp2((s_scr[b, rows, :] - m) * (SCALE * LOG2E))
                s_scr[b, rows, :] = e
                e_scr[b, rows, :] = e.astype(bf16)
                tot = tot + fold(e, jnp.sum)
        den = jnp.sum(tot, axis=0, keepdims=True)
        inv = 1.0 / den
        o = (dot(vt[:, :n], e_scr[b, :n, :]) / den).astype(bf16)
        ot[o_row(h), cols] = o
        delta = jnp.sum(d_t.astype(f32) * o.astype(f32), axis=0, keepdims=True)
        for c in range(j + 1):
            dp = dot(v[c * QB:(c + 1) * QB, :], d_t)
            for at, rows in strips(c):
                p = s_scr[b, rows, :] * inv
                p_scr[b, rows, :] = p.astype(bf16)
                d_scr[b, rows, :] = (p * (dp[at:at + strip] - delta)).astype(bf16)
        dvt[:, :n] += dot_nt(d_t, p_scr[b, :n, :])
        dkt[:, :n] += dot_nt(q_t, d_scr[b, :n, :])
        g = dot(kt[:, :n], d_scr[b, :n, :]) * SCALE
        co, si = cos[:, cols], sin[:, cols]
        x, y = g[:TURN], g[TURN:]
        dq[heads[h], cols] = jnp.concatenate([x * co + y * si, y * co - x * si], axis=0).astype(bf16)

    m = scores(0)
    for i in range(len(work)):
        later = scores(i + 1) if i + 1 < len(work) else None
        rest(i, m)
        m = later


def tail_kernel(qt, do_t, k, kt, v, vt, rt, dyc, wqk, wqkp, wvo, wvop, gain, hidden, dy, pos, cos, sin,
                result, grad_x, gq, gk, gv, go, gout,
                two, ks, kts, vs, vts, rts, ots, dqo, dqp, dkvo, dkvp, dkt, dvt, s_scr, e_scr, p_scr, d_scr, dycs, part, buf1, buf2, buf3, fin, own, onat, dnat, xs, gacc, gpart, gpeer, gz, gy, gx,
                send_sems, recv_sems, swap_sems, trade_send, trade_recv, local_sems):
    comm = OldComm(trade_send, trade_recv, local_sems)
    comm.used = DUO * HEADS
    f32, bf16 = jnp.float32, jnp.bfloat16
    core, peer = comm.core, comm.peer()
    a1, a2 = two.at[0], two.at[1]
    comm.announce()
    sc = Scatter(comm, part, (buf1, buf2, buf3), fin, (gq, gk, gv, go), send_sems, recv_sems, swap_sems)
    plan = Plan()
    loads = [comm.local(s, d) for s, d in ((qt, a1), (do_t, a2), (k, ks), (kt, kts), (v, vs), (vt, vts))]
    load_r = comm.local(rt, rts)
    later = [comm.local(s, d) for s, d in ((dyc, dycs), (hidden, xs))]
    dkt[...] = jnp.zeros_like(dkt)
    dvt[...] = jnp.zeros_like(dvt)

    @pl.loop(0, TOKENS // LANES)
    def _(i):
        want = lax.broadcasted_iota(jnp.int32, (LANES, ROWS), 0) + i * LANES
        own[tile_at(i, LANES), :] = jnp.where(want == pos[...], 1.0, 0.0).astype(bf16)

    with scope('wait_q'):
        for c in loads:
            c.wait()

    def emit(stages):
        for u, stage in stages:
            with scope(f'u{u}_s{stage}'):
                sc.run(u, stage)

    def after(cost):
        plan.now += cost
        return plan.due()

    def head_trades(h):
        row = tile_at(core * HEADS + h, LANES)
        mine = tile_at(h, LANES)
        return [pltpu.make_async_remote_copy(src_ref=s, dst_ref=d, send_sem=trade_send.at[i], recv_sem=trade_recv.at[i], device_id=peer, device_id_type=MESH)
                for s, d, i in ((ots.at[row], ots.at[row], h), (dqo.at[mine], dqp.at[mine], HEADS + h))]

    def gradient(place, left, right, mul):
        with scope('grad'):
            @pl.loop(0, DUO)
            def _(z):
                g = mul(left[tile_at(z, HALF), :], right())
                for i in range(DUO):
                    part[place + i, tile_at(z, DUO)] = g[:, i * LANES:(i + 1) * LANES].reshape(DUO, RING, RING, CHIP, LANES)

    PAIRS = HEADS // DUO
    attended, paired = [], []
    for g in range(PAIRS):
        attended.append(after(5.2))
        plan.now += 1.6
        plan.start(DUO * g)
        plan.start(DUO * g + 1)
        paired.append(plan.due())
    load_r.wait()

    @pl.loop(0, PAIRS)
    def _(g):
        def at(table):
            for i in range(PAIRS):
                if table[i]:
                    pl.when(g == i)(functools.partial(emit, table[i]))

        heads = [tile_at(DUO * g + i, LANES) for i in range(DUO)]
        with scope('attend'):
            attend(heads, a1, a2, ks, kts, vs, vts, cos, sin, lambda i: tile_at(core * HEADS + DUO * g + i, LANES), ots, dqo, dkt, dvt, s_scr, e_scr, p_scr, d_scr)

        @pl.when(g == 0)
        def _():
            with scope('entry'):
                comm.meet()
        for i in range(DUO):
            for c in head_trades(DUO * g + i):
                c.start()
        at(attended)
        gradient(DUO * g, rts, lambda: dqo[tile_at(g, PAIR), :], dot_nt)
        at(paired)

    def beat(cost, *starts):
        plan.now += cost
        for u in starts:
            plan.start(u)
        emit(plan.due())

    wkv, wkvp = e_scr.reshape(DIM, PAIR), p_scr.reshape(DIM, PAIR)
    later += [comm.local(src.at[:, pl.ds(at, LANES)], dst.at[:, pl.ds(to, LANES)]) for srcs, dst in (((wqk, wvo), wkv), ((wqkp, wvop), wkvp)) for src, at, to in ((srcs[0], HALF, 0), (srcs[1], 0, LANES))]
    wqp_loads = [comm.local(wqkp.at[tile_at(i, HALF), pl.ds(0, HALF)], two.at[i]) for i in range(DUO)]
    key = dkt[...] * SCALE
    co, si, x, y = cos[...], sin[...], key[:TURN], key[TURN:]
    dkvo[:LANES, :] = jnp.concatenate([x * co + y * si, y * co - x * si], axis=0).astype(bf16)
    dkvo[LANES:, :] = dvt[...].astype(bf16)
    comm.trade(dkvo, dkvp)
    gradient(UNIT_K, rts, lambda: dkvo[...], dot_nt)
    beat(2.0, UNIT_K, UNIT_V)
    wq_load = comm.local(wqk.at[:, pl.ds(0, HALF)], rts)
    for c in later:
        c.wait()
    with scope('trades'):
        for h in range(HEADS):
            for c in head_trades(h):
                c.wait()

    waiting = list(range(RING))

    def output_gradients(force=False):
        while waiting:
            first = 10 + DUO * waiting[0]
            before = [PLACE[u] for u in (first, first + 1) if PLACE[u] < HEADS]
            if force:
                emit(plan.rush(before))
            if any(u in plan.stage for u in before):
                return
            for u in before:
                sc.drain_sends(u)
            i = waiting.pop(0)
            gradient(PLACE[first], ots, lambda: dycs[:, i * PAIR:(i + 1) * PAIR], dot)
            plan.start(first)
            plan.start(first + 1)
            beat(1.5)

    def piece(cost):
        beat(cost)
        output_gradients()

    def unsort(at, src_t, n):
        with scope('unsort'):
            dnat[at:at + n, :] = dot(src_t[:n, :], own[...]).astype(bf16)

    output_gradients()
    for i in range(DUO):
        with scope('unsort_o'):
            @pl.loop(0, DUO)
            def _(j):
                r = pl.ds(pl.multiple_of(i * HALF + j * ROWS, ROWS), ROWS)
                onat[:, r] = dot(ots[r, :], own[...]).astype(bf16).T
        piece(1.4)
    for c in comm.exchanged:
        c.wait_recv()
    unsort(0, dqo, HALF)
    dy_loads = [comm.local(dy.at[:, tile_at(i, HALF)], dqo.at[tile_at(i, ROWS)]) for i in range(DUO)]
    piece(1.2)
    unsort(HALF, dqp, HALF)
    piece(1.2)
    unsort(DUO * HALF, dkvo, PAIR)
    unsort(DUO * HALF + PAIR, dkvp, PAIR)
    piece(0.7)
    wq_load.wait()
    for c in wqp_loads + dy_loads:
        c.wait()
    gacc[...] = jnp.zeros_like(gacc)

    def dr_parts(half, r):
        return [s_scr.at[half, r(i * PAIR), :] for i in range(RING)]

    def back(block):
        with scope('dr'):
            @pl.loop(0, DUO)
            def _(half):
                c = tile_at(half, HALF)
                left = jnp.concatenate([rts[c, :], two[half], wkv[c, :], wkvp[c, :]], axis=1)
                acc = dot(left, dnat[:, block * PAIR:(block + 1) * PAIR])
                for i, ref in enumerate(dr_parts(half, lambda at: pl.ds(at, PAIR))):
                    ref[...] = acc[i * PAIR:(i + 1) * PAIR, :].T
        piece(3.4)
        with scope('back'):
            @pl.loop(0, SHARE)
            def _(j):
                q = pl.ds(pl.multiple_of(block * PAIR + j * SHARE, SHARE), SHARE)
                d = jnp.concatenate([ref[...] for half in range(DUO) for ref in dr_parts(half, lambda at: pl.ds(pl.multiple_of(at + j * SHARE, SHARE), SHARE))], axis=1)
                x = xs[q, :].astype(f32)
                inv = lax.rsqrt(jnp.mean(x * x, axis=-1, keepdims=True) + RMS_EPS)
                unit = x * inv
                gacc[...] += jnp.sum((d * unit).reshape(DUO, SUBS, DIM), axis=0)
                dg = d * gain[0:1, :]
                new = inv * (dg - unit * jnp.mean(dg * unit, axis=-1, keepdims=True))
                for half in range(DUO):
                    r = pl.ds(pl.multiple_of(half * ROWS + block * PAIR + j * SHARE, SHARE), SHARE)
                    dqo[r, :] = (dqo[r, :].astype(f32) + new[:, half * HALF:(half + 1) * HALF]).astype(bf16)
        piece(3.6)

    back(0)
    back(1)
    wo_loads = [comm.local(wvo.at[:, pl.ds(LANES, HALF)], rts)] + [comm.local(wvop.at[tile_at(i, HALF), pl.ds(LANES, HALF)], two.at[i]) for i in range(DUO)]
    for i in range(DUO):
        comm.store(dqo.at[tile_at(i, ROWS)], grad_x.at[:, tile_at(i, HALF)])
    total = jnp.sum(gacc[...], axis=0, keepdims=True)
    gpart[...] = jnp.zeros_like(gpart)
    for i in range(RING):
        for j in range(RING):
            gpart[i, j:j + 1, :] = total[:, (i * RING + j) * LANES:(i * RING + j + 1) * LANES]
    stage = [comm.send(gpart, gpeer, peer)]
    output_gradients(True)

    def project_out(col, weights, i):
        with scope('project'):
            @pl.loop(DUO * i, DUO * i + DUO)
            def _(j):
                c = tile_at(j, PAIR)
                dst = pl.ds(pl.multiple_of(col + j * PAIR, PAIR), PAIR)
                xs[:, dst] = (xs[:, dst].astype(f32) + dot(onat[...], weights(c))).astype(bf16)
        beat(1.3)

    def own_half(c):
        return rts[:, c]

    def other_half(c):
        return jnp.concatenate([a1[:, c], a2[:, c]], axis=0)

    for c in wo_loads:
        c.wait()
    project_out(core * HALF, own_half, 0)
    for c in stage:
        c.wait_recv()
    for j in range(RING):
        gz[j] = gpart[j] + gpeer[j]
    stage = [comm.send(gz.at[step(comm.pos, 'z', hop)], gz.at[TRIO + hop], comm.far('z', hop)) for hop in (1, DUO, TRIO)]
    project_out(core * HALF, own_half, 1)
    for c in stage:
        c.wait_recv()
    gy[0] = (gz[comm.pos['z']] + gz[RING]) + (gz[5] + gz[6])
    stage = [comm.send(gy.at[0], gy.at[hop], comm.far('y', hop)) for hop in (1, DUO, TRIO)]
    project_out((1 - core) * HALF, other_half, 0)
    for c in stage:
        c.wait_recv()
    gx[0] = (gy[0] + gy[1]) + (gy[DUO] + gy[TRIO])
    stage = [comm.send(gx.at[0], gx.at[hop], comm.far('x', hop)) for hop in (1, DUO, TRIO)]
    project_out((1 - core) * HALF, other_half, 1)
    comm.store(xs, result)
    for c in stage:
        c.wait_recv()
    gpeer[0] = (gx[0] + gx[1]) + (gx[DUO] + gx[TRIO])
    mine = jnp.broadcast_to(gpeer[0, pl.ds(comm.pos['y'], 1), :], (SUBS, LANES))
    gout[...] = pltpu.roll(mine, LANES - (comm.pos['x'] * CHIP + core * SHARE), 1)
    emit(plan.rush(tuple(range(N_UNITS))))
    with scope('finish'):
        sc.finish()
        for c in comm.sent + comm.exchanged:
            c.wait_send()
        for c in comm.stored:
            c.wait()


def tail(qt, do_t, k, kt, v, vt, rt, dyc, wqk, wqkp, wvo, wvop, gain, hidden, dy, pos, cos, sin):
    bf16, f32 = jnp.bfloat16, jnp.float32
    any_ = pl.BlockSpec(memory_space=pl.ANY)
    vmem = pl.BlockSpec(memory_space=pltpu.VMEM)
    S = lambda shape, d=bf16: jax.ShapeDtypeStruct(shape, d)
    V = lambda shape, d=bf16: pltpu.VMEM(shape, d)
    D = lambda n: pltpu.SemaphoreType.DMA((n,))
    sq, tall, wide = (HALF, TOKENS), (TOKENS, LANES), (LANES, TOKENS)
    mine, kv = (ROWS, DIM), (PAIR, TOKENS)
    return pl.pallas_call(
        tail_kernel,
        out_shape=[S(mine), S(mine), S((SHARE, DIM), f32), S((SHARE, PAIR), f32), S((SHARE, PAIR), f32), S((SHARE, DIM), f32), S((SUBS, LANES), f32)],
        in_specs=[any_] * 12 + [vmem] + [any_] * DUO + [vmem] * TRIO,
        out_specs=[any_] * 6 + [vmem],
        scratch_shapes=[V((DUO,) + sq), V(tall), V(wide), V(tall), V(wide), V((DIM, TOKENS)), V((DIM, TOKENS)), V(sq), V(sq), V(kv), V(kv), V(wide, f32), V(wide, f32),
                        V((DUO, TOKENS, QB), f32), V((DUO, TOKENS, QB)), V((DUO, TOKENS, QB)), V((DUO, TOKENS, QB)), V(sq), V((14, RING, RING, RING, CHIP, LANES), f32),
                        V((TRIO, SLOTS, 6, RING, RING, SHARE, LANES), f32), V((TRIO, SLOTS, 6, RING, SHARE, LANES), f32), V((TRIO, SLOTS, 6, SHARE, LANES), f32), V((N_UNITS, CHIP, LANES), f32), V((TOKENS, ROWS)), V(mine), V((DUO * QKV, ROWS)), V(mine),
                        V((SUBS, DIM), f32), V((RING, SUBS, LANES), f32), V((RING, SUBS, LANES), f32), V((7, SUBS, LANES), f32), V((RING, SUBS, LANES), f32), V((RING, SUBS, LANES), f32),
                        D(N_UNITS * 18), D(N_UNITS * 18), D(TRIO * N_UNITS), D(DUO * HEADS + SHARE), D(DUO * HEADS + SHARE), D(CHIP)],
        compiler_params=pltpu.CompilerParams(collective_id=1, has_side_effects=True, vmem_limit_bytes=67043328),
        name='tail',
    )(qt, do_t, k, kt, v, vt, rt, dyc, wqk, wqkp, wvo, wvop, gain, hidden, dy, pos, cos, sin)


def settle_kernel(n, *refs):
    ins, gain, outs, gain_out, bufs, sems = refs[:n], refs[n], refs[n + 1:DUO * n + 1], refs[DUO * n + 1], refs[DUO * n + DUO:-1], refs[-1]
    jobs = []
    for a, o, b in zip(ins, outs, bufs):
        size = a.shape[0] // RING if a.shape[0] == ROWS else a.shape[0]
        jobs += [tuple(r.at[pl.ds(i, size)] for r in (a, b, o)) for i in range(0, a.shape[0], size)]
    takes = [pltpu.make_async_copy(a, b, sems.at[0, i]) for i, (a, b, _) in enumerate(jobs)]
    puts = [pltpu.make_async_copy(b, o, sems.at[1, i]) for i, (_, b, o) in enumerate(jobs)]
    for c in takes:
        c.start()
    gain_out[...] = gain[0:1, :SHARE]
    for take, put in zip(takes, puts):
        take.wait()
        put.start()
    for c in puts:
        c.wait()


def settle(*arrays):
    *large, gain = arrays
    any_, vmem = pl.BlockSpec(memory_space=pl.ANY), pl.BlockSpec(memory_space=pltpu.VMEM)
    return pl.pallas_call(
        functools.partial(settle_kernel, len(large)),
        out_shape=[jax.ShapeDtypeStruct(a.shape, a.dtype) for a in large] + [jax.ShapeDtypeStruct((1, SHARE), gain.dtype)],
        in_specs=[any_] * len(large) + [vmem],
        out_specs=[any_] * len(large) + [vmem],
        scratch_shapes=[pltpu.VMEM(a.shape, a.dtype) for a in large] + [pltpu.SemaphoreType.DMA((DUO, 12))],
        name='settle',
    )(*arrays)


def rope_tables():
    j = np.arange(HEAD_DIM // DUO, dtype=np.float64) / (HEAD_DIM // DUO)
    freq = (ROPE_THETA ** -j).astype(np.float32)
    angle = freq[:, None] * np.arange(TOKENS, dtype=np.float32)[None, :]
    return np.cos(angle.astype(np.float64)).astype(np.float32), np.sin(angle.astype(np.float64)).astype(np.float32)


def solution(mesh):
    def shard_fn(hidden, tok_pos, grad_out, norm_gain, w_query, w_key, w_value, w_out):
        hidden, grad_out = hidden[0], grad_out[0]
        cos_t, sin_t = (jnp.asarray(t) for t in rope_tables())
        *parts, gain = head(hidden, grad_out, w_query, w_key, w_value, w_out, tok_pos, norm_gain.reshape(1, SHARE), cos_t, sin_t)
        parts = [p.reshape(DIM, GROUP) if p.ndim > DUO else p for p in parts]
        result, grad_hidden, gq, gk, gv, go, gout = settle(*tail(*parts, gain, hidden, grad_out, tok_pos, cos_t, sin_t))
        return result[None], grad_hidden[None], gq, gk, gv, go, gout.reshape(SHARE)

    row_spec, pos_spec = P('fsdp', 'cp', None), P('fsdp', 'cp')
    weight_spec, gain_spec = P(('fsdp', 'cp'), None), P(('fsdp', 'cp'))
    return jax.shard_map(shard_fn, mesh=mesh, in_specs=(row_spec, pos_spec, row_spec, gain_spec, weight_spec, weight_spec, weight_spec, weight_spec), out_specs=(row_spec, row_spec, weight_spec, weight_spec, weight_spec, weight_spec, gain_spec), check_vma=False)
```

```python
import functools
import jax
import jax.numpy as jnp
import numpy as np
from jax import lax
from jax.experimental import pallas as pl
from jax.experimental.pallas import tpu as pltpu
from jax.sharding import PartitionSpec as P

LANES, SUBS, RING, TRIO, DUO = 128, 8, 4, 3, 2
PAIR, ROWS, CHIP, SHARE, TURN = 256, 512, 32, 16, 64
HEAD_DIM = LANES
ROPE_THETA = 1000000.0
RMS_EPS = 1e-5
SCALE = HEAD_DIM ** -0.5
LOG2E = 1.4426950408889634

MESH = pl.DeviceIdType.MESH
AXES = ('x', 'y', 'z')
ORDERS = (('x', 'y', 'z'), ('y', 'z', 'x'), ('z', 'x', 'y'))
ALL = pl.ds(0, RING)


def torus():
    f = lax.axis_index('fsdp')
    return {'x': lax.rem(f, RING), 'y': lax.rem(lax.div(f, RING), RING), 'z': lax.div(f, SHARE)}


def step(pos, axis, hop):
    return lax.rem(pos[axis] + hop, RING)


class Batch:
    def __init__(self, comm):
        self.comm, self.index = comm, comm.used
        comm.used += 1

    def _copy(self, src, dst, device):
        send, recv, _ = self.comm.sems
        return pltpu.make_async_remote_copy(src_ref=src, dst_ref=dst, send_sem=send.at[self.index], recv_sem=recv.at[self.index], device_id=device, device_id_type=MESH)

    def send(self, src, dst, device):
        self._copy(src, dst, device).start()
        return self

    def arrived(self, whole):
        self._copy(whole, whole, self.comm.peer()).wait_recv()

    def sent(self, whole):
        self._copy(whole, whole, self.comm.peer()).wait_send()


class Comm:
    def __init__(self, send_sems, recv_sems, local_sems):
        self.pos = torus()
        self.core = lax.axis_index('cp')
        self.sems = (send_sems, recv_sems, local_sems)
        self.used = self.used_local = 0
        self.stored = []

    def far(self, axis, hop):
        p = dict(self.pos)
        p[axis] = step(self.pos, axis, hop)
        return {'fsdp': (p['z'] * RING + p['y']) * RING + p['x'], 'cp': self.core}

    def peer(self):
        return {'fsdp': lax.axis_index('fsdp'), 'cp': 1 - self.core}

    def announce(self):
        sem = pltpu.get_barrier_semaphore()
        for axis in AXES:
            for hop in (1, DUO, TRIO):
                pl.semaphore_signal(sem, inc=1, device_id=self.far(axis, hop), device_id_type=MESH)
        pl.semaphore_signal(sem, inc=1, device_id=self.peer(), device_id_type=MESH)

    def meet(self):
        pl.semaphore_wait(pltpu.get_barrier_semaphore(), 10)

    def ring(self, batch, src, slots, axis):
        for hop in (1, DUO, TRIO):
            batch.send(src, slots.at[hop], self.far(axis, hop))

    def local(self, src, dst):
        i = self.used_local
        self.used_local += 1
        c = pltpu.make_async_copy(src, dst, self.sems[DUO].at[i])
        c.start()
        return c

    def store(self, src, dst):
        self.stored.append(self.local(src, dst))


class OldComm:
    def __init__(self, send_sems, recv_sems, local_sems):
        self.pos = torus()
        self.core = lax.axis_index('cp')
        self.sems = (send_sems, recv_sems, local_sems)
        self.used = self.used_local = 0
        self.sent, self.exchanged, self.stored = [], [], []

    def far(self, axis, hop):
        p = dict(self.pos)
        p[axis] = step(self.pos, axis, hop)
        return {'fsdp': (p['z'] * RING + p['y']) * RING + p['x'], 'cp': self.core}

    def peer(self):
        return {'fsdp': lax.axis_index('fsdp'), 'cp': 1 - self.core}

    def announce(self):
        sem = pltpu.get_barrier_semaphore()
        for axis in AXES:
            for hop in (1, DUO, TRIO):
                pl.semaphore_signal(sem, inc=1, device_id=self.far(axis, hop), device_id_type=MESH)
        pl.semaphore_signal(sem, inc=1, device_id=self.peer(), device_id_type=MESH)

    def meet(self):
        pl.semaphore_wait(pltpu.get_barrier_semaphore(), 10)

    def barrier(self):
        self.announce()
        self.meet()

    def _copy(self, src, dst, device):
        i = self.used
        self.used += 1
        c = pltpu.make_async_remote_copy(src_ref=src, dst_ref=dst, send_sem=self.sems[0].at[i], recv_sem=self.sems[1].at[i], device_id=device, device_id_type=MESH)
        c.start()
        return c

    def send(self, src, dst, device):
        c = self._copy(src, dst, device)
        self.sent.append(c)
        return c

    def trade(self, src, dst):
        self.exchanged.append(self._copy(src, dst, self.peer()))

    def local(self, src, dst):
        i = self.used_local
        self.used_local += 1
        c = pltpu.make_async_copy(src, dst, self.sems[DUO].at[i])
        c.start()
        return c

    def store(self, src, dst):
        self.stored.append(self.local(src, dst))

    def finish(self):
        for c in self.sent:
            c.wait_send()
        for c in self.exchanged:
            c.wait_send()
            c.wait_recv()
        for c in self.stored:
            c.wait()


def pick(ref, sel, cols):
    return ref.at[sel['z'], sel['y'], sel['x'], :, pl.ds(cols[0], cols[1])]


def sem_scratch(remote, local):
    return [pltpu.SemaphoreType.DMA((remote,)), pltpu.SemaphoreType.DMA((remote,)), pltpu.SemaphoreType.DMA((local,))]


def add_into(dst, *srcs, fresh=False):
    def add(idx):
        total, *rest = [s[idx] for s in (srcs if fresh else (dst,) + srcs)]
        for more in rest:
            total = total + more
        dst[idx] = total

    if len(dst.shape) > TRIO:
        @pl.loop(0, dst.shape[0])
        def _(i):
            add((i,))
    else:
        add(Ellipsis)


QK_COLORS = ((0, PAIR, LANES), (384, LANES, PAIR), (768, PAIR, LANES))
VO_COLORS = ((0, LANES, PAIR), (384, PAIR, LANES), (768, LANES, PAIR))
TOKENS = 1024
DIM = 2048
HALF = 1024
QKV = 1280
GROUP = 1152


def scope(name):
    return jax.named_scope(name)


def dot(a, b):
    return jnp.dot(a, b, preferred_element_type=jnp.float32)


def dot_nt(a, b):
    return lax.dot_general(a, b, (((1,), (1,)), ((), ())), preferred_element_type=jnp.float32)


def tile_at(i, n):
    return pl.ds(pl.multiple_of(i * n, n), n)


class Gather:
    def __init__(self, comm, ref, colors, land):
        self.comm, self.ref, self.colors, self.land = comm, ref, colors, land
        self.held = [dict(comm.pos) for _ in colors]
        self.batches = []

    def parts(self, k):
        lo, na, nb = self.colors[k]
        return (lo, na), (lo + na, nb)

    def move(self, batch, s, cols, to):
        batch.send(pick(self.ref, s, cols), pick(self.ref, s, cols), to)

    def at(self, k, hop):
        d = ORDERS[k][self.phase]
        return dict(self.held[k], **{d: step(self.comm.pos, d, hop)})

    def begin(self, phase):
        self.phase = phase
        self.up, self.dn, self.rest = ([Batch(self.comm) for _ in range(TRIO)] for _ in range(TRIO))
        self.batches += self.up + self.dn + self.rest
        for k in range(TRIO):
            a, b = self.parts(k)
            d = ORDERS[k][phase]
            up, dn, s = self.comm.far(d, 1), self.comm.far(d, TRIO), self.held[k]
            self.move(self.up[k], s, a, up)
            self.move(self.dn[k], s, b, dn)
            self.move(self.rest[k], s, b, up)
            self.move(self.rest[k], s, a, dn)
            if phase == 0:
                for cols in (a, b):
                    self.move(self.rest[k], s, cols, self.comm.far(d, DUO))
        if phase == DUO:
            for k in range(TRIO):
                for cols in self.parts(k):
                    self.land(self.ref, self.held[k], cols)

    def forward(self):
        for k in range(TRIO):
            a, b = self.parts(k)
            d = ORDERS[k][self.phase]
            for batch, hop, cols, to in ((self.up[k], TRIO, a, 1), (self.dn[k], 1, b, TRIO)):
                s = self.at(k, hop)
                batch.arrived(pick(self.ref, s, cols))
                if self.phase:
                    self.move(self.rest[k], s, cols, self.comm.far(d, to))
                if self.phase == DUO:
                    self.land(self.ref, s, cols)

    def end(self):
        for k in range(TRIO):
            a, b = self.parts(k)
            d = ORDERS[k][self.phase]
            two = dict(self.held[k], **{d: pl.ds(0, DUO)})
            self.rest[k].arrived(pick(self.ref, two, (a[0], a[1] + b[1])))
            if self.phase == DUO:
                for hop, cols in ((TRIO, b), (1, a), (DUO, a), (DUO, b)):
                    self.land(self.ref, self.at(k, hop), cols)
            for batch, s, cols in ((self.up[k], self.held[k], a), (self.dn[k], self.held[k], b), (self.rest[k], two, (a[0], a[1] + b[1]))):
                batch.spent = pick(self.ref, s, cols)
            self.held[k] = dict(self.held[k], **{d: ALL})

    def finish(self):
        for batch in self.batches:
            batch.sent(batch.spent)


def head_kernel(hidden, dy, wq, wk, wv, wo, pos, gain_in, cos_t, sin_t,
                qt_o, dot_o, k_o, kt_o, v_o, vt_o, rt_o, dyc_o, wqk_o, wqkp_o, wvo_o, wvop_o, gain_o,
                hid2, dy2, dys, rs, rt, wqk, wvo, wpeer, pi, pos2, qt, dot_s, kk, kt, vv, vt, gain, gtile, gbuf, gx, gy, gz, *sems):
    comm = Comm(*sems)
    pos_c, core = comm.pos, comm.core
    bf16, f32 = jnp.bfloat16, jnp.float32
    peer = comm.peer()
    rows = tile_at(core, SHARE)
    mine_qk = wqk.at[pos_c['z'], pos_c['y'], pos_c['x'], rows]
    mine_vo = wvo.at[pos_c['z'], pos_c['y'], pos_c['x'], rows]

    def weight_parts(c):
        return ((wq.at[:, tile_at(c, HALF)], mine_qk.at[:, pl.ds(0, HALF)]), (wk.at[:, tile_at(c, LANES)], mine_qk.at[:, pl.ds(HALF, LANES)]),
                (wv.at[:, tile_at(c, LANES)], mine_vo.at[:, pl.ds(0, LANES)]), (wo.at[:, tile_at(c, HALF)], mine_vo.at[:, pl.ds(LANES, HALF)]))

    loads = [comm.local(s, d) for s, d in weight_parts(core)]
    load_x = [comm.local(hidden, hid2.at[pl.ds(0, ROWS)]), comm.local(dy, dy2.at[pl.ds(0, ROWS)])]
    share = lax.broadcasted_iota(jnp.int32, (SUBS, LANES), 1) // SHARE
    gtile[...] = jnp.where(share == pos_c['x'] * DUO + core, jnp.broadcast_to(jnp.concatenate([gain_in[...]] * SUBS, axis=1), (SUBS, LANES)), 0.0)
    comm.announce()
    with scope('entry'):
        comm.meet()
    swap_w, swap_pos, swap_dy, swap_x, peers_qk, peers_vo = (Batch(comm) for _ in range(6))
    gain_c, gain_x, gain_y, gain_z = (Batch(comm) for _ in range(RING))
    for s, d in weight_parts(1 - core):
        swap_w.send(s, d, peer)
    gain_c.send(gtile, gbuf, peer)
    swap_pos.send(pos, pos2, peer)
    for c in loads:
        c.wait()
    with scope('wait_w'):
        swapped = wqk.at[pos_c['z'], pos_c['y'], pos_c['x']]
        swap_w.arrived(swapped)

    def land_qk(ref, s, cols):
        peers_qk.send(pick(ref, s, cols), pick(wqkp_o, s, cols), peer)

    def land_vo(ref, s, cols):
        peers_vo.send(pick(ref, s, cols), pick(wpeer, s, cols), peer)

    g1 = Gather(comm, wqk, QK_COLORS, land_qk)
    g2 = Gather(comm, wvo, VO_COLORS, land_vo)
    g1.begin(0)
    g2.begin(0)
    swap_dy.send(dy, dy2.at[pl.ds(ROWS, ROWS)], peer)
    gain_c.arrived(gbuf)
    gx[0] = gtile[...] + gbuf[...]
    comm.ring(gain_x, gx.at[0], gx, 'x')

    swap_pos.arrived(pos2)

    @pl.loop(0, TOKENS // LANES)
    def _(i):
        want = lax.broadcasted_iota(jnp.int32, (LANES, ROWS), 0) + i * LANES
        for h, have in enumerate((pos, pos2)):
            pi[tile_at(i, LANES), h * ROWS:(h + 1) * ROWS] = jnp.where(want == have[...], 1.0, 0.0).astype(bf16)

    def sort(dst, src, first, last):
        with scope('sort'):
            @pl.loop(first, last)
            def _(j):
                c = tile_at(j, PAIR)
                dst[:, c] = dot(pi[...], src[:, c]).astype(bf16)

    with scope('p0_end'):
        for g in (g1, g2):
            g.forward()
            g.end()
    g1.begin(1)
    g2.begin(1)
    swap_x.send(hidden, hid2.at[pl.ds(ROWS, ROWS)], peer)
    with scope('p0_gain'):
        gain_x.arrived(gx.at[pl.ds(1, TRIO)])
    gy[pos_c['y']] = (gx[0] + gx[1]) + (gx[DUO] + gx[TRIO])
    for hop in (1, DUO, TRIO):
        gain_y.send(gy.at[pos_c['y']], gy.at[pos_c['y']], comm.far('y', hop))
    with scope('wait_dy'):
        load_x[1].wait()
        swap_dy.arrived(dy2.at[pl.ds(ROWS, ROWS)])
    sort(dys, dy2, 0, 5)
    with scope('p1_fwd'):
        g1.forward()
        g2.forward()
    gain_y.arrived(gy.at[pl.ds(1, TRIO)])
    for j in range(RING):
        gz[pos_c['z'], j] = gy[j]
    for hop in (1, DUO, TRIO):
        gain_z.send(gz.at[pos_c['z']], gz.at[pos_c['z']], comm.far('z', hop))
    sort(dys, dy2, 5, SUBS)
    comm.store(dys.at[:, tile_at(core, HALF)], dyc_o)
    with scope('p1_end'):
        g1.end()
        g1.begin(DUO)
        g2.end()
    with scope('wait_x'):
        load_x[0].wait()
        swap_x.arrived(hid2.at[pl.ds(ROWS, ROWS)])
    sort(rs, hid2, 0, SUBS)
    with scope('gain'):
        gain_z.arrived(gz.at[pl.ds(1, TRIO)])
    for i in range(RING):
        for j in range(RING):
            gain[:, (i * RING + j) * LANES:(i * RING + j + 1) * LANES] = gz[i, j]
    comm.store(gain, gain_o)

    def norm(first, last):
        with scope('norm'):
            @pl.loop(first, last)
            def _(i):
                r = tile_at(i, CHIP)
                x = rs[r, :].astype(f32)
                inv = lax.rsqrt(jnp.mean(x * x, axis=-1, keepdims=True) + RMS_EPS)
                rs[r, :] = (x * inv * gain[0:1, :]).astype(bf16)

    with scope('p2q_fwd'):
        g1.forward()
    g2.begin(DUO)
    norm(0, TOKENS // CHIP)
    with scope('r_t'):
        @pl.loop(0, DIM // PAIR)
        def _(i):
            c = tile_at(i, PAIR)

            @pl.loop(0, TOKENS // PAIR)
            def _(j):
                r = tile_at(j, PAIR)
                rt[c, r] = rs[r, c].T
    comm.store(rt, rt_o)
    with scope('p2q_end'):
        g1.end()
    comm.store(wqk, wqk_o)
    w_qk, w_vo, w_peer = wqk.reshape(DIM, GROUP), wvo.reshape(DIM, GROUP), wpeer.reshape(DIM, GROUP)

    def rotated(x, r):
        cos, sin = cos_t[:, r], sin_t[:, r]
        cos = jnp.concatenate([cos, cos], axis=0).T
        sin = jnp.concatenate([-sin, sin], axis=0).T
        return (x * cos + pltpu.roll(x, TURN, 1) * sin).astype(bf16)

    def queries(first, last):
        with scope('q'):
            @pl.loop(first, last)
            def _(t):
                x = dot(rs[...], w_qk[:, tile_at(t, PAIR)])
                for i in range(RING):
                    r = slice(i * PAIR, (i + 1) * PAIR)
                    for h in range(DUO):
                        qt[tile_at(DUO * t + h, LANES), r] = rotated(x[r, h * LANES:(h + 1) * LANES], r).T

    queries(0, DUO)
    with scope('p2o_fwd'):
        g2.forward()
    queries(DUO, RING)

    @pl.loop(0, DUO)
    def _(i):
        r = tile_at(i, ROWS)
        key = rotated(dot(rs[r, :], w_qk[:, HALF:]), r)
        kk[r, :] = key
        kt[:, r] = key.T
    for src, dst in ((kk, k_o), (kt, kt_o), (qt, qt_o)):
        comm.store(src, dst)
    with scope('p2o_end'):
        g2.end()
    with scope('vals'):
        @pl.loop(0, DUO)
        def _(i):
            r = tile_at(i, ROWS)
            val = dot(rs[r, :], w_vo[:, :LANES]).astype(bf16)
            vv[r, :] = val
            vt[:, r] = val.T
    for src, dst in ((vv, v_o), (vt, vt_o)):
        comm.store(src, dst)
    with scope('wo_peer'):
        peers_vo.arrived(wpeer)
    comm.store(wvo, wvo_o)
    comm.store(wpeer, wvop_o)

    with scope('do_t'):
        r = tile_at(core, HALF)

        @pl.loop(0, TOKENS // PAIR)
        def _(j):
            t = tile_at(j, PAIR)
            w_rows = jnp.concatenate([w_vo[r, LANES:], w_peer[r, LANES:]], axis=1)
            d_rows = jnp.concatenate([dys[t, tile_at(core, HALF)], dys[t, tile_at(1 - core, HALF)]], axis=1)
            dot_s[:, t] = dot_nt(w_rows, d_rows).astype(bf16)
    comm.store(dot_s, dot_o)
    with scope('finish'):
        peers_qk.arrived(wqk)
        for batch, whole in ((swap_w, swapped), (swap_pos, pos2), (swap_dy, dy2.at[pl.ds(ROWS, ROWS)]), (swap_x, hid2.at[pl.ds(ROWS, ROWS)]), (peers_qk, wqk), (peers_vo, wvo),
                             (gain_c, gbuf), (gain_x, gx.at[pl.ds(1, TRIO)]), (gain_y, gy.at[pl.ds(1, TRIO)]), (gain_z, gz.at[pl.ds(1, TRIO)])):
            batch.sent(whole)
        g1.finish()
        g2.finish()
        for c in comm.stored:
            c.wait()


def head(hidden, dy, wq, wk, wv, wo, pos, gain, cos_t, sin_t):
    bf16, f32 = jnp.bfloat16, jnp.float32
    any_ = pl.BlockSpec(memory_space=pl.ANY)
    vmem = pl.BlockSpec(memory_space=pltpu.VMEM)
    S = lambda shape, d=bf16: jax.ShapeDtypeStruct(shape, d)
    V = lambda shape, d=bf16: pltpu.VMEM(shape, d)
    group = (RING, RING, RING, CHIP, GROUP)
    sq, tall, wide = (HALF, TOKENS), (TOKENS, LANES), (LANES, TOKENS)
    full = (TOKENS, DIM)
    return pl.pallas_call(
        head_kernel,
        out_shape=[S(sq), S(sq), S(tall), S(wide), S(tall), S(wide), S((DIM, TOKENS)), S((TOKENS, HALF)), S(group), S(group), S(group), S(group), S((SUBS, DIM), f32)],
        in_specs=[any_] * 6 + [vmem] * RING,
        out_specs=[any_] * 13,
        scratch_shapes=[V(full), V(full), V(full), V(full), V((DIM, TOKENS)), V(group), V(group), V(group), V((TOKENS, TOKENS)), V((1, ROWS), jnp.int32),
                        V(sq), V(sq), V(tall), V(wide), V(tall), V(wide), V((SUBS, DIM), f32), V((SUBS, LANES), f32), V((SUBS, LANES), f32), V((RING, SUBS, LANES), f32), V((RING, SUBS, LANES), f32), V((RING, RING, SUBS, LANES), f32)] + sem_scratch(TURN, 18),
        compiler_params=pltpu.CompilerParams(collective_id=0, has_side_effects=True, vmem_limit_bytes=60 * DUO**20),
        name='head',
    )(hidden, dy, wq, wk, wv, wo, pos, gain, cos_t, sin_t)


HEADS = SUBS
UNIT_K, UNIT_V = SUBS, 9
N_UNITS = 18
SLOTS = RING
LAST = 5
ABREAST = DUO
LINES = ((0, TRIO, 6, 9, 12, 15), (1, RING, 7, 10, 13, SHARE), (DUO, 5, SUBS, 11, 14, 17))
COLOR = {u: k for k, line in enumerate(LINES) for u in line}
RANK = {u: i for line in LINES for i, u in enumerate(line)}
BEFORE = {u: line[i - SLOTS] if i >= SLOTS else None for line in LINES for i, u in enumerate(line)}
PLACES = 12
PLACE = {u: u % PLACES for u in range(N_UNITS)}
WIRE = (2.85, 0.72, 0.36)
LATENCY = 2.6
STAGE_COST = 0.1


class Plan:
    def __init__(self):
        self.now, self.stage, self.ready, self.order, self.link = 0.0, {}, {}, [], {}
        self.mark = {}

    def _wire(self, u, phase, count):
        link = ORDERS[COLOR[u]][phase]
        t = max(self.link.get(link, 0.0), self.now)
        first = t + WIRE[phase] + LATENCY
        self.link[link] = t + WIRE[phase] * count
        return first if phase < DUO else self.link[link] + LATENCY

    def free(self, u, phase):
        if BEFORE[u] is None:
            return True
        done = self.mark.get((BEFORE[u], (DUO, RING, 5)[phase]))
        if done is None:
            return False
        sent = ((0, 1), (DUO, TRIO), (RING,))[phase]
        return any(self.mark.get((j, s), -1) > done and (j, s + 1) in self.mark for j in LINES[COLOR[u]] for s in sent)

    def run(self, u):
        stage = self.stage[u]
        self.order.append((u, stage))
        self.mark[u, stage] = len(self.order)
        self.now = max(self.now, self.ready[u]) + STAGE_COST
        self.stage[u] = stage + 1
        if stage == LAST:
            del self.stage[u]
        elif stage % DUO:
            self.ready[u] = self._wire(u, stage // DUO, 1)
        else:
            self.ready[u] = self._wire(u, stage // DUO, DUO)

    def blocked(self, u):
        stage = self.stage[u]
        if stage == 0 and sum(0 < self.stage.get(j, 0) <= DUO for j in LINES[COLOR[u]]) >= ABREAST:
            return True
        if stage == DUO and BEFORE[u] is not None and (BEFORE[u], LAST) not in self.mark:
            return True
        return stage in (0, DUO, RING) and not self.free(u, stage // DUO)

    def start(self, u):
        self.stage[u], self.ready[u] = 0, self.now

    def due(self):
        first = len(self.order)
        while True:
            ripe = [(self.ready[u], u) for u in self.stage if self.ready[u] <= self.now and not self.blocked(u)]
            if not ripe:
                return self.order[first:]
            self.run(min(ripe)[1])

    def vacated(self, u):
        return (u, DUO) in self.mark

    def rush(self, done):
        first = len(self.order)
        while not done():
            self.run(min((self.ready[u], u) for u in self.stage if not self.blocked(u))[1])
        return self.order[first:]


QB = PAIR
NBLK = TOKENS // QB
HALVES = (pl.ds(0, SHARE), pl.ds(SHARE, SHARE))


class Scatter:
    def __init__(self, comm, part, mid, bufs, fin, outs, send_sems, recv_sems, swap_sems):
        self.pos, self.part, self.mid, self.bufs, self.fin, self.outs = comm.pos, part, mid, bufs, fin, outs
        self.send_sems, self.recv_sems, self.swap_sems = send_sems, recv_sems, swap_sems
        self.near = {(a, hop): comm.far(a, hop) for a in AXES for hop in (1, DUO, TRIO)}
        self.hops = {(a, hop): step(comm.pos, a, hop) for a in AXES for hop in (1, DUO, TRIO)}
        self.peer, self.core = comm.peer(), comm.core
        self.keep, self.give = tile_at(comm.core, SHARE), tile_at(1 - comm.core, SHARE)
        self.drained = set()

    def slot(self, u):
        return COLOR[u], RANK[u] % SLOTS

    def buf(self, u, phase):
        return self.bufs[phase].at[self.slot(u)]

    def view(self, u, phase, hop, half=None):
        order = ORDERS[COLOR[u]]
        at = {a: ALL for a in AXES}
        for a in order[1:phase]:
            at[a] = self.pos[a]
        at[order[phase]] = self.hops[order[phase], hop] if hop else self.pos[order[phase]]
        rows = pl.ds(0, CHIP) if half is None else HALVES[half]
        if phase == 0:
            return self.part.at[PLACE[u], at['z'], at['y'], at['x'], rows, :]
        return self.mid.at[self.slot(u) + tuple(at[a] for a in 'zyx' if a != order[0]) + (rows, slice(None))]

    def copy(self, src, dst, sems, device):
        return pltpu.make_async_remote_copy(src_ref=src, dst_ref=dst, send_sem=sems[0], recv_sem=sems[1], device_id=device, device_id_type=MESH)

    def one(self, u, phase, name):
        axis = ORDERS[COLOR[u]][phase]
        if phase == DUO:
            src, to = self.view(u, DUO, name + 1), name + 1
        else:
            hop, half, to = ((DUO, 0, 1), (DUO, 1, TRIO), (1, 1, 1), (TRIO, 0, TRIO), (1, 0, 1), (TRIO, 1, TRIO))[name]
            src = self.view(u, phase, hop, half)
        i = (u * TRIO + phase) * 6 + name
        return self.copy(src, self.bufs[phase].at[self.slot(u) + (name,)], (self.send_sems.at[i], self.recv_sems.at[i]), self.near[axis, to])

    def send(self, u, phase, name):
        self.one(u, phase, name).start()

    def launch(self, u, phase):
        if BEFORE[u] is not None:
            self.drain(BEFORE[u], phase)
        for name in range(RING if phase < DUO else TRIO):
            self.send(u, phase, name)

    def arrived(self, u, phase, first, count):
        for name in range(first, first + count):
            self.one(u, phase, name).wait_recv()

    def drain(self, u, phase):
        if (u, phase) not in self.drained:
            self.drained.add((u, phase))
            for name in range(6 if phase < DUO else TRIO):
                self.one(u, phase, name).wait_send()

    def out(self, u):
        if u < HEADS:
            out, col = self.outs[0], self.core * HALF + u * LANES
        elif u < 10:
            out, col = self.outs[u - 7], self.core * LANES
        else:
            out, col = self.outs[TRIO], self.core * HALF + (u - 10) * LANES
        return out.at[:, pl.ds(pl.multiple_of(col, LANES), LANES)]

    def kept(self, u):
        return pltpu.make_async_copy(self.fin.at[u, self.keep], self.out(u), self.swap_sems.at[u])

    def run(self, u, stage):
        if stage == 0:
            return self.launch(u, 0)
        phase = (stage - 1) // DUO
        if stage == LAST:
            self.arrived(u, DUO, 0, TRIO)
            got = self.buf(u, DUO)
            self.fin[u] = self.view(u, DUO, 0)[...] + (got[0] + got[1] + got[DUO])
            self.copy(self.fin.at[u, self.give], self.out(u), (self.swap_sems.at[18 + u], self.swap_sems.at[36 + u]), self.peer).start()
            self.kept(u).start()
            return
        got = self.buf(u, phase)
        if stage % DUO:
            self.arrived(u, phase, 0, DUO)
            for name, hop in ((0, 1), (1, TRIO)):
                add_into(self.view(u, phase, hop, name), got.at[name])
                self.send(u, phase, name + RING)
            return
        self.arrived(u, phase, DUO, RING)
        if phase == 0 and BEFORE[u] is not None:
            self.drain(BEFORE[u], 1)
            self.drain(BEFORE[u], DUO)
        for half, names in ((0, (TRIO, RING)), (1, (DUO, 5))):
            if phase:
                add_into(self.view(u, phase, 0, half), *[got.at[name] for name in names])
            else:
                dst = self.mid.at[self.slot(u) + (ALL, ALL, HALVES[half], slice(None))]
                add_into(dst, self.view(u, 0, 0, half), *[got.at[name] for name in names], fresh=True)
        self.launch(u, phase + 1)

    def finish(self):
        for u in range(N_UNITS):
            for phase in range(TRIO):
                self.drain(u, phase)
        for u in range(N_UNITS):
            self.copy(self.fin.at[u, self.give], self.out(u), (self.swap_sems.at[18 + u], self.swap_sems.at[36 + u]), self.peer).wait()
        for u in range(N_UNITS):
            self.kept(u).wait()


def attend(heads, qt, do_t, k, kt, v, vt, cos, sin, o_row, ot, dq, dkt, dvt, s_scr, e_scr, p_scr, d_scr):
    f32, bf16 = jnp.float32, jnp.bfloat16
    strip = TURN
    work = [(h, j) for j in range(NBLK) for h in range(len(heads))]

    def strips(c):
        return [(i * strip, slice(c * QB + i * strip, c * QB + (i + 1) * strip)) for i in range(QB // strip)]

    def fold(x, op):
        return op(x.reshape(strip // SUBS, SUBS, QB), axis=0)

    def scores(i):
        (h, j), b = work[i], i % DUO
        q_t = qt[heads[h], j * QB:(j + 1) * QB]
        top = jnp.full((SUBS, QB), -jnp.inf, f32)
        for c in range(j + 1):
            tile = dot(k[c * QB:(c + 1) * QB, :], q_t)
            for at, rows in strips(c):
                s = tile[at:at + strip]
                if c == j:
                    seen = lax.broadcasted_iota(jnp.int32, (strip, QB), 0) + at <= lax.broadcasted_iota(jnp.int32, (strip, QB), 1)
                    s = jnp.where(seen, s, -jnp.inf)
                s_scr[b, rows, :] = s
                top = jnp.maximum(top, fold(s, jnp.max))
        return jnp.max(top, axis=0, keepdims=True)

    def rest(i, m):
        (h, j), b = work[i], i % DUO
        cols, n = slice(j * QB, (j + 1) * QB), (j + 1) * QB
        q_t, d_t = qt[heads[h], cols], do_t[heads[h], cols]
        tot = jnp.zeros((SUBS, QB), f32)
        for c in range(j + 1):
            for at, rows in strips(c):
                e = jnp.exp2((s_scr[b, rows, :] - m) * (SCALE * LOG2E))
                s_scr[b, rows, :] = e
                e_scr[b, rows, :] = e.astype(bf16)
                tot = tot + fold(e, jnp.sum)
        den = jnp.sum(tot, axis=0, keepdims=True)
        inv = 1.0 / den
        o = (dot(vt[:, :n], e_scr[b, :n, :]) / den).astype(bf16)
        ot[o_row(h), cols] = o
        delta = jnp.sum(d_t.astype(f32) * o.astype(f32), axis=0, keepdims=True)
        for c in range(j + 1):
            dp = dot(v[c * QB:(c + 1) * QB, :], d_t)
            for at, rows in strips(c):
                p = s_scr[b, rows, :] * inv
                p_scr[b, rows, :] = p.astype(bf16)
                d_scr[b, rows, :] = (p * (dp[at:at + strip] - delta)).astype(bf16)
        dvt[:, :n] += dot_nt(d_t, p_scr[b, :n, :])
        dkt[:, :n] += dot_nt(q_t, d_scr[b, :n, :])
        g = dot(kt[:, :n], d_scr[b, :n, :]) * SCALE
        co, si = cos[:, cols], sin[:, cols]
        x, y = g[:TURN], g[TURN:]
        dq[heads[h], cols] = jnp.concatenate([x * co + y * si, y * co - x * si], axis=0).astype(bf16)

    m = scores(0)
    for i in range(len(work)):
        later = scores(i + 1) if i + 1 < len(work) else None
        rest(i, m)
        m = later


def tail_kernel(qt, do_t, k, kt, v, vt, rt, dyc, wqk, wqkp, wvo, wvop, gain, hidden, dy, pos, cos, sin,
                result, grad_x, gq, gk, gv, go, gout,
                two, ks, kts, vs, vts, rts, ots, dqo, dqp, dkvo, dkvp, dkt, dvt, s_scr, e_scr, p_scr, d_scr, dycs, part, mid, buf1, buf2, buf3, fin, own, onat, dnat, xs, gacc, gpart, gpeer, gz, gy, gx,
                send_sems, recv_sems, swap_sems, trade_send, trade_recv, local_sems):
    comm = OldComm(trade_send, trade_recv, local_sems)
    comm.used = DUO * HEADS
    f32, bf16 = jnp.float32, jnp.bfloat16
    core, peer = comm.core, comm.peer()
    a1, a2 = two.at[0], two.at[1]
    comm.announce()
    sc = Scatter(comm, part, mid, (buf1, buf2, buf3), fin, (gq, gk, gv, go), send_sems, recv_sems, swap_sems)
    plan = Plan()
    loads = [comm.local(s, d) for s, d in ((qt, a1), (do_t, a2), (k, ks), (kt, kts), (v, vs), (vt, vts))]
    load_r = comm.local(rt, rts)
    later = [comm.local(s, d) for s, d in ((dyc, dycs), (hidden, xs))]
    dkt[...] = jnp.zeros_like(dkt)
    dvt[...] = jnp.zeros_like(dvt)

    @pl.loop(0, TOKENS // LANES)
    def _(i):
        want = lax.broadcasted_iota(jnp.int32, (LANES, ROWS), 0) + i * LANES
        own[tile_at(i, LANES), :] = jnp.where(want == pos[...], 1.0, 0.0).astype(bf16)

    with scope('wait_q'):
        for c in loads:
            c.wait()

    def emit(stages):
        for u, stage in stages:
            with scope(f'u{u}_s{stage}'):
                sc.run(u, stage)

    def after(cost):
        plan.now += cost
        return plan.due()

    def head_trades(h):
        row = tile_at(core * HEADS + h, LANES)
        mine = tile_at(h, LANES)
        return [pltpu.make_async_remote_copy(src_ref=s, dst_ref=d, send_sem=trade_send.at[i], recv_sem=trade_recv.at[i], device_id=peer, device_id_type=MESH)
                for s, d, i in ((ots.at[row], ots.at[row], h), (dqo.at[mine], dqp.at[mine], HEADS + h))]

    def gradient(place, left, right, mul):
        with scope('grad'):
            @pl.loop(0, DUO)
            def _(z):
                g = mul(left[tile_at(z, HALF), :], right())
                for i in range(DUO):
                    part[place + i, tile_at(z, DUO)] = g[:, i * LANES:(i + 1) * LANES].reshape(DUO, RING, RING, CHIP, LANES)

    PAIRS = HEADS // DUO
    attended, paired = [], []
    for g in range(PAIRS):
        attended.append(after(5.2))
        plan.now += 1.6
        plan.start(DUO * g)
        plan.start(DUO * g + 1)
        paired.append(plan.due())
    load_r.wait()

    @pl.loop(0, PAIRS)
    def _(g):
        def at(table):
            for i in range(PAIRS):
                if table[i]:
                    pl.when(g == i)(functools.partial(emit, table[i]))

        heads = [tile_at(DUO * g + i, LANES) for i in range(DUO)]
        with scope('attend'):
            attend(heads, a1, a2, ks, kts, vs, vts, cos, sin, lambda i: tile_at(core * HEADS + DUO * g + i, LANES), ots, dqo, dkt, dvt, s_scr, e_scr, p_scr, d_scr)

        @pl.when(g == 0)
        def _():
            with scope('entry'):
                comm.meet()
        for i in range(DUO):
            for c in head_trades(DUO * g + i):
                c.start()
        at(attended)
        gradient(DUO * g, rts, lambda: dqo[tile_at(g, PAIR), :], dot_nt)
        at(paired)

    def beat(cost, *starts):
        plan.now += cost
        for u in starts:
            plan.start(u)
        emit(plan.due())

    wkv, wkvp = e_scr.reshape(DIM, PAIR), p_scr.reshape(DIM, PAIR)
    later += [comm.local(src.at[:, pl.ds(at, LANES)], dst.at[:, pl.ds(to, LANES)]) for srcs, dst in (((wqk, wvo), wkv), ((wqkp, wvop), wkvp)) for src, at, to in ((srcs[0], HALF, 0), (srcs[1], 0, LANES))]
    wqp_loads = [comm.local(wqkp.at[tile_at(i, HALF), pl.ds(0, HALF)], two.at[i]) for i in range(DUO)]
    key = dkt[...] * SCALE
    co, si, x, y = cos[...], sin[...], key[:TURN], key[TURN:]
    dkvo[:LANES, :] = jnp.concatenate([x * co + y * si, y * co - x * si], axis=0).astype(bf16)
    dkvo[LANES:, :] = dvt[...].astype(bf16)
    comm.trade(dkvo, dkvp)
    gradient(UNIT_K, rts, lambda: dkvo[...], dot_nt)
    beat(2.0, UNIT_K, UNIT_V)
    wq_load = comm.local(wqk.at[:, pl.ds(0, HALF)], rts)
    for c in later:
        c.wait()
    with scope('trades'):
        for h in range(HEADS):
            for c in head_trades(h):
                c.wait()

    waiting = list(range(RING))

    def output_gradients(force=False):
        while waiting:
            first = 10 + DUO * waiting[0]
            before = [u for u in range(N_UNITS) if u < first and PLACE[u] in (PLACE[first], PLACE[first + 1])]
            if force:
                emit(plan.rush(lambda: all(map(plan.vacated, before))))
            if not all(map(plan.vacated, before)):
                return
            for u in before:
                sc.drain(u, 0)
            i = waiting.pop(0)
            gradient(PLACE[first], ots, lambda: dycs[:, i * PAIR:(i + 1) * PAIR], dot)
            plan.start(first)
            plan.start(first + 1)
            beat(1.5)

    def piece(cost):
        beat(cost)
        output_gradients()

    def unsort(at, src_t, n):
        with scope('unsort'):
            dnat[at:at + n, :] = dot(src_t[:n, :], own[...]).astype(bf16)

    output_gradients()
    for i in range(DUO):
        with scope('unsort_o'):
            @pl.loop(0, DUO)
            def _(j):
                r = pl.ds(pl.multiple_of(i * HALF + j * ROWS, ROWS), ROWS)
                onat[:, r] = dot(ots[r, :], own[...]).astype(bf16).T
        piece(1.4)
    for c in comm.exchanged:
        c.wait_recv()
    unsort(0, dqo, HALF)
    dy_loads = [comm.local(dy.at[:, tile_at(i, HALF)], dqo.at[tile_at(i, ROWS)]) for i in range(DUO)]
    piece(1.2)
    unsort(HALF, dqp, HALF)
    piece(1.2)
    unsort(DUO * HALF, dkvo, PAIR)
    unsort(DUO * HALF + PAIR, dkvp, PAIR)
    piece(0.7)
    wq_load.wait()
    for c in wqp_loads + dy_loads:
        c.wait()
    gacc[...] = jnp.zeros_like(gacc)

    def dr_parts(half, r):
        return [s_scr.at[half, r(i * PAIR), :] for i in range(RING)]

    def back(block):
        with scope('dr'):
            @pl.loop(0, DUO)
            def _(half):
                c = tile_at(half, HALF)
                left = jnp.concatenate([rts[c, :], two[half], wkv[c, :], wkvp[c, :]], axis=1)
                acc = dot(left, dnat[:, block * PAIR:(block + 1) * PAIR])
                for i, ref in enumerate(dr_parts(half, lambda at: pl.ds(at, PAIR))):
                    ref[...] = acc[i * PAIR:(i + 1) * PAIR, :].T
        piece(3.4)
        with scope('back'):
            @pl.loop(0, SHARE)
            def _(j):
                q = pl.ds(pl.multiple_of(block * PAIR + j * SHARE, SHARE), SHARE)
                d = jnp.concatenate([ref[...] for half in range(DUO) for ref in dr_parts(half, lambda at: pl.ds(pl.multiple_of(at + j * SHARE, SHARE), SHARE))], axis=1)
                x = xs[q, :].astype(f32)
                inv = lax.rsqrt(jnp.mean(x * x, axis=-1, keepdims=True) + RMS_EPS)
                unit = x * inv
                gacc[...] += jnp.sum((d * unit).reshape(DUO, SUBS, DIM), axis=0)
                dg = d * gain[0:1, :]
                new = inv * (dg - unit * jnp.mean(dg * unit, axis=-1, keepdims=True))
                for half in range(DUO):
                    r = pl.ds(pl.multiple_of(half * ROWS + block * PAIR + j * SHARE, SHARE), SHARE)
                    dqo[r, :] = (dqo[r, :].astype(f32) + new[:, half * HALF:(half + 1) * HALF]).astype(bf16)
        piece(3.6)

    back(0)
    back(1)
    wo_loads = [comm.local(wvo.at[:, pl.ds(LANES, HALF)], rts)] + [comm.local(wvop.at[tile_at(i, HALF), pl.ds(LANES, HALF)], two.at[i]) for i in range(DUO)]
    for i in range(DUO):
        comm.store(dqo.at[tile_at(i, ROWS)], grad_x.at[:, tile_at(i, HALF)])
    total = jnp.sum(gacc[...], axis=0, keepdims=True)
    gpart[...] = jnp.zeros_like(gpart)
    for i in range(RING):
        for j in range(RING):
            gpart[i, j:j + 1, :] = total[:, (i * RING + j) * LANES:(i * RING + j + 1) * LANES]
    stage = [comm.send(gpart, gpeer, peer)]
    output_gradients(True)

    def project_out(col, weights, i):
        with scope('project'):
            @pl.loop(DUO * i, DUO * i + DUO)
            def _(j):
                c = tile_at(j, PAIR)
                dst = pl.ds(pl.multiple_of(col + j * PAIR, PAIR), PAIR)
                xs[:, dst] = (xs[:, dst].astype(f32) + dot(onat[...], weights(c))).astype(bf16)
        beat(1.3)

    def own_half(c):
        return rts[:, c]

    def other_half(c):
        return jnp.concatenate([a1[:, c], a2[:, c]], axis=0)

    for c in wo_loads:
        c.wait()
    project_out(core * HALF, own_half, 0)
    for c in stage:
        c.wait_recv()
    for j in range(RING):
        gz[j] = gpart[j] + gpeer[j]
    stage = [comm.send(gz.at[step(comm.pos, 'z', hop)], gz.at[TRIO + hop], comm.far('z', hop)) for hop in (1, DUO, TRIO)]
    project_out(core * HALF, own_half, 1)
    for c in stage:
        c.wait_recv()
    gy[0] = (gz[comm.pos['z']] + gz[RING]) + (gz[5] + gz[6])
    stage = [comm.send(gy.at[0], gy.at[hop], comm.far('y', hop)) for hop in (1, DUO, TRIO)]
    project_out((1 - core) * HALF, other_half, 0)
    for c in stage:
        c.wait_recv()
    gx[0] = (gy[0] + gy[1]) + (gy[DUO] + gy[TRIO])
    stage = [comm.send(gx.at[0], gx.at[hop], comm.far('x', hop)) for hop in (1, DUO, TRIO)]
    project_out((1 - core) * HALF, other_half, 1)
    comm.store(xs, result)
    for c in stage:
        c.wait_recv()
    gpeer[0] = (gx[0] + gx[1]) + (gx[DUO] + gx[TRIO])
    mine = jnp.broadcast_to(gpeer[0, pl.ds(comm.pos['y'], 1), :], (SUBS, LANES))
    gout[...] = pltpu.roll(mine, LANES - (comm.pos['x'] * CHIP + core * SHARE), 1)
    emit(plan.rush(lambda: not plan.stage))
    with scope('finish'):
        sc.finish()
        for c in comm.sent + comm.exchanged:
            c.wait_send()
        for c in comm.stored:
            c.wait()


def tail(qt, do_t, k, kt, v, vt, rt, dyc, wqk, wqkp, wvo, wvop, gain, hidden, dy, pos, cos, sin):
    bf16, f32 = jnp.bfloat16, jnp.float32
    any_ = pl.BlockSpec(memory_space=pl.ANY)
    vmem = pl.BlockSpec(memory_space=pltpu.VMEM)
    S = lambda shape, d=bf16: jax.ShapeDtypeStruct(shape, d)
    V = lambda shape, d=bf16: pltpu.VMEM(shape, d)
    D = lambda n: pltpu.SemaphoreType.DMA((n,))
    sq, tall, wide = (HALF, TOKENS), (TOKENS, LANES), (LANES, TOKENS)
    mine, kv = (ROWS, DIM), (PAIR, TOKENS)
    return pl.pallas_call(
        tail_kernel,
        out_shape=[S(mine), S(mine), S((SHARE, DIM), f32), S((SHARE, PAIR), f32), S((SHARE, PAIR), f32), S((SHARE, DIM), f32), S((SUBS, LANES), f32)],
        in_specs=[any_] * 12 + [vmem] + [any_] * DUO + [vmem] * TRIO,
        out_specs=[any_] * 6 + [vmem],
        scratch_shapes=[V((DUO,) + sq), V(tall), V(wide), V(tall), V(wide), V((DIM, TOKENS)), V((DIM, TOKENS)), V(sq), V(sq), V(kv), V(kv), V(wide, f32), V(wide, f32),
                        V((DUO, TOKENS, QB), f32), V((DUO, TOKENS, QB)), V((DUO, TOKENS, QB)), V((DUO, TOKENS, QB)), V(sq), V((PLACES, RING, RING, RING, CHIP, LANES), f32), V((TRIO, SLOTS, RING, RING, CHIP, LANES), f32),
                        V((TRIO, SLOTS, 6, RING, RING, SHARE, LANES), f32), V((TRIO, SLOTS, 6, RING, SHARE, LANES), f32), V((TRIO, SLOTS, TRIO, CHIP, LANES), f32), V((N_UNITS, CHIP, LANES), f32), V((TOKENS, ROWS)), V(mine), V((DUO * QKV, ROWS)), V(mine),
                        V((SUBS, DIM), f32), V((RING, SUBS, LANES), f32), V((RING, SUBS, LANES), f32), V((7, SUBS, LANES), f32), V((RING, SUBS, LANES), f32), V((RING, SUBS, LANES), f32),
                        D(18 * N_UNITS), D(18 * N_UNITS), D(TRIO * N_UNITS), D(DUO * HEADS + SHARE), D(DUO * HEADS + SHARE), D(CHIP)],
        compiler_params=pltpu.CompilerParams(collective_id=1, has_side_effects=True, vmem_limit_bytes=67043328),
        name='tail',
    )(qt, do_t, k, kt, v, vt, rt, dyc, wqk, wqkp, wvo, wvop, gain, hidden, dy, pos, cos, sin)


def settle_kernel(n, *refs):
    ins, gain, outs, gain_out, bufs, sems = refs[:n], refs[n], refs[n + 1:DUO * n + 1], refs[DUO * n + 1], refs[DUO * n + DUO:-1], refs[-1]
    jobs = []
    for a, o, b in zip(ins, outs, bufs):
        size = a.shape[0] // RING if a.shape[0] == ROWS else a.shape[0]
        jobs += [tuple(r.at[pl.ds(i, size)] for r in (a, b, o)) for i in range(0, a.shape[0], size)]
    takes = [pltpu.make_async_copy(a, b, sems.at[0, i]) for i, (a, b, _) in enumerate(jobs)]
    puts = [pltpu.make_async_copy(b, o, sems.at[1, i]) for i, (_, b, o) in enumerate(jobs)]
    for c in takes:
        c.start()
    gain_out[...] = gain[0:1, :SHARE]
    for take, put in zip(takes, puts):
        take.wait()
        put.start()
    for c in puts:
        c.wait()


def settle(*arrays):
    *large, gain = arrays
    any_, vmem = pl.BlockSpec(memory_space=pl.ANY), pl.BlockSpec(memory_space=pltpu.VMEM)
    return pl.pallas_call(
        functools.partial(settle_kernel, len(large)),
        out_shape=[jax.ShapeDtypeStruct(a.shape, a.dtype) for a in large] + [jax.ShapeDtypeStruct((1, SHARE), gain.dtype)],
        in_specs=[any_] * len(large) + [vmem],
        out_specs=[any_] * len(large) + [vmem],
        scratch_shapes=[pltpu.VMEM(a.shape, a.dtype) for a in large] + [pltpu.SemaphoreType.DMA((DUO, 12))],
        name='settle',
    )(*arrays)


def rope_tables():
    j = np.arange(HEAD_DIM // DUO, dtype=np.float64) / (HEAD_DIM // DUO)
    freq = (ROPE_THETA ** -j).astype(np.float32)
    angle = freq[:, None] * np.arange(TOKENS, dtype=np.float32)[None, :]
    return np.cos(angle.astype(np.float64)).astype(np.float32), np.sin(angle.astype(np.float64)).astype(np.float32)


def solution(mesh):
    def shard_fn(hidden, tok_pos, grad_out, norm_gain, w_query, w_key, w_value, w_out):
        hidden, grad_out = hidden[0], grad_out[0]
        cos_t, sin_t = (jnp.asarray(t) for t in rope_tables())
        *parts, gain = head(hidden, grad_out, w_query, w_key, w_value, w_out, tok_pos, norm_gain.reshape(1, SHARE), cos_t, sin_t)
        parts = [p.reshape(DIM, GROUP) if p.ndim > DUO else p for p in parts]
        result, grad_hidden, gq, gk, gv, go, gout = settle(*tail(*parts, gain, hidden, grad_out, tok_pos, cos_t, sin_t))
        return result[None], grad_hidden[None], gq, gk, gv, go, gout.reshape(SHARE)

    row_spec, pos_spec = P('fsdp', 'cp', None), P('fsdp', 'cp')
    weight_spec, gain_spec = P(('fsdp', 'cp'), None), P(('fsdp', 'cp'))
    return jax.shard_map(shard_fn, mesh=mesh, in_specs=(row_spec, pos_spec, row_spec, gain_spec, weight_spec, weight_spec, weight_spec, weight_spec), out_specs=(row_spec, row_spec, weight_spec, weight_spec, weight_spec, weight_spec, gain_spec), check_vma=False)
```

```python
import functools
import jax
import jax.numpy as jnp
import numpy as np
from jax import lax
from jax.experimental import pallas as pl
from jax.experimental.pallas import tpu as pltpu
from jax.sharding import PartitionSpec as P

LANES, SUBS, RING, TRIO, DUO = 128, 8, 4, 3, 2
PAIR, ROWS, CHIP, SHARE, TURN = 256, 512, 32, 16, 64
HEAD_DIM = LANES
ROPE_THETA = 1000000.0
RMS_EPS = 1e-5
SCALE = HEAD_DIM ** -0.5
LOG2E = 1.4426950408889634

MESH = pl.DeviceIdType.MESH
AXES = ('x', 'y', 'z')
ORDERS = (('x', 'y', 'z'), ('y', 'z', 'x'), ('z', 'x', 'y'))
ALL = pl.ds(0, RING)


def torus():
    f = lax.axis_index('fsdp')
    return {'x': lax.rem(f, RING), 'y': lax.rem(lax.div(f, RING), RING), 'z': lax.div(f, SHARE)}


def step(pos, axis, hop):
    return lax.rem(pos[axis] + hop, RING)


class Batch:
    def __init__(self, comm):
        self.comm, self.index = comm, comm.used
        comm.used += 1

    def _copy(self, src, dst, device):
        send, recv, _ = self.comm.sems
        return pltpu.make_async_remote_copy(src_ref=src, dst_ref=dst, send_sem=send.at[self.index], recv_sem=recv.at[self.index], device_id=device, device_id_type=MESH)

    def send(self, src, dst, device):
        self._copy(src, dst, device).start()
        return self

    def arrived(self, whole):
        self._copy(whole, whole, self.comm.peer()).wait_recv()

    def sent(self, whole):
        self._copy(whole, whole, self.comm.peer()).wait_send()


class Comm:
    def __init__(self, send_sems, recv_sems, local_sems):
        self.pos = torus()
        self.core = lax.axis_index('cp')
        self.sems = (send_sems, recv_sems, local_sems)
        self.used = self.used_local = 0
        self.stored = []

    def far(self, axis, hop):
        p = dict(self.pos)
        p[axis] = step(self.pos, axis, hop)
        return {'fsdp': (p['z'] * RING + p['y']) * RING + p['x'], 'cp': self.core}

    def peer(self):
        return {'fsdp': lax.axis_index('fsdp'), 'cp': 1 - self.core}

    def announce(self):
        sem = pltpu.get_barrier_semaphore()
        for axis in AXES:
            for hop in (1, DUO, TRIO):
                pl.semaphore_signal(sem, inc=1, device_id=self.far(axis, hop), device_id_type=MESH)
        pl.semaphore_signal(sem, inc=1, device_id=self.peer(), device_id_type=MESH)

    def meet(self):
        pl.semaphore_wait(pltpu.get_barrier_semaphore(), 10)

    def ring(self, batch, src, slots, axis):
        for hop in (1, DUO, TRIO):
            batch.send(src, slots.at[hop], self.far(axis, hop))

    def local(self, src, dst):
        i = self.used_local
        self.used_local += 1
        c = pltpu.make_async_copy(src, dst, self.sems[DUO].at[i])
        c.start()
        return c

    def store(self, src, dst):
        self.stored.append(self.local(src, dst))


class OldComm:
    def __init__(self, send_sems, recv_sems, local_sems):
        self.pos = torus()
        self.core = lax.axis_index('cp')
        self.sems = (send_sems, recv_sems, local_sems)
        self.used = self.used_local = 0
        self.sent, self.exchanged, self.stored = [], [], []

    def far(self, axis, hop):
        p = dict(self.pos)
        p[axis] = step(self.pos, axis, hop)
        return {'fsdp': (p['z'] * RING + p['y']) * RING + p['x'], 'cp': self.core}

    def peer(self):
        return {'fsdp': lax.axis_index('fsdp'), 'cp': 1 - self.core}

    def announce(self):
        sem = pltpu.get_barrier_semaphore()
        for axis in AXES:
            for hop in (1, DUO, TRIO):
                pl.semaphore_signal(sem, inc=1, device_id=self.far(axis, hop), device_id_type=MESH)
        pl.semaphore_signal(sem, inc=1, device_id=self.peer(), device_id_type=MESH)

    def meet(self):
        pl.semaphore_wait(pltpu.get_barrier_semaphore(), 10)

    def barrier(self):
        self.announce()
        self.meet()

    def _copy(self, src, dst, device):
        i = self.used
        self.used += 1
        c = pltpu.make_async_remote_copy(src_ref=src, dst_ref=dst, send_sem=self.sems[0].at[i], recv_sem=self.sems[1].at[i], device_id=device, device_id_type=MESH)
        c.start()
        return c

    def send(self, src, dst, device):
        c = self._copy(src, dst, device)
        self.sent.append(c)
        return c

    def trade(self, src, dst):
        self.exchanged.append(self._copy(src, dst, self.peer()))

    def local(self, src, dst):
        i = self.used_local
        self.used_local += 1
        c = pltpu.make_async_copy(src, dst, self.sems[DUO].at[i])
        c.start()
        return c

    def store(self, src, dst):
        self.stored.append(self.local(src, dst))

    def finish(self):
        for c in self.sent:
            c.wait_send()
        for c in self.exchanged:
            c.wait_send()
            c.wait_recv()
        for c in self.stored:
            c.wait()


def pick(ref, sel, cols):
    return ref.at[sel['z'], sel['y'], sel['x'], :, pl.ds(cols[0], cols[1])]


def sem_scratch(remote, local):
    return [pltpu.SemaphoreType.DMA((remote,)), pltpu.SemaphoreType.DMA((remote,)), pltpu.SemaphoreType.DMA((local,))]


def add_into(dst, *srcs, fresh=False):
    def add(idx):
        total, *rest = [s[idx] for s in (srcs if fresh else (dst,) + srcs)]
        for more in rest:
            total = total + more
        dst[idx] = total

    if len(dst.shape) > TRIO:
        @pl.loop(0, dst.shape[0])
        def _(i):
            add((i,))
    else:
        add(Ellipsis)


QK_COLORS = ((0, PAIR, LANES), (384, LANES, PAIR), (768, PAIR, LANES))
VO_COLORS = ((0, LANES, PAIR), (384, PAIR, LANES), (768, LANES, PAIR))
TOKENS = 1024
DIM = 2048
HALF = 1024
QKV = 1280
GROUP = 1152


def scope(name):
    return jax.named_scope(name)


def dot(a, b):
    return jnp.dot(a, b, preferred_element_type=jnp.float32)


def dot_nt(a, b):
    return lax.dot_general(a, b, (((1,), (1,)), ((), ())), preferred_element_type=jnp.float32)


def tile_at(i, n):
    return pl.ds(pl.multiple_of(i * n, n), n)


class Gather:
    def __init__(self, comm, ref, colors, land):
        self.comm, self.ref, self.colors, self.land = comm, ref, colors, land
        self.held = [dict(comm.pos) for _ in colors]
        self.batches = []

    def parts(self, k):
        lo, na, nb = self.colors[k]
        return (lo, na), (lo + na, nb)

    def move(self, batch, s, cols, to):
        batch.send(pick(self.ref, s, cols), pick(self.ref, s, cols), to)

    def at(self, k, hop):
        d = ORDERS[k][self.phase]
        return dict(self.held[k], **{d: step(self.comm.pos, d, hop)})

    def begin(self, phase):
        self.phase = phase
        self.up, self.dn, self.rest = ([Batch(self.comm) for _ in range(TRIO)] for _ in range(TRIO))
        self.batches += self.up + self.dn + self.rest
        for k in range(TRIO):
            a, b = self.parts(k)
            d = ORDERS[k][phase]
            up, dn, s = self.comm.far(d, 1), self.comm.far(d, TRIO), self.held[k]
            self.move(self.up[k], s, a, up)
            self.move(self.dn[k], s, b, dn)
            self.move(self.rest[k], s, b, up)
            self.move(self.rest[k], s, a, dn)
            if phase == 0:
                for cols in (a, b):
                    self.move(self.rest[k], s, cols, self.comm.far(d, DUO))
        if phase == DUO:
            for k in range(TRIO):
                for cols in self.parts(k):
                    self.land(self.ref, self.held[k], cols)

    def forward(self):
        for k in range(TRIO):
            a, b = self.parts(k)
            d = ORDERS[k][self.phase]
            for batch, hop, cols, to in ((self.up[k], TRIO, a, 1), (self.dn[k], 1, b, TRIO)):
                s = self.at(k, hop)
                batch.arrived(pick(self.ref, s, cols))
                if self.phase:
                    self.move(self.rest[k], s, cols, self.comm.far(d, to))
                if self.phase == DUO:
                    self.land(self.ref, s, cols)

    def end(self):
        for k in range(TRIO):
            a, b = self.parts(k)
            d = ORDERS[k][self.phase]
            two = dict(self.held[k], **{d: pl.ds(0, DUO)})
            self.rest[k].arrived(pick(self.ref, two, (a[0], a[1] + b[1])))
            if self.phase == DUO:
                for hop, cols in ((TRIO, b), (1, a), (DUO, a), (DUO, b)):
                    self.land(self.ref, self.at(k, hop), cols)
            for batch, s, cols in ((self.up[k], self.held[k], a), (self.dn[k], self.held[k], b), (self.rest[k], two, (a[0], a[1] + b[1]))):
                batch.spent = pick(self.ref, s, cols)
            self.held[k] = dict(self.held[k], **{d: ALL})

    def finish(self):
        for batch in self.batches:
            batch.sent(batch.spent)


def head_kernel(hidden, dy, wq, wk, wv, wo, pos, gain_in, cos_t, sin_t,
                qt_o, dot_o, k_o, kt_o, v_o, vt_o, rt_o, dyc_o, wqk_o, wqkp_o, wvo_o, wvop_o, gain_o,
                hid2, dy2, dys, rs, rt, wqk, wvo, wpeer, pi, pos2, qt, dot_s, kk, kt, vv, vt, gain, gtile, gbuf, gx, gy, gz, *sems):
    comm = Comm(*sems)
    pos_c, core = comm.pos, comm.core
    bf16, f32 = jnp.bfloat16, jnp.float32
    peer = comm.peer()
    rows = tile_at(core, SHARE)
    mine_qk = wqk.at[pos_c['z'], pos_c['y'], pos_c['x'], rows]
    mine_vo = wvo.at[pos_c['z'], pos_c['y'], pos_c['x'], rows]

    def weight_parts(c):
        return ((wq.at[:, tile_at(c, HALF)], mine_qk.at[:, pl.ds(0, HALF)]), (wk.at[:, tile_at(c, LANES)], mine_qk.at[:, pl.ds(HALF, LANES)]),
                (wv.at[:, tile_at(c, LANES)], mine_vo.at[:, pl.ds(0, LANES)]), (wo.at[:, tile_at(c, HALF)], mine_vo.at[:, pl.ds(LANES, HALF)]))

    loads = [comm.local(s, d) for s, d in weight_parts(core)]
    load_x = [comm.local(hidden, hid2.at[pl.ds(0, ROWS)]), comm.local(dy, dy2.at[pl.ds(0, ROWS)])]
    share = lax.broadcasted_iota(jnp.int32, (SUBS, LANES), 1) // SHARE
    gtile[...] = jnp.where(share == pos_c['x'] * DUO + core, jnp.broadcast_to(jnp.concatenate([gain_in[...]] * SUBS, axis=1), (SUBS, LANES)), 0.0)
    comm.announce()
    with scope('entry'):
        comm.meet()
    swap_w, swap_pos, swap_dy, swap_x, peers_qk, peers_vo = (Batch(comm) for _ in range(6))
    gain_c, gain_x, gain_y, gain_z = (Batch(comm) for _ in range(RING))
    for s, d in weight_parts(1 - core):
        swap_w.send(s, d, peer)
    gain_c.send(gtile, gbuf, peer)
    swap_pos.send(pos, pos2, peer)
    for c in loads:
        c.wait()
    with scope('wait_w'):
        swapped = wqk.at[pos_c['z'], pos_c['y'], pos_c['x']]
        swap_w.arrived(swapped)

    def land_qk(ref, s, cols):
        peers_qk.send(pick(ref, s, cols), pick(wqkp_o, s, cols), peer)

    def land_vo(ref, s, cols):
        peers_vo.send(pick(ref, s, cols), pick(wpeer, s, cols), peer)

    g1 = Gather(comm, wqk, QK_COLORS, land_qk)
    g2 = Gather(comm, wvo, VO_COLORS, land_vo)
    g1.begin(0)
    g2.begin(0)
    swap_dy.send(dy, dy2.at[pl.ds(ROWS, ROWS)], peer)
    gain_c.arrived(gbuf)
    gx[0] = gtile[...] + gbuf[...]
    comm.ring(gain_x, gx.at[0], gx, 'x')

    swap_pos.arrived(pos2)

    @pl.loop(0, TOKENS // LANES)
    def _(i):
        want = lax.broadcasted_iota(jnp.int32, (LANES, ROWS), 0) + i * LANES
        for h, have in enumerate((pos, pos2)):
            pi[tile_at(i, LANES), h * ROWS:(h + 1) * ROWS] = jnp.where(want == have[...], 1.0, 0.0).astype(bf16)

    def sort(dst, src, first, last):
        with scope('sort'):
            @pl.loop(first, last)
            def _(j):
                c = tile_at(j, PAIR)
                dst[:, c] = dot(pi[...], src[:, c]).astype(bf16)

    with scope('p0_end'):
        for g in (g1, g2):
            g.forward()
            g.end()
    g1.begin(1)
    g2.begin(1)
    swap_x.send(hidden, hid2.at[pl.ds(ROWS, ROWS)], peer)
    with scope('p0_gain'):
        gain_x.arrived(gx.at[pl.ds(1, TRIO)])
    gy[pos_c['y']] = (gx[0] + gx[1]) + (gx[DUO] + gx[TRIO])
    for hop in (1, DUO, TRIO):
        gain_y.send(gy.at[pos_c['y']], gy.at[pos_c['y']], comm.far('y', hop))
    with scope('wait_dy'):
        load_x[1].wait()
        swap_dy.arrived(dy2.at[pl.ds(ROWS, ROWS)])
    sort(dys, dy2, 0, 5)
    with scope('p1_fwd'):
        g1.forward()
        g2.forward()
    gain_y.arrived(gy.at[pl.ds(1, TRIO)])
    for j in range(RING):
        gz[pos_c['z'], j] = gy[j]
    for hop in (1, DUO, TRIO):
        gain_z.send(gz.at[pos_c['z']], gz.at[pos_c['z']], comm.far('z', hop))
    sort(dys, dy2, 5, SUBS)
    comm.store(dys.at[:, tile_at(core, HALF)], dyc_o)
    with scope('p1_end'):
        g1.end()
        g1.begin(DUO)
        g2.end()
    with scope('wait_x'):
        load_x[0].wait()
        swap_x.arrived(hid2.at[pl.ds(ROWS, ROWS)])
    sort(rs, hid2, 0, SUBS)
    with scope('gain'):
        gain_z.arrived(gz.at[pl.ds(1, TRIO)])
    for i in range(RING):
        for j in range(RING):
            gain[:, (i * RING + j) * LANES:(i * RING + j + 1) * LANES] = gz[i, j]
    comm.store(gain, gain_o)

    def norm(first, last):
        with scope('norm'):
            @pl.loop(first, last)
            def _(i):
                r = tile_at(i, CHIP)
                x = rs[r, :].astype(f32)
                inv = lax.rsqrt(jnp.mean(x * x, axis=-1, keepdims=True) + RMS_EPS)
                rs[r, :] = (x * inv * gain[0:1, :]).astype(bf16)

    with scope('p2q_fwd'):
        g1.forward()
    g2.begin(DUO)
    norm(0, TOKENS // CHIP)
    with scope('r_t'):
        @pl.loop(0, DIM // PAIR)
        def _(i):
            c = tile_at(i, PAIR)

            @pl.loop(0, TOKENS // PAIR)
            def _(j):
                r = tile_at(j, PAIR)
                rt[c, r] = rs[r, c].T
    comm.store(rt, rt_o)
    with scope('p2q_end'):
        g1.end()
    comm.store(wqk, wqk_o)
    w_qk, w_vo, w_peer = wqk.reshape(DIM, GROUP), wvo.reshape(DIM, GROUP), wpeer.reshape(DIM, GROUP)

    def rotated(x, r):
        cos, sin = cos_t[:, r], sin_t[:, r]
        cos = jnp.concatenate([cos, cos], axis=0).T
        sin = jnp.concatenate([-sin, sin], axis=0).T
        return (x * cos + pltpu.roll(x, TURN, 1) * sin).astype(bf16)

    def queries(first, last):
        with scope('q'):
            @pl.loop(first, last)
            def _(t):
                x = dot(rs[...], w_qk[:, tile_at(t, PAIR)])
                for i in range(RING):
                    r = slice(i * PAIR, (i + 1) * PAIR)
                    for h in range(DUO):
                        qt[tile_at(DUO * t + h, LANES), r] = rotated(x[r, h * LANES:(h + 1) * LANES], r).T

    queries(0, DUO)
    with scope('p2o_fwd'):
        g2.forward()
    queries(DUO, RING)

    @pl.loop(0, DUO)
    def _(i):
        r = tile_at(i, ROWS)
        key = rotated(dot(rs[r, :], w_qk[:, HALF:]), r)
        kk[r, :] = key
        kt[:, r] = key.T
    for src, dst in ((kk, k_o), (kt, kt_o), (qt, qt_o)):
        comm.store(src, dst)
    with scope('p2o_end'):
        g2.end()
    with scope('vals'):
        @pl.loop(0, DUO)
        def _(i):
            r = tile_at(i, ROWS)
            val = dot(rs[r, :], w_vo[:, :LANES]).astype(bf16)
            vv[r, :] = val
            vt[:, r] = val.T
    for src, dst in ((vv, v_o), (vt, vt_o)):
        comm.store(src, dst)
    with scope('wo_peer'):
        peers_vo.arrived(wpeer)
    comm.store(wvo, wvo_o)
    comm.store(wpeer, wvop_o)

    with scope('do_t'):
        r = tile_at(core, HALF)

        @pl.loop(0, TOKENS // PAIR)
        def _(j):
            t = tile_at(j, PAIR)
            w_rows = jnp.concatenate([w_vo[r, LANES:], w_peer[r, LANES:]], axis=1)
            d_rows = jnp.concatenate([dys[t, tile_at(core, HALF)], dys[t, tile_at(1 - core, HALF)]], axis=1)
            dot_s[:, t] = dot_nt(w_rows, d_rows).astype(bf16)
    comm.store(dot_s, dot_o)
    with scope('finish'):
        peers_qk.arrived(wqk)
        for batch, whole in ((swap_w, swapped), (swap_pos, pos2), (swap_dy, dy2.at[pl.ds(ROWS, ROWS)]), (swap_x, hid2.at[pl.ds(ROWS, ROWS)]), (peers_qk, wqk), (peers_vo, wvo),
                             (gain_c, gbuf), (gain_x, gx.at[pl.ds(1, TRIO)]), (gain_y, gy.at[pl.ds(1, TRIO)]), (gain_z, gz.at[pl.ds(1, TRIO)])):
            batch.sent(whole)
        g1.finish()
        g2.finish()
        for c in comm.stored:
            c.wait()


def head(hidden, dy, wq, wk, wv, wo, pos, gain, cos_t, sin_t):
    bf16, f32 = jnp.bfloat16, jnp.float32
    any_ = pl.BlockSpec(memory_space=pl.ANY)
    vmem = pl.BlockSpec(memory_space=pltpu.VMEM)
    S = lambda shape, d=bf16: jax.ShapeDtypeStruct(shape, d)
    V = lambda shape, d=bf16: pltpu.VMEM(shape, d)
    group = (RING, RING, RING, CHIP, GROUP)
    sq, tall, wide = (HALF, TOKENS), (TOKENS, LANES), (LANES, TOKENS)
    full = (TOKENS, DIM)
    return pl.pallas_call(
        head_kernel,
        out_shape=[S(sq), S(sq), S(tall), S(wide), S(tall), S(wide), S((DIM, TOKENS)), S((TOKENS, HALF)), S(group), S(group), S(group), S(group), S((SUBS, DIM), f32)],
        in_specs=[any_] * 6 + [vmem] * RING,
        out_specs=[any_] * 13,
        scratch_shapes=[V(full), V(full), V(full), V(full), V((DIM, TOKENS)), V(group), V(group), V(group), V((TOKENS, TOKENS)), V((1, ROWS), jnp.int32),
                        V(sq), V(sq), V(tall), V(wide), V(tall), V(wide), V((SUBS, DIM), f32), V((SUBS, LANES), f32), V((SUBS, LANES), f32), V((RING, SUBS, LANES), f32), V((RING, SUBS, LANES), f32), V((RING, RING, SUBS, LANES), f32)] + sem_scratch(TURN, 18),
        compiler_params=pltpu.CompilerParams(collective_id=0, has_side_effects=True, vmem_limit_bytes=60 * DUO**20),
        name='head',
    )(hidden, dy, wq, wk, wv, wo, pos, gain, cos_t, sin_t)


HEADS = SUBS
UNIT_K, UNIT_V = SUBS, 9
N_UNITS = 18
SLOTS = RING
LAST = 5
ABREAST = DUO
LINES = ((0, TRIO, 6, 9, 12, 15), (1, RING, 7, 10, 13, SHARE), (DUO, 5, SUBS, 11, 14, 17))
COLOR = {u: k for k, line in enumerate(LINES) for u in line}
RANK = {u: i for line in LINES for i, u in enumerate(line)}
BEFORE = {u: line[i - SLOTS] if i >= SLOTS else None for line in LINES for i, u in enumerate(line)}
PLACES = 12
PLACE = {u: u % PLACES for u in range(N_UNITS)}
WIRE = (2.85, 0.72, 0.36)
LATENCY = 2.6
STAGE_COST = 0.1


class Plan:
    def __init__(self):
        self.now, self.stage, self.ready, self.order, self.link = 0.0, {}, {}, [], {}
        self.mark = {}

    def _wire(self, u, phase, count):
        link = ORDERS[COLOR[u]][phase]
        t = max(self.link.get(link, 0.0), self.now)
        first = t + WIRE[phase] + LATENCY
        self.link[link] = t + WIRE[phase] * count
        return first if phase < DUO else self.link[link] + LATENCY

    def free(self, u, phase):
        if BEFORE[u] is None:
            return True
        done = self.mark.get((BEFORE[u], (DUO, RING, 5)[phase]))
        if done is None:
            return False
        sent = ((0, 1), (DUO, TRIO), (RING,))[phase]
        return any(self.mark.get((j, s), -1) > done and (j, s + 1) in self.mark for j in LINES[COLOR[u]] for s in sent)

    def run(self, u):
        stage = self.stage[u]
        self.order.append((u, stage))
        self.mark[u, stage] = len(self.order)
        self.now = max(self.now, self.ready[u]) + STAGE_COST
        self.stage[u] = stage + 1
        if stage == LAST:
            del self.stage[u]
        elif stage % DUO:
            self.ready[u] = self._wire(u, stage // DUO, 1)
        else:
            self.ready[u] = self._wire(u, stage // DUO, DUO)

    def blocked(self, u):
        stage = self.stage[u]
        if stage == 0 and sum(0 < self.stage.get(j, 0) <= DUO for j in LINES[COLOR[u]]) >= ABREAST:
            return True
        if stage == DUO and BEFORE[u] is not None and (BEFORE[u], LAST) not in self.mark:
            return True
        return stage in (0, DUO, RING) and not self.free(u, stage // DUO)

    def start(self, u):
        self.stage[u], self.ready[u] = 0, self.now

    def due(self):
        first = len(self.order)
        while True:
            ripe = [(self.ready[u], u) for u in self.stage if self.ready[u] <= self.now and not self.blocked(u)]
            if not ripe:
                return self.order[first:]
            self.run(min(ripe)[1])

    def vacated(self, u):
        return (u, DUO) in self.mark

    def rush(self, done):
        first = len(self.order)
        while not done():
            self.run(min((self.ready[u], u) for u in self.stage if not self.blocked(u))[1])
        return self.order[first:]


QB = PAIR
NBLK = TOKENS // QB
HALVES = (pl.ds(0, SHARE), pl.ds(SHARE, SHARE))


class Scatter:
    def __init__(self, comm, part, mid, bufs, fin, outs, send_sems, recv_sems, swap_sems):
        self.pos, self.part, self.mid, self.bufs, self.fin, self.outs = comm.pos, part, mid, bufs, fin, outs
        self.send_sems, self.recv_sems, self.swap_sems = send_sems, recv_sems, swap_sems
        self.near = {(a, hop): comm.far(a, hop) for a in AXES for hop in (1, DUO, TRIO)}
        self.hops = {(a, hop): step(comm.pos, a, hop) for a in AXES for hop in (1, DUO, TRIO)}
        self.peer, self.core = comm.peer(), comm.core
        self.keep, self.give = tile_at(comm.core, SHARE), tile_at(1 - comm.core, SHARE)
        self.drained = set()

    def slot(self, u):
        return COLOR[u], RANK[u] % SLOTS

    def buf(self, u, phase):
        return self.bufs[phase].at[self.slot(u)]

    def view(self, u, phase, hop, half=None):
        order = ORDERS[COLOR[u]]
        at = {a: ALL for a in AXES}
        for a in order[1:phase]:
            at[a] = self.pos[a]
        at[order[phase]] = self.hops[order[phase], hop] if hop else self.pos[order[phase]]
        rows = pl.ds(0, CHIP) if half is None else HALVES[half]
        if phase == 0:
            return self.part.at[PLACE[u], at['z'], at['y'], at['x'], rows, :]
        return self.mid.at[self.slot(u) + tuple(at[a] for a in 'zyx' if a != order[0]) + (rows, slice(None))]

    def copy(self, src, dst, sems, device):
        return pltpu.make_async_remote_copy(src_ref=src, dst_ref=dst, send_sem=sems[0], recv_sem=sems[1], device_id=device, device_id_type=MESH)

    def sems(self, u, phase, kind=0):
        at = u * TRIO + phase
        return self.send_sems.at[at], self.recv_sems.at[DUO * at + kind]

    def send(self, u, phase, name):
        axis = ORDERS[COLOR[u]][phase]
        if phase == DUO:
            src, to = self.view(u, DUO, name + 1), name + 1
        else:
            hop, half, to = ((DUO, 0, 1), (DUO, 1, TRIO), (1, 1, 1), (TRIO, 0, TRIO), (1, 0, 1), (TRIO, 1, TRIO))[name]
            src = self.view(u, phase, hop, half)
        self.copy(src, self.buf(u, phase).at[name], self.sems(u, phase, int(name > 1 and phase < DUO)), self.near[axis, to]).start()

    def launch(self, u, phase):
        if BEFORE[u] is not None:
            self.drain(BEFORE[u], phase)
        for name in range(RING if phase < DUO else TRIO):
            self.send(u, phase, name)

    def arrived(self, u, phase, first, count):
        whole = self.buf(u, phase).at[pl.ds(first, count)]
        self.copy(whole, whole, self.sems(u, phase, int(first > 0)), self.peer).wait_recv()

    def drain(self, u, phase):
        if (u, phase) not in self.drained:
            self.drained.add((u, phase))
            whole = self.buf(u, phase)
            self.copy(whole, whole, self.sems(u, phase), self.peer).wait_send()

    def out(self, u):
        if u < HEADS:
            out, col = self.outs[0], self.core * HALF + u * LANES
        elif u < 10:
            out, col = self.outs[u - 7], self.core * LANES
        else:
            out, col = self.outs[TRIO], self.core * HALF + (u - 10) * LANES
        return out.at[:, pl.ds(pl.multiple_of(col, LANES), LANES)]

    def kept(self, u):
        return pltpu.make_async_copy(self.fin.at[u, self.keep], self.out(u), self.swap_sems.at[DUO + u])

    def run(self, u, stage):
        if stage == 0:
            return self.launch(u, 0)
        phase = (stage - 1) // DUO
        if stage == LAST:
            self.arrived(u, DUO, 0, TRIO)
            got = self.buf(u, DUO)
            self.fin[u] = self.view(u, DUO, 0)[...] + (got[0] + got[1] + got[DUO])
            self.copy(self.fin.at[u, self.give], self.out(u), (self.swap_sems.at[0], self.swap_sems.at[1]), self.peer).start()
            self.kept(u).start()
            return
        got = self.buf(u, phase)
        if stage % DUO:
            self.arrived(u, phase, 0, DUO)
            for name, hop in ((0, 1), (1, TRIO)):
                add_into(self.view(u, phase, hop, name), got.at[name])
                self.send(u, phase, name + RING)
            return
        self.arrived(u, phase, DUO, RING)
        if phase == 0 and BEFORE[u] is not None:
            self.drain(BEFORE[u], 1)
            self.drain(BEFORE[u], DUO)
        for half, names in ((0, (TRIO, RING)), (1, (DUO, 5))):
            if phase:
                add_into(self.view(u, phase, 0, half), *[got.at[name] for name in names])
            else:
                dst = self.mid.at[self.slot(u) + (ALL, ALL, HALVES[half], slice(None))]
                add_into(dst, self.view(u, 0, 0, half), *[got.at[name] for name in names], fresh=True)
        self.launch(u, phase + 1)

    def finish(self):
        for u in range(N_UNITS):
            for phase in range(TRIO):
                self.drain(u, phase)
        half = self.fin.at[:, pl.ds(0, SHARE)]
        swaps = self.copy(half, half, (self.swap_sems.at[0], self.swap_sems.at[1]), self.peer)
        swaps.wait_send()
        swaps.wait_recv()
        for u in range(N_UNITS):
            self.kept(u).wait()


def attend(heads, qt, do_t, k, kt, v, vt, cos, sin, o_row, ot, dq, dkt, dvt, s_scr, e_scr, p_scr, d_scr):
    f32, bf16 = jnp.float32, jnp.bfloat16
    strip = TURN
    work = [(h, j) for j in range(NBLK) for h in range(len(heads))]

    def strips(c):
        return [(i * strip, slice(c * QB + i * strip, c * QB + (i + 1) * strip)) for i in range(QB // strip)]

    def fold(x, op):
        return op(x.reshape(strip // SUBS, SUBS, QB), axis=0)

    def scores(i):
        (h, j), b = work[i], i % DUO
        q_t = qt[heads[h], j * QB:(j + 1) * QB]
        top = jnp.full((SUBS, QB), -jnp.inf, f32)
        for c in range(j + 1):
            tile = dot(k[c * QB:(c + 1) * QB, :], q_t)
            for at, rows in strips(c):
                s = tile[at:at + strip]
                if c == j:
                    seen = lax.broadcasted_iota(jnp.int32, (strip, QB), 0) + at <= lax.broadcasted_iota(jnp.int32, (strip, QB), 1)
                    s = jnp.where(seen, s, -jnp.inf)
                s_scr[b, rows, :] = s
                top = jnp.maximum(top, fold(s, jnp.max))
        return jnp.max(top, axis=0, keepdims=True)

    def rest(i, m):
        (h, j), b = work[i], i % DUO
        cols, n = slice(j * QB, (j + 1) * QB), (j + 1) * QB
        q_t, d_t = qt[heads[h], cols], do_t[heads[h], cols]
        tot = jnp.zeros((SUBS, QB), f32)
        for c in range(j + 1):
            for at, rows in strips(c):
                e = jnp.exp2((s_scr[b, rows, :] - m) * (SCALE * LOG2E))
                s_scr[b, rows, :] = e
                e_scr[b, rows, :] = e.astype(bf16)
                tot = tot + fold(e, jnp.sum)
        den = jnp.sum(tot, axis=0, keepdims=True)
        inv = 1.0 / den
        o = (dot(vt[:, :n], e_scr[b, :n, :]) / den).astype(bf16)
        ot[o_row(h), cols] = o
        delta = jnp.sum(d_t.astype(f32) * o.astype(f32), axis=0, keepdims=True)
        for c in range(j + 1):
            dp = dot(v[c * QB:(c + 1) * QB, :], d_t)
            for at, rows in strips(c):
                p = s_scr[b, rows, :] * inv
                p_scr[b, rows, :] = p.astype(bf16)
                d_scr[b, rows, :] = (p * (dp[at:at + strip] - delta)).astype(bf16)
        dvt[:, :n] += dot_nt(d_t, p_scr[b, :n, :])
        dkt[:, :n] += dot_nt(q_t, d_scr[b, :n, :])
        g = dot(kt[:, :n], d_scr[b, :n, :]) * SCALE
        co, si = cos[:, cols], sin[:, cols]
        x, y = g[:TURN], g[TURN:]
        dq[heads[h], cols] = jnp.concatenate([x * co + y * si, y * co - x * si], axis=0).astype(bf16)

    m = scores(0)
    for i in range(len(work)):
        later = scores(i + 1) if i + 1 < len(work) else None
        rest(i, m)
        m = later


def tail_kernel(qt, do_t, k, kt, v, vt, rt, dyc, wqk, wqkp, wvo, wvop, gain, hidden, dy, pos, cos, sin,
                result, grad_x, gq, gk, gv, go, gout,
                two, ks, kts, vs, vts, rts, ots, dqo, dqp, dkvo, dkvp, dkt, dvt, s_scr, e_scr, p_scr, d_scr, dycs, part, mid, buf1, buf2, buf3, fin, own, onat, dnat, xs, gacc, gpart, gpeer, gz, gy, gx,
                send_sems, recv_sems, swap_sems, trade_send, trade_recv, local_sems):
    comm = OldComm(trade_send, trade_recv, local_sems)
    comm.used = DUO * HEADS
    f32, bf16 = jnp.float32, jnp.bfloat16
    core, peer = comm.core, comm.peer()
    a1, a2 = two.at[0], two.at[1]
    comm.announce()
    sc = Scatter(comm, part, mid, (buf1, buf2, buf3), fin, (gq, gk, gv, go), send_sems, recv_sems, swap_sems)
    plan = Plan()
    loads = [comm.local(s, d) for s, d in ((qt, a1), (do_t, a2), (k, ks), (kt, kts), (v, vs), (vt, vts))]
    load_r = comm.local(rt, rts)
    later = [comm.local(s, d) for s, d in ((dyc, dycs), (hidden, xs))]
    dkt[...] = jnp.zeros_like(dkt)
    dvt[...] = jnp.zeros_like(dvt)

    @pl.loop(0, TOKENS // LANES)
    def _(i):
        want = lax.broadcasted_iota(jnp.int32, (LANES, ROWS), 0) + i * LANES
        own[tile_at(i, LANES), :] = jnp.where(want == pos[...], 1.0, 0.0).astype(bf16)

    with scope('wait_q'):
        for c in loads:
            c.wait()

    def emit(stages):
        for u, stage in stages:
            with scope(f'u{u}_s{stage}'):
                sc.run(u, stage)

    def after(cost):
        plan.now += cost
        return plan.due()

    def head_trades(h):
        row = tile_at(core * HEADS + h, LANES)
        mine = tile_at(h, LANES)
        return [pltpu.make_async_remote_copy(src_ref=s, dst_ref=d, send_sem=trade_send.at[i], recv_sem=trade_recv.at[i], device_id=peer, device_id_type=MESH)
                for s, d, i in ((ots.at[row], ots.at[row], h), (dqo.at[mine], dqp.at[mine], HEADS + h))]

    def gradient(place, left, right, mul):
        with scope('grad'):
            @pl.loop(0, DUO)
            def _(z):
                g = mul(left[tile_at(z, HALF), :], right())
                for i in range(DUO):
                    part[place + i, tile_at(z, DUO)] = g[:, i * LANES:(i + 1) * LANES].reshape(DUO, RING, RING, CHIP, LANES)

    PAIRS = HEADS // DUO
    attended, paired = [], []
    for g in range(PAIRS):
        attended.append(after(5.2))
        plan.now += 1.6
        plan.start(DUO * g)
        plan.start(DUO * g + 1)
        paired.append(plan.due())
    load_r.wait()

    @pl.loop(0, PAIRS)
    def _(g):
        def at(table):
            for i in range(PAIRS):
                if table[i]:
                    pl.when(g == i)(functools.partial(emit, table[i]))

        heads = [tile_at(DUO * g + i, LANES) for i in range(DUO)]
        with scope('attend'):
            attend(heads, a1, a2, ks, kts, vs, vts, cos, sin, lambda i: tile_at(core * HEADS + DUO * g + i, LANES), ots, dqo, dkt, dvt, s_scr, e_scr, p_scr, d_scr)

        @pl.when(g == 0)
        def _():
            with scope('entry'):
                comm.meet()
        for i in range(DUO):
            for c in head_trades(DUO * g + i):
                c.start()
        at(attended)
        gradient(DUO * g, rts, lambda: dqo[tile_at(g, PAIR), :], dot_nt)
        at(paired)

    def beat(cost, *starts):
        plan.now += cost
        for u in starts:
            plan.start(u)
        emit(plan.due())

    wkv, wkvp = e_scr.reshape(DIM, PAIR), p_scr.reshape(DIM, PAIR)
    later += [comm.local(src.at[:, pl.ds(at, LANES)], dst.at[:, pl.ds(to, LANES)]) for srcs, dst in (((wqk, wvo), wkv), ((wqkp, wvop), wkvp)) for src, at, to in ((srcs[0], HALF, 0), (srcs[1], 0, LANES))]
    wqp_loads = [comm.local(wqkp.at[tile_at(i, HALF), pl.ds(0, HALF)], two.at[i]) for i in range(DUO)]
    key = dkt[...] * SCALE
    co, si, x, y = cos[...], sin[...], key[:TURN], key[TURN:]
    dkvo[:LANES, :] = jnp.concatenate([x * co + y * si, y * co - x * si], axis=0).astype(bf16)
    dkvo[LANES:, :] = dvt[...].astype(bf16)
    comm.trade(dkvo, dkvp)
    gradient(UNIT_K, rts, lambda: dkvo[...], dot_nt)
    beat(2.0, UNIT_K, UNIT_V)
    wq_load = comm.local(wqk.at[:, pl.ds(0, HALF)], rts)
    for c in later:
        c.wait()
    with scope('trades'):
        for h in range(HEADS):
            for c in head_trades(h):
                c.wait()

    waiting = list(range(RING))

    def output_gradients(force=False):
        while waiting:
            first = 10 + DUO * waiting[0]
            before = [u for u in range(N_UNITS) if u < first and PLACE[u] in (PLACE[first], PLACE[first + 1])]
            if force:
                emit(plan.rush(lambda: all(map(plan.vacated, before))))
            if not all(map(plan.vacated, before)):
                return
            for u in before:
                sc.drain(u, 0)
            i = waiting.pop(0)
            gradient(PLACE[first], ots, lambda: dycs[:, i * PAIR:(i + 1) * PAIR], dot)
            plan.start(first)
            plan.start(first + 1)
            beat(1.5)

    def piece(cost):
        beat(cost)
        output_gradients()

    def unsort(at, src_t, n):
        with scope('unsort'):
            dnat[at:at + n, :] = dot(src_t[:n, :], own[...]).astype(bf16)

    output_gradients()
    for i in range(DUO):
        with scope('unsort_o'):
            @pl.loop(0, DUO)
            def _(j):
                r = pl.ds(pl.multiple_of(i * HALF + j * ROWS, ROWS), ROWS)
                onat[:, r] = dot(ots[r, :], own[...]).astype(bf16).T
        piece(1.4)
    for c in comm.exchanged:
        c.wait_recv()
    unsort(0, dqo, HALF)
    dy_loads = [comm.local(dy.at[:, tile_at(i, HALF)], dqo.at[tile_at(i, ROWS)]) for i in range(DUO)]
    piece(1.2)
    unsort(HALF, dqp, HALF)
    piece(1.2)
    unsort(DUO * HALF, dkvo, PAIR)
    unsort(DUO * HALF + PAIR, dkvp, PAIR)
    piece(0.7)
    wq_load.wait()
    for c in wqp_loads + dy_loads:
        c.wait()
    gacc[...] = jnp.zeros_like(gacc)

    def dr_parts(half, r):
        return [s_scr.at[half, r(i * PAIR), :] for i in range(RING)]

    def back(block):
        with scope('dr'):
            @pl.loop(0, DUO)
            def _(half):
                c = tile_at(half, HALF)
                left = jnp.concatenate([rts[c, :], two[half], wkv[c, :], wkvp[c, :]], axis=1)
                acc = dot(left, dnat[:, block * PAIR:(block + 1) * PAIR])
                for i, ref in enumerate(dr_parts(half, lambda at: pl.ds(at, PAIR))):
                    ref[...] = acc[i * PAIR:(i + 1) * PAIR, :].T
        piece(3.4)
        with scope('back'):
            @pl.loop(0, SHARE)
            def _(j):
                q = pl.ds(pl.multiple_of(block * PAIR + j * SHARE, SHARE), SHARE)
                d = jnp.concatenate([ref[...] for half in range(DUO) for ref in dr_parts(half, lambda at: pl.ds(pl.multiple_of(at + j * SHARE, SHARE), SHARE))], axis=1)
                x = xs[q, :].astype(f32)
                inv = lax.rsqrt(jnp.mean(x * x, axis=-1, keepdims=True) + RMS_EPS)
                unit = x * inv
                gacc[...] += jnp.sum((d * unit).reshape(DUO, SUBS, DIM), axis=0)
                dg = d * gain[0:1, :]
                new = inv * (dg - unit * jnp.mean(dg * unit, axis=-1, keepdims=True))
                for half in range(DUO):
                    r = pl.ds(pl.multiple_of(half * ROWS + block * PAIR + j * SHARE, SHARE), SHARE)
                    dqo[r, :] = (dqo[r, :].astype(f32) + new[:, half * HALF:(half + 1) * HALF]).astype(bf16)
        piece(3.6)

    back(0)
    back(1)
    wo_loads = [comm.local(wvo.at[:, pl.ds(LANES, HALF)], rts)] + [comm.local(wvop.at[tile_at(i, HALF), pl.ds(LANES, HALF)], two.at[i]) for i in range(DUO)]
    for i in range(DUO):
        comm.store(dqo.at[tile_at(i, ROWS)], grad_x.at[:, tile_at(i, HALF)])
    total = jnp.sum(gacc[...], axis=0, keepdims=True)
    gpart[...] = jnp.zeros_like(gpart)
    for i in range(RING):
        for j in range(RING):
            gpart[i, j:j + 1, :] = total[:, (i * RING + j) * LANES:(i * RING + j + 1) * LANES]
    stage = [comm.send(gpart, gpeer, peer)]
    output_gradients(True)

    def project_out(col, weights, i):
        with scope('project'):
            @pl.loop(DUO * i, DUO * i + DUO)
            def _(j):
                c = tile_at(j, PAIR)
                dst = pl.ds(pl.multiple_of(col + j * PAIR, PAIR), PAIR)
                xs[:, dst] = (xs[:, dst].astype(f32) + dot(onat[...], weights(c))).astype(bf16)
        beat(1.3)

    def own_half(c):
        return rts[:, c]

    def other_half(c):
        return jnp.concatenate([a1[:, c], a2[:, c]], axis=0)

    for c in wo_loads:
        c.wait()
    project_out(core * HALF, own_half, 0)
    for c in stage:
        c.wait_recv()
    for j in range(RING):
        gz[j] = gpart[j] + gpeer[j]
    stage = [comm.send(gz.at[step(comm.pos, 'z', hop)], gz.at[TRIO + hop], comm.far('z', hop)) for hop in (1, DUO, TRIO)]
    project_out(core * HALF, own_half, 1)
    for c in stage:
        c.wait_recv()
    gy[0] = (gz[comm.pos['z']] + gz[RING]) + (gz[5] + gz[6])
    stage = [comm.send(gy.at[0], gy.at[hop], comm.far('y', hop)) for hop in (1, DUO, TRIO)]
    project_out((1 - core) * HALF, other_half, 0)
    for c in stage:
        c.wait_recv()
    gx[0] = (gy[0] + gy[1]) + (gy[DUO] + gy[TRIO])
    stage = [comm.send(gx.at[0], gx.at[hop], comm.far('x', hop)) for hop in (1, DUO, TRIO)]
    project_out((1 - core) * HALF, other_half, 1)
    comm.store(xs, result)
    for c in stage:
        c.wait_recv()
    gpeer[0] = (gx[0] + gx[1]) + (gx[DUO] + gx[TRIO])
    mine = jnp.broadcast_to(gpeer[0, pl.ds(comm.pos['y'], 1), :], (SUBS, LANES))
    gout[...] = pltpu.roll(mine, LANES - (comm.pos['x'] * CHIP + core * SHARE), 1)
    emit(plan.rush(lambda: not plan.stage))
    with scope('finish'):
        sc.finish()
        for c in comm.sent + comm.exchanged:
            c.wait_send()
        for c in comm.stored:
            c.wait()


def tail(qt, do_t, k, kt, v, vt, rt, dyc, wqk, wqkp, wvo, wvop, gain, hidden, dy, pos, cos, sin):
    bf16, f32 = jnp.bfloat16, jnp.float32
    any_ = pl.BlockSpec(memory_space=pl.ANY)
    vmem = pl.BlockSpec(memory_space=pltpu.VMEM)
    S = lambda shape, d=bf16: jax.ShapeDtypeStruct(shape, d)
    V = lambda shape, d=bf16: pltpu.VMEM(shape, d)
    D = lambda n: pltpu.SemaphoreType.DMA((n,))
    sq, tall, wide = (HALF, TOKENS), (TOKENS, LANES), (LANES, TOKENS)
    mine, kv = (ROWS, DIM), (PAIR, TOKENS)
    return pl.pallas_call(
        tail_kernel,
        out_shape=[S(mine), S(mine), S((SHARE, DIM), f32), S((SHARE, PAIR), f32), S((SHARE, PAIR), f32), S((SHARE, DIM), f32), S((SUBS, LANES), f32)],
        in_specs=[any_] * 12 + [vmem] + [any_] * DUO + [vmem] * TRIO,
        out_specs=[any_] * 6 + [vmem],
        scratch_shapes=[V((DUO,) + sq), V(tall), V(wide), V(tall), V(wide), V((DIM, TOKENS)), V((DIM, TOKENS)), V(sq), V(sq), V(kv), V(kv), V(wide, f32), V(wide, f32),
                        V((DUO, TOKENS, QB), f32), V((DUO, TOKENS, QB)), V((DUO, TOKENS, QB)), V((DUO, TOKENS, QB)), V(sq), V((PLACES, RING, RING, RING, CHIP, LANES), f32), V((TRIO, SLOTS, RING, RING, CHIP, LANES), f32),
                        V((TRIO, SLOTS, 6, RING, RING, SHARE, LANES), f32), V((TRIO, SLOTS, 6, RING, SHARE, LANES), f32), V((TRIO, SLOTS, TRIO, CHIP, LANES), f32), V((N_UNITS, CHIP, LANES), f32), V((TOKENS, ROWS)), V(mine), V((DUO * QKV, ROWS)), V(mine),
                        V((SUBS, DIM), f32), V((RING, SUBS, LANES), f32), V((RING, SUBS, LANES), f32), V((7, SUBS, LANES), f32), V((RING, SUBS, LANES), f32), V((RING, SUBS, LANES), f32),
                        D(TRIO * N_UNITS), D(6 * N_UNITS), D(DUO + N_UNITS), D(DUO * HEADS + SHARE), D(DUO * HEADS + SHARE), D(CHIP)],
        compiler_params=pltpu.CompilerParams(collective_id=1, has_side_effects=True, vmem_limit_bytes=67043328),
        name='tail',
    )(qt, do_t, k, kt, v, vt, rt, dyc, wqk, wqkp, wvo, wvop, gain, hidden, dy, pos, cos, sin)


def settle_kernel(n, *refs):
    ins, gain, outs, gain_out, bufs, sems = refs[:n], refs[n], refs[n + 1:DUO * n + 1], refs[DUO * n + 1], refs[DUO * n + DUO:-1], refs[-1]
    jobs = []
    for a, o, b in zip(ins, outs, bufs):
        size = a.shape[0] // RING if a.shape[0] == ROWS else a.shape[0]
        jobs += [tuple(r.at[pl.ds(i, size)] for r in (a, b, o)) for i in range(0, a.shape[0], size)]
    takes = [pltpu.make_async_copy(a, b, sems.at[0, i]) for i, (a, b, _) in enumerate(jobs)]
    puts = [pltpu.make_async_copy(b, o, sems.at[1, i]) for i, (_, b, o) in enumerate(jobs)]
    for c in takes:
        c.start()
    gain_out[...] = gain[0:1, :SHARE]
    for take, put in zip(takes, puts):
        take.wait()
        put.start()
    for c in puts:
        c.wait()


def settle(*arrays):
    *large, gain = arrays
    any_, vmem = pl.BlockSpec(memory_space=pl.ANY), pl.BlockSpec(memory_space=pltpu.VMEM)
    return pl.pallas_call(
        functools.partial(settle_kernel, len(large)),
        out_shape=[jax.ShapeDtypeStruct(a.shape, a.dtype) for a in large] + [jax.ShapeDtypeStruct((1, SHARE), gain.dtype)],
        in_specs=[any_] * len(large) + [vmem],
        out_specs=[any_] * len(large) + [vmem],
        scratch_shapes=[pltpu.VMEM(a.shape, a.dtype) for a in large] + [pltpu.SemaphoreType.DMA((DUO, 12))],
        name='settle',
    )(*arrays)


def rope_tables():
    j = np.arange(HEAD_DIM // DUO, dtype=np.float64) / (HEAD_DIM // DUO)
    freq = (ROPE_THETA ** -j).astype(np.float32)
    angle = freq[:, None] * np.arange(TOKENS, dtype=np.float32)[None, :]
    return np.cos(angle.astype(np.float64)).astype(np.float32), np.sin(angle.astype(np.float64)).astype(np.float32)


def solution(mesh):
    def shard_fn(hidden, tok_pos, grad_out, norm_gain, w_query, w_key, w_value, w_out):
        hidden, grad_out = hidden[0], grad_out[0]
        cos_t, sin_t = (jnp.asarray(t) for t in rope_tables())
        *parts, gain = head(hidden, grad_out, w_query, w_key, w_value, w_out, tok_pos, norm_gain.reshape(1, SHARE), cos_t, sin_t)
        parts = [p.reshape(DIM, GROUP) if p.ndim > DUO else p for p in parts]
        result, grad_hidden, gq, gk, gv, go, gout = settle(*tail(*parts, gain, hidden, grad_out, tok_pos, cos_t, sin_t))
        return result[None], grad_hidden[None], gq, gk, gv, go, gout.reshape(SHARE)

    row_spec, pos_spec = P('fsdp', 'cp', None), P('fsdp', 'cp')
    weight_spec, gain_spec = P(('fsdp', 'cp'), None), P(('fsdp', 'cp'))
    return jax.shard_map(shard_fn, mesh=mesh, in_specs=(row_spec, pos_spec, row_spec, gain_spec, weight_spec, weight_spec, weight_spec, weight_spec), out_specs=(row_spec, row_spec, weight_spec, weight_spec, weight_spec, weight_spec, gain_spec), check_vma=False)
```

```python
import functools
import jax
import jax.numpy as jnp
import numpy as np
from jax import lax
from jax.experimental import pallas as pl
from jax.experimental.pallas import tpu as pltpu
from jax.sharding import PartitionSpec as P

LANES, SUBS, RING, TRIO, DUO = 128, 8, 4, 3, 2
PAIR, ROWS, CHIP, SHARE, TURN = 256, 512, 32, 16, 64
HEAD_DIM = LANES
ROPE_THETA = 1000000.0
RMS_EPS = 1e-5
SCALE = HEAD_DIM ** -0.5
LOG2E = 1.4426950408889634

MESH = pl.DeviceIdType.MESH
AXES = ('x', 'y', 'z')
ORDERS = (('x', 'y', 'z'), ('y', 'z', 'x'), ('z', 'x', 'y'))
ALL = pl.ds(0, RING)


def torus():
    f = lax.axis_index('fsdp')
    return {'x': lax.rem(f, RING), 'y': lax.rem(lax.div(f, RING), RING), 'z': lax.div(f, SHARE)}


def step(pos, axis, hop):
    return lax.rem(pos[axis] + hop, RING)


class Batch:
    def __init__(self, comm):
        self.comm, self.index = comm, comm.used
        comm.used += 1

    def _copy(self, src, dst, device):
        send, recv, _ = self.comm.sems
        return pltpu.make_async_remote_copy(src_ref=src, dst_ref=dst, send_sem=send.at[self.index], recv_sem=recv.at[self.index], device_id=device, device_id_type=MESH)

    def send(self, src, dst, device):
        self._copy(src, dst, device).start()
        return self

    def arrived(self, whole):
        self._copy(whole, whole, self.comm.peer()).wait_recv()

    def sent(self, whole):
        self._copy(whole, whole, self.comm.peer()).wait_send()


class Comm:
    def __init__(self, send_sems, recv_sems, local_sems):
        self.pos = torus()
        self.core = lax.axis_index('cp')
        self.sems = (send_sems, recv_sems, local_sems)
        self.used = self.used_local = 0
        self.stored = []

    def far(self, axis, hop):
        p = dict(self.pos)
        p[axis] = step(self.pos, axis, hop)
        return {'fsdp': (p['z'] * RING + p['y']) * RING + p['x'], 'cp': self.core}

    def peer(self):
        return {'fsdp': lax.axis_index('fsdp'), 'cp': 1 - self.core}

    def announce(self):
        sem = pltpu.get_barrier_semaphore()
        for axis in AXES:
            for hop in (1, DUO, TRIO):
                pl.semaphore_signal(sem, inc=1, device_id=self.far(axis, hop), device_id_type=MESH)
        pl.semaphore_signal(sem, inc=1, device_id=self.peer(), device_id_type=MESH)

    def meet(self):
        pl.semaphore_wait(pltpu.get_barrier_semaphore(), 10)

    def ring(self, batch, src, slots, axis):
        for hop in (1, DUO, TRIO):
            batch.send(src, slots.at[hop], self.far(axis, hop))

    def local(self, src, dst):
        i = self.used_local
        self.used_local += 1
        c = pltpu.make_async_copy(src, dst, self.sems[DUO].at[i])
        c.start()
        return c

    def store(self, src, dst):
        self.stored.append(self.local(src, dst))


class OldComm:
    def __init__(self, send_sems, recv_sems, local_sems):
        self.pos = torus()
        self.core = lax.axis_index('cp')
        self.sems = (send_sems, recv_sems, local_sems)
        self.used = self.used_local = 0
        self.sent, self.exchanged, self.stored = [], [], []

    def far(self, axis, hop):
        p = dict(self.pos)
        p[axis] = step(self.pos, axis, hop)
        return {'fsdp': (p['z'] * RING + p['y']) * RING + p['x'], 'cp': self.core}

    def peer(self):
        return {'fsdp': lax.axis_index('fsdp'), 'cp': 1 - self.core}

    def announce(self):
        sem = pltpu.get_barrier_semaphore()
        for axis in AXES:
            for hop in (1, DUO, TRIO):
                pl.semaphore_signal(sem, inc=1, device_id=self.far(axis, hop), device_id_type=MESH)
        pl.semaphore_signal(sem, inc=1, device_id=self.peer(), device_id_type=MESH)

    def meet(self):
        pl.semaphore_wait(pltpu.get_barrier_semaphore(), 10)

    def barrier(self):
        self.announce()
        self.meet()

    def _copy(self, src, dst, device):
        i = self.used
        self.used += 1
        c = pltpu.make_async_remote_copy(src_ref=src, dst_ref=dst, send_sem=self.sems[0].at[i], recv_sem=self.sems[1].at[i], device_id=device, device_id_type=MESH)
        c.start()
        return c

    def send(self, src, dst, device):
        c = self._copy(src, dst, device)
        self.sent.append(c)
        return c

    def trade(self, src, dst):
        self.exchanged.append(self._copy(src, dst, self.peer()))

    def local(self, src, dst):
        i = self.used_local
        self.used_local += 1
        c = pltpu.make_async_copy(src, dst, self.sems[DUO].at[i])
        c.start()
        return c

    def store(self, src, dst):
        self.stored.append(self.local(src, dst))

    def finish(self):
        for c in self.sent:
            c.wait_send()
        for c in self.exchanged:
            c.wait_send()
            c.wait_recv()
        for c in self.stored:
            c.wait()


def pick(ref, sel, cols):
    return ref.at[sel['z'], sel['y'], sel['x'], :, pl.ds(cols[0], cols[1])]


def sem_scratch(remote, local):
    return [pltpu.SemaphoreType.DMA((remote,)), pltpu.SemaphoreType.DMA((remote,)), pltpu.SemaphoreType.DMA((local,))]


def add_into(dst, *srcs, fresh=False):
    def add(idx):
        total, *rest = [s[idx] for s in (srcs if fresh else (dst,) + srcs)]
        for more in rest:
            total = total + more
        dst[idx] = total

    if len(dst.shape) > TRIO:
        @pl.loop(0, dst.shape[0])
        def _(i):
            add((i,))
    else:
        add(Ellipsis)


QK_COLORS = ((0, PAIR, LANES), (384, LANES, PAIR), (768, PAIR, LANES))
VO_COLORS = ((0, LANES, PAIR), (384, PAIR, LANES), (768, LANES, PAIR))
TOKENS = 1024
DIM = 2048
HALF = 1024
QKV = 1280
GROUP = 1152


def scope(name):
    return jax.named_scope(name)


def dot(a, b):
    return jnp.dot(a, b, preferred_element_type=jnp.float32)


def dot_nt(a, b):
    return lax.dot_general(a, b, (((1,), (1,)), ((), ())), preferred_element_type=jnp.float32)


def tile_at(i, n):
    return pl.ds(pl.multiple_of(i * n, n), n)


class Gather:
    def __init__(self, comm, ref, colors, land):
        self.comm, self.ref, self.colors, self.land = comm, ref, colors, land
        self.held = [dict(comm.pos) for _ in colors]
        self.batches = []

    def parts(self, k):
        lo, na, nb = self.colors[k]
        return (lo, na), (lo + na, nb)

    def move(self, batch, s, cols, to):
        batch.send(pick(self.ref, s, cols), pick(self.ref, s, cols), to)

    def at(self, k, hop):
        d = ORDERS[k][self.phase]
        return dict(self.held[k], **{d: step(self.comm.pos, d, hop)})

    def begin(self, phase):
        self.phase = phase
        self.up, self.dn, self.rest = ([Batch(self.comm) for _ in range(TRIO)] for _ in range(TRIO))
        self.batches += self.up + self.dn + self.rest
        for k in range(TRIO):
            a, b = self.parts(k)
            d = ORDERS[k][phase]
            up, dn, s = self.comm.far(d, 1), self.comm.far(d, TRIO), self.held[k]
            self.move(self.up[k], s, a, up)
            self.move(self.dn[k], s, b, dn)
            self.move(self.rest[k], s, b, up)
            self.move(self.rest[k], s, a, dn)
            if phase == 0:
                for cols in (a, b):
                    self.move(self.rest[k], s, cols, self.comm.far(d, DUO))
        if phase == DUO:
            for k in range(TRIO):
                for cols in self.parts(k):
                    self.land(self.ref, self.held[k], cols)

    def forward(self):
        for k in range(TRIO):
            a, b = self.parts(k)
            d = ORDERS[k][self.phase]
            for batch, hop, cols, to in ((self.up[k], TRIO, a, 1), (self.dn[k], 1, b, TRIO)):
                s = self.at(k, hop)
                batch.arrived(pick(self.ref, s, cols))
                if self.phase:
                    self.move(self.rest[k], s, cols, self.comm.far(d, to))
                if self.phase == DUO:
                    self.land(self.ref, s, cols)

    def end(self):
        for k in range(TRIO):
            a, b = self.parts(k)
            d = ORDERS[k][self.phase]
            two = dict(self.held[k], **{d: pl.ds(0, DUO)})
            self.rest[k].arrived(pick(self.ref, two, (a[0], a[1] + b[1])))
            if self.phase == DUO:
                for hop, cols in ((TRIO, b), (1, a), (DUO, a), (DUO, b)):
                    self.land(self.ref, self.at(k, hop), cols)
            for batch, s, cols in ((self.up[k], self.held[k], a), (self.dn[k], self.held[k], b), (self.rest[k], two, (a[0], a[1] + b[1]))):
                batch.spent = pick(self.ref, s, cols)
            self.held[k] = dict(self.held[k], **{d: ALL})

    def finish(self):
        for batch in self.batches:
            batch.sent(batch.spent)


def head_kernel(hidden, dy, wq, wk, wv, wo, pos, gain_in, cos_t, sin_t,
                qt_o, dot_o, k_o, kt_o, v_o, vt_o, rt_o, dyc_o, wqk_o, wqkp_o, wvo_o, wvop_o, gain_o,
                hid2, dy2, dys, rs, rt, wqk, wvo, wpeer, pi, pos2, qt, dot_s, kk, kt, vv, vt, gain, gtile, gbuf, gx, gy, gz, *sems):
    comm = Comm(*sems)
    pos_c, core = comm.pos, comm.core
    bf16, f32 = jnp.bfloat16, jnp.float32
    peer = comm.peer()
    rows = tile_at(core, SHARE)
    mine_qk = wqk.at[pos_c['z'], pos_c['y'], pos_c['x'], rows]
    mine_vo = wvo.at[pos_c['z'], pos_c['y'], pos_c['x'], rows]

    def weight_parts(c):
        return ((wq.at[:, tile_at(c, HALF)], mine_qk.at[:, pl.ds(0, HALF)]), (wk.at[:, tile_at(c, LANES)], mine_qk.at[:, pl.ds(HALF, LANES)]),
                (wv.at[:, tile_at(c, LANES)], mine_vo.at[:, pl.ds(0, LANES)]), (wo.at[:, tile_at(c, HALF)], mine_vo.at[:, pl.ds(LANES, HALF)]))

    loads = [comm.local(s, d) for s, d in weight_parts(core)]
    load_x = [comm.local(hidden, hid2.at[pl.ds(0, ROWS)]), comm.local(dy, dy2.at[pl.ds(0, ROWS)])]
    share = lax.broadcasted_iota(jnp.int32, (SUBS, LANES), 1) // SHARE
    gtile[...] = jnp.where(share == pos_c['x'] * DUO + core, jnp.broadcast_to(jnp.concatenate([gain_in[...]] * SUBS, axis=1), (SUBS, LANES)), 0.0)
    comm.announce()
    with scope('entry'):
        comm.meet()
    swap_w, swap_pos, swap_dy, swap_x, peers_qk, peers_vo = (Batch(comm) for _ in range(6))
    gain_c, gain_x, gain_y, gain_z = (Batch(comm) for _ in range(RING))
    for s, d in weight_parts(1 - core):
        swap_w.send(s, d, peer)
    gain_c.send(gtile, gbuf, peer)
    swap_pos.send(pos, pos2, peer)
    for c in loads:
        c.wait()
    with scope('wait_w'):
        swapped = wqk.at[pos_c['z'], pos_c['y'], pos_c['x']]
        swap_w.arrived(swapped)

    def land_qk(ref, s, cols):
        peers_qk.send(pick(ref, s, cols), pick(wqkp_o, s, cols), peer)

    def land_vo(ref, s, cols):
        peers_vo.send(pick(ref, s, cols), pick(wpeer, s, cols), peer)

    g1 = Gather(comm, wqk, QK_COLORS, land_qk)
    g2 = Gather(comm, wvo, VO_COLORS, land_vo)
    g1.begin(0)
    g2.begin(0)
    swap_dy.send(dy, dy2.at[pl.ds(ROWS, ROWS)], peer)
    gain_c.arrived(gbuf)
    gx[0] = gtile[...] + gbuf[...]
    comm.ring(gain_x, gx.at[0], gx, 'x')

    swap_pos.arrived(pos2)

    @pl.loop(0, TOKENS // LANES)
    def _(i):
        want = lax.broadcasted_iota(jnp.int32, (LANES, ROWS), 0) + i * LANES
        for h, have in enumerate((pos, pos2)):
            pi[tile_at(i, LANES), h * ROWS:(h + 1) * ROWS] = jnp.where(want == have[...], 1.0, 0.0).astype(bf16)

    def sort(dst, src, first, last):
        with scope('sort'):
            @pl.loop(first, last)
            def _(j):
                c = tile_at(j, PAIR)
                dst[:, c] = dot(pi[...], src[:, c]).astype(bf16)

    with scope('p0_end'):
        for g in (g1, g2):
            g.forward()
            g.end()
    g1.begin(1)
    g2.begin(1)
    swap_x.send(hidden, hid2.at[pl.ds(ROWS, ROWS)], peer)
    with scope('p0_gain'):
        gain_x.arrived(gx.at[pl.ds(1, TRIO)])
    gy[pos_c['y']] = (gx[0] + gx[1]) + (gx[DUO] + gx[TRIO])
    for hop in (1, DUO, TRIO):
        gain_y.send(gy.at[pos_c['y']], gy.at[pos_c['y']], comm.far('y', hop))
    with scope('wait_dy'):
        load_x[1].wait()
        swap_dy.arrived(dy2.at[pl.ds(ROWS, ROWS)])
    sort(dys, dy2, 0, 5)
    with scope('p1_fwd'):
        g1.forward()
        g2.forward()
    gain_y.arrived(gy.at[pl.ds(1, TRIO)])
    for j in range(RING):
        gz[pos_c['z'], j] = gy[j]
    for hop in (1, DUO, TRIO):
        gain_z.send(gz.at[pos_c['z']], gz.at[pos_c['z']], comm.far('z', hop))
    sort(dys, dy2, 5, SUBS)
    comm.store(dys.at[:, tile_at(core, HALF)], dyc_o)
    with scope('p1_end'):
        g1.end()
        g1.begin(DUO)
        g2.end()
    with scope('wait_x'):
        load_x[0].wait()
        swap_x.arrived(hid2.at[pl.ds(ROWS, ROWS)])
    sort(rs, hid2, 0, SUBS)
    with scope('gain'):
        gain_z.arrived(gz.at[pl.ds(1, TRIO)])
    for i in range(RING):
        for j in range(RING):
            gain[:, (i * RING + j) * LANES:(i * RING + j + 1) * LANES] = gz[i, j]
    comm.store(gain, gain_o)

    def norm(first, last):
        with scope('norm'):
            @pl.loop(first, last)
            def _(i):
                r = tile_at(i, CHIP)
                x = rs[r, :].astype(f32)
                inv = lax.rsqrt(jnp.mean(x * x, axis=-1, keepdims=True) + RMS_EPS)
                rs[r, :] = (x * inv * gain[0:1, :]).astype(bf16)

    with scope('p2q_fwd'):
        g1.forward()
    g2.begin(DUO)
    norm(0, TOKENS // CHIP)
    with scope('r_t'):
        @pl.loop(0, DIM // PAIR)
        def _(i):
            c = tile_at(i, PAIR)

            @pl.loop(0, TOKENS // PAIR)
            def _(j):
                r = tile_at(j, PAIR)
                rt[c, r] = rs[r, c].T
    comm.store(rt, rt_o)
    with scope('p2q_end'):
        g1.end()
    comm.store(wqk, wqk_o)
    w_qk, w_vo, w_peer = wqk.reshape(DIM, GROUP), wvo.reshape(DIM, GROUP), wpeer.reshape(DIM, GROUP)

    def rotated(x, r):
        cos, sin = cos_t[:, r], sin_t[:, r]
        cos = jnp.concatenate([cos, cos], axis=0).T
        sin = jnp.concatenate([-sin, sin], axis=0).T
        return (x * cos + pltpu.roll(x, TURN, 1) * sin).astype(bf16)

    def queries(first, last):
        with scope('q'):
            @pl.loop(first, last)
            def _(t):
                x = dot(rs[...], w_qk[:, tile_at(t, PAIR)])
                for i in range(RING):
                    r = slice(i * PAIR, (i + 1) * PAIR)
                    for h in range(DUO):
                        qt[tile_at(DUO * t + h, LANES), r] = rotated(x[r, h * LANES:(h + 1) * LANES], r).T

    queries(0, DUO)
    with scope('p2o_fwd'):
        g2.forward()
    queries(DUO, RING)

    @pl.loop(0, DUO)
    def _(i):
        r = tile_at(i, ROWS)
        key = rotated(dot(rs[r, :], w_qk[:, HALF:]), r)
        kk[r, :] = key
        kt[:, r] = key.T
    for src, dst in ((kk, k_o), (kt, kt_o), (qt, qt_o)):
        comm.store(src, dst)
    with scope('p2o_end'):
        g2.end()
    with scope('vals'):
        @pl.loop(0, DUO)
        def _(i):
            r = tile_at(i, ROWS)
            val = dot(rs[r, :], w_vo[:, :LANES]).astype(bf16)
            vv[r, :] = val
            vt[:, r] = val.T
    for src, dst in ((vv, v_o), (vt, vt_o)):
        comm.store(src, dst)
    with scope('wo_peer'):
        peers_vo.arrived(wpeer)
    comm.store(wvo, wvo_o)
    comm.store(wpeer, wvop_o)

    with scope('do_t'):
        r = tile_at(core, HALF)

        @pl.loop(0, TOKENS // PAIR)
        def _(j):
            t = tile_at(j, PAIR)
            w_rows = jnp.concatenate([w_vo[r, LANES:], w_peer[r, LANES:]], axis=1)
            d_rows = jnp.concatenate([dys[t, tile_at(core, HALF)], dys[t, tile_at(1 - core, HALF)]], axis=1)
            dot_s[:, t] = dot_nt(w_rows, d_rows).astype(bf16)
    comm.store(dot_s, dot_o)
    with scope('finish'):
        peers_qk.arrived(wqk)
        for batch, whole in ((swap_w, swapped), (swap_pos, pos2), (swap_dy, dy2.at[pl.ds(ROWS, ROWS)]), (swap_x, hid2.at[pl.ds(ROWS, ROWS)]), (peers_qk, wqk), (peers_vo, wvo),
                             (gain_c, gbuf), (gain_x, gx.at[pl.ds(1, TRIO)]), (gain_y, gy.at[pl.ds(1, TRIO)]), (gain_z, gz.at[pl.ds(1, TRIO)])):
            batch.sent(whole)
        g1.finish()
        g2.finish()
        for c in comm.stored:
            c.wait()


def head(hidden, dy, wq, wk, wv, wo, pos, gain, cos_t, sin_t):
    bf16, f32 = jnp.bfloat16, jnp.float32
    any_ = pl.BlockSpec(memory_space=pl.ANY)
    vmem = pl.BlockSpec(memory_space=pltpu.VMEM)
    S = lambda shape, d=bf16: jax.ShapeDtypeStruct(shape, d)
    V = lambda shape, d=bf16: pltpu.VMEM(shape, d)
    group = (RING, RING, RING, CHIP, GROUP)
    sq, tall, wide = (HALF, TOKENS), (TOKENS, LANES), (LANES, TOKENS)
    full = (TOKENS, DIM)
    return pl.pallas_call(
        head_kernel,
        out_shape=[S(sq), S(sq), S(tall), S(wide), S(tall), S(wide), S((DIM, TOKENS)), S((TOKENS, HALF)), S(group), S(group), S(group), S(group), S((SUBS, DIM), f32)],
        in_specs=[any_] * 6 + [vmem] * RING,
        out_specs=[any_] * 13,
        scratch_shapes=[V(full), V(full), V(full), V(full), V((DIM, TOKENS)), V(group), V(group), V(group), V((TOKENS, TOKENS)), V((1, ROWS), jnp.int32),
                        V(sq), V(sq), V(tall), V(wide), V(tall), V(wide), V((SUBS, DIM), f32), V((SUBS, LANES), f32), V((SUBS, LANES), f32), V((RING, SUBS, LANES), f32), V((RING, SUBS, LANES), f32), V((RING, RING, SUBS, LANES), f32)] + sem_scratch(TURN, 18),
        compiler_params=pltpu.CompilerParams(collective_id=0, has_side_effects=True, vmem_limit_bytes=60 * DUO**20),
        name='head',
    )(hidden, dy, wq, wk, wv, wo, pos, gain, cos_t, sin_t)


HEADS = SUBS
UNIT_K, UNIT_V = SUBS, 9
N_UNITS = 18
SLOTS = RING
LAST = 5
ABREAST = DUO
LINES = ((0, TRIO, 6, 9, 12, 15), (1, RING, 7, 10, 13, SHARE), (DUO, 5, SUBS, 11, 14, 17))
COLOR = {u: k for k, line in enumerate(LINES) for u in line}
RANK = {u: i for line in LINES for i, u in enumerate(line)}
BEFORE = {u: line[i - SLOTS] if i >= SLOTS else None for line in LINES for i, u in enumerate(line)}
PLACES = 12
PLACE = {u: u % PLACES for u in range(N_UNITS)}
WIRE = (2.85, 0.72, 0.36)
LATENCY = 2.6
STAGE_COST = 0.1


class Plan:
    def __init__(self):
        self.now, self.stage, self.ready, self.order, self.link = 0.0, {}, {}, [], {}
        self.mark = {}

    def _wire(self, u, phase, count):
        link = ORDERS[COLOR[u]][phase]
        t = max(self.link.get(link, 0.0), self.now)
        first = t + WIRE[phase] + LATENCY
        self.link[link] = t + WIRE[phase] * count
        return first if phase < DUO else self.link[link] + LATENCY

    def free(self, u, phase):
        if BEFORE[u] is None:
            return True
        done = self.mark.get((BEFORE[u], (DUO, RING, 5)[phase]))
        if done is None:
            return False
        sent = ((0, 1), (DUO, TRIO), (RING,))[phase]
        return any(self.mark.get((j, s), -1) > done and (j, s + 1) in self.mark for j in LINES[COLOR[u]] for s in sent)

    def run(self, u):
        stage = self.stage[u]
        self.order.append((u, stage))
        self.mark[u, stage] = len(self.order)
        self.now = max(self.now, self.ready[u]) + STAGE_COST
        self.stage[u] = stage + 1
        if stage == LAST:
            del self.stage[u]
        elif stage % DUO:
            self.ready[u] = self._wire(u, stage // DUO, 1)
        else:
            self.ready[u] = self._wire(u, stage // DUO, DUO)

    def blocked(self, u):
        stage = self.stage[u]
        if stage == 0 and sum(0 < self.stage.get(j, 0) <= DUO for j in LINES[COLOR[u]]) >= ABREAST:
            return True
        if stage == DUO and BEFORE[u] is not None and (BEFORE[u], LAST) not in self.mark:
            return True
        return stage in (0, DUO, RING) and not self.free(u, stage // DUO)

    def start(self, u):
        self.stage[u], self.ready[u] = 0, self.now

    def due(self):
        first = len(self.order)
        while True:
            ripe = [(self.ready[u], u) for u in self.stage if self.ready[u] <= self.now and not self.blocked(u)]
            if not ripe:
                return self.order[first:]
            self.run(min(ripe)[1])

    def vacated(self, u):
        return (u, DUO) in self.mark

    def rush(self, done):
        first = len(self.order)
        while not done():
            self.run(min((self.ready[u], u) for u in self.stage if not self.blocked(u))[1])
        return self.order[first:]


QB = PAIR
NBLK = TOKENS // QB
HALVES = (pl.ds(0, SHARE), pl.ds(SHARE, SHARE))


class Scatter:
    def __init__(self, comm, part, mid, bufs, fin, outs, send_sems, recv_sems, swap_sems):
        self.pos, self.part, self.mid, self.bufs, self.fin, self.outs = comm.pos, part, mid, bufs, fin, outs
        self.send_sems, self.recv_sems, self.swap_sems = send_sems, recv_sems, swap_sems
        self.near = {(a, hop): comm.far(a, hop) for a in AXES for hop in (1, DUO, TRIO)}
        self.hops = {(a, hop): step(comm.pos, a, hop) for a in AXES for hop in (1, DUO, TRIO)}
        self.peer, self.core = comm.peer(), comm.core
        self.keep, self.give = tile_at(comm.core, SHARE), tile_at(1 - comm.core, SHARE)
        self.drained = set()

    def slot(self, u):
        return COLOR[u], RANK[u] % SLOTS

    def buf(self, u, phase):
        return self.bufs[phase].at[self.slot(u)]

    def view(self, u, phase, hop, half=None):
        order = ORDERS[COLOR[u]]
        at = {a: ALL for a in AXES}
        for a in order[1:phase]:
            at[a] = self.pos[a]
        at[order[phase]] = self.hops[order[phase], hop] if hop else self.pos[order[phase]]
        rows = pl.ds(0, CHIP) if half is None else HALVES[half]
        if phase == 0:
            return self.part.at[PLACE[u], at['z'], at['y'], at['x'], rows, :]
        return self.mid.at[self.slot(u) + tuple(at[a] for a in 'zyx' if a != order[0]) + (rows, slice(None))]

    def copy(self, src, dst, sems, device):
        return pltpu.make_async_remote_copy(src_ref=src, dst_ref=dst, send_sem=sems[0], recv_sem=sems[1], device_id=device, device_id_type=MESH)

    def sems(self, u, phase, kind=0):
        at = u * TRIO + phase
        return self.send_sems.at[at], self.recv_sems.at[DUO * at + kind]

    def send(self, u, phase, name):
        axis = ORDERS[COLOR[u]][phase]
        if phase == DUO:
            src, to = self.view(u, DUO, name + 1), name + 1
        else:
            hop, half, to = ((DUO, 0, 1), (DUO, 1, TRIO), (1, 1, 1), (TRIO, 0, TRIO), (1, 0, 1), (TRIO, 1, TRIO))[name]
            src = self.view(u, phase, hop, half)
        self.copy(src, self.buf(u, phase).at[name], self.sems(u, phase, int(name > 1 and phase < DUO)), self.near[axis, to]).start()

    def launch(self, u, phase):
        if BEFORE[u] is not None:
            self.drain(BEFORE[u], phase)
        for name in range(RING if phase < DUO else TRIO):
            self.send(u, phase, name)

    def arrived(self, u, phase, first, count):
        whole = self.buf(u, phase).at[pl.ds(first, count)]
        self.copy(whole, whole, self.sems(u, phase, int(first > 0)), self.peer).wait_recv()

    def drain(self, u, phase):
        if (u, phase) not in self.drained:
            self.drained.add((u, phase))
            whole = self.buf(u, phase)
            self.copy(whole, whole, self.sems(u, phase), self.peer).wait_send()

    def out(self, u):
        if u < HEADS:
            out, col = self.outs[0], self.core * HALF + u * LANES
        elif u < 10:
            out, col = self.outs[u - 7], self.core * LANES
        else:
            out, col = self.outs[TRIO], self.core * HALF + (u - 10) * LANES
        return out.at[:, pl.ds(pl.multiple_of(col, LANES), LANES)]

    def kept(self, u):
        return pltpu.make_async_copy(self.fin.at[u, self.keep], self.out(u), self.swap_sems.at[DUO + u])

    def run(self, u, stage):
        if stage == 0:
            return self.launch(u, 0)
        phase = (stage - 1) // DUO
        if stage == LAST:
            self.arrived(u, DUO, 0, TRIO)
            got = self.buf(u, DUO)
            self.fin[u] = self.view(u, DUO, 0)[...] + (got[0] + got[1] + got[DUO])
            self.copy(self.fin.at[u, self.give], self.out(u), (self.swap_sems.at[0], self.swap_sems.at[1]), self.peer).start()
            self.kept(u).start()
            return
        got = self.buf(u, phase)
        if stage % DUO:
            self.arrived(u, phase, 0, DUO)
            for name, hop in ((0, 1), (1, TRIO)):
                add_into(self.view(u, phase, hop, name), got.at[name])
                self.send(u, phase, name + RING)
            return
        self.arrived(u, phase, DUO, RING)
        if phase == 0 and BEFORE[u] is not None:
            self.drain(BEFORE[u], 1)
            self.drain(BEFORE[u], DUO)
        for half, names in ((0, (TRIO, RING)), (1, (DUO, 5))):
            if phase:
                add_into(self.view(u, phase, 0, half), *[got.at[name] for name in names])
            else:
                dst = self.mid.at[self.slot(u) + (ALL, ALL, HALVES[half], slice(None))]
                add_into(dst, self.view(u, 0, 0, half), *[got.at[name] for name in names], fresh=True)
        self.launch(u, phase + 1)

    def finish(self):
        for u in range(N_UNITS):
            for phase in range(TRIO):
                self.drain(u, phase)
        half = self.fin.at[:, pl.ds(0, SHARE)]
        swaps = self.copy(half, half, (self.swap_sems.at[0], self.swap_sems.at[1]), self.peer)
        swaps.wait_send()
        swaps.wait_recv()
        for u in range(N_UNITS):
            self.kept(u).wait()


def attend(heads, qt, do_t, k, kt, v, vt, cos, sin, o_row, ot, dq, dkt, dvt, s_scr, e_scr, p_scr, d_scr):
    f32, bf16 = jnp.float32, jnp.bfloat16
    strip = TURN
    work = [(h, j) for j in range(NBLK) for h in range(len(heads))]

    def strips(c):
        return [(i * strip, slice(c * QB + i * strip, c * QB + (i + 1) * strip)) for i in range(QB // strip)]

    def fold(x, op):
        return op(x.reshape(strip // SUBS, SUBS, QB), axis=0)

    def scores(i):
        (h, j), b = work[i], i % DUO
        q_t = qt[heads[h], j * QB:(j + 1) * QB]
        top = jnp.full((SUBS, QB), -jnp.inf, f32)
        for c in range(j + 1):
            tile = dot(k[c * QB:(c + 1) * QB, :], q_t)
            for at, rows in strips(c):
                s = tile[at:at + strip]
                if c == j:
                    seen = lax.broadcasted_iota(jnp.int32, (strip, QB), 0) + at <= lax.broadcasted_iota(jnp.int32, (strip, QB), 1)
                    s = jnp.where(seen, s, -jnp.inf)
                s_scr[b, rows, :] = s
                top = jnp.maximum(top, fold(s, jnp.max))
        return jnp.max(top, axis=0, keepdims=True)

    def rest(i, m):
        (h, j), b = work[i], i % DUO
        cols, n = slice(j * QB, (j + 1) * QB), (j + 1) * QB
        q_t, d_t = qt[heads[h], cols], do_t[heads[h], cols]
        tot = jnp.zeros((SUBS, QB), f32)
        for c in range(j + 1):
            for at, rows in strips(c):
                e = jnp.exp2((s_scr[b, rows, :] - m) * (SCALE * LOG2E))
                s_scr[b, rows, :] = e
                e_scr[b, rows, :] = e.astype(bf16)
                tot = tot + fold(e, jnp.sum)
        den = jnp.sum(tot, axis=0, keepdims=True)
        inv = 1.0 / den
        o = (dot(vt[:, :n], e_scr[b, :n, :]) / den).astype(bf16)
        ot[o_row(h), cols] = o
        delta = jnp.sum(d_t.astype(f32) * o.astype(f32), axis=0, keepdims=True)
        for c in range(j + 1):
            dp = dot(v[c * QB:(c + 1) * QB, :], d_t)
            for at, rows in strips(c):
                p = s_scr[b, rows, :] * inv
                p_scr[b, rows, :] = p.astype(bf16)
                d_scr[b, rows, :] = (p * (dp[at:at + strip] - delta)).astype(bf16)
        dvt[:, :n] += dot_nt(d_t, p_scr[b, :n, :])
        dkt[:, :n] += dot_nt(q_t, d_scr[b, :n, :])
        g = dot(kt[:, :n], d_scr[b, :n, :]) * SCALE
        co, si = cos[:, cols], sin[:, cols]
        x, y = g[:TURN], g[TURN:]
        dq[heads[h], cols] = jnp.concatenate([x * co + y * si, y * co - x * si], axis=0).astype(bf16)

    m = scores(0)
    for i in range(len(work)):
        later = scores(i + 1) if i + 1 < len(work) else None
        rest(i, m)
        m = later


def tail_kernel(qt, do_t, k, kt, v, vt, rt, dyc, wqk, wqkp, wvo, wvop, gain, hidden, dy, pos, cos, sin,
                result, grad_x, gq, gk, gv, go, gout,
                two, ks, kts, vs, vts, rts, ots, dqo, dqp, dkvo, dkvp, dkt, dvt, s_scr, e_scr, p_scr, d_scr, dycs, part, mid, buf1, buf2, buf3, fin, own, onat, dnat, xs, gacc, gpart, gpeer, gz, gy, gx,
                send_sems, recv_sems, swap_sems, trade_send, trade_recv, local_sems):
    comm = OldComm(trade_send, trade_recv, local_sems)
    comm.used = DUO * HEADS
    f32, bf16 = jnp.float32, jnp.bfloat16
    core, peer = comm.core, comm.peer()
    a1, a2 = two.at[0], two.at[1]
    comm.announce()
    sc = Scatter(comm, part, mid, (buf1, buf2, buf3), fin, (gq, gk, gv, go), send_sems, recv_sems, swap_sems)
    plan = Plan()
    some, most = pl.ds(0, PAIR), pl.ds(PAIR, HALF - PAIR)
    loads = [comm.local(s, d) for s, d in ((qt.at[some], two.at[0, some]), (k, ks), (do_t.at[some], two.at[1, some]), (vt, vts), (v, vs), (kt, kts))]
    dkt[...] = jnp.zeros_like(dkt)
    dvt[...] = jnp.zeros_like(dvt)
    with scope('wait_q'):
        for c in loads:
            c.wait()
    loads = [comm.local(s, d) for s, d in ((rt, rts), (qt.at[most], two.at[0, most]), (do_t.at[most], two.at[1, most]))]
    later = [comm.local(s, d) for s, d in ((dyc, dycs), (hidden, xs))]

    def emit(stages):
        for u, stage in stages:
            with scope(f'u{u}_s{stage}'):
                sc.run(u, stage)

    def after(cost):
        plan.now += cost
        return plan.due()

    def head_trades(h):
        row = tile_at(core * HEADS + h, LANES)
        mine = tile_at(h, LANES)
        return [pltpu.make_async_remote_copy(src_ref=s, dst_ref=d, send_sem=trade_send.at[i], recv_sem=trade_recv.at[i], device_id=peer, device_id_type=MESH)
                for s, d, i in ((ots.at[row], ots.at[row], h), (dqo.at[mine], dqp.at[mine], HEADS + h))]

    def gradient(place, left, right, mul):
        with scope('grad'):
            @pl.loop(0, DUO)
            def _(z):
                g = mul(left[tile_at(z, HALF), :], right())
                for i in range(DUO):
                    part[place + i, tile_at(z, DUO)] = g[:, i * LANES:(i + 1) * LANES].reshape(DUO, RING, RING, CHIP, LANES)

    PAIRS = HEADS // DUO
    attended, paired = [], []
    for g in range(PAIRS):
        attended.append(after(5.2))
        plan.now += 1.6
        plan.start(DUO * g)
        plan.start(DUO * g + 1)
        paired.append(plan.due())

    @pl.loop(0, PAIRS)
    def _(g):
        def at(table):
            for i in range(PAIRS):
                if table[i]:
                    pl.when(g == i)(functools.partial(emit, table[i]))

        heads = [tile_at(DUO * g + i, LANES) for i in range(DUO)]
        with scope('attend'):
            attend(heads, a1, a2, ks, kts, vs, vts, cos, sin, lambda i: tile_at(core * HEADS + DUO * g + i, LANES), ots, dqo, dkt, dvt, s_scr, e_scr, p_scr, d_scr)

        @pl.when(g == 0)
        def _():
            with scope('entry'):
                comm.meet()
                for c in loads:
                    c.wait()
        for i in range(DUO):
            for c in head_trades(DUO * g + i):
                c.start()
        at(attended)
        gradient(DUO * g, rts, lambda: dqo[tile_at(g, PAIR), :], dot_nt)
        at(paired)

    def beat(cost, *starts):
        plan.now += cost
        for u in starts:
            plan.start(u)
        emit(plan.due())

    wkv, wkvp = e_scr.reshape(DIM, PAIR), p_scr.reshape(DIM, PAIR)
    later += [comm.local(src.at[:, pl.ds(at, LANES)], dst.at[:, pl.ds(to, LANES)]) for srcs, dst in (((wqk, wvo), wkv), ((wqkp, wvop), wkvp)) for src, at, to in ((srcs[0], HALF, 0), (srcs[1], 0, LANES))]
    wqp_loads = [comm.local(wqkp.at[tile_at(i, HALF), pl.ds(0, HALF)], two.at[i]) for i in range(DUO)]
    key = dkt[...] * SCALE
    co, si, x, y = cos[...], sin[...], key[:TURN], key[TURN:]
    dkvo[:LANES, :] = jnp.concatenate([x * co + y * si, y * co - x * si], axis=0).astype(bf16)
    dkvo[LANES:, :] = dvt[...].astype(bf16)
    comm.trade(dkvo, dkvp)
    gradient(UNIT_K, rts, lambda: dkvo[...], dot_nt)
    beat(2.0, UNIT_K, UNIT_V)
    wq_load = comm.local(wqk.at[:, pl.ds(0, HALF)], rts)
    for c in later:
        c.wait()
    with scope('trades'):
        for h in range(HEADS):
            for c in head_trades(h):
                c.wait()

    waiting = list(range(RING))

    def output_gradients(force=False):
        while waiting:
            first = 10 + DUO * waiting[0]
            before = [u for u in range(N_UNITS) if u < first and PLACE[u] in (PLACE[first], PLACE[first + 1])]
            if force:
                emit(plan.rush(lambda: all(map(plan.vacated, before))))
            if not all(map(plan.vacated, before)):
                return
            for u in before:
                sc.drain(u, 0)
            i = waiting.pop(0)
            gradient(PLACE[first], ots, lambda: dycs[:, i * PAIR:(i + 1) * PAIR], dot)
            plan.start(first)
            plan.start(first + 1)
            beat(1.5)

    def piece(cost):
        beat(cost)
        output_gradients()

    @pl.loop(0, TOKENS // LANES)
    def _(i):
        want = lax.broadcasted_iota(jnp.int32, (LANES, ROWS), 0) + i * LANES
        own[tile_at(i, LANES), :] = jnp.where(want == pos[...], 1.0, 0.0).astype(bf16)

    def unsort(at, src_t, n):
        with scope('unsort'):
            dnat[at:at + n, :] = dot(src_t[:n, :], own[...]).astype(bf16)

    output_gradients()
    for i in range(DUO):
        with scope('unsort_o'):
            @pl.loop(0, DUO)
            def _(j):
                r = pl.ds(pl.multiple_of(i * HALF + j * ROWS, ROWS), ROWS)
                onat[:, r] = dot(ots[r, :], own[...]).astype(bf16).T
        piece(1.4)
    for c in comm.exchanged:
        c.wait_recv()
    unsort(0, dqo, HALF)
    dy_loads = [comm.local(dy.at[:, tile_at(i, HALF)], dqo.at[tile_at(i, ROWS)]) for i in range(DUO)]
    piece(1.2)
    unsort(HALF, dqp, HALF)
    piece(1.2)
    unsort(DUO * HALF, dkvo, PAIR)
    unsort(DUO * HALF + PAIR, dkvp, PAIR)
    piece(0.7)
    wq_load.wait()
    for c in wqp_loads + dy_loads:
        c.wait()
    gacc[...] = jnp.zeros_like(gacc)

    def dr_parts(half, r):
        return [s_scr.at[half, r(i * PAIR), :] for i in range(RING)]

    def back(block):
        with scope('dr'):
            @pl.loop(0, DUO)
            def _(half):
                c = tile_at(half, HALF)
                left = jnp.concatenate([rts[c, :], two[half], wkv[c, :], wkvp[c, :]], axis=1)
                acc = dot(left, dnat[:, block * PAIR:(block + 1) * PAIR])
                for i, ref in enumerate(dr_parts(half, lambda at: pl.ds(at, PAIR))):
                    ref[...] = acc[i * PAIR:(i + 1) * PAIR, :].T
        piece(3.4)
        with scope('back'):
            @pl.loop(0, SHARE)
            def _(j):
                q = pl.ds(pl.multiple_of(block * PAIR + j * SHARE, SHARE), SHARE)
                d = jnp.concatenate([ref[...] for half in range(DUO) for ref in dr_parts(half, lambda at: pl.ds(pl.multiple_of(at + j * SHARE, SHARE), SHARE))], axis=1)
                x = xs[q, :].astype(f32)
                inv = lax.rsqrt(jnp.mean(x * x, axis=-1, keepdims=True) + RMS_EPS)
                unit = x * inv
                gacc[...] += jnp.sum((d * unit).reshape(DUO, SUBS, DIM), axis=0)
                dg = d * gain[0:1, :]
                new = inv * (dg - unit * jnp.mean(dg * unit, axis=-1, keepdims=True))
                for half in range(DUO):
                    r = pl.ds(pl.multiple_of(half * ROWS + block * PAIR + j * SHARE, SHARE), SHARE)
                    dqo[r, :] = (dqo[r, :].astype(f32) + new[:, half * HALF:(half + 1) * HALF]).astype(bf16)
        piece(3.6)

    back(0)
    back(1)
    wo_loads = [comm.local(wvo.at[:, pl.ds(LANES, HALF)], rts)] + [comm.local(wvop.at[tile_at(i, HALF), pl.ds(LANES, HALF)], two.at[i]) for i in range(DUO)]
    for i in range(DUO):
        comm.store(dqo.at[tile_at(i, ROWS)], grad_x.at[:, tile_at(i, HALF)])
    total = jnp.sum(gacc[...], axis=0, keepdims=True)
    gpart[...] = jnp.zeros_like(gpart)
    for i in range(RING):
        for j in range(RING):
            gpart[i, j:j + 1, :] = total[:, (i * RING + j) * LANES:(i * RING + j + 1) * LANES]
    stage = [comm.send(gpart, gpeer, peer)]
    output_gradients(True)

    def project_out(col, weights, i):
        with scope('project'):
            @pl.loop(DUO * i, DUO * i + DUO)
            def _(j):
                c = tile_at(j, PAIR)
                dst = pl.ds(pl.multiple_of(col + j * PAIR, PAIR), PAIR)
                xs[:, dst] = (xs[:, dst].astype(f32) + dot(onat[...], weights(c))).astype(bf16)
        beat(1.3)

    def own_half(c):
        return rts[:, c]

    def other_half(c):
        return jnp.concatenate([a1[:, c], a2[:, c]], axis=0)

    for c in wo_loads:
        c.wait()
    project_out(core * HALF, own_half, 0)
    for c in stage:
        c.wait_recv()
    for j in range(RING):
        gz[j] = gpart[j] + gpeer[j]
    stage = [comm.send(gz.at[step(comm.pos, 'z', hop)], gz.at[TRIO + hop], comm.far('z', hop)) for hop in (1, DUO, TRIO)]
    project_out(core * HALF, own_half, 1)
    for c in stage:
        c.wait_recv()
    gy[0] = (gz[comm.pos['z']] + gz[RING]) + (gz[5] + gz[6])
    stage = [comm.send(gy.at[0], gy.at[hop], comm.far('y', hop)) for hop in (1, DUO, TRIO)]
    project_out((1 - core) * HALF, other_half, 0)
    for c in stage:
        c.wait_recv()
    gx[0] = (gy[0] + gy[1]) + (gy[DUO] + gy[TRIO])
    stage = [comm.send(gx.at[0], gx.at[hop], comm.far('x', hop)) for hop in (1, DUO, TRIO)]
    project_out((1 - core) * HALF, other_half, 1)
    comm.store(xs, result)
    for c in stage:
        c.wait_recv()
    gpeer[0] = (gx[0] + gx[1]) + (gx[DUO] + gx[TRIO])
    mine = jnp.broadcast_to(gpeer[0, pl.ds(comm.pos['y'], 1), :], (SUBS, LANES))
    gout[...] = pltpu.roll(mine, LANES - (comm.pos['x'] * CHIP + core * SHARE), 1)
    emit(plan.rush(lambda: not plan.stage))
    with scope('finish'):
        sc.finish()
        for c in comm.sent + comm.exchanged:
            c.wait_send()
        for c in comm.stored:
            c.wait()


def tail(qt, do_t, k, kt, v, vt, rt, dyc, wqk, wqkp, wvo, wvop, gain, hidden, dy, pos, cos, sin):
    bf16, f32 = jnp.bfloat16, jnp.float32
    any_ = pl.BlockSpec(memory_space=pl.ANY)
    vmem = pl.BlockSpec(memory_space=pltpu.VMEM)
    S = lambda shape, d=bf16: jax.ShapeDtypeStruct(shape, d)
    V = lambda shape, d=bf16: pltpu.VMEM(shape, d)
    D = lambda n: pltpu.SemaphoreType.DMA((n,))
    sq, tall, wide = (HALF, TOKENS), (TOKENS, LANES), (LANES, TOKENS)
    mine, kv = (ROWS, DIM), (PAIR, TOKENS)
    return pl.pallas_call(
        tail_kernel,
        out_shape=[S(mine), S(mine), S((SHARE, DIM), f32), S((SHARE, PAIR), f32), S((SHARE, PAIR), f32), S((SHARE, DIM), f32), S((SUBS, LANES), f32)],
        in_specs=[any_] * 12 + [vmem] + [any_] * DUO + [vmem] * TRIO,
        out_specs=[any_] * 6 + [vmem],
        scratch_shapes=[V((DUO,) + sq), V(tall), V(wide), V(tall), V(wide), V((DIM, TOKENS)), V((DIM, TOKENS)), V(sq), V(sq), V(kv), V(kv), V(wide, f32), V(wide, f32),
                        V((DUO, TOKENS, QB), f32), V((DUO, TOKENS, QB)), V((DUO, TOKENS, QB)), V((DUO, TOKENS, QB)), V(sq), V((PLACES, RING, RING, RING, CHIP, LANES), f32), V((TRIO, SLOTS, RING, RING, CHIP, LANES), f32),
                        V((TRIO, SLOTS, 6, RING, RING, SHARE, LANES), f32), V((TRIO, SLOTS, 6, RING, SHARE, LANES), f32), V((TRIO, SLOTS, TRIO, CHIP, LANES), f32), V((N_UNITS, CHIP, LANES), f32), V((TOKENS, ROWS)), V(mine), V((DUO * QKV, ROWS)), V(mine),
                        V((SUBS, DIM), f32), V((RING, SUBS, LANES), f32), V((RING, SUBS, LANES), f32), V((7, SUBS, LANES), f32), V((RING, SUBS, LANES), f32), V((RING, SUBS, LANES), f32),
                        D(TRIO * N_UNITS), D(6 * N_UNITS), D(DUO + N_UNITS), D(DUO * HEADS + SHARE), D(DUO * HEADS + SHARE), D(CHIP)],
        compiler_params=pltpu.CompilerParams(collective_id=1, has_side_effects=True, vmem_limit_bytes=67043328),
        name='tail',
    )(qt, do_t, k, kt, v, vt, rt, dyc, wqk, wqkp, wvo, wvop, gain, hidden, dy, pos, cos, sin)


def settle_kernel(n, *refs):
    ins, gain, outs, gain_out, bufs, sems = refs[:n], refs[n], refs[n + 1:DUO * n + 1], refs[DUO * n + 1], refs[DUO * n + DUO:-1], refs[-1]
    jobs = []
    for a, o, b in zip(ins, outs, bufs):
        size = a.shape[0] // RING if a.shape[0] == ROWS else a.shape[0]
        jobs += [tuple(r.at[pl.ds(i, size)] for r in (a, b, o)) for i in range(0, a.shape[0], size)]
    takes = [pltpu.make_async_copy(a, b, sems.at[0, i]) for i, (a, b, _) in enumerate(jobs)]
    puts = [pltpu.make_async_copy(b, o, sems.at[1, i]) for i, (_, b, o) in enumerate(jobs)]
    for c in takes:
        c.start()
    gain_out[...] = gain[0:1, :SHARE]
    for take, put in zip(takes, puts):
        take.wait()
        put.start()
    for c in puts:
        c.wait()


def settle(*arrays):
    *large, gain = arrays
    any_, vmem = pl.BlockSpec(memory_space=pl.ANY), pl.BlockSpec(memory_space=pltpu.VMEM)
    return pl.pallas_call(
        functools.partial(settle_kernel, len(large)),
        out_shape=[jax.ShapeDtypeStruct(a.shape, a.dtype) for a in large] + [jax.ShapeDtypeStruct((1, SHARE), gain.dtype)],
        in_specs=[any_] * len(large) + [vmem],
        out_specs=[any_] * len(large) + [vmem],
        scratch_shapes=[pltpu.VMEM(a.shape, a.dtype) for a in large] + [pltpu.SemaphoreType.DMA((DUO, 12))],
        name='settle',
    )(*arrays)


def rope_tables():
    j = np.arange(HEAD_DIM // DUO, dtype=np.float64) / (HEAD_DIM // DUO)
    freq = (ROPE_THETA ** -j).astype(np.float32)
    angle = freq[:, None] * np.arange(TOKENS, dtype=np.float32)[None, :]
    return np.cos(angle.astype(np.float64)).astype(np.float32), np.sin(angle.astype(np.float64)).astype(np.float32)


def solution(mesh):
    def shard_fn(hidden, tok_pos, grad_out, norm_gain, w_query, w_key, w_value, w_out):
        hidden, grad_out = hidden[0], grad_out[0]
        cos_t, sin_t = (jnp.asarray(t) for t in rope_tables())
        *parts, gain = head(hidden, grad_out, w_query, w_key, w_value, w_out, tok_pos, norm_gain.reshape(1, SHARE), cos_t, sin_t)
        parts = [p.reshape(DIM, GROUP) if p.ndim > DUO else p for p in parts]
        result, grad_hidden, gq, gk, gv, go, gout = settle(*tail(*parts, gain, hidden, grad_out, tok_pos, cos_t, sin_t))
        return result[None], grad_hidden[None], gq, gk, gv, go, gout.reshape(SHARE)

    row_spec, pos_spec = P('fsdp', 'cp', None), P('fsdp', 'cp')
    weight_spec, gain_spec = P(('fsdp', 'cp'), None), P(('fsdp', 'cp'))
    return jax.shard_map(shard_fn, mesh=mesh, in_specs=(row_spec, pos_spec, row_spec, gain_spec, weight_spec, weight_spec, weight_spec, weight_spec), out_specs=(row_spec, row_spec, weight_spec, weight_spec, weight_spec, weight_spec, gain_spec), check_vma=False)
```

```python
import functools
import jax
import jax.numpy as jnp
import numpy as np
from jax import lax
from jax.experimental import pallas as pl
from jax.experimental.pallas import tpu as pltpu
from jax.sharding import PartitionSpec as P

LANES, SUBS, RING, TRIO, DUO = 128, 8, 4, 3, 2
PAIR, ROWS, CHIP, SHARE, TURN = 256, 512, 32, 16, 64
HEAD_DIM = LANES
ROPE_THETA = 1000000.0
RMS_EPS = 1e-5
SCALE = HEAD_DIM ** -0.5
LOG2E = 1.4426950408889634

MESH = pl.DeviceIdType.MESH
AXES = ('x', 'y', 'z')
ORDERS = (('x', 'y', 'z'), ('y', 'z', 'x'), ('z', 'x', 'y'))
ALL = pl.ds(0, RING)


def torus():
    f = lax.axis_index('fsdp')
    return {'x': lax.rem(f, RING), 'y': lax.rem(lax.div(f, RING), RING), 'z': lax.div(f, SHARE)}


def step(pos, axis, hop):
    return lax.rem(pos[axis] + hop, RING)


class Batch:
    def __init__(self, comm):
        self.comm, self.index = comm, comm.used
        comm.used += 1

    def _copy(self, src, dst, device):
        send, recv, _ = self.comm.sems
        return pltpu.make_async_remote_copy(src_ref=src, dst_ref=dst, send_sem=send.at[self.index], recv_sem=recv.at[self.index], device_id=device, device_id_type=MESH)

    def send(self, src, dst, device):
        self._copy(src, dst, device).start()
        return self

    def arrived(self, whole):
        self._copy(whole, whole, self.comm.peer()).wait_recv()

    def sent(self, whole):
        self._copy(whole, whole, self.comm.peer()).wait_send()


class Comm:
    def __init__(self, send_sems, recv_sems, local_sems):
        self.pos = torus()
        self.core = lax.axis_index('cp')
        self.sems = (send_sems, recv_sems, local_sems)
        self.used = self.used_local = 0
        self.stored = []

    def far(self, axis, hop):
        p = dict(self.pos)
        p[axis] = step(self.pos, axis, hop)
        return {'fsdp': (p['z'] * RING + p['y']) * RING + p['x'], 'cp': self.core}

    def peer(self):
        return {'fsdp': lax.axis_index('fsdp'), 'cp': 1 - self.core}

    def announce(self):
        sem = pltpu.get_barrier_semaphore()
        for axis in AXES:
            for hop in (1, DUO, TRIO):
                pl.semaphore_signal(sem, inc=1, device_id=self.far(axis, hop), device_id_type=MESH)
        pl.semaphore_signal(sem, inc=1, device_id=self.peer(), device_id_type=MESH)

    def meet(self):
        pl.semaphore_wait(pltpu.get_barrier_semaphore(), 10)

    def ring(self, batch, src, slots, axis):
        for hop in (1, DUO, TRIO):
            batch.send(src, slots.at[hop], self.far(axis, hop))

    def local(self, src, dst):
        i = self.used_local
        self.used_local += 1
        c = pltpu.make_async_copy(src, dst, self.sems[DUO].at[i])
        c.start()
        return c

    def store(self, src, dst):
        self.stored.append(self.local(src, dst))


class OldComm:
    def __init__(self, send_sems, recv_sems, local_sems):
        self.pos = torus()
        self.core = lax.axis_index('cp')
        self.sems = (send_sems, recv_sems, local_sems)
        self.used = self.used_local = 0
        self.sent, self.exchanged, self.stored = [], [], []

    def far(self, axis, hop):
        p = dict(self.pos)
        p[axis] = step(self.pos, axis, hop)
        return {'fsdp': (p['z'] * RING + p['y']) * RING + p['x'], 'cp': self.core}

    def peer(self):
        return {'fsdp': lax.axis_index('fsdp'), 'cp': 1 - self.core}

    def announce(self):
        sem = pltpu.get_barrier_semaphore()
        for axis in AXES:
            for hop in (1, DUO, TRIO):
                pl.semaphore_signal(sem, inc=1, device_id=self.far(axis, hop), device_id_type=MESH)
        pl.semaphore_signal(sem, inc=1, device_id=self.peer(), device_id_type=MESH)

    def meet(self):
        pl.semaphore_wait(pltpu.get_barrier_semaphore(), 10)

    def barrier(self):
        self.announce()
        self.meet()

    def _copy(self, src, dst, device):
        i = self.used
        self.used += 1
        c = pltpu.make_async_remote_copy(src_ref=src, dst_ref=dst, send_sem=self.sems[0].at[i], recv_sem=self.sems[1].at[i], device_id=device, device_id_type=MESH)
        c.start()
        return c

    def send(self, src, dst, device):
        c = self._copy(src, dst, device)
        self.sent.append(c)
        return c

    def trade(self, src, dst):
        self.exchanged.append(self._copy(src, dst, self.peer()))

    def local(self, src, dst):
        i = self.used_local
        self.used_local += 1
        c = pltpu.make_async_copy(src, dst, self.sems[DUO].at[i])
        c.start()
        return c

    def store(self, src, dst):
        self.stored.append(self.local(src, dst))

    def finish(self):
        for c in self.sent:
            c.wait_send()
        for c in self.exchanged:
            c.wait_send()
            c.wait_recv()
        for c in self.stored:
            c.wait()


def pick(ref, sel, cols):
    return ref.at[sel['z'], sel['y'], sel['x'], :, pl.ds(cols[0], cols[1])]


def sem_scratch(remote, local):
    return [pltpu.SemaphoreType.DMA((remote,)), pltpu.SemaphoreType.DMA((remote,)), pltpu.SemaphoreType.DMA((local,))]


def add_into(dst, *srcs, fresh=False):
    def add(idx):
        total, *rest = [s[idx] for s in (srcs if fresh else (dst,) + srcs)]
        for more in rest:
            total = total + more
        dst[idx] = total

    if len(dst.shape) > TRIO:
        @pl.loop(0, dst.shape[0])
        def _(i):
            add((i,))
    else:
        add(Ellipsis)


QK_COLORS = ((0, PAIR, LANES), (384, LANES, PAIR), (768, PAIR, LANES))
VO_COLORS = ((0, LANES, PAIR), (384, PAIR, LANES), (768, LANES, PAIR))
TOKENS = 1024
DIM = 2048
HALF = 1024
QKV = 1280
GROUP = 1152


def scope(name):
    return jax.named_scope(name)


def dot(a, b):
    return jnp.dot(a, b, preferred_element_type=jnp.float32)


def dot_nt(a, b):
    return lax.dot_general(a, b, (((1,), (1,)), ((), ())), preferred_element_type=jnp.float32)


def tile_at(i, n):
    return pl.ds(pl.multiple_of(i * n, n), n)


class Gather:
    def __init__(self, comm, ref, colors, land):
        self.comm, self.ref, self.colors, self.land = comm, ref, colors, land
        self.held = [dict(comm.pos) for _ in colors]
        self.batches = []

    def parts(self, k):
        lo, na, nb = self.colors[k]
        return (lo, na), (lo + na, nb)

    def move(self, batch, s, cols, to):
        batch.send(pick(self.ref, s, cols), pick(self.ref, s, cols), to)

    def at(self, k, hop):
        d = ORDERS[k][self.phase]
        return dict(self.held[k], **{d: step(self.comm.pos, d, hop)})

    def begin(self, phase):
        self.phase = phase
        self.up, self.dn, self.rest = ([Batch(self.comm) for _ in range(TRIO)] for _ in range(TRIO))
        self.batches += self.up + self.dn + self.rest
        for k in range(TRIO):
            a, b = self.parts(k)
            d = ORDERS[k][phase]
            up, dn, s = self.comm.far(d, 1), self.comm.far(d, TRIO), self.held[k]
            self.move(self.up[k], s, a, up)
            self.move(self.dn[k], s, b, dn)
            self.move(self.rest[k], s, b, up)
            self.move(self.rest[k], s, a, dn)
            if phase == 0:
                for cols in (a, b):
                    self.move(self.rest[k], s, cols, self.comm.far(d, DUO))
        if phase == DUO:
            for k in range(TRIO):
                for cols in self.parts(k):
                    self.land(self.ref, self.held[k], cols)

    def forward(self):
        for k in range(TRIO):
            a, b = self.parts(k)
            d = ORDERS[k][self.phase]
            for batch, hop, cols, to in ((self.up[k], TRIO, a, 1), (self.dn[k], 1, b, TRIO)):
                s = self.at(k, hop)
                batch.arrived(pick(self.ref, s, cols))
                if self.phase:
                    self.move(self.rest[k], s, cols, self.comm.far(d, to))
                if self.phase == DUO:
                    self.land(self.ref, s, cols)

    def end(self):
        for k in range(TRIO):
            a, b = self.parts(k)
            d = ORDERS[k][self.phase]
            two = dict(self.held[k], **{d: pl.ds(0, DUO)})
            self.rest[k].arrived(pick(self.ref, two, (a[0], a[1] + b[1])))
            if self.phase == DUO:
                for hop, cols in ((TRIO, b), (1, a), (DUO, a), (DUO, b)):
                    self.land(self.ref, self.at(k, hop), cols)
            for batch, s, cols in ((self.up[k], self.held[k], a), (self.dn[k], self.held[k], b), (self.rest[k], two, (a[0], a[1] + b[1]))):
                batch.spent = pick(self.ref, s, cols)
            self.held[k] = dict(self.held[k], **{d: ALL})

    def finish(self):
        for batch in self.batches:
            batch.sent(batch.spent)


def head_kernel(hidden, dy, wq, wk, wv, wo, pos, gain_in, cos_t, sin_t,
                qt_o, dot_o, k_o, kt_o, v_o, vt_o, rt_o, dyc_o, wqk_o, wqkp_o, wvo_o, wvop_o, gain_o,
                hid2, dy2, dys, rs, rt, wqk, wvo, wpeer, pi, pos2, qt, dot_s, kk, kt, vv, vt, gain, gtile, gbuf, gx, gy, gz, *sems):
    comm = Comm(*sems)
    pos_c, core = comm.pos, comm.core
    bf16, f32 = jnp.bfloat16, jnp.float32
    peer = comm.peer()
    rows = tile_at(core, SHARE)
    mine_qk = wqk.at[pos_c['z'], pos_c['y'], pos_c['x'], rows]
    mine_vo = wvo.at[pos_c['z'], pos_c['y'], pos_c['x'], rows]

    def weight_parts(c):
        return ((wq.at[:, tile_at(c, HALF)], mine_qk.at[:, pl.ds(0, HALF)]), (wk.at[:, tile_at(c, LANES)], mine_qk.at[:, pl.ds(HALF, LANES)]),
                (wv.at[:, tile_at(c, LANES)], mine_vo.at[:, pl.ds(0, LANES)]), (wo.at[:, tile_at(c, HALF)], mine_vo.at[:, pl.ds(LANES, HALF)]))

    loads = [comm.local(s, d) for s, d in weight_parts(core)]
    load_x = [comm.local(hidden, hid2.at[pl.ds(0, ROWS)]), comm.local(dy, dy2.at[pl.ds(0, ROWS)])]
    share = lax.broadcasted_iota(jnp.int32, (SUBS, LANES), 1) // SHARE
    gtile[...] = jnp.where(share == pos_c['x'] * DUO + core, jnp.broadcast_to(jnp.concatenate([gain_in[...]] * SUBS, axis=1), (SUBS, LANES)), 0.0)
    comm.announce()
    with scope('entry'):
        comm.meet()
    swap_w, swap_pos, swap_dy, swap_x, peers_qk, peers_vo = (Batch(comm) for _ in range(6))
    gain_c, gain_x, gain_y, gain_z = (Batch(comm) for _ in range(RING))
    for s, d in weight_parts(1 - core):
        swap_w.send(s, d, peer)
    gain_c.send(gtile, gbuf, peer)
    swap_pos.send(pos, pos2, peer)
    for c in loads:
        c.wait()
    with scope('wait_w'):
        swapped = wqk.at[pos_c['z'], pos_c['y'], pos_c['x']]
        swap_w.arrived(swapped)

    def land_qk(ref, s, cols):
        peers_qk.send(pick(ref, s, cols), pick(wqkp_o, s, cols), peer)

    def land_vo(ref, s, cols):
        peers_vo.send(pick(ref, s, cols), pick(wpeer, s, cols), peer)

    g1 = Gather(comm, wqk, QK_COLORS, land_qk)
    g2 = Gather(comm, wvo, VO_COLORS, land_vo)
    g1.begin(0)
    g2.begin(0)
    swap_dy.send(dy, dy2.at[pl.ds(ROWS, ROWS)], peer)
    gain_c.arrived(gbuf)
    gx[0] = gtile[...] + gbuf[...]
    comm.ring(gain_x, gx.at[0], gx, 'x')

    swap_pos.arrived(pos2)

    @pl.loop(0, TOKENS // LANES)
    def _(i):
        want = lax.broadcasted_iota(jnp.int32, (LANES, ROWS), 0) + i * LANES
        for h, have in enumerate((pos, pos2)):
            pi[tile_at(i, LANES), h * ROWS:(h + 1) * ROWS] = jnp.where(want == have[...], 1.0, 0.0).astype(bf16)

    def sort(dst, src, first, last):
        with scope('sort'):
            @pl.loop(first, last)
            def _(j):
                c = tile_at(j, PAIR)
                dst[:, c] = dot(pi[...], src[:, c]).astype(bf16)

    with scope('p0_end'):
        g1.forward()
        g1.end()
    g1.begin(1)
    g2.forward()
    g2.end()
    swap_x.send(hidden, hid2.at[pl.ds(ROWS, ROWS)], peer)
    gain_x.arrived(gx.at[pl.ds(1, TRIO)])
    gy[pos_c['y']] = (gx[0] + gx[1]) + (gx[DUO] + gx[TRIO])
    for hop in (1, DUO, TRIO):
        gain_y.send(gy.at[pos_c['y']], gy.at[pos_c['y']], comm.far('y', hop))
    with scope('wait_dy'):
        load_x[1].wait()
        swap_dy.arrived(dy2.at[pl.ds(ROWS, ROWS)])
    sort(dys, dy2, 0, RING)
    with scope('p1q_fwd'):
        g1.forward()
    g2.begin(1)
    sort(dys, dy2, RING, SUBS)
    comm.store(dys.at[:, tile_at(core, HALF)], dyc_o)
    with scope('p1q_end'):
        g1.end()
    g1.begin(DUO)
    with scope('p1o_fwd'):
        g2.forward()
    gain_y.arrived(gy.at[pl.ds(1, TRIO)])
    for j in range(RING):
        gz[pos_c['z'], j] = gy[j]
    for hop in (1, DUO, TRIO):
        gain_z.send(gz.at[pos_c['z']], gz.at[pos_c['z']], comm.far('z', hop))
    with scope('wait_x'):
        load_x[0].wait()
        swap_x.arrived(hid2.at[pl.ds(ROWS, ROWS)])
    sort(rs, hid2, 0, SUBS)
    with scope('p1o_end'):
        g2.end()
    with scope('gain'):
        gain_z.arrived(gz.at[pl.ds(1, TRIO)])
    for i in range(RING):
        for j in range(RING):
            gain[:, (i * RING + j) * LANES:(i * RING + j + 1) * LANES] = gz[i, j]
    comm.store(gain, gain_o)

    def norm(first, last):
        with scope('norm'):
            @pl.loop(first, last)
            def _(i):
                r = tile_at(i, CHIP)
                x = rs[r, :].astype(f32)
                inv = lax.rsqrt(jnp.mean(x * x, axis=-1, keepdims=True) + RMS_EPS)
                rs[r, :] = (x * inv * gain[0:1, :]).astype(bf16)

    with scope('p2q_fwd'):
        g1.forward()
    g2.begin(DUO)
    norm(0, TOKENS // CHIP)
    with scope('r_t'):
        @pl.loop(0, DIM // PAIR)
        def _(i):
            c = tile_at(i, PAIR)

            @pl.loop(0, TOKENS // PAIR)
            def _(j):
                r = tile_at(j, PAIR)
                rt[c, r] = rs[r, c].T
    comm.store(rt, rt_o)
    with scope('p2q_end'):
        g1.end()
    comm.store(wqk, wqk_o)
    w_qk, w_vo, w_peer = wqk.reshape(DIM, GROUP), wvo.reshape(DIM, GROUP), wpeer.reshape(DIM, GROUP)

    def rotated(x, r):
        cos, sin = cos_t[:, r], sin_t[:, r]
        cos = jnp.concatenate([cos, cos], axis=0).T
        sin = jnp.concatenate([-sin, sin], axis=0).T
        return (x * cos + pltpu.roll(x, TURN, 1) * sin).astype(bf16)

    def queries(first, last):
        with scope('q'):
            @pl.loop(first, last)
            def _(t):
                x = dot(rs[...], w_qk[:, tile_at(t, PAIR)])
                for i in range(RING):
                    r = slice(i * PAIR, (i + 1) * PAIR)
                    for h in range(DUO):
                        qt[tile_at(DUO * t + h, LANES), r] = rotated(x[r, h * LANES:(h + 1) * LANES], r).T

    queries(0, DUO)
    with scope('p2o_fwd'):
        g2.forward()
    queries(DUO, RING)

    @pl.loop(0, DUO)
    def _(i):
        r = tile_at(i, ROWS)
        key = rotated(dot(rs[r, :], w_qk[:, HALF:]), r)
        kk[r, :] = key
        kt[:, r] = key.T
    for src, dst in ((kk, k_o), (kt, kt_o), (qt, qt_o)):
        comm.store(src, dst)
    with scope('p2o_end'):
        g2.end()
    with scope('vals'):
        @pl.loop(0, DUO)
        def _(i):
            r = tile_at(i, ROWS)
            val = dot(rs[r, :], w_vo[:, :LANES]).astype(bf16)
            vv[r, :] = val
            vt[:, r] = val.T
    for src, dst in ((vv, v_o), (vt, vt_o)):
        comm.store(src, dst)
    with scope('wo_peer'):
        peers_vo.arrived(wpeer)
    comm.store(wvo, wvo_o)
    comm.store(wpeer, wvop_o)

    with scope('do_t'):
        r = tile_at(core, HALF)

        @pl.loop(0, TOKENS // PAIR)
        def _(j):
            t = tile_at(j, PAIR)
            w_rows = jnp.concatenate([w_vo[r, LANES:], w_peer[r, LANES:]], axis=1)
            d_rows = jnp.concatenate([dys[t, tile_at(core, HALF)], dys[t, tile_at(1 - core, HALF)]], axis=1)
            dot_s[:, t] = dot_nt(w_rows, d_rows).astype(bf16)
    comm.store(dot_s, dot_o)
    with scope('finish'):
        peers_qk.arrived(wqk)
        for batch, whole in ((swap_w, swapped), (swap_pos, pos2), (swap_dy, dy2.at[pl.ds(ROWS, ROWS)]), (swap_x, hid2.at[pl.ds(ROWS, ROWS)]), (peers_qk, wqk), (peers_vo, wvo),
                             (gain_c, gbuf), (gain_x, gx.at[pl.ds(1, TRIO)]), (gain_y, gy.at[pl.ds(1, TRIO)]), (gain_z, gz.at[pl.ds(1, TRIO)])):
            batch.sent(whole)
        g1.finish()
        g2.finish()
        for c in comm.stored:
            c.wait()


def head(hidden, dy, wq, wk, wv, wo, pos, gain, cos_t, sin_t):
    bf16, f32 = jnp.bfloat16, jnp.float32
    any_ = pl.BlockSpec(memory_space=pl.ANY)
    vmem = pl.BlockSpec(memory_space=pltpu.VMEM)
    S = lambda shape, d=bf16: jax.ShapeDtypeStruct(shape, d)
    V = lambda shape, d=bf16: pltpu.VMEM(shape, d)
    group = (RING, RING, RING, CHIP, GROUP)
    sq, tall, wide = (HALF, TOKENS), (TOKENS, LANES), (LANES, TOKENS)
    full = (TOKENS, DIM)
    return pl.pallas_call(
        head_kernel,
        out_shape=[S(sq), S(sq), S(tall), S(wide), S(tall), S(wide), S((DIM, TOKENS)), S((TOKENS, HALF)), S(group), S(group), S(group), S(group), S((SUBS, DIM), f32)],
        in_specs=[any_] * 6 + [vmem] * RING,
        out_specs=[any_] * 13,
        scratch_shapes=[V(full), V(full), V(full), V(full), V((DIM, TOKENS)), V(group), V(group), V(group), V((TOKENS, TOKENS)), V((1, ROWS), jnp.int32),
                        V(sq), V(sq), V(tall), V(wide), V(tall), V(wide), V((SUBS, DIM), f32), V((SUBS, LANES), f32), V((SUBS, LANES), f32), V((RING, SUBS, LANES), f32), V((RING, SUBS, LANES), f32), V((RING, RING, SUBS, LANES), f32)] + sem_scratch(TURN, 18),
        compiler_params=pltpu.CompilerParams(collective_id=0, has_side_effects=True, vmem_limit_bytes=60 * DUO**20),
        name='head',
    )(hidden, dy, wq, wk, wv, wo, pos, gain, cos_t, sin_t)


HEADS = SUBS
UNIT_K, UNIT_V = SUBS, 9
N_UNITS = 18
GAIN = N_UNITS
SLOTS = RING
LAST = 5
ABREAST = DUO
LINES = ((0, TRIO, 6, 9, 12, 15), (1, RING, 7, 10, 13, SHARE), (DUO, 5, SUBS, 11, 14, 17))
COLOR = {u: k for k, line in enumerate(LINES) for u in line}
RANK = {u: i for line in LINES for i, u in enumerate(line)}
BEFORE = {u: line[i - SLOTS] if i >= SLOTS else None for line in LINES for i, u in enumerate(line)}
PLACES = 12
PLACE = {u: u % PLACES for u in range(N_UNITS)}
WIRE = (2.85, 0.72, 0.36)
LATENCY = 2.6
STAGE_COST = 0.1
GAIN_STEP = 4.0


class Plan:
    def __init__(self):
        self.now, self.stage, self.ready, self.order, self.link = 0.0, {}, {}, [], {}
        self.mark = {}

    def _wire(self, u, phase, count):
        link = ORDERS[COLOR[u]][phase]
        t = max(self.link.get(link, 0.0), self.now)
        first = t + WIRE[phase] + LATENCY
        self.link[link] = t + WIRE[phase] * count
        return first if phase < DUO else self.link[link] + LATENCY

    def free(self, u, phase):
        if BEFORE[u] is None:
            return True
        done = self.mark.get((BEFORE[u], (DUO, RING, 5)[phase]))
        if done is None:
            return False
        sent = ((0, 1), (DUO, TRIO), (RING,))[phase]
        return any(self.mark.get((j, s), -1) > done and (j, s + 1) in self.mark for j in LINES[COLOR[u]] for s in sent)

    def run(self, u):
        stage = self.stage[u]
        self.order.append((u, stage))
        self.mark[u, stage] = len(self.order)
        self.now = max(self.now, self.ready[u]) + STAGE_COST
        self.stage[u] = stage + 1
        if stage == (RING if u == GAIN else LAST):
            del self.stage[u]
        elif u == GAIN:
            self.ready[u] = self.now + GAIN_STEP
        elif stage % DUO:
            self.ready[u] = self._wire(u, stage // DUO, 1)
        else:
            self.ready[u] = self._wire(u, stage // DUO, DUO)

    def blocked(self, u):
        stage = self.stage[u]
        if u == GAIN:
            return False
        if stage == 0 and sum(0 < self.stage.get(j, 0) <= DUO for j in LINES[COLOR[u]]) >= ABREAST:
            return True
        if stage == DUO and BEFORE[u] is not None and (BEFORE[u], LAST) not in self.mark:
            return True
        return stage in (0, DUO, RING) and not self.free(u, stage // DUO)

    def start(self, u):
        self.stage[u], self.ready[u] = 0, self.now

    def due(self):
        first = len(self.order)
        while True:
            ripe = [(self.ready[u], u) for u in self.stage if self.ready[u] <= self.now and not self.blocked(u)]
            if not ripe:
                return self.order[first:]
            self.run(min(ripe)[1])

    def vacated(self, u):
        return (u, DUO) in self.mark

    def rush(self, done):
        first = len(self.order)
        while not done():
            self.run(min((self.ready[u], u) for u in self.stage if not self.blocked(u))[1])
        return self.order[first:]


QB = PAIR
NBLK = TOKENS // QB
HALVES = (pl.ds(0, SHARE), pl.ds(SHARE, SHARE))


class Scatter:
    def __init__(self, comm, part, mid, bufs, fin, outs, send_sems, recv_sems, swap_sems):
        self.pos, self.part, self.mid, self.bufs, self.fin, self.outs = comm.pos, part, mid, bufs, fin, outs
        self.send_sems, self.recv_sems, self.swap_sems = send_sems, recv_sems, swap_sems
        self.near = {(a, hop): comm.far(a, hop) for a in AXES for hop in (1, DUO, TRIO)}
        self.hops = {(a, hop): step(comm.pos, a, hop) for a in AXES for hop in (1, DUO, TRIO)}
        self.peer, self.core = comm.peer(), comm.core
        self.keep, self.give = tile_at(comm.core, SHARE), tile_at(1 - comm.core, SHARE)
        self.drained = set()

    def slot(self, u):
        return COLOR[u], RANK[u] % SLOTS

    def buf(self, u, phase):
        return self.bufs[phase].at[self.slot(u)]

    def view(self, u, phase, hop, half=None):
        order = ORDERS[COLOR[u]]
        at = {a: ALL for a in AXES}
        for a in order[1:phase]:
            at[a] = self.pos[a]
        at[order[phase]] = self.hops[order[phase], hop] if hop else self.pos[order[phase]]
        rows = pl.ds(0, CHIP) if half is None else HALVES[half]
        if phase == 0:
            return self.part.at[PLACE[u], at['z'], at['y'], at['x'], rows, :]
        return self.mid.at[self.slot(u) + tuple(at[a] for a in 'zyx' if a != order[0]) + (rows, slice(None))]

    def copy(self, src, dst, sems, device):
        return pltpu.make_async_remote_copy(src_ref=src, dst_ref=dst, send_sem=sems[0], recv_sem=sems[1], device_id=device, device_id_type=MESH)

    def sems(self, u, phase, kind=0):
        at = u * TRIO + phase
        return self.send_sems.at[at], self.recv_sems.at[DUO * at + kind]

    def send(self, u, phase, name):
        axis = ORDERS[COLOR[u]][phase]
        if phase == DUO:
            src, to = self.view(u, DUO, name + 1), name + 1
        else:
            hop, half, to = ((DUO, 0, 1), (DUO, 1, TRIO), (1, 1, 1), (TRIO, 0, TRIO), (1, 0, 1), (TRIO, 1, TRIO))[name]
            src = self.view(u, phase, hop, half)
        self.copy(src, self.buf(u, phase).at[name], self.sems(u, phase, int(name > 1 and phase < DUO)), self.near[axis, to]).start()

    def launch(self, u, phase):
        if BEFORE[u] is not None:
            self.drain(BEFORE[u], phase)
        for name in range(RING if phase < DUO else TRIO):
            self.send(u, phase, name)

    def arrived(self, u, phase, first, count):
        whole = self.buf(u, phase).at[pl.ds(first, count)]
        self.copy(whole, whole, self.sems(u, phase, int(first > 0)), self.peer).wait_recv()

    def drain(self, u, phase):
        if (u, phase) not in self.drained:
            self.drained.add((u, phase))
            whole = self.buf(u, phase)
            self.copy(whole, whole, self.sems(u, phase), self.peer).wait_send()

    def out(self, u):
        if u < HEADS:
            out, col = self.outs[0], self.core * HALF + u * LANES
        elif u < 10:
            out, col = self.outs[u - 7], self.core * LANES
        else:
            out, col = self.outs[TRIO], self.core * HALF + (u - 10) * LANES
        return out.at[:, pl.ds(pl.multiple_of(col, LANES), LANES)]

    def kept(self, u):
        return pltpu.make_async_copy(self.fin.at[u, self.keep], self.out(u), self.swap_sems.at[DUO + u])

    def run(self, u, stage):
        if stage == 0:
            return self.launch(u, 0)
        phase = (stage - 1) // DUO
        if stage == LAST:
            self.arrived(u, DUO, 0, TRIO)
            got = self.buf(u, DUO)
            self.fin[u] = self.view(u, DUO, 0)[...] + (got[0] + got[1] + got[DUO])
            self.copy(self.fin.at[u, self.give], self.out(u), (self.swap_sems.at[0], self.swap_sems.at[1]), self.peer).start()
            self.kept(u).start()
            return
        got = self.buf(u, phase)
        if stage % DUO:
            self.arrived(u, phase, 0, DUO)
            for name, hop in ((0, 1), (1, TRIO)):
                add_into(self.view(u, phase, hop, name), got.at[name])
                self.send(u, phase, name + RING)
            return
        self.arrived(u, phase, DUO, RING)
        if phase == 0 and BEFORE[u] is not None:
            self.drain(BEFORE[u], 1)
            self.drain(BEFORE[u], DUO)
        for half, names in ((0, (TRIO, RING)), (1, (DUO, 5))):
            if phase:
                add_into(self.view(u, phase, 0, half), *[got.at[name] for name in names])
            else:
                dst = self.mid.at[self.slot(u) + (ALL, ALL, HALVES[half], slice(None))]
                add_into(dst, self.view(u, 0, 0, half), *[got.at[name] for name in names], fresh=True)
        self.launch(u, phase + 1)

    def finish(self):
        for u in range(N_UNITS):
            for phase in range(TRIO):
                self.drain(u, phase)
        half = self.fin.at[:, pl.ds(0, SHARE)]
        swaps = self.copy(half, half, (self.swap_sems.at[0], self.swap_sems.at[1]), self.peer)
        swaps.wait_send()
        swaps.wait_recv()
        for u in range(N_UNITS):
            self.kept(u).wait()


def attend(heads, qt, do_t, k, kt, v, vt, cos, sin, o_row, ot, dq, dkt, dvt, s_scr, e_scr, p_scr, d_scr):
    f32, bf16 = jnp.float32, jnp.bfloat16
    strip = TURN
    work = [(h, j) for j in range(NBLK) for h in range(len(heads))]

    def strips(c):
        return [(i * strip, slice(c * QB + i * strip, c * QB + (i + 1) * strip)) for i in range(QB // strip)]

    def fold(x, op):
        return op(x.reshape(strip // SUBS, SUBS, QB), axis=0)

    def scores(i):
        (h, j), b = work[i], i % DUO
        q_t = qt[heads[h], j * QB:(j + 1) * QB]
        top = jnp.full((SUBS, QB), -jnp.inf, f32)
        for c in range(j + 1):
            tile = dot(k[c * QB:(c + 1) * QB, :], q_t)
            for at, rows in strips(c):
                s = tile[at:at + strip]
                if c == j:
                    seen = lax.broadcasted_iota(jnp.int32, (strip, QB), 0) + at <= lax.broadcasted_iota(jnp.int32, (strip, QB), 1)
                    s = jnp.where(seen, s, -jnp.inf)
                s_scr[b, rows, :] = s
                top = jnp.maximum(top, fold(s, jnp.max))
        return jnp.max(top, axis=0, keepdims=True)

    def rest(i, m):
        (h, j), b = work[i], i % DUO
        cols, n = slice(j * QB, (j + 1) * QB), (j + 1) * QB
        q_t, d_t = qt[heads[h], cols], do_t[heads[h], cols]
        tot = jnp.zeros((SUBS, QB), f32)
        for c in range(j + 1):
            for at, rows in strips(c):
                e = jnp.exp2((s_scr[b, rows, :] - m) * (SCALE * LOG2E))
                s_scr[b, rows, :] = e
                e_scr[b, rows, :] = e.astype(bf16)
                tot = tot + fold(e, jnp.sum)
        den = jnp.sum(tot, axis=0, keepdims=True)
        inv = 1.0 / den
        o = (dot(vt[:, :n], e_scr[b, :n, :]) / den).astype(bf16)
        ot[o_row(h), cols] = o
        delta = jnp.sum(d_t.astype(f32) * o.astype(f32), axis=0, keepdims=True)
        for c in range(j + 1):
            dp = dot(v[c * QB:(c + 1) * QB, :], d_t)
            for at, rows in strips(c):
                p = s_scr[b, rows, :] * inv
                p_scr[b, rows, :] = p.astype(bf16)
                d_scr[b, rows, :] = (p * (dp[at:at + strip] - delta)).astype(bf16)
        dvt[:, :n] += dot_nt(d_t, p_scr[b, :n, :])
        dkt[:, :n] += dot_nt(q_t, d_scr[b, :n, :])
        g = dot(kt[:, :n], d_scr[b, :n, :]) * SCALE
        co, si = cos[:, cols], sin[:, cols]
        x, y = g[:TURN], g[TURN:]
        dq[heads[h], cols] = jnp.concatenate([x * co + y * si, y * co - x * si], axis=0).astype(bf16)

    m = scores(0)
    for i in range(len(work)):
        later = scores(i + 1) if i + 1 < len(work) else None
        rest(i, m)
        m = later


def tail_kernel(qt, do_t, k, kt, v, vt, rt, dyc, wqk, wqkp, wvo, wvop, gain, hidden, dy, pos, cos, sin,
                result, grad_x, gq, gk, gv, go, gout,
                two, ks, kts, vs, vts, rts, ots, dqo, dqp, dkvo, dkvp, dkt, dvt, s_scr, e_scr, p_scr, d_scr, dycs, part, mid, buf1, buf2, buf3, fin, own, onat, dnat, xs, gacc, gpart, gpeer, gz, gy, gx,
                send_sems, recv_sems, swap_sems, trade_send, trade_recv, local_sems):
    comm = OldComm(trade_send, trade_recv, local_sems)
    comm.used = DUO * HEADS
    f32, bf16 = jnp.float32, jnp.bfloat16
    core, peer = comm.core, comm.peer()
    a1, a2 = two.at[0], two.at[1]
    comm.announce()
    sc = Scatter(comm, part, mid, (buf1, buf2, buf3), fin, (gq, gk, gv, go), send_sems, recv_sems, swap_sems)
    plan = Plan()
    some, most = pl.ds(0, PAIR), pl.ds(PAIR, HALF - PAIR)
    loads = [comm.local(s, d) for s, d in ((qt.at[some], two.at[0, some]), (k, ks), (do_t.at[some], two.at[1, some]), (vt, vts), (v, vs), (kt, kts))]
    dkt[...] = jnp.zeros_like(dkt)
    dvt[...] = jnp.zeros_like(dvt)
    with scope('wait_q'):
        for c in loads:
            c.wait()
    loads = [comm.local(s, d) for s, d in ((rt, rts), (qt.at[most], two.at[0, most]), (do_t.at[most], two.at[1, most]))]
    later = [comm.local(s, d) for s, d in ((dyc, dycs), (hidden, xs))]

    def emit(stages):
        for u, stage in stages:
            with scope(f'u{u}_s{stage}'):
                if u == GAIN:
                    sum_gain(stage)
                else:
                    sc.run(u, stage)

    def after(cost):
        plan.now += cost
        return plan.due()

    def head_trades(h):
        row = tile_at(core * HEADS + h, LANES)
        mine = tile_at(h, LANES)
        return [pltpu.make_async_remote_copy(src_ref=s, dst_ref=d, send_sem=trade_send.at[i], recv_sem=trade_recv.at[i], device_id=peer, device_id_type=MESH)
                for s, d, i in ((ots.at[row], ots.at[row], h), (dqo.at[mine], dqp.at[mine], HEADS + h))]

    def gradient(place, left, right, mul):
        with scope('grad'):
            @pl.loop(0, DUO)
            def _(z):
                g = mul(left[tile_at(z, HALF), :], right())
                for i in range(DUO):
                    part[place + i, tile_at(z, DUO)] = g[:, i * LANES:(i + 1) * LANES].reshape(DUO, RING, RING, CHIP, LANES)

    PAIRS = HEADS // DUO
    attended, paired = [], []
    for g in range(PAIRS):
        attended.append(after(5.2))
        plan.now += 1.6
        plan.start(DUO * g)
        plan.start(DUO * g + 1)
        paired.append(plan.due())

    @pl.loop(0, PAIRS)
    def _(g):
        def at(table):
            for i in range(PAIRS):
                if table[i]:
                    pl.when(g == i)(functools.partial(emit, table[i]))

        heads = [tile_at(DUO * g + i, LANES) for i in range(DUO)]
        with scope('attend'):
            attend(heads, a1, a2, ks, kts, vs, vts, cos, sin, lambda i: tile_at(core * HEADS + DUO * g + i, LANES), ots, dqo, dkt, dvt, s_scr, e_scr, p_scr, d_scr)

        @pl.when(g == 0)
        def _():
            with scope('entry'):
                comm.meet()
                for c in loads:
                    c.wait()
        for i in range(DUO):
            for c in head_trades(DUO * g + i):
                c.start()
        at(attended)
        gradient(DUO * g, rts, lambda: dqo[tile_at(g, PAIR), :], dot_nt)
        at(paired)

    def beat(cost, *starts):
        plan.now += cost
        for u in starts:
            plan.start(u)
        emit(plan.due())

    wkv, wkvp = e_scr.reshape(DIM, PAIR), p_scr.reshape(DIM, PAIR)
    later += [comm.local(src.at[:, pl.ds(at, LANES)], dst.at[:, pl.ds(to, LANES)]) for srcs, dst in (((wqk, wvo), wkv), ((wqkp, wvop), wkvp)) for src, at, to in ((srcs[0], HALF, 0), (srcs[1], 0, LANES))]
    wqp_loads = [comm.local(wqkp.at[tile_at(i, HALF), pl.ds(0, HALF)], two.at[i]) for i in range(DUO)]
    key = dkt[...] * SCALE
    co, si, x, y = cos[...], sin[...], key[:TURN], key[TURN:]
    dkvo[:LANES, :] = jnp.concatenate([x * co + y * si, y * co - x * si], axis=0).astype(bf16)
    dkvo[LANES:, :] = dvt[...].astype(bf16)
    comm.trade(dkvo, dkvp)
    gradient(UNIT_K, rts, lambda: dkvo[...], dot_nt)
    beat(2.0, UNIT_K, UNIT_V)
    wq_load = comm.local(wqk.at[:, pl.ds(0, HALF)], rts)
    for c in later:
        c.wait()
    with scope('trades'):
        for h in range(HEADS):
            for c in head_trades(h):
                c.wait()

    waiting = list(range(RING))

    def output_gradients(force=False):
        while waiting:
            first = 10 + DUO * waiting[0]
            before = [u for u in range(N_UNITS) if u < first and PLACE[u] in (PLACE[first], PLACE[first + 1])]
            if force:
                emit(plan.rush(lambda: all(map(plan.vacated, before))))
            if not all(map(plan.vacated, before)):
                return
            for u in before:
                sc.drain(u, 0)
            i = waiting.pop(0)
            gradient(PLACE[first], ots, lambda: dycs[:, i * PAIR:(i + 1) * PAIR], dot)
            plan.start(first)
            plan.start(first + 1)
            beat(1.5)

    def piece(cost):
        beat(cost)
        output_gradients()

    def ticking(n, cost, body):
        tables = [after(cost) for _ in range(n)]

        @pl.loop(0, n)
        def _(i):
            body(i)
            for j, table in enumerate(tables):
                if table:
                    pl.when(i == j)(functools.partial(emit, table))
        output_gradients()

    @pl.loop(0, TOKENS // LANES)
    def _(i):
        want = lax.broadcasted_iota(jnp.int32, (LANES, ROWS), 0) + i * LANES
        own[tile_at(i, LANES), :] = jnp.where(want == pos[...], 1.0, 0.0).astype(bf16)

    def unsort(at, src_t, n):
        with scope('unsort'):
            dnat[at:at + n, :] = dot(src_t[:n, :], own[...]).astype(bf16)

    output_gradients()
    for i in range(DUO):
        with scope('unsort_o'):
            @pl.loop(0, DUO)
            def _(j):
                r = pl.ds(pl.multiple_of(i * HALF + j * ROWS, ROWS), ROWS)
                onat[:, r] = dot(ots[r, :], own[...]).astype(bf16).T
        piece(1.4)
    for c in comm.exchanged:
        c.wait_recv()
    unsort(0, dqo, HALF)
    dy_loads = [comm.local(dy.at[:, tile_at(i, HALF)], dqo.at[tile_at(i, ROWS)]) for i in range(DUO)]
    piece(1.2)
    unsort(HALF, dqp, HALF)
    piece(1.2)
    unsort(DUO * HALF, dkvo, PAIR)
    unsort(DUO * HALF + PAIR, dkvp, PAIR)
    piece(0.7)
    wq_load.wait()
    for c in wqp_loads + dy_loads:
        c.wait()
    gacc[...] = jnp.zeros_like(gacc)

    def dr_parts(half, r):
        return [s_scr.at[half, r(i * PAIR), :] for i in range(RING)]

    def back(block, then):
        def dr(half):
            with scope('dr'):
                c = tile_at(half, HALF)
                left = jnp.concatenate([rts[c, :], two[half], wkv[c, :], wkvp[c, :]], axis=1)
                acc = dot(left, dnat[:, block * PAIR:(block + 1) * PAIR])
                for i, ref in enumerate(dr_parts(half, lambda at: pl.ds(at, PAIR))):
                    ref[...] = acc[i * PAIR:(i + 1) * PAIR, :].T

        def norm(part):
            with scope('back'):
                @pl.loop(0, RING)
                def _(i):
                    j = part * RING + i
                    q = pl.ds(pl.multiple_of(block * PAIR + j * SHARE, SHARE), SHARE)
                    d = jnp.concatenate([ref[...] for half in range(DUO) for ref in dr_parts(half, lambda at: pl.ds(pl.multiple_of(at + j * SHARE, SHARE), SHARE))], axis=1)
                    x = xs[q, :].astype(f32)
                    inv = lax.rsqrt(jnp.mean(x * x, axis=-1, keepdims=True) + RMS_EPS)
                    unit = x * inv
                    gacc[...] += jnp.sum((d * unit).reshape(DUO, SUBS, DIM), axis=0)
                    dg = d * gain[0:1, :]
                    new = inv * (dg - unit * jnp.mean(dg * unit, axis=-1, keepdims=True))
                    for half in range(DUO):
                        r = pl.ds(pl.multiple_of(half * ROWS + block * PAIR + j * SHARE, SHARE), SHARE)
                        dqo[r, :] = (dqo[r, :].astype(f32) + new[:, half * HALF:(half + 1) * HALF]).astype(bf16)

        ticking(DUO, 1.7, dr)
        then()
        ticking(RING, 0.92, norm)

    back(0, lambda: None)
    wo_loads = []
    back(1, lambda: wo_loads.extend([comm.local(wvo.at[:, pl.ds(LANES, HALF)], rts)] + [comm.local(wvop.at[tile_at(i, HALF), pl.ds(LANES, HALF)], two.at[i]) for i in range(DUO)]))
    for i in range(DUO):
        comm.store(dqo.at[tile_at(i, ROWS)], grad_x.at[:, tile_at(i, HALF)])
    total = jnp.sum(gacc[...], axis=0, keepdims=True)
    gpart[...] = jnp.zeros_like(gpart)
    for i in range(RING):
        for j in range(RING):
            gpart[i, j:j + 1, :] = total[:, (i * RING + j) * LANES:(i * RING + j + 1) * LANES]

    arrivals = []

    def sum_gain(stage):
        for c in arrivals:
            c.wait_recv()
        del arrivals[:]
        if stage == 0:
            arrivals.append(comm.send(gpart, gpeer, peer))
        elif stage == 1:
            for j in range(RING):
                gz[j] = gpart[j] + gpeer[j]
            arrivals.extend(comm.send(gz.at[step(comm.pos, 'z', hop)], gz.at[TRIO + hop], comm.far('z', hop)) for hop in (1, DUO, TRIO))
        elif stage == DUO:
            gy[0] = (gz[comm.pos['z']] + gz[RING]) + (gz[5] + gz[6])
            arrivals.extend(comm.send(gy.at[0], gy.at[hop], comm.far('y', hop)) for hop in (1, DUO, TRIO))
        elif stage == TRIO:
            gx[0] = (gy[0] + gy[1]) + (gy[DUO] + gy[TRIO])
            arrivals.extend(comm.send(gx.at[0], gx.at[hop], comm.far('x', hop)) for hop in (1, DUO, TRIO))
        else:
            gpeer[0] = (gx[0] + gx[1]) + (gx[DUO] + gx[TRIO])
            mine = jnp.broadcast_to(gpeer[0, pl.ds(comm.pos['y'], 1), :], (SUBS, LANES))
            gout[...] = pltpu.roll(mine, LANES - (comm.pos['x'] * CHIP + core * SHARE), 1)

    plan.start(GAIN)
    beat(0.2)
    output_gradients(True)

    def project_out(col, weights, i):
        with scope('project'):
            @pl.loop(DUO * i, DUO * i + DUO)
            def _(j):
                c = tile_at(j, PAIR)
                dst = pl.ds(pl.multiple_of(col + j * PAIR, PAIR), PAIR)
                xs[:, dst] = (xs[:, dst].astype(f32) + dot(onat[...], weights(c))).astype(bf16)
        beat(1.55)

    def own_half(c):
        return rts[:, c]

    def other_half(c):
        return jnp.concatenate([a1[:, c], a2[:, c]], axis=0)

    for c in wo_loads:
        c.wait()
    for col, weights in ((core * HALF, own_half), ((1 - core) * HALF, other_half)):
        for i in range(DUO):
            project_out(col, weights, i)
    comm.store(xs, result)
    emit(plan.rush(lambda: not plan.stage))
    with scope('finish'):
        sc.finish()
        for c in comm.sent + comm.exchanged:
            c.wait_send()
        for c in comm.stored:
            c.wait()


def tail(qt, do_t, k, kt, v, vt, rt, dyc, wqk, wqkp, wvo, wvop, gain, hidden, dy, pos, cos, sin):
    bf16, f32 = jnp.bfloat16, jnp.float32
    any_ = pl.BlockSpec(memory_space=pl.ANY)
    vmem = pl.BlockSpec(memory_space=pltpu.VMEM)
    S = lambda shape, d=bf16: jax.ShapeDtypeStruct(shape, d)
    V = lambda shape, d=bf16: pltpu.VMEM(shape, d)
    D = lambda n: pltpu.SemaphoreType.DMA((n,))
    sq, tall, wide = (HALF, TOKENS), (TOKENS, LANES), (LANES, TOKENS)
    mine, kv = (ROWS, DIM), (PAIR, TOKENS)
    return pl.pallas_call(
        tail_kernel,
        out_shape=[S(mine), S(mine), S((SHARE, DIM), f32), S((SHARE, PAIR), f32), S((SHARE, PAIR), f32), S((SHARE, DIM), f32), S((SUBS, LANES), f32)],
        in_specs=[any_] * 12 + [vmem] + [any_] * DUO + [vmem] * TRIO,
        out_specs=[any_] * 6 + [vmem],
        scratch_shapes=[V((DUO,) + sq), V(tall), V(wide), V(tall), V(wide), V((DIM, TOKENS)), V((DIM, TOKENS)), V(sq), V(sq), V(kv), V(kv), V(wide, f32), V(wide, f32),
                        V((DUO, TOKENS, QB), f32), V((DUO, TOKENS, QB)), V((DUO, TOKENS, QB)), V((DUO, TOKENS, QB)), V(sq), V((PLACES, RING, RING, RING, CHIP, LANES), f32), V((TRIO, SLOTS, RING, RING, CHIP, LANES), f32),
                        V((TRIO, SLOTS, 6, RING, RING, SHARE, LANES), f32), V((TRIO, SLOTS, 6, RING, SHARE, LANES), f32), V((TRIO, SLOTS, TRIO, CHIP, LANES), f32), V((N_UNITS, CHIP, LANES), f32), V((TOKENS, ROWS)), V(mine), V((DUO * QKV, ROWS)), V(mine),
                        V((SUBS, DIM), f32), V((RING, SUBS, LANES), f32), V((RING, SUBS, LANES), f32), V((7, SUBS, LANES), f32), V((RING, SUBS, LANES), f32), V((RING, SUBS, LANES), f32),
                        D(TRIO * N_UNITS), D(6 * N_UNITS), D(DUO + N_UNITS), D(DUO * HEADS + SHARE), D(DUO * HEADS + SHARE), D(CHIP)],
        compiler_params=pltpu.CompilerParams(collective_id=1, has_side_effects=True, vmem_limit_bytes=67043328),
        name='tail',
    )(qt, do_t, k, kt, v, vt, rt, dyc, wqk, wqkp, wvo, wvop, gain, hidden, dy, pos, cos, sin)


def settle_kernel(n, *refs):
    ins, gain, outs, gain_out, bufs, sems = refs[:n], refs[n], refs[n + 1:DUO * n + 1], refs[DUO * n + 1], refs[DUO * n + DUO:-1], refs[-1]
    jobs = []
    for a, o, b in zip(ins, outs, bufs):
        size = a.shape[0] // RING if a.shape[0] == ROWS else a.shape[0]
        jobs += [tuple(r.at[pl.ds(i, size)] for r in (a, b, o)) for i in range(0, a.shape[0], size)]
    takes = [pltpu.make_async_copy(a, b, sems.at[0, i]) for i, (a, b, _) in enumerate(jobs)]
    puts = [pltpu.make_async_copy(b, o, sems.at[1, i]) for i, (_, b, o) in enumerate(jobs)]
    for c in takes:
        c.start()
    gain_out[...] = gain[0:1, :SHARE]
    for take, put in zip(takes, puts):
        take.wait()
        put.start()
    for c in puts:
        c.wait()


def settle(*arrays):
    *large, gain = arrays
    any_, vmem = pl.BlockSpec(memory_space=pl.ANY), pl.BlockSpec(memory_space=pltpu.VMEM)
    return pl.pallas_call(
        functools.partial(settle_kernel, len(large)),
        out_shape=[jax.ShapeDtypeStruct(a.shape, a.dtype) for a in large] + [jax.ShapeDtypeStruct((1, SHARE), gain.dtype)],
        in_specs=[any_] * len(large) + [vmem],
        out_specs=[any_] * len(large) + [vmem],
        scratch_shapes=[pltpu.VMEM(a.shape, a.dtype) for a in large] + [pltpu.SemaphoreType.DMA((DUO, 12))],
        name='settle',
    )(*arrays)


def rope_tables():
    j = np.arange(HEAD_DIM // DUO, dtype=np.float64) / (HEAD_DIM // DUO)
    freq = (ROPE_THETA ** -j).astype(np.float32)
    angle = freq[:, None] * np.arange(TOKENS, dtype=np.float32)[None, :]
    return np.cos(angle.astype(np.float64)).astype(np.float32), np.sin(angle.astype(np.float64)).astype(np.float32)


def solution(mesh):
    def shard_fn(hidden, tok_pos, grad_out, norm_gain, w_query, w_key, w_value, w_out):
        hidden, grad_out = hidden[0], grad_out[0]
        cos_t, sin_t = (jnp.asarray(t) for t in rope_tables())
        *parts, gain = head(hidden, grad_out, w_query, w_key, w_value, w_out, tok_pos, norm_gain.reshape(1, SHARE), cos_t, sin_t)
        parts = [p.reshape(DIM, GROUP) if p.ndim > DUO else p for p in parts]
        result, grad_hidden, gq, gk, gv, go, gout = settle(*tail(*parts, gain, hidden, grad_out, tok_pos, cos_t, sin_t))
        return result[None], grad_hidden[None], gq, gk, gv, go, gout.reshape(SHARE)

    row_spec, pos_spec = P('fsdp', 'cp', None), P('fsdp', 'cp')
    weight_spec, gain_spec = P(('fsdp', 'cp'), None), P(('fsdp', 'cp'))
    return jax.shard_map(shard_fn, mesh=mesh, in_specs=(row_spec, pos_spec, row_spec, gain_spec, weight_spec, weight_spec, weight_spec, weight_spec), out_specs=(row_spec, row_spec, weight_spec, weight_spec, weight_spec, weight_spec, gain_spec), check_vma=False)
```

```python
import functools
import jax
import jax.numpy as jnp
import numpy as np
from jax import lax
from jax.experimental import pallas as pl
from jax.experimental.pallas import tpu as pltpu
from jax.sharding import PartitionSpec as P

LANES, SUBS, RING, TRIO, DUO = 128, 8, 4, 3, 2
PAIR, ROWS, CHIP, SHARE, TURN = 256, 512, 32, 16, 64
HEAD_DIM = LANES
ROPE_THETA = 1000000.0
RMS_EPS = 1e-5
SCALE = HEAD_DIM ** -0.5
LOG2E = 1.4426950408889634

MESH = pl.DeviceIdType.MESH
AXES = ('x', 'y', 'z')
ORDERS = (('x', 'y', 'z'), ('y', 'z', 'x'), ('z', 'x', 'y'))
ALL = pl.ds(0, RING)


def torus():
    f = lax.axis_index('fsdp')
    return {'x': lax.rem(f, RING), 'y': lax.rem(lax.div(f, RING), RING), 'z': lax.div(f, SHARE)}


def step(pos, axis, hop):
    return lax.rem(pos[axis] + hop, RING)


class Batch:
    def __init__(self, comm):
        self.comm, self.index = comm, comm.used
        comm.used += 1

    def _copy(self, src, dst, device):
        send, recv, _ = self.comm.sems
        return pltpu.make_async_remote_copy(src_ref=src, dst_ref=dst, send_sem=send.at[self.index], recv_sem=recv.at[self.index], device_id=device, device_id_type=MESH)

    def send(self, src, dst, device):
        self._copy(src, dst, device).start()
        return self

    def arrived(self, whole):
        self._copy(whole, whole, self.comm.peer()).wait_recv()

    def sent(self, whole):
        self._copy(whole, whole, self.comm.peer()).wait_send()


class Comm:
    def __init__(self, send_sems, recv_sems, local_sems):
        self.pos = torus()
        self.core = lax.axis_index('cp')
        self.sems = (send_sems, recv_sems, local_sems)
        self.used = self.used_local = 0
        self.stored = []

    def far(self, axis, hop):
        p = dict(self.pos)
        p[axis] = step(self.pos, axis, hop)
        return {'fsdp': (p['z'] * RING + p['y']) * RING + p['x'], 'cp': self.core}

    def peer(self):
        return {'fsdp': lax.axis_index('fsdp'), 'cp': 1 - self.core}

    def aside(self, dy, dx):
        return {'fsdp': (self.pos['z'] * RING + step(self.pos, 'y', dy)) * RING + step(self.pos, 'x', dx), 'cp': self.core}

    def announce(self, corners=()):
        sem = pltpu.get_barrier_semaphore()
        for axis in AXES:
            for hop in (1, DUO, TRIO):
                pl.semaphore_signal(sem, inc=1, device_id=self.far(axis, hop), device_id_type=MESH)
        for dy, dx in corners:
            pl.semaphore_signal(sem, inc=1, device_id=self.aside(dy, dx), device_id_type=MESH)
        pl.semaphore_signal(sem, inc=1, device_id=self.peer(), device_id_type=MESH)

    def meet(self, corners=()):
        pl.semaphore_wait(pltpu.get_barrier_semaphore(), 10 + len(corners))

    def ring(self, batch, src, slots, axis):
        for hop in (1, DUO, TRIO):
            batch.send(src, slots.at[hop], self.far(axis, hop))

    def local(self, src, dst):
        i = self.used_local
        self.used_local += 1
        c = pltpu.make_async_copy(src, dst, self.sems[DUO].at[i])
        c.start()
        return c

    def store(self, src, dst):
        self.stored.append(self.local(src, dst))


class Singles(Comm):
    def __init__(self, *sems):
        super().__init__(*sems)
        self.sent, self.exchanged = [], []

    def _copy(self, src, dst, device):
        i = self.used
        self.used += 1
        c = pltpu.make_async_remote_copy(src_ref=src, dst_ref=dst, send_sem=self.sems[0].at[i], recv_sem=self.sems[1].at[i], device_id=device, device_id_type=MESH)
        c.start()
        return c

    def send(self, src, dst, device):
        c = self._copy(src, dst, device)
        self.sent.append(c)
        return c

    def trade(self, src, dst):
        self.exchanged.append(self._copy(src, dst, self.peer()))


def pick(ref, sel, cols):
    return ref.at[sel['z'], sel['y'], sel['x'], :, pl.ds(cols[0], cols[1])]


def sem_scratch(remote, local):
    return [pltpu.SemaphoreType.DMA((remote,)), pltpu.SemaphoreType.DMA((remote,)), pltpu.SemaphoreType.DMA((local,))]


def add_into(dst, *srcs, fresh=False):
    def add(idx):
        total, *rest = [s[idx] for s in (srcs if fresh else (dst,) + srcs)]
        for more in rest:
            total = total + more
        dst[idx] = total

    if len(dst.shape) > TRIO:
        @pl.loop(0, dst.shape[0])
        def _(i):
            add((i,))
    else:
        add(Ellipsis)


QK_COLORS = ((0, PAIR, LANES), (384, LANES, PAIR), (768, PAIR, LANES))
VO_COLORS = ((0, LANES, PAIR), (384, PAIR, LANES), (768, LANES, PAIR))
TOKENS = 1024
DIM = 2048
HALF = 1024
QKV = 1280
GROUP = 1152


def scope(name):
    return jax.named_scope(name)


def dot(a, b):
    return jnp.dot(a, b, preferred_element_type=jnp.float32)


def dot_nt(a, b):
    return lax.dot_general(a, b, (((1,), (1,)), ((), ())), preferred_element_type=jnp.float32)


def tile_at(i, n):
    return pl.ds(pl.multiple_of(i * n, n), n)


class Gather:
    def __init__(self, comm, ref, colors, land):
        self.comm, self.ref, self.colors, self.land = comm, ref, colors, land
        self.held = [dict(comm.pos) for _ in colors]
        self.batches = []

    def parts(self, k):
        lo, na, nb = self.colors[k]
        return (lo, na), (lo + na, nb)

    def move(self, batch, s, cols, to):
        batch.send(pick(self.ref, s, cols), pick(self.ref, s, cols), to)

    def at(self, k, hop):
        d = ORDERS[k][self.phase]
        return dict(self.held[k], **{d: step(self.comm.pos, d, hop)})

    def begin(self, phase):
        self.phase = phase
        self.up, self.dn, self.rest = ([Batch(self.comm) for _ in range(TRIO)] for _ in range(TRIO))
        self.batches += self.up + self.dn + self.rest
        for k in range(TRIO):
            a, b = self.parts(k)
            d = ORDERS[k][phase]
            up, dn, s = self.comm.far(d, 1), self.comm.far(d, TRIO), self.held[k]
            self.move(self.up[k], s, a, up)
            self.move(self.dn[k], s, b, dn)
            self.move(self.rest[k], s, b, up)
            self.move(self.rest[k], s, a, dn)
            if phase == 0:
                for cols in (a, b):
                    self.move(self.rest[k], s, cols, self.comm.far(d, DUO))
        if phase == DUO:
            for k in range(TRIO):
                for cols in self.parts(k):
                    self.land(self.ref, self.held[k], cols)

    def forward(self):
        for k in range(TRIO):
            a, b = self.parts(k)
            d = ORDERS[k][self.phase]
            for batch, hop, cols, to in ((self.up[k], TRIO, a, 1), (self.dn[k], 1, b, TRIO)):
                s = self.at(k, hop)
                batch.arrived(pick(self.ref, s, cols))
                if self.phase:
                    self.move(self.rest[k], s, cols, self.comm.far(d, to))
                if self.phase == DUO:
                    self.land(self.ref, s, cols)

    def end(self):
        for k in range(TRIO):
            a, b = self.parts(k)
            d = ORDERS[k][self.phase]
            two = dict(self.held[k], **{d: pl.ds(0, DUO)})
            self.rest[k].arrived(pick(self.ref, two, (a[0], a[1] + b[1])))
            if self.phase == DUO:
                for hop, cols in ((TRIO, b), (1, a), (DUO, a), (DUO, b)):
                    self.land(self.ref, self.at(k, hop), cols)
            for batch, s, cols in ((self.up[k], self.held[k], a), (self.dn[k], self.held[k], b), (self.rest[k], two, (a[0], a[1] + b[1]))):
                batch.spent = pick(self.ref, s, cols)
            self.held[k] = dict(self.held[k], **{d: ALL})

    def finish(self):
        for batch in self.batches:
            batch.sent(batch.spent)


def head_kernel(hidden, dy, wq, wk, wv, wo, pos, gain_in, cos_t, sin_t,
                qt_o, dot_o, k_o, kt_o, v_o, vt_o, rt_o, dyc_o, wqk_o, wqkp_o, wvo_o, wvop_o, gain_o,
                hid2, dy2, dys, rs, rt, wqk, wvo, wpeer, pi, pos2, qt, dot_s, kk, kt, vv, vt, gain, gtile, gbuf, gx, gy, gz, *sems):
    comm = Comm(*sems)
    pos_c, core = comm.pos, comm.core
    bf16, f32 = jnp.bfloat16, jnp.float32
    peer = comm.peer()
    rows = tile_at(core, SHARE)
    mine_qk = wqk.at[pos_c['z'], pos_c['y'], pos_c['x'], rows]
    mine_vo = wvo.at[pos_c['z'], pos_c['y'], pos_c['x'], rows]

    def weight_parts(c):
        return ((wq.at[:, tile_at(c, HALF)], mine_qk.at[:, pl.ds(0, HALF)]), (wk.at[:, tile_at(c, LANES)], mine_qk.at[:, pl.ds(HALF, LANES)]),
                (wv.at[:, tile_at(c, LANES)], mine_vo.at[:, pl.ds(0, LANES)]), (wo.at[:, tile_at(c, HALF)], mine_vo.at[:, pl.ds(LANES, HALF)]))

    loads = [comm.local(s, d) for s, d in weight_parts(core)]
    load_x = [comm.local(hidden, hid2.at[pl.ds(0, ROWS)]), comm.local(dy, dy2.at[pl.ds(0, ROWS)])]
    share = lax.broadcasted_iota(jnp.int32, (SUBS, LANES), 1) // SHARE
    gtile[...] = jnp.where(share == pos_c['x'] * DUO + core, jnp.broadcast_to(jnp.concatenate([gain_in[...]] * SUBS, axis=1), (SUBS, LANES)), 0.0)
    comm.announce()
    with scope('entry'):
        comm.meet()
    swap_w, swap_pos, swap_dy, swap_x, peers_qk, peers_vo = (Batch(comm) for _ in range(6))
    gain_c, gain_x, gain_y, gain_z = (Batch(comm) for _ in range(RING))
    for s, d in weight_parts(1 - core):
        swap_w.send(s, d, peer)
    gain_c.send(gtile, gbuf, peer)
    swap_pos.send(pos, pos2, peer)
    for c in loads:
        c.wait()
    with scope('wait_w'):
        swapped = wqk.at[pos_c['z'], pos_c['y'], pos_c['x']]
        swap_w.arrived(swapped)

    def land_qk(ref, s, cols):
        peers_qk.send(pick(ref, s, cols), pick(wqkp_o, s, cols), peer)

    def land_vo(ref, s, cols):
        peers_vo.send(pick(ref, s, cols), pick(wpeer, s, cols), peer)

    g1 = Gather(comm, wqk, QK_COLORS, land_qk)
    g2 = Gather(comm, wvo, VO_COLORS, land_vo)
    g1.begin(0)
    g2.begin(0)
    swap_dy.send(dy, dy2.at[pl.ds(ROWS, ROWS)], peer)
    gain_c.arrived(gbuf)
    gx[0] = gtile[...] + gbuf[...]
    comm.ring(gain_x, gx.at[0], gx, 'x')

    swap_pos.arrived(pos2)

    @pl.loop(0, TOKENS // LANES)
    def _(i):
        want = lax.broadcasted_iota(jnp.int32, (LANES, ROWS), 0) + i * LANES
        for h, have in enumerate((pos, pos2)):
            pi[tile_at(i, LANES), h * ROWS:(h + 1) * ROWS] = jnp.where(want == have[...], 1.0, 0.0).astype(bf16)

    def sort(dst, src, first, last):
        with scope('sort'):
            @pl.loop(first, last)
            def _(j):
                c = tile_at(j, PAIR)
                dst[:, c] = dot(pi[...], src[:, c]).astype(bf16)

    with scope('p0_end'):
        for g in (g1, g2):
            g.forward()
            g.end()
            g.begin(1)
    swap_x.send(hidden, hid2.at[pl.ds(ROWS, ROWS)], peer)
    gain_x.arrived(gx.at[pl.ds(1, TRIO)])
    gy[pos_c['y']] = (gx[0] + gx[1]) + (gx[DUO] + gx[TRIO])
    for hop in (1, DUO, TRIO):
        gain_y.send(gy.at[pos_c['y']], gy.at[pos_c['y']], comm.far('y', hop))
    with scope('wait_dy'):
        load_x[1].wait()
        swap_dy.arrived(dy2.at[pl.ds(ROWS, ROWS)])
    sort(dys, dy2, 0, RING)
    with scope('p1q_fwd'):
        g1.forward()
    sort(dys, dy2, RING, 6)
    with scope('p1o_fwd'):
        g2.forward()
    sort(dys, dy2, 6, SUBS)
    with scope('p1q_end'):
        g1.end()
    g1.begin(DUO)
    comm.store(dys.at[:, tile_at(core, HALF)], dyc_o)
    gain_y.arrived(gy.at[pl.ds(1, TRIO)])
    for j in range(RING):
        gz[pos_c['z'], j] = gy[j]
    for hop in (1, DUO, TRIO):
        gain_z.send(gz.at[pos_c['z']], gz.at[pos_c['z']], comm.far('z', hop))
    with scope('p1o_end'):
        g2.end()
    with scope('wait_x'):
        load_x[0].wait()
        swap_x.arrived(hid2.at[pl.ds(ROWS, ROWS)])
    sort(rs, hid2, 0, SUBS)
    with scope('p2q_fwd'):
        g1.forward()
    g2.begin(DUO)
    with scope('gain'):
        gain_z.arrived(gz.at[pl.ds(1, TRIO)])
    for i in range(RING):
        for j in range(RING):
            gain[:, (i * RING + j) * LANES:(i * RING + j + 1) * LANES] = gz[i, j]
    comm.store(gain, gain_o)

    def norm(first, last):
        with scope('norm'):
            @pl.loop(first, last)
            def _(i):
                r = tile_at(i, CHIP)
                x = rs[r, :].astype(f32)
                inv = lax.rsqrt(jnp.mean(x * x, axis=-1, keepdims=True) + RMS_EPS)
                rs[r, :] = (x * inv * gain[0:1, :]).astype(bf16)

    norm(0, TOKENS // CHIP)
    with scope('r_t'):
        @pl.loop(0, DIM // PAIR)
        def _(i):
            c = tile_at(i, PAIR)

            @pl.loop(0, TOKENS // PAIR)
            def _(j):
                r = tile_at(j, PAIR)
                rt[c, r] = rs[r, c].T
    comm.store(rt, rt_o)
    with scope('p2q_end'):
        g1.end()
    comm.store(wqk, wqk_o)
    w_qk, w_vo, w_peer = wqk.reshape(DIM, GROUP), wvo.reshape(DIM, GROUP), wpeer.reshape(DIM, GROUP)

    def rotated(x, r):
        cos, sin = cos_t[:, r], sin_t[:, r]
        cos = jnp.concatenate([cos, cos], axis=0).T
        sin = jnp.concatenate([-sin, sin], axis=0).T
        return (x * cos + pltpu.roll(x, TURN, 1) * sin).astype(bf16)

    def queries(first, last):
        with scope('q'):
            @pl.loop(first, last)
            def _(t):
                x = dot(rs[...], w_qk[:, tile_at(t, PAIR)])
                for i in range(RING):
                    r = slice(i * PAIR, (i + 1) * PAIR)
                    for h in range(DUO):
                        qt[tile_at(DUO * t + h, LANES), r] = rotated(x[r, h * LANES:(h + 1) * LANES], r).T

    queries(0, DUO)
    with scope('p2o_fwd'):
        g2.forward()
    queries(DUO, RING)

    @pl.loop(0, DUO)
    def _(i):
        r = tile_at(i, ROWS)
        key = rotated(dot(rs[r, :], w_qk[:, HALF:]), r)
        kk[r, :] = key
        kt[:, r] = key.T
    for src, dst in ((kk, k_o), (kt, kt_o), (qt, qt_o)):
        comm.store(src, dst)
    with scope('p2o_end'):
        g2.end()
    with scope('vals'):
        @pl.loop(0, DUO)
        def _(i):
            r = tile_at(i, ROWS)
            val = dot(rs[r, :], w_vo[:, :LANES]).astype(bf16)
            vv[r, :] = val
            vt[:, r] = val.T
    for src, dst in ((vv, v_o), (vt, vt_o)):
        comm.store(src, dst)
    with scope('wo_peer'):
        peers_vo.arrived(wpeer)
    comm.store(wvo, wvo_o)
    comm.store(wpeer, wvop_o)

    with scope('do_t'):
        r = tile_at(core, HALF)

        @pl.loop(0, TOKENS // PAIR)
        def _(j):
            t = tile_at(j, PAIR)
            w_rows = jnp.concatenate([w_vo[r, LANES:], w_peer[r, LANES:]], axis=1)
            d_rows = jnp.concatenate([dys[t, tile_at(core, HALF)], dys[t, tile_at(1 - core, HALF)]], axis=1)
            dot_s[:, t] = dot_nt(w_rows, d_rows).astype(bf16)
    comm.store(dot_s, dot_o)
    with scope('finish'):
        peers_qk.arrived(wqk)
        for batch, whole in ((swap_w, swapped), (swap_pos, pos2), (swap_dy, dy2.at[pl.ds(ROWS, ROWS)]), (swap_x, hid2.at[pl.ds(ROWS, ROWS)]), (peers_qk, wqk), (peers_vo, wvo),
                             (gain_c, gbuf), (gain_x, gx.at[pl.ds(1, TRIO)]), (gain_y, gy.at[pl.ds(1, TRIO)]), (gain_z, gz.at[pl.ds(1, TRIO)])):
            batch.sent(whole)
        g1.finish()
        g2.finish()
        for c in comm.stored:
            c.wait()


def head(hidden, dy, wq, wk, wv, wo, pos, gain, cos_t, sin_t):
    bf16, f32 = jnp.bfloat16, jnp.float32
    any_ = pl.BlockSpec(memory_space=pl.ANY)
    vmem = pl.BlockSpec(memory_space=pltpu.VMEM)
    S = lambda shape, d=bf16: jax.ShapeDtypeStruct(shape, d)
    V = lambda shape, d=bf16: pltpu.VMEM(shape, d)
    group = (RING, RING, RING, CHIP, GROUP)
    sq, tall, wide = (HALF, TOKENS), (TOKENS, LANES), (LANES, TOKENS)
    full = (TOKENS, DIM)
    return pl.pallas_call(
        head_kernel,
        out_shape=[S(sq), S(sq), S(tall), S(wide), S(tall), S(wide), S((DIM, TOKENS)), S((TOKENS, HALF)), S(group), S(group), S(group), S(group), S((SUBS, DIM), f32)],
        in_specs=[any_] * 6 + [vmem] * RING,
        out_specs=[any_] * 13,
        scratch_shapes=[V(full), V(full), V(full), V(full), V((DIM, TOKENS)), V(group), V(group), V(group), V((TOKENS, TOKENS)), V((1, ROWS), jnp.int32),
                        V(sq), V(sq), V(tall), V(wide), V(tall), V(wide), V((SUBS, DIM), f32), V((SUBS, LANES), f32), V((SUBS, LANES), f32), V((RING, SUBS, LANES), f32), V((RING, SUBS, LANES), f32), V((RING, RING, SUBS, LANES), f32)] + sem_scratch(TURN, 18),
        compiler_params=pltpu.CompilerParams(collective_id=0, has_side_effects=True, vmem_limit_bytes=60 * DUO**20),
        name='head',
    )(hidden, dy, wq, wk, wv, wo, pos, gain, cos_t, sin_t)


HEADS = SUBS
UNIT_K, UNIT_V = SUBS, 9
N_UNITS = 18
GAIN = N_UNITS
SLOTS = RING
LAST = 5
ABREAST = DUO
LINES = ((0, TRIO, 6, 9, 12, 15), (1, RING, 7, 10, 13, SHARE), (DUO, 5, SUBS, 11, 14, 17))
COLOR = {u: k for k, line in enumerate(LINES) for u in line}
RANK = {u: i for line in LINES for i, u in enumerate(line)}
SWAPPED = ()
ORDER = {u: ORDERS[k] if u not in SWAPPED else (ORDERS[k][0], ORDERS[k][DUO], ORDERS[k][1]) for u, k in COLOR.items()}
BEFORE = {u: line[i - SLOTS] if i >= SLOTS else None for line in LINES for i, u in enumerate(line)}
PLACES = 12
PLACE = {u: u % PLACES for u in range(N_UNITS)}
WIRE = (2.85, 0.72, 0.36)
LATENCY = 2.6
STAGE_COST = 0.1
GAIN_STEP = 6.0


class Plan:
    def __init__(self):
        self.now, self.stage, self.ready, self.order, self.link = 0.0, {}, {}, [], {}
        self.mark = {}

    def _wire(self, u, phase, count):
        link = ORDER[u][phase]
        t = max(self.link.get(link, 0.0), self.now)
        first = t + WIRE[phase] + LATENCY
        self.link[link] = t + WIRE[phase] * count
        return first if phase < DUO else self.link[link] + LATENCY

    def free(self, u, phase):
        if BEFORE[u] is None:
            return True
        done = self.mark.get((BEFORE[u], (DUO, RING, 5)[phase]))
        if done is None:
            return False
        sent = ((0, 1), (DUO, TRIO), (RING,))[phase]
        return any(self.mark.get((j, s), -1) > done and (j, s + 1) in self.mark for j, order in ORDER.items() if order[phase] == ORDER[u][phase] for s in sent)

    def run(self, u):
        stage = self.stage[u]
        self.order.append((u, stage))
        self.mark[u, stage] = len(self.order)
        self.now = max(self.now, self.ready[u]) + STAGE_COST
        self.stage[u] = stage + 1
        if stage == (TRIO if u == GAIN else LAST):
            del self.stage[u]
        elif u == GAIN:
            self.ready[u] = self.now + GAIN_STEP
        elif stage % DUO:
            self.ready[u] = self._wire(u, stage // DUO, 1)
        else:
            self.ready[u] = self._wire(u, stage // DUO, DUO)

    def blocked(self, u):
        stage = self.stage[u]
        if u == GAIN:
            return False
        if stage == 0 and sum(0 < self.stage.get(j, 0) <= DUO for j in LINES[COLOR[u]]) >= ABREAST:
            return True
        if stage == DUO and BEFORE[u] is not None and (BEFORE[u], LAST) not in self.mark:
            return True
        return stage in (0, DUO, RING) and not self.free(u, stage // DUO)

    def start(self, u):
        self.stage[u], self.ready[u] = 0, self.now

    def due(self):
        first = len(self.order)
        while True:
            ripe = [(self.ready[u], u) for u in self.stage if self.ready[u] <= self.now and not self.blocked(u)]
            if not ripe:
                return self.order[first:]
            self.run(min(ripe)[1])

    def vacated(self, u):
        return (u, DUO) in self.mark

    def rush(self, done):
        first = len(self.order)
        while not done():
            self.run(min((self.ready[u], u) for u in self.stage if not self.blocked(u))[1])
        return self.order[first:]


QB = PAIR
NBLK = TOKENS // QB
HALVES = (pl.ds(0, SHARE), pl.ds(SHARE, SHARE))
PLANE = tuple((dy, dx) for dy in range(RING) for dx in range(RING) if dy or dx)
CORNERS = tuple((dy, dx) for dy, dx in PLANE if dy and dx)


class Scatter:
    def __init__(self, comm, part, mid, bufs, fin, outs, send_sems, recv_sems, swap_sems):
        self.pos, self.part, self.mid, self.bufs, self.fin, self.outs = comm.pos, part, mid, bufs, fin, outs
        self.send_sems, self.recv_sems, self.swap_sems = send_sems, recv_sems, swap_sems
        self.near = {(a, hop): comm.far(a, hop) for a in AXES for hop in (1, DUO, TRIO)}
        self.hops = {(a, hop): step(comm.pos, a, hop) for a in AXES for hop in (1, DUO, TRIO)}
        self.peer, self.core = comm.peer(), comm.core
        self.keep, self.give = tile_at(comm.core, SHARE), tile_at(1 - comm.core, SHARE)
        self.drained = set()

    def slot(self, u):
        return COLOR[u], RANK[u] % SLOTS

    def buf(self, u, phase):
        return self.bufs[phase].at[self.slot(u)]

    def view(self, u, phase, hop, half=None):
        order = ORDER[u]
        at = {a: ALL for a in AXES}
        for a in order[1:phase]:
            at[a] = self.pos[a]
        at[order[phase]] = self.hops[order[phase], hop] if hop else self.pos[order[phase]]
        rows = pl.ds(0, CHIP) if half is None else HALVES[half]
        if phase == 0:
            return self.part.at[PLACE[u], at['z'], at['y'], at['x'], rows, :]
        return self.mid.at[self.slot(u) + tuple(at[a] for a in 'zyx' if a != order[0]) + (rows, slice(None))]

    def copy(self, src, dst, sems, device):
        return pltpu.make_async_remote_copy(src_ref=src, dst_ref=dst, send_sem=sems[0], recv_sem=sems[1], device_id=device, device_id_type=MESH)

    def sems(self, u, phase, kind=0):
        at = u * TRIO + phase
        return self.send_sems.at[at], self.recv_sems.at[DUO * at + kind]

    def send(self, u, phase, name):
        axis = ORDER[u][phase]
        if phase == DUO:
            src, to = self.view(u, DUO, name + 1), name + 1
        else:
            hop, half, to = ((DUO, 0, 1), (DUO, 1, TRIO), (1, 1, 1), (TRIO, 0, TRIO), (1, 0, 1), (TRIO, 1, TRIO))[name]
            src = self.view(u, phase, hop, half)
        self.copy(src, self.buf(u, phase).at[name], self.sems(u, phase, int(name > 1 and phase < DUO)), self.near[axis, to]).start()

    def launch(self, u, phase):
        if BEFORE[u] is not None:
            self.drain(BEFORE[u], phase)
        for name in range(RING if phase < DUO else TRIO):
            self.send(u, phase, name)

    def arrived(self, u, phase, first, count):
        whole = self.buf(u, phase).at[pl.ds(first, count)]
        self.copy(whole, whole, self.sems(u, phase, int(first > 0)), self.peer).wait_recv()

    def drain(self, u, phase):
        if (u, phase) not in self.drained:
            self.drained.add((u, phase))
            whole = self.buf(u, phase)
            self.copy(whole, whole, self.sems(u, phase), self.peer).wait_send()

    def out(self, u):
        if u < HEADS:
            out, col = self.outs[0], self.core * HALF + u * LANES
        elif u < 10:
            out, col = self.outs[u - 7], self.core * LANES
        else:
            out, col = self.outs[TRIO], self.core * HALF + (u - 10) * LANES
        return out.at[:, pl.ds(pl.multiple_of(col, LANES), LANES)]

    def kept(self, u):
        return pltpu.make_async_copy(self.fin.at[u, self.keep], self.out(u), self.swap_sems.at[DUO + u])

    def run(self, u, stage):
        if stage == 0:
            return self.launch(u, 0)
        phase = (stage - 1) // DUO
        if stage == LAST:
            self.arrived(u, DUO, 0, TRIO)
            got = self.buf(u, DUO)
            self.fin[u] = self.view(u, DUO, 0)[...] + (got[0] + got[1] + got[DUO])
            self.copy(self.fin.at[u, self.give], self.out(u), (self.swap_sems.at[0], self.swap_sems.at[1]), self.peer).start()
            self.kept(u).start()
            return
        got = self.buf(u, phase)
        if stage % DUO:
            self.arrived(u, phase, 0, DUO)
            for name, hop in ((0, 1), (1, TRIO)):
                add_into(self.view(u, phase, hop, name), got.at[name])
                self.send(u, phase, name + RING)
            return
        self.arrived(u, phase, DUO, RING)
        if phase == 0 and BEFORE[u] is not None:
            self.drain(BEFORE[u], 1)
            self.drain(BEFORE[u], DUO)
        for half, names in ((0, (TRIO, RING)), (1, (DUO, 5))):
            if phase:
                add_into(self.view(u, phase, 0, half), *[got.at[name] for name in names])
            else:
                dst = self.mid.at[self.slot(u) + (ALL, ALL, HALVES[half], slice(None))]
                add_into(dst, self.view(u, 0, 0, half), *[got.at[name] for name in names], fresh=True)
        self.launch(u, phase + 1)

    def finish(self):
        for u in range(N_UNITS):
            for phase in range(TRIO):
                self.drain(u, phase)
        half = self.fin.at[:, pl.ds(0, SHARE)]
        swaps = self.copy(half, half, (self.swap_sems.at[0], self.swap_sems.at[1]), self.peer)
        swaps.wait_send()
        swaps.wait_recv()
        for u in range(N_UNITS):
            self.kept(u).wait()


def attend(heads, qt, do_t, k, kt, v, vt, cos, sin, o_row, ot, dq, dkt, dvt, s_scr, e_scr, p_scr, d_scr):
    f32, bf16 = jnp.float32, jnp.bfloat16
    strip = TURN
    work = [(h, j) for j in range(NBLK) for h in range(len(heads))]

    def strips(c):
        return [(i * strip, slice(c * QB + i * strip, c * QB + (i + 1) * strip)) for i in range(QB // strip)]

    def fold(x, op):
        return op(x.reshape(strip // SUBS, SUBS, QB), axis=0)

    def scores(i):
        (h, j), b = work[i], i % DUO
        q_t = qt[heads[h], j * QB:(j + 1) * QB]
        top = jnp.full((SUBS, QB), -jnp.inf, f32)
        for c in range(j + 1):
            tile = dot(k[c * QB:(c + 1) * QB, :], q_t)
            for at, rows in strips(c):
                s = tile[at:at + strip]
                if c == j:
                    seen = lax.broadcasted_iota(jnp.int32, (strip, QB), 0) + at <= lax.broadcasted_iota(jnp.int32, (strip, QB), 1)
                    s = jnp.where(seen, s, -jnp.inf)
                s_scr[b, rows, :] = s
                top = jnp.maximum(top, fold(s, jnp.max))
        return jnp.max(top, axis=0, keepdims=True)

    def rest(i, m):
        (h, j), b = work[i], i % DUO
        cols, n = slice(j * QB, (j + 1) * QB), (j + 1) * QB
        q_t, d_t = qt[heads[h], cols], do_t[heads[h], cols]
        tot = jnp.zeros((SUBS, QB), f32)
        for c in range(j + 1):
            for at, rows in strips(c):
                e = jnp.exp2((s_scr[b, rows, :] - m) * (SCALE * LOG2E))
                s_scr[b, rows, :] = e
                e_scr[b, rows, :] = e.astype(bf16)
                tot = tot + fold(e, jnp.sum)
        den = jnp.sum(tot, axis=0, keepdims=True)
        inv = 1.0 / den
        o = (dot(vt[:, :n], e_scr[b, :n, :]) / den).astype(bf16)
        ot[o_row(h), cols] = o
        delta = jnp.sum(d_t.astype(f32) * o.astype(f32), axis=0, keepdims=True)
        for c in range(j + 1):
            dp = dot(v[c * QB:(c + 1) * QB, :], d_t)
            for at, rows in strips(c):
                p = s_scr[b, rows, :] * inv
                p_scr[b, rows, :] = p.astype(bf16)
                d_scr[b, rows, :] = (p * (dp[at:at + strip] - delta)).astype(bf16)
        dvt[:, :n] += dot_nt(d_t, p_scr[b, :n, :])
        dkt[:, :n] += dot_nt(q_t, d_scr[b, :n, :])
        g = dot(kt[:, :n], d_scr[b, :n, :]) * SCALE
        co, si = cos[:, cols], sin[:, cols]
        x, y = g[:TURN], g[TURN:]
        dq[heads[h], cols] = jnp.concatenate([x * co + y * si, y * co - x * si], axis=0).astype(bf16)

    m = scores(0)
    for i in range(len(work)):
        later = scores(i + 1) if i + 1 < len(work) else None
        rest(i, m)
        m = later


def tail_kernel(qt, do_t, k, kt, v, vt, rt, dyc, wqk, wqkp, wvo, wvop, gain, hidden, dy, pos, cos, sin,
                result, grad_x, gq, gk, gv, go, gout,
                two, ks, kts, vs, vts, rts, ots, dqo, dqp, dkvo, dkvp, dkt, dvt, s_scr, e_scr, p_scr, d_scr, dycs, part, mid, buf1, buf2, buf3, fin, own, onat, dnat, xs, gacc, gpart, gpeer, gz, gx,
                send_sems, recv_sems, swap_sems, trade_send, trade_recv, local_sems):
    comm = Singles(trade_send, trade_recv, local_sems)
    comm.used = DUO * HEADS
    f32, bf16 = jnp.float32, jnp.bfloat16
    core, peer = comm.core, comm.peer()
    a1, a2 = two.at[0], two.at[1]
    comm.announce(CORNERS)
    sc = Scatter(comm, part, mid, (buf1, buf2, buf3), fin, (gq, gk, gv, go), send_sems, recv_sems, swap_sems)
    plan = Plan()
    some, most = pl.ds(0, PAIR), pl.ds(PAIR, HALF - PAIR)
    loads = [comm.local(s, d) for s, d in ((qt.at[some], two.at[0, some]), (k, ks), (do_t.at[some], two.at[1, some]), (vt, vts), (v, vs), (kt, kts))]
    dkt[...] = jnp.zeros_like(dkt)
    dvt[...] = jnp.zeros_like(dvt)
    with scope('wait_q'):
        for c in loads:
            c.wait()
    loads = [comm.local(s, d) for s, d in ((rt, rts), (qt.at[most], two.at[0, most]), (do_t.at[most], two.at[1, most]))]
    later = [comm.local(s, d) for s, d in ((dyc, dycs), (hidden, xs))]

    def emit(stages):
        for u, stage in stages:
            with scope(f'u{u}_s{stage}'):
                if u == GAIN:
                    sum_gain(stage)
                else:
                    sc.run(u, stage)

    def after(cost):
        plan.now += cost
        return plan.due()

    def head_trades(h):
        row = tile_at(core * HEADS + h, LANES)
        mine = tile_at(h, LANES)
        return [pltpu.make_async_remote_copy(src_ref=s, dst_ref=d, send_sem=trade_send.at[i], recv_sem=trade_recv.at[i], device_id=peer, device_id_type=MESH)
                for s, d, i in ((ots.at[row], ots.at[row], h), (dqo.at[mine], dqp.at[mine], HEADS + h))]

    def gradient(place, count, left, right, mul):
        with scope('grad'):
            @pl.loop(0, DUO)
            def _(z):
                g = mul(left[tile_at(z, HALF), :], right())
                for i in range(count):
                    part[place + i, tile_at(z, DUO)] = g[:, i * LANES:(i + 1) * LANES].reshape(DUO, RING, RING, CHIP, LANES)

    PAIRS = HEADS // DUO
    attended, paired = [], []
    for g in range(PAIRS):
        attended.append(after(5.2))
        plan.now += 1.6
        plan.start(DUO * g)
        plan.start(DUO * g + 1)
        paired.append(plan.due())

    @pl.loop(0, PAIRS)
    def _(g):
        def at(table):
            for i in range(PAIRS):
                if table[i]:
                    pl.when(g == i)(functools.partial(emit, table[i]))

        heads = [tile_at(DUO * g + i, LANES) for i in range(DUO)]
        with scope('attend'):
            attend(heads, a1, a2, ks, kts, vs, vts, cos, sin, lambda i: tile_at(core * HEADS + DUO * g + i, LANES), ots, dqo, dkt, dvt, s_scr, e_scr, p_scr, d_scr)

        @pl.when(g == 0)
        def _():
            with scope('entry'):
                comm.meet(CORNERS)
                for c in loads:
                    c.wait()
        for i in range(DUO):
            for c in head_trades(DUO * g + i):
                c.start()
        at(attended)
        gradient(DUO * g, DUO, rts, lambda: dqo[tile_at(g, PAIR), :], dot_nt)
        at(paired)

    def beat(cost, *starts):
        plan.now += cost
        for u in starts:
            plan.start(u)
        emit(plan.due())

    wkv, wkvp = e_scr.reshape(DIM, PAIR), p_scr.reshape(DIM, PAIR)
    later += [comm.local(src.at[:, pl.ds(at, LANES)], dst.at[:, pl.ds(to, LANES)]) for srcs, dst in (((wqk, wvo), wkv), ((wqkp, wvop), wkvp)) for src, at, to in ((srcs[0], HALF, 0), (srcs[1], 0, LANES))]
    wqp_loads = [comm.local(wqkp.at[tile_at(i, HALF), pl.ds(0, HALF)], two.at[i]) for i in range(DUO)]
    key = dkt[...] * SCALE
    co, si, x, y = cos[...], sin[...], key[:TURN], key[TURN:]
    dkvo[:LANES, :] = jnp.concatenate([x * co + y * si, y * co - x * si], axis=0).astype(bf16)
    dkvo[LANES:, :] = dvt[...].astype(bf16)
    comm.trade(dkvo, dkvp)
    gradient(UNIT_K, DUO, rts, lambda: dkvo[...], dot_nt)
    beat(2.0, UNIT_K, UNIT_V)
    wq_load = comm.local(wqk.at[:, pl.ds(0, HALF)], rts)
    for c in later:
        c.wait()
    with scope('trades'):
        for h in range(HEADS):
            for c in head_trades(h):
                c.wait()

    waiting = list(range(RING))

    def output_gradients(force=False):
        while waiting:
            first = 10 + DUO * waiting[0]
            before = [u for u in range(N_UNITS) if u < first and PLACE[u] in (PLACE[first], PLACE[first + 1])]
            if force:
                emit(plan.rush(lambda: all(map(plan.vacated, before))))
            if not all(map(plan.vacated, before)):
                return
            for u in before:
                sc.drain(u, 0)
            i = waiting.pop(0)
            gradient(PLACE[first], DUO, ots, lambda: dycs[:, i * PAIR:(i + 1) * PAIR], dot)
            plan.start(first)
            plan.start(first + 1)
            beat(1.5)

    def piece(cost):
        beat(cost)
        output_gradients()

    def ticking(n, cost, body):
        tables = [after(cost) for _ in range(n)]

        @pl.loop(0, n)
        def _(i):
            body(i)
            for j, table in enumerate(tables):
                if table:
                    pl.when(i == j)(functools.partial(emit, table))
        output_gradients()

    @pl.loop(0, TOKENS // LANES)
    def _(i):
        want = lax.broadcasted_iota(jnp.int32, (LANES, ROWS), 0) + i * LANES
        own[tile_at(i, LANES), :] = jnp.where(want == pos[...], 1.0, 0.0).astype(bf16)

    def unsort(at, src_t, n):
        with scope('unsort'):
            dnat[at:at + n, :] = dot(src_t[:n, :], own[...]).astype(bf16)

    output_gradients()
    for c in comm.exchanged:
        c.wait_recv()
    unsort(0, dqo, HALF)
    dy_loads = [comm.local(dy.at[:, tile_at(i, HALF)], dqo.at[tile_at(i, ROWS)]) for i in range(DUO)]
    piece(1.2)
    unsort(HALF, dqp, HALF)
    piece(1.2)
    unsort(DUO * HALF, dkvo, PAIR)
    unsort(DUO * HALF + PAIR, dkvp, PAIR)
    piece(0.7)
    wq_load.wait()
    for c in wqp_loads + dy_loads:
        c.wait()
    gacc[...] = jnp.zeros_like(gacc)

    def dr_parts(half, r):
        return [s_scr.at[half, r(i * PAIR), :] for i in range(RING)]

    def back(block, then):
        def dr(half):
            with scope('dr'):
                c = tile_at(half, HALF)
                left = jnp.concatenate([rts[c, :], two[half], wkv[c, :], wkvp[c, :]], axis=1)
                acc = dot(left, dnat[:, block * PAIR:(block + 1) * PAIR])
                for i, ref in enumerate(dr_parts(half, lambda at: pl.ds(at, PAIR))):
                    ref[...] = acc[i * PAIR:(i + 1) * PAIR, :].T

        def norm(part):
            with scope('back'):
                @pl.loop(0, RING)
                def _(i):
                    j = part * RING + i
                    q = pl.ds(pl.multiple_of(block * PAIR + j * SHARE, SHARE), SHARE)
                    d = jnp.concatenate([ref[...] for half in range(DUO) for ref in dr_parts(half, lambda at: pl.ds(pl.multiple_of(at + j * SHARE, SHARE), SHARE))], axis=1)
                    x = xs[q, :].astype(f32)
                    inv = lax.rsqrt(jnp.mean(x * x, axis=-1, keepdims=True) + RMS_EPS)
                    unit = x * inv
                    gacc[...] += jnp.sum((d * unit).reshape(DUO, SUBS, DIM), axis=0)
                    dg = d * gain[0:1, :]
                    new = inv * (dg - unit * jnp.mean(dg * unit, axis=-1, keepdims=True))
                    for half in range(DUO):
                        r = pl.ds(pl.multiple_of(half * ROWS + block * PAIR + j * SHARE, SHARE), SHARE)
                        dqo[r, :] = (dqo[r, :].astype(f32) + new[:, half * HALF:(half + 1) * HALF]).astype(bf16)

        ticking(DUO, 1.7, dr)
        then()
        ticking(RING, 0.92, norm)

    back(0, lambda: None)
    wo_loads = []
    back(1, lambda: wo_loads.extend([comm.local(wvo.at[:, pl.ds(LANES, HALF)], rts)] + [comm.local(wvop.at[tile_at(i, HALF), pl.ds(LANES, HALF)], two.at[i]) for i in range(DUO)]))
    for i in range(DUO):
        comm.store(dqo.at[tile_at(i, ROWS)], grad_x.at[:, tile_at(i, HALF)])
    total = jnp.sum(gacc[...], axis=0, keepdims=True)
    gpart[...] = jnp.zeros_like(gpart)
    for i in range(RING):
        for j in range(RING):
            gpart[i, j:j + 1, :] = total[:, (i * RING + j) * LANES:(i * RING + j + 1) * LANES]

    arrivals = []

    def sum_gain(stage):
        for c in arrivals:
            c.wait_recv()
        del arrivals[:]
        if stage == 0:
            arrivals.append(comm.send(gpart, gpeer, peer))
        elif stage == 1:
            for j in range(RING):
                gz[j] = gpart[j] + gpeer[j]
            arrivals.extend(comm.send(gz.at[step(comm.pos, 'z', hop)], gz.at[TRIO + hop], comm.far('z', hop)) for hop in (1, DUO, TRIO))
        elif stage == DUO:
            gx[0, 0] = (gz[comm.pos['z']] + gz[RING]) + (gz[5] + gz[6])
            for dy, dx in PLANE:
                arrivals.append(comm.send(gx.at[0, 0], gx.at[dy, dx], comm.aside(dy, dx)))
        else:
            gpeer[0] = sum(gx[dy, dx] for dy, dx in PLANE) + gx[0, 0]
            mine = jnp.broadcast_to(gpeer[0, pl.ds(comm.pos['y'], 1), :], (SUBS, LANES))
            gout[...] = pltpu.roll(mine, LANES - (comm.pos['x'] * CHIP + core * SHARE), 1)

    plan.start(GAIN)
    beat(0.2)
    for i in range(DUO):
        with scope('unsort_o'):
            @pl.loop(0, DUO)
            def _(j):
                r = pl.ds(pl.multiple_of(i * HALF + j * ROWS, ROWS), ROWS)
                onat[:, r] = dot(ots[r, :], own[...]).astype(bf16).T
        piece(1.4)
    output_gradients(True)

    def project_out(col, weights, i):
        with scope('project'):
            @pl.loop(DUO * i, DUO * i + DUO)
            def _(j):
                c = tile_at(j, PAIR)
                dst = pl.ds(pl.multiple_of(col + j * PAIR, PAIR), PAIR)
                xs[:, dst] = (xs[:, dst].astype(f32) + dot(onat[...], weights(c))).astype(bf16)
        beat(1.55)

    def own_half(c):
        return rts[:, c]

    def other_half(c):
        return jnp.concatenate([a1[:, c], a2[:, c]], axis=0)

    for c in wo_loads:
        c.wait()
    for col, weights in ((core * HALF, own_half), ((1 - core) * HALF, other_half)):
        for i in range(DUO):
            project_out(col, weights, i)
    comm.store(xs, result)
    emit(plan.rush(lambda: not plan.stage))
    with scope('finish'):
        sc.finish()
        for c in comm.sent + comm.exchanged:
            c.wait_send()
        for c in comm.stored:
            c.wait()


def tail(qt, do_t, k, kt, v, vt, rt, dyc, wqk, wqkp, wvo, wvop, gain, hidden, dy, pos, cos, sin):
    bf16, f32 = jnp.bfloat16, jnp.float32
    any_ = pl.BlockSpec(memory_space=pl.ANY)
    vmem = pl.BlockSpec(memory_space=pltpu.VMEM)
    S = lambda shape, d=bf16: jax.ShapeDtypeStruct(shape, d)
    V = lambda shape, d=bf16: pltpu.VMEM(shape, d)
    D = lambda n: pltpu.SemaphoreType.DMA((n,))
    sq, tall, wide = (HALF, TOKENS), (TOKENS, LANES), (LANES, TOKENS)
    mine, kv = (ROWS, DIM), (PAIR, TOKENS)
    return pl.pallas_call(
        tail_kernel,
        out_shape=[S(mine), S(mine), S((SHARE, DIM), f32), S((SHARE, PAIR), f32), S((SHARE, PAIR), f32), S((SHARE, DIM), f32), S((SUBS, LANES), f32)],
        in_specs=[any_] * 12 + [vmem] + [any_] * DUO + [vmem] * TRIO,
        out_specs=[any_] * 6 + [vmem],
        scratch_shapes=[V((DUO,) + sq), V(tall), V(wide), V(tall), V(wide), V((DIM, TOKENS)), V((DIM, TOKENS)), V(sq), V(sq), V(kv), V(kv), V(wide, f32), V(wide, f32),
                        V((DUO, TOKENS, QB), f32), V((DUO, TOKENS, QB)), V((DUO, TOKENS, QB)), V((DUO, TOKENS, QB)), V(sq), V((PLACES, RING, RING, RING, CHIP, LANES), f32), V((TRIO, SLOTS, RING, RING, CHIP, LANES), f32),
                        V((TRIO, SLOTS, 6, RING, RING, SHARE, LANES), f32), V((TRIO, SLOTS, 6, RING, SHARE, LANES), f32), V((TRIO, SLOTS, TRIO, CHIP, LANES), f32), V((N_UNITS, CHIP, LANES), f32), V((TOKENS, ROWS)), V(mine), V((DUO * QKV, ROWS)), V(mine),
                        V((SUBS, DIM), f32), V((RING, SUBS, LANES), f32), V((RING, SUBS, LANES), f32), V((7, SUBS, LANES), f32), V((RING, RING, SUBS, LANES), f32),
                        D(TRIO * N_UNITS), D(6 * N_UNITS), D(DUO + N_UNITS), D(DUO * HEADS + 20), D(DUO * HEADS + 20), D(CHIP)],
        compiler_params=pltpu.CompilerParams(collective_id=1, has_side_effects=True, vmem_limit_bytes=67043328),
        name='tail',
    )(qt, do_t, k, kt, v, vt, rt, dyc, wqk, wqkp, wvo, wvop, gain, hidden, dy, pos, cos, sin)


def settle_kernel(n, *refs):
    ins, gain, outs, gain_out, bufs, sems = refs[:n], refs[n], refs[n + 1:DUO * n + 1], refs[DUO * n + 1], refs[DUO * n + DUO:-1], refs[-1]
    jobs = []
    for a, o, b in zip(ins, outs, bufs):
        size = a.shape[0] // RING if a.shape[0] == ROWS else a.shape[0]
        jobs += [tuple(r.at[pl.ds(i, size)] for r in (a, b, o)) for i in range(0, a.shape[0], size)]
    takes = [pltpu.make_async_copy(a, b, sems.at[0, i]) for i, (a, b, _) in enumerate(jobs)]
    puts = [pltpu.make_async_copy(b, o, sems.at[1, i]) for i, (_, b, o) in enumerate(jobs)]
    for c in takes:
        c.start()
    gain_out[...] = gain[0:1, :SHARE]
    for take, put in zip(takes, puts):
        take.wait()
        put.start()
    for c in puts:
        c.wait()


def settle(*arrays):
    *large, gain = arrays
    any_, vmem = pl.BlockSpec(memory_space=pl.ANY), pl.BlockSpec(memory_space=pltpu.VMEM)
    return pl.pallas_call(
        functools.partial(settle_kernel, len(large)),
        out_shape=[jax.ShapeDtypeStruct(a.shape, a.dtype) for a in large] + [jax.ShapeDtypeStruct((1, SHARE), gain.dtype)],
        in_specs=[any_] * len(large) + [vmem],
        out_specs=[any_] * len(large) + [vmem],
        scratch_shapes=[pltpu.VMEM(a.shape, a.dtype) for a in large] + [pltpu.SemaphoreType.DMA((DUO, 12))],
        name='settle',
    )(*arrays)


def rope_tables():
    j = np.arange(HEAD_DIM // DUO, dtype=np.float64) / (HEAD_DIM // DUO)
    freq = (ROPE_THETA ** -j).astype(np.float32)
    angle = freq[:, None] * np.arange(TOKENS, dtype=np.float32)[None, :]
    return np.cos(angle.astype(np.float64)).astype(np.float32), np.sin(angle.astype(np.float64)).astype(np.float32)


def solution(mesh):
    def shard_fn(hidden, tok_pos, grad_out, norm_gain, w_query, w_key, w_value, w_out):
        hidden, grad_out = hidden[0], grad_out[0]
        cos_t, sin_t = (jnp.asarray(t) for t in rope_tables())
        *parts, gain = head(hidden, grad_out, w_query, w_key, w_value, w_out, tok_pos, norm_gain.reshape(1, SHARE), cos_t, sin_t)
        parts = [p.reshape(DIM, GROUP) if p.ndim > DUO else p for p in parts]
        result, grad_hidden, gq, gk, gv, go, gout = settle(*tail(*parts, gain, hidden, grad_out, tok_pos, cos_t, sin_t))
        return result[None], grad_hidden[None], gq, gk, gv, go, gout.reshape(SHARE)

    row_spec, pos_spec = P('fsdp', 'cp', None), P('fsdp', 'cp')
    weight_spec, gain_spec = P(('fsdp', 'cp'), None), P(('fsdp', 'cp'))
    return jax.shard_map(shard_fn, mesh=mesh, in_specs=(row_spec, pos_spec, row_spec, gain_spec, weight_spec, weight_spec, weight_spec, weight_spec), out_specs=(row_spec, row_spec, weight_spec, weight_spec, weight_spec, weight_spec, gain_spec), check_vma=False)
```

```python
import functools
import jax
import jax.numpy as jnp
import numpy as np
from jax import lax
from jax.experimental import pallas as pl
from jax.experimental.pallas import tpu as pltpu
from jax.sharding import PartitionSpec as P

LANES, SUBS, RING, TRIO, DUO = 128, 8, 4, 3, 2
PAIR, ROWS, CHIP, SHARE, TURN = 256, 512, 32, 16, 64
HEAD_DIM = LANES
ROPE_THETA = 1000000.0
RMS_EPS = 1e-5
SCALE = HEAD_DIM ** -0.5
LOG2E = 1.4426950408889634

MESH = pl.DeviceIdType.MESH
AXES = ('x', 'y', 'z')
ORDERS = (('x', 'y', 'z'), ('y', 'z', 'x'), ('z', 'x', 'y'))
ALL = pl.ds(0, RING)


def torus():
    f = lax.axis_index('fsdp')
    return {'x': lax.rem(f, RING), 'y': lax.rem(lax.div(f, RING), RING), 'z': lax.div(f, SHARE)}


def step(pos, axis, hop):
    return lax.rem(pos[axis] + hop, RING)


class Batch:
    def __init__(self, comm):
        self.comm, self.index = comm, comm.used
        comm.used += 1

    def _copy(self, src, dst, device):
        send, recv, _ = self.comm.sems
        return pltpu.make_async_remote_copy(src_ref=src, dst_ref=dst, send_sem=send.at[self.index], recv_sem=recv.at[self.index], device_id=device, device_id_type=MESH)

    def send(self, src, dst, device):
        self._copy(src, dst, device).start()
        return self

    def arrived(self, whole):
        self._copy(whole, whole, self.comm.peer()).wait_recv()

    def sent(self, whole):
        self._copy(whole, whole, self.comm.peer()).wait_send()


class Comm:
    def __init__(self, send_sems, recv_sems, local_sems):
        self.pos = torus()
        self.core = lax.axis_index('cp')
        self.sems = (send_sems, recv_sems, local_sems)
        self.used = self.used_local = 0
        self.stored = []

    def far(self, axis, hop):
        p = dict(self.pos)
        p[axis] = step(self.pos, axis, hop)
        return {'fsdp': (p['z'] * RING + p['y']) * RING + p['x'], 'cp': self.core}

    def peer(self):
        return {'fsdp': lax.axis_index('fsdp'), 'cp': 1 - self.core}

    def aside(self, dy, dx):
        return {'fsdp': (self.pos['z'] * RING + step(self.pos, 'y', dy)) * RING + step(self.pos, 'x', dx), 'cp': self.core}

    def announce(self, corners=()):
        sem = pltpu.get_barrier_semaphore()
        for axis in AXES:
            for hop in (1, DUO, TRIO):
                pl.semaphore_signal(sem, inc=1, device_id=self.far(axis, hop), device_id_type=MESH)
        for dy, dx in corners:
            pl.semaphore_signal(sem, inc=1, device_id=self.aside(dy, dx), device_id_type=MESH)
        pl.semaphore_signal(sem, inc=1, device_id=self.peer(), device_id_type=MESH)

    def meet(self, corners=()):
        pl.semaphore_wait(pltpu.get_barrier_semaphore(), 10 + len(corners))

    def ring(self, batch, src, slots, axis):
        for hop in (1, DUO, TRIO):
            batch.send(src, slots.at[hop], self.far(axis, hop))

    def local(self, src, dst):
        i = self.used_local
        self.used_local += 1
        c = pltpu.make_async_copy(src, dst, self.sems[DUO].at[i])
        c.start()
        return c

    def store(self, src, dst):
        self.stored.append(self.local(src, dst))


class Singles(Comm):
    def __init__(self, *sems):
        super().__init__(*sems)
        self.sent, self.exchanged = [], []

    def _copy(self, src, dst, device):
        i = self.used
        self.used += 1
        c = pltpu.make_async_remote_copy(src_ref=src, dst_ref=dst, send_sem=self.sems[0].at[i], recv_sem=self.sems[1].at[i], device_id=device, device_id_type=MESH)
        c.start()
        return c

    def send(self, src, dst, device):
        c = self._copy(src, dst, device)
        self.sent.append(c)
        return c

    def trade(self, src, dst):
        self.exchanged.append(self._copy(src, dst, self.peer()))


def pick(ref, sel, piece):
    lo, cols, first, rows = piece
    return ref.at[sel['z'], sel['y'], sel['x'], pl.ds(first, rows), pl.ds(lo, cols)]


def sem_scratch(remote, local):
    return [pltpu.SemaphoreType.DMA((remote,)), pltpu.SemaphoreType.DMA((remote,)), pltpu.SemaphoreType.DMA((local,))]


def add_into(dst, *srcs, fresh=False):
    def add(idx):
        total, *rest = [s[idx] for s in (srcs if fresh else (dst,) + srcs)]
        for more in rest:
            total = total + more
        dst[idx] = total

    if len(dst.shape) > TRIO:
        @pl.loop(0, dst.shape[0])
        def _(i):
            add((i,))
    else:
        add(Ellipsis)


def columns(lo, na, nb):
    return (lo, na, 0, CHIP), (lo + na, nb, 0, CHIP)


def strip(lo):
    return (lo, LANES, 0, SHARE), (lo, LANES, SHARE, SHARE)


QK_COLORS = (columns(0, PAIR, LANES), columns(384, LANES, PAIR), columns(768, PAIR, LANES))
VO_COLORS = (columns(0, LANES, PAIR), columns(384, PAIR, LANES), columns(768, LANES, PAIR))
VO_FIRST = (columns(0, LANES, LANES), columns(384, LANES, LANES), columns(768, LANES, LANES))
VO_LAST = (strip(PAIR), strip(640), strip(1024))
TOKENS = 1024
DIM = 2048
HALF = 1024
QKV = 1280
GROUP = 1152


def scope(name):
    return jax.named_scope(name)


def dot(a, b):
    return jnp.dot(a, b, preferred_element_type=jnp.float32)


def dot_nt(a, b):
    return lax.dot_general(a, b, (((1,), (1,)), ((), ())), preferred_element_type=jnp.float32)


def tile_at(i, n):
    return pl.ds(pl.multiple_of(i * n, n), n)


class Gather:
    def __init__(self, comm, ref, colors, land, held=None):
        self.comm, self.ref, self.colors, self.land = comm, ref, colors, land
        self.held = list(held or [dict(comm.pos) for _ in colors])
        self.batches = []

    def move(self, batch, s, piece, to):
        batch.send(pick(self.ref, s, piece), pick(self.ref, s, piece), to)

    def at(self, k, hop):
        d = ORDERS[k][self.phase]
        return dict(self.held[k], **{d: step(self.comm.pos, d, hop)})

    def begin(self, phase):
        self.phase = phase
        self.up, self.dn, self.rest = ([Batch(self.comm) for _ in range(TRIO)] for _ in range(TRIO))
        self.batches += self.up + self.dn + self.rest
        for k, (a, b) in enumerate(self.colors):
            d = ORDERS[k][phase]
            up, dn, s = self.comm.far(d, 1), self.comm.far(d, TRIO), self.held[k]
            self.move(self.up[k], s, a, up)
            self.move(self.dn[k], s, b, dn)
            self.move(self.rest[k], s, b, up)
            self.move(self.rest[k], s, a, dn)
            if phase == 0:
                for piece in (a, b):
                    self.move(self.rest[k], s, piece, self.comm.far(d, DUO))
        if phase == DUO:
            for k, pieces in enumerate(self.colors):
                for piece in pieces:
                    self.land(self.ref, self.held[k], piece)

    def forward(self):
        for k, (a, b) in enumerate(self.colors):
            d = ORDERS[k][self.phase]
            for batch, hop, piece, to in ((self.up[k], TRIO, a, 1), (self.dn[k], 1, b, TRIO)):
                s = self.at(k, hop)
                batch.arrived(pick(self.ref, s, piece))
                if self.phase:
                    self.move(self.rest[k], s, piece, self.comm.far(d, to))
                if self.phase == DUO:
                    self.land(self.ref, s, piece)

    def end(self):
        for k, (a, b) in enumerate(self.colors):
            d = ORDERS[k][self.phase]
            two = dict(self.held[k], **{d: pl.ds(0, DUO)})
            both = (a[0], max(a[0] + a[1], b[0] + b[1]) - a[0], 0, CHIP)
            self.rest[k].arrived(pick(self.ref, two, both))
            if self.phase == DUO:
                for hop, piece in ((TRIO, b), (1, a), (DUO, a), (DUO, b)):
                    self.land(self.ref, self.at(k, hop), piece)
            for batch, s, piece in ((self.up[k], self.held[k], a), (self.dn[k], self.held[k], b), (self.rest[k], two, both)):
                batch.spent = pick(self.ref, s, piece)
            self.held[k] = dict(self.held[k], **{d: ALL})

    def finish(self):
        for batch in self.batches:
            batch.sent(batch.spent)


def head_kernel(hidden, dy, wq, wk, wv, wo, pos, gain_in, cos_t, sin_t,
                qt_o, dot_o, k_o, kt_o, v_o, vt_o, rt_o, dyc_o, wqk_o, wqkp_o, wvo_o, wvop_o, gain_o,
                hid2, dy2, dys, rs, rt, wqk, wvo, wpeer, pi, pos2, qt, dot_s, kk, kt, vv, vt, part, gain, gtile, gbuf, gx, gy, gz, *sems):
    comm = Comm(*sems)
    pos_c, core = comm.pos, comm.core
    bf16, f32 = jnp.bfloat16, jnp.float32
    peer = comm.peer()
    rows = tile_at(core, SHARE)
    mine_qk = wqk.at[pos_c['z'], pos_c['y'], pos_c['x'], rows]
    mine_vo = wvo.at[pos_c['z'], pos_c['y'], pos_c['x'], rows]

    def weight_parts(c):
        return ((wq.at[:, tile_at(c, HALF)], mine_qk.at[:, pl.ds(0, HALF)]), (wk.at[:, tile_at(c, LANES)], mine_qk.at[:, pl.ds(HALF, LANES)]),
                (wv.at[:, tile_at(c, LANES)], mine_vo.at[:, pl.ds(0, LANES)]), (wo.at[:, tile_at(c, HALF)], mine_vo.at[:, pl.ds(LANES, HALF)]))

    loads = [comm.local(s, d) for s, d in weight_parts(core)]
    load_x = [comm.local(hidden, hid2.at[pl.ds(0, ROWS)]), comm.local(dy, dy2.at[pl.ds(0, ROWS)])]
    share = lax.broadcasted_iota(jnp.int32, (SUBS, LANES), 1) // SHARE
    gtile[...] = jnp.where(share == pos_c['x'] * DUO + core, jnp.broadcast_to(jnp.concatenate([gain_in[...]] * SUBS, axis=1), (SUBS, LANES)), 0.0)
    comm.announce()
    with scope('entry'):
        comm.meet()
    swap_w, swap_pos, swap_dy, swap_x, peers_qk, peers_vo, peers_o = (Batch(comm) for _ in range(7))
    gain_c, gain_x, gain_y, gain_z = (Batch(comm) for _ in range(RING))
    for s, d in weight_parts(1 - core):
        swap_w.send(s, d, peer)
    gain_c.send(gtile, gbuf, peer)
    swap_pos.send(pos, pos2, peer)
    for c in loads:
        c.wait()
    with scope('wait_w'):
        swapped = wqk.at[pos_c['z'], pos_c['y'], pos_c['x']]
        swap_w.arrived(swapped)

    def land_qk(ref, s, cols):
        peers_qk.send(pick(ref, s, cols), pick(wqkp_o, s, cols), peer)

    def land_vo(ref, s, cols):
        (peers_vo if cols[0] % 384 < PAIR else peers_o).send(pick(ref, s, cols), pick(wpeer, s, cols), peer)

    g1 = Gather(comm, wqk, QK_COLORS, land_qk)
    g2 = Gather(comm, wvo, VO_COLORS, land_vo)
    g1.begin(0)
    g2.begin(0)
    swap_dy.send(dy, dy2.at[pl.ds(ROWS, ROWS)], peer)
    gain_c.arrived(gbuf)
    gx[0] = gtile[...] + gbuf[...]
    comm.ring(gain_x, gx.at[0], gx, 'x')

    swap_pos.arrived(pos2)

    @pl.loop(0, TOKENS // LANES)
    def _(i):
        want = lax.broadcasted_iota(jnp.int32, (LANES, ROWS), 0) + i * LANES
        for h, have in enumerate((pos, pos2)):
            pi[tile_at(i, LANES), h * ROWS:(h + 1) * ROWS] = jnp.where(want == have[...], 1.0, 0.0).astype(bf16)

    def sort(dst, src, first, last):
        with scope('sort'):
            @pl.loop(first, last)
            def _(j):
                c = tile_at(j, PAIR)
                dst[:, c] = dot(pi[...], src[:, c]).astype(bf16)

    with scope('p0_end'):
        for g in (g1, g2):
            g.forward()
            g.end()
            g.begin(1)
    swap_x.send(hidden, hid2.at[pl.ds(ROWS, ROWS)], peer)
    gain_x.arrived(gx.at[pl.ds(1, TRIO)])
    gy[pos_c['y']] = (gx[0] + gx[1]) + (gx[DUO] + gx[TRIO])
    for hop in (1, DUO, TRIO):
        gain_y.send(gy.at[pos_c['y']], gy.at[pos_c['y']], comm.far('y', hop))
    with scope('wait_dy'):
        load_x[1].wait()
        swap_dy.arrived(dy2.at[pl.ds(ROWS, ROWS)])
    sort(dys, dy2, 0, RING)
    with scope('p1q_fwd'):
        g1.forward()
    sort(dys, dy2, RING, 6)
    with scope('p1o_fwd'):
        g2.forward()
    sort(dys, dy2, 6, SUBS)
    with scope('p1q_end'):
        g1.end()
    gain_y.arrived(gy.at[pl.ds(1, TRIO)])
    for j in range(RING):
        gz[pos_c['z'], j] = gy[j]
    for hop in (1, DUO, TRIO):
        gain_z.send(gz.at[pos_c['z']], gz.at[pos_c['z']], comm.far('z', hop))
    g1.begin(DUO)
    comm.store(dys.at[:, tile_at(core, HALF)], dyc_o)
    with scope('p1o_end'):
        g2.end()
    with scope('wait_x'):
        load_x[0].wait()
        swap_x.arrived(hid2.at[pl.ds(ROWS, ROWS)])
    sort(rs, hid2, 0, SUBS)
    with scope('p2q_fwd'):
        g1.forward()
    g2a, g2b = (Gather(comm, wvo, colors, land_vo, g2.held) for colors in (VO_FIRST, VO_LAST))
    g2a.begin(DUO)
    with scope('gain'):
        gain_z.arrived(gz.at[pl.ds(1, TRIO)])
    for i in range(RING):
        for j in range(RING):
            gain[:, (i * RING + j) * LANES:(i * RING + j + 1) * LANES] = gz[i, j]
    comm.store(gain, gain_o)

    def norm(first, last):
        with scope('norm'):
            @pl.loop(first, last)
            def _(i):
                r = tile_at(i, CHIP)
                x = rs[r, :].astype(f32)
                inv = lax.rsqrt(jnp.mean(x * x, axis=-1, keepdims=True) + RMS_EPS)
                rs[r, :] = (x * inv * gain[0:1, :]).astype(bf16)

    norm(0, TOKENS // CHIP)
    with scope('r_t'):
        @pl.loop(0, DIM // PAIR)
        def _(i):
            c = tile_at(i, PAIR)

            @pl.loop(0, TOKENS // PAIR)
            def _(j):
                r = tile_at(j, PAIR)
                rt[c, r] = rs[r, c].T
    comm.store(rt, rt_o)
    with scope('p2q_end'):
        g1.end()
    comm.store(wqk, wqk_o)
    w_qk, w_vo, w_peer = wqk.reshape(DIM, GROUP), wvo.reshape(DIM, GROUP), wpeer.reshape(DIM, GROUP)

    def rotated(x, r):
        cos, sin = cos_t[:, r], sin_t[:, r]
        cos = jnp.concatenate([cos, cos], axis=0).T
        sin = jnp.concatenate([-sin, sin], axis=0).T
        return (x * cos + pltpu.roll(x, TURN, 1) * sin).astype(bf16)

    def queries(first, last):
        with scope('q'):
            @pl.loop(first, last)
            def _(t):
                x = dot(rs[...], w_qk[:, tile_at(t, PAIR)])
                for i in range(RING):
                    r = slice(i * PAIR, (i + 1) * PAIR)
                    for h in range(DUO):
                        qt[tile_at(DUO * t + h, LANES), r] = rotated(x[r, h * LANES:(h + 1) * LANES], r).T

    queries(0, DUO)
    with scope('p2o_fwd'):
        g2a.forward()
    g2b.begin(DUO)
    queries(DUO, RING)

    @pl.loop(0, DUO)
    def _(i):
        r = tile_at(i, ROWS)
        key = rotated(dot(rs[r, :], w_qk[:, HALF:]), r)
        kk[r, :] = key
        kt[:, r] = key.T
    for src, dst in ((kk, k_o), (kt, kt_o), (qt, qt_o)):
        comm.store(src, dst)
    with scope('p2o_end'):
        g2a.end()
    with scope('vals'):
        @pl.loop(0, DUO)
        def _(i):
            r = tile_at(i, ROWS)
            val = dot(rs[r, :], w_vo[:, :LANES]).astype(bf16)
            vv[r, :] = val
            vt[:, r] = val.T
    for src, dst in ((vv, v_o), (vt, vt_o)):
        comm.store(src, dst)
    with scope('last_fwd'):
        g2b.forward()
    with scope('wo_peer'):
        peers_vo.arrived(wvo.at[:, :, :, :, pl.ds(0, 768)])

    mine = tile_at(core, HALF)

    def do_part(j, cols):
        t = tile_at(j, PAIR)
        left = jnp.concatenate([w[mine, LANES + lo:LANES + lo + n] for w in (w_vo, w_peer) for lo, n in cols], axis=1)
        right = jnp.concatenate([dys[t, pl.ds(pl.multiple_of(half * HALF + lo, LANES), n)] for half in (core, 1 - core) for lo, n in cols], axis=1)
        return dot_nt(left, right)

    with scope('do_t1'):
        @pl.loop(0, TOKENS // PAIR)
        def _(j):
            part[:, tile_at(j, PAIR)] = do_part(j, ((0, LANES), (PAIR, PAIR), (640, PAIR)))
    with scope('last_end'):
        g2b.end()
    with scope('last_peer'):
        peers_o.arrived(wvo.at[:, :, :, :, pl.ds(0, 384)])
    comm.store(wvo, wvo_o)
    comm.store(wpeer, wvop_o)
    with scope('do_t2'):
        @pl.loop(0, TOKENS // PAIR)
        def _(j):
            t = tile_at(j, PAIR)
            dot_s[:, t] = (part[:, t] + do_part(j, ((LANES, LANES), (ROWS, LANES), (896, LANES)))).astype(bf16)
    comm.store(dot_s, dot_o)
    with scope('finish'):
        peers_qk.arrived(wqk)
        for batch, whole in ((swap_w, swapped), (swap_pos, pos2), (swap_dy, dy2.at[pl.ds(ROWS, ROWS)]), (swap_x, hid2.at[pl.ds(ROWS, ROWS)]), (peers_qk, wqk), (peers_vo, wvo.at[:, :, :, :, pl.ds(0, 768)]), (peers_o, wvo.at[:, :, :, :, pl.ds(0, 384)]),
                             (gain_c, gbuf), (gain_x, gx.at[pl.ds(1, TRIO)]), (gain_y, gy.at[pl.ds(1, TRIO)]), (gain_z, gz.at[pl.ds(1, TRIO)])):
            batch.sent(whole)
        for g in (g1, g2, g2a, g2b):
            g.finish()
        for c in comm.stored:
            c.wait()


def head(hidden, dy, wq, wk, wv, wo, pos, gain, cos_t, sin_t):
    bf16, f32 = jnp.bfloat16, jnp.float32
    any_ = pl.BlockSpec(memory_space=pl.ANY)
    vmem = pl.BlockSpec(memory_space=pltpu.VMEM)
    S = lambda shape, d=bf16: jax.ShapeDtypeStruct(shape, d)
    V = lambda shape, d=bf16: pltpu.VMEM(shape, d)
    group = (RING, RING, RING, CHIP, GROUP)
    sq, tall, wide = (HALF, TOKENS), (TOKENS, LANES), (LANES, TOKENS)
    full = (TOKENS, DIM)
    return pl.pallas_call(
        head_kernel,
        out_shape=[S(sq), S(sq), S(tall), S(wide), S(tall), S(wide), S((DIM, TOKENS)), S((TOKENS, HALF)), S(group), S(group), S(group), S(group), S((SUBS, DIM), f32)],
        in_specs=[any_] * 6 + [vmem] * RING,
        out_specs=[any_] * 13,
        scratch_shapes=[V(full), V(full), V(full), V(full), V((DIM, TOKENS)), V(group), V(group), V(group), V((TOKENS, TOKENS)), V((1, ROWS), jnp.int32),
                        V(sq), V(sq), V(tall), V(wide), V(tall), V(wide), V(sq, f32), V((SUBS, DIM), f32), V((SUBS, LANES), f32), V((SUBS, LANES), f32), V((RING, SUBS, LANES), f32), V((RING, SUBS, LANES), f32), V((RING, RING, SUBS, LANES), f32)] + sem_scratch(74, 18),
        compiler_params=pltpu.CompilerParams(collective_id=0, has_side_effects=True, vmem_limit_bytes=60 * DUO**20),
        name='head',
    )(hidden, dy, wq, wk, wv, wo, pos, gain, cos_t, sin_t)


HEADS = SUBS
UNIT_K, UNIT_V = SUBS, 9
N_UNITS = 18
GAIN = N_UNITS
SLOTS = RING
LAST = 5
ABREAST = DUO
LINES = ((0, TRIO, 6, 9, 12, 15), (1, RING, 7, 10, 13, SHARE), (DUO, 5, SUBS, 11, 14, 17))
COLOR = {u: k for k, line in enumerate(LINES) for u in line}
RANK = {u: i for line in LINES for i, u in enumerate(line)}
SWAPPED = ()
ORDER = {u: ORDERS[k] if u not in SWAPPED else (ORDERS[k][0], ORDERS[k][DUO], ORDERS[k][1]) for u, k in COLOR.items()}
BEFORE = {u: line[i - SLOTS] if i >= SLOTS else None for line in LINES for i, u in enumerate(line)}
PLACES = 12
PLACE = {u: u % PLACES for u in range(N_UNITS)}
WIRE = (2.82, 0.71, 0.36)
LATENCY = 2.2
STAGE_COST = 0.08


class Plan:
    def __init__(self):
        self.now, self.stage, self.ready, self.order, self.link = 0.0, {}, {}, [], {}
        self.mark = {}

    def _wire(self, u, phase, count):
        link = ORDER[u][phase]
        t = max(self.link.get(link, 0.0), self.now)
        first = t + WIRE[phase] + LATENCY
        self.link[link] = t + WIRE[phase] * count
        return first if phase < DUO else self.link[link] + LATENCY

    def free(self, u, phase):
        if BEFORE[u] is None:
            return True
        done = self.mark.get((BEFORE[u], (DUO, RING, 5)[phase]))
        if done is None:
            return False
        sent = ((0, 1), (DUO, TRIO), (RING,))[phase]
        return any(self.mark.get((j, s), -1) > done and (j, s + 1) in self.mark for j, order in ORDER.items() if order[phase] == ORDER[u][phase] for s in sent)

    def run(self, u):
        stage = self.stage[u]
        self.order.append((u, stage))
        self.mark[u, stage] = len(self.order)
        self.now = max(self.now, self.ready[u]) + STAGE_COST
        self.stage[u] = stage + 1
        if stage == (TRIO if u == GAIN else LAST):
            del self.stage[u]
        elif u == GAIN:
            self.ready[u] = max([self.now] + [self.link.get(a, 0.0) for a in ('', 'z', 'xy')[stage]]) + DUO * LATENCY
        elif stage % DUO:
            self.ready[u] = self._wire(u, stage // DUO, 1)
        else:
            self.ready[u] = self._wire(u, stage // DUO, DUO)

    def blocked(self, u):
        stage = self.stage[u]
        if u == GAIN:
            return False
        if stage == 0 and sum(0 < self.stage.get(j, 0) <= DUO for j in LINES[COLOR[u]]) >= ABREAST:
            return True
        if stage == DUO and BEFORE[u] is not None and (BEFORE[u], LAST) not in self.mark:
            return True
        return stage in (0, DUO, RING) and not self.free(u, stage // DUO)

    def start(self, u):
        self.stage[u], self.ready[u] = 0, self.now

    def due(self):
        first = len(self.order)
        while True:
            ripe = [(self.ready[u], u) for u in self.stage if self.ready[u] <= self.now and not self.blocked(u)]
            if not ripe:
                return self.order[first:]
            self.run(min(ripe)[1])

    def vacated(self, u):
        return (u, DUO) in self.mark

    def rush(self, done):
        first = len(self.order)
        while not done():
            self.run(min((self.ready[u], u) for u in self.stage if not self.blocked(u))[1])
        return self.order[first:]


QB = PAIR
NBLK = TOKENS // QB
HALVES = (pl.ds(0, SHARE), pl.ds(SHARE, SHARE))
PLANE = tuple((dy, dx) for dy in range(RING) for dx in range(RING) if dy or dx)
CORNERS = tuple((dy, dx) for dy, dx in PLANE if dy and dx)


class Scatter:
    def __init__(self, comm, part, mid, bufs, fin, outs, send_sems, recv_sems, swap_sems):
        self.pos, self.part, self.mid, self.bufs, self.fin, self.outs = comm.pos, part, mid, bufs, fin, outs
        self.send_sems, self.recv_sems, self.swap_sems = send_sems, recv_sems, swap_sems
        self.near = {(a, hop): comm.far(a, hop) for a in AXES for hop in (1, DUO, TRIO)}
        self.hops = {(a, hop): step(comm.pos, a, hop) for a in AXES for hop in (1, DUO, TRIO)}
        self.peer, self.core = comm.peer(), comm.core
        self.keep, self.give = tile_at(comm.core, SHARE), tile_at(1 - comm.core, SHARE)
        self.drained = set()

    def slot(self, u):
        return COLOR[u], RANK[u] % SLOTS

    def buf(self, u, phase):
        return self.bufs[phase].at[self.slot(u)]

    def view(self, u, phase, hop, half=None):
        order = ORDER[u]
        at = {a: ALL for a in AXES}
        for a in order[1:phase]:
            at[a] = self.pos[a]
        at[order[phase]] = self.hops[order[phase], hop] if hop else self.pos[order[phase]]
        rows = pl.ds(0, CHIP) if half is None else HALVES[half]
        if phase == 0:
            return self.part.at[PLACE[u], at['z'], at['y'], at['x'], rows, :]
        return self.mid.at[self.slot(u) + tuple(at[a] for a in 'zyx' if a != order[0]) + (rows, slice(None))]

    def copy(self, src, dst, sems, device):
        return pltpu.make_async_remote_copy(src_ref=src, dst_ref=dst, send_sem=sems[0], recv_sem=sems[1], device_id=device, device_id_type=MESH)

    def sems(self, u, phase, kind=0):
        at = u * TRIO + phase
        return self.send_sems.at[at], self.recv_sems.at[DUO * at + kind]

    def send(self, u, phase, name):
        axis = ORDER[u][phase]
        if phase == DUO:
            src, to = self.view(u, DUO, name + 1), name + 1
        else:
            hop, half, to = ((DUO, 0, 1), (DUO, 1, TRIO), (1, 1, 1), (TRIO, 0, TRIO), (1, 0, 1), (TRIO, 1, TRIO))[name]
            src = self.view(u, phase, hop, half)
        self.copy(src, self.buf(u, phase).at[name], self.sems(u, phase, int(name > 1 and phase < DUO)), self.near[axis, to]).start()

    def launch(self, u, phase):
        if BEFORE[u] is not None:
            self.drain(BEFORE[u], phase)
        for name in range(RING if phase < DUO else TRIO):
            self.send(u, phase, name)

    def arrived(self, u, phase, first, count):
        whole = self.buf(u, phase).at[pl.ds(first, count)]
        self.copy(whole, whole, self.sems(u, phase, int(first > 0)), self.peer).wait_recv()

    def drain(self, u, phase):
        if (u, phase) not in self.drained:
            self.drained.add((u, phase))
            whole = self.buf(u, phase)
            self.copy(whole, whole, self.sems(u, phase), self.peer).wait_send()

    def out(self, u):
        if u < HEADS:
            out, col = self.outs[0], self.core * HALF + u * LANES
        elif u < 10:
            out, col = self.outs[u - 7], self.core * LANES
        else:
            out, col = self.outs[TRIO], self.core * HALF + (u - 10) * LANES
        return out.at[:, pl.ds(pl.multiple_of(col, LANES), LANES)]

    def kept(self, u):
        return pltpu.make_async_copy(self.fin.at[u, self.keep], self.out(u), self.swap_sems.at[DUO + u])

    def run(self, u, stage):
        if stage == 0:
            return self.launch(u, 0)
        phase = (stage - 1) // DUO
        if stage == LAST:
            self.arrived(u, DUO, 0, TRIO)
            got = self.buf(u, DUO)
            self.fin[u] = self.view(u, DUO, 0)[...] + (got[0] + got[1] + got[DUO])
            self.copy(self.fin.at[u, self.give], self.out(u), (self.swap_sems.at[0], self.swap_sems.at[1]), self.peer).start()
            self.kept(u).start()
            return
        got = self.buf(u, phase)
        if stage % DUO:
            self.arrived(u, phase, 0, DUO)
            for name, hop in ((0, 1), (1, TRIO)):
                add_into(self.view(u, phase, hop, name), got.at[name])
                self.send(u, phase, name + RING)
            return
        self.arrived(u, phase, DUO, RING)
        if phase == 0 and BEFORE[u] is not None:
            self.drain(BEFORE[u], 1)
            self.drain(BEFORE[u], DUO)
        for half, names in ((0, (TRIO, RING)), (1, (DUO, 5))):
            if phase:
                add_into(self.view(u, phase, 0, half), *[got.at[name] for name in names])
            else:
                dst = self.mid.at[self.slot(u) + (ALL, ALL, HALVES[half], slice(None))]
                add_into(dst, self.view(u, 0, 0, half), *[got.at[name] for name in names], fresh=True)
        self.launch(u, phase + 1)

    def finish(self):
        for u in range(N_UNITS):
            for phase in range(TRIO):
                self.drain(u, phase)
        half = self.fin.at[:, pl.ds(0, SHARE)]
        swaps = self.copy(half, half, (self.swap_sems.at[0], self.swap_sems.at[1]), self.peer)
        swaps.wait_send()
        swaps.wait_recv()
        for u in range(N_UNITS):
            self.kept(u).wait()


def attend(heads, qt, do_t, k, kt, v, vt, cos, sin, o_row, ot, dq, dkt, dvt, s_scr, e_scr, p_scr, d_scr):
    f32, bf16 = jnp.float32, jnp.bfloat16
    strip = TURN
    work = [(h, j) for j in range(NBLK) for h in range(len(heads))]

    def strips(c):
        return [(i * strip, slice(c * QB + i * strip, c * QB + (i + 1) * strip)) for i in range(QB // strip)]

    def fold(x, op):
        return op(x.reshape(strip // SUBS, SUBS, QB), axis=0)

    def scores(i):
        (h, j), b = work[i], i % DUO
        q_t = qt[heads[h], j * QB:(j + 1) * QB]
        top = jnp.full((SUBS, QB), -jnp.inf, f32)
        for c in range(j + 1):
            tile = dot(k[c * QB:(c + 1) * QB, :], q_t)
            for at, rows in strips(c):
                s = tile[at:at + strip]
                if c == j:
                    seen = lax.broadcasted_iota(jnp.int32, (strip, QB), 0) + at <= lax.broadcasted_iota(jnp.int32, (strip, QB), 1)
                    s = jnp.where(seen, s, -jnp.inf)
                s_scr[b, rows, :] = s
                top = jnp.maximum(top, fold(s, jnp.max))
        return jnp.max(top, axis=0, keepdims=True)

    def rest(i, m):
        (h, j), b = work[i], i % DUO
        cols, n = slice(j * QB, (j + 1) * QB), (j + 1) * QB
        q_t, d_t = qt[heads[h], cols], do_t[heads[h], cols]
        tot = jnp.zeros((SUBS, QB), f32)
        for c in range(j + 1):
            for at, rows in strips(c):
                e = jnp.exp2((s_scr[b, rows, :] - m) * (SCALE * LOG2E))
                s_scr[b, rows, :] = e
                e_scr[b, rows, :] = e.astype(bf16)
                tot = tot + fold(e, jnp.sum)
        den = jnp.sum(tot, axis=0, keepdims=True)
        inv = 1.0 / den
        o = (dot(vt[:, :n], e_scr[b, :n, :]) / den).astype(bf16)
        ot[o_row(h), cols] = o
        delta = jnp.sum(d_t.astype(f32) * o.astype(f32), axis=0, keepdims=True)
        for c in range(j + 1):
            dp = dot(v[c * QB:(c + 1) * QB, :], d_t)
            for at, rows in strips(c):
                p = s_scr[b, rows, :] * inv
                p_scr[b, rows, :] = p.astype(bf16)
                d_scr[b, rows, :] = (p * (dp[at:at + strip] - delta)).astype(bf16)
        dvt[:, :n] += dot_nt(d_t, p_scr[b, :n, :])
        dkt[:, :n] += dot_nt(q_t, d_scr[b, :n, :])
        g = dot(kt[:, :n], d_scr[b, :n, :]) * SCALE
        co, si = cos[:, cols], sin[:, cols]
        x, y = g[:TURN], g[TURN:]
        dq[heads[h], cols] = jnp.concatenate([x * co + y * si, y * co - x * si], axis=0).astype(bf16)

    m = scores(0)
    for i in range(len(work)):
        later = scores(i + 1) if i + 1 < len(work) else None
        rest(i, m)
        m = later


def tail_kernel(qt, do_t, k, kt, v, vt, rt, dyc, wqk, wqkp, wvo, wvop, gain, hidden, dy, pos, cos, sin,
                result, grad_x, gq, gk, gv, go, gout,
                two, ks, kts, vs, vts, rts, ots, dqo, dqp, dkvo, dkvp, dkt, dvt, s_scr, e_scr, p_scr, d_scr, dycs, part, mid, buf1, buf2, buf3, fin, own, onat, dnat, xs, gacc, gpart, gpeer, gz, gx,
                send_sems, recv_sems, swap_sems, trade_send, trade_recv, local_sems):
    comm = Singles(trade_send, trade_recv, local_sems)
    comm.used = DUO * HEADS
    f32, bf16 = jnp.float32, jnp.bfloat16
    core, peer = comm.core, comm.peer()
    a1, a2 = two.at[0], two.at[1]
    comm.announce(CORNERS)
    sc = Scatter(comm, part, mid, (buf1, buf2, buf3), fin, (gq, gk, gv, go), send_sems, recv_sems, swap_sems)
    plan = Plan()
    some, most = pl.ds(0, PAIR), pl.ds(PAIR, HALF - PAIR)
    loads = [comm.local(s, d) for s, d in ((qt.at[some], two.at[0, some]), (k, ks), (do_t.at[some], two.at[1, some]), (vt, vts), (v, vs), (kt, kts))]
    dkt[...] = jnp.zeros_like(dkt)
    dvt[...] = jnp.zeros_like(dvt)
    with scope('wait_q'):
        for c in loads:
            c.wait()
    loads = [comm.local(s, d) for s, d in ((rt, rts), (qt.at[most], two.at[0, most]), (do_t.at[most], two.at[1, most]))]
    later = [comm.local(s, d) for s, d in ((dyc, dycs), (hidden, xs))]

    def emit(stages):
        for u, stage in stages:
            with scope(f'u{u}_s{stage}'):
                if u == GAIN:
                    sum_gain(stage)
                else:
                    sc.run(u, stage)

    def after(cost):
        plan.now += cost
        return plan.due()

    def head_trades(h):
        row = tile_at(core * HEADS + h, LANES)
        mine = tile_at(h, LANES)
        return [pltpu.make_async_remote_copy(src_ref=s, dst_ref=d, send_sem=trade_send.at[i], recv_sem=trade_recv.at[i], device_id=peer, device_id_type=MESH)
                for s, d, i in ((ots.at[row], ots.at[row], h), (dqo.at[mine], dqp.at[mine], HEADS + h))]

    def gradient(place, count, left, right, mul):
        with scope('grad'):
            @pl.loop(0, DUO)
            def _(z):
                g = mul(left[tile_at(z, HALF), :], right())
                for i in range(count):
                    part[place + i, tile_at(z, DUO)] = g[:, i * LANES:(i + 1) * LANES].reshape(DUO, RING, RING, CHIP, LANES)

    PAIRS = HEADS // DUO
    attended, paired = [], []
    for g in range(PAIRS):
        attended.append(after(5.1))
        plan.now += 1.5
        plan.start(DUO * g)
        plan.start(DUO * g + 1)
        paired.append(plan.due())

    @pl.loop(0, PAIRS)
    def _(g):
        def at(table):
            for i in range(PAIRS):
                if table[i]:
                    pl.when(g == i)(functools.partial(emit, table[i]))

        heads = [tile_at(DUO * g + i, LANES) for i in range(DUO)]
        with scope('attend'):
            attend(heads, a1, a2, ks, kts, vs, vts, cos, sin, lambda i: tile_at(core * HEADS + DUO * g + i, LANES), ots, dqo, dkt, dvt, s_scr, e_scr, p_scr, d_scr)

        @pl.when(g == 0)
        def _():
            with scope('entry'):
                comm.meet(CORNERS)
                for c in loads:
                    c.wait()
        for i in range(DUO):
            for c in head_trades(DUO * g + i):
                c.start()
        at(attended)
        gradient(DUO * g, DUO, rts, lambda: dqo[tile_at(g, PAIR), :], dot_nt)
        at(paired)

    def beat(cost, *starts):
        plan.now += cost
        for u in starts:
            plan.start(u)
        emit(plan.due())

    wkv, wkvp = e_scr.reshape(DIM, PAIR), p_scr.reshape(DIM, PAIR)
    later += [comm.local(src.at[:, pl.ds(at, LANES)], dst.at[:, pl.ds(to, LANES)]) for srcs, dst in (((wqk, wvo), wkv), ((wqkp, wvop), wkvp)) for src, at, to in ((srcs[0], HALF, 0), (srcs[1], 0, LANES))]
    wqp_loads = [comm.local(wqkp.at[tile_at(i, HALF), pl.ds(0, HALF)], two.at[i]) for i in range(DUO)]
    key = dkt[...] * SCALE
    co, si, x, y = cos[...], sin[...], key[:TURN], key[TURN:]
    dkvo[:LANES, :] = jnp.concatenate([x * co + y * si, y * co - x * si], axis=0).astype(bf16)
    dkvo[LANES:, :] = dvt[...].astype(bf16)
    comm.trade(dkvo, dkvp)
    gradient(UNIT_K, DUO, rts, lambda: dkvo[...], dot_nt)
    beat(1.8, UNIT_K, UNIT_V)
    wq_load = comm.local(wqk.at[:, pl.ds(0, HALF)], rts)
    for c in later:
        c.wait()
    with scope('trades'):
        for h in range(HEADS):
            for c in head_trades(h):
                c.wait()

    waiting = list(range(RING))

    def output_gradients(force=False):
        while waiting:
            first = 10 + DUO * waiting[0]
            before = [u for u in range(N_UNITS) if u < first and PLACE[u] in (PLACE[first], PLACE[first + 1])]
            if force:
                emit(plan.rush(lambda: all(map(plan.vacated, before))))
            if not all(map(plan.vacated, before)):
                return
            for u in before:
                sc.drain(u, 0)
            i = waiting.pop(0)
            gradient(PLACE[first], DUO, ots, lambda: dycs[:, i * PAIR:(i + 1) * PAIR], dot)
            plan.start(first)
            plan.start(first + 1)
            beat(1.5)

    def piece(cost):
        beat(cost)
        output_gradients()

    def ticking(n, cost, body):
        tables = [after(cost) for _ in range(n)]

        @pl.loop(0, n)
        def _(i):
            body(i)
            for j, table in enumerate(tables):
                if table:
                    pl.when(i == j)(functools.partial(emit, table))
        output_gradients()

    @pl.loop(0, TOKENS // LANES)
    def _(i):
        want = lax.broadcasted_iota(jnp.int32, (LANES, ROWS), 0) + i * LANES
        own[tile_at(i, LANES), :] = jnp.where(want == pos[...], 1.0, 0.0).astype(bf16)

    def unsort(at, src_t, n):
        with scope('unsort'):
            dnat[at:at + n, :] = dot(src_t[:n, :], own[...]).astype(bf16)

    output_gradients()
    for c in comm.exchanged:
        c.wait_recv()
    unsort(0, dqo, HALF)
    dy_loads = [comm.local(dy.at[:, tile_at(i, HALF)], dqo.at[tile_at(i, ROWS)]) for i in range(DUO)]
    piece(1.2)
    unsort(HALF, dqp, HALF)
    piece(1.2)
    unsort(DUO * HALF, dkvo, PAIR)
    unsort(DUO * HALF + PAIR, dkvp, PAIR)
    piece(0.7)
    wq_load.wait()
    for c in wqp_loads + dy_loads:
        c.wait()
    gacc[...] = jnp.zeros_like(gacc)

    def dr_parts(half, r):
        return [s_scr.at[half, r(i * PAIR), :] for i in range(RING)]

    def back(block, then):
        def dr(half):
            with scope('dr'):
                c = tile_at(half, HALF)
                left = jnp.concatenate([rts[c, :], two[half], wkv[c, :], wkvp[c, :]], axis=1)
                acc = dot(left, dnat[:, block * PAIR:(block + 1) * PAIR])
                for i, ref in enumerate(dr_parts(half, lambda at: pl.ds(at, PAIR))):
                    ref[...] = acc[i * PAIR:(i + 1) * PAIR, :].T

        def norm(part):
            with scope('back'):
                @pl.loop(0, RING)
                def _(i):
                    j = part * RING + i
                    q = pl.ds(pl.multiple_of(block * PAIR + j * SHARE, SHARE), SHARE)
                    d = jnp.concatenate([ref[...] for half in range(DUO) for ref in dr_parts(half, lambda at: pl.ds(pl.multiple_of(at + j * SHARE, SHARE), SHARE))], axis=1)
                    x = xs[q, :].astype(f32)
                    inv = lax.rsqrt(jnp.mean(x * x, axis=-1, keepdims=True) + RMS_EPS)
                    unit = x * inv
                    gacc[...] += jnp.sum((d * unit).reshape(DUO, SUBS, DIM), axis=0)
                    dg = d * gain[0:1, :]
                    new = inv * (dg - unit * jnp.mean(dg * unit, axis=-1, keepdims=True))
                    for half in range(DUO):
                        r = pl.ds(pl.multiple_of(half * ROWS + block * PAIR + j * SHARE, SHARE), SHARE)
                        dqo[r, :] = (dqo[r, :].astype(f32) + new[:, half * HALF:(half + 1) * HALF]).astype(bf16)

        ticking(DUO, 1.6, dr)
        then()
        ticking(RING, 0.92, norm)

    back(0, lambda: None)
    wo_loads = []
    back(1, lambda: wo_loads.extend([comm.local(wvo.at[:, pl.ds(LANES, HALF)], rts)] + [comm.local(wvop.at[tile_at(i, HALF), pl.ds(LANES, HALF)], two.at[i]) for i in range(DUO)]))
    for i in range(DUO):
        comm.store(dqo.at[tile_at(i, ROWS)], grad_x.at[:, tile_at(i, HALF)])
    total = jnp.sum(gacc[...], axis=0, keepdims=True)
    gpart[...] = jnp.zeros_like(gpart)
    for i in range(RING):
        for j in range(RING):
            gpart[i, j:j + 1, :] = total[:, (i * RING + j) * LANES:(i * RING + j + 1) * LANES]

    arrivals = []

    def sum_gain(stage):
        for c in arrivals:
            c.wait_recv()
        del arrivals[:]
        if stage == 0:
            arrivals.append(comm.send(gpart, gpeer, peer))
        elif stage == 1:
            for j in range(RING):
                gz[j] = gpart[j] + gpeer[j]
            arrivals.extend(comm.send(gz.at[step(comm.pos, 'z', hop)], gz.at[TRIO + hop], comm.far('z', hop)) for hop in (1, DUO, TRIO))
        elif stage == DUO:
            gx[0, 0] = (gz[comm.pos['z']] + gz[RING]) + (gz[5] + gz[6])
            for dy, dx in PLANE:
                arrivals.append(comm.send(gx.at[0, 0], gx.at[dy, dx], comm.aside(dy, dx)))
        else:
            gpeer[0] = sum(gx[dy, dx] for dy, dx in PLANE) + gx[0, 0]
            mine = jnp.broadcast_to(gpeer[0, pl.ds(comm.pos['y'], 1), :], (SUBS, LANES))
            gout[...] = pltpu.roll(mine, LANES - (comm.pos['x'] * CHIP + core * SHARE), 1)

    plan.start(GAIN)
    beat(0.2)
    for i in range(DUO):
        with scope('unsort_o'):
            @pl.loop(0, DUO)
            def _(j):
                r = pl.ds(pl.multiple_of(i * HALF + j * ROWS, ROWS), ROWS)
                onat[:, r] = dot(ots[r, :], own[...]).astype(bf16).T
        piece(1.58)
    output_gradients(True)

    def project_out(col, weights, i):
        with scope('project'):
            @pl.loop(DUO * i, DUO * i + DUO)
            def _(j):
                c = tile_at(j, PAIR)
                dst = pl.ds(pl.multiple_of(col + j * PAIR, PAIR), PAIR)
                xs[:, dst] = (xs[:, dst].astype(f32) + dot(onat[...], weights(c))).astype(bf16)
        beat(1.48)

    def own_half(c):
        return rts[:, c]

    def other_half(c):
        return jnp.concatenate([a1[:, c], a2[:, c]], axis=0)

    for c in wo_loads:
        c.wait()
    for col, weights in ((core * HALF, own_half), ((1 - core) * HALF, other_half)):
        for i in range(DUO):
            project_out(col, weights, i)
    comm.store(xs, result)
    emit(plan.rush(lambda: not plan.stage))
    with scope('finish'):
        sc.finish()
        for c in comm.sent + comm.exchanged:
            c.wait_send()
        for c in comm.stored:
            c.wait()


def tail(qt, do_t, k, kt, v, vt, rt, dyc, wqk, wqkp, wvo, wvop, gain, hidden, dy, pos, cos, sin):
    bf16, f32 = jnp.bfloat16, jnp.float32
    any_ = pl.BlockSpec(memory_space=pl.ANY)
    vmem = pl.BlockSpec(memory_space=pltpu.VMEM)
    S = lambda shape, d=bf16: jax.ShapeDtypeStruct(shape, d)
    V = lambda shape, d=bf16: pltpu.VMEM(shape, d)
    D = lambda n: pltpu.SemaphoreType.DMA((n,))
    sq, tall, wide = (HALF, TOKENS), (TOKENS, LANES), (LANES, TOKENS)
    mine, kv = (ROWS, DIM), (PAIR, TOKENS)
    return pl.pallas_call(
        tail_kernel,
        out_shape=[S(mine), S(mine), S((SHARE, DIM), f32), S((SHARE, PAIR), f32), S((SHARE, PAIR), f32), S((SHARE, DIM), f32), S((SUBS, LANES), f32)],
        in_specs=[any_] * 12 + [vmem] + [any_] * DUO + [vmem] * TRIO,
        out_specs=[any_] * 6 + [vmem],
        scratch_shapes=[V((DUO,) + sq), V(tall), V(wide), V(tall), V(wide), V((DIM, TOKENS)), V((DIM, TOKENS)), V(sq), V(sq), V(kv), V(kv), V(wide, f32), V(wide, f32),
                        V((DUO, TOKENS, QB), f32), V((DUO, TOKENS, QB)), V((DUO, TOKENS, QB)), V((DUO, TOKENS, QB)), V(sq), V((PLACES, RING, RING, RING, CHIP, LANES), f32), V((TRIO, SLOTS, RING, RING, CHIP, LANES), f32),
                        V((TRIO, SLOTS, 6, RING, RING, SHARE, LANES), f32), V((TRIO, SLOTS, 6, RING, SHARE, LANES), f32), V((TRIO, SLOTS, TRIO, CHIP, LANES), f32), V((N_UNITS, CHIP, LANES), f32), V((TOKENS, ROWS)), V(mine), V((DUO * QKV, ROWS)), V(mine),
                        V((SUBS, DIM), f32), V((RING, SUBS, LANES), f32), V((RING, SUBS, LANES), f32), V((7, SUBS, LANES), f32), V((RING, RING, SUBS, LANES), f32),
                        D(TRIO * N_UNITS), D(6 * N_UNITS), D(DUO + N_UNITS), D(DUO * HEADS + 20), D(DUO * HEADS + 20), D(CHIP)],
        compiler_params=pltpu.CompilerParams(collective_id=1, has_side_effects=True, vmem_limit_bytes=67043328),
        name='tail',
    )(qt, do_t, k, kt, v, vt, rt, dyc, wqk, wqkp, wvo, wvop, gain, hidden, dy, pos, cos, sin)


def settle_kernel(n, *refs):
    ins, gain, outs, gain_out, bufs, sems = refs[:n], refs[n], refs[n + 1:DUO * n + 1], refs[DUO * n + 1], refs[DUO * n + DUO:-1], refs[-1]
    jobs = []
    for a, o, b in zip(ins, outs, bufs):
        size = a.shape[0] // RING if a.shape[0] == ROWS else a.shape[0]
        jobs += [tuple(r.at[pl.ds(i, size)] for r in (a, b, o)) for i in range(0, a.shape[0], size)]
    takes = [pltpu.make_async_copy(a, b, sems.at[0, i]) for i, (a, b, _) in enumerate(jobs)]
    puts = [pltpu.make_async_copy(b, o, sems.at[1, i]) for i, (_, b, o) in enumerate(jobs)]
    for c in takes:
        c.start()
    gain_out[...] = gain[0:1, :SHARE]
    for take, put in zip(takes, puts):
        take.wait()
        put.start()
    for c in puts:
        c.wait()


def settle(*arrays):
    *large, gain = arrays
    any_, vmem = pl.BlockSpec(memory_space=pl.ANY), pl.BlockSpec(memory_space=pltpu.VMEM)
    return pl.pallas_call(
        functools.partial(settle_kernel, len(large)),
        out_shape=[jax.ShapeDtypeStruct(a.shape, a.dtype) for a in large] + [jax.ShapeDtypeStruct((1, SHARE), gain.dtype)],
        in_specs=[any_] * len(large) + [vmem],
        out_specs=[any_] * len(large) + [vmem],
        scratch_shapes=[pltpu.VMEM(a.shape, a.dtype) for a in large] + [pltpu.SemaphoreType.DMA((DUO, 12))],
        name='settle',
    )(*arrays)


def rope_tables():
    j = np.arange(HEAD_DIM // DUO, dtype=np.float64) / (HEAD_DIM // DUO)
    freq = (ROPE_THETA ** -j).astype(np.float32)
    angle = freq[:, None] * np.arange(TOKENS, dtype=np.float32)[None, :]
    return np.cos(angle.astype(np.float64)).astype(np.float32), np.sin(angle.astype(np.float64)).astype(np.float32)


def solution(mesh):
    def shard_fn(hidden, tok_pos, grad_out, norm_gain, w_query, w_key, w_value, w_out):
        hidden, grad_out = hidden[0], grad_out[0]
        cos_t, sin_t = (jnp.asarray(t) for t in rope_tables())
        *parts, gain = head(hidden, grad_out, w_query, w_key, w_value, w_out, tok_pos, norm_gain.reshape(1, SHARE), cos_t, sin_t)
        parts = [p.reshape(DIM, GROUP) if p.ndim > DUO else p for p in parts]
        result, grad_hidden, gq, gk, gv, go, gout = settle(*tail(*parts, gain, hidden, grad_out, tok_pos, cos_t, sin_t))
        return result[None], grad_hidden[None], gq, gk, gv, go, gout.reshape(SHARE)

    row_spec, pos_spec = P('fsdp', 'cp', None), P('fsdp', 'cp')
    weight_spec, gain_spec = P(('fsdp', 'cp'), None), P(('fsdp', 'cp'))
    return jax.shard_map(shard_fn, mesh=mesh, in_specs=(row_spec, pos_spec, row_spec, gain_spec, weight_spec, weight_spec, weight_spec, weight_spec), out_specs=(row_spec, row_spec, weight_spec, weight_spec, weight_spec, weight_spec, gain_spec), check_vma=False)
```

```python
import functools
import jax
import jax.numpy as jnp
import numpy as np
from jax import lax
from jax.experimental import pallas as pl
from jax.experimental.pallas import tpu as pltpu
from jax.sharding import PartitionSpec as P

LANES, SUBS, RING, TRIO, DUO = 128, 8, 4, 3, 2
PAIR, ROWS, CHIP, SHARE, TURN = 256, 512, 32, 16, 64
HEAD_DIM = LANES
ROPE_THETA = 1000000.0
RMS_EPS = 1e-5
SCALE = HEAD_DIM ** -0.5
LOG2E = 1.4426950408889634

MESH = pl.DeviceIdType.MESH
AXES = ('x', 'y', 'z')
ORDERS = (('x', 'y', 'z'), ('y', 'z', 'x'), ('z', 'x', 'y'))
ALL = pl.ds(0, RING)


def torus():
    f = lax.axis_index('fsdp')
    return {'x': lax.rem(f, RING), 'y': lax.rem(lax.div(f, RING), RING), 'z': lax.div(f, SHARE)}


def step(pos, axis, hop):
    return lax.rem(pos[axis] + hop, RING)


class Batch:
    def __init__(self, comm):
        self.comm, self.index = comm, comm.used
        comm.used += 1

    def _copy(self, src, dst, device):
        send, recv, _ = self.comm.sems
        return pltpu.make_async_remote_copy(src_ref=src, dst_ref=dst, send_sem=send.at[self.index], recv_sem=recv.at[self.index], device_id=device, device_id_type=MESH)

    def send(self, src, dst, device):
        self._copy(src, dst, device).start()
        return self

    def arrived(self, whole):
        self._copy(whole, whole, self.comm.peer()).wait_recv()

    def sent(self, whole):
        self._copy(whole, whole, self.comm.peer()).wait_send()


class Comm:
    def __init__(self, send_sems, recv_sems, local_sems):
        self.pos = torus()
        self.core = lax.axis_index('cp')
        self.sems = (send_sems, recv_sems, local_sems)
        self.used = self.used_local = 0
        self.stored = []

    def far(self, axis, hop):
        p = dict(self.pos)
        p[axis] = step(self.pos, axis, hop)
        return {'fsdp': (p['z'] * RING + p['y']) * RING + p['x'], 'cp': self.core}

    def peer(self):
        return {'fsdp': lax.axis_index('fsdp'), 'cp': 1 - self.core}

    def aside(self, dy, dx):
        return {'fsdp': (self.pos['z'] * RING + step(self.pos, 'y', dy)) * RING + step(self.pos, 'x', dx), 'cp': self.core}

    def announce(self, corners=()):
        sem = pltpu.get_barrier_semaphore()
        for axis in AXES:
            for hop in (1, DUO, TRIO):
                pl.semaphore_signal(sem, inc=1, device_id=self.far(axis, hop), device_id_type=MESH)
        for dy, dx in corners:
            pl.semaphore_signal(sem, inc=1, device_id=self.aside(dy, dx), device_id_type=MESH)
        pl.semaphore_signal(sem, inc=1, device_id=self.peer(), device_id_type=MESH)

    def meet(self, corners=()):
        pl.semaphore_wait(pltpu.get_barrier_semaphore(), 10 + len(corners))

    def ring(self, batch, src, slots, axis):
        for hop in (1, DUO, TRIO):
            batch.send(src, slots.at[hop], self.far(axis, hop))

    def local(self, src, dst):
        i = self.used_local
        self.used_local += 1
        c = pltpu.make_async_copy(src, dst, self.sems[DUO].at[i])
        c.start()
        return c

    def store(self, src, dst):
        self.stored.append(self.local(src, dst))


class Singles(Comm):
    def __init__(self, *sems):
        super().__init__(*sems)
        self.sent, self.exchanged = [], []

    def _copy(self, src, dst, device):
        i = self.used
        self.used += 1
        c = pltpu.make_async_remote_copy(src_ref=src, dst_ref=dst, send_sem=self.sems[0].at[i], recv_sem=self.sems[1].at[i], device_id=device, device_id_type=MESH)
        c.start()
        return c

    def send(self, src, dst, device):
        c = self._copy(src, dst, device)
        self.sent.append(c)
        return c

    def trade(self, src, dst):
        self.exchanged.append(self._copy(src, dst, self.peer()))


def pick(ref, sel, piece):
    lo, cols, first, rows = piece
    return ref.at[sel['z'], sel['y'], sel['x'], pl.ds(first, rows), pl.ds(lo, cols)]


def sem_scratch(remote, local):
    return [pltpu.SemaphoreType.DMA((remote,)), pltpu.SemaphoreType.DMA((remote,)), pltpu.SemaphoreType.DMA((local,))]


def add_into(dst, *srcs, fresh=False):
    def add(idx):
        total, *rest = [s[idx] for s in (srcs if fresh else (dst,) + srcs)]
        for more in rest:
            total = total + more
        dst[idx] = total

    if len(dst.shape) > TRIO:
        @pl.loop(0, dst.shape[0])
        def _(i):
            add((i,))
    else:
        add(Ellipsis)


def columns(lo, na, nb):
    return (lo, na, 0, CHIP), (lo + na, nb, 0, CHIP)


def strip(lo):
    return (lo, LANES, 0, SHARE), (lo, LANES, SHARE, SHARE)


QK_COLORS = (columns(0, PAIR, LANES), columns(384, LANES, PAIR), columns(768, PAIR, LANES))
VO_COLORS = (columns(0, LANES, PAIR), columns(384, PAIR, LANES), columns(768, LANES, PAIR))
QK_FIRST = (columns(0, LANES, LANES), columns(384, LANES, LANES), columns(768, LANES, LANES))
QK_LAST = (strip(PAIR), strip(640), strip(1024))
TOKENS = 1024
DIM = 2048
HALF = 1024
QKV = 1280
GROUP = 1152


def scope(name):
    return jax.named_scope(name)


def dot(a, b):
    return jnp.dot(a, b, preferred_element_type=jnp.float32)


def dot_nt(a, b):
    return lax.dot_general(a, b, (((1,), (1,)), ((), ())), preferred_element_type=jnp.float32)


def tile_at(i, n):
    return pl.ds(pl.multiple_of(i * n, n), n)


class Gather:
    def __init__(self, comm, ref, colors, land, held=None):
        self.comm, self.ref, self.colors, self.land = comm, ref, colors, land
        self.held = list(held or [dict(comm.pos) for _ in colors])
        self.batches = []

    def move(self, batch, s, piece, to):
        batch.send(pick(self.ref, s, piece), pick(self.ref, s, piece), to)

    def at(self, k, hop):
        d = ORDERS[k][self.phase]
        return dict(self.held[k], **{d: step(self.comm.pos, d, hop)})

    def begin(self, phase):
        self.phase = phase
        self.up, self.dn, self.rest = ([Batch(self.comm) for _ in range(TRIO)] for _ in range(TRIO))
        self.batches += self.up + self.dn + self.rest
        for k, (a, b) in enumerate(self.colors):
            d = ORDERS[k][phase]
            up, dn, s = self.comm.far(d, 1), self.comm.far(d, TRIO), self.held[k]
            self.move(self.up[k], s, a, up)
            self.move(self.dn[k], s, b, dn)
            self.move(self.rest[k], s, b, up)
            self.move(self.rest[k], s, a, dn)
            if phase == 0:
                for piece in (a, b):
                    self.move(self.rest[k], s, piece, self.comm.far(d, DUO))
        if phase == DUO:
            for k, pieces in enumerate(self.colors):
                for piece in pieces:
                    self.land(self.ref, self.held[k], piece)

    def forward(self):
        for k, (a, b) in enumerate(self.colors):
            d = ORDERS[k][self.phase]
            for batch, hop, piece, to in ((self.up[k], TRIO, a, 1), (self.dn[k], 1, b, TRIO)):
                s = self.at(k, hop)
                batch.arrived(pick(self.ref, s, piece))
                if self.phase:
                    self.move(self.rest[k], s, piece, self.comm.far(d, to))
                if self.phase == DUO:
                    self.land(self.ref, s, piece)

    def end(self):
        for k, (a, b) in enumerate(self.colors):
            d = ORDERS[k][self.phase]
            two = dict(self.held[k], **{d: pl.ds(0, DUO)})
            both = (a[0], max(a[0] + a[1], b[0] + b[1]) - a[0], 0, CHIP)
            self.rest[k].arrived(pick(self.ref, two, both))
            if self.phase == DUO:
                for hop, piece in ((TRIO, b), (1, a), (DUO, a), (DUO, b)):
                    self.land(self.ref, self.at(k, hop), piece)
            for batch, s, piece in ((self.up[k], self.held[k], a), (self.dn[k], self.held[k], b), (self.rest[k], two, both)):
                batch.spent = pick(self.ref, s, piece)
            self.held[k] = dict(self.held[k], **{d: ALL})

    def finish(self):
        for batch in self.batches:
            batch.sent(batch.spent)


def head_kernel(hidden, dy, wq, wk, wv, wo, pos, gain_in, cos_t, sin_t,
                qt_o, dot_o, k_o, kt_o, v_o, vt_o, rt_o, dyc_o, wqk_o, wqkp_o, wvo_o, wvop_o, gain_o,
                hid2, dy2, dys, rs, rt, wqk, wvo, wpeer, pi, pos2, qt, dot_s, kk, kt, vv, vt, gain, gtile, gbuf, gx, gy, gz, *sems):
    comm = Comm(*sems)
    pos_c, core = comm.pos, comm.core
    bf16, f32 = jnp.bfloat16, jnp.float32
    peer = comm.peer()
    rows = tile_at(core, SHARE)
    mine_qk = wqk.at[pos_c['z'], pos_c['y'], pos_c['x'], rows]
    mine_vo = wvo.at[pos_c['z'], pos_c['y'], pos_c['x'], rows]

    def weight_parts(c):
        return ((wq.at[:, tile_at(c, HALF)], mine_qk.at[:, pl.ds(0, HALF)]), (wk.at[:, tile_at(c, LANES)], mine_qk.at[:, pl.ds(HALF, LANES)]),
                (wv.at[:, tile_at(c, LANES)], mine_vo.at[:, pl.ds(0, LANES)]), (wo.at[:, tile_at(c, HALF)], mine_vo.at[:, pl.ds(LANES, HALF)]))

    loads = [comm.local(s, d) for s, d in weight_parts(core)]
    load_x = [comm.local(hidden, hid2.at[pl.ds(0, ROWS)]), comm.local(dy, dy2.at[pl.ds(0, ROWS)])]
    share = lax.broadcasted_iota(jnp.int32, (SUBS, LANES), 1) // SHARE
    gtile[...] = jnp.where(share == pos_c['x'] * DUO + core, jnp.broadcast_to(jnp.concatenate([gain_in[...]] * SUBS, axis=1), (SUBS, LANES)), 0.0)
    comm.announce()
    with scope('entry'):
        comm.meet()
    swap_w, swap_pos, swap_dy, swap_x, peers_qk, peers_vo = (Batch(comm) for _ in range(6))
    gain_c, gain_x, gain_y, gain_z = (Batch(comm) for _ in range(RING))
    for s, d in weight_parts(1 - core):
        swap_w.send(s, d, peer)
    gain_c.send(gtile, gbuf, peer)
    swap_pos.send(pos, pos2, peer)
    for c in loads:
        c.wait()
    with scope('wait_w'):
        swapped = wqk.at[pos_c['z'], pos_c['y'], pos_c['x']]
        swap_w.arrived(swapped)

    def land_qk(ref, s, cols):
        peers_qk.send(pick(ref, s, cols), pick(wqkp_o, s, cols), peer)

    def land_vo(ref, s, cols):
        peers_vo.send(pick(ref, s, cols), pick(wpeer, s, cols), peer)

    g1 = Gather(comm, wvo, VO_COLORS, land_vo)
    g2 = Gather(comm, wqk, QK_COLORS, land_qk)
    g1.begin(0)
    g2.begin(0)
    swap_dy.send(dy, dy2.at[pl.ds(ROWS, ROWS)], peer)
    gain_c.arrived(gbuf)
    gx[0] = gtile[...] + gbuf[...]
    comm.ring(gain_x, gx.at[0], gx, 'x')

    swap_pos.arrived(pos2)

    @pl.loop(0, TOKENS // LANES)
    def _(i):
        want = lax.broadcasted_iota(jnp.int32, (LANES, ROWS), 0) + i * LANES
        for h, have in enumerate((pos, pos2)):
            pi[tile_at(i, LANES), h * ROWS:(h + 1) * ROWS] = jnp.where(want == have[...], 1.0, 0.0).astype(bf16)

    def sort(dst, src, first, last):
        with scope('sort'):
            @pl.loop(first, last)
            def _(j):
                c = tile_at(j, PAIR)
                dst[:, c] = dot(pi[...], src[:, c]).astype(bf16)

    with scope('p0_end'):
        for g in (g1, g2):
            g.forward()
            g.end()
            g.begin(1)
    swap_x.send(hidden, hid2.at[pl.ds(ROWS, ROWS)], peer)
    gain_x.arrived(gx.at[pl.ds(1, TRIO)])
    gy[pos_c['y']] = (gx[0] + gx[1]) + (gx[DUO] + gx[TRIO])
    for hop in (1, DUO, TRIO):
        gain_y.send(gy.at[pos_c['y']], gy.at[pos_c['y']], comm.far('y', hop))
    with scope('wait_dy'):
        load_x[1].wait()
        swap_dy.arrived(dy2.at[pl.ds(ROWS, ROWS)])
    sort(dys, dy2, 0, RING)
    with scope('p1a_fwd'):
        g1.forward()
    sort(dys, dy2, RING, 6)
    with scope('p1b_fwd'):
        g2.forward()
    sort(dys, dy2, 6, SUBS)
    with scope('p1a_end'):
        g1.end()
    gain_y.arrived(gy.at[pl.ds(1, TRIO)])
    for j in range(RING):
        gz[pos_c['z'], j] = gy[j]
    for hop in (1, DUO, TRIO):
        gain_z.send(gz.at[pos_c['z']], gz.at[pos_c['z']], comm.far('z', hop))
    g1.begin(DUO)
    comm.store(dys.at[:, tile_at(core, HALF)], dyc_o)
    with scope('p1b_end'):
        g2.end()
    with scope('wait_x'):
        load_x[0].wait()
        swap_x.arrived(hid2.at[pl.ds(ROWS, ROWS)])
    sort(rs, hid2, 0, SUBS)
    with scope('p2q_fwd'):
        g1.forward()
    g2a, g2b = (Gather(comm, wqk, colors, land_qk, g2.held) for colors in (QK_FIRST, QK_LAST))
    g2a.begin(DUO)
    with scope('gain'):
        gain_z.arrived(gz.at[pl.ds(1, TRIO)])
    for i in range(RING):
        for j in range(RING):
            gain[:, (i * RING + j) * LANES:(i * RING + j + 1) * LANES] = gz[i, j]
    comm.store(gain, gain_o)

    def norm(first, last):
        with scope('norm'):
            @pl.loop(first, last)
            def _(i):
                r = tile_at(i, CHIP)
                x = rs[r, :].astype(f32)
                inv = lax.rsqrt(jnp.mean(x * x, axis=-1, keepdims=True) + RMS_EPS)
                rs[r, :] = (x * inv * gain[0:1, :]).astype(bf16)

    norm(0, TOKENS // CHIP)
    with scope('r_t'):
        @pl.loop(0, DIM // PAIR)
        def _(i):
            c = tile_at(i, PAIR)

            @pl.loop(0, TOKENS // PAIR)
            def _(j):
                r = tile_at(j, PAIR)
                rt[c, r] = rs[r, c].T
    comm.store(rt, rt_o)
    with scope('p2o_end'):
        g1.end()
    w_qk, w_vo, w_peer = wqk.reshape(DIM, GROUP), wvo.reshape(DIM, GROUP), wpeer.reshape(DIM, GROUP)
    with scope('vals'):
        @pl.loop(0, DUO)
        def _(i):
            r = tile_at(i, ROWS)
            val = dot(rs[r, :], w_vo[:, :LANES]).astype(bf16)
            vv[r, :] = val
            vt[:, r] = val.T
    for src, dst in ((wvo, wvo_o), (vv, v_o), (vt, vt_o)):
        comm.store(src, dst)
    with scope('p2q_fwd'):
        g2a.forward()
    g2b.begin(DUO)
    with scope('wo_peer'):
        peers_vo.arrived(wpeer)
    comm.store(wpeer, wvop_o)
    with scope('do_t'):
        mine = tile_at(core, HALF)

        @pl.loop(0, TOKENS // PAIR)
        def _(j):
            t = tile_at(j, PAIR)
            w_rows = jnp.concatenate([w_vo[mine, LANES:], w_peer[mine, LANES:]], axis=1)
            d_rows = jnp.concatenate([dys[t, mine], dys[t, tile_at(1 - core, HALF)]], axis=1)
            dot_s[:, t] = dot_nt(w_rows, d_rows).astype(bf16)
    comm.store(dot_s, dot_o)

    def rotated(x, r):
        cos, sin = cos_t[:, r], sin_t[:, r]
        cos = jnp.concatenate([cos, cos], axis=0).T
        sin = jnp.concatenate([-sin, sin], axis=0).T
        return (x * cos + pltpu.roll(x, TURN, 1) * sin).astype(bf16)

    def queries(columns, heads):
        x = dot(rs[...], columns)
        for i in range(RING):
            r = slice(i * PAIR, (i + 1) * PAIR)
            for h, head in enumerate(heads):
                qt[tile_at(head, LANES), r] = rotated(x[r, h * LANES:(h + 1) * LANES], r).T

    with scope('p2q_end'):
        g2a.end()

    def pairs(first, last):
        with scope('q'):
            @pl.loop(first, last)
            def _(t):
                queries(w_qk[:, pl.ds(pl.multiple_of(t * 384, LANES), PAIR)], (TRIO * t, TRIO * t + 1))

    pairs(0, 1)
    with scope('last_fwd'):
        g2b.forward()
    pairs(1, TRIO)
    with scope('last_end'):
        g2b.end()
    comm.store(wqk, wqk_o)
    with scope('q_last'):
        queries(jnp.concatenate([w_qk[:, PAIR:384], w_qk[:, 640:768]], axis=1), (DUO, 5))
    comm.store(qt, qt_o)
    with scope('keys'):
        @pl.loop(0, DUO)
        def _(i):
            r = tile_at(i, ROWS)
            key = rotated(dot(rs[r, :], w_qk[:, HALF:]), r)
            kk[r, :] = key
            kt[:, r] = key.T
    for src, dst in ((kk, k_o), (kt, kt_o)):
        comm.store(src, dst)
    with scope('finish'):
        peers_qk.arrived(wqk)
        for batch, whole in ((swap_w, swapped), (swap_pos, pos2), (swap_dy, dy2.at[pl.ds(ROWS, ROWS)]), (swap_x, hid2.at[pl.ds(ROWS, ROWS)]), (peers_qk, wqk), (peers_vo, wvo),
                             (gain_c, gbuf), (gain_x, gx.at[pl.ds(1, TRIO)]), (gain_y, gy.at[pl.ds(1, TRIO)]), (gain_z, gz.at[pl.ds(1, TRIO)])):
            batch.sent(whole)
        for g in (g1, g2, g2a, g2b):
            g.finish()
        for c in comm.stored:
            c.wait()


def head(hidden, dy, wq, wk, wv, wo, pos, gain, cos_t, sin_t):
    bf16, f32 = jnp.bfloat16, jnp.float32
    any_ = pl.BlockSpec(memory_space=pl.ANY)
    vmem = pl.BlockSpec(memory_space=pltpu.VMEM)
    S = lambda shape, d=bf16: jax.ShapeDtypeStruct(shape, d)
    V = lambda shape, d=bf16: pltpu.VMEM(shape, d)
    group = (RING, RING, RING, CHIP, GROUP)
    sq, tall, wide = (HALF, TOKENS), (TOKENS, LANES), (LANES, TOKENS)
    full = (TOKENS, DIM)
    return pl.pallas_call(
        head_kernel,
        out_shape=[S(sq), S(sq), S(tall), S(wide), S(tall), S(wide), S((DIM, TOKENS)), S((TOKENS, HALF)), S(group), S(group), S(group), S(group), S((SUBS, DIM), f32)],
        in_specs=[any_] * 6 + [vmem] * RING,
        out_specs=[any_] * 13,
        scratch_shapes=[V(full), V(full), V(full), V(full), V((DIM, TOKENS)), V(group), V(group), V(group), V((TOKENS, TOKENS)), V((1, ROWS), jnp.int32),
                        V(sq), V(sq), V(tall), V(wide), V(tall), V(wide), V((SUBS, DIM), f32), V((SUBS, LANES), f32), V((SUBS, LANES), f32), V((RING, SUBS, LANES), f32), V((RING, SUBS, LANES), f32), V((RING, RING, SUBS, LANES), f32)] + sem_scratch(73, 18),
        compiler_params=pltpu.CompilerParams(collective_id=0, has_side_effects=True, vmem_limit_bytes=60 * DUO**20),
        name='head',
    )(hidden, dy, wq, wk, wv, wo, pos, gain, cos_t, sin_t)


HEADS = SUBS
UNIT_K, UNIT_V = SUBS, 9
N_UNITS = 18
GAIN = N_UNITS
SLOTS = RING
LAST = 5
ABREAST = DUO
LINES = ((0, TRIO, 6, 9, 12, 15), (1, RING, 7, 10, 13, SHARE), (DUO, 5, SUBS, 11, 14, 17))
COLOR = {u: k for k, line in enumerate(LINES) for u in line}
RANK = {u: i for line in LINES for i, u in enumerate(line)}
SWAPPED = ()
ORDER = {u: ORDERS[k] if u not in SWAPPED else (ORDERS[k][0], ORDERS[k][DUO], ORDERS[k][1]) for u, k in COLOR.items()}
BEFORE = {u: line[i - SLOTS] if i >= SLOTS else None for line in LINES for i, u in enumerate(line)}
PLACES = 12
PLACE = {u: u % PLACES for u in range(N_UNITS)}
WIRE = (2.82, 0.71, 0.36)
LATENCY = 2.2
STAGE_COST = 0.08


class Plan:
    def __init__(self):
        self.now, self.stage, self.ready, self.order, self.link = 0.0, {}, {}, [], {}
        self.mark = {}

    def _wire(self, u, phase, count):
        link = ORDER[u][phase]
        t = max(self.link.get(link, 0.0), self.now)
        first = t + WIRE[phase] + LATENCY
        self.link[link] = t + WIRE[phase] * count
        return first if phase < DUO else self.link[link] + LATENCY

    def free(self, u, phase):
        if BEFORE[u] is None:
            return True
        done = self.mark.get((BEFORE[u], (DUO, RING, 5)[phase]))
        if done is None:
            return False
        sent = ((0, 1), (DUO, TRIO), (RING,))[phase]
        return any(self.mark.get((j, s), -1) > done and (j, s + 1) in self.mark for j, order in ORDER.items() if order[phase] == ORDER[u][phase] for s in sent)

    def run(self, u):
        stage = self.stage[u]
        self.order.append((u, stage))
        self.mark[u, stage] = len(self.order)
        self.now = max(self.now, self.ready[u]) + STAGE_COST
        self.stage[u] = stage + 1
        if stage == (TRIO if u == GAIN else LAST):
            del self.stage[u]
        elif u == GAIN:
            self.ready[u] = max([self.now] + [self.link.get(a, 0.0) for a in ('', 'z', 'xy')[stage]]) + DUO * LATENCY
        elif stage % DUO:
            self.ready[u] = self._wire(u, stage // DUO, 1)
        else:
            self.ready[u] = self._wire(u, stage // DUO, DUO)

    def blocked(self, u):
        stage = self.stage[u]
        if u == GAIN:
            return False
        if stage == 0 and sum(0 < self.stage.get(j, 0) <= DUO for j in LINES[COLOR[u]]) >= ABREAST:
            return True
        if stage == DUO and BEFORE[u] is not None and (BEFORE[u], LAST) not in self.mark:
            return True
        return stage in (0, DUO, RING) and not self.free(u, stage // DUO)

    def start(self, u):
        self.stage[u], self.ready[u] = 0, self.now

    def due(self):
        first = len(self.order)
        while True:
            ripe = [(self.ready[u], u) for u in self.stage if self.ready[u] <= self.now and not self.blocked(u)]
            if not ripe:
                return self.order[first:]
            self.run(min(ripe)[1])

    def vacated(self, u):
        return (u, DUO) in self.mark

    def rush(self, done):
        first = len(self.order)
        while not done():
            self.run(min((self.ready[u], u) for u in self.stage if not self.blocked(u))[1])
        return self.order[first:]


QB = PAIR
NBLK = TOKENS // QB
HALVES = (pl.ds(0, SHARE), pl.ds(SHARE, SHARE))
PLANE = tuple((dy, dx) for dy in range(RING) for dx in range(RING) if dy or dx)
CORNERS = tuple((dy, dx) for dy, dx in PLANE if dy and dx)


class Scatter:
    def __init__(self, comm, part, mid, bufs, fin, outs, send_sems, recv_sems, swap_sems):
        self.pos, self.part, self.mid, self.bufs, self.fin, self.outs = comm.pos, part, mid, bufs, fin, outs
        self.send_sems, self.recv_sems, self.swap_sems = send_sems, recv_sems, swap_sems
        self.near = {(a, hop): comm.far(a, hop) for a in AXES for hop in (1, DUO, TRIO)}
        self.hops = {(a, hop): step(comm.pos, a, hop) for a in AXES for hop in (1, DUO, TRIO)}
        self.peer, self.core = comm.peer(), comm.core
        self.keep, self.give = tile_at(comm.core, SHARE), tile_at(1 - comm.core, SHARE)
        self.drained = set()

    def slot(self, u):
        return COLOR[u], RANK[u] % SLOTS

    def buf(self, u, phase):
        return self.bufs[phase].at[self.slot(u)]

    def view(self, u, phase, hop, half=None):
        order = ORDER[u]
        at = {a: ALL for a in AXES}
        for a in order[1:phase]:
            at[a] = self.pos[a]
        at[order[phase]] = self.hops[order[phase], hop] if hop else self.pos[order[phase]]
        rows = pl.ds(0, CHIP) if half is None else HALVES[half]
        if phase == 0:
            return self.part.at[PLACE[u], at['z'], at['y'], at['x'], rows, :]
        return self.mid.at[self.slot(u) + tuple(at[a] for a in 'zyx' if a != order[0]) + (rows, slice(None))]

    def copy(self, src, dst, sems, device):
        return pltpu.make_async_remote_copy(src_ref=src, dst_ref=dst, send_sem=sems[0], recv_sem=sems[1], device_id=device, device_id_type=MESH)

    def sems(self, u, phase, kind=0):
        at = u * TRIO + phase
        return self.send_sems.at[at], self.recv_sems.at[DUO * at + kind]

    def send(self, u, phase, name):
        axis = ORDER[u][phase]
        if phase == DUO:
            src, to = self.view(u, DUO, name + 1), name + 1
        else:
            hop, half, to = ((DUO, 0, 1), (DUO, 1, TRIO), (1, 1, 1), (TRIO, 0, TRIO), (1, 0, 1), (TRIO, 1, TRIO))[name]
            src = self.view(u, phase, hop, half)
        self.copy(src, self.buf(u, phase).at[name], self.sems(u, phase, int(name > 1 and phase < DUO)), self.near[axis, to]).start()

    def launch(self, u, phase):
        if BEFORE[u] is not None:
            self.drain(BEFORE[u], phase)
        for name in range(RING if phase < DUO else TRIO):
            self.send(u, phase, name)

    def arrived(self, u, phase, first, count):
        whole = self.buf(u, phase).at[pl.ds(first, count)]
        self.copy(whole, whole, self.sems(u, phase, int(first > 0)), self.peer).wait_recv()

    def drain(self, u, phase):
        if (u, phase) not in self.drained:
            self.drained.add((u, phase))
            whole = self.buf(u, phase)
            self.copy(whole, whole, self.sems(u, phase), self.peer).wait_send()

    def out(self, u):
        if u < HEADS:
            out, col = self.outs[0], self.core * HALF + u * LANES
        elif u < 10:
            out, col = self.outs[u - 7], self.core * LANES
        else:
            out, col = self.outs[TRIO], self.core * HALF + (u - 10) * LANES
        return out.at[:, pl.ds(pl.multiple_of(col, LANES), LANES)]

    def kept(self, u):
        return pltpu.make_async_copy(self.fin.at[u, self.keep], self.out(u), self.swap_sems.at[DUO + u])

    def run(self, u, stage):
        if stage == 0:
            return self.launch(u, 0)
        phase = (stage - 1) // DUO
        if stage == LAST:
            self.arrived(u, DUO, 0, TRIO)
            got = self.buf(u, DUO)
            self.fin[u] = self.view(u, DUO, 0)[...] + (got[0] + got[1] + got[DUO])
            self.copy(self.fin.at[u, self.give], self.out(u), (self.swap_sems.at[0], self.swap_sems.at[1]), self.peer).start()
            self.kept(u).start()
            return
        got = self.buf(u, phase)
        if stage % DUO:
            self.arrived(u, phase, 0, DUO)
            for name, hop in ((0, 1), (1, TRIO)):
                add_into(self.view(u, phase, hop, name), got.at[name])
                self.send(u, phase, name + RING)
            return
        self.arrived(u, phase, DUO, RING)
        if phase == 0 and BEFORE[u] is not None:
            self.drain(BEFORE[u], 1)
            self.drain(BEFORE[u], DUO)
        for half, names in ((0, (TRIO, RING)), (1, (DUO, 5))):
            if phase:
                add_into(self.view(u, phase, 0, half), *[got.at[name] for name in names])
            else:
                dst = self.mid.at[self.slot(u) + (ALL, ALL, HALVES[half], slice(None))]
                add_into(dst, self.view(u, 0, 0, half), *[got.at[name] for name in names], fresh=True)
        self.launch(u, phase + 1)

    def finish(self):
        for u in range(N_UNITS):
            for phase in range(TRIO):
                self.drain(u, phase)
        half = self.fin.at[:, pl.ds(0, SHARE)]
        swaps = self.copy(half, half, (self.swap_sems.at[0], self.swap_sems.at[1]), self.peer)
        swaps.wait_send()
        swaps.wait_recv()
        for u in range(N_UNITS):
            self.kept(u).wait()


def attend(heads, qt, do_t, k, kt, v, vt, cos, sin, o_row, ot, dq, dkt, dvt, s_scr, e_scr, p_scr, d_scr):
    f32, bf16 = jnp.float32, jnp.bfloat16
    strip = TURN
    work = [(h, j) for j in range(NBLK) for h in range(len(heads))]

    def strips(c):
        return [(i * strip, slice(c * QB + i * strip, c * QB + (i + 1) * strip)) for i in range(QB // strip)]

    def fold(x, op):
        return op(x.reshape(strip // SUBS, SUBS, QB), axis=0)

    def scores(i):
        (h, j), b = work[i], i % DUO
        q_t = qt[heads[h], j * QB:(j + 1) * QB]
        top = jnp.full((SUBS, QB), -jnp.inf, f32)
        for c in range(j + 1):
            tile = dot(k[c * QB:(c + 1) * QB, :], q_t)
            for at, rows in strips(c):
                s = tile[at:at + strip]
                if c == j:
                    seen = lax.broadcasted_iota(jnp.int32, (strip, QB), 0) + at <= lax.broadcasted_iota(jnp.int32, (strip, QB), 1)
                    s = jnp.where(seen, s, -jnp.inf)
                s_scr[b, rows, :] = s
                top = jnp.maximum(top, fold(s, jnp.max))
        return jnp.max(top, axis=0, keepdims=True)

    def rest(i, m):
        (h, j), b = work[i], i % DUO
        cols, n = slice(j * QB, (j + 1) * QB), (j + 1) * QB
        q_t, d_t = qt[heads[h], cols], do_t[heads[h], cols]
        tot = jnp.zeros((SUBS, QB), f32)
        for c in range(j + 1):
            for at, rows in strips(c):
                e = jnp.exp2((s_scr[b, rows, :] - m) * (SCALE * LOG2E))
                s_scr[b, rows, :] = e
                e_scr[b, rows, :] = e.astype(bf16)
                tot = tot + fold(e, jnp.sum)
        den = jnp.sum(tot, axis=0, keepdims=True)
        inv = 1.0 / den
        o = (dot(vt[:, :n], e_scr[b, :n, :]) / den).astype(bf16)
        ot[o_row(h), cols] = o
        delta = jnp.sum(d_t.astype(f32) * o.astype(f32), axis=0, keepdims=True)
        for c in range(j + 1):
            dp = dot(v[c * QB:(c + 1) * QB, :], d_t)
            for at, rows in strips(c):
                p = s_scr[b, rows, :] * inv
                p_scr[b, rows, :] = p.astype(bf16)
                d_scr[b, rows, :] = (p * (dp[at:at + strip] - delta)).astype(bf16)
        dvt[:, :n] += dot_nt(d_t, p_scr[b, :n, :])
        dkt[:, :n] += dot_nt(q_t, d_scr[b, :n, :])
        g = dot(kt[:, :n], d_scr[b, :n, :]) * SCALE
        co, si = cos[:, cols], sin[:, cols]
        x, y = g[:TURN], g[TURN:]
        dq[heads[h], cols] = jnp.concatenate([x * co + y * si, y * co - x * si], axis=0).astype(bf16)

    m = scores(0)
    for i in range(len(work)):
        later = scores(i + 1) if i + 1 < len(work) else None
        rest(i, m)
        m = later


def tail_kernel(qt, do_t, k, kt, v, vt, rt, dyc, wqk, wqkp, wvo, wvop, gain, hidden, dy, pos, cos, sin,
                result, grad_x, gq, gk, gv, go, gout,
                two, ks, kts, vs, vts, rts, ots, dqo, dqp, dkvo, dkvp, dkt, dvt, s_scr, e_scr, p_scr, d_scr, dycs, part, mid, buf1, buf2, buf3, fin, own, onat, dnat, xs, gacc, gpart, gpeer, gz, gx,
                send_sems, recv_sems, swap_sems, trade_send, trade_recv, local_sems):
    comm = Singles(trade_send, trade_recv, local_sems)
    comm.used = DUO * HEADS
    f32, bf16 = jnp.float32, jnp.bfloat16
    core, peer = comm.core, comm.peer()
    a1, a2 = two.at[0], two.at[1]
    comm.announce(CORNERS)
    sc = Scatter(comm, part, mid, (buf1, buf2, buf3), fin, (gq, gk, gv, go), send_sems, recv_sems, swap_sems)
    plan = Plan()
    some, most = pl.ds(0, PAIR), pl.ds(PAIR, HALF - PAIR)
    loads = [comm.local(s, d) for s, d in ((qt.at[some], two.at[0, some]), (k, ks), (do_t.at[some], two.at[1, some]), (vt, vts), (v, vs), (kt, kts))]
    dkt[...] = jnp.zeros_like(dkt)
    dvt[...] = jnp.zeros_like(dvt)
    with scope('wait_q'):
        for c in loads:
            c.wait()
    loads = [comm.local(s, d) for s, d in ((rt, rts), (qt.at[most], two.at[0, most]), (do_t.at[most], two.at[1, most]))]
    later = [comm.local(s, d) for s, d in ((dyc, dycs), (hidden, xs))]

    def emit(stages):
        for u, stage in stages:
            with scope(f'u{u}_s{stage}'):
                if u == GAIN:
                    sum_gain(stage)
                else:
                    sc.run(u, stage)

    def after(cost):
        plan.now += cost
        return plan.due()

    def head_trades(h):
        row = tile_at(core * HEADS + h, LANES)
        mine = tile_at(h, LANES)
        return [pltpu.make_async_remote_copy(src_ref=s, dst_ref=d, send_sem=trade_send.at[i], recv_sem=trade_recv.at[i], device_id=peer, device_id_type=MESH)
                for s, d, i in ((ots.at[row], ots.at[row], h), (dqo.at[mine], dqp.at[mine], HEADS + h))]

    def gradient(place, count, left, right, mul):
        with scope('grad'):
            @pl.loop(0, DUO)
            def _(z):
                g = mul(left[tile_at(z, HALF), :], right())
                for i in range(count):
                    part[place + i, tile_at(z, DUO)] = g[:, i * LANES:(i + 1) * LANES].reshape(DUO, RING, RING, CHIP, LANES)

    PAIRS = HEADS // DUO
    attended, paired = [], []
    for g in range(PAIRS):
        attended.append(after(5.1))
        plan.now += 1.5
        plan.start(DUO * g)
        plan.start(DUO * g + 1)
        paired.append(plan.due())

    @pl.loop(0, PAIRS)
    def _(g):
        def at(table):
            for i in range(PAIRS):
                if table[i]:
                    pl.when(g == i)(functools.partial(emit, table[i]))

        heads = [tile_at(DUO * g + i, LANES) for i in range(DUO)]
        with scope('attend'):
            attend(heads, a1, a2, ks, kts, vs, vts, cos, sin, lambda i: tile_at(core * HEADS + DUO * g + i, LANES), ots, dqo, dkt, dvt, s_scr, e_scr, p_scr, d_scr)

        @pl.when(g == 0)
        def _():
            with scope('entry'):
                comm.meet(CORNERS)
                for c in loads:
                    c.wait()
        for i in range(DUO):
            for c in head_trades(DUO * g + i):
                c.start()
        at(attended)
        gradient(DUO * g, DUO, rts, lambda: dqo[tile_at(g, PAIR), :], dot_nt)
        at(paired)

    def beat(cost, *starts):
        plan.now += cost
        for u in starts:
            plan.start(u)
        emit(plan.due())

    wkv, wkvp = e_scr.reshape(DIM, PAIR), p_scr.reshape(DIM, PAIR)
    later += [comm.local(src.at[:, pl.ds(at, LANES)], dst.at[:, pl.ds(to, LANES)]) for srcs, dst in (((wqk, wvo), wkv), ((wqkp, wvop), wkvp)) for src, at, to in ((srcs[0], HALF, 0), (srcs[1], 0, LANES))]
    wqp_loads = [comm.local(wqkp.at[tile_at(i, HALF), pl.ds(0, HALF)], two.at[i]) for i in range(DUO)]
    key = dkt[...] * SCALE
    co, si, x, y = cos[...], sin[...], key[:TURN], key[TURN:]
    dkvo[:LANES, :] = jnp.concatenate([x * co + y * si, y * co - x * si], axis=0).astype(bf16)
    dkvo[LANES:, :] = dvt[...].astype(bf16)
    comm.trade(dkvo, dkvp)
    gradient(UNIT_K, DUO, rts, lambda: dkvo[...], dot_nt)
    beat(1.8, UNIT_K, UNIT_V)
    wq_load = comm.local(wqk.at[:, pl.ds(0, HALF)], rts)
    for c in later:
        c.wait()
    with scope('trades'):
        for h in range(HEADS):
            for c in head_trades(h):
                c.wait()

    waiting = list(range(RING))

    def output_gradients(force=False):
        while waiting:
            first = 10 + DUO * waiting[0]
            before = [u for u in range(N_UNITS) if u < first and PLACE[u] in (PLACE[first], PLACE[first + 1])]
            if force:
                emit(plan.rush(lambda: all(map(plan.vacated, before))))
            if not all(map(plan.vacated, before)):
                return
            for u in before:
                sc.drain(u, 0)
            i = waiting.pop(0)
            gradient(PLACE[first], DUO, ots, lambda: dycs[:, i * PAIR:(i + 1) * PAIR], dot)
            plan.start(first)
            plan.start(first + 1)
            beat(1.5)

    def piece(cost):
        beat(cost)
        output_gradients()

    def ticking(n, cost, body):
        tables = [after(cost) for _ in range(n)]

        @pl.loop(0, n)
        def _(i):
            body(i)
            for j, table in enumerate(tables):
                if table:
                    pl.when(i == j)(functools.partial(emit, table))
        output_gradients()

    @pl.loop(0, TOKENS // LANES)
    def _(i):
        want = lax.broadcasted_iota(jnp.int32, (LANES, ROWS), 0) + i * LANES
        own[tile_at(i, LANES), :] = jnp.where(want == pos[...], 1.0, 0.0).astype(bf16)

    def unsort(at, src_t, n):
        with scope('unsort'):
            dnat[at:at + n, :] = dot(src_t[:n, :], own[...]).astype(bf16)

    output_gradients()
    for c in comm.exchanged:
        c.wait_recv()
    unsort(0, dqo, HALF)
    dy_loads = [comm.local(dy.at[:, tile_at(i, HALF)], dqo.at[tile_at(i, ROWS)]) for i in range(DUO)]
    piece(1.2)
    unsort(HALF, dqp, HALF)
    piece(1.2)
    unsort(DUO * HALF, dkvo, PAIR)
    unsort(DUO * HALF + PAIR, dkvp, PAIR)
    piece(0.7)
    wq_load.wait()
    for c in wqp_loads + dy_loads:
        c.wait()
    gacc[...] = jnp.zeros_like(gacc)

    def dr_parts(half, r):
        return [s_scr.at[half, r(i * PAIR), :] for i in range(RING)]

    def back(block, then):
        def dr(half):
            with scope('dr'):
                c = tile_at(half, HALF)
                left = jnp.concatenate([rts[c, :], two[half], wkv[c, :], wkvp[c, :]], axis=1)
                acc = dot(left, dnat[:, block * PAIR:(block + 1) * PAIR])
                for i, ref in enumerate(dr_parts(half, lambda at: pl.ds(at, PAIR))):
                    ref[...] = acc[i * PAIR:(i + 1) * PAIR, :].T

        def norm(part):
            with scope('back'):
                @pl.loop(0, RING)
                def _(i):
                    j = part * RING + i
                    q = pl.ds(pl.multiple_of(block * PAIR + j * SHARE, SHARE), SHARE)
                    d = jnp.concatenate([ref[...] for half in range(DUO) for ref in dr_parts(half, lambda at: pl.ds(pl.multiple_of(at + j * SHARE, SHARE), SHARE))], axis=1)
                    x = xs[q, :].astype(f32)
                    inv = lax.rsqrt(jnp.mean(x * x, axis=-1, keepdims=True) + RMS_EPS)
                    unit = x * inv
                    gacc[...] += jnp.sum((d * unit).reshape(DUO, SUBS, DIM), axis=0)
                    dg = d * gain[0:1, :]
                    new = inv * (dg - unit * jnp.mean(dg * unit, axis=-1, keepdims=True))
                    for half in range(DUO):
                        r = pl.ds(pl.multiple_of(half * ROWS + block * PAIR + j * SHARE, SHARE), SHARE)
                        dqo[r, :] = (dqo[r, :].astype(f32) + new[:, half * HALF:(half + 1) * HALF]).astype(bf16)

        ticking(DUO, 1.6, dr)
        then()
        ticking(RING, 0.92, norm)

    back(0, lambda: None)
    wo_loads = []
    back(1, lambda: wo_loads.extend([comm.local(wvo.at[:, pl.ds(LANES, HALF)], rts)] + [comm.local(wvop.at[tile_at(i, HALF), pl.ds(LANES, HALF)], two.at[i]) for i in range(DUO)]))
    for i in range(DUO):
        comm.store(dqo.at[tile_at(i, ROWS)], grad_x.at[:, tile_at(i, HALF)])
    total = jnp.sum(gacc[...], axis=0, keepdims=True)
    gpart[...] = jnp.zeros_like(gpart)
    for i in range(RING):
        for j in range(RING):
            gpart[i, j:j + 1, :] = total[:, (i * RING + j) * LANES:(i * RING + j + 1) * LANES]

    arrivals = []

    def sum_gain(stage):
        for c in arrivals:
            c.wait_recv()
        del arrivals[:]
        if stage == 0:
            arrivals.append(comm.send(gpart, gpeer, peer))
        elif stage == 1:
            for j in range(RING):
                gz[j] = gpart[j] + gpeer[j]
            arrivals.extend(comm.send(gz.at[step(comm.pos, 'z', hop)], gz.at[TRIO + hop], comm.far('z', hop)) for hop in (1, DUO, TRIO))
        elif stage == DUO:
            gx[0, 0] = (gz[comm.pos['z']] + gz[RING]) + (gz[5] + gz[6])
            for dy, dx in PLANE:
                arrivals.append(comm.send(gx.at[0, 0], gx.at[dy, dx], comm.aside(dy, dx)))
        else:
            gpeer[0] = sum(gx[dy, dx] for dy, dx in PLANE) + gx[0, 0]
            mine = jnp.broadcast_to(gpeer[0, pl.ds(comm.pos['y'], 1), :], (SUBS, LANES))
            gout[...] = pltpu.roll(mine, LANES - (comm.pos['x'] * CHIP + core * SHARE), 1)

    plan.start(GAIN)
    beat(0.2)
    for i in range(DUO):
        with scope('unsort_o'):
            @pl.loop(0, DUO)
            def _(j):
                r = pl.ds(pl.multiple_of(i * HALF + j * ROWS, ROWS), ROWS)
                onat[:, r] = dot(ots[r, :], own[...]).astype(bf16).T
        piece(1.58)
    output_gradients(True)

    def project_out(col, weights, i):
        with scope('project'):
            @pl.loop(DUO * i, DUO * i + DUO)
            def _(j):
                c = tile_at(j, PAIR)
                dst = pl.ds(pl.multiple_of(col + j * PAIR, PAIR), PAIR)
                xs[:, dst] = (xs[:, dst].astype(f32) + dot(onat[...], weights(c))).astype(bf16)
        beat(1.48)

    def own_half(c):
        return rts[:, c]

    def other_half(c):
        return jnp.concatenate([a1[:, c], a2[:, c]], axis=0)

    for c in wo_loads:
        c.wait()
    for col, weights in ((core * HALF, own_half), ((1 - core) * HALF, other_half)):
        for i in range(DUO):
            project_out(col, weights, i)
    comm.store(xs, result)
    emit(plan.rush(lambda: not plan.stage))
    with scope('finish'):
        sc.finish()
        for c in comm.sent + comm.exchanged:
            c.wait_send()
        for c in comm.stored:
            c.wait()


def tail(qt, do_t, k, kt, v, vt, rt, dyc, wqk, wqkp, wvo, wvop, gain, hidden, dy, pos, cos, sin):
    bf16, f32 = jnp.bfloat16, jnp.float32
    any_ = pl.BlockSpec(memory_space=pl.ANY)
    vmem = pl.BlockSpec(memory_space=pltpu.VMEM)
    S = lambda shape, d=bf16: jax.ShapeDtypeStruct(shape, d)
    V = lambda shape, d=bf16: pltpu.VMEM(shape, d)
    D = lambda n: pltpu.SemaphoreType.DMA((n,))
    sq, tall, wide = (HALF, TOKENS), (TOKENS, LANES), (LANES, TOKENS)
    mine, kv = (ROWS, DIM), (PAIR, TOKENS)
    return pl.pallas_call(
        tail_kernel,
        out_shape=[S(mine), S(mine), S((SHARE, DIM), f32), S((SHARE, PAIR), f32), S((SHARE, PAIR), f32), S((SHARE, DIM), f32), S((SUBS, LANES), f32)],
        in_specs=[any_] * 12 + [vmem] + [any_] * DUO + [vmem] * TRIO,
        out_specs=[any_] * 6 + [vmem],
        scratch_shapes=[V((DUO,) + sq), V(tall), V(wide), V(tall), V(wide), V((DIM, TOKENS)), V((DIM, TOKENS)), V(sq), V(sq), V(kv), V(kv), V(wide, f32), V(wide, f32),
                        V((DUO, TOKENS, QB), f32), V((DUO, TOKENS, QB)), V((DUO, TOKENS, QB)), V((DUO, TOKENS, QB)), V(sq), V((PLACES, RING, RING, RING, CHIP, LANES), f32), V((TRIO, SLOTS, RING, RING, CHIP, LANES), f32),
                        V((TRIO, SLOTS, 6, RING, RING, SHARE, LANES), f32), V((TRIO, SLOTS, 6, RING, SHARE, LANES), f32), V((TRIO, SLOTS, TRIO, CHIP, LANES), f32), V((N_UNITS, CHIP, LANES), f32), V((TOKENS, ROWS)), V(mine), V((DUO * QKV, ROWS)), V(mine),
                        V((SUBS, DIM), f32), V((RING, SUBS, LANES), f32), V((RING, SUBS, LANES), f32), V((7, SUBS, LANES), f32), V((RING, RING, SUBS, LANES), f32),
                        D(TRIO * N_UNITS), D(6 * N_UNITS), D(DUO + N_UNITS), D(DUO * HEADS + 20), D(DUO * HEADS + 20), D(CHIP)],
        compiler_params=pltpu.CompilerParams(collective_id=1, has_side_effects=True, vmem_limit_bytes=67043328),
        name='tail',
    )(qt, do_t, k, kt, v, vt, rt, dyc, wqk, wqkp, wvo, wvop, gain, hidden, dy, pos, cos, sin)


def settle_kernel(n, *refs):
    ins, gain, outs, gain_out, bufs, sems = refs[:n], refs[n], refs[n + 1:DUO * n + 1], refs[DUO * n + 1], refs[DUO * n + DUO:-1], refs[-1]
    jobs = []
    for a, o, b in zip(ins, outs, bufs):
        size = a.shape[0] // RING if a.shape[0] == ROWS else a.shape[0]
        jobs += [tuple(r.at[pl.ds(i, size)] for r in (a, b, o)) for i in range(0, a.shape[0], size)]
    takes = [pltpu.make_async_copy(a, b, sems.at[0, i]) for i, (a, b, _) in enumerate(jobs)]
    puts = [pltpu.make_async_copy(b, o, sems.at[1, i]) for i, (_, b, o) in enumerate(jobs)]
    for c in takes:
        c.start()
    gain_out[...] = gain[0:1, :SHARE]
    for take, put in zip(takes, puts):
        take.wait()
        put.start()
    for c in puts:
        c.wait()


def settle(*arrays):
    *large, gain = arrays
    any_, vmem = pl.BlockSpec(memory_space=pl.ANY), pl.BlockSpec(memory_space=pltpu.VMEM)
    return pl.pallas_call(
        functools.partial(settle_kernel, len(large)),
        out_shape=[jax.ShapeDtypeStruct(a.shape, a.dtype) for a in large] + [jax.ShapeDtypeStruct((1, SHARE), gain.dtype)],
        in_specs=[any_] * len(large) + [vmem],
        out_specs=[any_] * len(large) + [vmem],
        scratch_shapes=[pltpu.VMEM(a.shape, a.dtype) for a in large] + [pltpu.SemaphoreType.DMA((DUO, 12))],
        name='settle',
    )(*arrays)


def rope_tables():
    j = np.arange(HEAD_DIM // DUO, dtype=np.float64) / (HEAD_DIM // DUO)
    freq = (ROPE_THETA ** -j).astype(np.float32)
    angle = freq[:, None] * np.arange(TOKENS, dtype=np.float32)[None, :]
    return np.cos(angle.astype(np.float64)).astype(np.float32), np.sin(angle.astype(np.float64)).astype(np.float32)


def solution(mesh):
    def shard_fn(hidden, tok_pos, grad_out, norm_gain, w_query, w_key, w_value, w_out):
        hidden, grad_out = hidden[0], grad_out[0]
        cos_t, sin_t = (jnp.asarray(t) for t in rope_tables())
        *parts, gain = head(hidden, grad_out, w_query, w_key, w_value, w_out, tok_pos, norm_gain.reshape(1, SHARE), cos_t, sin_t)
        parts = [p.reshape(DIM, GROUP) if p.ndim > DUO else p for p in parts]
        result, grad_hidden, gq, gk, gv, go, gout = settle(*tail(*parts, gain, hidden, grad_out, tok_pos, cos_t, sin_t))
        return result[None], grad_hidden[None], gq, gk, gv, go, gout.reshape(SHARE)

    row_spec, pos_spec = P('fsdp', 'cp', None), P('fsdp', 'cp')
    weight_spec, gain_spec = P(('fsdp', 'cp'), None), P(('fsdp', 'cp'))
    return jax.shard_map(shard_fn, mesh=mesh, in_specs=(row_spec, pos_spec, row_spec, gain_spec, weight_spec, weight_spec, weight_spec, weight_spec), out_specs=(row_spec, row_spec, weight_spec, weight_spec, weight_spec, weight_spec, gain_spec), check_vma=False)
```

```python
import functools
import jax
import jax.numpy as jnp
import numpy as np
from jax import lax
from jax.experimental import pallas as pl
from jax.experimental.pallas import tpu as pltpu
from jax.sharding import PartitionSpec as P

LANES, SUBS, RING, TRIO, DUO = 128, 8, 4, 3, 2
PAIR, ROWS, CHIP, SHARE, TURN = 256, 512, 32, 16, 64
HEAD_DIM = LANES
ROPE_THETA = 1000000.0
RMS_EPS = 1e-5
SCALE = HEAD_DIM ** -0.5
LOG2E = 1.4426950408889634

MESH = pl.DeviceIdType.MESH
AXES = ('x', 'y', 'z')
ORDERS = (('x', 'y', 'z'), ('y', 'z', 'x'), ('z', 'x', 'y'))
ALL = pl.ds(0, RING)


def torus():
    f = lax.axis_index('fsdp')
    return {'x': lax.rem(f, RING), 'y': lax.rem(lax.div(f, RING), RING), 'z': lax.div(f, SHARE)}


def step(pos, axis, hop):
    return lax.rem(pos[axis] + hop, RING)


class Batch:
    def __init__(self, comm):
        self.comm, self.index = comm, comm.used
        comm.used += 1

    def _copy(self, src, dst, device):
        send, recv, _ = self.comm.sems
        return pltpu.make_async_remote_copy(src_ref=src, dst_ref=dst, send_sem=send.at[self.index], recv_sem=recv.at[self.index], device_id=device, device_id_type=MESH)

    def send(self, src, dst, device):
        self._copy(src, dst, device).start()
        return self

    def arrived(self, whole):
        self._copy(whole, whole, self.comm.peer()).wait_recv()

    def sent(self, whole):
        self._copy(whole, whole, self.comm.peer()).wait_send()


class Comm:
    def __init__(self, send_sems, recv_sems, local_sems):
        self.pos = torus()
        self.core = lax.axis_index('cp')
        self.sems = (send_sems, recv_sems, local_sems)
        self.used = self.used_local = 0
        self.stored = []

    def far(self, axis, hop):
        p = dict(self.pos)
        p[axis] = step(self.pos, axis, hop)
        return {'fsdp': (p['z'] * RING + p['y']) * RING + p['x'], 'cp': self.core}

    def peer(self):
        return {'fsdp': lax.axis_index('fsdp'), 'cp': 1 - self.core}

    def aside(self, dy, dx):
        return {'fsdp': (self.pos['z'] * RING + step(self.pos, 'y', dy)) * RING + step(self.pos, 'x', dx), 'cp': self.core}

    def announce(self, corners=()):
        sem = pltpu.get_barrier_semaphore()
        for axis in AXES:
            for hop in (1, DUO, TRIO):
                pl.semaphore_signal(sem, inc=1, device_id=self.far(axis, hop), device_id_type=MESH)
        for dy, dx in corners:
            pl.semaphore_signal(sem, inc=1, device_id=self.aside(dy, dx), device_id_type=MESH)
        pl.semaphore_signal(sem, inc=1, device_id=self.peer(), device_id_type=MESH)

    def meet(self, corners=()):
        pl.semaphore_wait(pltpu.get_barrier_semaphore(), 10 + len(corners))

    def ring(self, batch, src, slots, axis):
        for hop in (1, DUO, TRIO):
            batch.send(src, slots.at[hop], self.far(axis, hop))

    def local(self, src, dst):
        i = self.used_local
        self.used_local += 1
        c = pltpu.make_async_copy(src, dst, self.sems[DUO].at[i])
        c.start()
        return c

    def store(self, src, dst):
        self.stored.append(self.local(src, dst))


class Singles(Comm):
    def __init__(self, *sems):
        super().__init__(*sems)
        self.sent, self.exchanged = [], []

    def _copy(self, src, dst, device):
        i = self.used
        self.used += 1
        c = pltpu.make_async_remote_copy(src_ref=src, dst_ref=dst, send_sem=self.sems[0].at[i], recv_sem=self.sems[1].at[i], device_id=device, device_id_type=MESH)
        c.start()
        return c

    def send(self, src, dst, device):
        c = self._copy(src, dst, device)
        self.sent.append(c)
        return c

    def trade(self, src, dst):
        self.exchanged.append(self._copy(src, dst, self.peer()))


def pick(ref, sel, piece):
    lo, cols, first, rows = piece
    return ref.at[sel['z'], sel['y'], sel['x'], pl.ds(first, rows), pl.ds(lo, cols)]


def sem_scratch(remote, local):
    return [pltpu.SemaphoreType.DMA((remote,)), pltpu.SemaphoreType.DMA((remote,)), pltpu.SemaphoreType.DMA((local,))]


def add_into(dst, *srcs, fresh=False):
    def add(idx):
        total, *rest = [s[idx] for s in (srcs if fresh else (dst,) + srcs)]
        for more in rest:
            total = total + more
        dst[idx] = total

    if len(dst.shape) > TRIO:
        @pl.loop(0, dst.shape[0])
        def _(i):
            add((i,))
    else:
        add(Ellipsis)


def columns(lo, na, nb):
    return (lo, na, 0, CHIP), (lo + na, nb, 0, CHIP)


def strip(lo):
    return (lo, LANES, 0, SHARE), (lo, LANES, SHARE, SHARE)


QK_COLORS = (columns(0, PAIR, LANES), columns(384, LANES, PAIR), columns(768, PAIR, LANES))
VO_COLORS = (columns(0, LANES, PAIR), columns(384, PAIR, LANES), columns(768, LANES, PAIR))
QK_FIRST = (columns(0, LANES, LANES), columns(384, LANES, LANES), columns(768, LANES, LANES))
QK_LAST = (strip(PAIR), strip(640), strip(1024))
TOKENS = 1024
DIM = 2048
HALF = 1024
QKV = 1280
GROUP = 1152


def scope(name):
    return jax.named_scope(name)


def dot(a, b):
    return jnp.dot(a, b, preferred_element_type=jnp.float32)


def dot_nt(a, b):
    return lax.dot_general(a, b, (((1,), (1,)), ((), ())), preferred_element_type=jnp.float32)


def tile_at(i, n):
    return pl.ds(pl.multiple_of(i * n, n), n)


class Gather:
    def __init__(self, comm, ref, colors, land, held=None):
        self.comm, self.ref, self.colors, self.land = comm, ref, colors, land
        self.held = list(held or [dict(comm.pos) for _ in colors])
        self.batches = []

    def move(self, batch, s, piece, to):
        batch.send(pick(self.ref, s, piece), pick(self.ref, s, piece), to)

    def at(self, k, hop):
        d = ORDERS[k][self.phase]
        return dict(self.held[k], **{d: step(self.comm.pos, d, hop)})

    def begin(self, phase):
        self.phase = phase
        self.up, self.dn, self.rest = ([Batch(self.comm) for _ in range(TRIO)] for _ in range(TRIO))
        self.batches += self.up + self.dn + self.rest
        for k, (a, b) in enumerate(self.colors):
            d = ORDERS[k][phase]
            up, dn, s = self.comm.far(d, 1), self.comm.far(d, TRIO), self.held[k]
            self.move(self.up[k], s, a, up)
            self.move(self.dn[k], s, b, dn)
            self.move(self.rest[k], s, b, up)
            self.move(self.rest[k], s, a, dn)
            if phase == 0:
                for piece in (a, b):
                    self.move(self.rest[k], s, piece, self.comm.far(d, DUO))
        if phase == DUO:
            for k, pieces in enumerate(self.colors):
                for piece in pieces:
                    self.land(self.ref, self.held[k], piece)

    def forward(self):
        for k, (a, b) in enumerate(self.colors):
            d = ORDERS[k][self.phase]
            for batch, hop, piece, to in ((self.up[k], TRIO, a, 1), (self.dn[k], 1, b, TRIO)):
                s = self.at(k, hop)
                batch.arrived(pick(self.ref, s, piece))
                if self.phase:
                    self.move(self.rest[k], s, piece, self.comm.far(d, to))
                if self.phase == DUO:
                    self.land(self.ref, s, piece)

    def end(self):
        for k, (a, b) in enumerate(self.colors):
            d = ORDERS[k][self.phase]
            two = dict(self.held[k], **{d: pl.ds(0, DUO)})
            both = (a[0], max(a[0] + a[1], b[0] + b[1]) - a[0], 0, CHIP)
            self.rest[k].arrived(pick(self.ref, two, both))
            if self.phase == DUO:
                for hop, piece in ((TRIO, b), (1, a), (DUO, a), (DUO, b)):
                    self.land(self.ref, self.at(k, hop), piece)
            for batch, s, piece in ((self.up[k], self.held[k], a), (self.dn[k], self.held[k], b), (self.rest[k], two, both)):
                batch.spent = pick(self.ref, s, piece)
            self.held[k] = dict(self.held[k], **{d: ALL})

    def finish(self):
        for batch in self.batches:
            batch.sent(batch.spent)


def head_kernel(hidden, dy, wq, wk, wv, wo, pos, gain_in, cos_t, sin_t,
                qt_o, dot_o, k_o, kt_o, v_o, vt_o, rt_o, dyc_o, wqk_o, wqkp_o, wvo_o, wvop_o, gain_o,
                hid2, dy2, dys, rs, rt, wqk, wvo, wpeer, pi, pos2, qt, dot_s, kk, kt, vv, vt, gain, gtile, gbuf, gx, gy, gz, *sems):
    comm = Comm(*sems)
    pos_c, core = comm.pos, comm.core
    bf16, f32 = jnp.bfloat16, jnp.float32
    peer = comm.peer()
    rows = tile_at(core, SHARE)
    mine_qk = wqk.at[pos_c['z'], pos_c['y'], pos_c['x'], rows]
    mine_vo = wvo.at[pos_c['z'], pos_c['y'], pos_c['x'], rows]

    def weight_parts(c):
        return ((wq.at[:, tile_at(c, HALF)], mine_qk.at[:, pl.ds(0, HALF)]), (wk.at[:, tile_at(c, LANES)], mine_qk.at[:, pl.ds(HALF, LANES)]),
                (wv.at[:, tile_at(c, LANES)], mine_vo.at[:, pl.ds(0, LANES)]), (wo.at[:, tile_at(c, HALF)], mine_vo.at[:, pl.ds(LANES, HALF)]))

    loads = [comm.local(s, d) for s, d in weight_parts(core)]
    load_x = [comm.local(hidden, hid2.at[pl.ds(0, ROWS)]), comm.local(dy, dy2.at[pl.ds(0, ROWS)])]
    share = lax.broadcasted_iota(jnp.int32, (SUBS, LANES), 1) // SHARE
    gtile[...] = jnp.where(share == pos_c['x'] * DUO + core, jnp.broadcast_to(jnp.concatenate([gain_in[...]] * SUBS, axis=1), (SUBS, LANES)), 0.0)
    comm.announce()
    with scope('entry'):
        comm.meet()
    swap_w, swap_pos, swap_dy, swap_x, peers_qk, peers_vo = (Batch(comm) for _ in range(6))
    gain_c, gain_x, gain_y, gain_z = (Batch(comm) for _ in range(RING))
    for s, d in weight_parts(1 - core):
        swap_w.send(s, d, peer)
    gain_c.send(gtile, gbuf, peer)
    swap_pos.send(pos, pos2, peer)
    for c in loads:
        c.wait()
    with scope('wait_w'):
        swapped = wqk.at[pos_c['z'], pos_c['y'], pos_c['x']]
        swap_w.arrived(swapped)

    def land_qk(ref, s, cols):
        peers_qk.send(pick(ref, s, cols), pick(wqkp_o, s, cols), peer)

    def land_vo(ref, s, cols):
        peers_vo.send(pick(ref, s, cols), pick(wpeer, s, cols), peer)

    g1 = Gather(comm, wvo, VO_COLORS, land_vo)
    g2 = Gather(comm, wqk, QK_COLORS, land_qk)
    g1.begin(0)
    g2.begin(0)
    gain_c.arrived(gbuf)
    gx[0] = gtile[...] + gbuf[...]
    comm.ring(gain_x, gx.at[0], gx, 'x')

    swap_pos.arrived(pos2)

    @pl.loop(0, TOKENS // LANES)
    def _(i):
        want = lax.broadcasted_iota(jnp.int32, (LANES, ROWS), 0) + i * LANES
        for h, have in enumerate((pos, pos2)):
            pi[tile_at(i, LANES), h * ROWS:(h + 1) * ROWS] = jnp.where(want == have[...], 1.0, 0.0).astype(bf16)

    def sort(dst, src, first, last):
        with scope('sort'):
            @pl.loop(first, last)
            def _(j):
                c = tile_at(j, PAIR)
                dst[:, c] = dot(pi[...], src[:, c]).astype(bf16)

    swap_dy.send(dy, dy2.at[pl.ds(ROWS, ROWS)], peer)
    with scope('p0_end'):
        for g in (g1, g2):
            g.forward()
            g.end()
            g.begin(1)
    swap_x.send(hidden, hid2.at[pl.ds(ROWS, ROWS)], peer)
    gain_x.arrived(gx.at[pl.ds(1, TRIO)])
    gy[pos_c['y']] = (gx[0] + gx[1]) + (gx[DUO] + gx[TRIO])
    for hop in (1, DUO, TRIO):
        gain_y.send(gy.at[pos_c['y']], gy.at[pos_c['y']], comm.far('y', hop))
    with scope('wait_dy'):
        load_x[1].wait()
        swap_dy.arrived(dy2.at[pl.ds(ROWS, ROWS)])
    sort(dys, dy2, 0, RING)
    with scope('p1a_fwd'):
        g1.forward()
    sort(dys, dy2, RING, 6)
    with scope('p1b_fwd'):
        g2.forward()
    sort(dys, dy2, 6, SUBS)
    with scope('p1a_end'):
        g1.end()
    gain_y.arrived(gy.at[pl.ds(1, TRIO)])
    for j in range(RING):
        gz[pos_c['z'], j] = gy[j]
    for hop in (1, DUO, TRIO):
        gain_z.send(gz.at[pos_c['z']], gz.at[pos_c['z']], comm.far('z', hop))
    g1.begin(DUO)
    comm.store(dys.at[:, tile_at(core, HALF)], dyc_o)
    with scope('p1b_end'):
        g2.end()
    with scope('wait_x'):
        load_x[0].wait()
        swap_x.arrived(hid2.at[pl.ds(ROWS, ROWS)])
    sort(rs, hid2, 0, SUBS)
    with scope('p2q_fwd'):
        g1.forward()
    g2a, g2b = (Gather(comm, wqk, colors, land_qk, g2.held) for colors in (QK_FIRST, QK_LAST))
    g2a.begin(DUO)
    with scope('gain'):
        gain_z.arrived(gz.at[pl.ds(1, TRIO)])
    for i in range(RING):
        for j in range(RING):
            gain[:, (i * RING + j) * LANES:(i * RING + j + 1) * LANES] = gz[i, j]
    comm.store(gain, gain_o)

    def norm(first, last):
        with scope('norm'):
            @pl.loop(first, last)
            def _(i):
                r = tile_at(i, CHIP)
                x = rs[r, :].astype(f32)
                inv = lax.rsqrt(jnp.mean(x * x, axis=-1, keepdims=True) + RMS_EPS)
                rs[r, :] = (x * inv * gain[0:1, :]).astype(bf16)

    norm(0, TOKENS // CHIP)
    with scope('r_t'):
        @pl.loop(0, DIM // PAIR)
        def _(i):
            c = tile_at(i, PAIR)

            @pl.loop(0, TOKENS // PAIR)
            def _(j):
                r = tile_at(j, PAIR)
                rt[c, r] = rs[r, c].T
    comm.store(rt, rt_o)
    with scope('p2o_end'):
        g1.end()
    w_qk, w_vo, w_peer = wqk.reshape(DIM, GROUP), wvo.reshape(DIM, GROUP), wpeer.reshape(DIM, GROUP)
    with scope('vals'):
        @pl.loop(0, DUO)
        def _(i):
            r = tile_at(i, ROWS)
            val = dot(rs[r, :], w_vo[:, :LANES]).astype(bf16)
            vv[r, :] = val
            vt[:, r] = val.T
    for src, dst in ((wvo, wvo_o), (vv, v_o), (vt, vt_o)):
        comm.store(src, dst)
    with scope('p2q_fwd'):
        g2a.forward()
    g2b.begin(DUO)
    with scope('wo_peer'):
        peers_vo.arrived(wpeer)
    comm.store(wpeer, wvop_o)
    with scope('do_t'):
        mine = tile_at(core, HALF)

        @pl.loop(0, TOKENS // PAIR)
        def _(j):
            t = tile_at(j, PAIR)
            w_rows = jnp.concatenate([w_vo[mine, LANES:], w_peer[mine, LANES:]], axis=1)
            d_rows = jnp.concatenate([dys[t, mine], dys[t, tile_at(1 - core, HALF)]], axis=1)
            dot_s[:, t] = dot_nt(w_rows, d_rows).astype(bf16)
    comm.store(dot_s, dot_o)

    def rotated(x, r):
        cos, sin = cos_t[:, r], sin_t[:, r]
        cos = jnp.concatenate([cos, cos], axis=0).T
        sin = jnp.concatenate([-sin, sin], axis=0).T
        return (x * cos + pltpu.roll(x, TURN, 1) * sin).astype(bf16)

    def queries(columns, heads):
        x = dot(rs[...], columns)
        for i in range(RING):
            r = slice(i * PAIR, (i + 1) * PAIR)
            for h, head in enumerate(heads):
                qt[tile_at(head, LANES), r] = rotated(x[r, h * LANES:(h + 1) * LANES], r).T

    with scope('p2q_end'):
        g2a.end()

    def pairs(first, last):
        with scope('q'):
            @pl.loop(first, last)
            def _(t):
                queries(w_qk[:, pl.ds(pl.multiple_of(t * 384, LANES), PAIR)], (TRIO * t, TRIO * t + 1))

    pairs(0, 1)
    with scope('last_fwd'):
        g2b.forward()
    pairs(1, TRIO)
    with scope('last_end'):
        g2b.end()
    comm.store(wqk, wqk_o)
    with scope('q_last'):
        queries(jnp.concatenate([w_qk[:, PAIR:384], w_qk[:, 640:768]], axis=1), (DUO, 5))
    comm.store(qt, qt_o)
    with scope('keys'):
        @pl.loop(0, DUO)
        def _(i):
            r = tile_at(i, ROWS)
            key = rotated(dot(rs[r, :], w_qk[:, HALF:]), r)
            kk[r, :] = key
            kt[:, r] = key.T
    for src, dst in ((kk, k_o), (kt, kt_o)):
        comm.store(src, dst)
    with scope('finish'):
        peers_qk.arrived(wqk)
        for batch, whole in ((swap_w, swapped), (swap_pos, pos2), (swap_dy, dy2.at[pl.ds(ROWS, ROWS)]), (swap_x, hid2.at[pl.ds(ROWS, ROWS)]), (peers_qk, wqk), (peers_vo, wvo),
                             (gain_c, gbuf), (gain_x, gx.at[pl.ds(1, TRIO)]), (gain_y, gy.at[pl.ds(1, TRIO)]), (gain_z, gz.at[pl.ds(1, TRIO)])):
            batch.sent(whole)
        for g in (g1, g2, g2a, g2b):
            g.finish()
        for c in comm.stored:
            c.wait()


def head(hidden, dy, wq, wk, wv, wo, pos, gain, cos_t, sin_t):
    bf16, f32 = jnp.bfloat16, jnp.float32
    any_ = pl.BlockSpec(memory_space=pl.ANY)
    vmem = pl.BlockSpec(memory_space=pltpu.VMEM)
    S = lambda shape, d=bf16: jax.ShapeDtypeStruct(shape, d)
    V = lambda shape, d=bf16: pltpu.VMEM(shape, d)
    group = (RING, RING, RING, CHIP, GROUP)
    sq, tall, wide = (HALF, TOKENS), (TOKENS, LANES), (LANES, TOKENS)
    full = (TOKENS, DIM)
    return pl.pallas_call(
        head_kernel,
        out_shape=[S(sq), S(sq), S(tall), S(wide), S(tall), S(wide), S((DIM, TOKENS)), S((TOKENS, HALF)), S(group), S(group), S(group), S(group), S((SUBS, DIM), f32)],
        in_specs=[any_] * 6 + [vmem] * RING,
        out_specs=[any_] * 13,
        scratch_shapes=[V(full), V(full), V(full), V(full), V((DIM, TOKENS)), V(group), V(group), V(group), V((TOKENS, TOKENS)), V((1, ROWS), jnp.int32),
                        V(sq), V(sq), V(tall), V(wide), V(tall), V(wide), V((SUBS, DIM), f32), V((SUBS, LANES), f32), V((SUBS, LANES), f32), V((RING, SUBS, LANES), f32), V((RING, SUBS, LANES), f32), V((RING, RING, SUBS, LANES), f32)] + sem_scratch(73, 18),
        compiler_params=pltpu.CompilerParams(collective_id=0, has_side_effects=True, vmem_limit_bytes=60 * DUO**20),
        name='head',
    )(hidden, dy, wq, wk, wv, wo, pos, gain, cos_t, sin_t)


HEADS = SUBS
UNIT_K, UNIT_V = SUBS, 9
N_UNITS = 18
GAIN = N_UNITS
SLOTS = RING
LAST = 5
ABREAST = DUO
LINES = ((0, TRIO, 6, 9, 12, 15), (1, RING, 7, 10, 13, SHARE), (DUO, 5, SUBS, 11, 14, 17))
COLOR = {u: k for k, line in enumerate(LINES) for u in line}
RANK = {u: i for line in LINES for i, u in enumerate(line)}
SWAPPED = (1, TRIO, RING, SUBS, 10)
ORDER = {u: ORDERS[k] if u not in SWAPPED else (ORDERS[k][0], ORDERS[k][DUO], ORDERS[k][1]) for u, k in COLOR.items()}
BEFORE = {u: line[i - SLOTS] if i >= SLOTS else None for line in LINES for i, u in enumerate(line)}
PLACES = 12
PLACE = {u: u % PLACES for u in range(N_UNITS)}
WIRE = (2.82, 0.71, 0.36)
LATENCY = 2.4
STAGE_COST = 0.08


class Plan:
    def __init__(self):
        self.now, self.stage, self.ready, self.order, self.link = 0.0, {}, {}, [], {}
        self.mark = {}

    def _wire(self, u, phase, count):
        link = ORDER[u][phase]
        t = max(self.link.get(link, 0.0), self.now)
        first = t + WIRE[phase] + LATENCY
        self.link[link] = t + WIRE[phase] * count
        return first if phase < DUO else self.link[link] + LATENCY

    def free(self, u, phase):
        if BEFORE[u] is None:
            return True
        done = self.mark.get((BEFORE[u], (DUO, RING, 5)[phase]))
        if done is None:
            return False
        sent = ((0, 1), (DUO, TRIO), (RING,))[phase]
        return any(self.mark.get((j, s), -1) > done and (j, s + 1) in self.mark for j, order in ORDER.items() if order[phase] == ORDER[u][phase] for s in sent)

    def run(self, u):
        stage = self.stage[u]
        self.order.append((u, stage))
        self.mark[u, stage] = len(self.order)
        self.now = max(self.now, self.ready[u]) + STAGE_COST
        self.stage[u] = stage + 1
        if stage == (TRIO if u == GAIN else LAST):
            del self.stage[u]
        elif u == GAIN:
            self.ready[u] = max([self.now] + [self.link.get(a, 0.0) for a in ('', 'z', 'xy')[stage]]) + DUO * LATENCY
        elif stage % DUO:
            self.ready[u] = self._wire(u, stage // DUO, 1)
        else:
            self.ready[u] = self._wire(u, stage // DUO, DUO)

    def blocked(self, u):
        stage = self.stage[u]
        if u == GAIN:
            return False
        if stage == 0 and sum(0 < self.stage.get(j, 0) <= DUO for j in LINES[COLOR[u]]) >= ABREAST:
            return True
        if stage == DUO and BEFORE[u] is not None and (BEFORE[u], LAST) not in self.mark:
            return True
        return stage in (0, DUO, RING) and not self.free(u, stage // DUO)

    def start(self, u):
        self.stage[u], self.ready[u] = 0, self.now

    def due(self):
        first = len(self.order)
        while True:
            ripe = [(self.ready[u], u) for u in self.stage if self.ready[u] <= self.now and not self.blocked(u)]
            if not ripe:
                return self.order[first:]
            self.run(min(ripe)[1])

    def vacated(self, u):
        return (u, DUO) in self.mark

    def rush(self, done):
        first = len(self.order)
        while not done():
            self.run(min((self.ready[u], u) for u in self.stage if not self.blocked(u))[1])
        return self.order[first:]


QB = PAIR
NBLK = TOKENS // QB
HALVES = (pl.ds(0, SHARE), pl.ds(SHARE, SHARE))
PLANE = tuple((dy, dx) for dy in range(RING) for dx in range(RING) if dy or dx)
CORNERS = tuple((dy, dx) for dy, dx in PLANE if dy and dx)


class Scatter:
    def __init__(self, comm, part, mid, bufs, fin, outs, send_sems, recv_sems, swap_sems):
        self.pos, self.part, self.mid, self.bufs, self.fin, self.outs = comm.pos, part, mid, bufs, fin, outs
        self.send_sems, self.recv_sems, self.swap_sems = send_sems, recv_sems, swap_sems
        self.near = {(a, hop): comm.far(a, hop) for a in AXES for hop in (1, DUO, TRIO)}
        self.hops = {(a, hop): step(comm.pos, a, hop) for a in AXES for hop in (1, DUO, TRIO)}
        self.peer, self.core = comm.peer(), comm.core
        self.keep, self.give = tile_at(comm.core, SHARE), tile_at(1 - comm.core, SHARE)
        self.drained = set()

    def slot(self, u):
        return COLOR[u], RANK[u] % SLOTS

    def buf(self, u, phase):
        return self.bufs[phase].at[self.slot(u)]

    def view(self, u, phase, hop, half=None):
        order = ORDER[u]
        at = {a: ALL for a in AXES}
        for a in order[1:phase]:
            at[a] = self.pos[a]
        at[order[phase]] = self.hops[order[phase], hop] if hop else self.pos[order[phase]]
        rows = pl.ds(0, CHIP) if half is None else HALVES[half]
        if phase == 0:
            return self.part.at[PLACE[u], at['z'], at['y'], at['x'], rows, :]
        return self.mid.at[self.slot(u) + tuple(at[a] for a in 'zyx' if a != order[0]) + (rows, slice(None))]

    def copy(self, src, dst, sems, device):
        return pltpu.make_async_remote_copy(src_ref=src, dst_ref=dst, send_sem=sems[0], recv_sem=sems[1], device_id=device, device_id_type=MESH)

    def sems(self, u, phase, kind=0):
        k, i = self.slot(u)
        at = (k * SLOTS + i) * TRIO + phase
        return self.send_sems.at[at], self.recv_sems.at[DUO * at + kind]

    def send(self, u, phase, name):
        axis = ORDER[u][phase]
        if phase == DUO:
            src, to = self.view(u, DUO, name + 1), name + 1
        else:
            hop, half, to = ((DUO, 0, 1), (DUO, 1, TRIO), (1, 1, 1), (TRIO, 0, TRIO), (1, 0, 1), (TRIO, 1, TRIO))[name]
            src = self.view(u, phase, hop, half)
        self.copy(src, self.buf(u, phase).at[name], self.sems(u, phase, int(name > 1 and phase < DUO)), self.near[axis, to]).start()

    def launch(self, u, phase):
        if BEFORE[u] is not None:
            self.drain(BEFORE[u], phase)
        for name in range(RING if phase < DUO else TRIO):
            self.send(u, phase, name)

    def arrived(self, u, phase, first, count):
        whole = self.buf(u, phase).at[pl.ds(first, count)]
        self.copy(whole, whole, self.sems(u, phase, int(first > 0)), self.peer).wait_recv()

    def drain(self, u, phase):
        if (u, phase) not in self.drained:
            self.drained.add((u, phase))
            whole = self.buf(u, phase)
            self.copy(whole, whole, self.sems(u, phase), self.peer).wait_send()

    def out(self, u):
        if u < HEADS:
            out, col = self.outs[0], self.core * HALF + u * LANES
        elif u < 10:
            out, col = self.outs[u - 7], self.core * LANES
        else:
            out, col = self.outs[TRIO], self.core * HALF + (u - 10) * LANES
        return out.at[:, pl.ds(pl.multiple_of(col, LANES), LANES)]

    def kept(self, u):
        return pltpu.make_async_copy(self.fin.at[u, self.keep], self.out(u), self.swap_sems.at[DUO + u])

    def run(self, u, stage):
        if stage == 0:
            return self.launch(u, 0)
        phase = (stage - 1) // DUO
        if stage == LAST:
            self.arrived(u, DUO, 0, TRIO)
            got = self.buf(u, DUO)
            self.fin[u] = self.view(u, DUO, 0)[...] + (got[0] + got[1] + got[DUO])
            self.copy(self.fin.at[u, self.give], self.out(u), (self.swap_sems.at[0], self.swap_sems.at[1]), self.peer).start()
            self.kept(u).start()
            return
        got = self.buf(u, phase)
        if stage % DUO:
            self.arrived(u, phase, 0, DUO)
            for name, hop in ((0, 1), (1, TRIO)):
                add_into(self.view(u, phase, hop, name), got.at[name])
                self.send(u, phase, name + RING)
            return
        self.arrived(u, phase, DUO, RING)
        if phase == 0 and BEFORE[u] is not None:
            self.drain(BEFORE[u], 1)
            self.drain(BEFORE[u], DUO)
        for half, names in ((0, (TRIO, RING)), (1, (DUO, 5))):
            if phase:
                add_into(self.view(u, phase, 0, half), *[got.at[name] for name in names])
            else:
                dst = self.mid.at[self.slot(u) + (ALL, ALL, HALVES[half], slice(None))]
                add_into(dst, self.view(u, 0, 0, half), *[got.at[name] for name in names], fresh=True)
        self.launch(u, phase + 1)

    def finish(self):
        for u in range(N_UNITS):
            for phase in range(TRIO):
                self.drain(u, phase)
        half = self.fin.at[:, pl.ds(0, SHARE)]
        swaps = self.copy(half, half, (self.swap_sems.at[0], self.swap_sems.at[1]), self.peer)
        swaps.wait_send()
        swaps.wait_recv()
        for u in range(N_UNITS):
            self.kept(u).wait()


def attend(heads, qt, do_t, k, kt, v, vt, cos, sin, o_row, ot, dq, dkt, dvt, s_scr, e_scr, p_scr, d_scr):
    f32, bf16 = jnp.float32, jnp.bfloat16
    strip = TURN
    work = [(h, j) for j in range(NBLK) for h in range(len(heads))]

    def strips(c):
        return [(i * strip, slice(c * QB + i * strip, c * QB + (i + 1) * strip)) for i in range(QB // strip)]

    def fold(x, op):
        return op(x.reshape(strip // SUBS, SUBS, QB), axis=0)

    def scores(i):
        (h, j), b = work[i], i % DUO
        q_t = qt[heads[h], j * QB:(j + 1) * QB]
        top = jnp.full((SUBS, QB), -jnp.inf, f32)
        for c in range(j + 1):
            tile = dot(k[c * QB:(c + 1) * QB, :], q_t)
            for at, rows in strips(c):
                s = tile[at:at + strip]
                if c == j:
                    seen = lax.broadcasted_iota(jnp.int32, (strip, QB), 0) + at <= lax.broadcasted_iota(jnp.int32, (strip, QB), 1)
                    s = jnp.where(seen, s, -jnp.inf)
                s_scr[b, rows, :] = s
                top = jnp.maximum(top, fold(s, jnp.max))
        return jnp.max(top, axis=0, keepdims=True)

    def rest(i, m):
        (h, j), b = work[i], i % DUO
        cols, n = slice(j * QB, (j + 1) * QB), (j + 1) * QB
        q_t, d_t = qt[heads[h], cols], do_t[heads[h], cols]
        tot = jnp.zeros((SUBS, QB), f32)
        for c in range(j + 1):
            for at, rows in strips(c):
                e = jnp.exp2((s_scr[b, rows, :] - m) * (SCALE * LOG2E))
                s_scr[b, rows, :] = e
                e_scr[b, rows, :] = e.astype(bf16)
                tot = tot + fold(e, jnp.sum)
        den = jnp.sum(tot, axis=0, keepdims=True)
        inv = 1.0 / den
        o = (dot(vt[:, :n], e_scr[b, :n, :]) / den).astype(bf16)
        ot[o_row(h), cols] = o
        delta = jnp.sum(d_t.astype(f32) * o.astype(f32), axis=0, keepdims=True)
        for c in range(j + 1):
            dp = dot(v[c * QB:(c + 1) * QB, :], d_t)
            for at, rows in strips(c):
                p = s_scr[b, rows, :] * inv
                p_scr[b, rows, :] = p.astype(bf16)
                d_scr[b, rows, :] = (p * (dp[at:at + strip] - delta)).astype(bf16)
        dvt[:, :n] += dot_nt(d_t, p_scr[b, :n, :])
        dkt[:, :n] += dot_nt(q_t, d_scr[b, :n, :])
        g = dot(kt[:, :n], d_scr[b, :n, :]) * SCALE
        co, si = cos[:, cols], sin[:, cols]
        x, y = g[:TURN], g[TURN:]
        dq[heads[h], cols] = jnp.concatenate([x * co + y * si, y * co - x * si], axis=0).astype(bf16)

    m = scores(0)
    for i in range(len(work)):
        later = scores(i + 1) if i + 1 < len(work) else None
        rest(i, m)
        m = later


def tail_kernel(qt, do_t, k, kt, v, vt, rt, dyc, wqk, wqkp, wvo, wvop, gain, hidden, dy, pos, cos, sin,
                result, grad_x, gq, gk, gv, go, gout,
                two, ks, kts, vs, vts, rts, ots, dqo, dqp, dkvo, dkvp, dkt, dvt, s_scr, e_scr, p_scr, d_scr, dycs, part, mid, buf1, buf2, buf3, fin, own, onat, dnat, xs, gacc, gpart, gpeer, gz, gx,
                send_sems, recv_sems, swap_sems, trade_send, trade_recv, local_sems):
    comm = Singles(trade_send, trade_recv, local_sems)
    comm.used = DUO * HEADS
    f32, bf16 = jnp.float32, jnp.bfloat16
    core, peer = comm.core, comm.peer()
    a1, a2 = two.at[0], two.at[1]
    comm.announce(CORNERS)
    sc = Scatter(comm, part, mid, (buf1, buf2, buf3), fin, (gq, gk, gv, go), send_sems, recv_sems, swap_sems)
    plan = Plan()
    some, most = pl.ds(0, PAIR), pl.ds(PAIR, HALF - PAIR)
    loads = [comm.local(s, d) for s, d in ((qt.at[some], two.at[0, some]), (k, ks), (do_t.at[some], two.at[1, some]), (vt, vts), (v, vs), (kt, kts))]
    dkt[...] = jnp.zeros_like(dkt)
    dvt[...] = jnp.zeros_like(dvt)
    with scope('wait_q'):
        for c in loads:
            c.wait()
    loads = [comm.local(s, d) for s, d in ((rt, rts), (qt.at[most], two.at[0, most]), (do_t.at[most], two.at[1, most]))]
    later = [comm.local(s, d) for s, d in ((dyc, dycs), (hidden, xs))]

    def emit(stages):
        for u, stage in stages:
            with scope(f'u{u}_s{stage}'):
                if u == GAIN:
                    sum_gain(stage)
                else:
                    sc.run(u, stage)

    def after(cost):
        plan.now += cost
        return plan.due()

    def head_trades(h):
        row = tile_at(core * HEADS + h, LANES)
        mine = tile_at(h, LANES)
        return [pltpu.make_async_remote_copy(src_ref=s, dst_ref=d, send_sem=trade_send.at[i], recv_sem=trade_recv.at[i], device_id=peer, device_id_type=MESH)
                for s, d, i in ((ots.at[row], ots.at[row], h), (dqo.at[mine], dqp.at[mine], HEADS + h))]

    def gradient(place, count, left, right, mul):
        with scope('grad'):
            @pl.loop(0, DUO)
            def _(z):
                g = mul(left[tile_at(z, HALF), :], right())
                for i in range(count):
                    part[place + i, tile_at(z, DUO)] = g[:, i * LANES:(i + 1) * LANES].reshape(DUO, RING, RING, CHIP, LANES)

    PAIRS = HEADS // DUO
    attended, paired = [], []
    for g in range(PAIRS):
        attended.append(after(5.1))
        plan.now += 1.5
        plan.start(DUO * g)
        plan.start(DUO * g + 1)
        paired.append(plan.due())

    @pl.loop(0, PAIRS)
    def _(g):
        def at(table):
            for i in range(PAIRS):
                if table[i]:
                    pl.when(g == i)(functools.partial(emit, table[i]))

        heads = [tile_at(DUO * g + i, LANES) for i in range(DUO)]
        with scope('attend'):
            attend(heads, a1, a2, ks, kts, vs, vts, cos, sin, lambda i: tile_at(core * HEADS + DUO * g + i, LANES), ots, dqo, dkt, dvt, s_scr, e_scr, p_scr, d_scr)

        @pl.when(g == 0)
        def _():
            with scope('entry'):
                comm.meet(CORNERS)
                for c in loads:
                    c.wait()
        for i in range(DUO):
            for c in head_trades(DUO * g + i):
                c.start()
        at(attended)
        gradient(DUO * g, DUO, rts, lambda: dqo[tile_at(g, PAIR), :], dot_nt)
        at(paired)

    def beat(cost, *starts):
        plan.now += cost
        for u in starts:
            plan.start(u)
        emit(plan.due())

    wkv, wkvp = e_scr.reshape(DIM, PAIR), p_scr.reshape(DIM, PAIR)
    later += [comm.local(src.at[:, pl.ds(at, LANES)], dst.at[:, pl.ds(to, LANES)]) for srcs, dst in (((wqk, wvo), wkv), ((wqkp, wvop), wkvp)) for src, at, to in ((srcs[0], HALF, 0), (srcs[1], 0, LANES))]
    wqp_loads = [comm.local(wqkp.at[tile_at(i, HALF), pl.ds(0, HALF)], two.at[i]) for i in range(DUO)]
    key = dkt[...] * SCALE
    co, si, x, y = cos[...], sin[...], key[:TURN], key[TURN:]
    dkvo[:LANES, :] = jnp.concatenate([x * co + y * si, y * co - x * si], axis=0).astype(bf16)
    dkvo[LANES:, :] = dvt[...].astype(bf16)
    comm.trade(dkvo, dkvp)
    gradient(UNIT_K, DUO, rts, lambda: dkvo[...], dot_nt)
    beat(1.8, UNIT_K, UNIT_V)
    wq_load = comm.local(wqk.at[:, pl.ds(0, HALF)], rts)
    for c in later:
        c.wait()
    with scope('trades'):
        for h in range(HEADS):
            for c in head_trades(h):
                c.wait()

    waiting = list(range(RING))

    def output_gradients(force=False):
        while waiting:
            first = 10 + DUO * waiting[0]
            before = [u for u in range(N_UNITS) if u < first and PLACE[u] in (PLACE[first], PLACE[first + 1])]
            if force:
                emit(plan.rush(lambda: all(map(plan.vacated, before))))
            if not all(map(plan.vacated, before)):
                return
            for u in before:
                sc.drain(u, 0)
            i = waiting.pop(0)
            gradient(PLACE[first], DUO, ots, lambda: dycs[:, i * PAIR:(i + 1) * PAIR], dot)
            plan.start(first)
            plan.start(first + 1)
            beat(1.5)

    def piece(cost):
        beat(cost)
        output_gradients()

    def ticking(n, cost, body):
        tables = [after(cost) for _ in range(n)]

        @pl.loop(0, n)
        def _(i):
            body(i)
            for j, table in enumerate(tables):
                if table:
                    pl.when(i == j)(functools.partial(emit, table))
        output_gradients()

    @pl.loop(0, TOKENS // LANES)
    def _(i):
        want = lax.broadcasted_iota(jnp.int32, (LANES, ROWS), 0) + i * LANES
        own[tile_at(i, LANES), :] = jnp.where(want == pos[...], 1.0, 0.0).astype(bf16)

    def unsort(at, src_t, n):
        with scope('unsort'):
            dnat[at:at + n, :] = dot(src_t[:n, :], own[...]).astype(bf16)

    output_gradients()
    for c in comm.exchanged:
        c.wait_recv()
    unsort(0, dqo, HALF)
    dy_loads = [comm.local(dy.at[:, tile_at(i, HALF)], dqo.at[tile_at(i, ROWS)]) for i in range(DUO)]
    piece(1.2)
    unsort(HALF, dqp, HALF)
    piece(1.2)
    unsort(DUO * HALF, dkvo, PAIR)
    unsort(DUO * HALF + PAIR, dkvp, PAIR)
    piece(0.7)
    wq_load.wait()
    for c in wqp_loads + dy_loads:
        c.wait()
    gacc[...] = jnp.zeros_like(gacc)

    def dr_parts(half, r):
        return [s_scr.at[half, r(i * PAIR), :] for i in range(RING)]

    def back(block, then):
        def dr(half):
            with scope('dr'):
                c = tile_at(half, HALF)
                left = jnp.concatenate([rts[c, :], two[half], wkv[c, :], wkvp[c, :]], axis=1)
                acc = dot(left, dnat[:, block * PAIR:(block + 1) * PAIR])
                for i, ref in enumerate(dr_parts(half, lambda at: pl.ds(at, PAIR))):
                    ref[...] = acc[i * PAIR:(i + 1) * PAIR, :].T

        def norm(part):
            with scope('back'):
                @pl.loop(0, RING)
                def _(i):
                    j = part * RING + i
                    q = pl.ds(pl.multiple_of(block * PAIR + j * SHARE, SHARE), SHARE)
                    d = jnp.concatenate([ref[...] for half in range(DUO) for ref in dr_parts(half, lambda at: pl.ds(pl.multiple_of(at + j * SHARE, SHARE), SHARE))], axis=1)
                    x = xs[q, :].astype(f32)
                    inv = lax.rsqrt(jnp.mean(x * x, axis=-1, keepdims=True) + RMS_EPS)
                    unit = x * inv
                    gacc[...] += jnp.sum((d * unit).reshape(DUO, SUBS, DIM), axis=0)
                    dg = d * gain[0:1, :]
                    new = inv * (dg - unit * jnp.mean(dg * unit, axis=-1, keepdims=True))
                    for half in range(DUO):
                        r = pl.ds(pl.multiple_of(half * ROWS + block * PAIR + j * SHARE, SHARE), SHARE)
                        dqo[r, :] = (dqo[r, :].astype(f32) + new[:, half * HALF:(half + 1) * HALF]).astype(bf16)

        ticking(DUO, 1.6, dr)
        then()
        ticking(RING, 0.92, norm)

    back(0, lambda: None)
    wo_loads = []
    back(1, lambda: wo_loads.extend([comm.local(wvo.at[:, pl.ds(LANES, HALF)], rts)] + [comm.local(wvop.at[tile_at(i, HALF), pl.ds(LANES, HALF)], two.at[i]) for i in range(DUO)]))
    for i in range(DUO):
        comm.store(dqo.at[tile_at(i, ROWS)], grad_x.at[:, tile_at(i, HALF)])
    total = jnp.sum(gacc[...], axis=0, keepdims=True)
    gpart[...] = jnp.zeros_like(gpart)
    for i in range(RING):
        for j in range(RING):
            gpart[i, j:j + 1, :] = total[:, (i * RING + j) * LANES:(i * RING + j + 1) * LANES]

    gain_c, gain_z, gain_p = (Batch(comm) for _ in range(TRIO))

    def sum_gain(stage):
        if stage == 0:
            gain_c.send(gpart, gpeer, peer)
        elif stage == 1:
            gain_c.arrived(gpeer)
            for j in range(RING):
                gz[j] = gpart[j] + gpeer[j]
            for hop in (1, DUO, TRIO):
                gain_z.send(gz.at[step(comm.pos, 'z', hop)], gz.at[TRIO + hop], comm.far('z', hop))
        elif stage == DUO:
            gain_z.arrived(gz.at[pl.ds(RING, TRIO)])
            gx[0] = (gz[comm.pos['z']] + gz[RING]) + (gz[5] + gz[6])
            for dy, dx in PLANE:
                gain_p.send(gx.at[0], gx.at[dy * RING + dx], comm.aside(dy, dx))
        else:
            gain_p.arrived(gx.at[pl.ds(1, 15)])
            gpeer[0] = jnp.sum(gx[...], axis=0)
            mine = jnp.broadcast_to(gpeer[0, pl.ds(comm.pos['y'], 1), :], (SUBS, LANES))
            gout[...] = pltpu.roll(mine, LANES - (comm.pos['x'] * CHIP + core * SHARE), 1)

    plan.start(GAIN)
    beat(0.2)
    for i in range(DUO):
        with scope('unsort_o'):
            @pl.loop(0, DUO)
            def _(j):
                r = pl.ds(pl.multiple_of(i * HALF + j * ROWS, ROWS), ROWS)
                onat[:, r] = dot(ots[r, :], own[...]).astype(bf16).T
        piece(1.58)
    output_gradients(True)

    def project_out(col, weights, i):
        with scope('project'):
            @pl.loop(DUO * i, DUO * i + DUO)
            def _(j):
                c = tile_at(j, PAIR)
                dst = pl.ds(pl.multiple_of(col + j * PAIR, PAIR), PAIR)
                xs[:, dst] = (xs[:, dst].astype(f32) + dot(onat[...], weights(c))).astype(bf16)
        beat(1.48)

    def own_half(c):
        return rts[:, c]

    def other_half(c):
        return jnp.concatenate([a1[:, c], a2[:, c]], axis=0)

    for c in wo_loads:
        c.wait()
    for col, weights in ((core * HALF, own_half), ((1 - core) * HALF, other_half)):
        for i in range(DUO):
            project_out(col, weights, i)
    comm.store(xs, result)
    emit(plan.rush(lambda: not plan.stage))
    with scope('finish'):
        sc.finish()
        for batch, whole in ((gain_c, gpart), (gain_z, gz.at[pl.ds(RING, TRIO)]), (gain_p, gx.at[pl.ds(1, 15)])):
            batch.sent(whole)
        for c in comm.exchanged:
            c.wait_send()
        for c in comm.stored:
            c.wait()


def tail(qt, do_t, k, kt, v, vt, rt, dyc, wqk, wqkp, wvo, wvop, gain, hidden, dy, pos, cos, sin):
    bf16, f32 = jnp.bfloat16, jnp.float32
    any_ = pl.BlockSpec(memory_space=pl.ANY)
    vmem = pl.BlockSpec(memory_space=pltpu.VMEM)
    S = lambda shape, d=bf16: jax.ShapeDtypeStruct(shape, d)
    V = lambda shape, d=bf16: pltpu.VMEM(shape, d)
    D = lambda n: pltpu.SemaphoreType.DMA((n,))
    sq, tall, wide = (HALF, TOKENS), (TOKENS, LANES), (LANES, TOKENS)
    mine, kv = (ROWS, DIM), (PAIR, TOKENS)
    return pl.pallas_call(
        tail_kernel,
        out_shape=[S(mine), S(mine), S((SHARE, DIM), f32), S((SHARE, PAIR), f32), S((SHARE, PAIR), f32), S((SHARE, DIM), f32), S((SUBS, LANES), f32)],
        in_specs=[any_] * 12 + [vmem] + [any_] * DUO + [vmem] * TRIO,
        out_specs=[any_] * 6 + [vmem],
        scratch_shapes=[V((DUO,) + sq), V(tall), V(wide), V(tall), V(wide), V((DIM, TOKENS)), V((DIM, TOKENS)), V(sq), V(sq), V(kv), V(kv), V(wide, f32), V(wide, f32),
                        V((DUO, TOKENS, QB), f32), V((DUO, TOKENS, QB)), V((DUO, TOKENS, QB)), V((DUO, TOKENS, QB)), V(sq), V((PLACES, RING, RING, RING, CHIP, LANES), f32), V((TRIO, SLOTS, RING, RING, CHIP, LANES), f32),
                        V((TRIO, SLOTS, 6, RING, RING, SHARE, LANES), f32), V((TRIO, SLOTS, 6, RING, SHARE, LANES), f32), V((TRIO, SLOTS, TRIO, CHIP, LANES), f32), V((N_UNITS, CHIP, LANES), f32), V((TOKENS, ROWS)), V(mine), V((DUO * QKV, ROWS)), V(mine),
                        V((SUBS, DIM), f32), V((RING, SUBS, LANES), f32), V((RING, SUBS, LANES), f32), V((7, SUBS, LANES), f32), V((SHARE, SUBS, LANES), f32),
                        D(9 * SLOTS), D(18 * SLOTS), D(DUO + N_UNITS), D(DUO * HEADS + RING), D(DUO * HEADS + RING), D(28)],
        compiler_params=pltpu.CompilerParams(collective_id=1, has_side_effects=True, vmem_limit_bytes=67043328),
        name='tail',
    )(qt, do_t, k, kt, v, vt, rt, dyc, wqk, wqkp, wvo, wvop, gain, hidden, dy, pos, cos, sin)


def settle_kernel(n, *refs):
    ins, gain, outs, gain_out, bufs, sems = refs[:n], refs[n], refs[n + 1:DUO * n + 1], refs[DUO * n + 1], refs[DUO * n + DUO:-1], refs[-1]
    jobs = []
    for a, o, b in zip(ins, outs, bufs):
        size = a.shape[0] // RING if a.shape[0] == ROWS else a.shape[0]
        jobs += [tuple(r.at[pl.ds(i, size)] for r in (a, b, o)) for i in range(0, a.shape[0], size)]
    takes = [pltpu.make_async_copy(a, b, sems.at[0, i]) for i, (a, b, _) in enumerate(jobs)]
    puts = [pltpu.make_async_copy(b, o, sems.at[1, i]) for i, (_, b, o) in enumerate(jobs)]
    for c in takes:
        c.start()
    gain_out[...] = gain[0:1, :SHARE]
    for take, put in zip(takes, puts):
        take.wait()
        put.start()
    for c in puts:
        c.wait()


def settle(*arrays):
    *large, gain = arrays
    any_, vmem = pl.BlockSpec(memory_space=pl.ANY), pl.BlockSpec(memory_space=pltpu.VMEM)
    return pl.pallas_call(
        functools.partial(settle_kernel, len(large)),
        out_shape=[jax.ShapeDtypeStruct(a.shape, a.dtype) for a in large] + [jax.ShapeDtypeStruct((1, SHARE), gain.dtype)],
        in_specs=[any_] * len(large) + [vmem],
        out_specs=[any_] * len(large) + [vmem],
        scratch_shapes=[pltpu.VMEM(a.shape, a.dtype) for a in large] + [pltpu.SemaphoreType.DMA((DUO, 12))],
        name='settle',
    )(*arrays)


def rope_tables():
    j = np.arange(HEAD_DIM // DUO, dtype=np.float64) / (HEAD_DIM // DUO)
    freq = (ROPE_THETA ** -j).astype(np.float32)
    angle = freq[:, None] * np.arange(TOKENS, dtype=np.float32)[None, :]
    return np.cos(angle.astype(np.float64)).astype(np.float32), np.sin(angle.astype(np.float64)).astype(np.float32)


def solution(mesh):
    def shard_fn(hidden, tok_pos, grad_out, norm_gain, w_query, w_key, w_value, w_out):
        hidden, grad_out = hidden[0], grad_out[0]
        cos_t, sin_t = (jnp.asarray(t) for t in rope_tables())
        *parts, gain = head(hidden, grad_out, w_query, w_key, w_value, w_out, tok_pos, norm_gain.reshape(1, SHARE), cos_t, sin_t)
        parts = [p.reshape(DIM, GROUP) if p.ndim > DUO else p for p in parts]
        result, grad_hidden, gq, gk, gv, go, gout = settle(*tail(*parts, gain, hidden, grad_out, tok_pos, cos_t, sin_t))
        return result[None], grad_hidden[None], gq, gk, gv, go, gout.reshape(SHARE)

    row_spec, pos_spec = P('fsdp', 'cp', None), P('fsdp', 'cp')
    weight_spec, gain_spec = P(('fsdp', 'cp'), None), P(('fsdp', 'cp'))
    return jax.shard_map(shard_fn, mesh=mesh, in_specs=(row_spec, pos_spec, row_spec, gain_spec, weight_spec, weight_spec, weight_spec, weight_spec), out_specs=(row_spec, row_spec, weight_spec, weight_spec, weight_spec, weight_spec, gain_spec), check_vma=False)
```

```python
import functools
import jax
import jax.numpy as jnp
import numpy as np
from jax import lax
from jax.experimental import pallas as pl
from jax.experimental.pallas import tpu as pltpu
from jax.sharding import PartitionSpec as P

LANES, SUBS, RING, TRIO, DUO = 128, 8, 4, 3, 2
PAIR, ROWS, CHIP, SHARE, TURN = 256, 512, 32, 16, 64
HEAD_DIM = LANES
ROPE_THETA = 1000000.0
RMS_EPS = 1e-5
SCALE = HEAD_DIM ** -0.5
LOG2E = 1.4426950408889634

MESH = pl.DeviceIdType.MESH
AXES = ('x', 'y', 'z')
ORDERS = (('x', 'y', 'z'), ('y', 'z', 'x'), ('z', 'x', 'y'))
ALL = pl.ds(0, RING)


def torus():
    f = lax.axis_index('fsdp')
    return {'x': lax.rem(f, RING), 'y': lax.rem(lax.div(f, RING), RING), 'z': lax.div(f, SHARE)}


def step(pos, axis, hop):
    return lax.rem(pos[axis] + hop, RING)


class Batch:
    def __init__(self, comm):
        self.comm, self.index = comm, comm.used
        comm.used += 1

    def _copy(self, src, dst, device):
        send, recv, _ = self.comm.sems
        return pltpu.make_async_remote_copy(src_ref=src, dst_ref=dst, send_sem=send.at[self.index], recv_sem=recv.at[self.index], device_id=device, device_id_type=MESH)

    def send(self, src, dst, device):
        self._copy(src, dst, device).start()
        return self

    def arrived(self, whole):
        self._copy(whole, whole, self.comm.peer()).wait_recv()

    def sent(self, whole):
        self._copy(whole, whole, self.comm.peer()).wait_send()


class Comm:
    def __init__(self, send_sems, recv_sems, local_sems):
        self.pos = torus()
        self.core = lax.axis_index('cp')
        self.sems = (send_sems, recv_sems, local_sems)
        self.used = self.used_local = 0
        self.stored = []

    def far(self, axis, hop):
        p = dict(self.pos)
        p[axis] = step(self.pos, axis, hop)
        return {'fsdp': (p['z'] * RING + p['y']) * RING + p['x'], 'cp': self.core}

    def peer(self):
        return {'fsdp': lax.axis_index('fsdp'), 'cp': 1 - self.core}

    def aside(self, dy, dx):
        return {'fsdp': (self.pos['z'] * RING + step(self.pos, 'y', dy)) * RING + step(self.pos, 'x', dx), 'cp': self.core}

    def announce(self, corners=()):
        sem = pltpu.get_barrier_semaphore()
        for axis in AXES:
            for hop in (1, DUO, TRIO):
                pl.semaphore_signal(sem, inc=1, device_id=self.far(axis, hop), device_id_type=MESH)
        for dy, dx in corners:
            pl.semaphore_signal(sem, inc=1, device_id=self.aside(dy, dx), device_id_type=MESH)
        pl.semaphore_signal(sem, inc=1, device_id=self.peer(), device_id_type=MESH)

    def meet(self, corners=()):
        pl.semaphore_wait(pltpu.get_barrier_semaphore(), 10 + len(corners))

    def ring(self, batch, src, slots, axis):
        for hop in (1, DUO, TRIO):
            batch.send(src, slots.at[hop], self.far(axis, hop))

    def local(self, src, dst):
        i = self.used_local
        self.used_local += 1
        c = pltpu.make_async_copy(src, dst, self.sems[DUO].at[i])
        c.start()
        return c

    def store(self, src, dst):
        self.stored.append(self.local(src, dst))


class Singles(Comm):
    def __init__(self, *sems):
        super().__init__(*sems)
        self.sent, self.exchanged = [], []

    def _copy(self, src, dst, device):
        i = self.used
        self.used += 1
        c = pltpu.make_async_remote_copy(src_ref=src, dst_ref=dst, send_sem=self.sems[0].at[i], recv_sem=self.sems[1].at[i], device_id=device, device_id_type=MESH)
        c.start()
        return c

    def send(self, src, dst, device):
        c = self._copy(src, dst, device)
        self.sent.append(c)
        return c

    def trade(self, src, dst):
        self.exchanged.append(self._copy(src, dst, self.peer()))


def pick(ref, sel, piece):
    lo, cols, first, rows = piece
    return ref.at[sel['z'], sel['y'], sel['x'], pl.ds(first, rows), pl.ds(lo, cols)]


def sem_scratch(remote, local):
    return [pltpu.SemaphoreType.DMA((remote,)), pltpu.SemaphoreType.DMA((remote,)), pltpu.SemaphoreType.DMA((local,))]


def add_into(dst, *srcs, fresh=False):
    def add(idx):
        total, *rest = [s[idx] for s in (srcs if fresh else (dst,) + srcs)]
        for more in rest:
            total = total + more
        dst[idx] = total

    if len(dst.shape) > TRIO:
        @pl.loop(0, dst.shape[0])
        def _(i):
            add((i,))
    else:
        add(Ellipsis)


def columns(lo, na, nb):
    return (lo, na, 0, CHIP), (lo + na, nb, 0, CHIP)


def strip(lo):
    return (lo, LANES, 0, SHARE), (lo, LANES, SHARE, SHARE)


QK_COLORS = (columns(0, PAIR, LANES), columns(384, LANES, PAIR), columns(768, PAIR, LANES))
VO_COLORS = (columns(0, LANES, PAIR), columns(384, PAIR, LANES), columns(768, LANES, PAIR))
QK_FIRST = (columns(0, LANES, LANES), columns(384, LANES, LANES), columns(768, LANES, LANES))
QK_LAST = (strip(PAIR), strip(640), strip(1024))
TOKENS = 1024
DIM = 2048
HALF = 1024
QKV = 1280
GROUP = 1152


def scope(name):
    return jax.named_scope(name)


def dot(a, b):
    return jnp.dot(a, b, preferred_element_type=jnp.float32)


def dot_nt(a, b):
    return lax.dot_general(a, b, (((1,), (1,)), ((), ())), preferred_element_type=jnp.float32)


def tile_at(i, n):
    return pl.ds(pl.multiple_of(i * n, n), n)


class Gather:
    def __init__(self, comm, ref, colors, land, held=None):
        self.comm, self.ref, self.colors, self.land = comm, ref, colors, land
        self.held = list(held or [dict(comm.pos) for _ in colors])
        self.spent = []

    def move(self, batch, s, piece, to):
        batch.send(pick(self.ref, s, piece), pick(self.ref, s, piece), to)

    def at(self, k, hop):
        d = ORDERS[k][self.phase]
        return dict(self.held[k], **{d: step(self.comm.pos, d, hop)})

    def begin(self, phase):
        self.phase = phase
        self.rest = Batch(self.comm)
        if phase == 0:
            for k, pieces in enumerate(self.colors):
                for piece in pieces:
                    for hop in (DUO, 1, TRIO):
                        self.move(self.rest, self.held[k], piece, self.comm.far(ORDERS[k][0], hop))
            return
        self.up, self.dn = ([Batch(self.comm) for _ in range(TRIO)] for _ in range(DUO))
        for k, (a, b) in enumerate(self.colors):
            d = ORDERS[k][phase]
            up, dn, s = self.comm.far(d, 1), self.comm.far(d, TRIO), self.held[k]
            self.move(self.up[k], s, a, up)
            self.move(self.dn[k], s, b, dn)
            self.move(self.rest, s, b, up)
            self.move(self.rest, s, a, dn)
        if phase == DUO:
            for k, pieces in enumerate(self.colors):
                for piece in pieces:
                    self.land(self.ref, self.held[k], piece)

    def forward(self):
        for k, (a, b) in enumerate(self.colors):
            d = ORDERS[k][self.phase]
            for batch, hop, piece, to in ((self.up[k], TRIO, a, 1), (self.dn[k], 1, b, TRIO)):
                s = self.at(k, hop)
                batch.arrived(pick(self.ref, s, piece))
                self.move(self.rest, s, piece, self.comm.far(d, to))
                if self.phase == DUO:
                    self.land(self.ref, s, piece)
                self.spent.append((batch, pick(self.ref, self.held[k], piece)))

    def end(self):
        axis = ORDERS[0][self.phase]
        blocks = dict(self.held[0], **{axis: pl.ds(0, DUO if self.phase else TRIO)})
        width = sum(max(a[0] + a[1], b[0] + b[1]) - a[0] for a, b in self.colors)
        whole = pick(self.ref, blocks, (0, width, 0, CHIP))
        self.rest.arrived(whole)
        self.spent.append((self.rest, whole))
        for k, (a, b) in enumerate(self.colors):
            if self.phase == DUO:
                for hop, piece in ((TRIO, b), (1, a), (DUO, a), (DUO, b)):
                    self.land(self.ref, self.at(k, hop), piece)
            self.held[k] = dict(self.held[k], **{ORDERS[k][self.phase]: ALL})

    def finish(self):
        for batch, whole in self.spent:
            batch.sent(whole)


def head_kernel(hidden, dy, wq, wk, wv, wo, pos, gain_in, cos_t, sin_t,
                qt_o, dot_o, k_o, kt_o, v_o, vt_o, rt_o, dyc_o, wqk_o, wqkp_o, wvo_o, wvop_o, gain_o,
                hid2, dy2, dys, rs, rt, wqk, wvo, wpeer, pi, pos2, qt, dot_s, kk, kt, vv, vt, gain, gtile, gbuf, gx, gy, gz, *sems):
    comm = Comm(*sems)
    pos_c, core = comm.pos, comm.core
    bf16, f32 = jnp.bfloat16, jnp.float32
    peer = comm.peer()
    rows = tile_at(core, SHARE)
    mine_qk = wqk.at[pos_c['z'], pos_c['y'], pos_c['x'], rows]
    mine_vo = wvo.at[pos_c['z'], pos_c['y'], pos_c['x'], rows]

    def weight_parts(c):
        return ((wq.at[:, tile_at(c, HALF)], mine_qk.at[:, pl.ds(0, HALF)]), (wk.at[:, tile_at(c, LANES)], mine_qk.at[:, pl.ds(HALF, LANES)]),
                (wv.at[:, tile_at(c, LANES)], mine_vo.at[:, pl.ds(0, LANES)]), (wo.at[:, tile_at(c, HALF)], mine_vo.at[:, pl.ds(LANES, HALF)]))

    loads = [comm.local(s, d) for s, d in weight_parts(core)]
    load_x = [comm.local(hidden, hid2.at[pl.ds(0, ROWS)]), comm.local(dy, dy2.at[pl.ds(0, ROWS)])]
    share = lax.broadcasted_iota(jnp.int32, (SUBS, LANES), 1) // SHARE
    gtile[...] = jnp.where(share == pos_c['x'] * DUO + core, jnp.broadcast_to(jnp.concatenate([gain_in[...]] * SUBS, axis=1), (SUBS, LANES)), 0.0)
    comm.announce()
    with scope('entry'):
        comm.meet()
    swap_w, swap_pos, swap_dy, swap_x, peers_qk, peers_vo = (Batch(comm) for _ in range(6))
    gain_c, gain_x, gain_y, gain_z = (Batch(comm) for _ in range(RING))
    for s, d in weight_parts(1 - core):
        swap_w.send(s, d, peer)
    gain_c.send(gtile, gbuf, peer)
    swap_pos.send(pos, pos2, peer)
    for c in loads:
        c.wait()
    with scope('wait_w'):
        swapped = wqk.at[pos_c['z'], pos_c['y'], pos_c['x']]
        swap_w.arrived(swapped)

    def land_qk(ref, s, cols):
        peers_qk.send(pick(ref, s, cols), pick(wqkp_o, s, cols), peer)

    def land_vo(ref, s, cols):
        peers_vo.send(pick(ref, s, cols), pick(wpeer, s, cols), peer)

    g1 = Gather(comm, wvo, VO_COLORS, land_vo)
    g2 = Gather(comm, wqk, QK_COLORS, land_qk)
    g1.begin(0)
    g2.begin(0)
    gain_c.arrived(gbuf)
    gx[0] = gtile[...] + gbuf[...]
    comm.ring(gain_x, gx.at[0], gx, 'x')

    swap_pos.arrived(pos2)

    @pl.loop(0, TOKENS // LANES)
    def _(i):
        want = lax.broadcasted_iota(jnp.int32, (LANES, ROWS), 0) + i * LANES
        for h, have in enumerate((pos, pos2)):
            pi[tile_at(i, LANES), h * ROWS:(h + 1) * ROWS] = jnp.where(want == have[...], 1.0, 0.0).astype(bf16)

    def sort(dst, src, first, last):
        with scope('sort'):
            @pl.loop(first, last)
            def _(j):
                c = tile_at(j, PAIR)
                dst[:, c] = dot(pi[...], src[:, c]).astype(bf16)

    swap_dy.send(dy, dy2.at[pl.ds(ROWS, ROWS)], peer)
    with scope('p0_end'):
        for g in (g1, g2):
            g.end()
            g.begin(1)
    swap_x.send(hidden, hid2.at[pl.ds(ROWS, ROWS)], peer)
    gain_x.arrived(gx.at[pl.ds(1, TRIO)])
    gy[pos_c['y']] = (gx[0] + gx[1]) + (gx[DUO] + gx[TRIO])
    for hop in (1, DUO, TRIO):
        gain_y.send(gy.at[pos_c['y']], gy.at[pos_c['y']], comm.far('y', hop))
    with scope('wait_dy'):
        load_x[1].wait()
        swap_dy.arrived(dy2.at[pl.ds(ROWS, ROWS)])
    sort(dys, dy2, 0, RING)
    with scope('p1a_fwd'):
        g1.forward()
    sort(dys, dy2, RING, 6)
    with scope('p1b_fwd'):
        g2.forward()
    sort(dys, dy2, 6, SUBS)
    with scope('p1a_end'):
        g1.end()
    gain_y.arrived(gy.at[pl.ds(1, TRIO)])
    for j in range(RING):
        gz[pos_c['z'], j] = gy[j]
    for hop in (1, DUO, TRIO):
        gain_z.send(gz.at[pos_c['z']], gz.at[pos_c['z']], comm.far('z', hop))
    g1.begin(DUO)
    comm.store(dys.at[:, tile_at(core, HALF)], dyc_o)
    with scope('p1b_end'):
        g2.end()
    with scope('wait_x'):
        load_x[0].wait()
        swap_x.arrived(hid2.at[pl.ds(ROWS, ROWS)])
    sort(rs, hid2, 0, SUBS)
    with scope('p2q_fwd'):
        g1.forward()
    g2a, g2b = (Gather(comm, wqk, colors, land_qk, g2.held) for colors in (QK_FIRST, QK_LAST))
    g2a.begin(DUO)
    with scope('gain'):
        gain_z.arrived(gz.at[pl.ds(1, TRIO)])
    for i in range(RING):
        for j in range(RING):
            gain[:, (i * RING + j) * LANES:(i * RING + j + 1) * LANES] = gz[i, j]
    comm.store(gain, gain_o)

    def norm(first, last):
        with scope('norm'):
            @pl.loop(first, last)
            def _(i):
                r = tile_at(i, CHIP)
                x = rs[r, :].astype(f32)
                inv = lax.rsqrt(jnp.mean(x * x, axis=-1, keepdims=True) + RMS_EPS)
                rs[r, :] = (x * inv * gain[0:1, :]).astype(bf16)

    norm(0, TOKENS // CHIP)
    with scope('r_t'):
        @pl.loop(0, DIM // PAIR)
        def _(i):
            c = tile_at(i, PAIR)

            @pl.loop(0, TOKENS // PAIR)
            def _(j):
                r = tile_at(j, PAIR)
                rt[c, r] = rs[r, c].T
    comm.store(rt, rt_o)
    with scope('p2o_end'):
        g1.end()
    w_qk, w_vo, w_peer = wqk.reshape(DIM, GROUP), wvo.reshape(DIM, GROUP), wpeer.reshape(DIM, GROUP)
    with scope('vals'):
        @pl.loop(0, DUO)
        def _(i):
            r = tile_at(i, ROWS)
            val = dot(rs[r, :], w_vo[:, :LANES]).astype(bf16)
            vv[r, :] = val
            vt[:, r] = val.T
    for src, dst in ((wvo, wvo_o), (vv, v_o), (vt, vt_o)):
        comm.store(src, dst)
    with scope('p2q_fwd'):
        g2a.forward()
    g2b.begin(DUO)
    with scope('wo_peer'):
        peers_vo.arrived(wpeer)
    comm.store(wpeer, wvop_o)
    with scope('do_t'):
        mine = tile_at(core, HALF)

        @pl.loop(0, TOKENS // PAIR)
        def _(j):
            t = tile_at(j, PAIR)
            w_rows = jnp.concatenate([w_vo[mine, LANES:], w_peer[mine, LANES:]], axis=1)
            d_rows = jnp.concatenate([dys[t, mine], dys[t, tile_at(1 - core, HALF)]], axis=1)
            dot_s[:, t] = dot_nt(w_rows, d_rows).astype(bf16)
    comm.store(dot_s, dot_o)

    def rotated(x, r):
        cos, sin = cos_t[:, r], sin_t[:, r]
        cos = jnp.concatenate([cos, cos], axis=0).T
        sin = jnp.concatenate([-sin, sin], axis=0).T
        return (x * cos + pltpu.roll(x, TURN, 1) * sin).astype(bf16)

    def queries(columns, heads):
        x = dot(rs[...], columns)
        for i in range(RING):
            r = slice(i * PAIR, (i + 1) * PAIR)
            for h, head in enumerate(heads):
                qt[tile_at(head, LANES), r] = rotated(x[r, h * LANES:(h + 1) * LANES], r).T

    with scope('p2q_end'):
        g2a.end()

    def pairs(first, last):
        with scope('q'):
            @pl.loop(first, last)
            def _(t):
                queries(w_qk[:, pl.ds(pl.multiple_of(t * 384, LANES), PAIR)], (TRIO * t, TRIO * t + 1))

    pairs(0, 1)
    with scope('last_fwd'):
        g2b.forward()
    pairs(1, TRIO)
    with scope('last_end'):
        g2b.end()
    comm.store(wqk, wqk_o)
    with scope('q_last'):
        x = dot(rs[...], jnp.concatenate([w_qk[:, PAIR:384], w_qk[:, 640:768], w_qk[:, HALF:]], axis=1))
        for i in range(RING):
            r = slice(i * PAIR, (i + 1) * PAIR)
            key = rotated(x[r, PAIR:], r)
            kk[r, :] = key
            kt[:, r] = key.T
            for h, head in enumerate((DUO, 5)):
                qt[tile_at(head, LANES), r] = rotated(x[r, h * LANES:(h + 1) * LANES], r).T
    for src, dst in ((kk, k_o), (kt, kt_o), (qt, qt_o)):
        comm.store(src, dst)
    with scope('finish'):
        peers_qk.arrived(wqk)
        for batch, whole in ((swap_w, swapped), (swap_pos, pos2), (swap_dy, dy2.at[pl.ds(ROWS, ROWS)]), (swap_x, hid2.at[pl.ds(ROWS, ROWS)]), (peers_qk, wqk), (peers_vo, wvo),
                             (gain_c, gbuf), (gain_x, gx.at[pl.ds(1, TRIO)]), (gain_y, gy.at[pl.ds(1, TRIO)]), (gain_z, gz.at[pl.ds(1, TRIO)])):
            batch.sent(whole)
        for g in (g1, g2, g2a, g2b):
            g.finish()
        for c in comm.stored:
            c.wait()


def head(hidden, dy, wq, wk, wv, wo, pos, gain, cos_t, sin_t):
    bf16, f32 = jnp.bfloat16, jnp.float32
    any_ = pl.BlockSpec(memory_space=pl.ANY)
    vmem = pl.BlockSpec(memory_space=pltpu.VMEM)
    S = lambda shape, d=bf16: jax.ShapeDtypeStruct(shape, d)
    V = lambda shape, d=bf16: pltpu.VMEM(shape, d)
    group = (RING, RING, RING, CHIP, GROUP)
    sq, tall, wide = (HALF, TOKENS), (TOKENS, LANES), (LANES, TOKENS)
    full = (TOKENS, DIM)
    return pl.pallas_call(
        head_kernel,
        out_shape=[S(sq), S(sq), S(tall), S(wide), S(tall), S(wide), S((DIM, TOKENS)), S((TOKENS, HALF)), S(group), S(group), S(group), S(group), S((SUBS, DIM), f32)],
        in_specs=[any_] * 6 + [vmem] * RING,
        out_specs=[any_] * 13,
        scratch_shapes=[V(full), V(full), V(full), V(full), V((DIM, TOKENS)), V(group), V(group), V(group), V((TOKENS, TOKENS)), V((1, ROWS), jnp.int32),
                        V(sq), V(sq), V(tall), V(wide), V(tall), V(wide), V((SUBS, DIM), f32), V((SUBS, LANES), f32), V((SUBS, LANES), f32), V((RING, SUBS, LANES), f32), V((RING, SUBS, LANES), f32), V((RING, RING, SUBS, LANES), f32)] + sem_scratch(47, 18),
        compiler_params=pltpu.CompilerParams(collective_id=0, has_side_effects=True, vmem_limit_bytes=60 * DUO**20),
        name='head',
    )(hidden, dy, wq, wk, wv, wo, pos, gain, cos_t, sin_t)


HEADS = SUBS
UNIT_K, UNIT_V = SUBS, 9
N_UNITS = 18
GAIN = N_UNITS
SLOTS = RING
LAST = 5
ABREAST = DUO
LINES = ((0, TRIO, 6, 9, 12, 15), (1, RING, 7, 10, 13, SHARE), (DUO, 5, SUBS, 11, 14, 17))
COLOR = {u: k for k, line in enumerate(LINES) for u in line}
RANK = {u: i for line in LINES for i, u in enumerate(line)}
SWAPPED = (1, TRIO, RING, SUBS, 10)
ORDER = {u: ORDERS[k] if u not in SWAPPED else (ORDERS[k][0], ORDERS[k][DUO], ORDERS[k][1]) for u, k in COLOR.items()}
BEFORE = {u: line[i - SLOTS] if i >= SLOTS else None for line in LINES for i, u in enumerate(line)}
PLACES = 12
PLACE = {u: u % PLACES for u in range(N_UNITS)}
WIRE = (2.82, 0.71, 0.36)
LATENCY = 2.4
STAGE_COST = 0.08


class Plan:
    def __init__(self):
        self.now, self.stage, self.ready, self.order, self.link = 0.0, {}, {}, [], {}
        self.mark = {}

    def _wire(self, u, phase, count):
        link = ORDER[u][phase]
        t = max(self.link.get(link, 0.0), self.now)
        first = t + WIRE[phase] + LATENCY
        self.link[link] = t + WIRE[phase] * count
        return first if phase < DUO else self.link[link] + LATENCY

    def free(self, u, phase):
        if BEFORE[u] is None:
            return True
        done = self.mark.get((BEFORE[u], (DUO, RING, 5)[phase]))
        if done is None:
            return False
        sent = ((0, 1), (DUO, TRIO), (RING,))[phase]
        return any(self.mark.get((j, s), -1) > done and (j, s + 1) in self.mark for j, order in ORDER.items() if order[phase] == ORDER[u][phase] for s in sent)

    def run(self, u):
        stage = self.stage[u]
        self.order.append((u, stage))
        self.mark[u, stage] = len(self.order)
        self.now = max(self.now, self.ready[u]) + STAGE_COST
        self.stage[u] = stage + 1
        if stage == (TRIO if u == GAIN else LAST):
            del self.stage[u]
        elif u == GAIN:
            self.ready[u] = max([self.now] + [self.link.get(a, 0.0) for a in ('', 'z', 'xy')[stage]]) + DUO * LATENCY
        elif stage % DUO:
            self.ready[u] = self._wire(u, stage // DUO, 1)
        else:
            self.ready[u] = self._wire(u, stage // DUO, DUO)

    def blocked(self, u):
        stage = self.stage[u]
        if u == GAIN:
            return False
        if stage == 0 and sum(0 < self.stage.get(j, 0) <= DUO for j in LINES[COLOR[u]]) >= ABREAST:
            return True
        if stage == DUO and BEFORE[u] is not None and (BEFORE[u], LAST) not in self.mark:
            return True
        return stage in (0, DUO, RING) and not self.free(u, stage // DUO)

    def start(self, u):
        self.stage[u], self.ready[u] = 0, self.now

    def due(self):
        first = len(self.order)
        while True:
            ripe = [(self.ready[u], u) for u in self.stage if self.ready[u] <= self.now and not self.blocked(u)]
            if not ripe:
                return self.order[first:]
            self.run(min(ripe)[1])

    def vacated(self, u):
        return (u, DUO) in self.mark

    def rush(self, done):
        first = len(self.order)
        while not done():
            self.run(min((self.ready[u], u) for u in self.stage if not self.blocked(u))[1])
        return self.order[first:]


QB = PAIR
PAIRS = HEADS // DUO
NBLK = TOKENS // QB
HALVES = (pl.ds(0, SHARE), pl.ds(SHARE, SHARE))
PLANE = tuple((dy, dx) for dy in range(RING) for dx in range(RING) if dy or dx)
CORNERS = tuple((dy, dx) for dy, dx in PLANE if dy and dx)


class Scatter:
    def __init__(self, comm, part, mid, bufs, fin, outs, send_sems, recv_sems, swap_sems):
        self.pos, self.part, self.mid, self.bufs, self.fin, self.outs = comm.pos, part, mid, bufs, fin, outs
        self.send_sems, self.recv_sems, self.swap_sems = send_sems, recv_sems, swap_sems
        self.near = {(a, hop): comm.far(a, hop) for a in AXES for hop in (1, DUO, TRIO)}
        self.hops = {(a, hop): step(comm.pos, a, hop) for a in AXES for hop in (1, DUO, TRIO)}
        self.peer, self.core = comm.peer(), comm.core
        self.keep, self.give = tile_at(comm.core, SHARE), tile_at(1 - comm.core, SHARE)
        self.drained = set()

    def slot(self, u):
        return COLOR[u], RANK[u] % SLOTS

    def buf(self, u, phase):
        return self.bufs[phase].at[self.slot(u)]

    def view(self, u, phase, hop, half=None):
        order = ORDER[u]
        at = {a: ALL for a in AXES}
        for a in order[1:phase]:
            at[a] = self.pos[a]
        at[order[phase]] = self.hops[order[phase], hop] if hop else self.pos[order[phase]]
        rows = pl.ds(0, CHIP) if half is None else HALVES[half]
        if phase == 0:
            return self.part.at[PLACE[u], at['z'], at['y'], at['x'], rows, :]
        return self.mid.at[self.slot(u) + tuple(at[a] for a in 'zyx' if a != order[0]) + (rows, slice(None))]

    def copy(self, src, dst, sems, device):
        return pltpu.make_async_remote_copy(src_ref=src, dst_ref=dst, send_sem=sems[0], recv_sem=sems[1], device_id=device, device_id_type=MESH)

    def sems(self, u, phase, kind=0):
        k, i = self.slot(u)
        at = (k * SLOTS + i) * TRIO + phase
        return self.send_sems.at[at], self.recv_sems.at[(k * SLOTS + i) * 5 + DUO * phase + kind]

    def send(self, u, phase, name):
        axis = ORDER[u][phase]
        if phase == DUO:
            src, to = self.view(u, DUO, name + 1), name + 1
        else:
            hop, half, to = ((DUO, 0, 1), (DUO, 1, TRIO), (1, 1, 1), (TRIO, 0, TRIO), (1, 0, 1), (TRIO, 1, TRIO))[name]
            src = self.view(u, phase, hop, half)
        self.copy(src, self.buf(u, phase).at[name], self.sems(u, phase, int(name > 1 and phase < DUO)), self.near[axis, to]).start()

    def launch(self, u, phase):
        if BEFORE[u] is not None:
            self.drain(BEFORE[u], phase)
        for name in range(RING if phase < DUO else TRIO):
            self.send(u, phase, name)

    def arrived(self, u, phase, first, count):
        whole = self.buf(u, phase).at[pl.ds(first, count)]
        self.copy(whole, whole, self.sems(u, phase, int(first > 0)), self.peer).wait_recv()

    def drain(self, u, phase):
        if (u, phase) not in self.drained:
            self.drained.add((u, phase))
            whole = self.buf(u, phase)
            self.copy(whole, whole, self.sems(u, phase), self.peer).wait_send()

    def out(self, u):
        if u < HEADS:
            out, col = self.outs[0], self.core * HALF + u * LANES
        elif u < 10:
            out, col = self.outs[u - 7], self.core * LANES
        else:
            out, col = self.outs[TRIO], self.core * HALF + (u - 10) * LANES
        return out.at[:, pl.ds(pl.multiple_of(col, LANES), LANES)]

    def kept(self, u):
        return pltpu.make_async_copy(self.fin.at[u, self.keep], self.out(u), self.swap_sems.at[DUO + u])

    def run(self, u, stage):
        if stage == 0:
            return self.launch(u, 0)
        phase = (stage - 1) // DUO
        if stage == LAST:
            self.arrived(u, DUO, 0, TRIO)
            got = self.buf(u, DUO)
            self.fin[u] = self.view(u, DUO, 0)[...] + (got[0] + got[1] + got[DUO])
            self.copy(self.fin.at[u, self.give], self.out(u), (self.swap_sems.at[0], self.swap_sems.at[1]), self.peer).start()
            self.kept(u).start()
            return
        got = self.buf(u, phase)
        if stage % DUO:
            self.arrived(u, phase, 0, DUO)
            for name, hop in ((0, 1), (1, TRIO)):
                add_into(self.view(u, phase, hop, name), got.at[name])
                self.send(u, phase, name + RING)
            return
        self.arrived(u, phase, DUO, RING)
        if phase == 0 and BEFORE[u] is not None:
            self.drain(BEFORE[u], 1)
            self.drain(BEFORE[u], DUO)
        for half, names in ((0, (TRIO, RING)), (1, (DUO, 5))):
            if phase:
                add_into(self.view(u, phase, 0, half), *[got.at[name] for name in names])
            else:
                dst = self.mid.at[self.slot(u) + (ALL, ALL, HALVES[half], slice(None))]
                add_into(dst, self.view(u, 0, 0, half), *[got.at[name] for name in names], fresh=True)
        self.launch(u, phase + 1)

    def finish(self):
        for u in range(N_UNITS):
            for phase in range(TRIO):
                self.drain(u, phase)
        half = self.fin.at[:, pl.ds(0, SHARE)]
        swaps = self.copy(half, half, (self.swap_sems.at[0], self.swap_sems.at[1]), self.peer)
        swaps.wait_send()
        swaps.wait_recv()
        for u in range(N_UNITS):
            self.kept(u).wait()


def attend(heads, qt, do_t, k, kt, v, vt, cos, sin, o_row, ot, dq, dkt, dvt, s_scr, e_scr, p_scr, d_scr):
    f32, bf16 = jnp.float32, jnp.bfloat16
    strip = TURN
    work = [(h, j) for j in range(NBLK) for h in range(len(heads))]

    def strips(c):
        return [(i * strip, slice(c * QB + i * strip, c * QB + (i + 1) * strip)) for i in range(QB // strip)]

    def fold(x, op):
        return op(x.reshape(strip // SUBS, SUBS, QB), axis=0)

    def scores(i):
        (h, j), b = work[i], i % DUO
        q_t = qt[heads[h], j * QB:(j + 1) * QB]
        top = jnp.full((SUBS, QB), -jnp.inf, f32)
        for c in range(j + 1):
            tile = dot(k[c * QB:(c + 1) * QB, :], q_t)
            for at, rows in strips(c):
                s = tile[at:at + strip]
                if c == j:
                    seen = lax.broadcasted_iota(jnp.int32, (strip, QB), 0) + at <= lax.broadcasted_iota(jnp.int32, (strip, QB), 1)
                    s = jnp.where(seen, s, -jnp.inf)
                s_scr[b, rows, :] = s
                top = jnp.maximum(top, fold(s, jnp.max))
        return jnp.max(top, axis=0, keepdims=True)

    def rest(i, m):
        (h, j), b = work[i], i % DUO
        cols, n = slice(j * QB, (j + 1) * QB), (j + 1) * QB
        q_t, d_t = qt[heads[h], cols], do_t[heads[h], cols]
        tot = jnp.zeros((SUBS, QB), f32)
        for c in range(j + 1):
            for at, rows in strips(c):
                e = jnp.exp2((s_scr[b, rows, :] - m) * (SCALE * LOG2E))
                s_scr[b, rows, :] = e
                e_scr[b, rows, :] = e.astype(bf16)
                tot = tot + fold(e, jnp.sum)
        den = jnp.sum(tot, axis=0, keepdims=True)
        inv = 1.0 / den
        o = (dot(vt[:, :n], e_scr[b, :n, :]) / den).astype(bf16)
        ot[o_row(h), cols] = o
        delta = jnp.sum(d_t.astype(f32) * o.astype(f32), axis=0, keepdims=True)
        for c in range(j + 1):
            dp = dot(v[c * QB:(c + 1) * QB, :], d_t)
            for at, rows in strips(c):
                p = s_scr[b, rows, :] * inv
                p_scr[b, rows, :] = p.astype(bf16)
                d_scr[b, rows, :] = (p * (dp[at:at + strip] - delta)).astype(bf16)
        dvt[:, :n] += dot_nt(d_t, p_scr[b, :n, :])
        dkt[:, :n] += dot_nt(q_t, d_scr[b, :n, :])
        g = dot(kt[:, :n], d_scr[b, :n, :]) * SCALE
        co, si = cos[:, cols], sin[:, cols]
        x, y = g[:TURN], g[TURN:]
        dq[heads[h], cols] = jnp.concatenate([x * co + y * si, y * co - x * si], axis=0).astype(bf16)

    m = scores(0)
    for i in range(len(work)):
        later = scores(i + 1) if i + 1 < len(work) else None
        rest(i, m)
        m = later


def tail_kernel(qt, do_t, k, kt, v, vt, rt, dyc, wqk, wqkp, wvo, wvop, gain, hidden, dy, pos, cos, sin,
                result, grad_x, gq, gk, gv, go, gout,
                two, ks, kts, vs, vts, rts, ots, dqo, dqp, dkvo, dkvp, dkt, dvt, s_scr, e_scr, p_scr, d_scr, dycs, part, mid, buf1, buf2, buf3, fin, own, onat, dnat, xs, gacc, gpart, gpeer, gz, gx,
                send_sems, recv_sems, swap_sems, trade_send, trade_recv, local_sems):
    comm = Singles(trade_send, trade_recv, local_sems)
    comm.used = HEADS
    f32, bf16 = jnp.float32, jnp.bfloat16
    core, peer = comm.core, comm.peer()
    a1, a2 = two.at[0], two.at[1]
    comm.announce(CORNERS)
    sc = Scatter(comm, part, mid, (buf1, buf2, buf3), fin, (gq, gk, gv, go), send_sems, recv_sems, swap_sems)
    plan = Plan()
    some, most = pl.ds(0, PAIR), pl.ds(PAIR, HALF - PAIR)
    loads = [comm.local(s, d) for s, d in ((qt.at[some], two.at[0, some]), (k, ks), (do_t.at[some], two.at[1, some]), (vt, vts), (v, vs), (kt, kts))]
    dkt[...] = jnp.zeros_like(dkt)
    dvt[...] = jnp.zeros_like(dvt)
    with scope('wait_q'):
        for c in loads:
            c.wait()
    loads = [comm.local(s, d) for s, d in ((rt, rts), (qt.at[most], two.at[0, most]), (do_t.at[most], two.at[1, most]))]
    later = [comm.local(s, d) for s, d in ((dyc, dycs), (hidden, xs))]

    def emit(stages):
        for u, stage in stages:
            with scope(f'u{u}_s{stage}'):
                if u == GAIN:
                    sum_gain(stage)
                else:
                    sc.run(u, stage)

    def after(cost):
        plan.now += cost
        return plan.due()

    def head_trades(g):
        row = pl.ds(pl.multiple_of((core * HEADS + DUO * g) * LANES, PAIR), PAIR)
        mine = tile_at(g, PAIR)
        return [pltpu.make_async_remote_copy(src_ref=s, dst_ref=d, send_sem=trade_send.at[i], recv_sem=trade_recv.at[i], device_id=peer, device_id_type=MESH)
                for s, d, i in ((ots.at[row], ots.at[row], g), (dqo.at[mine], dqp.at[mine], PAIRS + g))]

    def gradient(place, count, left, right, mul):
        with scope('grad'):
            @pl.loop(0, DUO)
            def _(z):
                g = mul(left[tile_at(z, HALF), :], right())
                for i in range(count):
                    part[place + i, tile_at(z, DUO)] = g[:, i * LANES:(i + 1) * LANES].reshape(DUO, RING, RING, CHIP, LANES)

    attended, paired = [], []
    for g in range(PAIRS):
        attended.append(after(5.1))
        plan.now += 1.5
        plan.start(DUO * g)
        plan.start(DUO * g + 1)
        paired.append(plan.due())

    @pl.loop(0, PAIRS)
    def _(g):
        def at(table):
            for i in range(PAIRS):
                if table[i]:
                    pl.when(g == i)(functools.partial(emit, table[i]))

        heads = [tile_at(DUO * g + i, LANES) for i in range(DUO)]
        with scope('attend'):
            attend(heads, a1, a2, ks, kts, vs, vts, cos, sin, lambda i: tile_at(core * HEADS + DUO * g + i, LANES), ots, dqo, dkt, dvt, s_scr, e_scr, p_scr, d_scr)

        @pl.when(g == 0)
        def _():
            with scope('entry'):
                comm.meet(CORNERS)
                for c in loads:
                    c.wait()
        for c in head_trades(g):
            c.start()
        at(attended)
        gradient(DUO * g, DUO, rts, lambda: dqo[tile_at(g, PAIR), :], dot_nt)
        at(paired)

    def beat(cost, *starts):
        plan.now += cost
        for u in starts:
            plan.start(u)
        emit(plan.due())

    wkv, wkvp = e_scr.reshape(DIM, PAIR), p_scr.reshape(DIM, PAIR)
    later += [comm.local(src.at[:, pl.ds(at, LANES)], dst.at[:, pl.ds(to, LANES)]) for srcs, dst in (((wqk, wvo), wkv), ((wqkp, wvop), wkvp)) for src, at, to in ((srcs[0], HALF, 0), (srcs[1], 0, LANES))]
    wqp_loads = [comm.local(wqkp.at[tile_at(i, HALF), pl.ds(0, HALF)], two.at[i]) for i in range(DUO)]
    key = dkt[...] * SCALE
    co, si, x, y = cos[...], sin[...], key[:TURN], key[TURN:]
    dkvo[:LANES, :] = jnp.concatenate([x * co + y * si, y * co - x * si], axis=0).astype(bf16)
    dkvo[LANES:, :] = dvt[...].astype(bf16)
    comm.trade(dkvo, dkvp)
    gradient(UNIT_K, DUO, rts, lambda: dkvo[...], dot_nt)
    beat(1.8, UNIT_K, UNIT_V)
    wq_load = comm.local(wqk.at[:, pl.ds(0, HALF)], rts)
    for c in later:
        c.wait()
    with scope('trades'):
        for g in range(PAIRS):
            for c in head_trades(g):
                c.wait()

    waiting = list(range(RING))

    def output_gradients(force=False):
        while waiting:
            first = 10 + DUO * waiting[0]
            before = [u for u in range(N_UNITS) if u < first and PLACE[u] in (PLACE[first], PLACE[first + 1])]
            if force:
                emit(plan.rush(lambda: all(map(plan.vacated, before))))
            if not all(map(plan.vacated, before)):
                return
            for u in before:
                sc.drain(u, 0)
            i = waiting.pop(0)
            gradient(PLACE[first], DUO, ots, lambda: dycs[:, i * PAIR:(i + 1) * PAIR], dot)
            plan.start(first)
            plan.start(first + 1)
            beat(1.5)

    def piece(cost):
        beat(cost)
        output_gradients()

    def ticking(n, cost, body):
        tables = [after(cost) for _ in range(n)]

        @pl.loop(0, n)
        def _(i):
            body(i)
            for j, table in enumerate(tables):
                if table:
                    pl.when(i == j)(functools.partial(emit, table))
        output_gradients()

    @pl.loop(0, TOKENS // LANES)
    def _(i):
        want = lax.broadcasted_iota(jnp.int32, (LANES, ROWS), 0) + i * LANES
        own[tile_at(i, LANES), :] = jnp.where(want == pos[...], 1.0, 0.0).astype(bf16)

    def unsort(at, src_t, n):
        with scope('unsort'):
            dnat[at:at + n, :] = dot(src_t[:n, :], own[...]).astype(bf16)

    output_gradients()
    for c in comm.exchanged:
        c.wait_recv()
    unsort(0, dqo, HALF)
    dy_loads = [comm.local(dy.at[:, tile_at(i, HALF)], dqo.at[tile_at(i, ROWS)]) for i in range(DUO)]
    piece(1.2)
    unsort(HALF, dqp, HALF)
    piece(1.2)
    unsort(DUO * HALF, dkvo, PAIR)
    unsort(DUO * HALF + PAIR, dkvp, PAIR)
    piece(0.7)
    wq_load.wait()
    for c in wqp_loads + dy_loads:
        c.wait()
    gacc[...] = jnp.zeros_like(gacc)

    def dr_parts(half, r):
        return [s_scr.at[half, r(i * PAIR), :] for i in range(RING)]

    def back(block, then):
        def dr(half):
            with scope('dr'):
                c = tile_at(half, HALF)
                left = jnp.concatenate([rts[c, :], two[half], wkv[c, :], wkvp[c, :]], axis=1)
                acc = dot(left, dnat[:, block * PAIR:(block + 1) * PAIR])
                for i, ref in enumerate(dr_parts(half, lambda at: pl.ds(at, PAIR))):
                    ref[...] = acc[i * PAIR:(i + 1) * PAIR, :].T

        def norm(part):
            with scope('back'):
                @pl.loop(0, RING)
                def _(i):
                    j = part * RING + i
                    q = pl.ds(pl.multiple_of(block * PAIR + j * SHARE, SHARE), SHARE)
                    d = jnp.concatenate([ref[...] for half in range(DUO) for ref in dr_parts(half, lambda at: pl.ds(pl.multiple_of(at + j * SHARE, SHARE), SHARE))], axis=1)
                    x = xs[q, :].astype(f32)
                    inv = lax.rsqrt(jnp.mean(x * x, axis=-1, keepdims=True) + RMS_EPS)
                    unit = x * inv
                    gacc[...] += jnp.sum((d * unit).reshape(DUO, SUBS, DIM), axis=0)
                    dg = d * gain[0:1, :]
                    new = inv * (dg - unit * jnp.mean(dg * unit, axis=-1, keepdims=True))
                    for half in range(DUO):
                        r = pl.ds(pl.multiple_of(half * ROWS + block * PAIR + j * SHARE, SHARE), SHARE)
                        dqo[r, :] = (dqo[r, :].astype(f32) + new[:, half * HALF:(half + 1) * HALF]).astype(bf16)

        ticking(DUO, 1.6, dr)
        then()
        ticking(RING, 0.92, norm)

    back(0, lambda: None)
    wo_loads = []
    back(1, lambda: wo_loads.extend([comm.local(wvo.at[:, pl.ds(LANES, HALF)], rts)] + [comm.local(wvop.at[tile_at(i, HALF), pl.ds(LANES, HALF)], two.at[i]) for i in range(DUO)]))
    for i in range(DUO):
        comm.store(dqo.at[tile_at(i, ROWS)], grad_x.at[:, tile_at(i, HALF)])
    total = jnp.sum(gacc[...], axis=0, keepdims=True)
    gpart[...] = jnp.zeros_like(gpart)
    for i in range(RING):
        for j in range(RING):
            gpart[i, j:j + 1, :] = total[:, (i * RING + j) * LANES:(i * RING + j + 1) * LANES]

    gain_c, gain_z, gain_p = (Batch(comm) for _ in range(TRIO))

    def sum_gain(stage):
        if stage == 0:
            gain_c.send(gpart, gpeer, peer)
        elif stage == 1:
            gain_c.arrived(gpeer)
            for j in range(RING):
                gz[j] = gpart[j] + gpeer[j]
            for hop in (1, DUO, TRIO):
                gain_z.send(gz.at[step(comm.pos, 'z', hop)], gz.at[TRIO + hop], comm.far('z', hop))
        elif stage == DUO:
            gain_z.arrived(gz.at[pl.ds(RING, TRIO)])
            gx[0] = (gz[comm.pos['z']] + gz[RING]) + (gz[5] + gz[6])
            for dy, dx in PLANE:
                gain_p.send(gx.at[0], gx.at[dy * RING + dx], comm.aside(dy, dx))
        else:
            gain_p.arrived(gx.at[pl.ds(1, 15)])
            gpeer[0] = jnp.sum(gx[...], axis=0)
            mine = jnp.broadcast_to(gpeer[0, pl.ds(comm.pos['y'], 1), :], (SUBS, LANES))
            gout[...] = pltpu.roll(mine, LANES - (comm.pos['x'] * CHIP + core * SHARE), 1)

    plan.start(GAIN)
    beat(0.2)
    for i in range(DUO):
        with scope('unsort_o'):
            @pl.loop(0, DUO)
            def _(j):
                r = pl.ds(pl.multiple_of(i * HALF + j * ROWS, ROWS), ROWS)
                onat[:, r] = dot(ots[r, :], own[...]).astype(bf16).T
        piece(1.58)
    output_gradients(True)

    def project_out(col, weights, i):
        with scope('project'):
            @pl.loop(DUO * i, DUO * i + DUO)
            def _(j):
                c = tile_at(j, PAIR)
                dst = pl.ds(pl.multiple_of(col + j * PAIR, PAIR), PAIR)
                xs[:, dst] = (xs[:, dst].astype(f32) + dot(onat[...], weights(c))).astype(bf16)
        beat(1.48)

    def own_half(c):
        return rts[:, c]

    def other_half(c):
        return jnp.concatenate([a1[:, c], a2[:, c]], axis=0)

    for c in wo_loads:
        c.wait()
    for col, weights in ((core * HALF, own_half), ((1 - core) * HALF, other_half)):
        for i in range(DUO):
            project_out(col, weights, i)
    comm.store(xs, result)
    emit(plan.rush(lambda: not plan.stage))
    with scope('finish'):
        sc.finish()
        for batch, whole in ((gain_c, gpart), (gain_z, gz.at[pl.ds(RING, TRIO)]), (gain_p, gx.at[pl.ds(1, 15)])):
            batch.sent(whole)
        for c in comm.exchanged:
            c.wait_send()
        for c in comm.stored:
            c.wait()


def tail(qt, do_t, k, kt, v, vt, rt, dyc, wqk, wqkp, wvo, wvop, gain, hidden, dy, pos, cos, sin):
    bf16, f32 = jnp.bfloat16, jnp.float32
    any_ = pl.BlockSpec(memory_space=pl.ANY)
    vmem = pl.BlockSpec(memory_space=pltpu.VMEM)
    S = lambda shape, d=bf16: jax.ShapeDtypeStruct(shape, d)
    V = lambda shape, d=bf16: pltpu.VMEM(shape, d)
    D = lambda n: pltpu.SemaphoreType.DMA((n,))
    sq, tall, wide = (HALF, TOKENS), (TOKENS, LANES), (LANES, TOKENS)
    mine, kv = (ROWS, DIM), (PAIR, TOKENS)
    return pl.pallas_call(
        tail_kernel,
        out_shape=[S(mine), S(mine), S((SHARE, DIM), f32), S((SHARE, PAIR), f32), S((SHARE, PAIR), f32), S((SHARE, DIM), f32), S((SUBS, LANES), f32)],
        in_specs=[any_] * 12 + [vmem] + [any_] * DUO + [vmem] * TRIO,
        out_specs=[any_] * 6 + [vmem],
        scratch_shapes=[V((DUO,) + sq), V(tall), V(wide), V(tall), V(wide), V((DIM, TOKENS)), V((DIM, TOKENS)), V(sq), V(sq), V(kv), V(kv), V(wide, f32), V(wide, f32),
                        V((DUO, TOKENS, QB), f32), V((DUO, TOKENS, QB)), V((DUO, TOKENS, QB)), V((DUO, TOKENS, QB)), V(sq), V((PLACES, RING, RING, RING, CHIP, LANES), f32), V((TRIO, SLOTS, RING, RING, CHIP, LANES), f32),
                        V((TRIO, SLOTS, 6, RING, RING, SHARE, LANES), f32), V((TRIO, SLOTS, 6, RING, SHARE, LANES), f32), V((TRIO, SLOTS, TRIO, CHIP, LANES), f32), V((N_UNITS, CHIP, LANES), f32), V((TOKENS, ROWS)), V(mine), V((DUO * QKV, ROWS)), V(mine),
                        V((SUBS, DIM), f32), V((RING, SUBS, LANES), f32), V((RING, SUBS, LANES), f32), V((7, SUBS, LANES), f32), V((SHARE, SUBS, LANES), f32),
                        D(9 * SLOTS), D(15 * SLOTS), D(DUO + N_UNITS), D(HEADS + RING), D(HEADS + RING), D(26)],
        compiler_params=pltpu.CompilerParams(collective_id=1, has_side_effects=True, vmem_limit_bytes=67043328),
        name='tail',
    )(qt, do_t, k, kt, v, vt, rt, dyc, wqk, wqkp, wvo, wvop, gain, hidden, dy, pos, cos, sin)


def settle_kernel(n, *refs):
    ins, gain, outs, gain_out, bufs, sems = refs[:n], refs[n], refs[n + 1:DUO * n + 1], refs[DUO * n + 1], refs[DUO * n + DUO:-1], refs[-1]
    jobs = []
    for a, o, b in zip(ins, outs, bufs):
        size = a.shape[0] // RING if a.shape[0] == ROWS else a.shape[0]
        jobs += [tuple(r.at[pl.ds(i, size)] for r in (a, b, o)) for i in range(0, a.shape[0], size)]
    takes = [pltpu.make_async_copy(a, b, sems.at[0, i]) for i, (a, b, _) in enumerate(jobs)]
    puts = [pltpu.make_async_copy(b, o, sems.at[1, i]) for i, (_, b, o) in enumerate(jobs)]
    for c in takes:
        c.start()
    gain_out[...] = gain[0:1, :SHARE]
    for take, put in zip(takes, puts):
        take.wait()
        put.start()
    for c in puts:
        c.wait()


def settle(*arrays):
    *large, gain = arrays
    any_, vmem = pl.BlockSpec(memory_space=pl.ANY), pl.BlockSpec(memory_space=pltpu.VMEM)
    return pl.pallas_call(
        functools.partial(settle_kernel, len(large)),
        out_shape=[jax.ShapeDtypeStruct(a.shape, a.dtype) for a in large] + [jax.ShapeDtypeStruct((1, SHARE), gain.dtype)],
        in_specs=[any_] * len(large) + [vmem],
        out_specs=[any_] * len(large) + [vmem],
        scratch_shapes=[pltpu.VMEM(a.shape, a.dtype) for a in large] + [pltpu.SemaphoreType.DMA((DUO, 12))],
        name='settle',
    )(*arrays)


def rope_tables():
    j = np.arange(HEAD_DIM // DUO, dtype=np.float64) / (HEAD_DIM // DUO)
    freq = (ROPE_THETA ** -j).astype(np.float32)
    angle = freq[:, None] * np.arange(TOKENS, dtype=np.float32)[None, :]
    return np.cos(angle.astype(np.float64)).astype(np.float32), np.sin(angle.astype(np.float64)).astype(np.float32)


def solution(mesh):
    def shard_fn(hidden, tok_pos, grad_out, norm_gain, w_query, w_key, w_value, w_out):
        hidden, grad_out = hidden[0], grad_out[0]
        cos_t, sin_t = (jnp.asarray(t) for t in rope_tables())
        *parts, gain = head(hidden, grad_out, w_query, w_key, w_value, w_out, tok_pos, norm_gain.reshape(1, SHARE), cos_t, sin_t)
        parts = [p.reshape(DIM, GROUP) if p.ndim > DUO else p for p in parts]
        result, grad_hidden, gq, gk, gv, go, gout = settle(*tail(*parts, gain, hidden, grad_out, tok_pos, cos_t, sin_t))
        return result[None], grad_hidden[None], gq, gk, gv, go, gout.reshape(SHARE)

    row_spec, pos_spec = P('fsdp', 'cp', None), P('fsdp', 'cp')
    weight_spec, gain_spec = P(('fsdp', 'cp'), None), P(('fsdp', 'cp'))
    return jax.shard_map(shard_fn, mesh=mesh, in_specs=(row_spec, pos_spec, row_spec, gain_spec, weight_spec, weight_spec, weight_spec, weight_spec), out_specs=(row_spec, row_spec, weight_spec, weight_spec, weight_spec, weight_spec, gain_spec), check_vma=False)
```

```python
import functools
import jax
import jax.numpy as jnp
import numpy as np
from jax import lax
from jax.experimental import pallas as pl
from jax.experimental.pallas import tpu as pltpu
from jax.sharding import PartitionSpec as P

LANES, SUBS, RING, TRIO, DUO = 128, 8, 4, 3, 2
PAIR, ROWS, CHIP, SHARE, TURN = 256, 512, 32, 16, 64
HEAD_DIM = LANES
ROPE_THETA = 1000000.0
RMS_EPS = 1e-5
SCALE = HEAD_DIM ** -0.5
LOG2E = 1.4426950408889634

MESH = pl.DeviceIdType.MESH
AXES = ('x', 'y', 'z')
ORDERS = (('x', 'y', 'z'), ('y', 'z', 'x'), ('z', 'x', 'y'))
ALL = pl.ds(0, RING)


def torus():
    f = lax.axis_index('fsdp')
    return {'x': lax.rem(f, RING), 'y': lax.rem(lax.div(f, RING), RING), 'z': lax.div(f, SHARE)}


def step(pos, axis, hop):
    return lax.rem(pos[axis] + hop, RING)


class Batch:
    def __init__(self, comm):
        self.comm, self.index = comm, comm.used
        comm.used += 1

    def _copy(self, src, dst, device):
        send, recv, _ = self.comm.sems
        return pltpu.make_async_remote_copy(src_ref=src, dst_ref=dst, send_sem=send.at[self.index], recv_sem=recv.at[self.index], device_id=device, device_id_type=MESH)

    def send(self, src, dst, device):
        self._copy(src, dst, device).start()
        return self

    def arrived(self, whole):
        self._copy(whole, whole, self.comm.peer()).wait_recv()

    def sent(self, whole):
        self._copy(whole, whole, self.comm.peer()).wait_send()


class Comm:
    def __init__(self, send_sems, recv_sems, local_sems):
        self.pos = torus()
        self.core = lax.axis_index('cp')
        self.sems = (send_sems, recv_sems, local_sems)
        self.used = self.used_local = 0
        self.stored = []

    def far(self, axis, hop):
        p = dict(self.pos)
        p[axis] = step(self.pos, axis, hop)
        return {'fsdp': (p['z'] * RING + p['y']) * RING + p['x'], 'cp': self.core}

    def peer(self):
        return {'fsdp': lax.axis_index('fsdp'), 'cp': 1 - self.core}

    def aside(self, dy, dx):
        return {'fsdp': (self.pos['z'] * RING + step(self.pos, 'y', dy)) * RING + step(self.pos, 'x', dx), 'cp': self.core}

    def announce(self, corners=()):
        sem = pltpu.get_barrier_semaphore()
        for axis in AXES:
            for hop in (1, DUO, TRIO):
                pl.semaphore_signal(sem, inc=1, device_id=self.far(axis, hop), device_id_type=MESH)
        for dy, dx in corners:
            pl.semaphore_signal(sem, inc=1, device_id=self.aside(dy, dx), device_id_type=MESH)
        pl.semaphore_signal(sem, inc=1, device_id=self.peer(), device_id_type=MESH)

    def meet(self, corners=()):
        pl.semaphore_wait(pltpu.get_barrier_semaphore(), 10 + len(corners))

    def ring(self, batch, src, slots, axis):
        for hop in (1, DUO, TRIO):
            batch.send(src, slots.at[hop], self.far(axis, hop))

    def local(self, src, dst):
        i = self.used_local
        self.used_local += 1
        c = pltpu.make_async_copy(src, dst, self.sems[DUO].at[i])
        c.start()
        return c

    def store(self, src, dst):
        self.stored.append(self.local(src, dst))


class Singles(Comm):
    def __init__(self, *sems):
        super().__init__(*sems)
        self.sent, self.exchanged = [], []

    def _copy(self, src, dst, device):
        i = self.used
        self.used += 1
        c = pltpu.make_async_remote_copy(src_ref=src, dst_ref=dst, send_sem=self.sems[0].at[i], recv_sem=self.sems[1].at[i], device_id=device, device_id_type=MESH)
        c.start()
        return c

    def send(self, src, dst, device):
        c = self._copy(src, dst, device)
        self.sent.append(c)
        return c

    def trade(self, src, dst):
        self.exchanged.append(self._copy(src, dst, self.peer()))


def pick(ref, sel, piece):
    lo, cols, first, rows = piece
    return ref.at[sel['z'], sel['y'], sel['x'], pl.ds(first, rows), pl.ds(lo, cols)]


def sem_scratch(remote, local):
    return [pltpu.SemaphoreType.DMA((remote,)), pltpu.SemaphoreType.DMA((remote,)), pltpu.SemaphoreType.DMA((local,))]


def add_into(dst, *srcs, fresh=False):
    def add(idx):
        total, *rest = [s[idx] for s in (srcs if fresh else (dst,) + srcs)]
        for more in rest:
            total = total + more
        dst[idx] = total

    if len(dst.shape) > TRIO:
        @pl.loop(0, dst.shape[0])
        def _(i):
            add((i,))
    else:
        add(Ellipsis)


def columns(lo, na, nb):
    return (lo, na, 0, CHIP), (lo + na, nb, 0, CHIP)


def strip(lo):
    return (lo, LANES, 0, SHARE), (lo, LANES, SHARE, SHARE)


QK_COLORS = (columns(0, PAIR, LANES), columns(384, LANES, PAIR), columns(768, PAIR, LANES))
VO_COLORS = (columns(0, LANES, PAIR), columns(384, PAIR, LANES), columns(768, LANES, PAIR))
QK_FIRST = (columns(0, LANES, LANES), columns(384, LANES, LANES), columns(768, LANES, LANES))
QK_LAST = (strip(PAIR), strip(640), strip(1024))
TOKENS = 1024
DIM = 2048
HALF = 1024
QKV = 1280
GROUP = 1152


def scope(name):
    return jax.named_scope(name)


def dot(a, b):
    return jnp.dot(a, b, preferred_element_type=jnp.float32)


def dot_nt(a, b):
    return lax.dot_general(a, b, (((1,), (1,)), ((), ())), preferred_element_type=jnp.float32)


def tile_at(i, n):
    return pl.ds(pl.multiple_of(i * n, n), n)


class Gather:
    def __init__(self, comm, ref, colors, land, held=None):
        self.comm, self.ref, self.colors, self.land = comm, ref, colors, land
        self.held = list(held or [dict(comm.pos) for _ in colors])
        self.spent = []

    def move(self, batch, s, piece, to):
        batch.send(pick(self.ref, s, piece), pick(self.ref, s, piece), to)

    def at(self, k, hop):
        d = ORDERS[k][self.phase]
        return dict(self.held[k], **{d: step(self.comm.pos, d, hop)})

    def begin(self, phase):
        self.phase = phase
        self.rest = Batch(self.comm)
        if phase == 0:
            for hop in (DUO, 1, TRIO):
                for k, (a, b) in enumerate(self.colors):
                    self.move(self.rest, self.held[k], (a[0], a[1] + b[1], 0, CHIP), self.comm.far(ORDERS[k][0], hop))
            return
        self.up, self.dn = ([Batch(self.comm) for _ in range(TRIO)] for _ in range(DUO))
        for k, (a, b) in enumerate(self.colors):
            d = ORDERS[k][phase]
            up, dn, s = self.comm.far(d, 1), self.comm.far(d, TRIO), self.held[k]
            self.move(self.up[k], s, a, up)
            self.move(self.dn[k], s, b, dn)
            self.move(self.rest, s, b, up)
            self.move(self.rest, s, a, dn)
        if phase == DUO:
            for k, pieces in enumerate(self.colors):
                for piece in pieces:
                    self.land(self.ref, self.held[k], piece)

    def forward(self):
        for k, (a, b) in enumerate(self.colors):
            d = ORDERS[k][self.phase]
            for batch, hop, piece, to in ((self.up[k], TRIO, a, 1), (self.dn[k], 1, b, TRIO)):
                s = self.at(k, hop)
                batch.arrived(pick(self.ref, s, piece))
                self.move(self.rest, s, piece, self.comm.far(d, to))
                if self.phase == DUO:
                    self.land(self.ref, s, piece)
                self.spent.append((batch, pick(self.ref, self.held[k], piece)))

    def end(self):
        axis = ORDERS[0][self.phase]
        blocks = dict(self.held[0], **{axis: pl.ds(0, DUO if self.phase else TRIO)})
        width = sum(max(a[0] + a[1], b[0] + b[1]) - a[0] for a, b in self.colors)
        whole = pick(self.ref, blocks, (0, width, 0, CHIP))
        self.rest.arrived(whole)
        self.spent.append((self.rest, whole))
        for k, (a, b) in enumerate(self.colors):
            if self.phase == DUO:
                for hop, piece in ((TRIO, b), (1, a), (DUO, a), (DUO, b)):
                    self.land(self.ref, self.at(k, hop), piece)
            self.held[k] = dict(self.held[k], **{ORDERS[k][self.phase]: ALL})

    def finish(self):
        for batch, whole in self.spent:
            batch.sent(whole)


def head_kernel(hidden, dy, wq, wk, wv, wo, pos, gain_in, cos_t, sin_t,
                qt_o, dot_o, k_o, kt_o, v_o, vt_o, rt_o, dyc_o, wqk_o, wqkp_o, wvo_o, wvop_o, gain_o,
                hid2, dy2, dys, rs, rt, wqk, wvo, wpeer, pi, pos2, qt, dot_s, kk, kt, vv, vt, gain, gtile, gbuf, gx, gy, gz, *sems):
    comm = Comm(*sems)
    pos_c, core = comm.pos, comm.core
    bf16, f32 = jnp.bfloat16, jnp.float32
    peer = comm.peer()
    rows = tile_at(core, SHARE)
    mine_qk = wqk.at[pos_c['z'], pos_c['y'], pos_c['x'], rows]
    mine_vo = wvo.at[pos_c['z'], pos_c['y'], pos_c['x'], rows]

    def weight_parts(c):
        return ((wq.at[:, tile_at(c, HALF)], mine_qk.at[:, pl.ds(0, HALF)]), (wk.at[:, tile_at(c, LANES)], mine_qk.at[:, pl.ds(HALF, LANES)]),
                (wv.at[:, tile_at(c, LANES)], mine_vo.at[:, pl.ds(0, LANES)]), (wo.at[:, tile_at(c, HALF)], mine_vo.at[:, pl.ds(LANES, HALF)]))

    loads = [comm.local(s, d) for s, d in weight_parts(core)]
    load_x = [comm.local(hidden, hid2.at[pl.ds(0, ROWS)]), comm.local(dy, dy2.at[pl.ds(0, ROWS)])]
    share = lax.broadcasted_iota(jnp.int32, (SUBS, LANES), 1) // SHARE
    gtile[...] = jnp.where(share == pos_c['x'] * DUO + core, jnp.broadcast_to(jnp.concatenate([gain_in[...]] * SUBS, axis=1), (SUBS, LANES)), 0.0)
    comm.announce()
    with scope('entry'):
        comm.meet()
    swap_w, swap_pos, swap_dy, swap_x, peers_qk, peers_vo = (Batch(comm) for _ in range(6))
    gain_c, gain_x, gain_y, gain_z = (Batch(comm) for _ in range(RING))
    for s, d in weight_parts(1 - core):
        swap_w.send(s, d, peer)
    gain_c.send(gtile, gbuf, peer)
    swap_pos.send(pos, pos2, peer)
    for c in loads:
        c.wait()
    with scope('wait_w'):
        swapped = wqk.at[pos_c['z'], pos_c['y'], pos_c['x']]
        swap_w.arrived(swapped)

    def land_qk(ref, s, cols):
        peers_qk.send(pick(ref, s, cols), pick(wqkp_o, s, cols), peer)

    def land_vo(ref, s, cols):
        peers_vo.send(pick(ref, s, cols), pick(wpeer, s, cols), peer)

    g1 = Gather(comm, wvo, VO_COLORS, land_vo)
    g2 = Gather(comm, wqk, QK_COLORS, land_qk)
    g1.begin(0)
    g2.begin(0)
    gain_c.arrived(gbuf)
    gx[0] = gtile[...] + gbuf[...]
    comm.ring(gain_x, gx.at[0], gx, 'x')

    swap_pos.arrived(pos2)

    @pl.loop(0, TOKENS // LANES)
    def _(i):
        want = lax.broadcasted_iota(jnp.int32, (LANES, ROWS), 0) + i * LANES
        for h, have in enumerate((pos, pos2)):
            pi[tile_at(i, LANES), h * ROWS:(h + 1) * ROWS] = jnp.where(want == have[...], 1.0, 0.0).astype(bf16)

    def sort(dst, src, first, last):
        with scope('sort'):
            @pl.loop(first, last)
            def _(j):
                c = tile_at(j, PAIR)
                dst[:, c] = dot(pi[...], src[:, c]).astype(bf16)

    swap_dy.send(dy, dy2.at[pl.ds(ROWS, ROWS)], peer)
    with scope('p0_end'):
        for g in (g1, g2):
            g.end()
            g.begin(1)
    swap_x.send(hidden, hid2.at[pl.ds(ROWS, ROWS)], peer)
    gain_x.arrived(gx.at[pl.ds(1, TRIO)])
    gy[pos_c['y']] = (gx[0] + gx[1]) + (gx[DUO] + gx[TRIO])
    for hop in (1, DUO, TRIO):
        gain_y.send(gy.at[pos_c['y']], gy.at[pos_c['y']], comm.far('y', hop))
    with scope('wait_dy'):
        load_x[1].wait()
        swap_dy.arrived(dy2.at[pl.ds(ROWS, ROWS)])
    sort(dys, dy2, 0, RING)
    with scope('p1a_fwd'):
        g1.forward()
    sort(dys, dy2, RING, 6)
    with scope('p1b_fwd'):
        g2.forward()
    sort(dys, dy2, 6, SUBS)
    with scope('p1a_end'):
        g1.end()
    gain_y.arrived(gy.at[pl.ds(1, TRIO)])
    for j in range(RING):
        gz[pos_c['z'], j] = gy[j]
    for hop in (1, DUO, TRIO):
        gain_z.send(gz.at[pos_c['z']], gz.at[pos_c['z']], comm.far('z', hop))
    g1.begin(DUO)
    comm.store(dys.at[:, tile_at(core, HALF)], dyc_o)
    with scope('p1b_end'):
        g2.end()
    with scope('wait_x'):
        load_x[0].wait()
        swap_x.arrived(hid2.at[pl.ds(ROWS, ROWS)])
    sort(rs, hid2, 0, SUBS)
    with scope('p2q_fwd'):
        g1.forward()
    g2a, g2b = (Gather(comm, wqk, colors, land_qk, g2.held) for colors in (QK_FIRST, QK_LAST))
    g2a.begin(DUO)
    with scope('gain'):
        gain_z.arrived(gz.at[pl.ds(1, TRIO)])
    for i in range(RING):
        for j in range(RING):
            gain[:, (i * RING + j) * LANES:(i * RING + j + 1) * LANES] = gz[i, j]
    comm.store(gain, gain_o)

    def norm(first, last):
        with scope('norm'):
            @pl.loop(first, last)
            def _(i):
                r = tile_at(i, CHIP)
                x = rs[r, :].astype(f32)
                inv = lax.rsqrt(jnp.mean(x * x, axis=-1, keepdims=True) + RMS_EPS)
                rs[r, :] = (x * inv * gain[0:1, :]).astype(bf16)

    norm(0, TOKENS // CHIP)
    with scope('r_t'):
        @pl.loop(0, DIM // PAIR)
        def _(i):
            c = tile_at(i, PAIR)

            @pl.loop(0, TOKENS // PAIR)
            def _(j):
                r = tile_at(j, PAIR)
                rt[c, r] = rs[r, c].T
    comm.store(rt, rt_o)
    with scope('p2o_end'):
        g1.end()
    w_qk, w_vo, w_peer = wqk.reshape(DIM, GROUP), wvo.reshape(DIM, GROUP), wpeer.reshape(DIM, GROUP)
    with scope('vals'):
        @pl.loop(0, DUO)
        def _(i):
            r = tile_at(i, ROWS)
            val = dot(rs[r, :], w_vo[:, :LANES]).astype(bf16)
            vv[r, :] = val
            vt[:, r] = val.T
    for src, dst in ((wvo, wvo_o), (vv, v_o), (vt, vt_o)):
        comm.store(src, dst)
    with scope('p2q_fwd'):
        g2a.forward()
    g2b.begin(DUO)
    with scope('wo_peer'):
        peers_vo.arrived(wpeer)
    comm.store(wpeer, wvop_o)
    with scope('do_t'):
        mine = tile_at(core, HALF)

        @pl.loop(0, TOKENS // PAIR)
        def _(j):
            t = tile_at(j, PAIR)
            w_rows = jnp.concatenate([w_vo[mine, LANES:], w_peer[mine, LANES:]], axis=1)
            d_rows = jnp.concatenate([dys[t, mine], dys[t, tile_at(1 - core, HALF)]], axis=1)
            dot_s[:, t] = dot_nt(w_rows, d_rows).astype(bf16)
    comm.store(dot_s, dot_o)

    def rotated(x, r):
        cos, sin = cos_t[:, r], sin_t[:, r]
        cos = jnp.concatenate([cos, cos], axis=0).T
        sin = jnp.concatenate([-sin, sin], axis=0).T
        return (x * cos + pltpu.roll(x, TURN, 1) * sin).astype(bf16)

    def queries(columns, heads):
        x = dot(rs[...], columns)
        for i in range(RING):
            r = slice(i * PAIR, (i + 1) * PAIR)
            for h, head in enumerate(heads):
                qt[tile_at(head, LANES), r] = rotated(x[r, h * LANES:(h + 1) * LANES], r).T

    with scope('p2q_end'):
        g2a.end()

    def pairs(first, last):
        with scope('q'):
            @pl.loop(first, last)
            def _(t):
                queries(w_qk[:, pl.ds(pl.multiple_of(t * 384, LANES), PAIR)], (TRIO * t, TRIO * t + 1))

    pairs(0, 1)
    with scope('last_fwd'):
        g2b.forward()
    pairs(1, TRIO)
    for t in range(TRIO):
        two_heads = pl.ds(t * 384, PAIR)
        comm.store(qt.at[two_heads], qt_o.at[two_heads])
    with scope('last_end'):
        g2b.end()
    comm.store(wqk, wqk_o)
    with scope('q_last'):
        x = dot(rs[...], jnp.concatenate([w_qk[:, PAIR:384], w_qk[:, 640:768], w_qk[:, HALF:]], axis=1))
        for i in range(RING):
            r = slice(i * PAIR, (i + 1) * PAIR)
            key = rotated(x[r, PAIR:], r)
            kk[r, :] = key
            kt[:, r] = key.T
            for h, head in enumerate((DUO, 5)):
                qt[tile_at(head, LANES), r] = rotated(x[r, h * LANES:(h + 1) * LANES], r).T
    for src, dst in ((kk, k_o), (kt, kt_o)) + tuple((qt.at[tile_at(h, LANES)], qt_o.at[tile_at(h, LANES)]) for h in (DUO, 5)):
        comm.store(src, dst)
    with scope('finish'):
        peers_qk.arrived(wqk)
        for batch, whole in ((swap_w, swapped), (swap_pos, pos2), (swap_dy, dy2.at[pl.ds(ROWS, ROWS)]), (swap_x, hid2.at[pl.ds(ROWS, ROWS)]), (peers_qk, wqk), (peers_vo, wvo),
                             (gain_c, gbuf), (gain_x, gx.at[pl.ds(1, TRIO)]), (gain_y, gy.at[pl.ds(1, TRIO)]), (gain_z, gz.at[pl.ds(1, TRIO)])):
            batch.sent(whole)
        for g in (g1, g2, g2a, g2b):
            g.finish()
        for c in comm.stored:
            c.wait()


def head(hidden, dy, wq, wk, wv, wo, pos, gain, cos_t, sin_t):
    bf16, f32 = jnp.bfloat16, jnp.float32
    any_ = pl.BlockSpec(memory_space=pl.ANY)
    vmem = pl.BlockSpec(memory_space=pltpu.VMEM)
    S = lambda shape, d=bf16: jax.ShapeDtypeStruct(shape, d)
    V = lambda shape, d=bf16: pltpu.VMEM(shape, d)
    group = (RING, RING, RING, CHIP, GROUP)
    sq, tall, wide = (HALF, TOKENS), (TOKENS, LANES), (LANES, TOKENS)
    full = (TOKENS, DIM)
    return pl.pallas_call(
        head_kernel,
        out_shape=[S(sq), S(sq), S(tall), S(wide), S(tall), S(wide), S((DIM, TOKENS)), S((TOKENS, HALF)), S(group), S(group), S(group), S(group), S((SUBS, DIM), f32)],
        in_specs=[any_] * 6 + [vmem] * RING,
        out_specs=[any_] * 13,
        scratch_shapes=[V(full), V(full), V(full), V(full), V((DIM, TOKENS)), V(group), V(group), V(group), V((TOKENS, TOKENS)), V((1, ROWS), jnp.int32),
                        V(sq), V(sq), V(tall), V(wide), V(tall), V(wide), V((SUBS, DIM), f32), V((SUBS, LANES), f32), V((SUBS, LANES), f32), V((RING, SUBS, LANES), f32), V((RING, SUBS, LANES), f32), V((RING, RING, SUBS, LANES), f32)] + sem_scratch(47, 22),
        compiler_params=pltpu.CompilerParams(collective_id=0, has_side_effects=True, vmem_limit_bytes=60 * DUO**20),
        name='head',
    )(hidden, dy, wq, wk, wv, wo, pos, gain, cos_t, sin_t)


HEADS = SUBS
UNIT_K, UNIT_V = SUBS, 9
N_UNITS = 18
GAIN = N_UNITS
SLOTS = RING
LAST = 5
ABREAST = DUO
LINES = ((0, TRIO, 6, 9, 12, 15), (1, RING, 7, 10, 13, SHARE), (DUO, 5, SUBS, 11, 14, 17))
COLOR = {u: k for k, line in enumerate(LINES) for u in line}
RANK = {u: i for line in LINES for i, u in enumerate(line)}
SWAPPED = (1, TRIO, RING, SUBS, 10)
ORDER = {u: ORDERS[k] if u not in SWAPPED else (ORDERS[k][0], ORDERS[k][DUO], ORDERS[k][1]) for u, k in COLOR.items()}
BEFORE = {u: line[i - SLOTS] if i >= SLOTS else None for line in LINES for i, u in enumerate(line)}
PLACES = 12
PLACE = {u: u % PLACES for u in range(N_UNITS)}
WIRE = (2.82, 0.71, 0.36)
LATENCY = 2.4
STAGE_COST = 0.08


class Plan:
    def __init__(self):
        self.now, self.stage, self.ready, self.order, self.link = 0.0, {}, {}, [], {}
        self.mark = {}

    def _wire(self, u, phase, count):
        link = ORDER[u][phase]
        t = max(self.link.get(link, 0.0), self.now)
        first = t + WIRE[phase] + LATENCY
        self.link[link] = t + WIRE[phase] * count
        return first if phase < DUO else self.link[link] + LATENCY

    def free(self, u, phase):
        if BEFORE[u] is None:
            return True
        done = self.mark.get((BEFORE[u], (DUO, RING, 5)[phase]))
        if done is None:
            return False
        sent = ((0, 1), (DUO, TRIO), (RING,))[phase]
        return any(self.mark.get((j, s), -1) > done and (j, s + 1) in self.mark for j, order in ORDER.items() if order[phase] == ORDER[u][phase] for s in sent)

    def run(self, u):
        stage = self.stage[u]
        self.order.append((u, stage))
        self.mark[u, stage] = len(self.order)
        self.now = max(self.now, self.ready[u]) + STAGE_COST
        self.stage[u] = stage + 1
        if stage == (TRIO if u == GAIN else LAST):
            del self.stage[u]
        elif u == GAIN:
            self.ready[u] = max([self.now] + [self.link.get(a, 0.0) for a in ('', 'z', 'xy')[stage]]) + DUO * LATENCY
        elif stage % DUO:
            self.ready[u] = self._wire(u, stage // DUO, 1)
        else:
            self.ready[u] = self._wire(u, stage // DUO, DUO)

    def blocked(self, u):
        stage = self.stage[u]
        if u == GAIN:
            return False
        if stage == 0 and sum(0 < self.stage.get(j, 0) <= DUO for j in LINES[COLOR[u]]) >= ABREAST:
            return True
        if stage == DUO and BEFORE[u] is not None and (BEFORE[u], LAST) not in self.mark:
            return True
        return stage in (0, DUO, RING) and not self.free(u, stage // DUO)

    def start(self, u):
        self.stage[u], self.ready[u] = 0, self.now

    def due(self):
        first = len(self.order)
        while True:
            ripe = [(self.ready[u], u) for u in self.stage if self.ready[u] <= self.now and not self.blocked(u)]
            if not ripe:
                return self.order[first:]
            self.run(min(ripe)[1])

    def vacated(self, u):
        return (u, DUO) in self.mark

    def rush(self, done):
        first = len(self.order)
        while not done():
            self.run(min((self.ready[u], u) for u in self.stage if not self.blocked(u))[1])
        return self.order[first:]


QB = PAIR
PAIRS = HEADS // DUO
NBLK = TOKENS // QB
HALVES = (pl.ds(0, SHARE), pl.ds(SHARE, SHARE))
PLANE = tuple((dy, dx) for dy in range(RING) for dx in range(RING) if dy or dx)
CORNERS = tuple((dy, dx) for dy, dx in PLANE if dy and dx)


class Scatter:
    def __init__(self, comm, part, mid, bufs, fin, outs, send_sems, recv_sems, swap_sems):
        self.pos, self.part, self.mid, self.bufs, self.fin, self.outs = comm.pos, part, mid, bufs, fin, outs
        self.send_sems, self.recv_sems, self.swap_sems = send_sems, recv_sems, swap_sems
        self.near = {(a, hop): comm.far(a, hop) for a in AXES for hop in (1, DUO, TRIO)}
        self.hops = {(a, hop): step(comm.pos, a, hop) for a in AXES for hop in (1, DUO, TRIO)}
        self.peer, self.core = comm.peer(), comm.core
        self.keep, self.give = tile_at(comm.core, SHARE), tile_at(1 - comm.core, SHARE)
        self.drained = set()

    def slot(self, u):
        return COLOR[u], RANK[u] % SLOTS

    def buf(self, u, phase):
        return self.bufs[phase].at[self.slot(u)]

    def view(self, u, phase, hop, half=None):
        order = ORDER[u]
        at = {a: ALL for a in AXES}
        for a in order[1:phase]:
            at[a] = self.pos[a]
        at[order[phase]] = self.hops[order[phase], hop] if hop else self.pos[order[phase]]
        rows = pl.ds(0, CHIP) if half is None else HALVES[half]
        if phase == 0:
            return self.part.at[PLACE[u], at['z'], at['y'], at['x'], rows, :]
        return self.mid.at[self.slot(u) + tuple(at[a] for a in 'zyx' if a != order[0]) + (rows, slice(None))]

    def copy(self, src, dst, sems, device):
        return pltpu.make_async_remote_copy(src_ref=src, dst_ref=dst, send_sem=sems[0], recv_sem=sems[1], device_id=device, device_id_type=MESH)

    def sems(self, u, phase, kind=0):
        k, i = self.slot(u)
        at = (k * SLOTS + i) * TRIO + phase
        return self.send_sems.at[at], self.recv_sems.at[(k * SLOTS + i) * 5 + DUO * phase + kind]

    def send(self, u, phase, name):
        axis = ORDER[u][phase]
        if phase == DUO:
            src, to = self.view(u, DUO, name + 1), name + 1
        else:
            hop, half, to = ((DUO, 0, 1), (DUO, 1, TRIO), (1, 1, 1), (TRIO, 0, TRIO), (1, 0, 1), (TRIO, 1, TRIO))[name]
            src = self.view(u, phase, hop, half)
        self.copy(src, self.buf(u, phase).at[name], self.sems(u, phase, int(name > 1 and phase < DUO)), self.near[axis, to]).start()

    def launch(self, u, phase):
        if BEFORE[u] is not None:
            self.drain(BEFORE[u], phase)
        for name in range(RING if phase < DUO else TRIO):
            self.send(u, phase, name)

    def arrived(self, u, phase, first, count):
        whole = self.buf(u, phase).at[pl.ds(first, count)]
        self.copy(whole, whole, self.sems(u, phase, int(first > 0)), self.peer).wait_recv()

    def drain(self, u, phase):
        if (u, phase) not in self.drained:
            self.drained.add((u, phase))
            whole = self.buf(u, phase)
            self.copy(whole, whole, self.sems(u, phase), self.peer).wait_send()

    def out(self, u):
        if u < HEADS:
            out, col = self.outs[0], self.core * HALF + u * LANES
        elif u < 10:
            out, col = self.outs[u - 7], self.core * LANES
        else:
            out, col = self.outs[TRIO], self.core * HALF + (u - 10) * LANES
        return out.at[:, pl.ds(pl.multiple_of(col, LANES), LANES)]

    def kept(self, u):
        return pltpu.make_async_copy(self.fin.at[u, self.keep], self.out(u), self.swap_sems.at[DUO + u])

    def run(self, u, stage):
        if stage == 0:
            return self.launch(u, 0)
        phase = (stage - 1) // DUO
        if stage == LAST:
            self.arrived(u, DUO, 0, TRIO)
            got = self.buf(u, DUO)
            self.fin[u] = self.view(u, DUO, 0)[...] + (got[0] + got[1] + got[DUO])
            self.copy(self.fin.at[u, self.give], self.out(u), (self.swap_sems.at[0], self.swap_sems.at[1]), self.peer).start()
            self.kept(u).start()
            return
        got = self.buf(u, phase)
        if stage % DUO:
            self.arrived(u, phase, 0, DUO)
            for name, hop in ((0, 1), (1, TRIO)):
                add_into(self.view(u, phase, hop, name), got.at[name])
                self.send(u, phase, name + RING)
            return
        self.arrived(u, phase, DUO, RING)
        if phase == 0 and BEFORE[u] is not None:
            self.drain(BEFORE[u], 1)
            self.drain(BEFORE[u], DUO)
        for half, names in ((0, (TRIO, RING)), (1, (DUO, 5))):
            if phase:
                add_into(self.view(u, phase, 0, half), *[got.at[name] for name in names])
            else:
                dst = self.mid.at[self.slot(u) + (ALL, ALL, HALVES[half], slice(None))]
                add_into(dst, self.view(u, 0, 0, half), *[got.at[name] for name in names], fresh=True)
        self.launch(u, phase + 1)

    def finish(self):
        for u in range(N_UNITS):
            for phase in range(TRIO):
                self.drain(u, phase)
        half = self.fin.at[:, pl.ds(0, SHARE)]
        swaps = self.copy(half, half, (self.swap_sems.at[0], self.swap_sems.at[1]), self.peer)
        swaps.wait_send()
        swaps.wait_recv()
        for u in range(N_UNITS):
            self.kept(u).wait()


def attend(heads, qt, do_t, k, kt, v, vt, cos, sin, o_row, ot, dq, dkt, dvt, s_scr, e_scr, p_scr, d_scr):
    f32, bf16 = jnp.float32, jnp.bfloat16
    strip = TURN
    work = [(h, j) for j in range(NBLK) for h in range(len(heads))]

    def strips(c):
        return [(i * strip, slice(c * QB + i * strip, c * QB + (i + 1) * strip)) for i in range(QB // strip)]

    def fold(x, op):
        return op(x.reshape(strip // SUBS, SUBS, QB), axis=0)

    def scores(i):
        (h, j), b = work[i], i % DUO
        q_t = qt[heads[h], j * QB:(j + 1) * QB]
        top = jnp.full((SUBS, QB), -jnp.inf, f32)
        for c in range(j + 1):
            tile = dot(k[c * QB:(c + 1) * QB, :], q_t)
            for at, rows in strips(c):
                s = tile[at:at + strip]
                if c == j:
                    seen = lax.broadcasted_iota(jnp.int32, (strip, QB), 0) + at <= lax.broadcasted_iota(jnp.int32, (strip, QB), 1)
                    s = jnp.where(seen, s, -jnp.inf)
                s_scr[b, rows, :] = s
                top = jnp.maximum(top, fold(s, jnp.max))
        return jnp.max(top, axis=0, keepdims=True)

    def rest(i, m):
        (h, j), b = work[i], i % DUO
        cols, n = slice(j * QB, (j + 1) * QB), (j + 1) * QB
        q_t, d_t = qt[heads[h], cols], do_t[heads[h], cols]
        tot = jnp.zeros((SUBS, QB), f32)
        for c in range(j + 1):
            for at, rows in strips(c):
                e = jnp.exp2((s_scr[b, rows, :] - m) * (SCALE * LOG2E))
                s_scr[b, rows, :] = e
                e_scr[b, rows, :] = e.astype(bf16)
                tot = tot + fold(e, jnp.sum)
        den = jnp.sum(tot, axis=0, keepdims=True)
        inv = 1.0 / den
        o = (dot(vt[:, :n], e_scr[b, :n, :]) / den).astype(bf16)
        ot[o_row(h), cols] = o
        delta = jnp.sum(d_t.astype(f32) * o.astype(f32), axis=0, keepdims=True)
        for c in range(j + 1):
            dp = dot(v[c * QB:(c + 1) * QB, :], d_t)
            for at, rows in strips(c):
                p = s_scr[b, rows, :] * inv
                p_scr[b, rows, :] = p.astype(bf16)
                d_scr[b, rows, :] = (p * (dp[at:at + strip] - delta)).astype(bf16)
        dvt[:, :n] += dot_nt(d_t, p_scr[b, :n, :])
        dkt[:, :n] += dot_nt(q_t, d_scr[b, :n, :])
        g = dot(kt[:, :n], d_scr[b, :n, :]) * SCALE
        co, si = cos[:, cols], sin[:, cols]
        x, y = g[:TURN], g[TURN:]
        dq[heads[h], cols] = jnp.concatenate([x * co + y * si, y * co - x * si], axis=0).astype(bf16)

    m = scores(0)
    for i in range(len(work)):
        later = scores(i + 1) if i + 1 < len(work) else None
        rest(i, m)
        m = later


def tail_kernel(qt, do_t, k, kt, v, vt, rt, dyc, wqk, wqkp, wvo, wvop, gain, hidden, dy, pos, cos, sin,
                result, grad_x, gq, gk, gv, go, gout,
                two, ks, kts, vs, vts, rts, ots, dqo, dqp, dkvo, dkvp, dkt, dvt, s_scr, e_scr, p_scr, d_scr, dycs, part, mid, buf1, buf2, buf3, fin, own, onat, dnat, xs, gacc, gpart, gpeer, gz, gx,
                send_sems, recv_sems, swap_sems, trade_send, trade_recv, local_sems):
    comm = Singles(trade_send, trade_recv, local_sems)
    comm.used = HEADS
    f32, bf16 = jnp.float32, jnp.bfloat16
    core, peer = comm.core, comm.peer()
    a1, a2 = two.at[0], two.at[1]
    comm.announce(CORNERS)
    sc = Scatter(comm, part, mid, (buf1, buf2, buf3), fin, (gq, gk, gv, go), send_sems, recv_sems, swap_sems)
    plan = Plan()
    some, most = pl.ds(0, PAIR), pl.ds(PAIR, HALF - PAIR)
    loads = [comm.local(s, d) for s, d in ((qt.at[some], two.at[0, some]), (k, ks), (do_t.at[some], two.at[1, some]), (vt, vts), (v, vs), (kt, kts))]
    dkt[...] = jnp.zeros_like(dkt)
    dvt[...] = jnp.zeros_like(dvt)
    with scope('wait_q'):
        for c in loads:
            c.wait()
    loads = [comm.local(s, d) for s, d in ((rt, rts), (qt.at[most], two.at[0, most]), (do_t.at[most], two.at[1, most]))]
    later = [comm.local(s, d) for s, d in ((dyc, dycs), (hidden, xs))]

    def emit(stages):
        for u, stage in stages:
            with scope(f'u{u}_s{stage}'):
                if u == GAIN:
                    sum_gain(stage)
                else:
                    sc.run(u, stage)

    def after(cost):
        plan.now += cost
        return plan.due()

    def head_trades(g):
        row = pl.ds(pl.multiple_of((core * HEADS + DUO * g) * LANES, PAIR), PAIR)
        mine = tile_at(g, PAIR)
        return [pltpu.make_async_remote_copy(src_ref=s, dst_ref=d, send_sem=trade_send.at[i], recv_sem=trade_recv.at[i], device_id=peer, device_id_type=MESH)
                for s, d, i in ((ots.at[row], ots.at[row], g), (dqo.at[mine], dqp.at[mine], PAIRS + g))]

    def gradient(place, count, left, right, mul):
        with scope('grad'):
            @pl.loop(0, DUO)
            def _(z):
                g = mul(left[tile_at(z, HALF), :], right())
                for i in range(count):
                    part[place + i, tile_at(z, DUO)] = g[:, i * LANES:(i + 1) * LANES].reshape(DUO, RING, RING, CHIP, LANES)

    attended, paired = [], []
    for g in range(PAIRS):
        attended.append(after(5.1))
        plan.now += 1.5
        plan.start(DUO * g)
        plan.start(DUO * g + 1)
        paired.append(plan.due())

    @pl.loop(0, PAIRS)
    def _(g):
        def at(table):
            for i in range(PAIRS):
                if table[i]:
                    pl.when(g == i)(functools.partial(emit, table[i]))

        heads = [tile_at(DUO * g + i, LANES) for i in range(DUO)]
        with scope('attend'):
            attend(heads, a1, a2, ks, kts, vs, vts, cos, sin, lambda i: tile_at(core * HEADS + DUO * g + i, LANES), ots, dqo, dkt, dvt, s_scr, e_scr, p_scr, d_scr)

        @pl.when(g == 0)
        def _():
            with scope('entry'):
                comm.meet(CORNERS)
                for c in loads:
                    c.wait()
        for c in head_trades(g):
            c.start()
        at(attended)
        gradient(DUO * g, DUO, rts, lambda: dqo[tile_at(g, PAIR), :], dot_nt)
        at(paired)

    def beat(cost, *starts):
        plan.now += cost
        for u in starts:
            plan.start(u)
        emit(plan.due())

    wkv, wkvp = e_scr.reshape(DIM, PAIR), p_scr.reshape(DIM, PAIR)
    later += [comm.local(src.at[:, pl.ds(at, LANES)], dst.at[:, pl.ds(to, LANES)]) for srcs, dst in (((wqk, wvo), wkv), ((wqkp, wvop), wkvp)) for src, at, to in ((srcs[0], HALF, 0), (srcs[1], 0, LANES))]
    wqp_loads = [comm.local(wqkp.at[tile_at(i, HALF), pl.ds(0, HALF)], two.at[i]) for i in range(DUO)]
    key = dkt[...] * SCALE
    co, si, x, y = cos[...], sin[...], key[:TURN], key[TURN:]
    dkvo[:LANES, :] = jnp.concatenate([x * co + y * si, y * co - x * si], axis=0).astype(bf16)
    dkvo[LANES:, :] = dvt[...].astype(bf16)
    comm.trade(dkvo, dkvp)
    gradient(UNIT_K, DUO, rts, lambda: dkvo[...], dot_nt)
    beat(1.8, UNIT_K, UNIT_V)
    wq_load = comm.local(wqk.at[:, pl.ds(0, HALF)], rts)
    for c in later:
        c.wait()
    with scope('trades'):
        for g in range(PAIRS):
            for c in head_trades(g):
                c.wait()

    waiting = list(range(RING))

    def output_gradients(force=False):
        while waiting:
            first = 10 + DUO * waiting[0]
            before = [u for u in range(N_UNITS) if u < first and PLACE[u] in (PLACE[first], PLACE[first + 1])]
            if force:
                emit(plan.rush(lambda: all(map(plan.vacated, before))))
            if not all(map(plan.vacated, before)):
                return
            for u in before:
                sc.drain(u, 0)
            i = waiting.pop(0)
            gradient(PLACE[first], DUO, ots, lambda: dycs[:, i * PAIR:(i + 1) * PAIR], dot)
            plan.start(first)
            plan.start(first + 1)
            beat(1.5)

    def piece(cost):
        beat(cost)
        output_gradients()

    def ticking(n, cost, body):
        tables = [after(cost) for _ in range(n)]

        @pl.loop(0, n)
        def _(i):
            body(i)
            for j, table in enumerate(tables):
                if table:
                    pl.when(i == j)(functools.partial(emit, table))
        output_gradients()

    @pl.loop(0, TOKENS // LANES)
    def _(i):
        want = lax.broadcasted_iota(jnp.int32, (LANES, ROWS), 0) + i * LANES
        own[tile_at(i, LANES), :] = jnp.where(want == pos[...], 1.0, 0.0).astype(bf16)

    def unsort(at, src_t, n):
        with scope('unsort'):
            dnat[at:at + n, :] = dot(src_t[:n, :], own[...]).astype(bf16)

    output_gradients()
    for c in comm.exchanged:
        c.wait_recv()
    unsort(0, dqo, HALF)
    dy_loads = [comm.local(dy.at[:, tile_at(i, HALF)], dqo.at[tile_at(i, ROWS)]) for i in range(DUO)]
    piece(1.2)
    unsort(HALF, dqp, HALF)
    piece(1.2)
    unsort(DUO * HALF, dkvo, PAIR)
    unsort(DUO * HALF + PAIR, dkvp, PAIR)
    piece(0.7)
    wq_load.wait()
    for c in wqp_loads + dy_loads:
        c.wait()
    gacc[...] = jnp.zeros_like(gacc)

    def dr_parts(half, r):
        return [s_scr.at[half, r(i * PAIR), :] for i in range(RING)]

    def back(block, then):
        def dr(half):
            with scope('dr'):
                c = tile_at(half, HALF)
                left = jnp.concatenate([rts[c, :], two[half], wkv[c, :], wkvp[c, :]], axis=1)
                acc = dot(left, dnat[:, block * PAIR:(block + 1) * PAIR])
                for i, ref in enumerate(dr_parts(half, lambda at: pl.ds(at, PAIR))):
                    ref[...] = acc[i * PAIR:(i + 1) * PAIR, :].T

        def norm(part):
            with scope('back'):
                @pl.loop(0, RING)
                def _(i):
                    j = part * RING + i
                    q = pl.ds(pl.multiple_of(block * PAIR + j * SHARE, SHARE), SHARE)
                    d = jnp.concatenate([ref[...] for half in range(DUO) for ref in dr_parts(half, lambda at: pl.ds(pl.multiple_of(at + j * SHARE, SHARE), SHARE))], axis=1)
                    x = xs[q, :].astype(f32)
                    inv = lax.rsqrt(jnp.mean(x * x, axis=-1, keepdims=True) + RMS_EPS)
                    unit = x * inv
                    gacc[...] += jnp.sum((d * unit).reshape(DUO, SUBS, DIM), axis=0)
                    dg = d * gain[0:1, :]
                    new = inv * (dg - unit * jnp.mean(dg * unit, axis=-1, keepdims=True))
                    for half in range(DUO):
                        r = pl.ds(pl.multiple_of(half * ROWS + block * PAIR + j * SHARE, SHARE), SHARE)
                        dqo[r, :] = (dqo[r, :].astype(f32) + new[:, half * HALF:(half + 1) * HALF]).astype(bf16)

        ticking(DUO, 1.6, dr)
        then()
        ticking(RING, 0.92, norm)

    back(0, lambda: None)
    wo_loads = []
    back(1, lambda: wo_loads.extend([comm.local(wvo.at[:, pl.ds(LANES, HALF)], rts)] + [comm.local(wvop.at[tile_at(i, HALF), pl.ds(LANES, HALF)], two.at[i]) for i in range(DUO)]))
    for i in range(DUO):
        comm.store(dqo.at[tile_at(i, ROWS)], grad_x.at[:, tile_at(i, HALF)])
    total = jnp.sum(gacc[...], axis=0, keepdims=True)
    gpart[...] = jnp.zeros_like(gpart)
    for i in range(RING):
        for j in range(RING):
            gpart[i, j:j + 1, :] = total[:, (i * RING + j) * LANES:(i * RING + j + 1) * LANES]

    gain_c, gain_z, gain_p = (Batch(comm) for _ in range(TRIO))

    def sum_gain(stage):
        if stage == 0:
            gain_c.send(gpart, gpeer, peer)
        elif stage == 1:
            gain_c.arrived(gpeer)
            for j in range(RING):
                gz[j] = gpart[j] + gpeer[j]
            for hop in (1, DUO, TRIO):
                gain_z.send(gz.at[step(comm.pos, 'z', hop)], gz.at[TRIO + hop], comm.far('z', hop))
        elif stage == DUO:
            gain_z.arrived(gz.at[pl.ds(RING, TRIO)])
            gx[0] = (gz[comm.pos['z']] + gz[RING]) + (gz[5] + gz[6])
            for dy, dx in PLANE:
                gain_p.send(gx.at[0], gx.at[dy * RING + dx], comm.aside(dy, dx))
        else:
            gain_p.arrived(gx.at[pl.ds(1, 15)])
            gpeer[0] = jnp.sum(gx[...], axis=0)
            mine = jnp.broadcast_to(gpeer[0, pl.ds(comm.pos['y'], 1), :], (SUBS, LANES))
            gout[...] = pltpu.roll(mine, LANES - (comm.pos['x'] * CHIP + core * SHARE), 1)

    plan.start(GAIN)
    beat(0.2)
    for i in range(DUO):
        with scope('unsort_o'):
            @pl.loop(0, DUO)
            def _(j):
                r = pl.ds(pl.multiple_of(i * HALF + j * ROWS, ROWS), ROWS)
                onat[:, r] = dot(ots[r, :], own[...]).astype(bf16).T
        piece(1.58)
    output_gradients(True)

    def project_out(col, weights, i):
        with scope('project'):
            @pl.loop(DUO * i, DUO * i + DUO)
            def _(j):
                c = tile_at(j, PAIR)
                dst = pl.ds(pl.multiple_of(col + j * PAIR, PAIR), PAIR)
                xs[:, dst] = (xs[:, dst].astype(f32) + dot(onat[...], weights(c))).astype(bf16)
        beat(1.48)

    def own_half(c):
        return rts[:, c]

    def other_half(c):
        return jnp.concatenate([a1[:, c], a2[:, c]], axis=0)

    for c in wo_loads:
        c.wait()
    for col, weights in ((core * HALF, own_half), ((1 - core) * HALF, other_half)):
        for i in range(DUO):
            project_out(col, weights, i)
    comm.store(xs, result)
    emit(plan.rush(lambda: not plan.stage))
    with scope('finish'):
        sc.finish()
        for batch, whole in ((gain_c, gpart), (gain_z, gz.at[pl.ds(RING, TRIO)]), (gain_p, gx.at[pl.ds(1, 15)])):
            batch.sent(whole)
        for c in comm.exchanged:
            c.wait_send()
        for c in comm.stored:
            c.wait()


def tail(qt, do_t, k, kt, v, vt, rt, dyc, wqk, wqkp, wvo, wvop, gain, hidden, dy, pos, cos, sin):
    bf16, f32 = jnp.bfloat16, jnp.float32
    any_ = pl.BlockSpec(memory_space=pl.ANY)
    vmem = pl.BlockSpec(memory_space=pltpu.VMEM)
    S = lambda shape, d=bf16: jax.ShapeDtypeStruct(shape, d)
    V = lambda shape, d=bf16: pltpu.VMEM(shape, d)
    D = lambda n: pltpu.SemaphoreType.DMA((n,))
    sq, tall, wide = (HALF, TOKENS), (TOKENS, LANES), (LANES, TOKENS)
    mine, kv = (ROWS, DIM), (PAIR, TOKENS)
    return pl.pallas_call(
        tail_kernel,
        out_shape=[S(mine), S(mine), S((SHARE, DIM), f32), S((SHARE, PAIR), f32), S((SHARE, PAIR), f32), S((SHARE, DIM), f32), S((SUBS, LANES), f32)],
        in_specs=[any_] * 12 + [vmem] + [any_] * DUO + [vmem] * TRIO,
        out_specs=[any_] * 6 + [vmem],
        scratch_shapes=[V((DUO,) + sq), V(tall), V(wide), V(tall), V(wide), V((DIM, TOKENS)), V((DIM, TOKENS)), V(sq), V(sq), V(kv), V(kv), V(wide, f32), V(wide, f32),
                        V((DUO, TOKENS, QB), f32), V((DUO, TOKENS, QB)), V((DUO, TOKENS, QB)), V((DUO, TOKENS, QB)), V(sq), V((PLACES, RING, RING, RING, CHIP, LANES), f32), V((TRIO, SLOTS, RING, RING, CHIP, LANES), f32),
                        V((TRIO, SLOTS, 6, RING, RING, SHARE, LANES), f32), V((TRIO, SLOTS, 6, RING, SHARE, LANES), f32), V((TRIO, SLOTS, TRIO, CHIP, LANES), f32), V((N_UNITS, CHIP, LANES), f32), V((TOKENS, ROWS)), V(mine), V((DUO * QKV, ROWS)), V(mine),
                        V((SUBS, DIM), f32), V((RING, SUBS, LANES), f32), V((RING, SUBS, LANES), f32), V((7, SUBS, LANES), f32), V((SHARE, SUBS, LANES), f32),
                        D(9 * SLOTS), D(15 * SLOTS), D(DUO + N_UNITS), D(HEADS + RING), D(HEADS + RING), D(26)],
        compiler_params=pltpu.CompilerParams(collective_id=1, has_side_effects=True, vmem_limit_bytes=67043328),
        name='tail',
    )(qt, do_t, k, kt, v, vt, rt, dyc, wqk, wqkp, wvo, wvop, gain, hidden, dy, pos, cos, sin)


def settle_kernel(n, *refs):
    ins, gain, outs, gain_out, bufs, sems = refs[:n], refs[n], refs[n + 1:DUO * n + 1], refs[DUO * n + 1], refs[DUO * n + DUO:-1], refs[-1]
    jobs = []
    for a, o, b in zip(ins, outs, bufs):
        size = a.shape[0] // RING if a.shape[0] == ROWS else a.shape[0]
        jobs += [tuple(r.at[pl.ds(i, size)] for r in (a, b, o)) for i in range(0, a.shape[0], size)]
    takes = [pltpu.make_async_copy(a, b, sems.at[0, i]) for i, (a, b, _) in enumerate(jobs)]
    puts = [pltpu.make_async_copy(b, o, sems.at[1, i]) for i, (_, b, o) in enumerate(jobs)]
    for c in takes:
        c.start()
    gain_out[...] = gain[0:1, :SHARE]
    for take, put in zip(takes, puts):
        take.wait()
        put.start()
    for c in puts:
        c.wait()


def settle(*arrays):
    *large, gain = arrays
    any_, vmem = pl.BlockSpec(memory_space=pl.ANY), pl.BlockSpec(memory_space=pltpu.VMEM)
    return pl.pallas_call(
        functools.partial(settle_kernel, len(large)),
        out_shape=[jax.ShapeDtypeStruct(a.shape, a.dtype) for a in large] + [jax.ShapeDtypeStruct((1, SHARE), gain.dtype)],
        in_specs=[any_] * len(large) + [vmem],
        out_specs=[any_] * len(large) + [vmem],
        scratch_shapes=[pltpu.VMEM(a.shape, a.dtype) for a in large] + [pltpu.SemaphoreType.DMA((DUO, 12))],
        name='settle',
    )(*arrays)


def rope_tables():
    j = np.arange(HEAD_DIM // DUO, dtype=np.float64) / (HEAD_DIM // DUO)
    freq = (ROPE_THETA ** -j).astype(np.float32)
    angle = freq[:, None] * np.arange(TOKENS, dtype=np.float32)[None, :]
    return np.cos(angle.astype(np.float64)).astype(np.float32), np.sin(angle.astype(np.float64)).astype(np.float32)


def solution(mesh):
    def shard_fn(hidden, tok_pos, grad_out, norm_gain, w_query, w_key, w_value, w_out):
        hidden, grad_out = hidden[0], grad_out[0]
        cos_t, sin_t = (jnp.asarray(t) for t in rope_tables())
        *parts, gain = head(hidden, grad_out, w_query, w_key, w_value, w_out, tok_pos, norm_gain.reshape(1, SHARE), cos_t, sin_t)
        parts = [p.reshape(DIM, GROUP) if p.ndim > DUO else p for p in parts]
        result, grad_hidden, gq, gk, gv, go, gout = settle(*tail(*parts, gain, hidden, grad_out, tok_pos, cos_t, sin_t))
        return result[None], grad_hidden[None], gq, gk, gv, go, gout.reshape(SHARE)

    row_spec, pos_spec = P('fsdp', 'cp', None), P('fsdp', 'cp')
    weight_spec, gain_spec = P(('fsdp', 'cp'), None), P(('fsdp', 'cp'))
    return jax.shard_map(shard_fn, mesh=mesh, in_specs=(row_spec, pos_spec, row_spec, gain_spec, weight_spec, weight_spec, weight_spec, weight_spec), out_specs=(row_spec, row_spec, weight_spec, weight_spec, weight_spec, weight_spec, gain_spec), check_vma=False)
```

```python
import functools
import jax
import jax.numpy as jnp
import numpy as np
from jax import lax
from jax.experimental import pallas as pl
from jax.experimental.pallas import tpu as pltpu
from jax.sharding import PartitionSpec as P

LANES, SUBS, RING, TRIO, DUO = 128, 8, 4, 3, 2
PAIR, ROWS, CHIP, SHARE, TURN = 256, 512, 32, 16, 64
HEAD_DIM = LANES
ROPE_THETA = 1000000.0
RMS_EPS = 1e-5
SCALE = HEAD_DIM ** -0.5
LOG2E = 1.4426950408889634

MESH = pl.DeviceIdType.MESH
AXES = ('x', 'y', 'z')
ORDERS = (('x', 'y', 'z'), ('y', 'z', 'x'), ('z', 'x', 'y'))
ALL = pl.ds(0, RING)


def torus():
    f = lax.axis_index('fsdp')
    return {'x': lax.rem(f, RING), 'y': lax.rem(lax.div(f, RING), RING), 'z': lax.div(f, SHARE)}


def step(pos, axis, hop):
    return lax.rem(pos[axis] + hop, RING)


class Batch:
    def __init__(self, comm):
        self.comm, self.index = comm, comm.used
        comm.used += 1

    def _copy(self, src, dst, device):
        send, recv, _ = self.comm.sems
        return pltpu.make_async_remote_copy(src_ref=src, dst_ref=dst, send_sem=send.at[self.index], recv_sem=recv.at[self.index], device_id=device, device_id_type=MESH)

    def send(self, src, dst, device):
        self._copy(src, dst, device).start()
        return self

    def arrived(self, whole):
        self._copy(whole, whole, self.comm.peer()).wait_recv()

    def sent(self, whole):
        self._copy(whole, whole, self.comm.peer()).wait_send()


class Comm:
    def __init__(self, send_sems, recv_sems, local_sems):
        self.pos = torus()
        self.core = lax.axis_index('cp')
        self.sems = (send_sems, recv_sems, local_sems)
        self.used = self.used_local = 0
        self.stored = []

    def far(self, axis, hop):
        p = dict(self.pos)
        p[axis] = step(self.pos, axis, hop)
        return {'fsdp': (p['z'] * RING + p['y']) * RING + p['x'], 'cp': self.core}

    def peer(self):
        return {'fsdp': lax.axis_index('fsdp'), 'cp': 1 - self.core}

    def aside(self, dy, dx):
        return {'fsdp': (self.pos['z'] * RING + step(self.pos, 'y', dy)) * RING + step(self.pos, 'x', dx), 'cp': self.core}

    def announce(self, corners=()):
        sem = pltpu.get_barrier_semaphore()
        for axis in AXES:
            for hop in (1, DUO, TRIO):
                pl.semaphore_signal(sem, inc=1, device_id=self.far(axis, hop), device_id_type=MESH)
        for dy, dx in corners:
            pl.semaphore_signal(sem, inc=1, device_id=self.aside(dy, dx), device_id_type=MESH)
        pl.semaphore_signal(sem, inc=1, device_id=self.peer(), device_id_type=MESH)

    def meet(self, corners=()):
        pl.semaphore_wait(pltpu.get_barrier_semaphore(), 10 + len(corners))

    def ring(self, batch, src, slots, axis):
        for hop in (1, DUO, TRIO):
            batch.send(src, slots.at[hop], self.far(axis, hop))

    def local(self, src, dst):
        i = self.used_local
        self.used_local += 1
        c = pltpu.make_async_copy(src, dst, self.sems[DUO].at[i])
        c.start()
        return c

    def store(self, src, dst):
        self.stored.append(self.local(src, dst))


class Singles(Comm):
    def __init__(self, *sems):
        super().__init__(*sems)
        self.sent, self.exchanged = [], []

    def _copy(self, src, dst, device):
        i = self.used
        self.used += 1
        c = pltpu.make_async_remote_copy(src_ref=src, dst_ref=dst, send_sem=self.sems[0].at[i], recv_sem=self.sems[1].at[i], device_id=device, device_id_type=MESH)
        c.start()
        return c

    def send(self, src, dst, device):
        c = self._copy(src, dst, device)
        self.sent.append(c)
        return c

    def trade(self, src, dst):
        self.exchanged.append(self._copy(src, dst, self.peer()))


def pick(ref, sel, piece):
    lo, cols, first, rows = piece
    return ref.at[sel['z'], sel['y'], sel['x'], pl.ds(first, rows), pl.ds(lo, cols)]


def sem_scratch(remote, local):
    return [pltpu.SemaphoreType.DMA((remote,)), pltpu.SemaphoreType.DMA((remote,)), pltpu.SemaphoreType.DMA((local,))]


def add_into(dst, *srcs, fresh=False):
    def add(idx):
        total, *rest = [s[idx] for s in (srcs if fresh else (dst,) + srcs)]
        for more in rest:
            total = total + more
        dst[idx] = total

    if len(dst.shape) > TRIO:
        @pl.loop(0, dst.shape[0])
        def _(i):
            add((i,))
    else:
        add(Ellipsis)


def columns(lo, na, nb):
    return (lo, na, 0, CHIP), (lo + na, nb, 0, CHIP)


def strip(lo):
    return (lo, LANES, 0, SHARE), (lo, LANES, SHARE, SHARE)


QK_COLORS = (columns(0, PAIR, LANES), columns(384, LANES, PAIR), columns(768, PAIR, LANES))
VO_COLORS = (columns(0, LANES, PAIR), columns(384, PAIR, LANES), columns(768, LANES, PAIR))
QK_FIRST = (columns(0, LANES, LANES), columns(384, LANES, LANES), columns(768, LANES, LANES))
QK_LAST = (strip(PAIR), strip(640), strip(1024))
TOKENS = 1024
DIM = 2048
HALF = 1024
QKV = 1280
GROUP = 1152


def scope(name):
    return jax.named_scope(name)


def dot(a, b):
    return jnp.dot(a, b, preferred_element_type=jnp.float32)


def dot_nt(a, b):
    return lax.dot_general(a, b, (((1,), (1,)), ((), ())), preferred_element_type=jnp.float32)


def tile_at(i, n):
    return pl.ds(pl.multiple_of(i * n, n), n)


class Gather:
    def __init__(self, comm, ref, colors, land, held=None):
        self.comm, self.ref, self.colors, self.land = comm, ref, colors, land
        self.held = list(held or [dict(comm.pos) for _ in colors])
        self.spent = []

    def move(self, batch, s, piece, to):
        batch.send(pick(self.ref, s, piece), pick(self.ref, s, piece), to)

    def at(self, k, hop):
        d = ORDERS[k][self.phase]
        return dict(self.held[k], **{d: step(self.comm.pos, d, hop)})

    def begin(self, phase):
        self.phase = phase
        self.rest = Batch(self.comm)
        if phase == 0:
            for hop in (DUO, 1, TRIO):
                for k, (a, b) in enumerate(self.colors):
                    self.move(self.rest, self.held[k], (a[0], a[1] + b[1], 0, CHIP), self.comm.far(ORDERS[k][0], hop))
            return
        self.up, self.dn = ([Batch(self.comm) for _ in range(TRIO)] for _ in range(DUO))
        for k, (a, b) in enumerate(self.colors):
            d = ORDERS[k][phase]
            up, dn, s = self.comm.far(d, 1), self.comm.far(d, TRIO), self.held[k]
            self.move(self.up[k], s, a, up)
            self.move(self.dn[k], s, b, dn)
            self.move(self.rest, s, b, up)
            self.move(self.rest, s, a, dn)
        if phase == DUO:
            for k, pieces in enumerate(self.colors):
                for piece in pieces:
                    self.land(self.ref, self.held[k], piece)

    def forward(self):
        for k, (a, b) in enumerate(self.colors):
            d = ORDERS[k][self.phase]
            for batch, hop, piece, to in ((self.up[k], TRIO, a, 1), (self.dn[k], 1, b, TRIO)):
                s = self.at(k, hop)
                batch.arrived(pick(self.ref, s, piece))
                self.move(self.rest, s, piece, self.comm.far(d, to))
                if self.phase == DUO:
                    self.land(self.ref, s, piece)
                self.spent.append((batch, pick(self.ref, self.held[k], piece)))

    def end(self):
        axis = ORDERS[0][self.phase]
        blocks = dict(self.held[0], **{axis: pl.ds(0, DUO if self.phase else TRIO)})
        width = sum(max(a[0] + a[1], b[0] + b[1]) - a[0] for a, b in self.colors)
        whole = pick(self.ref, blocks, (0, width, 0, CHIP))
        self.rest.arrived(whole)
        self.spent.append((self.rest, whole))
        for k, (a, b) in enumerate(self.colors):
            if self.phase == DUO:
                for hop, piece in ((TRIO, b), (1, a), (DUO, a), (DUO, b)):
                    self.land(self.ref, self.at(k, hop), piece)
            self.held[k] = dict(self.held[k], **{ORDERS[k][self.phase]: ALL})

    def finish(self):
        for batch, whole in self.spent:
            batch.sent(whole)


def head_kernel(hidden, dy, wq, wk, wv, wo, pos, gain_in, cos_t, sin_t,
                qt_o, dot_o, k_o, kt_o, v_o, vt_o, rt_o, dyc_o, wqk_o, wqkp_o, wvo_o, wvop_o, gain_o,
                hid2, dy2, dys, rs, rt, wqk, wvo, wpeer, pi, pos2, qt, dot_s, kk, kt, vv, vt, gain, gtile, gbuf, gx, gy, gz, *sems):
    comm = Comm(*sems)
    comm.announce()
    pos_c, core = comm.pos, comm.core
    bf16, f32 = jnp.bfloat16, jnp.float32
    peer = comm.peer()
    rows = tile_at(core, SHARE)
    mine_qk = wqk.at[pos_c['z'], pos_c['y'], pos_c['x'], rows]
    mine_vo = wvo.at[pos_c['z'], pos_c['y'], pos_c['x'], rows]

    def weight_parts(c):
        return ((wq.at[:, tile_at(c, HALF)], mine_qk.at[:, pl.ds(0, HALF)]), (wk.at[:, tile_at(c, LANES)], mine_qk.at[:, pl.ds(HALF, LANES)]),
                (wv.at[:, tile_at(c, LANES)], mine_vo.at[:, pl.ds(0, LANES)]), (wo.at[:, tile_at(c, HALF)], mine_vo.at[:, pl.ds(LANES, HALF)]))

    loads = [comm.local(s, d) for s, d in weight_parts(core)]
    load_x = [comm.local(hidden, hid2.at[pl.ds(0, ROWS)]), comm.local(dy, dy2.at[pl.ds(0, ROWS)])]
    share = lax.broadcasted_iota(jnp.int32, (SUBS, LANES), 1) // SHARE
    gtile[...] = jnp.where(share == pos_c['x'] * DUO + core, jnp.broadcast_to(jnp.concatenate([gain_in[...]] * SUBS, axis=1), (SUBS, LANES)), 0.0)
    with scope('entry'):
        comm.meet()
    swap_w, swap_pos, swap_dy, swap_x, peers_qk, peers_vo = (Batch(comm) for _ in range(6))
    gain_c, gain_x, gain_y, gain_z = (Batch(comm) for _ in range(RING))
    for s, d in weight_parts(1 - core):
        swap_w.send(s, d, peer)
    gain_c.send(gtile, gbuf, peer)
    swap_pos.send(pos, pos2, peer)
    for c in loads:
        c.wait()
    with scope('wait_w'):
        swapped = wqk.at[pos_c['z'], pos_c['y'], pos_c['x']]
        swap_w.arrived(swapped)

    def land_qk(ref, s, cols):
        peers_qk.send(pick(ref, s, cols), pick(wqkp_o, s, cols), peer)

    def land_vo(ref, s, cols):
        peers_vo.send(pick(ref, s, cols), pick(wpeer, s, cols), peer)

    g1 = Gather(comm, wvo, VO_COLORS, land_vo)
    g2 = Gather(comm, wqk, QK_COLORS, land_qk)
    g1.begin(0)
    g2.begin(0)
    gain_c.arrived(gbuf)
    gx[0] = gtile[...] + gbuf[...]
    comm.ring(gain_x, gx.at[0], gx, 'x')

    swap_pos.arrived(pos2)

    @pl.loop(0, TOKENS // LANES)
    def _(i):
        want = lax.broadcasted_iota(jnp.int32, (LANES, ROWS), 0) + i * LANES
        for h, have in enumerate((pos, pos2)):
            pi[tile_at(i, LANES), h * ROWS:(h + 1) * ROWS] = jnp.where(want == have[...], 1.0, 0.0).astype(bf16)

    def sort(dst, src, first, last):
        with scope('sort'):
            @pl.loop(first, last)
            def _(j):
                c = tile_at(j, PAIR)
                dst[:, c] = dot(pi[...], src[:, c]).astype(bf16)

    swap_dy.send(dy, dy2.at[pl.ds(ROWS, ROWS)], peer)
    with scope('p0_end'):
        for g in (g1, g2):
            g.end()
            g.begin(1)
    swap_x.send(hidden, hid2.at[pl.ds(ROWS, ROWS)], peer)
    gain_x.arrived(gx.at[pl.ds(1, TRIO)])
    gy[pos_c['y']] = (gx[0] + gx[1]) + (gx[DUO] + gx[TRIO])
    for hop in (1, DUO, TRIO):
        gain_y.send(gy.at[pos_c['y']], gy.at[pos_c['y']], comm.far('y', hop))
    with scope('wait_dy'):
        load_x[1].wait()
        swap_dy.arrived(dy2.at[pl.ds(ROWS, ROWS)])
    sort(dys, dy2, 0, RING)
    with scope('p1a_fwd'):
        g1.forward()
    sort(dys, dy2, RING, 6)
    with scope('p1b_fwd'):
        g2.forward()
    sort(dys, dy2, 6, SUBS)
    with scope('p1a_end'):
        g1.end()
    gain_y.arrived(gy.at[pl.ds(1, TRIO)])
    for j in range(RING):
        gz[pos_c['z'], j] = gy[j]
    for hop in (1, DUO, TRIO):
        gain_z.send(gz.at[pos_c['z']], gz.at[pos_c['z']], comm.far('z', hop))
    g1.begin(DUO)
    comm.store(dys.at[:, tile_at(core, HALF)], dyc_o)
    with scope('p1b_end'):
        g2.end()
    with scope('wait_x'):
        load_x[0].wait()
        swap_x.arrived(hid2.at[pl.ds(ROWS, ROWS)])
    sort(rs, hid2, 0, SUBS)
    with scope('p2q_fwd'):
        g1.forward()
    g2a, g2b = (Gather(comm, wqk, colors, land_qk, g2.held) for colors in (QK_FIRST, QK_LAST))
    g2a.begin(DUO)
    with scope('gain'):
        gain_z.arrived(gz.at[pl.ds(1, TRIO)])
    for i in range(RING):
        for j in range(RING):
            gain[:, (i * RING + j) * LANES:(i * RING + j + 1) * LANES] = gz[i, j]
    comm.store(gain, gain_o)

    def norm(first, last):
        with scope('norm'):
            @pl.loop(first, last)
            def _(i):
                r = tile_at(i, CHIP)
                x = rs[r, :].astype(f32)
                inv = lax.rsqrt(jnp.mean(x * x, axis=-1, keepdims=True) + RMS_EPS)
                rs[r, :] = (x * inv * gain[0:1, :]).astype(bf16)

    norm(0, TOKENS // CHIP)
    with scope('r_t'):
        @pl.loop(0, DIM // PAIR)
        def _(i):
            c = tile_at(i, PAIR)

            @pl.loop(0, TOKENS // PAIR)
            def _(j):
                r = tile_at(j, PAIR)
                rt[c, r] = rs[r, c].T
    comm.store(rt, rt_o)
    with scope('p2o_end'):
        g1.end()
    w_qk, w_vo, w_peer = wqk.reshape(DIM, GROUP), wvo.reshape(DIM, GROUP), wpeer.reshape(DIM, GROUP)
    with scope('vals'):
        @pl.loop(0, DUO)
        def _(i):
            r = tile_at(i, ROWS)
            val = dot(rs[r, :], w_vo[:, :LANES]).astype(bf16)
            vv[r, :] = val
            vt[:, r] = val.T
    for src, dst in ((wvo, wvo_o), (vv, v_o), (vt, vt_o)):
        comm.store(src, dst)
    with scope('p2q_fwd'):
        g2a.forward()
    g2b.begin(DUO)
    with scope('wo_peer'):
        peers_vo.arrived(wpeer)
    comm.store(wpeer, wvop_o)
    with scope('do_t'):
        mine = tile_at(core, HALF)

        @pl.loop(0, TOKENS // PAIR)
        def _(j):
            t = tile_at(j, PAIR)
            w_rows = jnp.concatenate([w_vo[mine, LANES:], w_peer[mine, LANES:]], axis=1)
            d_rows = jnp.concatenate([dys[t, mine], dys[t, tile_at(1 - core, HALF)]], axis=1)
            dot_s[:, t] = dot_nt(w_rows, d_rows).astype(bf16)
    comm.store(dot_s, dot_o)

    def rotated(x, r):
        cos, sin = cos_t[:, r], sin_t[:, r]
        cos = jnp.concatenate([cos, cos], axis=0).T
        sin = jnp.concatenate([-sin, sin], axis=0).T
        return (x * cos + pltpu.roll(x, TURN, 1) * sin).astype(bf16)

    def queries(columns, heads):
        x = dot(rs[...], columns)
        for i in range(RING):
            r = slice(i * PAIR, (i + 1) * PAIR)
            for h, head in enumerate(heads):
                qt[tile_at(head, LANES), r] = rotated(x[r, h * LANES:(h + 1) * LANES], r).T

    with scope('p2q_end'):
        g2a.end()

    def pairs(first, last):
        with scope('q'):
            @pl.loop(first, last)
            def _(t):
                queries(w_qk[:, pl.ds(pl.multiple_of(t * 384, LANES), PAIR)], (TRIO * t, TRIO * t + 1))

    pairs(0, 1)
    with scope('last_fwd'):
        g2b.forward()
    pairs(1, TRIO)
    for t in range(TRIO):
        two_heads = pl.ds(t * 384, PAIR)
        comm.store(qt.at[two_heads], qt_o.at[two_heads])
    with scope('last_end'):
        g2b.end()
    comm.store(wqk, wqk_o)
    with scope('q_last'):
        x = dot(rs[...], jnp.concatenate([w_qk[:, PAIR:384], w_qk[:, 640:768], w_qk[:, HALF:]], axis=1))
        for i in range(RING):
            r = slice(i * PAIR, (i + 1) * PAIR)
            key = rotated(x[r, PAIR:], r)
            kk[r, :] = key
            kt[:, r] = key.T
            for h, head in enumerate((DUO, 5)):
                qt[tile_at(head, LANES), r] = rotated(x[r, h * LANES:(h + 1) * LANES], r).T
    for src, dst in ((kk, k_o), (kt, kt_o)) + tuple((qt.at[tile_at(h, LANES)], qt_o.at[tile_at(h, LANES)]) for h in (DUO, 5)):
        comm.store(src, dst)
    with scope('finish'):
        peers_qk.arrived(wqk)
        for batch, whole in ((swap_w, swapped), (swap_pos, pos2), (swap_dy, dy2.at[pl.ds(ROWS, ROWS)]), (swap_x, hid2.at[pl.ds(ROWS, ROWS)]), (peers_qk, wqk), (peers_vo, wvo),
                             (gain_c, gbuf), (gain_x, gx.at[pl.ds(1, TRIO)]), (gain_y, gy.at[pl.ds(1, TRIO)]), (gain_z, gz.at[pl.ds(1, TRIO)])):
            batch.sent(whole)
        for g in (g1, g2, g2a, g2b):
            g.finish()
        for c in comm.stored:
            c.wait()


def head(hidden, dy, wq, wk, wv, wo, pos, gain, cos_t, sin_t):
    bf16, f32 = jnp.bfloat16, jnp.float32
    any_ = pl.BlockSpec(memory_space=pl.ANY)
    vmem = pl.BlockSpec(memory_space=pltpu.VMEM)
    S = lambda shape, d=bf16: jax.ShapeDtypeStruct(shape, d)
    V = lambda shape, d=bf16: pltpu.VMEM(shape, d)
    group = (RING, RING, RING, CHIP, GROUP)
    sq, tall, wide = (HALF, TOKENS), (TOKENS, LANES), (LANES, TOKENS)
    full = (TOKENS, DIM)
    return pl.pallas_call(
        head_kernel,
        out_shape=[S(sq), S(sq), S(tall), S(wide), S(tall), S(wide), S((DIM, TOKENS)), S((TOKENS, HALF)), S(group), S(group), S(group), S(group), S((SUBS, DIM), f32)],
        in_specs=[any_] * 6 + [vmem] * RING,
        out_specs=[any_] * 13,
        scratch_shapes=[V(full), V(full), V(full), V(full), V((DIM, TOKENS)), V(group), V(group), V(group), V((TOKENS, TOKENS)), V((1, ROWS), jnp.int32),
                        V(sq), V(sq), V(tall), V(wide), V(tall), V(wide), V((SUBS, DIM), f32), V((SUBS, LANES), f32), V((SUBS, LANES), f32), V((RING, SUBS, LANES), f32), V((RING, SUBS, LANES), f32), V((RING, RING, SUBS, LANES), f32)] + sem_scratch(47, 22),
        compiler_params=pltpu.CompilerParams(collective_id=0, has_side_effects=True, vmem_limit_bytes=60 * DUO**20),
        name='head',
    )(hidden, dy, wq, wk, wv, wo, pos, gain, cos_t, sin_t)


HEADS = SUBS
UNIT_K, UNIT_V = SUBS, 9
N_UNITS = 18
GAIN = N_UNITS
SLOTS = RING
LAST = 5
ABREAST = DUO
LINES = ((0, TRIO, 6, 9, 12, 15), (1, RING, 7, 10, 13, SHARE), (DUO, 5, SUBS, 11, 14, 17))
COLOR = {u: k for k, line in enumerate(LINES) for u in line}
RANK = {u: i for line in LINES for i, u in enumerate(line)}
SWAPPED = (1, TRIO, RING, SUBS, 10)
ORDER = {u: ORDERS[k] if u not in SWAPPED else (ORDERS[k][0], ORDERS[k][DUO], ORDERS[k][1]) for u, k in COLOR.items()}
BEFORE = {u: line[i - SLOTS] if i >= SLOTS else None for line in LINES for i, u in enumerate(line)}
PLACES = 12
PLACE = {u: u % PLACES for u in range(N_UNITS)}
WIRE = (2.82, 0.71, 0.36)
LATENCY = 2.4
STAGE_COST = 0.08


class Plan:
    def __init__(self):
        self.now, self.stage, self.ready, self.order, self.link = 0.0, {}, {}, [], {}
        self.mark = {}

    def _wire(self, u, phase, count):
        link = ORDER[u][phase]
        t = max(self.link.get(link, 0.0), self.now)
        first = t + WIRE[phase] + LATENCY
        self.link[link] = t + WIRE[phase] * count
        return first if phase < DUO else self.link[link] + LATENCY

    def free(self, u, phase):
        if BEFORE[u] is None:
            return True
        done = self.mark.get((BEFORE[u], (DUO, RING, 5)[phase]))
        if done is None:
            return False
        sent = ((0, 1), (DUO, TRIO), (RING,))[phase]
        return any(self.mark.get((j, s), -1) > done and (j, s + 1) in self.mark for j, order in ORDER.items() if order[phase] == ORDER[u][phase] for s in sent)

    def run(self, u):
        stage = self.stage[u]
        self.order.append((u, stage))
        self.mark[u, stage] = len(self.order)
        self.now = max(self.now, self.ready[u]) + STAGE_COST
        self.stage[u] = stage + 1
        if stage == (TRIO if u == GAIN else LAST):
            del self.stage[u]
        elif u == GAIN:
            self.ready[u] = max([self.now] + [self.link.get(a, 0.0) for a in ('', 'z', 'xy')[stage]]) + DUO * LATENCY
        elif stage % DUO:
            self.ready[u] = self._wire(u, stage // DUO, 1)
        else:
            self.ready[u] = self._wire(u, stage // DUO, DUO)

    def blocked(self, u):
        stage = self.stage[u]
        if u == GAIN:
            return False
        if stage == 0 and sum(0 < self.stage.get(j, 0) <= DUO for j in LINES[COLOR[u]]) >= ABREAST:
            return True
        if stage == DUO and BEFORE[u] is not None and (BEFORE[u], LAST) not in self.mark:
            return True
        return stage in (0, DUO, RING) and not self.free(u, stage // DUO)

    def start(self, u):
        self.stage[u], self.ready[u] = 0, self.now

    def due(self):
        first = len(self.order)
        while True:
            ripe = [(self.ready[u], u) for u in self.stage if self.ready[u] <= self.now and not self.blocked(u)]
            if not ripe:
                return self.order[first:]
            self.run(min(ripe)[1])

    def vacated(self, u):
        return (u, DUO) in self.mark

    def rush(self, done):
        first = len(self.order)
        while not done():
            self.run(min((self.ready[u], u) for u in self.stage if not self.blocked(u))[1])
        return self.order[first:]


QB = PAIR
PAIRS = HEADS // DUO
NBLK = TOKENS // QB
HALVES = (pl.ds(0, SHARE), pl.ds(SHARE, SHARE))
PLANE = tuple((dy, dx) for dy in range(RING) for dx in range(RING) if dy or dx)
CORNERS = tuple((dy, dx) for dy, dx in PLANE if dy and dx)


class Scatter:
    def __init__(self, comm, part, mid, bufs, fin, outs, send_sems, recv_sems, swap_sems):
        self.pos, self.part, self.mid, self.bufs, self.fin, self.outs = comm.pos, part, mid, bufs, fin, outs
        self.send_sems, self.recv_sems, self.swap_sems = send_sems, recv_sems, swap_sems
        self.near = {(a, hop): comm.far(a, hop) for a in AXES for hop in (1, DUO, TRIO)}
        self.hops = {(a, hop): step(comm.pos, a, hop) for a in AXES for hop in (1, DUO, TRIO)}
        self.peer, self.core = comm.peer(), comm.core
        self.keep, self.give = tile_at(comm.core, SHARE), tile_at(1 - comm.core, SHARE)
        self.drained = set()

    def slot(self, u):
        return COLOR[u], RANK[u] % SLOTS

    def buf(self, u, phase):
        return self.bufs[phase].at[self.slot(u)]

    def view(self, u, phase, hop, half=None):
        order = ORDER[u]
        at = {a: ALL for a in AXES}
        for a in order[1:phase]:
            at[a] = self.pos[a]
        at[order[phase]] = self.hops[order[phase], hop] if hop else self.pos[order[phase]]
        rows = pl.ds(0, CHIP) if half is None else HALVES[half]
        if phase == 0:
            return self.part.at[PLACE[u], at['z'], at['y'], at['x'], rows, :]
        return self.mid.at[self.slot(u) + tuple(at[a] for a in 'zyx' if a != order[0]) + (rows, slice(None))]

    def copy(self, src, dst, sems, device):
        return pltpu.make_async_remote_copy(src_ref=src, dst_ref=dst, send_sem=sems[0], recv_sem=sems[1], device_id=device, device_id_type=MESH)

    def sems(self, u, phase, kind=0):
        k, i = self.slot(u)
        at = (k * SLOTS + i) * TRIO + phase
        return self.send_sems.at[at], self.recv_sems.at[(k * SLOTS + i) * 5 + DUO * phase + kind]

    def send(self, u, phase, name):
        axis = ORDER[u][phase]
        if phase == DUO:
            src, to = self.view(u, DUO, name + 1), name + 1
        else:
            hop, half, to = ((DUO, 0, 1), (DUO, 1, TRIO), (1, 1, 1), (TRIO, 0, TRIO), (1, 0, 1), (TRIO, 1, TRIO))[name]
            src = self.view(u, phase, hop, half)
        self.copy(src, self.buf(u, phase).at[name], self.sems(u, phase, int(name > 1 and phase < DUO)), self.near[axis, to]).start()

    def launch(self, u, phase):
        if BEFORE[u] is not None:
            self.drain(BEFORE[u], phase)
        for name in range(RING if phase < DUO else TRIO):
            self.send(u, phase, name)

    def arrived(self, u, phase, first, count):
        whole = self.buf(u, phase).at[pl.ds(first, count)]
        self.copy(whole, whole, self.sems(u, phase, int(first > 0)), self.peer).wait_recv()

    def drain(self, u, phase):
        if (u, phase) not in self.drained:
            self.drained.add((u, phase))
            whole = self.buf(u, phase)
            self.copy(whole, whole, self.sems(u, phase), self.peer).wait_send()

    def out(self, u):
        if u < HEADS:
            out, col = self.outs[0], self.core * HALF + u * LANES
        elif u < 10:
            out, col = self.outs[u - 7], self.core * LANES
        else:
            out, col = self.outs[TRIO], self.core * HALF + (u - 10) * LANES
        return out.at[:, pl.ds(pl.multiple_of(col, LANES), LANES)]

    def kept(self, u):
        return pltpu.make_async_copy(self.fin.at[u, self.keep], self.out(u), self.swap_sems.at[DUO + u])

    def run(self, u, stage):
        if stage == 0:
            return self.launch(u, 0)
        phase = (stage - 1) // DUO
        if stage == LAST:
            self.arrived(u, DUO, 0, TRIO)
            got = self.buf(u, DUO)
            self.fin[u] = self.view(u, DUO, 0)[...] + (got[0] + got[1] + got[DUO])
            self.copy(self.fin.at[u, self.give], self.out(u), (self.swap_sems.at[0], self.swap_sems.at[1]), self.peer).start()
            self.kept(u).start()
            return
        got = self.buf(u, phase)
        if stage % DUO:
            self.arrived(u, phase, 0, DUO)
            for name, hop in ((0, 1), (1, TRIO)):
                add_into(self.view(u, phase, hop, name), got.at[name])
                self.send(u, phase, name + RING)
            return
        self.arrived(u, phase, DUO, RING)
        if phase == 0 and BEFORE[u] is not None:
            self.drain(BEFORE[u], 1)
            self.drain(BEFORE[u], DUO)
        for half, names in ((0, (TRIO, RING)), (1, (DUO, 5))):
            if phase:
                add_into(self.view(u, phase, 0, half), *[got.at[name] for name in names])
            else:
                dst = self.mid.at[self.slot(u) + (ALL, ALL, HALVES[half], slice(None))]
                add_into(dst, self.view(u, 0, 0, half), *[got.at[name] for name in names], fresh=True)
        self.launch(u, phase + 1)

    def finish(self):
        for u in range(N_UNITS):
            for phase in range(TRIO):
                self.drain(u, phase)
        half = self.fin.at[:, pl.ds(0, SHARE)]
        swaps = self.copy(half, half, (self.swap_sems.at[0], self.swap_sems.at[1]), self.peer)
        swaps.wait_send()
        swaps.wait_recv()
        for u in range(N_UNITS):
            self.kept(u).wait()


def attend(heads, qt, do_t, k, kt, v, vt, cos, sin, o_row, ot, dq, dkt, dvt, s_scr, e_scr, p_scr, d_scr):
    f32, bf16 = jnp.float32, jnp.bfloat16
    strip = TURN
    work = [(h, j) for j in range(NBLK) for h in range(len(heads))]

    def strips(c):
        return [(i * strip, slice(c * QB + i * strip, c * QB + (i + 1) * strip)) for i in range(QB // strip)]

    def fold(x, op):
        return op(x.reshape(strip // SUBS, SUBS, QB), axis=0)

    def scores(i):
        (h, j), b = work[i], i % DUO
        q_t = qt[heads[h], j * QB:(j + 1) * QB]
        top = jnp.full((SUBS, QB), -jnp.inf, f32)
        for c in range(j + 1):
            tile = dot(k[c * QB:(c + 1) * QB, :], q_t)
            for at, rows in strips(c):
                s = tile[at:at + strip]
                if c == j:
                    seen = lax.broadcasted_iota(jnp.int32, (strip, QB), 0) + at <= lax.broadcasted_iota(jnp.int32, (strip, QB), 1)
                    s = jnp.where(seen, s, -jnp.inf)
                s_scr[b, rows, :] = s
                top = jnp.maximum(top, fold(s, jnp.max))
        return jnp.max(top, axis=0, keepdims=True)

    def rest(i, m):
        (h, j), b = work[i], i % DUO
        cols, n = slice(j * QB, (j + 1) * QB), (j + 1) * QB
        q_t, d_t = qt[heads[h], cols], do_t[heads[h], cols]
        tot = jnp.zeros((SUBS, QB), f32)
        for c in range(j + 1):
            for at, rows in strips(c):
                e = jnp.exp2((s_scr[b, rows, :] - m) * (SCALE * LOG2E))
                s_scr[b, rows, :] = e
                e_scr[b, rows, :] = e.astype(bf16)
                tot = tot + fold(e, jnp.sum)
        den = jnp.sum(tot, axis=0, keepdims=True)
        inv = 1.0 / den
        o = (dot(vt[:, :n], e_scr[b, :n, :]) / den).astype(bf16)
        ot[o_row(h), cols] = o
        delta = jnp.sum(d_t.astype(f32) * o.astype(f32), axis=0, keepdims=True)
        for c in range(j + 1):
            dp = dot(v[c * QB:(c + 1) * QB, :], d_t)
            for at, rows in strips(c):
                p = s_scr[b, rows, :] * inv
                p_scr[b, rows, :] = p.astype(bf16)
                d_scr[b, rows, :] = (p * (dp[at:at + strip] - delta)).astype(bf16)
        dvt[:, :n] += dot_nt(d_t, p_scr[b, :n, :])
        dkt[:, :n] += dot_nt(q_t, d_scr[b, :n, :])
        g = dot(kt[:, :n], d_scr[b, :n, :]) * SCALE
        co, si = cos[:, cols], sin[:, cols]
        x, y = g[:TURN], g[TURN:]
        dq[heads[h], cols] = jnp.concatenate([x * co + y * si, y * co - x * si], axis=0).astype(bf16)

    m = scores(0)
    for i in range(len(work)):
        later = scores(i + 1) if i + 1 < len(work) else None
        rest(i, m)
        m = later


def tail_kernel(qt, do_t, k, kt, v, vt, rt, dyc, wqk, wqkp, wvo, wvop, gain, hidden, dy, pos, cos, sin,
                result, grad_x, gq, gk, gv, go, gout,
                two, ks, kts, vs, vts, rts, ots, dqo, dqp, dkvo, dkvp, dkt, dvt, s_scr, e_scr, p_scr, d_scr, dycs, part, mid, buf1, buf2, buf3, fin, own, onat, dnat, xs, gacc, gpart, gpeer, gz, gx,
                send_sems, recv_sems, swap_sems, trade_send, trade_recv, local_sems):
    comm = Singles(trade_send, trade_recv, local_sems)
    comm.used = HEADS
    f32, bf16 = jnp.float32, jnp.bfloat16
    core, peer = comm.core, comm.peer()
    a1, a2 = two.at[0], two.at[1]
    comm.announce(CORNERS)
    sc = Scatter(comm, part, mid, (buf1, buf2, buf3), fin, (gq, gk, gv, go), send_sems, recv_sems, swap_sems)
    plan = Plan()
    some, most = pl.ds(0, PAIR), pl.ds(PAIR, HALF - PAIR)
    loads = [comm.local(s, d) for s, d in ((qt.at[some], two.at[0, some]), (k, ks), (do_t.at[some], two.at[1, some]), (vt, vts), (v, vs), (kt, kts))]
    dkt[...] = jnp.zeros_like(dkt)
    dvt[...] = jnp.zeros_like(dvt)
    with scope('wait_q'):
        for c in loads:
            c.wait()
    loads = [comm.local(s, d) for s, d in ((rt, rts), (qt.at[most], two.at[0, most]), (do_t.at[most], two.at[1, most]))]
    later = [comm.local(s, d) for s, d in ((dyc, dycs), (hidden, xs))]

    def emit(stages):
        for u, stage in stages:
            with scope(f'u{u}_s{stage}'):
                if u == GAIN:
                    sum_gain(stage)
                else:
                    sc.run(u, stage)

    def after(cost):
        plan.now += cost
        return plan.due()

    def head_trades(g):
        row = pl.ds(pl.multiple_of((core * HEADS + DUO * g) * LANES, PAIR), PAIR)
        mine = tile_at(g, PAIR)
        return [pltpu.make_async_remote_copy(src_ref=s, dst_ref=d, send_sem=trade_send.at[i], recv_sem=trade_recv.at[i], device_id=peer, device_id_type=MESH)
                for s, d, i in ((ots.at[row], ots.at[row], g), (dqo.at[mine], dqp.at[mine], PAIRS + g))]

    def gradient(place, count, left, right, mul):
        with scope('grad'):
            @pl.loop(0, DUO)
            def _(z):
                g = mul(left[tile_at(z, HALF), :], right())
                for i in range(count):
                    part[place + i, tile_at(z, DUO)] = g[:, i * LANES:(i + 1) * LANES].reshape(DUO, RING, RING, CHIP, LANES)

    attended, paired = [], []
    for g in range(PAIRS):
        attended.append(after(5.1))
        plan.now += 1.5
        plan.start(DUO * g)
        plan.start(DUO * g + 1)
        paired.append(plan.due())

    @pl.loop(0, PAIRS)
    def _(g):
        def at(table):
            for i in range(PAIRS):
                if table[i]:
                    pl.when(g == i)(functools.partial(emit, table[i]))

        heads = [tile_at(DUO * g + i, LANES) for i in range(DUO)]
        with scope('attend'):
            attend(heads, a1, a2, ks, kts, vs, vts, cos, sin, lambda i: tile_at(core * HEADS + DUO * g + i, LANES), ots, dqo, dkt, dvt, s_scr, e_scr, p_scr, d_scr)

        @pl.when(g == 0)
        def _():
            with scope('entry'):
                comm.meet(CORNERS)
                for c in loads:
                    c.wait()
        for c in head_trades(g):
            c.start()
        at(attended)
        gradient(DUO * g, DUO, rts, lambda: dqo[tile_at(g, PAIR), :], dot_nt)
        at(paired)

    def beat(cost, *starts):
        plan.now += cost
        for u in starts:
            plan.start(u)
        emit(plan.due())

    wkv, wkvp = e_scr.reshape(DIM, PAIR), p_scr.reshape(DIM, PAIR)
    later += [comm.local(src.at[:, pl.ds(at, LANES)], dst.at[:, pl.ds(to, LANES)]) for srcs, dst in (((wqk, wvo), wkv), ((wqkp, wvop), wkvp)) for src, at, to in ((srcs[0], HALF, 0), (srcs[1], 0, LANES))]
    wqp_loads = [comm.local(wqkp.at[tile_at(i, HALF), pl.ds(0, HALF)], two.at[i]) for i in range(DUO)]
    key = dkt[...] * SCALE
    co, si, x, y = cos[...], sin[...], key[:TURN], key[TURN:]
    dkvo[:LANES, :] = jnp.concatenate([x * co + y * si, y * co - x * si], axis=0).astype(bf16)
    dkvo[LANES:, :] = dvt[...].astype(bf16)
    comm.trade(dkvo, dkvp)
    gradient(UNIT_K, DUO, rts, lambda: dkvo[...], dot_nt)
    beat(1.8, UNIT_K, UNIT_V)
    wq_load = comm.local(wqk.at[:, pl.ds(0, HALF)], rts)
    for c in later:
        c.wait()
    with scope('trades'):
        for g in range(PAIRS):
            for c in head_trades(g):
                c.wait()

    waiting = list(range(RING))

    def output_gradients(force=False):
        while waiting:
            first = 10 + DUO * waiting[0]
            before = [u for u in range(N_UNITS) if u < first and PLACE[u] in (PLACE[first], PLACE[first + 1])]
            if force:
                emit(plan.rush(lambda: all(map(plan.vacated, before))))
            if not all(map(plan.vacated, before)):
                return
            for u in before:
                sc.drain(u, 0)
            i = waiting.pop(0)
            gradient(PLACE[first], DUO, ots, lambda: dycs[:, i * PAIR:(i + 1) * PAIR], dot)
            plan.start(first)
            plan.start(first + 1)
            beat(1.5)

    def piece(cost):
        beat(cost)
        output_gradients()

    def ticking(n, cost, body):
        tables = [after(cost) for _ in range(n)]

        @pl.loop(0, n)
        def _(i):
            body(i)
            for j, table in enumerate(tables):
                if table:
                    pl.when(i == j)(functools.partial(emit, table))
        output_gradients()

    @pl.loop(0, TOKENS // LANES)
    def _(i):
        want = lax.broadcasted_iota(jnp.int32, (LANES, ROWS), 0) + i * LANES
        own[tile_at(i, LANES), :] = jnp.where(want == pos[...], 1.0, 0.0).astype(bf16)

    def unsort(at, src_t, n):
        with scope('unsort'):
            dnat[at:at + n, :] = dot(src_t[:n, :], own[...]).astype(bf16)

    output_gradients()
    for c in comm.exchanged:
        c.wait_recv()
    unsort(0, dqo, HALF)
    dy_loads = [comm.local(dy.at[:, tile_at(i, HALF)], dqo.at[tile_at(i, ROWS)]) for i in range(DUO)]
    piece(1.2)
    unsort(HALF, dqp, HALF)
    piece(1.2)
    unsort(DUO * HALF, dkvo, PAIR)
    unsort(DUO * HALF + PAIR, dkvp, PAIR)
    piece(0.7)
    wq_load.wait()
    for c in wqp_loads + dy_loads:
        c.wait()
    gacc[...] = jnp.zeros_like(gacc)

    def dr_parts(half, r):
        return [s_scr.at[half, r(i * PAIR), :] for i in range(RING)]

    def back(block, then):
        def dr(half):
            with scope('dr'):
                c = tile_at(half, HALF)
                left = jnp.concatenate([rts[c, :], two[half], wkv[c, :], wkvp[c, :]], axis=1)
                acc = dot(left, dnat[:, block * PAIR:(block + 1) * PAIR])
                for i, ref in enumerate(dr_parts(half, lambda at: pl.ds(at, PAIR))):
                    ref[...] = acc[i * PAIR:(i + 1) * PAIR, :].T

        def norm(part):
            with scope('back'):
                @pl.loop(0, RING)
                def _(i):
                    j = part * RING + i
                    q = pl.ds(pl.multiple_of(block * PAIR + j * SHARE, SHARE), SHARE)
                    d = jnp.concatenate([ref[...] for half in range(DUO) for ref in dr_parts(half, lambda at: pl.ds(pl.multiple_of(at + j * SHARE, SHARE), SHARE))], axis=1)
                    x = xs[q, :].astype(f32)
                    inv = lax.rsqrt(jnp.mean(x * x, axis=-1, keepdims=True) + RMS_EPS)
                    unit = x * inv
                    gacc[...] += jnp.sum((d * unit).reshape(DUO, SUBS, DIM), axis=0)
                    dg = d * gain[0:1, :]
                    new = inv * (dg - unit * jnp.mean(dg * unit, axis=-1, keepdims=True))
                    for half in range(DUO):
                        r = pl.ds(pl.multiple_of(half * ROWS + block * PAIR + j * SHARE, SHARE), SHARE)
                        dqo[r, :] = (dqo[r, :].astype(f32) + new[:, half * HALF:(half + 1) * HALF]).astype(bf16)

        ticking(DUO, 1.6, dr)
        then()
        ticking(RING, 0.92, norm)

    back(0, lambda: None)
    wo_loads = []
    back(1, lambda: wo_loads.extend([comm.local(wvo.at[:, pl.ds(LANES, HALF)], rts)] + [comm.local(wvop.at[tile_at(i, HALF), pl.ds(LANES, HALF)], two.at[i]) for i in range(DUO)]))
    for i in range(DUO):
        comm.store(dqo.at[tile_at(i, ROWS)], grad_x.at[:, tile_at(i, HALF)])
    total = jnp.sum(gacc[...], axis=0, keepdims=True)
    gpart[...] = jnp.zeros_like(gpart)
    for i in range(RING):
        for j in range(RING):
            gpart[i, j:j + 1, :] = total[:, (i * RING + j) * LANES:(i * RING + j + 1) * LANES]

    gain_c, gain_z, gain_p = (Batch(comm) for _ in range(TRIO))

    def sum_gain(stage):
        if stage == 0:
            gain_c.send(gpart, gpeer, peer)
        elif stage == 1:
            gain_c.arrived(gpeer)
            for j in range(RING):
                gz[j] = gpart[j] + gpeer[j]
            for hop in (1, DUO, TRIO):
                gain_z.send(gz.at[step(comm.pos, 'z', hop)], gz.at[TRIO + hop], comm.far('z', hop))
        elif stage == DUO:
            gain_z.arrived(gz.at[pl.ds(RING, TRIO)])
            gx[0] = (gz[comm.pos['z']] + gz[RING]) + (gz[5] + gz[6])
            for dy, dx in PLANE:
                gain_p.send(gx.at[0], gx.at[dy * RING + dx], comm.aside(dy, dx))
        else:
            gain_p.arrived(gx.at[pl.ds(1, 15)])
            gpeer[0] = jnp.sum(gx[...], axis=0)
            mine = jnp.broadcast_to(gpeer[0, pl.ds(comm.pos['y'], 1), :], (SUBS, LANES))
            gout[...] = pltpu.roll(mine, LANES - (comm.pos['x'] * CHIP + core * SHARE), 1)

    plan.start(GAIN)
    beat(0.2)
    for i in range(DUO):
        with scope('unsort_o'):
            @pl.loop(0, DUO)
            def _(j):
                r = pl.ds(pl.multiple_of(i * HALF + j * ROWS, ROWS), ROWS)
                onat[:, r] = dot(ots[r, :], own[...]).astype(bf16).T
        piece(1.58)
    output_gradients(True)

    def project_out(col, weights, i):
        with scope('project'):
            @pl.loop(DUO * i, DUO * i + DUO)
            def _(j):
                c = tile_at(j, PAIR)
                dst = pl.ds(pl.multiple_of(col + j * PAIR, PAIR), PAIR)
                xs[:, dst] = (xs[:, dst].astype(f32) + dot(onat[...], weights(c))).astype(bf16)
        beat(1.48)

    def own_half(c):
        return rts[:, c]

    def other_half(c):
        return jnp.concatenate([a1[:, c], a2[:, c]], axis=0)

    for c in wo_loads:
        c.wait()
    for col, weights in ((core * HALF, own_half), ((1 - core) * HALF, other_half)):
        for i in range(DUO):
            project_out(col, weights, i)
    comm.store(xs, result)
    emit(plan.rush(lambda: not plan.stage))
    with scope('finish'):
        sc.finish()
        for batch, whole in ((gain_c, gpart), (gain_z, gz.at[pl.ds(RING, TRIO)]), (gain_p, gx.at[pl.ds(1, 15)])):
            batch.sent(whole)
        for c in comm.exchanged:
            c.wait_send()
        for c in comm.stored:
            c.wait()


def tail(qt, do_t, k, kt, v, vt, rt, dyc, wqk, wqkp, wvo, wvop, gain, hidden, dy, pos, cos, sin):
    bf16, f32 = jnp.bfloat16, jnp.float32
    any_ = pl.BlockSpec(memory_space=pl.ANY)
    vmem = pl.BlockSpec(memory_space=pltpu.VMEM)
    S = lambda shape, d=bf16: jax.ShapeDtypeStruct(shape, d)
    V = lambda shape, d=bf16: pltpu.VMEM(shape, d)
    D = lambda n: pltpu.SemaphoreType.DMA((n,))
    sq, tall, wide = (HALF, TOKENS), (TOKENS, LANES), (LANES, TOKENS)
    mine, kv = (ROWS, DIM), (PAIR, TOKENS)
    return pl.pallas_call(
        tail_kernel,
        out_shape=[S(mine), S(mine), S((SHARE, DIM), f32), S((SHARE, PAIR), f32), S((SHARE, PAIR), f32), S((SHARE, DIM), f32), S((SUBS, LANES), f32)],
        in_specs=[any_] * 12 + [vmem] + [any_] * DUO + [vmem] * TRIO,
        out_specs=[any_] * 6 + [vmem],
        scratch_shapes=[V((DUO,) + sq), V(tall), V(wide), V(tall), V(wide), V((DIM, TOKENS)), V((DIM, TOKENS)), V(sq), V(sq), V(kv), V(kv), V(wide, f32), V(wide, f32),
                        V((DUO, TOKENS, QB), f32), V((DUO, TOKENS, QB)), V((DUO, TOKENS, QB)), V((DUO, TOKENS, QB)), V(sq), V((PLACES, RING, RING, RING, CHIP, LANES), f32), V((TRIO, SLOTS, RING, RING, CHIP, LANES), f32),
                        V((TRIO, SLOTS, 6, RING, RING, SHARE, LANES), f32), V((TRIO, SLOTS, 6, RING, SHARE, LANES), f32), V((TRIO, SLOTS, TRIO, CHIP, LANES), f32), V((N_UNITS, CHIP, LANES), f32), V((TOKENS, ROWS)), V(mine), V((DUO * QKV, ROWS)), V(mine),
                        V((SUBS, DIM), f32), V((RING, SUBS, LANES), f32), V((RING, SUBS, LANES), f32), V((7, SUBS, LANES), f32), V((SHARE, SUBS, LANES), f32),
                        D(9 * SLOTS), D(15 * SLOTS), D(DUO + N_UNITS), D(HEADS + RING), D(HEADS + RING), D(26)],
        compiler_params=pltpu.CompilerParams(collective_id=1, has_side_effects=True, vmem_limit_bytes=67043328),
        name='tail',
    )(qt, do_t, k, kt, v, vt, rt, dyc, wqk, wqkp, wvo, wvop, gain, hidden, dy, pos, cos, sin)


def settle_kernel(n, *refs):
    ins, gain, outs, gain_out, bufs, sems = refs[:n], refs[n], refs[n + 1:DUO * n + 1], refs[DUO * n + 1], refs[DUO * n + DUO:-1], refs[-1]
    jobs = []
    for a, o, b in zip(ins, outs, bufs):
        size = a.shape[0] // RING if a.shape[0] == ROWS else a.shape[0]
        jobs += [tuple(r.at[pl.ds(i, size)] for r in (a, b, o)) for i in range(0, a.shape[0], size)]
    takes = [pltpu.make_async_copy(a, b, sems.at[0, i]) for i, (a, b, _) in enumerate(jobs)]
    puts = [pltpu.make_async_copy(b, o, sems.at[1, i]) for i, (_, b, o) in enumerate(jobs)]
    for c in takes:
        c.start()
    gain_out[...] = gain[0:1, :SHARE]
    for take, put in zip(takes, puts):
        take.wait()
        put.start()
    for c in puts:
        c.wait()


def settle(*arrays):
    *large, gain = arrays
    any_, vmem = pl.BlockSpec(memory_space=pl.ANY), pl.BlockSpec(memory_space=pltpu.VMEM)
    return pl.pallas_call(
        functools.partial(settle_kernel, len(large)),
        out_shape=[jax.ShapeDtypeStruct(a.shape, a.dtype) for a in large] + [jax.ShapeDtypeStruct((1, SHARE), gain.dtype)],
        in_specs=[any_] * len(large) + [vmem],
        out_specs=[any_] * len(large) + [vmem],
        scratch_shapes=[pltpu.VMEM(a.shape, a.dtype) for a in large] + [pltpu.SemaphoreType.DMA((DUO, 12))],
        name='settle',
    )(*arrays)


def rope_tables():
    j = np.arange(HEAD_DIM // DUO, dtype=np.float64) / (HEAD_DIM // DUO)
    freq = (ROPE_THETA ** -j).astype(np.float32)
    angle = freq[:, None] * np.arange(TOKENS, dtype=np.float32)[None, :]
    return np.cos(angle.astype(np.float64)).astype(np.float32), np.sin(angle.astype(np.float64)).astype(np.float32)


def solution(mesh):
    def shard_fn(hidden, tok_pos, grad_out, norm_gain, w_query, w_key, w_value, w_out):
        hidden, grad_out = hidden[0], grad_out[0]
        cos_t, sin_t = (jnp.asarray(t) for t in rope_tables())
        *parts, gain = head(hidden, grad_out, w_query, w_key, w_value, w_out, tok_pos, norm_gain.reshape(1, SHARE), cos_t, sin_t)
        parts = [p.reshape(DIM, GROUP) if p.ndim > DUO else p for p in parts]
        result, grad_hidden, gq, gk, gv, go, gout = settle(*tail(*parts, gain, hidden, grad_out, tok_pos, cos_t, sin_t))
        return result[None], grad_hidden[None], gq, gk, gv, go, gout.reshape(SHARE)

    row_spec, pos_spec = P('fsdp', 'cp', None), P('fsdp', 'cp')
    weight_spec, gain_spec = P(('fsdp', 'cp'), None), P(('fsdp', 'cp'))
    return jax.shard_map(shard_fn, mesh=mesh, in_specs=(row_spec, pos_spec, row_spec, gain_spec, weight_spec, weight_spec, weight_spec, weight_spec), out_specs=(row_spec, row_spec, weight_spec, weight_spec, weight_spec, weight_spec, gain_spec), check_vma=False)
```

```python
import functools
import jax
import jax.numpy as jnp
import numpy as np
from jax import lax
from jax.experimental import pallas as pl
from jax.experimental.pallas import tpu as pltpu
from jax.sharding import PartitionSpec as P

LANES, SUBS, RING, TRIO, DUO = 128, 8, 4, 3, 2
PAIR, ROWS, CHIP, SHARE, TURN = 256, 512, 32, 16, 64
HEAD_DIM = LANES
ROPE_THETA = 1000000.0
RMS_EPS = 1e-5
SCALE = HEAD_DIM ** -0.5
LOG2E = 1.4426950408889634

MESH = pl.DeviceIdType.MESH
AXES = ('x', 'y', 'z')
ORDERS = (('x', 'y', 'z'), ('y', 'z', 'x'), ('z', 'x', 'y'))
ALL = pl.ds(0, RING)


def torus():
    f = lax.axis_index('fsdp')
    return {'x': lax.rem(f, RING), 'y': lax.rem(lax.div(f, RING), RING), 'z': lax.div(f, SHARE)}


def step(pos, axis, hop):
    return lax.rem(pos[axis] + hop, RING)


class Batch:
    def __init__(self, comm):
        self.comm, self.index = comm, comm.used
        comm.used += 1

    def _copy(self, src, dst, device):
        send, recv, _ = self.comm.sems
        return pltpu.make_async_remote_copy(src_ref=src, dst_ref=dst, send_sem=send.at[self.index], recv_sem=recv.at[self.index], device_id=device, device_id_type=MESH)

    def send(self, src, dst, device):
        self._copy(src, dst, device).start()
        return self

    def arrived(self, whole):
        self._copy(whole, whole, self.comm.peer()).wait_recv()

    def sent(self, whole):
        self._copy(whole, whole, self.comm.peer()).wait_send()


class Comm:
    def __init__(self, send_sems, recv_sems, local_sems):
        self.pos = torus()
        self.core = lax.axis_index('cp')
        self.sems = (send_sems, recv_sems, local_sems)
        self.used = self.used_local = 0
        self.stored = []

    def far(self, axis, hop):
        p = dict(self.pos)
        p[axis] = step(self.pos, axis, hop)
        return {'fsdp': (p['z'] * RING + p['y']) * RING + p['x'], 'cp': self.core}

    def peer(self):
        return {'fsdp': lax.axis_index('fsdp'), 'cp': 1 - self.core}

    def aside(self, dy, dx):
        return {'fsdp': (self.pos['z'] * RING + step(self.pos, 'y', dy)) * RING + step(self.pos, 'x', dx), 'cp': self.core}

    def announce(self, corners=()):
        sem = pltpu.get_barrier_semaphore()
        for axis in AXES:
            for hop in (1, DUO, TRIO):
                pl.semaphore_signal(sem, inc=1, device_id=self.far(axis, hop), device_id_type=MESH)
        for dy, dx in corners:
            pl.semaphore_signal(sem, inc=1, device_id=self.aside(dy, dx), device_id_type=MESH)
        pl.semaphore_signal(sem, inc=1, device_id=self.peer(), device_id_type=MESH)

    def meet(self, corners=()):
        pl.semaphore_wait(pltpu.get_barrier_semaphore(), 10 + len(corners))

    def ring(self, batch, src, slots, axis):
        for hop in (1, DUO, TRIO):
            batch.send(src, slots.at[hop], self.far(axis, hop))

    def local(self, src, dst):
        i = self.used_local
        self.used_local += 1
        c = pltpu.make_async_copy(src, dst, self.sems[DUO].at[i])
        c.start()
        return c

    def store(self, src, dst):
        self.stored.append(self.local(src, dst))


class Singles(Comm):
    def __init__(self, *sems):
        super().__init__(*sems)
        self.sent, self.exchanged = [], []

    def _copy(self, src, dst, device):
        i = self.used
        self.used += 1
        c = pltpu.make_async_remote_copy(src_ref=src, dst_ref=dst, send_sem=self.sems[0].at[i], recv_sem=self.sems[1].at[i], device_id=device, device_id_type=MESH)
        c.start()
        return c

    def send(self, src, dst, device):
        c = self._copy(src, dst, device)
        self.sent.append(c)
        return c

    def trade(self, src, dst):
        self.exchanged.append(self._copy(src, dst, self.peer()))


def pick(ref, sel, piece):
    lo, cols, first, rows = piece
    return ref.at[sel['z'], sel['y'], sel['x'], pl.ds(first, rows), pl.ds(lo, cols)]


def sem_scratch(remote, local):
    return [pltpu.SemaphoreType.DMA((remote,)), pltpu.SemaphoreType.DMA((remote,)), pltpu.SemaphoreType.DMA((local,))]


def add_into(dst, *srcs, fresh=False):
    def add(idx):
        total, *rest = [s[idx] for s in (srcs if fresh else (dst,) + srcs)]
        for more in rest:
            total = total + more
        dst[idx] = total

    if len(dst.shape) > TRIO:
        @pl.loop(0, dst.shape[0])
        def _(i):
            add((i,))
    else:
        add(Ellipsis)


def halves(lo, n):
    return (lo, n, 0, SHARE), (lo, n, SHARE, SHARE)


GROUPS = (halves(0, 384), halves(384, 384), halves(768, 384))
QK_FIRST = (halves(0, PAIR), halves(384, PAIR), halves(768, PAIR))
QK_LAST = (halves(PAIR, LANES), halves(640, LANES), halves(1024, LANES))
TOKENS = 1024
DIM = 2048
HALF = 1024
QKV = 1280
GROUP = 1152


def scope(name):
    return jax.named_scope(name)


def dot(a, b):
    return jnp.dot(a, b, preferred_element_type=jnp.float32)


def dot_nt(a, b):
    return lax.dot_general(a, b, (((1,), (1,)), ((), ())), preferred_element_type=jnp.float32)


def tile_at(i, n):
    return pl.ds(pl.multiple_of(i * n, n), n)


class Gather:
    def __init__(self, comm, ref, colors, land, held=None):
        self.comm, self.ref, self.colors, self.land = comm, ref, colors, land
        self.held = list(held or [dict(comm.pos) for _ in colors])
        self.spent = []

    def move(self, batch, s, piece, to):
        batch.send(pick(self.ref, s, piece), pick(self.ref, s, piece), to)

    def at(self, k, hop):
        d = ORDERS[k][self.phase]
        return dict(self.held[k], **{d: step(self.comm.pos, d, hop)})

    def begin(self, phase):
        self.phase = phase
        self.rest = Batch(self.comm)
        if phase == 0:
            for hop in (DUO, 1, TRIO):
                for k, (a, _) in enumerate(self.colors):
                    self.move(self.rest, self.held[k], (a[0], a[1], 0, CHIP), self.comm.far(ORDERS[k][0], hop))
            return
        self.up, self.dn = ([Batch(self.comm) for _ in range(TRIO)] for _ in range(DUO))
        for k, (a, b) in enumerate(self.colors):
            d = ORDERS[k][phase]
            up, dn, s = self.comm.far(d, 1), self.comm.far(d, TRIO), self.held[k]
            self.move(self.up[k], s, a, up)
            self.move(self.dn[k], s, b, dn)
            self.move(self.rest, s, b, up)
            self.move(self.rest, s, a, dn)
        if phase == DUO:
            for k, pieces in enumerate(self.colors):
                for piece in pieces:
                    self.land(self.ref, self.held[k], piece)

    def forward(self):
        for k, (a, b) in enumerate(self.colors):
            d = ORDERS[k][self.phase]
            for batch, hop, piece, to in ((self.up[k], TRIO, a, 1), (self.dn[k], 1, b, TRIO)):
                s = self.at(k, hop)
                batch.arrived(pick(self.ref, s, piece))
                self.move(self.rest, s, piece, self.comm.far(d, to))
                if self.phase == DUO:
                    self.land(self.ref, s, piece)
                self.spent.append((batch, pick(self.ref, self.held[k], piece)))

    def end(self):
        axis = ORDERS[0][self.phase]
        blocks = dict(self.held[0], **{axis: pl.ds(0, DUO if self.phase else TRIO)})
        width = sum(a[1] for a, _ in self.colors)
        whole = pick(self.ref, blocks, (0, width, 0, CHIP))
        self.rest.arrived(whole)
        self.spent.append((self.rest, whole))
        for k, (a, b) in enumerate(self.colors):
            if self.phase == DUO:
                for hop, piece in ((TRIO, b), (1, a), (DUO, a), (DUO, b)):
                    self.land(self.ref, self.at(k, hop), piece)
            self.held[k] = dict(self.held[k], **{ORDERS[k][self.phase]: ALL})

    def finish(self):
        for batch, whole in self.spent:
            batch.sent(whole)


def head_kernel(hidden, dy, wq, wk, wv, wo, pos, gain_in, cos_t, sin_t,
                qt_o, dot_o, k_o, kt_o, v_o, vt_o, rt_o, dyc_o, wqk_o, wqkp_o, wvo_o, wvop_o, gain_o,
                hid2, dy2, dys, rs, rt, wqk, wvo, wpeer, pi, pos2, qt, dot_s, kk, kt, vv, vt, gain, gtile, gbuf, gx, gy, gz, *sems):
    comm = Comm(*sems)
    comm.announce()
    pos_c, core = comm.pos, comm.core
    bf16, f32 = jnp.bfloat16, jnp.float32
    peer = comm.peer()
    rows = tile_at(core, SHARE)
    mine_qk = wqk.at[pos_c['z'], pos_c['y'], pos_c['x'], rows]
    mine_vo = wvo.at[pos_c['z'], pos_c['y'], pos_c['x'], rows]

    def weight_parts(c):
        return ((wq.at[:, tile_at(c, HALF)], mine_qk.at[:, pl.ds(0, HALF)]), (wk.at[:, tile_at(c, LANES)], mine_qk.at[:, pl.ds(HALF, LANES)]),
                (wv.at[:, tile_at(c, LANES)], mine_vo.at[:, pl.ds(0, LANES)]), (wo.at[:, tile_at(c, HALF)], mine_vo.at[:, pl.ds(LANES, HALF)]))

    loads = [comm.local(s, d) for s, d in weight_parts(core)]
    load_x = [comm.local(hidden, hid2.at[pl.ds(0, ROWS)]), comm.local(dy, dy2.at[pl.ds(0, ROWS)])]
    share = lax.broadcasted_iota(jnp.int32, (SUBS, LANES), 1) // SHARE
    gtile[...] = jnp.where(share == pos_c['x'] * DUO + core, jnp.broadcast_to(jnp.concatenate([gain_in[...]] * SUBS, axis=1), (SUBS, LANES)), 0.0)
    with scope('entry'):
        comm.meet()
    swap_w, swap_pos, swap_dy, swap_x, peers_qk, peers_vo = (Batch(comm) for _ in range(6))
    gain_c, gain_x, gain_y, gain_z = (Batch(comm) for _ in range(RING))
    for s, d in weight_parts(1 - core):
        swap_w.send(s, d, peer)
    gain_c.send(gtile, gbuf, peer)
    swap_pos.send(pos, pos2, peer)
    for c in loads:
        c.wait()
    with scope('wait_w'):
        swapped = wqk.at[pos_c['z'], pos_c['y'], pos_c['x']]
        swap_w.arrived(swapped)

    def land_qk(ref, s, cols):
        peers_qk.send(pick(ref, s, cols), pick(wqkp_o, s, cols), peer)

    def land_vo(ref, s, cols):
        peers_vo.send(pick(ref, s, cols), pick(wpeer, s, cols), peer)

    g1 = Gather(comm, wvo, GROUPS, land_vo)
    g2 = Gather(comm, wqk, GROUPS, land_qk)
    g1.begin(0)
    g2.begin(0)
    gain_c.arrived(gbuf)
    gx[0] = gtile[...] + gbuf[...]
    comm.ring(gain_x, gx.at[0], gx, 'x')

    swap_pos.arrived(pos2)

    @pl.loop(0, TOKENS // LANES)
    def _(i):
        want = lax.broadcasted_iota(jnp.int32, (LANES, ROWS), 0) + i * LANES
        for h, have in enumerate((pos, pos2)):
            pi[tile_at(i, LANES), h * ROWS:(h + 1) * ROWS] = jnp.where(want == have[...], 1.0, 0.0).astype(bf16)

    def sort(dst, src, first, last):
        with scope('sort'):
            @pl.loop(first, last)
            def _(j):
                c = tile_at(j, PAIR)
                dst[:, c] = dot(pi[...], src[:, c]).astype(bf16)

    swap_dy.send(dy, dy2.at[pl.ds(ROWS, ROWS)], peer)
    with scope('p0_end'):
        for g in (g1, g2):
            g.end()
            g.begin(1)
    swap_x.send(hidden, hid2.at[pl.ds(ROWS, ROWS)], peer)
    gain_x.arrived(gx.at[pl.ds(1, TRIO)])
    gy[pos_c['y']] = (gx[0] + gx[1]) + (gx[DUO] + gx[TRIO])
    for hop in (1, DUO, TRIO):
        gain_y.send(gy.at[pos_c['y']], gy.at[pos_c['y']], comm.far('y', hop))
    with scope('wait_dy'):
        load_x[1].wait()
        swap_dy.arrived(dy2.at[pl.ds(ROWS, ROWS)])
    sort(dys, dy2, 0, RING)
    with scope('p1a_fwd'):
        g1.forward()
    sort(dys, dy2, RING, 6)
    with scope('p1b_fwd'):
        g2.forward()
    sort(dys, dy2, 6, SUBS)
    with scope('p1a_end'):
        g1.end()
    gain_y.arrived(gy.at[pl.ds(1, TRIO)])
    for j in range(RING):
        gz[pos_c['z'], j] = gy[j]
    for hop in (1, DUO, TRIO):
        gain_z.send(gz.at[pos_c['z']], gz.at[pos_c['z']], comm.far('z', hop))
    g1.begin(DUO)
    comm.store(dys.at[:, tile_at(core, HALF)], dyc_o)
    with scope('p1b_end'):
        g2.end()
    with scope('wait_x'):
        load_x[0].wait()
        swap_x.arrived(hid2.at[pl.ds(ROWS, ROWS)])
    sort(rs, hid2, 0, SUBS)
    with scope('p2q_fwd'):
        g1.forward()
    g2a, g2b = (Gather(comm, wqk, colors, land_qk, g2.held) for colors in (QK_FIRST, QK_LAST))
    g2a.begin(DUO)
    with scope('gain'):
        gain_z.arrived(gz.at[pl.ds(1, TRIO)])
    for i in range(RING):
        for j in range(RING):
            gain[:, (i * RING + j) * LANES:(i * RING + j + 1) * LANES] = gz[i, j]
    comm.store(gain, gain_o)

    def norm(first, last):
        with scope('norm'):
            @pl.loop(first, last)
            def _(i):
                r = tile_at(i, CHIP)
                x = rs[r, :].astype(f32)
                inv = lax.rsqrt(jnp.mean(x * x, axis=-1, keepdims=True) + RMS_EPS)
                rs[r, :] = (x * inv * gain[0:1, :]).astype(bf16)

    norm(0, TOKENS // CHIP)
    with scope('r_t'):
        @pl.loop(0, DIM // PAIR)
        def _(i):
            c = tile_at(i, PAIR)

            @pl.loop(0, TOKENS // PAIR)
            def _(j):
                r = tile_at(j, PAIR)
                rt[c, r] = rs[r, c].T
    comm.store(rt, rt_o)
    with scope('p2o_end'):
        g1.end()
    w_qk, w_vo, w_peer = wqk.reshape(DIM, GROUP), wvo.reshape(DIM, GROUP), wpeer.reshape(DIM, GROUP)
    with scope('vals'):
        @pl.loop(0, DUO)
        def _(i):
            r = tile_at(i, ROWS)
            val = dot(rs[r, :], w_vo[:, :LANES]).astype(bf16)
            vv[r, :] = val
            vt[:, r] = val.T
    for src, dst in ((wvo, wvo_o), (vv, v_o), (vt, vt_o)):
        comm.store(src, dst)
    with scope('p2q_fwd'):
        g2a.forward()
    g2b.begin(DUO)
    with scope('wo_peer'):
        peers_vo.arrived(wpeer)
    comm.store(wpeer, wvop_o)
    with scope('do_t'):
        mine = tile_at(core, HALF)

        @pl.loop(0, TOKENS // PAIR)
        def _(j):
            t = tile_at(j, PAIR)
            w_rows = jnp.concatenate([w_vo[mine, LANES:], w_peer[mine, LANES:]], axis=1)
            d_rows = jnp.concatenate([dys[t, mine], dys[t, tile_at(1 - core, HALF)]], axis=1)
            dot_s[:, t] = dot_nt(w_rows, d_rows).astype(bf16)
    comm.store(dot_s, dot_o)

    def rotated(x, r):
        cos, sin = cos_t[:, r], sin_t[:, r]
        cos = jnp.concatenate([cos, cos], axis=0).T
        sin = jnp.concatenate([-sin, sin], axis=0).T
        return (x * cos + pltpu.roll(x, TURN, 1) * sin).astype(bf16)

    def queries(columns, heads):
        x = dot(rs[...], columns)
        for i in range(RING):
            r = slice(i * PAIR, (i + 1) * PAIR)
            for h, head in enumerate(heads):
                qt[tile_at(head, LANES), r] = rotated(x[r, h * LANES:(h + 1) * LANES], r).T

    with scope('p2q_end'):
        g2a.end()

    def pairs(first, last):
        with scope('q'):
            @pl.loop(first, last)
            def _(t):
                queries(w_qk[:, pl.ds(pl.multiple_of(t * 384, LANES), PAIR)], (TRIO * t, TRIO * t + 1))

    with scope('last_fwd'):
        g2b.forward()
    pairs(0, TRIO)
    for t in range(TRIO):
        two_heads = pl.ds(t * 384, PAIR)
        comm.store(qt.at[two_heads], qt_o.at[two_heads])
    with scope('last_end'):
        g2b.end()
    comm.store(wqk, wqk_o)
    with scope('q_last'):
        x = dot(rs[...], jnp.concatenate([w_qk[:, PAIR:384], w_qk[:, 640:768], w_qk[:, HALF:]], axis=1))
        for i in range(RING):
            r = slice(i * PAIR, (i + 1) * PAIR)
            key = rotated(x[r, PAIR:], r)
            kk[r, :] = key
            kt[:, r] = key.T
            for h, head in enumerate((DUO, 5)):
                qt[tile_at(head, LANES), r] = rotated(x[r, h * LANES:(h + 1) * LANES], r).T
    for src, dst in ((kk, k_o), (kt, kt_o)) + tuple((qt.at[tile_at(h, LANES)], qt_o.at[tile_at(h, LANES)]) for h in (DUO, 5)):
        comm.store(src, dst)
    with scope('finish'):
        peers_qk.arrived(wqk)
        for batch, whole in ((swap_w, swapped), (swap_pos, pos2), (swap_dy, dy2.at[pl.ds(ROWS, ROWS)]), (swap_x, hid2.at[pl.ds(ROWS, ROWS)]), (peers_qk, wqk), (peers_vo, wvo),
                             (gain_c, gbuf), (gain_x, gx.at[pl.ds(1, TRIO)]), (gain_y, gy.at[pl.ds(1, TRIO)]), (gain_z, gz.at[pl.ds(1, TRIO)])):
            batch.sent(whole)
        for g in (g1, g2, g2a, g2b):
            g.finish()
        for c in comm.stored:
            c.wait()


def head(hidden, dy, wq, wk, wv, wo, pos, gain, cos_t, sin_t):
    bf16, f32 = jnp.bfloat16, jnp.float32
    any_ = pl.BlockSpec(memory_space=pl.ANY)
    vmem = pl.BlockSpec(memory_space=pltpu.VMEM)
    S = lambda shape, d=bf16: jax.ShapeDtypeStruct(shape, d)
    V = lambda shape, d=bf16: pltpu.VMEM(shape, d)
    group = (RING, RING, RING, CHIP, GROUP)
    sq, tall, wide = (HALF, TOKENS), (TOKENS, LANES), (LANES, TOKENS)
    full = (TOKENS, DIM)
    return pl.pallas_call(
        head_kernel,
        out_shape=[S(sq), S(sq), S(tall), S(wide), S(tall), S(wide), S((DIM, TOKENS)), S((TOKENS, HALF)), S(group), S(group), S(group), S(group), S((SUBS, DIM), f32)],
        in_specs=[any_] * 6 + [vmem] * RING,
        out_specs=[any_] * 13,
        scratch_shapes=[V(full), V(full), V(full), V(full), V((DIM, TOKENS)), V(group), V(group), V(group), V((TOKENS, TOKENS)), V((1, ROWS), jnp.int32),
                        V(sq), V(sq), V(tall), V(wide), V(tall), V(wide), V((SUBS, DIM), f32), V((SUBS, LANES), f32), V((SUBS, LANES), f32), V((RING, SUBS, LANES), f32), V((RING, SUBS, LANES), f32), V((RING, RING, SUBS, LANES), f32)] + sem_scratch(47, 22),
        compiler_params=pltpu.CompilerParams(collective_id=0, has_side_effects=True, vmem_limit_bytes=60 * DUO**20),
        name='head',
    )(hidden, dy, wq, wk, wv, wo, pos, gain, cos_t, sin_t)


HEADS = SUBS
UNIT_K, UNIT_V = SUBS, 9
N_UNITS = 18
GAIN = N_UNITS
SLOTS = RING
LAST = 5
ABREAST = DUO
LINES = ((0, TRIO, 6, 9, 12, 15), (1, RING, 7, 10, 13, SHARE), (DUO, 5, SUBS, 11, 14, 17))
COLOR = {u: k for k, line in enumerate(LINES) for u in line}
RANK = {u: i for line in LINES for i, u in enumerate(line)}
SWAPPED = (1, TRIO, RING, SUBS, 10)
ORDER = {u: ORDERS[k] if u not in SWAPPED else (ORDERS[k][0], ORDERS[k][DUO], ORDERS[k][1]) for u, k in COLOR.items()}
BEFORE = {u: line[i - SLOTS] if i >= SLOTS else None for line in LINES for i, u in enumerate(line)}
PLACES = 12
PLACE = {u: u % PLACES for u in range(N_UNITS)}
WIRE = (2.82, 0.71, 0.36)
LATENCY = 2.4
STAGE_COST = 0.08


class Plan:
    def __init__(self):
        self.now, self.stage, self.ready, self.order, self.link = 0.0, {}, {}, [], {}
        self.mark = {}

    def _wire(self, u, phase, count):
        link = ORDER[u][phase]
        t = max(self.link.get(link, 0.0), self.now)
        first = t + WIRE[phase] + LATENCY
        self.link[link] = t + WIRE[phase] * count
        return first if phase < DUO else self.link[link] + LATENCY

    def free(self, u, phase):
        if BEFORE[u] is None:
            return True
        done = self.mark.get((BEFORE[u], (DUO, RING, 5)[phase]))
        if done is None:
            return False
        sent = ((0, 1), (DUO, TRIO), (RING,))[phase]
        return any(self.mark.get((j, s), -1) > done and (j, s + 1) in self.mark for j, order in ORDER.items() if order[phase] == ORDER[u][phase] for s in sent)

    def run(self, u):
        stage = self.stage[u]
        self.order.append((u, stage))
        self.mark[u, stage] = len(self.order)
        self.now = max(self.now, self.ready[u]) + STAGE_COST
        self.stage[u] = stage + 1
        if stage == (TRIO if u == GAIN else LAST):
            del self.stage[u]
        elif u == GAIN:
            self.ready[u] = max([self.now] + [self.link.get(a, 0.0) for a in ('', 'z', 'xy')[stage]]) + DUO * LATENCY
        elif stage % DUO:
            self.ready[u] = self._wire(u, stage // DUO, 1)
        else:
            self.ready[u] = self._wire(u, stage // DUO, DUO)

    def blocked(self, u):
        stage = self.stage[u]
        if u == GAIN:
            return False
        if stage == 0 and sum(0 < self.stage.get(j, 0) <= DUO for j in LINES[COLOR[u]]) >= ABREAST:
            return True
        if stage == DUO and BEFORE[u] is not None and (BEFORE[u], LAST) not in self.mark:
            return True
        return stage in (0, DUO, RING) and not self.free(u, stage // DUO)

    def start(self, u):
        self.stage[u], self.ready[u] = 0, self.now

    def due(self):
        first = len(self.order)
        while True:
            ripe = [(self.ready[u], u) for u in self.stage if self.ready[u] <= self.now and not self.blocked(u)]
            if not ripe:
                return self.order[first:]
            self.run(min(ripe)[1])

    def vacated(self, u):
        return (u, DUO) in self.mark

    def rush(self, done):
        first = len(self.order)
        while not done():
            self.run(min((self.ready[u], u) for u in self.stage if not self.blocked(u))[1])
        return self.order[first:]


QB = PAIR
PAIRS = HEADS // DUO
NBLK = TOKENS // QB
HALVES = (pl.ds(0, SHARE), pl.ds(SHARE, SHARE))
PLANE = tuple((dy, dx) for dy in range(RING) for dx in range(RING) if dy or dx)
CORNERS = tuple((dy, dx) for dy, dx in PLANE if dy and dx)


class Scatter:
    def __init__(self, comm, part, mid, bufs, fin, outs, send_sems, recv_sems, swap_sems):
        self.pos, self.part, self.mid, self.bufs, self.fin, self.outs = comm.pos, part, mid, bufs, fin, outs
        self.send_sems, self.recv_sems, self.swap_sems = send_sems, recv_sems, swap_sems
        self.near = {(a, hop): comm.far(a, hop) for a in AXES for hop in (1, DUO, TRIO)}
        self.hops = {(a, hop): step(comm.pos, a, hop) for a in AXES for hop in (1, DUO, TRIO)}
        self.peer, self.core = comm.peer(), comm.core
        self.keep, self.give = tile_at(comm.core, SHARE), tile_at(1 - comm.core, SHARE)
        self.drained = set()

    def slot(self, u):
        return COLOR[u], RANK[u] % SLOTS

    def buf(self, u, phase):
        return self.bufs[phase].at[self.slot(u)]

    def view(self, u, phase, hop, half=None):
        order = ORDER[u]
        at = {a: ALL for a in AXES}
        for a in order[1:phase]:
            at[a] = self.pos[a]
        at[order[phase]] = self.hops[order[phase], hop] if hop else self.pos[order[phase]]
        rows = pl.ds(0, CHIP) if half is None else HALVES[half]
        if phase == 0:
            return self.part.at[PLACE[u], at['z'], at['y'], at['x'], rows, :]
        return self.mid.at[self.slot(u) + tuple(at[a] for a in 'zyx' if a != order[0]) + (rows, slice(None))]

    def copy(self, src, dst, sems, device):
        return pltpu.make_async_remote_copy(src_ref=src, dst_ref=dst, send_sem=sems[0], recv_sem=sems[1], device_id=device, device_id_type=MESH)

    def sems(self, u, phase, kind=0):
        k, i = self.slot(u)
        at = (k * SLOTS + i) * TRIO + phase
        return self.send_sems.at[at], self.recv_sems.at[(k * SLOTS + i) * 5 + DUO * phase + kind]

    def send(self, u, phase, name):
        axis = ORDER[u][phase]
        if phase == DUO:
            src, to = self.view(u, DUO, name + 1), name + 1
        else:
            hop, half, to = ((DUO, 0, 1), (DUO, 1, TRIO), (1, 1, 1), (TRIO, 0, TRIO), (1, 0, 1), (TRIO, 1, TRIO))[name]
            src = self.view(u, phase, hop, half)
        self.copy(src, self.buf(u, phase).at[name], self.sems(u, phase, int(name > 1 and phase < DUO)), self.near[axis, to]).start()

    def launch(self, u, phase):
        if BEFORE[u] is not None:
            self.drain(BEFORE[u], phase)
        for name in range(RING if phase < DUO else TRIO):
            self.send(u, phase, name)

    def arrived(self, u, phase, first, count):
        whole = self.buf(u, phase).at[pl.ds(first, count)]
        self.copy(whole, whole, self.sems(u, phase, int(first > 0)), self.peer).wait_recv()

    def drain(self, u, phase):
        if (u, phase) not in self.drained:
            self.drained.add((u, phase))
            whole = self.buf(u, phase)
            self.copy(whole, whole, self.sems(u, phase), self.peer).wait_send()

    def out(self, u):
        if u < HEADS:
            out, col = self.outs[0], self.core * HALF + u * LANES
        elif u < 10:
            out, col = self.outs[u - 7], self.core * LANES
        else:
            out, col = self.outs[TRIO], self.core * HALF + (u - 10) * LANES
        return out.at[:, pl.ds(pl.multiple_of(col, LANES), LANES)]

    def kept(self, u):
        return pltpu.make_async_copy(self.fin.at[u, self.keep], self.out(u), self.swap_sems.at[DUO + u])

    def run(self, u, stage):
        if stage == 0:
            return self.launch(u, 0)
        phase = (stage - 1) // DUO
        if stage == LAST:
            self.arrived(u, DUO, 0, TRIO)
            got = self.buf(u, DUO)
            self.fin[u] = self.view(u, DUO, 0)[...] + (got[0] + got[1] + got[DUO])
            self.copy(self.fin.at[u, self.give], self.out(u), (self.swap_sems.at[0], self.swap_sems.at[1]), self.peer).start()
            self.kept(u).start()
            return
        got = self.buf(u, phase)
        if stage % DUO:
            self.arrived(u, phase, 0, DUO)
            for name, hop in ((0, 1), (1, TRIO)):
                add_into(self.view(u, phase, hop, name), got.at[name])
                self.send(u, phase, name + RING)
            return
        self.arrived(u, phase, DUO, RING)
        if phase == 0 and BEFORE[u] is not None:
            self.drain(BEFORE[u], 1)
            self.drain(BEFORE[u], DUO)
        for half, names in ((0, (TRIO, RING)), (1, (DUO, 5))):
            if phase:
                add_into(self.view(u, phase, 0, half), *[got.at[name] for name in names])
            else:
                dst = self.mid.at[self.slot(u) + (ALL, ALL, HALVES[half], slice(None))]
                add_into(dst, self.view(u, 0, 0, half), *[got.at[name] for name in names], fresh=True)
        self.launch(u, phase + 1)

    def finish(self):
        for u in range(N_UNITS):
            for phase in range(TRIO):
                self.drain(u, phase)
        half = self.fin.at[:, pl.ds(0, SHARE)]
        swaps = self.copy(half, half, (self.swap_sems.at[0], self.swap_sems.at[1]), self.peer)
        swaps.wait_send()
        swaps.wait_recv()
        for u in range(N_UNITS):
            self.kept(u).wait()


def attend(heads, qt, do_t, k, kt, v, vt, cos, sin, o_row, ot, dq, dkt, dvt, s_scr, e_scr, p_scr, d_scr):
    f32, bf16 = jnp.float32, jnp.bfloat16
    strip = TURN
    work = [(h, j) for j in range(NBLK) for h in range(len(heads))]

    def strips(c):
        return [(i * strip, slice(c * QB + i * strip, c * QB + (i + 1) * strip)) for i in range(QB // strip)]

    def fold(x, op):
        return op(x.reshape(strip // SUBS, SUBS, QB), axis=0)

    def scores(i):
        (h, j), b = work[i], i % DUO
        q_t = qt[heads[h], j * QB:(j + 1) * QB]
        top = jnp.full((SUBS, QB), -jnp.inf, f32)
        for c in range(j + 1):
            tile = dot(k[c * QB:(c + 1) * QB, :], q_t)
            for at, rows in strips(c):
                s = tile[at:at + strip]
                if c == j:
                    seen = lax.broadcasted_iota(jnp.int32, (strip, QB), 0) + at <= lax.broadcasted_iota(jnp.int32, (strip, QB), 1)
                    s = jnp.where(seen, s, -jnp.inf)
                s_scr[b, rows, :] = s
                top = jnp.maximum(top, fold(s, jnp.max))
        return jnp.max(top, axis=0, keepdims=True)

    def rest(i, m):
        (h, j), b = work[i], i % DUO
        cols, n = slice(j * QB, (j + 1) * QB), (j + 1) * QB
        q_t, d_t = qt[heads[h], cols], do_t[heads[h], cols]
        tot = jnp.zeros((SUBS, QB), f32)
        for c in range(j + 1):
            for at, rows in strips(c):
                e = jnp.exp2((s_scr[b, rows, :] - m) * (SCALE * LOG2E))
                s_scr[b, rows, :] = e
                e_scr[b, rows, :] = e.astype(bf16)
                tot = tot + fold(e, jnp.sum)
        den = jnp.sum(tot, axis=0, keepdims=True)
        inv = 1.0 / den
        o = (dot(vt[:, :n], e_scr[b, :n, :]) / den).astype(bf16)
        ot[o_row(h), cols] = o
        delta = jnp.sum(d_t.astype(f32) * o.astype(f32), axis=0, keepdims=True)
        for c in range(j + 1):
            dp = dot(v[c * QB:(c + 1) * QB, :], d_t)
            for at, rows in strips(c):
                p = s_scr[b, rows, :] * inv
                p_scr[b, rows, :] = p.astype(bf16)
                d_scr[b, rows, :] = (p * (dp[at:at + strip] - delta)).astype(bf16)
        dvt[:, :n] += dot_nt(d_t, p_scr[b, :n, :])
        dkt[:, :n] += dot_nt(q_t, d_scr[b, :n, :])
        g = dot(kt[:, :n], d_scr[b, :n, :]) * SCALE
        co, si = cos[:, cols], sin[:, cols]
        x, y = g[:TURN], g[TURN:]
        dq[heads[h], cols] = jnp.concatenate([x * co + y * si, y * co - x * si], axis=0).astype(bf16)

    m = scores(0)
    for i in range(len(work)):
        later = scores(i + 1) if i + 1 < len(work) else None
        rest(i, m)
        m = later


def tail_kernel(qt, do_t, k, kt, v, vt, rt, dyc, wqk, wqkp, wvo, wvop, gain, hidden, dy, pos, cos, sin,
                result, grad_x, gq, gk, gv, go, gout,
                two, ks, kts, vs, vts, rts, ots, dqo, dqp, dkvo, dkvp, dkt, dvt, s_scr, e_scr, p_scr, d_scr, dycs, part, mid, buf1, buf2, buf3, fin, own, onat, dnat, xs, gacc, gpart, gpeer, gz, gx,
                send_sems, recv_sems, swap_sems, trade_send, trade_recv, local_sems):
    comm = Singles(trade_send, trade_recv, local_sems)
    comm.used = HEADS
    f32, bf16 = jnp.float32, jnp.bfloat16
    core, peer = comm.core, comm.peer()
    a1, a2 = two.at[0], two.at[1]
    sc = Scatter(comm, part, mid, (buf1, buf2, buf3), fin, (gq, gk, gv, go), send_sems, recv_sems, swap_sems)
    plan = Plan()
    some, most = pl.ds(0, PAIR), pl.ds(PAIR, HALF - PAIR)
    loads = [comm.local(s, d) for s, d in ((qt.at[some], two.at[0, some]), (k, ks), (do_t.at[some], two.at[1, some]), (vt, vts), (v, vs), (kt, kts))]
    comm.announce(CORNERS)
    dkt[...] = jnp.zeros_like(dkt)
    dvt[...] = jnp.zeros_like(dvt)
    with scope('wait_q'):
        for c in loads:
            c.wait()
    loads = [comm.local(s, d) for s, d in ((rt, rts), (qt.at[most], two.at[0, most]), (do_t.at[most], two.at[1, most]))]
    later = [comm.local(s, d) for s, d in ((dyc, dycs), (hidden, xs))]

    def emit(stages):
        for u, stage in stages:
            with scope(f'u{u}_s{stage}'):
                if u == GAIN:
                    sum_gain(stage)
                else:
                    sc.run(u, stage)

    def after(cost):
        plan.now += cost
        return plan.due()

    def head_trades(g):
        row = pl.ds(pl.multiple_of((core * HEADS + DUO * g) * LANES, PAIR), PAIR)
        mine = tile_at(g, PAIR)
        return [pltpu.make_async_remote_copy(src_ref=s, dst_ref=d, send_sem=trade_send.at[i], recv_sem=trade_recv.at[i], device_id=peer, device_id_type=MESH)
                for s, d, i in ((ots.at[row], ots.at[row], g), (dqo.at[mine], dqp.at[mine], PAIRS + g))]

    def gradient(place, count, left, right, mul):
        with scope('grad'):
            @pl.loop(0, DUO)
            def _(z):
                g = mul(left[tile_at(z, HALF), :], right())
                for i in range(count):
                    part[place + i, tile_at(z, DUO)] = g[:, i * LANES:(i + 1) * LANES].reshape(DUO, RING, RING, CHIP, LANES)

    attended, paired = [], []
    for g in range(PAIRS):
        attended.append(after(5.1))
        plan.now += 1.5
        plan.start(DUO * g)
        plan.start(DUO * g + 1)
        paired.append(plan.due())

    @pl.loop(0, PAIRS)
    def _(g):
        def at(table):
            for i in range(PAIRS):
                if table[i]:
                    pl.when(g == i)(functools.partial(emit, table[i]))

        heads = [tile_at(DUO * g + i, LANES) for i in range(DUO)]
        with scope('attend'):
            attend(heads, a1, a2, ks, kts, vs, vts, cos, sin, lambda i: tile_at(core * HEADS + DUO * g + i, LANES), ots, dqo, dkt, dvt, s_scr, e_scr, p_scr, d_scr)

        @pl.when(g == 0)
        def _():
            with scope('entry'):
                comm.meet(CORNERS)
                for c in loads:
                    c.wait()
        for c in head_trades(g):
            c.start()
        at(attended)
        gradient(DUO * g, DUO, rts, lambda: dqo[tile_at(g, PAIR), :], dot_nt)
        at(paired)

    def beat(cost, *starts):
        plan.now += cost
        for u in starts:
            plan.start(u)
        emit(plan.due())

    wkv, wkvp = e_scr.reshape(DIM, PAIR), p_scr.reshape(DIM, PAIR)
    later += [comm.local(src.at[:, pl.ds(at, LANES)], dst.at[:, pl.ds(to, LANES)]) for srcs, dst in (((wqk, wvo), wkv), ((wqkp, wvop), wkvp)) for src, at, to in ((srcs[0], HALF, 0), (srcs[1], 0, LANES))]
    wqp_loads = [comm.local(wqkp.at[tile_at(i, HALF), pl.ds(0, HALF)], two.at[i]) for i in range(DUO)]
    key = dkt[...] * SCALE
    co, si, x, y = cos[...], sin[...], key[:TURN], key[TURN:]
    dkvo[:LANES, :] = jnp.concatenate([x * co + y * si, y * co - x * si], axis=0).astype(bf16)
    dkvo[LANES:, :] = dvt[...].astype(bf16)
    comm.trade(dkvo, dkvp)
    gradient(UNIT_K, DUO, rts, lambda: dkvo[...], dot_nt)
    beat(1.8, UNIT_K, UNIT_V)
    wq_load = comm.local(wqk.at[:, pl.ds(0, HALF)], rts)
    for c in later:
        c.wait()
    with scope('trades'):
        for g in range(PAIRS):
            for c in head_trades(g):
                c.wait()

    waiting = list(range(RING))

    def output_gradients(force=False):
        while waiting:
            first = 10 + DUO * waiting[0]
            before = [u for u in range(N_UNITS) if u < first and PLACE[u] in (PLACE[first], PLACE[first + 1])]
            if force:
                emit(plan.rush(lambda: all(map(plan.vacated, before))))
            if not all(map(plan.vacated, before)):
                return
            for u in before:
                sc.drain(u, 0)
            i = waiting.pop(0)
            gradient(PLACE[first], DUO, ots, lambda: dycs[:, i * PAIR:(i + 1) * PAIR], dot)
            plan.start(first)
            plan.start(first + 1)
            beat(1.5)

    def piece(cost):
        beat(cost)
        output_gradients()

    def ticking(n, cost, body):
        tables = [after(cost) for _ in range(n)]

        @pl.loop(0, n)
        def _(i):
            body(i)
            for j, table in enumerate(tables):
                if table:
                    pl.when(i == j)(functools.partial(emit, table))
        output_gradients()

    @pl.loop(0, TOKENS // LANES)
    def _(i):
        want = lax.broadcasted_iota(jnp.int32, (LANES, ROWS), 0) + i * LANES
        own[tile_at(i, LANES), :] = jnp.where(want == pos[...], 1.0, 0.0).astype(bf16)

    def unsort(at, src_t, n):
        with scope('unsort'):
            dnat[at:at + n, :] = dot(src_t[:n, :], own[...]).astype(bf16)

    output_gradients()
    for c in comm.exchanged:
        c.wait_recv()
    unsort(0, dqo, HALF)
    dy_loads = [comm.local(dy.at[:, tile_at(i, HALF)], dqo.at[tile_at(i, ROWS)]) for i in range(DUO)]
    piece(1.2)
    unsort(HALF, dqp, HALF)
    piece(1.2)
    unsort(DUO * HALF, dkvo, PAIR)
    unsort(DUO * HALF + PAIR, dkvp, PAIR)
    piece(0.7)
    wq_load.wait()
    for c in wqp_loads + dy_loads:
        c.wait()
    gacc[...] = jnp.zeros_like(gacc)

    def dr_parts(half, r):
        return [s_scr.at[half, r(i * PAIR), :] for i in range(RING)]

    def back(block, then):
        def dr(half):
            with scope('dr'):
                c = tile_at(half, HALF)
                left = jnp.concatenate([rts[c, :], two[half], wkv[c, :], wkvp[c, :]], axis=1)
                acc = dot(left, dnat[:, block * PAIR:(block + 1) * PAIR])
                for i, ref in enumerate(dr_parts(half, lambda at: pl.ds(at, PAIR))):
                    ref[...] = acc[i * PAIR:(i + 1) * PAIR, :].T

        def norm(part):
            with scope('back'):
                @pl.loop(0, RING)
                def _(i):
                    j = part * RING + i
                    q = pl.ds(pl.multiple_of(block * PAIR + j * SHARE, SHARE), SHARE)
                    d = jnp.concatenate([ref[...] for half in range(DUO) for ref in dr_parts(half, lambda at: pl.ds(pl.multiple_of(at + j * SHARE, SHARE), SHARE))], axis=1)
                    x = xs[q, :].astype(f32)
                    inv = lax.rsqrt(jnp.mean(x * x, axis=-1, keepdims=True) + RMS_EPS)
                    unit = x * inv
                    gacc[...] += jnp.sum((d * unit).reshape(DUO, SUBS, DIM), axis=0)
                    dg = d * gain[0:1, :]
                    new = inv * (dg - unit * jnp.mean(dg * unit, axis=-1, keepdims=True))
                    for half in range(DUO):
                        r = pl.ds(pl.multiple_of(half * ROWS + block * PAIR + j * SHARE, SHARE), SHARE)
                        dqo[r, :] = (dqo[r, :].astype(f32) + new[:, half * HALF:(half + 1) * HALF]).astype(bf16)

        ticking(DUO, 1.6, dr)
        then()
        ticking(RING, 0.92, norm)

    back(0, lambda: None)
    wo_loads = []
    back(1, lambda: wo_loads.extend([comm.local(wvo.at[:, pl.ds(LANES, HALF)], rts)] + [comm.local(wvop.at[tile_at(i, HALF), pl.ds(LANES, HALF)], two.at[i]) for i in range(DUO)]))
    for i in range(DUO):
        comm.store(dqo.at[tile_at(i, ROWS)], grad_x.at[:, tile_at(i, HALF)])
    total = jnp.sum(gacc[...], axis=0, keepdims=True)
    gpart[...] = jnp.zeros_like(gpart)
    for i in range(RING):
        for j in range(RING):
            gpart[i, j:j + 1, :] = total[:, (i * RING + j) * LANES:(i * RING + j + 1) * LANES]

    gain_c, gain_z, gain_p = (Batch(comm) for _ in range(TRIO))

    def sum_gain(stage):
        if stage == 0:
            gain_c.send(gpart, gpeer, peer)
        elif stage == 1:
            gain_c.arrived(gpeer)
            for j in range(RING):
                gz[j] = gpart[j] + gpeer[j]
            for hop in (1, DUO, TRIO):
                gain_z.send(gz.at[step(comm.pos, 'z', hop)], gz.at[TRIO + hop], comm.far('z', hop))
        elif stage == DUO:
            gain_z.arrived(gz.at[pl.ds(RING, TRIO)])
            gx[0] = (gz[comm.pos['z']] + gz[RING]) + (gz[5] + gz[6])
            for dy, dx in PLANE:
                gain_p.send(gx.at[0], gx.at[dy * RING + dx], comm.aside(dy, dx))
        else:
            gain_p.arrived(gx.at[pl.ds(1, 15)])
            gpeer[0] = jnp.sum(gx[...], axis=0)
            mine = jnp.broadcast_to(gpeer[0, pl.ds(comm.pos['y'], 1), :], (SUBS, LANES))
            gout[...] = pltpu.roll(mine, LANES - (comm.pos['x'] * CHIP + core * SHARE), 1)

    plan.start(GAIN)
    beat(0.2)
    for i in range(DUO):
        with scope('unsort_o'):
            @pl.loop(0, DUO)
            def _(j):
                r = pl.ds(pl.multiple_of(i * HALF + j * ROWS, ROWS), ROWS)
                onat[:, r] = dot(ots[r, :], own[...]).astype(bf16).T
        piece(1.58)
    output_gradients(True)

    def project_out(col, weights, i):
        with scope('project'):
            @pl.loop(DUO * i, DUO * i + DUO)
            def _(j):
                c = tile_at(j, PAIR)
                dst = pl.ds(pl.multiple_of(col + j * PAIR, PAIR), PAIR)
                xs[:, dst] = (xs[:, dst].astype(f32) + dot(onat[...], weights(c))).astype(bf16)
        beat(1.48)

    def own_half(c):
        return rts[:, c]

    def other_half(c):
        return jnp.concatenate([a1[:, c], a2[:, c]], axis=0)

    for c in wo_loads:
        c.wait()
    for col, weights in ((core * HALF, own_half), ((1 - core) * HALF, other_half)):
        for i in range(DUO):
            project_out(col, weights, i)
    comm.store(xs, result)
    emit(plan.rush(lambda: not plan.stage))
    with scope('finish'):
        sc.finish()
        for batch, whole in ((gain_c, gpart), (gain_z, gz.at[pl.ds(RING, TRIO)]), (gain_p, gx.at[pl.ds(1, 15)])):
            batch.sent(whole)
        for c in comm.exchanged:
            c.wait_send()
        for c in comm.stored:
            c.wait()


def tail(qt, do_t, k, kt, v, vt, rt, dyc, wqk, wqkp, wvo, wvop, gain, hidden, dy, pos, cos, sin):
    bf16, f32 = jnp.bfloat16, jnp.float32
    any_ = pl.BlockSpec(memory_space=pl.ANY)
    vmem = pl.BlockSpec(memory_space=pltpu.VMEM)
    S = lambda shape, d=bf16: jax.ShapeDtypeStruct(shape, d)
    V = lambda shape, d=bf16: pltpu.VMEM(shape, d)
    D = lambda n: pltpu.SemaphoreType.DMA((n,))
    sq, tall, wide = (HALF, TOKENS), (TOKENS, LANES), (LANES, TOKENS)
    mine, kv = (ROWS, DIM), (PAIR, TOKENS)
    return pl.pallas_call(
        tail_kernel,
        out_shape=[S(mine), S(mine), S((SHARE, DIM), f32), S((SHARE, PAIR), f32), S((SHARE, PAIR), f32), S((SHARE, DIM), f32), S((SUBS, LANES), f32)],
        in_specs=[any_] * 12 + [vmem] + [any_] * DUO + [vmem] * TRIO,
        out_specs=[any_] * 6 + [vmem],
        scratch_shapes=[V((DUO,) + sq), V(tall), V(wide), V(tall), V(wide), V((DIM, TOKENS)), V((DIM, TOKENS)), V(sq), V(sq), V(kv), V(kv), V(wide, f32), V(wide, f32),
                        V((DUO, TOKENS, QB), f32), V((DUO, TOKENS, QB)), V((DUO, TOKENS, QB)), V((DUO, TOKENS, QB)), V(sq), V((PLACES, RING, RING, RING, CHIP, LANES), f32), V((TRIO, SLOTS, RING, RING, CHIP, LANES), f32),
                        V((TRIO, SLOTS, 6, RING, RING, SHARE, LANES), f32), V((TRIO, SLOTS, 6, RING, SHARE, LANES), f32), V((TRIO, SLOTS, TRIO, CHIP, LANES), f32), V((N_UNITS, CHIP, LANES), f32), V((TOKENS, ROWS)), V(mine), V((DUO * QKV, ROWS)), V(mine),
                        V((SUBS, DIM), f32), V((RING, SUBS, LANES), f32), V((RING, SUBS, LANES), f32), V((7, SUBS, LANES), f32), V((SHARE, SUBS, LANES), f32),
                        D(9 * SLOTS), D(15 * SLOTS), D(DUO + N_UNITS), D(HEADS + RING), D(HEADS + RING), D(26)],
        compiler_params=pltpu.CompilerParams(collective_id=1, has_side_effects=True, vmem_limit_bytes=67043328),
        name='tail',
    )(qt, do_t, k, kt, v, vt, rt, dyc, wqk, wqkp, wvo, wvop, gain, hidden, dy, pos, cos, sin)


def settle_kernel(n, *refs):
    ins, gain, outs, gain_out, bufs, sems = refs[:n], refs[n], refs[n + 1:DUO * n + 1], refs[DUO * n + 1], refs[DUO * n + DUO:-1], refs[-1]
    jobs = []
    for a, o, b in zip(ins, outs, bufs):
        size = a.shape[0] // RING if a.shape[0] == ROWS else a.shape[0]
        jobs += [tuple(r.at[pl.ds(i, size)] for r in (a, b, o)) for i in range(0, a.shape[0], size)]
    takes = [pltpu.make_async_copy(a, b, sems.at[0, i]) for i, (a, b, _) in enumerate(jobs)]
    puts = [pltpu.make_async_copy(b, o, sems.at[1, i]) for i, (_, b, o) in enumerate(jobs)]
    for c in takes:
        c.start()
    gain_out[...] = gain[0:1, :SHARE]
    for take, put in zip(takes, puts):
        take.wait()
        put.start()
    for c in puts:
        c.wait()


def settle(*arrays):
    *large, gain = arrays
    any_, vmem = pl.BlockSpec(memory_space=pl.ANY), pl.BlockSpec(memory_space=pltpu.VMEM)
    return pl.pallas_call(
        functools.partial(settle_kernel, len(large)),
        out_shape=[jax.ShapeDtypeStruct(a.shape, a.dtype) for a in large] + [jax.ShapeDtypeStruct((1, SHARE), gain.dtype)],
        in_specs=[any_] * len(large) + [vmem],
        out_specs=[any_] * len(large) + [vmem],
        scratch_shapes=[pltpu.VMEM(a.shape, a.dtype) for a in large] + [pltpu.SemaphoreType.DMA((DUO, 12))],
        name='settle',
    )(*arrays)


def rope_tables():
    j = np.arange(HEAD_DIM // DUO, dtype=np.float64) / (HEAD_DIM // DUO)
    freq = (ROPE_THETA ** -j).astype(np.float32)
    angle = freq[:, None] * np.arange(TOKENS, dtype=np.float32)[None, :]
    return np.cos(angle.astype(np.float64)).astype(np.float32), np.sin(angle.astype(np.float64)).astype(np.float32)


def solution(mesh):
    def shard_fn(hidden, tok_pos, grad_out, norm_gain, w_query, w_key, w_value, w_out):
        hidden, grad_out = hidden[0], grad_out[0]
        cos_t, sin_t = (jnp.asarray(t) for t in rope_tables())
        *parts, gain = head(hidden, grad_out, w_query, w_key, w_value, w_out, tok_pos, norm_gain.reshape(1, SHARE), cos_t, sin_t)
        parts = [p.reshape(DIM, GROUP) if p.ndim > DUO else p for p in parts]
        result, grad_hidden, gq, gk, gv, go, gout = settle(*tail(*parts, gain, hidden, grad_out, tok_pos, cos_t, sin_t))
        return result[None], grad_hidden[None], gq, gk, gv, go, gout.reshape(SHARE)

    row_spec, pos_spec = P('fsdp', 'cp', None), P('fsdp', 'cp')
    weight_spec, gain_spec = P(('fsdp', 'cp'), None), P(('fsdp', 'cp'))
    return jax.shard_map(shard_fn, mesh=mesh, in_specs=(row_spec, pos_spec, row_spec, gain_spec, weight_spec, weight_spec, weight_spec, weight_spec), out_specs=(row_spec, row_spec, weight_spec, weight_spec, weight_spec, weight_spec, gain_spec), check_vma=False)
```

```python
import functools
import jax
import jax.numpy as jnp
import numpy as np
from jax import lax
from jax.experimental import pallas as pl
from jax.experimental.pallas import tpu as pltpu
from jax.sharding import PartitionSpec as P

LANES, SUBS, RING, TRIO, DUO = 128, 8, 4, 3, 2
PAIR, ROWS, CHIP, SHARE, TURN = 256, 512, 32, 16, 64
HEAD_DIM = LANES
ROPE_THETA = 1000000.0
RMS_EPS = 1e-5
SCALE = HEAD_DIM ** -0.5
LOG2E = 1.4426950408889634

MESH = pl.DeviceIdType.MESH
AXES = ('x', 'y', 'z')
ORDERS = (('x', 'y', 'z'), ('y', 'z', 'x'), ('z', 'x', 'y'))
ALL = pl.ds(0, RING)


def torus():
    f = lax.axis_index('fsdp')
    return {'x': lax.rem(f, RING), 'y': lax.rem(lax.div(f, RING), RING), 'z': lax.div(f, SHARE)}


def step(pos, axis, hop):
    return lax.rem(pos[axis] + hop, RING)


class Batch:
    def __init__(self, comm):
        self.comm, self.index = comm, comm.used
        comm.used += 1

    def _copy(self, src, dst, device):
        send, recv, _ = self.comm.sems
        return pltpu.make_async_remote_copy(src_ref=src, dst_ref=dst, send_sem=send.at[self.index], recv_sem=recv.at[self.index], device_id=device, device_id_type=MESH)

    def send(self, src, dst, device):
        self._copy(src, dst, device).start()
        return self

    def arrived(self, whole):
        self._copy(whole, whole, self.comm.peer()).wait_recv()

    def sent(self, whole):
        self._copy(whole, whole, self.comm.peer()).wait_send()


class Comm:
    def __init__(self, send_sems, recv_sems, local_sems):
        self.pos = torus()
        self.core = lax.axis_index('cp')
        self.sems = (send_sems, recv_sems, local_sems)
        self.used = self.used_local = 0
        self.stored = []

    def far(self, axis, hop):
        p = dict(self.pos)
        p[axis] = step(self.pos, axis, hop)
        return {'fsdp': (p['z'] * RING + p['y']) * RING + p['x'], 'cp': self.core}

    def peer(self):
        return {'fsdp': lax.axis_index('fsdp'), 'cp': 1 - self.core}

    def aside(self, dy, dx):
        return {'fsdp': (self.pos['z'] * RING + step(self.pos, 'y', dy)) * RING + step(self.pos, 'x', dx), 'cp': self.core}

    def announce(self, corners=()):
        sem = pltpu.get_barrier_semaphore()
        for axis in AXES:
            for hop in (1, DUO, TRIO):
                pl.semaphore_signal(sem, inc=1, device_id=self.far(axis, hop), device_id_type=MESH)
        for dy, dx in corners:
            pl.semaphore_signal(sem, inc=1, device_id=self.aside(dy, dx), device_id_type=MESH)
        pl.semaphore_signal(sem, inc=1, device_id=self.peer(), device_id_type=MESH)

    def meet(self, corners=()):
        pl.semaphore_wait(pltpu.get_barrier_semaphore(), 10 + len(corners))

    def ring(self, batch, src, slots, axis):
        for hop in (1, DUO, TRIO):
            batch.send(src, slots.at[hop], self.far(axis, hop))

    def local(self, src, dst):
        i = self.used_local
        self.used_local += 1
        c = pltpu.make_async_copy(src, dst, self.sems[DUO].at[i])
        c.start()
        return c

    def store(self, src, dst):
        self.stored.append(self.local(src, dst))


class Singles(Comm):
    def __init__(self, *sems):
        super().__init__(*sems)
        self.sent, self.exchanged = [], []

    def _copy(self, src, dst, device):
        i = self.used
        self.used += 1
        c = pltpu.make_async_remote_copy(src_ref=src, dst_ref=dst, send_sem=self.sems[0].at[i], recv_sem=self.sems[1].at[i], device_id=device, device_id_type=MESH)
        c.start()
        return c

    def send(self, src, dst, device):
        c = self._copy(src, dst, device)
        self.sent.append(c)
        return c

    def trade(self, src, dst):
        self.exchanged.append(self._copy(src, dst, self.peer()))


def pick(ref, sel, piece):
    lo, cols, first, rows = piece
    return ref.at[sel['z'], sel['y'], sel['x'], pl.ds(first, rows), pl.ds(lo, cols)]


def sem_scratch(remote, local):
    return [pltpu.SemaphoreType.DMA((remote,)), pltpu.SemaphoreType.DMA((remote,)), pltpu.SemaphoreType.DMA((local,))]


def add_into(dst, *srcs, fresh=False):
    def add(idx):
        total, *rest = [s[idx] for s in (srcs if fresh else (dst,) + srcs)]
        for more in rest:
            total = total + more
        dst[idx] = total

    if len(dst.shape) > TRIO:
        @pl.loop(0, dst.shape[0])
        def _(i):
            add((i,))
    else:
        add(Ellipsis)


def halves(lo, n):
    return (lo, n, 0, SHARE), (lo, n, SHARE, SHARE)


GROUPS = (halves(0, 384), halves(384, 384), halves(768, 384))
QK_FIRST = (halves(0, PAIR), halves(384, PAIR), halves(768, PAIR))
QK_LAST = (halves(PAIR, LANES), halves(640, LANES), halves(1024, LANES))
TOKENS = 1024
DIM = 2048
HALF = 1024
QKV = 1280
GROUP = 1152


def scope(name):
    return jax.named_scope(name)


def dot(a, b):
    return jnp.dot(a, b, preferred_element_type=jnp.float32)


def dot_nt(a, b):
    return lax.dot_general(a, b, (((1,), (1,)), ((), ())), preferred_element_type=jnp.float32)


def tile_at(i, n):
    return pl.ds(pl.multiple_of(i * n, n), n)


class Gather:
    def __init__(self, comm, ref, colors, land, held=None):
        self.comm, self.ref, self.colors, self.land = comm, ref, colors, land
        self.held = list(held or [dict(comm.pos) for _ in colors])
        self.spent = []

    def move(self, batch, s, piece, to):
        batch.send(pick(self.ref, s, piece), pick(self.ref, s, piece), to)

    def at(self, k, hop):
        d = ORDERS[k][self.phase]
        return dict(self.held[k], **{d: step(self.comm.pos, d, hop)})

    def begin(self, phase):
        self.phase = phase
        self.rest = Batch(self.comm)
        if phase == 0:
            for hop in (DUO, 1, TRIO):
                for k, (a, _) in enumerate(self.colors):
                    self.move(self.rest, self.held[k], (a[0], a[1], 0, CHIP), self.comm.far(ORDERS[k][0], hop))
            return
        self.up, self.dn = ([Batch(self.comm) for _ in range(TRIO)] for _ in range(DUO))
        for k, (a, b) in enumerate(self.colors):
            d = ORDERS[k][phase]
            up, dn, s = self.comm.far(d, 1), self.comm.far(d, TRIO), self.held[k]
            self.move(self.up[k], s, a, up)
            self.move(self.dn[k], s, b, dn)
            self.move(self.rest, s, b, up)
            self.move(self.rest, s, a, dn)
        if phase == DUO:
            for k, pieces in enumerate(self.colors):
                for piece in pieces:
                    self.land(self.ref, self.held[k], piece)

    def forward(self):
        for k, (a, b) in enumerate(self.colors):
            d = ORDERS[k][self.phase]
            for batch, hop, piece, to in ((self.up[k], TRIO, a, 1), (self.dn[k], 1, b, TRIO)):
                s = self.at(k, hop)
                batch.arrived(pick(self.ref, s, piece))
                self.move(self.rest, s, piece, self.comm.far(d, to))
                if self.phase == DUO:
                    self.land(self.ref, s, piece)
                self.spent.append((batch, pick(self.ref, self.held[k], piece)))

    def end(self):
        axis = ORDERS[0][self.phase]
        blocks = dict(self.held[0], **{axis: pl.ds(0, DUO if self.phase else TRIO)})
        width = sum(a[1] for a, _ in self.colors)
        whole = pick(self.ref, blocks, (0, width, 0, CHIP))
        self.rest.arrived(whole)
        self.spent.append((self.rest, whole))
        for k, (a, b) in enumerate(self.colors):
            if self.phase == DUO:
                for hop, piece in ((TRIO, b), (1, a), (DUO, a), (DUO, b)):
                    self.land(self.ref, self.at(k, hop), piece)
            self.held[k] = dict(self.held[k], **{ORDERS[k][self.phase]: ALL})

    def finish(self):
        for batch, whole in self.spent:
            batch.sent(whole)


def head_kernel(hidden, dy, wq, wk, wv, wo, pos, gain_in, cos_t, sin_t,
                qt_o, dot_o, k_o, kt_o, v_o, vt_o, rt_o, dyc_o, wqk_o, wqkp_o, wvo_o, wvop_o, gain_o,
                hid2, dy2, dys, rs, rt, wqk, wvo, wpeer, pi, pos2, qt, dot_s, kk, kt, vv, vt, cosines, sines, gain, gtile, gbuf, gx, gy, gz, *sems):
    comm = Comm(*sems)
    comm.announce()
    pos_c, core = comm.pos, comm.core
    bf16, f32 = jnp.bfloat16, jnp.float32
    peer = comm.peer()
    rows = tile_at(core, SHARE)
    mine_qk = wqk.at[pos_c['z'], pos_c['y'], pos_c['x'], rows]
    mine_vo = wvo.at[pos_c['z'], pos_c['y'], pos_c['x'], rows]

    def weight_parts(c):
        return ((wq.at[:, tile_at(c, HALF)], mine_qk.at[:, pl.ds(0, HALF)]), (wk.at[:, tile_at(c, LANES)], mine_qk.at[:, pl.ds(HALF, LANES)]),
                (wv.at[:, tile_at(c, LANES)], mine_vo.at[:, pl.ds(0, LANES)]), (wo.at[:, tile_at(c, HALF)], mine_vo.at[:, pl.ds(LANES, HALF)]))

    loads = [comm.local(s, d) for s, d in weight_parts(core)]
    load_x = [comm.local(hidden, hid2.at[pl.ds(0, ROWS)]), comm.local(dy, dy2.at[pl.ds(0, ROWS)])]
    share = lax.broadcasted_iota(jnp.int32, (SUBS, LANES), 1) // SHARE
    gtile[...] = jnp.where(share == pos_c['x'] * DUO + core, jnp.broadcast_to(jnp.concatenate([gain_in[...]] * SUBS, axis=1), (SUBS, LANES)), 0.0)
    with scope('entry'):
        comm.meet()
    swap_w, swap_pos, swap_dy, swap_x, peers_qk, peers_vo = (Batch(comm) for _ in range(6))
    gain_c, gain_x, gain_y, gain_z = (Batch(comm) for _ in range(RING))
    for s, d in weight_parts(1 - core):
        swap_w.send(s, d, peer)
    gain_c.send(gtile, gbuf, peer)
    swap_pos.send(pos, pos2, peer)
    for c in loads:
        c.wait()
    with scope('wait_w'):
        swapped = wqk.at[pos_c['z'], pos_c['y'], pos_c['x']]
        swap_w.arrived(swapped)

    def land_qk(ref, s, cols):
        peers_qk.send(pick(ref, s, cols), pick(wqkp_o, s, cols), peer)

    def land_vo(ref, s, cols):
        peers_vo.send(pick(ref, s, cols), pick(wpeer, s, cols), peer)

    g1 = Gather(comm, wvo, GROUPS, land_vo)
    g2 = Gather(comm, wqk, GROUPS, land_qk)
    g1.begin(0)
    g2.begin(0)
    gain_c.arrived(gbuf)
    gx[0] = gtile[...] + gbuf[...]
    comm.ring(gain_x, gx.at[0], gx, 'x')

    swap_pos.arrived(pos2)

    @pl.loop(0, TOKENS // LANES)
    def _(i):
        want = lax.broadcasted_iota(jnp.int32, (LANES, ROWS), 0) + i * LANES
        for h, have in enumerate((pos, pos2)):
            pi[tile_at(i, LANES), h * ROWS:(h + 1) * ROWS] = jnp.where(want == have[...], 1.0, 0.0).astype(bf16)

    for i in range(RING):
        r = slice(i * PAIR, (i + 1) * PAIR)
        cos, sin = cos_t[:, r], sin_t[:, r]
        cosines[r, :] = jnp.concatenate([cos, cos], axis=0).T
        sines[r, :] = jnp.concatenate([-sin, sin], axis=0).T

    def sort(dst, src, first, last):
        with scope('sort'):
            @pl.loop(first, last)
            def _(j):
                c = tile_at(j, PAIR)
                dst[:, c] = dot(pi[...], src[:, c]).astype(bf16)

    swap_dy.send(dy, dy2.at[pl.ds(ROWS, ROWS)], peer)
    with scope('p0_end'):
        for g in (g1, g2):
            g.end()
            g.begin(1)
    swap_x.send(hidden, hid2.at[pl.ds(ROWS, ROWS)], peer)
    gain_x.arrived(gx.at[pl.ds(1, TRIO)])
    gy[pos_c['y']] = (gx[0] + gx[1]) + (gx[DUO] + gx[TRIO])
    for hop in (1, DUO, TRIO):
        gain_y.send(gy.at[pos_c['y']], gy.at[pos_c['y']], comm.far('y', hop))
    with scope('wait_dy'):
        load_x[1].wait()
        swap_dy.arrived(dy2.at[pl.ds(ROWS, ROWS)])
    sort(dys, dy2, 0, RING)
    with scope('p1a_fwd'):
        g1.forward()
    sort(dys, dy2, RING, 6)
    with scope('p1b_fwd'):
        g2.forward()
    sort(dys, dy2, 6, SUBS)
    with scope('p1a_end'):
        g1.end()
    gain_y.arrived(gy.at[pl.ds(1, TRIO)])
    for j in range(RING):
        gz[pos_c['z'], j] = gy[j]
    for hop in (1, DUO, TRIO):
        gain_z.send(gz.at[pos_c['z']], gz.at[pos_c['z']], comm.far('z', hop))
    g1.begin(DUO)
    comm.store(dys.at[:, tile_at(core, HALF)], dyc_o)
    with scope('p1b_end'):
        g2.end()
    with scope('wait_x'):
        load_x[0].wait()
        swap_x.arrived(hid2.at[pl.ds(ROWS, ROWS)])
    sort(rs, hid2, 0, SUBS)
    with scope('p2q_fwd'):
        g1.forward()
    g2a, g2b = (Gather(comm, wqk, colors, land_qk, g2.held) for colors in (QK_FIRST, QK_LAST))
    g2a.begin(DUO)
    with scope('gain'):
        gain_z.arrived(gz.at[pl.ds(1, TRIO)])
    for i in range(RING):
        for j in range(RING):
            gain[:, (i * RING + j) * LANES:(i * RING + j + 1) * LANES] = gz[i, j]
    comm.store(gain, gain_o)

    def norm(first, last):
        with scope('norm'):
            @pl.loop(first, last)
            def _(i):
                r = tile_at(i, CHIP)
                x = rs[r, :].astype(f32)
                inv = lax.rsqrt(jnp.mean(x * x, axis=-1, keepdims=True) + RMS_EPS)
                rs[r, :] = (x * inv * gain[0:1, :]).astype(bf16)

    norm(0, TOKENS // CHIP)
    with scope('r_t'):
        @pl.loop(0, DIM // PAIR)
        def _(i):
            c = tile_at(i, PAIR)

            @pl.loop(0, TOKENS // PAIR)
            def _(j):
                r = tile_at(j, PAIR)
                rt[c, r] = rs[r, c].T
    comm.store(rt, rt_o)
    with scope('p2o_end'):
        g1.end()
    w_qk, w_vo, w_peer = wqk.reshape(DIM, GROUP), wvo.reshape(DIM, GROUP), wpeer.reshape(DIM, GROUP)
    with scope('vals'):
        @pl.loop(0, DUO)
        def _(i):
            r = tile_at(i, ROWS)
            val = dot(rs[r, :], w_vo[:, :LANES]).astype(bf16)
            vv[r, :] = val
            vt[:, r] = val.T
    for src, dst in ((wvo, wvo_o), (vv, v_o), (vt, vt_o)):
        comm.store(src, dst)
    with scope('p2q_fwd'):
        g2a.forward()
    g2b.begin(DUO)
    with scope('wo_peer'):
        peers_vo.arrived(wpeer)
    comm.store(wpeer, wvop_o)
    with scope('do_t'):
        mine = tile_at(core, HALF)

        @pl.loop(0, TOKENS // PAIR)
        def _(j):
            t = tile_at(j, PAIR)
            w_rows = jnp.concatenate([w_vo[mine, LANES:], w_peer[mine, LANES:]], axis=1)
            d_rows = jnp.concatenate([dys[t, mine], dys[t, tile_at(1 - core, HALF)]], axis=1)
            dot_s[:, t] = dot_nt(w_rows, d_rows).astype(bf16)
    comm.store(dot_s, dot_o)

    def rotated(x, r):
        return (x * cosines[r, :] + pltpu.roll(x, TURN, 1) * sines[r, :]).astype(bf16)

    def queries(columns, heads):
        x = dot(rs[...], columns)
        for i in range(RING):
            r = slice(i * PAIR, (i + 1) * PAIR)
            for h, head in enumerate(heads):
                qt[tile_at(head, LANES), r] = rotated(x[r, h * LANES:(h + 1) * LANES], r).T

    with scope('p2q_end'):
        g2a.end()

    def pairs(first, last):
        with scope('q'):
            @pl.loop(first, last)
            def _(t):
                queries(w_qk[:, pl.ds(pl.multiple_of(t * 384, LANES), PAIR)], (TRIO * t, TRIO * t + 1))

    with scope('last_fwd'):
        g2b.forward()
    pairs(0, TRIO)
    for t in range(TRIO):
        two_heads = pl.ds(t * 384, PAIR)
        comm.store(qt.at[two_heads], qt_o.at[two_heads])
    with scope('last_end'):
        g2b.end()
    comm.store(wqk, wqk_o)
    with scope('q_last'):
        x = dot(rs[...], jnp.concatenate([w_qk[:, PAIR:384], w_qk[:, 640:768], w_qk[:, HALF:]], axis=1))
        for i in range(RING):
            r = slice(i * PAIR, (i + 1) * PAIR)
            key = rotated(x[r, PAIR:], r)
            kk[r, :] = key
            kt[:, r] = key.T
            for h, head in enumerate((DUO, 5)):
                qt[tile_at(head, LANES), r] = rotated(x[r, h * LANES:(h + 1) * LANES], r).T
    for src, dst in ((kk, k_o), (kt, kt_o)) + tuple((qt.at[tile_at(h, LANES)], qt_o.at[tile_at(h, LANES)]) for h in (DUO, 5)):
        comm.store(src, dst)
    with scope('finish'):
        peers_qk.arrived(wqk)
        for batch, whole in ((swap_w, swapped), (swap_pos, pos2), (swap_dy, dy2.at[pl.ds(ROWS, ROWS)]), (swap_x, hid2.at[pl.ds(ROWS, ROWS)]), (peers_qk, wqk), (peers_vo, wvo),
                             (gain_c, gbuf), (gain_x, gx.at[pl.ds(1, TRIO)]), (gain_y, gy.at[pl.ds(1, TRIO)]), (gain_z, gz.at[pl.ds(1, TRIO)])):
            batch.sent(whole)
        for g in (g1, g2, g2a, g2b):
            g.finish()
        for c in comm.stored:
            c.wait()


def head(hidden, dy, wq, wk, wv, wo, pos, gain, cos_t, sin_t):
    bf16, f32 = jnp.bfloat16, jnp.float32
    any_ = pl.BlockSpec(memory_space=pl.ANY)
    vmem = pl.BlockSpec(memory_space=pltpu.VMEM)
    S = lambda shape, d=bf16: jax.ShapeDtypeStruct(shape, d)
    V = lambda shape, d=bf16: pltpu.VMEM(shape, d)
    group = (RING, RING, RING, CHIP, GROUP)
    sq, tall, wide = (HALF, TOKENS), (TOKENS, LANES), (LANES, TOKENS)
    full = (TOKENS, DIM)
    return pl.pallas_call(
        head_kernel,
        out_shape=[S(sq), S(sq), S(tall), S(wide), S(tall), S(wide), S((DIM, TOKENS)), S((TOKENS, HALF)), S(group), S(group), S(group), S(group), S((SUBS, DIM), f32)],
        in_specs=[any_] * 6 + [vmem] * RING,
        out_specs=[any_] * 13,
        scratch_shapes=[V(full), V(full), V(full), V(full), V((DIM, TOKENS)), V(group), V(group), V(group), V((TOKENS, TOKENS)), V((1, ROWS), jnp.int32),
                        V(sq), V(sq), V(tall), V(wide), V(tall), V(wide), V(tall, f32), V(tall, f32), V((SUBS, DIM), f32), V((SUBS, LANES), f32), V((SUBS, LANES), f32), V((RING, SUBS, LANES), f32), V((RING, SUBS, LANES), f32), V((RING, RING, SUBS, LANES), f32)] + sem_scratch(47, 22),
        compiler_params=pltpu.CompilerParams(collective_id=0, has_side_effects=True, vmem_limit_bytes=60 * DUO**20),
        name='head',
    )(hidden, dy, wq, wk, wv, wo, pos, gain, cos_t, sin_t)


HEADS = SUBS
UNIT_K, UNIT_V = SUBS, 9
N_UNITS = 18
GAIN = N_UNITS
SLOTS = RING
LAST = 5
ABREAST = DUO
LINES = ((0, TRIO, 6, 9, 12, 15), (1, RING, 7, 10, 13, SHARE), (DUO, 5, SUBS, 11, 14, 17))
COLOR = {u: k for k, line in enumerate(LINES) for u in line}
RANK = {u: i for line in LINES for i, u in enumerate(line)}
SWAPPED = (1, TRIO, RING, SUBS, 10)
ORDER = {u: ORDERS[k] if u not in SWAPPED else (ORDERS[k][0], ORDERS[k][DUO], ORDERS[k][1]) for u, k in COLOR.items()}
BEFORE = {u: line[i - SLOTS] if i >= SLOTS else None for line in LINES for i, u in enumerate(line)}
PLACES = 12
PLACE = {u: u % PLACES for u in range(N_UNITS)}
WIRE = (2.82, 0.71, 0.36)
LATENCY = 2.4
STAGE_COST = 0.08


class Plan:
    def __init__(self):
        self.now, self.stage, self.ready, self.order, self.link = 0.0, {}, {}, [], {}
        self.mark = {}

    def _wire(self, u, phase, count):
        link = ORDER[u][phase]
        t = max(self.link.get(link, 0.0), self.now)
        first = t + WIRE[phase] + LATENCY
        self.link[link] = t + WIRE[phase] * count
        return first if phase < DUO else self.link[link] + LATENCY

    def free(self, u, phase):
        if BEFORE[u] is None:
            return True
        done = self.mark.get((BEFORE[u], (DUO, RING, 5)[phase]))
        if done is None:
            return False
        sent = ((0, 1), (DUO, TRIO), (RING,))[phase]
        return any(self.mark.get((j, s), -1) > done and (j, s + 1) in self.mark for j, order in ORDER.items() if order[phase] == ORDER[u][phase] for s in sent)

    def run(self, u):
        stage = self.stage[u]
        self.order.append((u, stage))
        self.mark[u, stage] = len(self.order)
        self.now = max(self.now, self.ready[u]) + STAGE_COST
        self.stage[u] = stage + 1
        if stage == (TRIO if u == GAIN else LAST):
            del self.stage[u]
        elif u == GAIN:
            self.ready[u] = max([self.now] + [self.link.get(a, 0.0) for a in ('', 'z', 'xy')[stage]]) + DUO * LATENCY
        elif stage % DUO:
            self.ready[u] = self._wire(u, stage // DUO, 1)
        else:
            self.ready[u] = self._wire(u, stage // DUO, DUO)

    def blocked(self, u):
        stage = self.stage[u]
        if u == GAIN:
            return False
        if stage == 0 and sum(0 < self.stage.get(j, 0) <= DUO for j in LINES[COLOR[u]]) >= ABREAST:
            return True
        if stage == DUO and BEFORE[u] is not None and (BEFORE[u], LAST) not in self.mark:
            return True
        return stage in (0, DUO, RING) and not self.free(u, stage // DUO)

    def start(self, u):
        self.stage[u], self.ready[u] = 0, self.now

    def due(self):
        first = len(self.order)
        while True:
            ripe = [(self.ready[u], u) for u in self.stage if self.ready[u] <= self.now and not self.blocked(u)]
            if not ripe:
                return self.order[first:]
            self.run(min(ripe)[1])

    def vacated(self, u):
        return (u, DUO) in self.mark

    def rush(self, done):
        first = len(self.order)
        while not done():
            self.run(min((self.ready[u], u) for u in self.stage if not self.blocked(u))[1])
        return self.order[first:]


QB = PAIR
PAIRS = HEADS // DUO
NBLK = TOKENS // QB
HALVES = (pl.ds(0, SHARE), pl.ds(SHARE, SHARE))
PLANE = tuple((dy, dx) for dy in range(RING) for dx in range(RING) if dy or dx)
CORNERS = tuple((dy, dx) for dy, dx in PLANE if dy and dx)


class Scatter:
    def __init__(self, comm, part, mid, bufs, fin, outs, send_sems, recv_sems, swap_sems):
        self.pos, self.part, self.mid, self.bufs, self.fin, self.outs = comm.pos, part, mid, bufs, fin, outs
        self.send_sems, self.recv_sems, self.swap_sems = send_sems, recv_sems, swap_sems
        self.near = {(a, hop): comm.far(a, hop) for a in AXES for hop in (1, DUO, TRIO)}
        self.hops = {(a, hop): step(comm.pos, a, hop) for a in AXES for hop in (1, DUO, TRIO)}
        self.peer, self.core = comm.peer(), comm.core
        self.keep, self.give = tile_at(comm.core, SHARE), tile_at(1 - comm.core, SHARE)
        self.drained = set()

    def slot(self, u):
        return COLOR[u], RANK[u] % SLOTS

    def buf(self, u, phase):
        return self.bufs[phase].at[self.slot(u)]

    def view(self, u, phase, hop, half=None):
        order = ORDER[u]
        at = {a: ALL for a in AXES}
        for a in order[1:phase]:
            at[a] = self.pos[a]
        at[order[phase]] = self.hops[order[phase], hop] if hop else self.pos[order[phase]]
        rows = pl.ds(0, CHIP) if half is None else HALVES[half]
        if phase == 0:
            return self.part.at[PLACE[u], at['z'], at['y'], at['x'], rows, :]
        return self.mid.at[self.slot(u) + tuple(at[a] for a in 'zyx' if a != order[0]) + (rows, slice(None))]

    def copy(self, src, dst, sems, device):
        return pltpu.make_async_remote_copy(src_ref=src, dst_ref=dst, send_sem=sems[0], recv_sem=sems[1], device_id=device, device_id_type=MESH)

    def sems(self, u, phase, kind=0):
        k, i = self.slot(u)
        at = (k * SLOTS + i) * TRIO + phase
        return self.send_sems.at[at], self.recv_sems.at[(k * SLOTS + i) * 5 + DUO * phase + kind]

    def send(self, u, phase, name):
        axis = ORDER[u][phase]
        if phase == DUO:
            src, to = self.view(u, DUO, name + 1), name + 1
        else:
            hop, half, to = ((DUO, 0, 1), (DUO, 1, TRIO), (1, 1, 1), (TRIO, 0, TRIO), (1, 0, 1), (TRIO, 1, TRIO))[name]
            src = self.view(u, phase, hop, half)
        self.copy(src, self.buf(u, phase).at[name], self.sems(u, phase, int(name > 1 and phase < DUO)), self.near[axis, to]).start()

    def launch(self, u, phase):
        if BEFORE[u] is not None:
            self.drain(BEFORE[u], phase)
        for name in range(RING if phase < DUO else TRIO):
            self.send(u, phase, name)

    def arrived(self, u, phase, first, count):
        whole = self.buf(u, phase).at[pl.ds(first, count)]
        self.copy(whole, whole, self.sems(u, phase, int(first > 0)), self.peer).wait_recv()

    def drain(self, u, phase):
        if (u, phase) not in self.drained:
            self.drained.add((u, phase))
            whole = self.buf(u, phase)
            self.copy(whole, whole, self.sems(u, phase), self.peer).wait_send()

    def out(self, u):
        if u < HEADS:
            out, col = self.outs[0], self.core * HALF + u * LANES
        elif u < 10:
            out, col = self.outs[u - 7], self.core * LANES
        else:
            out, col = self.outs[TRIO], self.core * HALF + (u - 10) * LANES
        return out.at[:, pl.ds(pl.multiple_of(col, LANES), LANES)]

    def kept(self, u):
        return pltpu.make_async_copy(self.fin.at[u, self.keep], self.out(u), self.swap_sems.at[DUO + u])

    def run(self, u, stage):
        if stage == 0:
            return self.launch(u, 0)
        phase = (stage - 1) // DUO
        if stage == LAST:
            self.arrived(u, DUO, 0, TRIO)
            got = self.buf(u, DUO)
            self.fin[u] = self.view(u, DUO, 0)[...] + (got[0] + got[1] + got[DUO])
            self.copy(self.fin.at[u, self.give], self.out(u), (self.swap_sems.at[0], self.swap_sems.at[1]), self.peer).start()
            self.kept(u).start()
            return
        got = self.buf(u, phase)
        if stage % DUO:
            self.arrived(u, phase, 0, DUO)
            for name, hop in ((0, 1), (1, TRIO)):
                add_into(self.view(u, phase, hop, name), got.at[name])
                self.send(u, phase, name + RING)
            return
        self.arrived(u, phase, DUO, RING)
        if phase == 0 and BEFORE[u] is not None:
            self.drain(BEFORE[u], 1)
            self.drain(BEFORE[u], DUO)
        for half, names in ((0, (TRIO, RING)), (1, (DUO, 5))):
            if phase:
                add_into(self.view(u, phase, 0, half), *[got.at[name] for name in names])
            else:
                dst = self.mid.at[self.slot(u) + (ALL, ALL, HALVES[half], slice(None))]
                add_into(dst, self.view(u, 0, 0, half), *[got.at[name] for name in names], fresh=True)
        self.launch(u, phase + 1)

    def finish(self):
        for u in range(N_UNITS):
            for phase in range(TRIO):
                self.drain(u, phase)
        half = self.fin.at[:, pl.ds(0, SHARE)]
        swaps = self.copy(half, half, (self.swap_sems.at[0], self.swap_sems.at[1]), self.peer)
        swaps.wait_send()
        swaps.wait_recv()
        for u in range(N_UNITS):
            self.kept(u).wait()


def attend(heads, qt, do_t, k, kt, v, vt, cos, sin, o_row, ot, dq, dkt, dvt, s_scr, e_scr, p_scr, d_scr):
    f32, bf16 = jnp.float32, jnp.bfloat16
    strip = TURN
    work = [(h, j) for j in range(NBLK) for h in range(len(heads))]

    def strips(c):
        return [(i * strip, slice(c * QB + i * strip, c * QB + (i + 1) * strip)) for i in range(QB // strip)]

    def fold(x, op):
        return op(x.reshape(strip // SUBS, SUBS, QB), axis=0)

    def scores(i):
        (h, j), b = work[i], i % DUO
        q_t = qt[heads[h], j * QB:(j + 1) * QB]
        top = jnp.full((SUBS, QB), -jnp.inf, f32)
        for c in range(j + 1):
            tile = dot(k[c * QB:(c + 1) * QB, :], q_t)
            for at, rows in strips(c):
                s = tile[at:at + strip]
                if c == j:
                    seen = lax.broadcasted_iota(jnp.int32, (strip, QB), 0) + at <= lax.broadcasted_iota(jnp.int32, (strip, QB), 1)
                    s = jnp.where(seen, s, -jnp.inf)
                s_scr[b, rows, :] = s
                top = jnp.maximum(top, fold(s, jnp.max))
        return jnp.max(top, axis=0, keepdims=True)

    def rest(i, m):
        (h, j), b = work[i], i % DUO
        cols, n = slice(j * QB, (j + 1) * QB), (j + 1) * QB
        q_t, d_t = qt[heads[h], cols], do_t[heads[h], cols]
        tot = jnp.zeros((SUBS, QB), f32)
        for c in range(j + 1):
            for at, rows in strips(c):
                e = jnp.exp2((s_scr[b, rows, :] - m) * (SCALE * LOG2E))
                s_scr[b, rows, :] = e
                e_scr[b, rows, :] = e.astype(bf16)
                tot = tot + fold(e, jnp.sum)
        den = jnp.sum(tot, axis=0, keepdims=True)
        inv = 1.0 / den
        o = (dot(vt[:, :n], e_scr[b, :n, :]) / den).astype(bf16)
        ot[o_row(h), cols] = o
        delta = jnp.sum(d_t.astype(f32) * o.astype(f32), axis=0, keepdims=True)
        for c in range(j + 1):
            dp = dot(v[c * QB:(c + 1) * QB, :], d_t)
            for at, rows in strips(c):
                p = s_scr[b, rows, :] * inv
                p_scr[b, rows, :] = p.astype(bf16)
                d_scr[b, rows, :] = (p * (dp[at:at + strip] - delta)).astype(bf16)
        dvt[:, :n] += dot_nt(d_t, p_scr[b, :n, :])
        dkt[:, :n] += dot_nt(q_t, d_scr[b, :n, :])
        g = dot(kt[:, :n], d_scr[b, :n, :]) * SCALE
        co, si = cos[:, cols], sin[:, cols]
        x, y = g[:TURN], g[TURN:]
        dq[heads[h], cols] = jnp.concatenate([x * co + y * si, y * co - x * si], axis=0).astype(bf16)

    m = scores(0)
    for i in range(len(work)):
        later = scores(i + 1) if i + 1 < len(work) else None
        rest(i, m)
        m = later


def tail_kernel(qt, do_t, k, kt, v, vt, rt, dyc, wqk, wqkp, wvo, wvop, gain, hidden, dy, pos, cos, sin,
                result, grad_x, gq, gk, gv, go, gout,
                two, ks, kts, vs, vts, rts, ots, dqo, dqp, dkvo, dkvp, dkt, dvt, s_scr, e_scr, p_scr, d_scr, dycs, part, mid, buf1, buf2, buf3, fin, own, onat, dnat, xs, gacc, gpart, gpeer, gz, gx,
                send_sems, recv_sems, swap_sems, trade_send, trade_recv, local_sems):
    comm = Singles(trade_send, trade_recv, local_sems)
    comm.used = HEADS
    f32, bf16 = jnp.float32, jnp.bfloat16
    core, peer = comm.core, comm.peer()
    a1, a2 = two.at[0], two.at[1]
    sc = Scatter(comm, part, mid, (buf1, buf2, buf3), fin, (gq, gk, gv, go), send_sems, recv_sems, swap_sems)
    plan = Plan()
    some, most = pl.ds(0, PAIR), pl.ds(PAIR, HALF - PAIR)
    loads = [comm.local(s, d) for s, d in ((qt.at[some], two.at[0, some]), (k, ks), (do_t.at[some], two.at[1, some]), (vt, vts), (v, vs), (kt, kts))]
    comm.announce(CORNERS)
    dkt[...] = jnp.zeros_like(dkt)
    dvt[...] = jnp.zeros_like(dvt)
    with scope('wait_q'):
        for c in loads:
            c.wait()
    loads = [comm.local(s, d) for s, d in ((rt, rts), (qt.at[most], two.at[0, most]), (do_t.at[most], two.at[1, most]))]
    later = [comm.local(s, d) for s, d in ((dyc, dycs), (hidden, xs))]

    def emit(stages):
        for u, stage in stages:
            with scope(f'u{u}_s{stage}'):
                if u == GAIN:
                    sum_gain(stage)
                else:
                    sc.run(u, stage)

    def after(cost):
        plan.now += cost
        return plan.due()

    def head_trades(g):
        row = pl.ds(pl.multiple_of((core * HEADS + DUO * g) * LANES, PAIR), PAIR)
        mine = tile_at(g, PAIR)
        return [pltpu.make_async_remote_copy(src_ref=s, dst_ref=d, send_sem=trade_send.at[i], recv_sem=trade_recv.at[i], device_id=peer, device_id_type=MESH)
                for s, d, i in ((ots.at[row], ots.at[row], g), (dqo.at[mine], dqp.at[mine], PAIRS + g))]

    def gradient(place, count, left, right, mul):
        with scope('grad'):
            @pl.loop(0, DUO)
            def _(z):
                g = mul(left[tile_at(z, HALF), :], right())
                for i in range(count):
                    part[place + i, tile_at(z, DUO)] = g[:, i * LANES:(i + 1) * LANES].reshape(DUO, RING, RING, CHIP, LANES)

    attended, paired = [], []
    for g in range(PAIRS):
        attended.append(after(5.1))
        plan.now += 1.5
        plan.start(DUO * g)
        plan.start(DUO * g + 1)
        paired.append(plan.due())

    @pl.loop(0, PAIRS)
    def _(g):
        def at(table):
            for i in range(PAIRS):
                if table[i]:
                    pl.when(g == i)(functools.partial(emit, table[i]))

        heads = [tile_at(DUO * g + i, LANES) for i in range(DUO)]
        with scope('attend'):
            attend(heads, a1, a2, ks, kts, vs, vts, cos, sin, lambda i: tile_at(core * HEADS + DUO * g + i, LANES), ots, dqo, dkt, dvt, s_scr, e_scr, p_scr, d_scr)

        @pl.when(g == 0)
        def _():
            with scope('entry'):
                comm.meet(CORNERS)
                for c in loads:
                    c.wait()
        for c in head_trades(g):
            c.start()
        at(attended)
        gradient(DUO * g, DUO, rts, lambda: dqo[tile_at(g, PAIR), :], dot_nt)
        at(paired)

    def beat(cost, *starts):
        plan.now += cost
        for u in starts:
            plan.start(u)
        emit(plan.due())

    wkv, wkvp = e_scr.reshape(DIM, PAIR), p_scr.reshape(DIM, PAIR)
    later += [comm.local(src.at[:, pl.ds(at, LANES)], dst.at[:, pl.ds(to, LANES)]) for srcs, dst in (((wqk, wvo), wkv), ((wqkp, wvop), wkvp)) for src, at, to in ((srcs[0], HALF, 0), (srcs[1], 0, LANES))]
    wqp_loads = [comm.local(wqkp.at[tile_at(i, HALF), pl.ds(0, HALF)], two.at[i]) for i in range(DUO)]
    key = dkt[...] * SCALE
    co, si, x, y = cos[...], sin[...], key[:TURN], key[TURN:]
    dkvo[:LANES, :] = jnp.concatenate([x * co + y * si, y * co - x * si], axis=0).astype(bf16)
    dkvo[LANES:, :] = dvt[...].astype(bf16)
    comm.trade(dkvo, dkvp)
    gradient(UNIT_K, DUO, rts, lambda: dkvo[...], dot_nt)
    beat(1.8, UNIT_K, UNIT_V)
    wq_load = comm.local(wqk.at[:, pl.ds(0, HALF)], rts)
    for c in later:
        c.wait()
    with scope('trades'):
        for g in range(PAIRS):
            for c in head_trades(g):
                c.wait()

    waiting = list(range(RING))

    def output_gradients(force=False):
        while waiting:
            first = 10 + DUO * waiting[0]
            before = [u for u in range(N_UNITS) if u < first and PLACE[u] in (PLACE[first], PLACE[first + 1])]
            if force:
                emit(plan.rush(lambda: all(map(plan.vacated, before))))
            if not all(map(plan.vacated, before)):
                return
            for u in before:
                sc.drain(u, 0)
            i = waiting.pop(0)
            gradient(PLACE[first], DUO, ots, lambda: dycs[:, i * PAIR:(i + 1) * PAIR], dot)
            plan.start(first)
            plan.start(first + 1)
            beat(1.5)

    def piece(cost):
        beat(cost)
        output_gradients()

    def ticking(n, cost, body):
        tables = [after(cost) for _ in range(n)]

        @pl.loop(0, n)
        def _(i):
            body(i)
            for j, table in enumerate(tables):
                if table:
                    pl.when(i == j)(functools.partial(emit, table))
        output_gradients()

    @pl.loop(0, TOKENS // LANES)
    def _(i):
        want = lax.broadcasted_iota(jnp.int32, (LANES, ROWS), 0) + i * LANES
        own[tile_at(i, LANES), :] = jnp.where(want == pos[...], 1.0, 0.0).astype(bf16)

    def unsort(at, src_t, n):
        with scope('unsort'):
            dnat[at:at + n, :] = dot(src_t[:n, :], own[...]).astype(bf16)

    output_gradients()
    for c in comm.exchanged:
        c.wait_recv()
    unsort(0, dqo, HALF)
    dy_loads = [comm.local(dy.at[:, tile_at(i, HALF)], dqo.at[tile_at(i, ROWS)]) for i in range(DUO)]
    piece(1.2)
    unsort(HALF, dqp, HALF)
    piece(1.2)
    unsort(DUO * HALF, dkvo, PAIR)
    unsort(DUO * HALF + PAIR, dkvp, PAIR)
    piece(0.7)
    wq_load.wait()
    for c in wqp_loads + dy_loads:
        c.wait()
    gacc[...] = jnp.zeros_like(gacc)

    def dr_parts(half, r):
        return [s_scr.at[half, r(i * PAIR), :] for i in range(RING)]

    def back(block, then):
        def dr(half):
            with scope('dr'):
                c = tile_at(half, HALF)
                left = jnp.concatenate([rts[c, :], two[half], wkv[c, :], wkvp[c, :]], axis=1)
                acc = dot(left, dnat[:, block * PAIR:(block + 1) * PAIR])
                for i, ref in enumerate(dr_parts(half, lambda at: pl.ds(at, PAIR))):
                    ref[...] = acc[i * PAIR:(i + 1) * PAIR, :].T

        def norm(part):
            with scope('back'):
                @pl.loop(0, RING)
                def _(i):
                    j = part * RING + i
                    q = pl.ds(pl.multiple_of(block * PAIR + j * SHARE, SHARE), SHARE)
                    d = jnp.concatenate([ref[...] for half in range(DUO) for ref in dr_parts(half, lambda at: pl.ds(pl.multiple_of(at + j * SHARE, SHARE), SHARE))], axis=1)
                    x = xs[q, :].astype(f32)
                    inv = lax.rsqrt(jnp.mean(x * x, axis=-1, keepdims=True) + RMS_EPS)
                    unit = x * inv
                    gacc[...] += jnp.sum((d * unit).reshape(DUO, SUBS, DIM), axis=0)
                    dg = d * gain[0:1, :]
                    new = inv * (dg - unit * jnp.mean(dg * unit, axis=-1, keepdims=True))
                    for half in range(DUO):
                        r = pl.ds(pl.multiple_of(half * ROWS + block * PAIR + j * SHARE, SHARE), SHARE)
                        dqo[r, :] = (dqo[r, :].astype(f32) + new[:, half * HALF:(half + 1) * HALF]).astype(bf16)

        ticking(DUO, 1.6, dr)
        then()
        ticking(RING, 0.92, norm)

    back(0, lambda: None)
    wo_loads = []
    back(1, lambda: wo_loads.extend([comm.local(wvo.at[:, pl.ds(LANES, HALF)], rts)] + [comm.local(wvop.at[tile_at(i, HALF), pl.ds(LANES, HALF)], two.at[i]) for i in range(DUO)]))
    for i in range(DUO):
        comm.store(dqo.at[tile_at(i, ROWS)], grad_x.at[:, tile_at(i, HALF)])
    total = jnp.sum(gacc[...], axis=0, keepdims=True)
    gpart[...] = jnp.zeros_like(gpart)
    for i in range(RING):
        for j in range(RING):
            gpart[i, j:j + 1, :] = total[:, (i * RING + j) * LANES:(i * RING + j + 1) * LANES]

    gain_c, gain_z, gain_p = (Batch(comm) for _ in range(TRIO))

    def sum_gain(stage):
        if stage == 0:
            gain_c.send(gpart, gpeer, peer)
        elif stage == 1:
            gain_c.arrived(gpeer)
            for j in range(RING):
                gz[j] = gpart[j] + gpeer[j]
            for hop in (1, DUO, TRIO):
                gain_z.send(gz.at[step(comm.pos, 'z', hop)], gz.at[TRIO + hop], comm.far('z', hop))
        elif stage == DUO:
            gain_z.arrived(gz.at[pl.ds(RING, TRIO)])
            gx[0] = (gz[comm.pos['z']] + gz[RING]) + (gz[5] + gz[6])
            for dy, dx in PLANE:
                gain_p.send(gx.at[0], gx.at[dy * RING + dx], comm.aside(dy, dx))
        else:
            gain_p.arrived(gx.at[pl.ds(1, 15)])
            gpeer[0] = jnp.sum(gx[...], axis=0)
            mine = jnp.broadcast_to(gpeer[0, pl.ds(comm.pos['y'], 1), :], (SUBS, LANES))
            gout[...] = pltpu.roll(mine, LANES - (comm.pos['x'] * CHIP + core * SHARE), 1)

    plan.start(GAIN)
    beat(0.2)
    for i in range(DUO):
        with scope('unsort_o'):
            @pl.loop(0, DUO)
            def _(j):
                r = pl.ds(pl.multiple_of(i * HALF + j * ROWS, ROWS), ROWS)
                onat[:, r] = dot(ots[r, :], own[...]).astype(bf16).T
        piece(1.58)
    output_gradients(True)

    def project_out(col, weights, i):
        with scope('project'):
            @pl.loop(DUO * i, DUO * i + DUO)
            def _(j):
                c = tile_at(j, PAIR)
                dst = pl.ds(pl.multiple_of(col + j * PAIR, PAIR), PAIR)
                xs[:, dst] = (xs[:, dst].astype(f32) + dot(onat[...], weights(c))).astype(bf16)
        beat(1.48)

    def own_half(c):
        return rts[:, c]

    def other_half(c):
        return jnp.concatenate([a1[:, c], a2[:, c]], axis=0)

    for c in wo_loads:
        c.wait()
    for col, weights in ((core * HALF, own_half), ((1 - core) * HALF, other_half)):
        for i in range(DUO):
            project_out(col, weights, i)
    comm.store(xs, result)
    emit(plan.rush(lambda: not plan.stage))
    with scope('finish'):
        sc.finish()
        for batch, whole in ((gain_c, gpart), (gain_z, gz.at[pl.ds(RING, TRIO)]), (gain_p, gx.at[pl.ds(1, 15)])):
            batch.sent(whole)
        for c in comm.exchanged:
            c.wait_send()
        for c in comm.stored:
            c.wait()


def tail(qt, do_t, k, kt, v, vt, rt, dyc, wqk, wqkp, wvo, wvop, gain, hidden, dy, pos, cos, sin):
    bf16, f32 = jnp.bfloat16, jnp.float32
    any_ = pl.BlockSpec(memory_space=pl.ANY)
    vmem = pl.BlockSpec(memory_space=pltpu.VMEM)
    S = lambda shape, d=bf16: jax.ShapeDtypeStruct(shape, d)
    V = lambda shape, d=bf16: pltpu.VMEM(shape, d)
    D = lambda n: pltpu.SemaphoreType.DMA((n,))
    sq, tall, wide = (HALF, TOKENS), (TOKENS, LANES), (LANES, TOKENS)
    mine, kv = (ROWS, DIM), (PAIR, TOKENS)
    return pl.pallas_call(
        tail_kernel,
        out_shape=[S(mine), S(mine), S((SHARE, DIM), f32), S((SHARE, PAIR), f32), S((SHARE, PAIR), f32), S((SHARE, DIM), f32), S((SUBS, LANES), f32)],
        in_specs=[any_] * 12 + [vmem] + [any_] * DUO + [vmem] * TRIO,
        out_specs=[any_] * 6 + [vmem],
        scratch_shapes=[V((DUO,) + sq), V(tall), V(wide), V(tall), V(wide), V((DIM, TOKENS)), V((DIM, TOKENS)), V(sq), V(sq), V(kv), V(kv), V(wide, f32), V(wide, f32),
                        V((DUO, TOKENS, QB), f32), V((DUO, TOKENS, QB)), V((DUO, TOKENS, QB)), V((DUO, TOKENS, QB)), V(sq), V((PLACES, RING, RING, RING, CHIP, LANES), f32), V((TRIO, SLOTS, RING, RING, CHIP, LANES), f32),
                        V((TRIO, SLOTS, 6, RING, RING, SHARE, LANES), f32), V((TRIO, SLOTS, 6, RING, SHARE, LANES), f32), V((TRIO, SLOTS, TRIO, CHIP, LANES), f32), V((N_UNITS, CHIP, LANES), f32), V((TOKENS, ROWS)), V(mine), V((DUO * QKV, ROWS)), V(mine),
                        V((SUBS, DIM), f32), V((RING, SUBS, LANES), f32), V((RING, SUBS, LANES), f32), V((7, SUBS, LANES), f32), V((SHARE, SUBS, LANES), f32),
                        D(9 * SLOTS), D(15 * SLOTS), D(DUO + N_UNITS), D(HEADS + RING), D(HEADS + RING), D(26)],
        compiler_params=pltpu.CompilerParams(collective_id=1, has_side_effects=True, vmem_limit_bytes=67043328),
        name='tail',
    )(qt, do_t, k, kt, v, vt, rt, dyc, wqk, wqkp, wvo, wvop, gain, hidden, dy, pos, cos, sin)


def settle_kernel(n, *refs):
    ins, gain, outs, gain_out, bufs, sems = refs[:n], refs[n], refs[n + 1:DUO * n + 1], refs[DUO * n + 1], refs[DUO * n + DUO:-1], refs[-1]
    jobs = []
    for a, o, b in zip(ins, outs, bufs):
        size = a.shape[0] // RING if a.shape[0] == ROWS else a.shape[0]
        jobs += [tuple(r.at[pl.ds(i, size)] for r in (a, b, o)) for i in range(0, a.shape[0], size)]
    takes = [pltpu.make_async_copy(a, b, sems.at[0, i]) for i, (a, b, _) in enumerate(jobs)]
    puts = [pltpu.make_async_copy(b, o, sems.at[1, i]) for i, (_, b, o) in enumerate(jobs)]
    for c in takes:
        c.start()
    gain_out[...] = gain[0:1, :SHARE]
    for take, put in zip(takes, puts):
        take.wait()
        put.start()
    for c in puts:
        c.wait()


def settle(*arrays):
    *large, gain = arrays
    any_, vmem = pl.BlockSpec(memory_space=pl.ANY), pl.BlockSpec(memory_space=pltpu.VMEM)
    return pl.pallas_call(
        functools.partial(settle_kernel, len(large)),
        out_shape=[jax.ShapeDtypeStruct(a.shape, a.dtype) for a in large] + [jax.ShapeDtypeStruct((1, SHARE), gain.dtype)],
        in_specs=[any_] * len(large) + [vmem],
        out_specs=[any_] * len(large) + [vmem],
        scratch_shapes=[pltpu.VMEM(a.shape, a.dtype) for a in large] + [pltpu.SemaphoreType.DMA((DUO, 12))],
        name='settle',
    )(*arrays)


def rope_tables():
    j = np.arange(HEAD_DIM // DUO, dtype=np.float64) / (HEAD_DIM // DUO)
    freq = (ROPE_THETA ** -j).astype(np.float32)
    angle = freq[:, None] * np.arange(TOKENS, dtype=np.float32)[None, :]
    return np.cos(angle.astype(np.float64)).astype(np.float32), np.sin(angle.astype(np.float64)).astype(np.float32)


def solution(mesh):
    def shard_fn(hidden, tok_pos, grad_out, norm_gain, w_query, w_key, w_value, w_out):
        hidden, grad_out = hidden[0], grad_out[0]
        cos_t, sin_t = (jnp.asarray(t) for t in rope_tables())
        *parts, gain = head(hidden, grad_out, w_query, w_key, w_value, w_out, tok_pos, norm_gain.reshape(1, SHARE), cos_t, sin_t)
        parts = [p.reshape(DIM, GROUP) if p.ndim > DUO else p for p in parts]
        result, grad_hidden, gq, gk, gv, go, gout = settle(*tail(*parts, gain, hidden, grad_out, tok_pos, cos_t, sin_t))
        return result[None], grad_hidden[None], gq, gk, gv, go, gout.reshape(SHARE)

    row_spec, pos_spec = P('fsdp', 'cp', None), P('fsdp', 'cp')
    weight_spec, gain_spec = P(('fsdp', 'cp'), None), P(('fsdp', 'cp'))
    return jax.shard_map(shard_fn, mesh=mesh, in_specs=(row_spec, pos_spec, row_spec, gain_spec, weight_spec, weight_spec, weight_spec, weight_spec), out_specs=(row_spec, row_spec, weight_spec, weight_spec, weight_spec, weight_spec, gain_spec), check_vma=False)
```

```python
import functools
import jax
import jax.numpy as jnp
import numpy as np
from jax import lax
from jax.experimental import pallas as pl
from jax.experimental.pallas import tpu as pltpu
from jax.sharding import PartitionSpec as P

LANES, SUBS, RING, TRIO, DUO = 128, 8, 4, 3, 2
PAIR, ROWS, CHIP, SHARE, TURN = 256, 512, 32, 16, 64
HEAD_DIM = LANES
ROPE_THETA = 1000000.0
RMS_EPS = 1e-5
SCALE = HEAD_DIM ** -0.5
LOG2E = 1.4426950408889634

MESH = pl.DeviceIdType.MESH
AXES = ('x', 'y', 'z')
ORDERS = (('x', 'y', 'z'), ('y', 'z', 'x'), ('z', 'x', 'y'))
ALL = pl.ds(0, RING)


def torus():
    f = lax.axis_index('fsdp')
    return {'x': lax.rem(f, RING), 'y': lax.rem(lax.div(f, RING), RING), 'z': lax.div(f, SHARE)}


def step(pos, axis, hop):
    return lax.rem(pos[axis] + hop, RING)


class Batch:
    def __init__(self, comm):
        self.comm, self.index = comm, comm.used
        comm.used += 1

    def _copy(self, src, dst, device):
        send, recv, _ = self.comm.sems
        return pltpu.make_async_remote_copy(src_ref=src, dst_ref=dst, send_sem=send.at[self.index], recv_sem=recv.at[self.index], device_id=device, device_id_type=MESH)

    def send(self, src, dst, device):
        self._copy(src, dst, device).start()
        return self

    def arrived(self, whole):
        self._copy(whole, whole, self.comm.peer()).wait_recv()

    def sent(self, whole):
        self._copy(whole, whole, self.comm.peer()).wait_send()


class Comm:
    def __init__(self, send_sems, recv_sems, local_sems):
        self.pos = torus()
        self.core = lax.axis_index('cp')
        self.sems = (send_sems, recv_sems, local_sems)
        self.used = self.used_local = 0
        self.stored = []

    def far(self, axis, hop):
        p = dict(self.pos)
        p[axis] = step(self.pos, axis, hop)
        return {'fsdp': (p['z'] * RING + p['y']) * RING + p['x'], 'cp': self.core}

    def peer(self):
        return {'fsdp': lax.axis_index('fsdp'), 'cp': 1 - self.core}

    def aside(self, dy, dx):
        return {'fsdp': (self.pos['z'] * RING + step(self.pos, 'y', dy)) * RING + step(self.pos, 'x', dx), 'cp': self.core}

    def announce(self, corners=()):
        sem = pltpu.get_barrier_semaphore()
        for axis in AXES:
            for hop in (1, DUO, TRIO):
                pl.semaphore_signal(sem, inc=1, device_id=self.far(axis, hop), device_id_type=MESH)
        for dy, dx in corners:
            pl.semaphore_signal(sem, inc=1, device_id=self.aside(dy, dx), device_id_type=MESH)
        pl.semaphore_signal(sem, inc=1, device_id=self.peer(), device_id_type=MESH)

    def meet(self, corners=()):
        pl.semaphore_wait(pltpu.get_barrier_semaphore(), 10 + len(corners))

    def ring(self, batch, src, slots, axis):
        for hop in (1, DUO, TRIO):
            batch.send(src, slots.at[hop], self.far(axis, hop))

    def local(self, src, dst):
        i = self.used_local
        self.used_local += 1
        c = pltpu.make_async_copy(src, dst, self.sems[DUO].at[i])
        c.start()
        return c

    def store(self, src, dst):
        self.stored.append(self.local(src, dst))


class Singles(Comm):
    def __init__(self, *sems):
        super().__init__(*sems)
        self.sent, self.exchanged = [], []

    def _copy(self, src, dst, device):
        i = self.used
        self.used += 1
        c = pltpu.make_async_remote_copy(src_ref=src, dst_ref=dst, send_sem=self.sems[0].at[i], recv_sem=self.sems[1].at[i], device_id=device, device_id_type=MESH)
        c.start()
        return c

    def send(self, src, dst, device):
        c = self._copy(src, dst, device)
        self.sent.append(c)
        return c

    def trade(self, src, dst):
        self.exchanged.append(self._copy(src, dst, self.peer()))


def pick(ref, sel, piece):
    lo, cols, first, rows = piece
    return ref.at[sel['z'], sel['y'], sel['x'], pl.ds(first, rows), pl.ds(lo, cols)]


def sem_scratch(remote, local):
    return [pltpu.SemaphoreType.DMA((remote,)), pltpu.SemaphoreType.DMA((remote,)), pltpu.SemaphoreType.DMA((local,))]


def add_into(dst, *srcs, fresh=False):
    def add(idx):
        total, *rest = [s[idx] for s in (srcs if fresh else (dst,) + srcs)]
        for more in rest:
            total = total + more
        dst[idx] = total

    if len(dst.shape) > TRIO:
        @pl.loop(0, dst.shape[0])
        def _(i):
            add((i,))
    else:
        add(Ellipsis)


def halves(lo, n):
    return (lo, n, 0, SHARE), (lo, n, SHARE, SHARE)


GROUPS = (halves(0, 384), halves(384, 384), halves(768, 384))
QK_FIRST = (halves(0, PAIR), halves(384, PAIR), halves(768, PAIR))
QK_LAST = (halves(PAIR, LANES), halves(640, LANES), halves(1024, LANES))
TOKENS = 1024
DIM = 2048
HALF = 1024
QKV = 1280
GROUP = 1152


def scope(name):
    return jax.named_scope(name)


def dot(a, b):
    return jnp.dot(a, b, preferred_element_type=jnp.float32)


def dot_nt(a, b):
    return lax.dot_general(a, b, (((1,), (1,)), ((), ())), preferred_element_type=jnp.float32)


def tile_at(i, n):
    return pl.ds(pl.multiple_of(i * n, n), n)


class Gather:
    def __init__(self, comm, ref, colors, land, held=None):
        self.comm, self.ref, self.colors, self.land = comm, ref, colors, land
        self.held = list(held or [dict(comm.pos) for _ in colors])
        self.spent = []

    def move(self, batch, s, piece, to):
        batch.send(pick(self.ref, s, piece), pick(self.ref, s, piece), to)

    def at(self, k, hop):
        d = ORDERS[k][self.phase]
        return dict(self.held[k], **{d: step(self.comm.pos, d, hop)})

    def begin(self, phase):
        self.phase = phase
        self.rest = Batch(self.comm)
        if phase == 0:
            for hop in (DUO, 1, TRIO):
                for k, (a, _) in enumerate(self.colors):
                    self.move(self.rest, self.held[k], (a[0], a[1], 0, CHIP), self.comm.far(ORDERS[k][0], hop))
            return
        self.up, self.dn = ([Batch(self.comm) for _ in range(TRIO)] for _ in range(DUO))
        for k, (a, b) in enumerate(self.colors):
            d = ORDERS[k][phase]
            up, dn, s = self.comm.far(d, 1), self.comm.far(d, TRIO), self.held[k]
            self.move(self.up[k], s, a, up)
            self.move(self.dn[k], s, b, dn)
            self.move(self.rest, s, b, up)
            self.move(self.rest, s, a, dn)
        if phase == DUO:
            for k, pieces in enumerate(self.colors):
                for piece in pieces:
                    self.land(self.ref, self.held[k], piece)

    def forward(self):
        for k, (a, b) in enumerate(self.colors):
            d = ORDERS[k][self.phase]
            for batch, hop, piece, to in ((self.up[k], TRIO, a, 1), (self.dn[k], 1, b, TRIO)):
                s = self.at(k, hop)
                batch.arrived(pick(self.ref, s, piece))
                self.move(self.rest, s, piece, self.comm.far(d, to))
                if self.phase == DUO:
                    self.land(self.ref, s, piece)
                self.spent.append((batch, pick(self.ref, self.held[k], piece)))

    def end(self):
        axis = ORDERS[0][self.phase]
        blocks = dict(self.held[0], **{axis: pl.ds(0, DUO if self.phase else TRIO)})
        width = sum(a[1] for a, _ in self.colors)
        whole = pick(self.ref, blocks, (0, width, 0, CHIP))
        self.rest.arrived(whole)
        self.spent.append((self.rest, whole))
        for k, (a, b) in enumerate(self.colors):
            if self.phase == DUO:
                for hop, piece in ((TRIO, b), (1, a), (DUO, a), (DUO, b)):
                    self.land(self.ref, self.at(k, hop), piece)
            self.held[k] = dict(self.held[k], **{ORDERS[k][self.phase]: ALL})

    def finish(self):
        for batch, whole in self.spent:
            batch.sent(whole)


def head_kernel(hidden, dy, wq, wk, wv, wo, pos, gain_in, cos_t, sin_t,
                qt_o, dot_o, k_o, kt_o, v_o, vt_o, rt_o, dyc_o, wqk_o, wqkp_o, wvo_o, wvop_o, gain_o,
                hid2, dy2, dys, rs, rt, wqk, wvo, wpeer, pi, pos2, qt, dot_s, kk, kt, vv, vt, cosines, sines, gain, gtile, gbuf, gx, gy, gz, *sems):
    comm = Comm(*sems)
    comm.announce()
    pos_c, core = comm.pos, comm.core
    bf16, f32 = jnp.bfloat16, jnp.float32
    peer = comm.peer()
    rows = tile_at(core, SHARE)
    mine_qk = wqk.at[pos_c['z'], pos_c['y'], pos_c['x'], rows]
    mine_vo = wvo.at[pos_c['z'], pos_c['y'], pos_c['x'], rows]

    def weight_parts(c):
        return ((wq.at[:, tile_at(c, HALF)], mine_qk.at[:, pl.ds(0, HALF)]), (wk.at[:, tile_at(c, LANES)], mine_qk.at[:, pl.ds(HALF, LANES)]),
                (wv.at[:, tile_at(c, LANES)], mine_vo.at[:, pl.ds(0, LANES)]), (wo.at[:, tile_at(c, HALF)], mine_vo.at[:, pl.ds(LANES, HALF)]))

    loads = [comm.local(s, d) for s, d in weight_parts(core)]
    load_x = [comm.local(hidden, hid2.at[pl.ds(0, ROWS)]), comm.local(dy, dy2.at[pl.ds(0, ROWS)])]
    share = lax.broadcasted_iota(jnp.int32, (SUBS, LANES), 1) // SHARE
    gtile[...] = jnp.where(share == pos_c['x'] * DUO + core, jnp.broadcast_to(jnp.concatenate([gain_in[...]] * SUBS, axis=1), (SUBS, LANES)), 0.0)
    with scope('entry'):
        comm.meet()
    swap_w, swap_pos, swap_dy, swap_x, peers_qk, peers_vo = (Batch(comm) for _ in range(6))
    gain_c, gain_x, gain_y, gain_z = (Batch(comm) for _ in range(RING))
    for s, d in weight_parts(1 - core):
        swap_w.send(s, d, peer)
    gain_c.send(gtile, gbuf, peer)
    swap_pos.send(pos, pos2, peer)
    for c in loads:
        c.wait()
    with scope('wait_w'):
        swapped = wqk.at[pos_c['z'], pos_c['y'], pos_c['x']]
        swap_w.arrived(swapped)

    def land_qk(ref, s, cols):
        peers_qk.send(pick(ref, s, cols), pick(wqkp_o, s, cols), peer)

    def land_vo(ref, s, cols):
        peers_vo.send(pick(ref, s, cols), pick(wpeer, s, cols), peer)

    g1 = Gather(comm, wvo, GROUPS, land_vo)
    g2 = Gather(comm, wqk, GROUPS, land_qk)
    g1.begin(0)
    g2.begin(0)
    gain_c.arrived(gbuf)
    gx[0] = gtile[...] + gbuf[...]
    comm.ring(gain_x, gx.at[0], gx, 'x')

    swap_pos.arrived(pos2)

    @pl.loop(0, TOKENS // LANES)
    def _(i):
        want = lax.broadcasted_iota(jnp.int32, (LANES, ROWS), 0) + i * LANES
        for h, have in enumerate((pos, pos2)):
            pi[tile_at(i, LANES), h * ROWS:(h + 1) * ROWS] = jnp.where(want == have[...], 1.0, 0.0).astype(bf16)

    for i in range(RING):
        r = slice(i * PAIR, (i + 1) * PAIR)
        cos, sin = cos_t[:, r], sin_t[:, r]
        cosines[r, :] = jnp.concatenate([cos, cos], axis=0).T
        sines[r, :] = jnp.concatenate([-sin, sin], axis=0).T

    def sort(dst, src, first, last):
        with scope('sort'):
            @pl.loop(first, last)
            def _(j):
                c = tile_at(j, PAIR)
                dst[:, c] = dot(pi[...], src[:, c]).astype(bf16)

    swap_dy.send(dy, dy2.at[pl.ds(ROWS, ROWS)], peer)
    with scope('p0_end'):
        for g in (g1, g2):
            g.end()
            g.begin(1)
    swap_x.send(hidden, hid2.at[pl.ds(ROWS, ROWS)], peer)
    gain_x.arrived(gx.at[pl.ds(1, TRIO)])
    gy[pos_c['y']] = (gx[0] + gx[1]) + (gx[DUO] + gx[TRIO])
    for hop in (1, DUO, TRIO):
        gain_y.send(gy.at[pos_c['y']], gy.at[pos_c['y']], comm.far('y', hop))
    with scope('wait_dy'):
        load_x[1].wait()
        swap_dy.arrived(dy2.at[pl.ds(ROWS, ROWS)])
    sort(dys, dy2, 0, RING)
    with scope('p1a_fwd'):
        g1.forward()
    sort(dys, dy2, RING, 6)
    with scope('p1b_fwd'):
        g2.forward()
    sort(dys, dy2, 6, SUBS)
    with scope('p1a_end'):
        g1.end()
    gain_y.arrived(gy.at[pl.ds(1, TRIO)])
    for j in range(RING):
        gz[pos_c['z'], j] = gy[j]
    for hop in (1, DUO, TRIO):
        gain_z.send(gz.at[pos_c['z']], gz.at[pos_c['z']], comm.far('z', hop))
    g1.begin(DUO)
    comm.store(dys.at[:, tile_at(core, HALF)], dyc_o)
    with scope('p1b_end'):
        g2.end()
    with scope('wait_x'):
        load_x[0].wait()
        swap_x.arrived(hid2.at[pl.ds(ROWS, ROWS)])
    sort(rs, hid2, 0, SUBS)
    with scope('p2q_fwd'):
        g1.forward()
    g2a, g2b = (Gather(comm, wqk, colors, land_qk, g2.held) for colors in (QK_FIRST, QK_LAST))
    g2a.begin(DUO)
    with scope('gain'):
        gain_z.arrived(gz.at[pl.ds(1, TRIO)])
    for i in range(RING):
        for j in range(RING):
            gain[:, (i * RING + j) * LANES:(i * RING + j + 1) * LANES] = gz[i, j]
    comm.store(gain, gain_o)

    def norm(first, last):
        with scope('norm'):
            @pl.loop(first, last)
            def _(i):
                r = tile_at(i, CHIP)
                x = rs[r, :].astype(f32)
                inv = lax.rsqrt(jnp.mean(x * x, axis=-1, keepdims=True) + RMS_EPS)
                rs[r, :] = (x * inv * gain[0:1, :]).astype(bf16)

    norm(0, TOKENS // CHIP)
    with scope('r_t'):
        @pl.loop(0, DIM // PAIR)
        def _(i):
            c = tile_at(i, PAIR)

            @pl.loop(0, TOKENS // PAIR)
            def _(j):
                r = tile_at(j, PAIR)
                rt[c, r] = rs[r, c].T
    comm.store(rt, rt_o)
    with scope('p2o_end'):
        g1.end()
    w_qk, w_vo, w_peer = wqk.reshape(DIM, GROUP), wvo.reshape(DIM, GROUP), wpeer.reshape(DIM, GROUP)
    with scope('vals'):
        @pl.loop(0, DUO)
        def _(i):
            r = tile_at(i, ROWS)
            val = dot(rs[r, :], w_vo[:, :LANES]).astype(bf16)
            vv[r, :] = val
            vt[:, r] = val.T
    for src, dst in ((wvo, wvo_o), (vv, v_o), (vt, vt_o)):
        comm.store(src, dst)
    with scope('p2q_fwd'):
        g2a.forward()
    g2b.begin(DUO)
    with scope('wo_peer'):
        peers_vo.arrived(wpeer)
    comm.store(wpeer, wvop_o)
    with scope('do_t'):
        mine = tile_at(core, HALF)

        @pl.loop(0, TOKENS // PAIR)
        def _(j):
            t = tile_at(j, PAIR)
            w_rows = jnp.concatenate([w_vo[mine, LANES:], w_peer[mine, LANES:]], axis=1)
            d_rows = jnp.concatenate([dys[t, mine], dys[t, tile_at(1 - core, HALF)]], axis=1)
            dot_s[:, t] = dot_nt(w_rows, d_rows).astype(bf16)
    comm.store(dot_s, dot_o)

    def rotated(x, r):
        return (x * cosines[r, :] + pltpu.roll(x, TURN, 1) * sines[r, :]).astype(bf16)

    def queries(columns, heads):
        for i in range(DUO):
            r = slice(i * ROWS, (i + 1) * ROWS)
            x = dot(rs[r, :], columns)
            for h, head in enumerate(heads):
                qt[tile_at(head, LANES), r] = rotated(x[:, h * LANES:(h + 1) * LANES], r).T

    with scope('p2q_end'):
        g2a.end()

    with scope('last_fwd'):
        g2b.forward()
    with scope('q'):
        for t in range(TRIO):
            queries(w_qk[:, t * 384:t * 384 + PAIR], (TRIO * t, TRIO * t + 1))
    for t in range(TRIO):
        two_heads = pl.ds(t * 384, PAIR)
        comm.store(qt.at[two_heads], qt_o.at[two_heads])
    with scope('last_end'):
        g2b.end()
    comm.store(wqk, wqk_o)
    with scope('q_last'):
        last = jnp.concatenate([w_qk[:, PAIR:384], w_qk[:, 640:768], w_qk[:, HALF:]], axis=1)
        for i in range(DUO):
            r = slice(i * ROWS, (i + 1) * ROWS)
            x = dot(rs[r, :], last)
            for h, head in enumerate((DUO, 5)):
                qt[tile_at(head, LANES), r] = rotated(x[:, h * LANES:(h + 1) * LANES], r).T
            key = rotated(x[:, PAIR:], r)
            kk[r, :] = key
            kt[:, r] = key.T
    for src, dst in ((kk, k_o), (kt, kt_o)) + tuple((qt.at[tile_at(h, LANES)], qt_o.at[tile_at(h, LANES)]) for h in (DUO, 5)):
        comm.store(src, dst)
    with scope('finish'):
        peers_qk.arrived(wqk)
        for batch, whole in ((swap_w, swapped), (swap_pos, pos2), (swap_dy, dy2.at[pl.ds(ROWS, ROWS)]), (swap_x, hid2.at[pl.ds(ROWS, ROWS)]), (peers_qk, wqk), (peers_vo, wvo),
                             (gain_c, gbuf), (gain_x, gx.at[pl.ds(1, TRIO)]), (gain_y, gy.at[pl.ds(1, TRIO)]), (gain_z, gz.at[pl.ds(1, TRIO)])):
            batch.sent(whole)
        for g in (g1, g2, g2a, g2b):
            g.finish()
        for c in comm.stored:
            c.wait()


def head(hidden, dy, wq, wk, wv, wo, pos, gain, cos_t, sin_t):
    bf16, f32 = jnp.bfloat16, jnp.float32
    any_ = pl.BlockSpec(memory_space=pl.ANY)
    vmem = pl.BlockSpec(memory_space=pltpu.VMEM)
    S = lambda shape, d=bf16: jax.ShapeDtypeStruct(shape, d)
    V = lambda shape, d=bf16: pltpu.VMEM(shape, d)
    group = (RING, RING, RING, CHIP, GROUP)
    sq, tall, wide = (HALF, TOKENS), (TOKENS, LANES), (LANES, TOKENS)
    full = (TOKENS, DIM)
    return pl.pallas_call(
        head_kernel,
        out_shape=[S(sq), S(sq), S(tall), S(wide), S(tall), S(wide), S((DIM, TOKENS)), S((TOKENS, HALF)), S(group), S(group), S(group), S(group), S((SUBS, DIM), f32)],
        in_specs=[any_] * 6 + [vmem] * RING,
        out_specs=[any_] * 13,
        scratch_shapes=[V(full), V(full), V(full), V(full), V((DIM, TOKENS)), V(group), V(group), V(group), V((TOKENS, TOKENS)), V((1, ROWS), jnp.int32),
                        V(sq), V(sq), V(tall), V(wide), V(tall), V(wide), V(tall, f32), V(tall, f32), V((SUBS, DIM), f32), V((SUBS, LANES), f32), V((SUBS, LANES), f32), V((RING, SUBS, LANES), f32), V((RING, SUBS, LANES), f32), V((RING, RING, SUBS, LANES), f32)] + sem_scratch(47, 22),
        compiler_params=pltpu.CompilerParams(collective_id=0, has_side_effects=True, vmem_limit_bytes=60 * DUO**20),
        name='head',
    )(hidden, dy, wq, wk, wv, wo, pos, gain, cos_t, sin_t)


HEADS = SUBS
UNIT_K, UNIT_V = SUBS, 9
N_UNITS = 18
GAIN = N_UNITS
SLOTS = RING
LAST = 5
ABREAST = DUO
LINES = ((0, TRIO, 6, 9, 12, 15), (1, RING, 7, 10, 13, SHARE), (DUO, 5, SUBS, 11, 14, 17))
COLOR = {u: k for k, line in enumerate(LINES) for u in line}
RANK = {u: i for line in LINES for i, u in enumerate(line)}
SWAPPED = (1, TRIO, RING, SUBS, 10)
ORDER = {u: ORDERS[k] if u not in SWAPPED else (ORDERS[k][0], ORDERS[k][DUO], ORDERS[k][1]) for u, k in COLOR.items()}
BEFORE = {u: line[i - SLOTS] if i >= SLOTS else None for line in LINES for i, u in enumerate(line)}
PLACES = 12
PLACE = {u: u % PLACES for u in range(N_UNITS)}
WIRE = (2.82, 0.71, 0.36)
LATENCY = 2.4
STAGE_COST = 0.08


class Plan:
    def __init__(self):
        self.now, self.stage, self.ready, self.order, self.link = 0.0, {}, {}, [], {}
        self.mark = {}

    def _wire(self, u, phase, count):
        link = ORDER[u][phase]
        t = max(self.link.get(link, 0.0), self.now)
        first = t + WIRE[phase] + LATENCY
        self.link[link] = t + WIRE[phase] * count
        return first if phase < DUO else self.link[link] + LATENCY

    def free(self, u, phase):
        if BEFORE[u] is None:
            return True
        done = self.mark.get((BEFORE[u], (DUO, RING, 5)[phase]))
        if done is None:
            return False
        sent = ((0, 1), (DUO, TRIO), (RING,))[phase]
        return any(self.mark.get((j, s), -1) > done and (j, s + 1) in self.mark for j, order in ORDER.items() if order[phase] == ORDER[u][phase] for s in sent)

    def run(self, u):
        stage = self.stage[u]
        self.order.append((u, stage))
        self.mark[u, stage] = len(self.order)
        self.now = max(self.now, self.ready[u]) + STAGE_COST
        self.stage[u] = stage + 1
        if stage == (TRIO if u == GAIN else LAST):
            del self.stage[u]
        elif u == GAIN:
            self.ready[u] = max([self.now] + [self.link.get(a, 0.0) for a in ('', 'z', 'xy')[stage]]) + DUO * LATENCY
        elif stage % DUO:
            self.ready[u] = self._wire(u, stage // DUO, 1)
        else:
            self.ready[u] = self._wire(u, stage // DUO, DUO)

    def blocked(self, u):
        stage = self.stage[u]
        if u == GAIN:
            return False
        if stage == 0 and sum(0 < self.stage.get(j, 0) <= DUO for j in LINES[COLOR[u]]) >= ABREAST:
            return True
        if stage == DUO and BEFORE[u] is not None and (BEFORE[u], LAST) not in self.mark:
            return True
        return stage in (0, DUO, RING) and not self.free(u, stage // DUO)

    def start(self, u):
        self.stage[u], self.ready[u] = 0, self.now

    def due(self):
        first = len(self.order)
        while True:
            ripe = [(self.ready[u], u) for u in self.stage if self.ready[u] <= self.now and not self.blocked(u)]
            if not ripe:
                return self.order[first:]
            self.run(min(ripe)[1])

    def vacated(self, u):
        return (u, DUO) in self.mark

    def rush(self, done):
        first = len(self.order)
        while not done():
            self.run(min((self.ready[u], u) for u in self.stage if not self.blocked(u))[1])
        return self.order[first:]


QB = PAIR
PAIRS = HEADS // DUO
NBLK = TOKENS // QB
HALVES = (pl.ds(0, SHARE), pl.ds(SHARE, SHARE))
PLANE = tuple((dy, dx) for dy in range(RING) for dx in range(RING) if dy or dx)
CORNERS = tuple((dy, dx) for dy, dx in PLANE if dy and dx)


class Scatter:
    def __init__(self, comm, part, mid, bufs, fin, outs, send_sems, recv_sems, swap_sems):
        self.pos, self.part, self.mid, self.bufs, self.fin, self.outs = comm.pos, part, mid, bufs, fin, outs
        self.send_sems, self.recv_sems, self.swap_sems = send_sems, recv_sems, swap_sems
        self.near = {(a, hop): comm.far(a, hop) for a in AXES for hop in (1, DUO, TRIO)}
        self.hops = {(a, hop): step(comm.pos, a, hop) for a in AXES for hop in (1, DUO, TRIO)}
        self.peer, self.core = comm.peer(), comm.core
        self.keep, self.give = tile_at(comm.core, SHARE), tile_at(1 - comm.core, SHARE)
        self.drained = set()

    def slot(self, u):
        return COLOR[u], RANK[u] % SLOTS

    def buf(self, u, phase):
        return self.bufs[phase].at[self.slot(u)]

    def view(self, u, phase, hop, half=None):
        order = ORDER[u]
        at = {a: ALL for a in AXES}
        for a in order[1:phase]:
            at[a] = self.pos[a]
        at[order[phase]] = self.hops[order[phase], hop] if hop else self.pos[order[phase]]
        rows = pl.ds(0, CHIP) if half is None else HALVES[half]
        if phase == 0:
            return self.part.at[PLACE[u], at['z'], at['y'], at['x'], rows, :]
        return self.mid.at[self.slot(u) + tuple(at[a] for a in 'zyx' if a != order[0]) + (rows, slice(None))]

    def copy(self, src, dst, sems, device):
        return pltpu.make_async_remote_copy(src_ref=src, dst_ref=dst, send_sem=sems[0], recv_sem=sems[1], device_id=device, device_id_type=MESH)

    def sems(self, u, phase, kind=0):
        k, i = self.slot(u)
        at = (k * SLOTS + i) * TRIO + phase
        return self.send_sems.at[at], self.recv_sems.at[(k * SLOTS + i) * 5 + DUO * phase + kind]

    def send(self, u, phase, name):
        axis = ORDER[u][phase]
        if phase == DUO:
            src, to = self.view(u, DUO, name + 1), name + 1
        else:
            hop, half, to = ((DUO, 0, 1), (DUO, 1, TRIO), (1, 1, 1), (TRIO, 0, TRIO), (1, 0, 1), (TRIO, 1, TRIO))[name]
            src = self.view(u, phase, hop, half)
        self.copy(src, self.buf(u, phase).at[name], self.sems(u, phase, int(name > 1 and phase < DUO)), self.near[axis, to]).start()

    def launch(self, u, phase):
        if BEFORE[u] is not None:
            self.drain(BEFORE[u], phase)
        for name in range(RING if phase < DUO else TRIO):
            self.send(u, phase, name)

    def arrived(self, u, phase, first, count):
        whole = self.buf(u, phase).at[pl.ds(first, count)]
        self.copy(whole, whole, self.sems(u, phase, int(first > 0)), self.peer).wait_recv()

    def drain(self, u, phase):
        if (u, phase) not in self.drained:
            self.drained.add((u, phase))
            whole = self.buf(u, phase)
            self.copy(whole, whole, self.sems(u, phase), self.peer).wait_send()

    def out(self, u):
        if u < HEADS:
            out, col = self.outs[0], self.core * HALF + u * LANES
        elif u < 10:
            out, col = self.outs[u - 7], self.core * LANES
        else:
            out, col = self.outs[TRIO], self.core * HALF + (u - 10) * LANES
        return out.at[:, pl.ds(pl.multiple_of(col, LANES), LANES)]

    def kept(self, u):
        return pltpu.make_async_copy(self.fin.at[u, self.keep], self.out(u), self.swap_sems.at[DUO + u])

    def run(self, u, stage):
        if stage == 0:
            return self.launch(u, 0)
        phase = (stage - 1) // DUO
        if stage == LAST:
            self.arrived(u, DUO, 0, TRIO)
            got = self.buf(u, DUO)
            self.fin[u] = self.view(u, DUO, 0)[...] + (got[0] + got[1] + got[DUO])
            self.copy(self.fin.at[u, self.give], self.out(u), (self.swap_sems.at[0], self.swap_sems.at[1]), self.peer).start()
            self.kept(u).start()
            return
        got = self.buf(u, phase)
        if stage % DUO:
            self.arrived(u, phase, 0, DUO)
            for name, hop in ((0, 1), (1, TRIO)):
                add_into(self.view(u, phase, hop, name), got.at[name])
                self.send(u, phase, name + RING)
            return
        self.arrived(u, phase, DUO, RING)
        if phase == 0 and BEFORE[u] is not None:
            self.drain(BEFORE[u], 1)
            self.drain(BEFORE[u], DUO)
        for half, names in ((0, (TRIO, RING)), (1, (DUO, 5))):
            if phase:
                add_into(self.view(u, phase, 0, half), *[got.at[name] for name in names])
            else:
                dst = self.mid.at[self.slot(u) + (ALL, ALL, HALVES[half], slice(None))]
                add_into(dst, self.view(u, 0, 0, half), *[got.at[name] for name in names], fresh=True)
        self.launch(u, phase + 1)

    def finish(self):
        for u in range(N_UNITS):
            for phase in range(TRIO):
                self.drain(u, phase)
        half = self.fin.at[:, pl.ds(0, SHARE)]
        swaps = self.copy(half, half, (self.swap_sems.at[0], self.swap_sems.at[1]), self.peer)
        swaps.wait_send()
        swaps.wait_recv()
        for u in range(N_UNITS):
            self.kept(u).wait()


def attend(heads, qt, do_t, k, kt, v, vt, cos, sin, o_row, ot, dq, dkt, dvt, s_scr, e_scr, p_scr, d_scr):
    f32, bf16 = jnp.float32, jnp.bfloat16
    strip = TURN
    work = [(h, j) for j in range(NBLK) for h in range(len(heads))]

    def strips(c):
        return [(i * strip, slice(c * QB + i * strip, c * QB + (i + 1) * strip)) for i in range(QB // strip)]

    def fold(x, op):
        return op(x.reshape(strip // SUBS, SUBS, QB), axis=0)

    def scores(i):
        (h, j), b = work[i], i % DUO
        q_t = qt[heads[h], j * QB:(j + 1) * QB]
        top = jnp.full((SUBS, QB), -jnp.inf, f32)
        for c in range(j + 1):
            tile = dot(k[c * QB:(c + 1) * QB, :], q_t)
            for at, rows in strips(c):
                s = tile[at:at + strip]
                if c == j:
                    seen = lax.broadcasted_iota(jnp.int32, (strip, QB), 0) + at <= lax.broadcasted_iota(jnp.int32, (strip, QB), 1)
                    s = jnp.where(seen, s, -jnp.inf)
                s_scr[b, rows, :] = s
                top = jnp.maximum(top, fold(s, jnp.max))
        return jnp.max(top, axis=0, keepdims=True)

    def rest(i, m):
        (h, j), b = work[i], i % DUO
        cols, n = slice(j * QB, (j + 1) * QB), (j + 1) * QB
        q_t, d_t = qt[heads[h], cols], do_t[heads[h], cols]
        tot = jnp.zeros((SUBS, QB), f32)
        for c in range(j + 1):
            for at, rows in strips(c):
                e = jnp.exp2((s_scr[b, rows, :] - m) * (SCALE * LOG2E))
                s_scr[b, rows, :] = e
                e_scr[b, rows, :] = e.astype(bf16)
                tot = tot + fold(e, jnp.sum)
        den = jnp.sum(tot, axis=0, keepdims=True)
        inv = 1.0 / den
        o = (dot(vt[:, :n], e_scr[b, :n, :]) / den).astype(bf16)
        ot[o_row(h), cols] = o
        delta = jnp.sum(d_t.astype(f32) * o.astype(f32), axis=0, keepdims=True)
        for c in range(j + 1):
            dp = dot(v[c * QB:(c + 1) * QB, :], d_t)
            for at, rows in strips(c):
                p = s_scr[b, rows, :] * inv
                p_scr[b, rows, :] = p.astype(bf16)
                d_scr[b, rows, :] = (p * (dp[at:at + strip] - delta)).astype(bf16)
        dvt[:, :n] += dot_nt(d_t, p_scr[b, :n, :])
        dkt[:, :n] += dot_nt(q_t, d_scr[b, :n, :])
        g = dot(kt[:, :n], d_scr[b, :n, :]) * SCALE
        co, si = cos[:, cols], sin[:, cols]
        x, y = g[:TURN], g[TURN:]
        dq[heads[h], cols] = jnp.concatenate([x * co + y * si, y * co - x * si], axis=0).astype(bf16)

    m = scores(0)
    for i in range(len(work)):
        later = scores(i + 1) if i + 1 < len(work) else None
        rest(i, m)
        m = later


def tail_kernel(qt, do_t, k, kt, v, vt, rt, dyc, wqk, wqkp, wvo, wvop, gain, hidden, dy, pos, cos, sin,
                result, grad_x, gq, gk, gv, go, gout,
                two, ks, kts, vs, vts, rts, ots, dqo, dqp, dkvo, dkvp, dkt, dvt, s_scr, e_scr, p_scr, d_scr, dycs, part, mid, buf1, buf2, buf3, fin, own, onat, dnat, xs, gacc, gpart, gpeer, gz, gx,
                send_sems, recv_sems, swap_sems, trade_send, trade_recv, local_sems):
    comm = Singles(trade_send, trade_recv, local_sems)
    comm.used = HEADS
    f32, bf16 = jnp.float32, jnp.bfloat16
    core, peer = comm.core, comm.peer()
    a1, a2 = two.at[0], two.at[1]
    sc = Scatter(comm, part, mid, (buf1, buf2, buf3), fin, (gq, gk, gv, go), send_sems, recv_sems, swap_sems)
    plan = Plan()
    some, most = pl.ds(0, PAIR), pl.ds(PAIR, HALF - PAIR)
    loads = [comm.local(s, d) for s, d in ((qt.at[some], two.at[0, some]), (k, ks), (do_t.at[some], two.at[1, some]), (vt, vts), (v, vs), (kt, kts))]
    comm.announce(CORNERS)
    dkt[...] = jnp.zeros_like(dkt)
    dvt[...] = jnp.zeros_like(dvt)
    with scope('wait_q'):
        for c in loads:
            c.wait()
    loads = [comm.local(s, d) for s, d in ((rt, rts), (qt.at[most], two.at[0, most]), (do_t.at[most], two.at[1, most]))]
    later = [comm.local(s, d) for s, d in ((dyc, dycs), (hidden, xs))]

    def emit(stages):
        for u, stage in stages:
            with scope(f'u{u}_s{stage}'):
                if u == GAIN:
                    sum_gain(stage)
                else:
                    sc.run(u, stage)

    def after(cost):
        plan.now += cost
        return plan.due()

    def head_trades(g):
        row = pl.ds(pl.multiple_of((core * HEADS + DUO * g) * LANES, PAIR), PAIR)
        mine = tile_at(g, PAIR)
        return [pltpu.make_async_remote_copy(src_ref=s, dst_ref=d, send_sem=trade_send.at[i], recv_sem=trade_recv.at[i], device_id=peer, device_id_type=MESH)
                for s, d, i in ((ots.at[row], ots.at[row], g), (dqo.at[mine], dqp.at[mine], PAIRS + g))]

    def gradient(place, count, left, right, mul):
        with scope('grad'):
            @pl.loop(0, DUO)
            def _(z):
                g = mul(left[tile_at(z, HALF), :], right())
                for i in range(count):
                    part[place + i, tile_at(z, DUO)] = g[:, i * LANES:(i + 1) * LANES].reshape(DUO, RING, RING, CHIP, LANES)

    attended, paired = [], []
    for g in range(PAIRS):
        attended.append(after(5.1))
        plan.now += 1.5
        plan.start(DUO * g)
        plan.start(DUO * g + 1)
        paired.append(plan.due())

    @pl.loop(0, PAIRS)
    def _(g):
        def at(table):
            for i in range(PAIRS):
                if table[i]:
                    pl.when(g == i)(functools.partial(emit, table[i]))

        heads = [tile_at(DUO * g + i, LANES) for i in range(DUO)]
        with scope('attend'):
            attend(heads, a1, a2, ks, kts, vs, vts, cos, sin, lambda i: tile_at(core * HEADS + DUO * g + i, LANES), ots, dqo, dkt, dvt, s_scr, e_scr, p_scr, d_scr)

        @pl.when(g == 0)
        def _():
            with scope('entry'):
                comm.meet(CORNERS)
                for c in loads:
                    c.wait()
        for c in head_trades(g):
            c.start()
        at(attended)
        gradient(DUO * g, DUO, rts, lambda: dqo[tile_at(g, PAIR), :], dot_nt)
        at(paired)

    def beat(cost, *starts):
        plan.now += cost
        for u in starts:
            plan.start(u)
        emit(plan.due())

    wkv, wkvp = e_scr.reshape(DIM, PAIR), p_scr.reshape(DIM, PAIR)
    later += [comm.local(src.at[:, pl.ds(at, LANES)], dst.at[:, pl.ds(to, LANES)]) for srcs, dst in (((wqk, wvo), wkv), ((wqkp, wvop), wkvp)) for src, at, to in ((srcs[0], HALF, 0), (srcs[1], 0, LANES))]
    wqp_loads = [comm.local(wqkp.at[tile_at(i, HALF), pl.ds(0, HALF)], two.at[i]) for i in range(DUO)]
    key = dkt[...] * SCALE
    co, si, x, y = cos[...], sin[...], key[:TURN], key[TURN:]
    dkvo[:LANES, :] = jnp.concatenate([x * co + y * si, y * co - x * si], axis=0).astype(bf16)
    dkvo[LANES:, :] = dvt[...].astype(bf16)
    comm.trade(dkvo, dkvp)
    gradient(UNIT_K, DUO, rts, lambda: dkvo[...], dot_nt)
    beat(1.8, UNIT_K, UNIT_V)
    wq_load = comm.local(wqk.at[:, pl.ds(0, HALF)], rts)
    for c in later:
        c.wait()
    with scope('trades'):
        for g in range(PAIRS):
            for c in head_trades(g):
                c.wait()

    waiting = list(range(RING))

    def output_gradients(force=False):
        while waiting:
            first = 10 + DUO * waiting[0]
            before = [u for u in range(N_UNITS) if u < first and PLACE[u] in (PLACE[first], PLACE[first + 1])]
            if force:
                emit(plan.rush(lambda: all(map(plan.vacated, before))))
            if not all(map(plan.vacated, before)):
                return
            for u in before:
                sc.drain(u, 0)
            i = waiting.pop(0)
            gradient(PLACE[first], DUO, ots, lambda: dycs[:, i * PAIR:(i + 1) * PAIR], dot)
            plan.start(first)
            plan.start(first + 1)
            beat(1.5)

    def piece(cost):
        beat(cost)
        output_gradients()

    def ticking(n, cost, body):
        tables = [after(cost) for _ in range(n)]

        @pl.loop(0, n)
        def _(i):
            body(i)
            for j, table in enumerate(tables):
                if table:
                    pl.when(i == j)(functools.partial(emit, table))
        output_gradients()

    @pl.loop(0, TOKENS // LANES)
    def _(i):
        want = lax.broadcasted_iota(jnp.int32, (LANES, ROWS), 0) + i * LANES
        own[tile_at(i, LANES), :] = jnp.where(want == pos[...], 1.0, 0.0).astype(bf16)

    def unsort(at, src_t, n):
        with scope('unsort'):
            dnat[at:at + n, :] = dot(src_t[:n, :], own[...]).astype(bf16)

    output_gradients()
    for c in comm.exchanged:
        c.wait_recv()
    unsort(0, dqo, HALF)
    dy_loads = [comm.local(dy.at[:, tile_at(i, HALF)], dqo.at[tile_at(i, ROWS)]) for i in range(DUO)]
    piece(1.2)
    unsort(HALF, dqp, HALF)
    piece(1.2)
    unsort(DUO * HALF, dkvo, PAIR)
    unsort(DUO * HALF + PAIR, dkvp, PAIR)
    piece(0.7)
    wq_load.wait()
    for c in wqp_loads + dy_loads:
        c.wait()
    gacc[...] = jnp.zeros_like(gacc)

    def dr_parts(half, r):
        return [s_scr.at[half, r(i * PAIR), :] for i in range(RING)]

    def back(block, then):
        def dr(half):
            with scope('dr'):
                c = tile_at(half, HALF)
                left = jnp.concatenate([rts[c, :], two[half], wkv[c, :], wkvp[c, :]], axis=1)
                acc = dot(left, dnat[:, block * PAIR:(block + 1) * PAIR])
                for i, ref in enumerate(dr_parts(half, lambda at: pl.ds(at, PAIR))):
                    ref[...] = acc[i * PAIR:(i + 1) * PAIR, :].T

        def norm(part):
            with scope('back'):
                @pl.loop(0, RING)
                def _(i):
                    j = part * RING + i
                    q = pl.ds(pl.multiple_of(block * PAIR + j * SHARE, SHARE), SHARE)
                    d = jnp.concatenate([ref[...] for half in range(DUO) for ref in dr_parts(half, lambda at: pl.ds(pl.multiple_of(at + j * SHARE, SHARE), SHARE))], axis=1)
                    x = xs[q, :].astype(f32)
                    inv = lax.rsqrt(jnp.mean(x * x, axis=-1, keepdims=True) + RMS_EPS)
                    unit = x * inv
                    gacc[...] += jnp.sum((d * unit).reshape(DUO, SUBS, DIM), axis=0)
                    dg = d * gain[0:1, :]
                    new = inv * (dg - unit * jnp.mean(dg * unit, axis=-1, keepdims=True))
                    for half in range(DUO):
                        r = pl.ds(pl.multiple_of(half * ROWS + block * PAIR + j * SHARE, SHARE), SHARE)
                        dqo[r, :] = (dqo[r, :].astype(f32) + new[:, half * HALF:(half + 1) * HALF]).astype(bf16)

        ticking(DUO, 1.6, dr)
        then()
        ticking(RING, 0.92, norm)

    back(0, lambda: None)
    wo_loads = []
    back(1, lambda: wo_loads.extend([comm.local(wvo.at[:, pl.ds(LANES, HALF)], rts)] + [comm.local(wvop.at[tile_at(i, HALF), pl.ds(LANES, HALF)], two.at[i]) for i in range(DUO)]))
    for i in range(DUO):
        comm.store(dqo.at[tile_at(i, ROWS)], grad_x.at[:, tile_at(i, HALF)])
    total = jnp.sum(gacc[...], axis=0, keepdims=True)
    gpart[...] = jnp.zeros_like(gpart)
    for i in range(RING):
        for j in range(RING):
            gpart[i, j:j + 1, :] = total[:, (i * RING + j) * LANES:(i * RING + j + 1) * LANES]

    gain_c, gain_z, gain_p = (Batch(comm) for _ in range(TRIO))

    def sum_gain(stage):
        if stage == 0:
            gain_c.send(gpart, gpeer, peer)
        elif stage == 1:
            gain_c.arrived(gpeer)
            for j in range(RING):
                gz[j] = gpart[j] + gpeer[j]
            for hop in (1, DUO, TRIO):
                gain_z.send(gz.at[step(comm.pos, 'z', hop)], gz.at[TRIO + hop], comm.far('z', hop))
        elif stage == DUO:
            gain_z.arrived(gz.at[pl.ds(RING, TRIO)])
            gx[0] = (gz[comm.pos['z']] + gz[RING]) + (gz[5] + gz[6])
            for dy, dx in PLANE:
                gain_p.send(gx.at[0], gx.at[dy * RING + dx], comm.aside(dy, dx))
        else:
            gain_p.arrived(gx.at[pl.ds(1, 15)])
            gpeer[0] = jnp.sum(gx[...], axis=0)
            mine = jnp.broadcast_to(gpeer[0, pl.ds(comm.pos['y'], 1), :], (SUBS, LANES))
            gout[...] = pltpu.roll(mine, LANES - (comm.pos['x'] * CHIP + core * SHARE), 1)

    plan.start(GAIN)
    beat(0.2)
    for i in range(DUO):
        with scope('unsort_o'):
            @pl.loop(0, DUO)
            def _(j):
                r = pl.ds(pl.multiple_of(i * HALF + j * ROWS, ROWS), ROWS)
                onat[:, r] = dot(ots[r, :], own[...]).astype(bf16).T
        piece(1.58)
    output_gradients(True)

    def project_out(col, weights, i):
        with scope('project'):
            @pl.loop(DUO * i, DUO * i + DUO)
            def _(j):
                c = tile_at(j, PAIR)
                dst = pl.ds(pl.multiple_of(col + j * PAIR, PAIR), PAIR)
                xs[:, dst] = (xs[:, dst].astype(f32) + dot(onat[...], weights(c))).astype(bf16)
        beat(1.48)

    def own_half(c):
        return rts[:, c]

    def other_half(c):
        return jnp.concatenate([a1[:, c], a2[:, c]], axis=0)

    for c in wo_loads:
        c.wait()
    for col, weights in ((core * HALF, own_half), ((1 - core) * HALF, other_half)):
        for i in range(DUO):
            project_out(col, weights, i)
    comm.store(xs, result)
    emit(plan.rush(lambda: not plan.stage))
    with scope('finish'):
        sc.finish()
        for batch, whole in ((gain_c, gpart), (gain_z, gz.at[pl.ds(RING, TRIO)]), (gain_p, gx.at[pl.ds(1, 15)])):
            batch.sent(whole)
        for c in comm.exchanged:
            c.wait_send()
        for c in comm.stored:
            c.wait()


def tail(qt, do_t, k, kt, v, vt, rt, dyc, wqk, wqkp, wvo, wvop, gain, hidden, dy, pos, cos, sin):
    bf16, f32 = jnp.bfloat16, jnp.float32
    any_ = pl.BlockSpec(memory_space=pl.ANY)
    vmem = pl.BlockSpec(memory_space=pltpu.VMEM)
    S = lambda shape, d=bf16: jax.ShapeDtypeStruct(shape, d)
    V = lambda shape, d=bf16: pltpu.VMEM(shape, d)
    D = lambda n: pltpu.SemaphoreType.DMA((n,))
    sq, tall, wide = (HALF, TOKENS), (TOKENS, LANES), (LANES, TOKENS)
    mine, kv = (ROWS, DIM), (PAIR, TOKENS)
    return pl.pallas_call(
        tail_kernel,
        out_shape=[S(mine), S(mine), S((SHARE, DIM), f32), S((SHARE, PAIR), f32), S((SHARE, PAIR), f32), S((SHARE, DIM), f32), S((SUBS, LANES), f32)],
        in_specs=[any_] * 12 + [vmem] + [any_] * DUO + [vmem] * TRIO,
        out_specs=[any_] * 6 + [vmem],
        scratch_shapes=[V((DUO,) + sq), V(tall), V(wide), V(tall), V(wide), V((DIM, TOKENS)), V((DIM, TOKENS)), V(sq), V(sq), V(kv), V(kv), V(wide, f32), V(wide, f32),
                        V((DUO, TOKENS, QB), f32), V((DUO, TOKENS, QB)), V((DUO, TOKENS, QB)), V((DUO, TOKENS, QB)), V(sq), V((PLACES, RING, RING, RING, CHIP, LANES), f32), V((TRIO, SLOTS, RING, RING, CHIP, LANES), f32),
                        V((TRIO, SLOTS, 6, RING, RING, SHARE, LANES), f32), V((TRIO, SLOTS, 6, RING, SHARE, LANES), f32), V((TRIO, SLOTS, TRIO, CHIP, LANES), f32), V((N_UNITS, CHIP, LANES), f32), V((TOKENS, ROWS)), V(mine), V((DUO * QKV, ROWS)), V(mine),
                        V((SUBS, DIM), f32), V((RING, SUBS, LANES), f32), V((RING, SUBS, LANES), f32), V((7, SUBS, LANES), f32), V((SHARE, SUBS, LANES), f32),
                        D(9 * SLOTS), D(15 * SLOTS), D(DUO + N_UNITS), D(HEADS + RING), D(HEADS + RING), D(26)],
        compiler_params=pltpu.CompilerParams(collective_id=1, has_side_effects=True, vmem_limit_bytes=67043328),
        name='tail',
    )(qt, do_t, k, kt, v, vt, rt, dyc, wqk, wqkp, wvo, wvop, gain, hidden, dy, pos, cos, sin)


def settle_kernel(n, *refs):
    ins, gain, outs, gain_out, bufs, sems = refs[:n], refs[n], refs[n + 1:DUO * n + 1], refs[DUO * n + 1], refs[DUO * n + DUO:-1], refs[-1]
    jobs = []
    for a, o, b in zip(ins, outs, bufs):
        size = a.shape[0] // RING if a.shape[0] == ROWS else a.shape[0]
        jobs += [tuple(r.at[pl.ds(i, size)] for r in (a, b, o)) for i in range(0, a.shape[0], size)]
    takes = [pltpu.make_async_copy(a, b, sems.at[0, i]) for i, (a, b, _) in enumerate(jobs)]
    puts = [pltpu.make_async_copy(b, o, sems.at[1, i]) for i, (_, b, o) in enumerate(jobs)]
    for c in takes:
        c.start()
    gain_out[...] = gain[0:1, :SHARE]
    for take, put in zip(takes, puts):
        take.wait()
        put.start()
    for c in puts:
        c.wait()


def settle(*arrays):
    *large, gain = arrays
    any_, vmem = pl.BlockSpec(memory_space=pl.ANY), pl.BlockSpec(memory_space=pltpu.VMEM)
    return pl.pallas_call(
        functools.partial(settle_kernel, len(large)),
        out_shape=[jax.ShapeDtypeStruct(a.shape, a.dtype) for a in large] + [jax.ShapeDtypeStruct((1, SHARE), gain.dtype)],
        in_specs=[any_] * len(large) + [vmem],
        out_specs=[any_] * len(large) + [vmem],
        scratch_shapes=[pltpu.VMEM(a.shape, a.dtype) for a in large] + [pltpu.SemaphoreType.DMA((DUO, 12))],
        name='settle',
    )(*arrays)


def rope_tables():
    j = np.arange(HEAD_DIM // DUO, dtype=np.float64) / (HEAD_DIM // DUO)
    freq = (ROPE_THETA ** -j).astype(np.float32)
    angle = freq[:, None] * np.arange(TOKENS, dtype=np.float32)[None, :]
    return np.cos(angle.astype(np.float64)).astype(np.float32), np.sin(angle.astype(np.float64)).astype(np.float32)


def solution(mesh):
    def shard_fn(hidden, tok_pos, grad_out, norm_gain, w_query, w_key, w_value, w_out):
        hidden, grad_out = hidden[0], grad_out[0]
        cos_t, sin_t = (jnp.asarray(t) for t in rope_tables())
        *parts, gain = head(hidden, grad_out, w_query, w_key, w_value, w_out, tok_pos, norm_gain.reshape(1, SHARE), cos_t, sin_t)
        parts = [p.reshape(DIM, GROUP) if p.ndim > DUO else p for p in parts]
        result, grad_hidden, gq, gk, gv, go, gout = settle(*tail(*parts, gain, hidden, grad_out, tok_pos, cos_t, sin_t))
        return result[None], grad_hidden[None], gq, gk, gv, go, gout.reshape(SHARE)

    row_spec, pos_spec = P('fsdp', 'cp', None), P('fsdp', 'cp')
    weight_spec, gain_spec = P(('fsdp', 'cp'), None), P(('fsdp', 'cp'))
    return jax.shard_map(shard_fn, mesh=mesh, in_specs=(row_spec, pos_spec, row_spec, gain_spec, weight_spec, weight_spec, weight_spec, weight_spec), out_specs=(row_spec, row_spec, weight_spec, weight_spec, weight_spec, weight_spec, gain_spec), check_vma=False)
```

```python
import functools
import jax
import jax.numpy as jnp
import numpy as np
from jax import lax
from jax.experimental import pallas as pl
from jax.experimental.pallas import tpu as pltpu
from jax.sharding import PartitionSpec as P

LANES, SUBS, RING, TRIO, DUO = 128, 8, 4, 3, 2
PAIR, ROWS, CHIP, SHARE, TURN = 256, 512, 32, 16, 64
HEAD_DIM = LANES
ROPE_THETA = 1000000.0
RMS_EPS = 1e-5
SCALE = HEAD_DIM ** -0.5
LOG2E = 1.4426950408889634

MESH = pl.DeviceIdType.MESH
AXES = ('x', 'y', 'z')
ORDERS = (('x', 'y', 'z'), ('y', 'z', 'x'), ('z', 'x', 'y'))
ALL = pl.ds(0, RING)


def torus():
    f = lax.axis_index('fsdp')
    return {'x': lax.rem(f, RING), 'y': lax.rem(lax.div(f, RING), RING), 'z': lax.div(f, SHARE)}


def step(pos, axis, hop):
    return lax.rem(pos[axis] + hop, RING)


class Batch:
    def __init__(self, comm):
        self.comm, self.index = comm, comm.used
        comm.used += 1

    def _copy(self, src, dst, device):
        send, recv, _ = self.comm.sems
        return pltpu.make_async_remote_copy(src_ref=src, dst_ref=dst, send_sem=send.at[self.index], recv_sem=recv.at[self.index], device_id=device, device_id_type=MESH)

    def send(self, src, dst, device):
        self._copy(src, dst, device).start()
        return self

    def arrived(self, whole):
        self._copy(whole, whole, self.comm.peer()).wait_recv()

    def sent(self, whole):
        self._copy(whole, whole, self.comm.peer()).wait_send()


class Comm:
    def __init__(self, send_sems, recv_sems, local_sems):
        self.pos = torus()
        self.core = lax.axis_index('cp')
        self.sems = (send_sems, recv_sems, local_sems)
        self.used = self.used_local = 0
        self.stored = []

    def far(self, axis, hop):
        p = dict(self.pos)
        p[axis] = step(self.pos, axis, hop)
        return {'fsdp': (p['z'] * RING + p['y']) * RING + p['x'], 'cp': self.core}

    def peer(self):
        return {'fsdp': lax.axis_index('fsdp'), 'cp': 1 - self.core}

    def aside(self, dy, dx):
        return {'fsdp': (self.pos['z'] * RING + step(self.pos, 'y', dy)) * RING + step(self.pos, 'x', dx), 'cp': self.core}

    def announce(self, corners=()):
        sem = pltpu.get_barrier_semaphore()
        for axis in AXES:
            for hop in (1, DUO, TRIO):
                pl.semaphore_signal(sem, inc=1, device_id=self.far(axis, hop), device_id_type=MESH)
        for dy, dx in corners:
            pl.semaphore_signal(sem, inc=1, device_id=self.aside(dy, dx), device_id_type=MESH)
        pl.semaphore_signal(sem, inc=1, device_id=self.peer(), device_id_type=MESH)

    def meet(self, corners=()):
        pl.semaphore_wait(pltpu.get_barrier_semaphore(), 10 + len(corners))

    def ring(self, batch, src, slots, axis):
        for hop in (1, DUO, TRIO):
            batch.send(src, slots.at[hop], self.far(axis, hop))

    def local(self, src, dst):
        i = self.used_local
        self.used_local += 1
        c = pltpu.make_async_copy(src, dst, self.sems[DUO].at[i])
        c.start()
        return c

    def store(self, src, dst):
        self.stored.append(self.local(src, dst))


class Singles(Comm):
    def __init__(self, *sems):
        super().__init__(*sems)
        self.sent, self.exchanged = [], []

    def _copy(self, src, dst, device):
        i = self.used
        self.used += 1
        c = pltpu.make_async_remote_copy(src_ref=src, dst_ref=dst, send_sem=self.sems[0].at[i], recv_sem=self.sems[1].at[i], device_id=device, device_id_type=MESH)
        c.start()
        return c

    def send(self, src, dst, device):
        c = self._copy(src, dst, device)
        self.sent.append(c)
        return c

    def trade(self, src, dst):
        self.exchanged.append(self._copy(src, dst, self.peer()))


def pick(ref, sel, piece):
    lo, cols, first, rows = piece
    return ref.at[sel['z'], sel['y'], sel['x'], pl.ds(first, rows), pl.ds(lo, cols)]


def sem_scratch(remote, local):
    return [pltpu.SemaphoreType.DMA((remote,)), pltpu.SemaphoreType.DMA((remote,)), pltpu.SemaphoreType.DMA((local,))]


def add_into(dst, *srcs, fresh=False):
    def add(idx):
        total, *rest = [s[idx] for s in (srcs if fresh else (dst,) + srcs)]
        for more in rest:
            total = total + more
        dst[idx] = total

    if len(dst.shape) > TRIO:
        @pl.loop(0, dst.shape[0])
        def _(i):
            add((i,))
    else:
        add(Ellipsis)


def halves(lo, n):
    return (lo, n, 0, SHARE), (lo, n, SHARE, SHARE)


GROUPS = (halves(0, 384), halves(384, 384), halves(768, 384))
QK_FIRST = (halves(0, PAIR), halves(384, PAIR), halves(768, PAIR))
QK_LAST = (halves(PAIR, LANES), halves(640, LANES), halves(1024, LANES))
TOKENS = 1024
DIM = 2048
HALF = 1024
QKV = 1280
GROUP = 1152


def scope(name):
    return jax.named_scope(name)


def dot(a, b):
    return jnp.dot(a, b, preferred_element_type=jnp.float32)


def dot_nt(a, b):
    return lax.dot_general(a, b, (((1,), (1,)), ((), ())), preferred_element_type=jnp.float32)


def tile_at(i, n):
    return pl.ds(pl.multiple_of(i * n, n), n)


class Gather:
    def __init__(self, comm, ref, colors, land, held=None):
        self.comm, self.ref, self.colors, self.land = comm, ref, colors, land
        self.held = list(held or [dict(comm.pos) for _ in colors])
        self.spent = []

    def move(self, batch, s, piece, to):
        batch.send(pick(self.ref, s, piece), pick(self.ref, s, piece), to)

    def at(self, k, hop):
        d = ORDERS[k][self.phase]
        return dict(self.held[k], **{d: step(self.comm.pos, d, hop)})

    def begin(self, phase):
        self.phase = phase
        self.rest = Batch(self.comm)
        if phase == 0:
            for hop in (DUO, 1, TRIO):
                for k, (a, _) in enumerate(self.colors):
                    self.move(self.rest, self.held[k], (a[0], a[1], 0, CHIP), self.comm.far(ORDERS[k][0], hop))
            return
        self.up, self.dn = ([Batch(self.comm) for _ in range(TRIO)] for _ in range(DUO))
        for k, (a, b) in enumerate(self.colors):
            d = ORDERS[k][phase]
            up, dn, s = self.comm.far(d, 1), self.comm.far(d, TRIO), self.held[k]
            self.move(self.up[k], s, a, up)
            self.move(self.dn[k], s, b, dn)
            self.move(self.rest, s, b, up)
            self.move(self.rest, s, a, dn)
        if phase == DUO:
            for k, pieces in enumerate(self.colors):
                for piece in pieces:
                    self.land(self.ref, self.held[k], piece)

    def forward(self):
        for k, (a, b) in enumerate(self.colors):
            d = ORDERS[k][self.phase]
            for batch, hop, piece, to in ((self.up[k], TRIO, a, 1), (self.dn[k], 1, b, TRIO)):
                s = self.at(k, hop)
                batch.arrived(pick(self.ref, s, piece))
                self.move(self.rest, s, piece, self.comm.far(d, to))
                if self.phase == DUO:
                    self.land(self.ref, s, piece)
                self.spent.append((batch, pick(self.ref, self.held[k], piece)))

    def end(self):
        axis = ORDERS[0][self.phase]
        blocks = dict(self.held[0], **{axis: pl.ds(0, DUO if self.phase else TRIO)})
        width = sum(a[1] for a, _ in self.colors)
        whole = pick(self.ref, blocks, (0, width, 0, CHIP))
        self.rest.arrived(whole)
        self.spent.append((self.rest, whole))
        for k, (a, b) in enumerate(self.colors):
            if self.phase == DUO:
                for hop, piece in ((TRIO, b), (1, a), (DUO, a), (DUO, b)):
                    self.land(self.ref, self.at(k, hop), piece)
            self.held[k] = dict(self.held[k], **{ORDERS[k][self.phase]: ALL})

    def finish(self):
        for batch, whole in self.spent:
            batch.sent(whole)


def head_kernel(hidden, dy, wq, wk, wv, wo, pos, gain_in, cos_t, sin_t,
                qt_o, dot_o, k_o, kt_o, v_o, vt_o, rt_o, dyc_o, wqk_o, wqkp_o, wvo_o, wvop_o, gain_o,
                hid2, dy2, dys, rs, rt, wqk, wvo, wpeer, pi, pos2, qt, dot_s, kk, kt, vv, vt, cosines, sines, gain, gtile, gbuf, gx, gy, gz, *sems):
    comm = Comm(*sems)
    comm.announce()
    pos_c, core = comm.pos, comm.core
    bf16, f32 = jnp.bfloat16, jnp.float32
    peer = comm.peer()
    rows = tile_at(core, SHARE)
    mine_qk = wqk.at[pos_c['z'], pos_c['y'], pos_c['x'], rows]
    mine_vo = wvo.at[pos_c['z'], pos_c['y'], pos_c['x'], rows]

    def weight_parts(c):
        return ((wq.at[:, tile_at(c, HALF)], mine_qk.at[:, pl.ds(0, HALF)]), (wk.at[:, tile_at(c, LANES)], mine_qk.at[:, pl.ds(HALF, LANES)]),
                (wv.at[:, tile_at(c, LANES)], mine_vo.at[:, pl.ds(0, LANES)]), (wo.at[:, tile_at(c, HALF)], mine_vo.at[:, pl.ds(LANES, HALF)]))

    loads = [comm.local(s, d) for s, d in weight_parts(core)]
    load_x = [comm.local(hidden, hid2.at[pl.ds(0, ROWS)]), comm.local(dy, dy2.at[pl.ds(0, ROWS)])]
    share = lax.broadcasted_iota(jnp.int32, (SUBS, LANES), 1) // SHARE
    gtile[...] = jnp.where(share == pos_c['x'] * DUO + core, jnp.broadcast_to(jnp.concatenate([gain_in[...]] * SUBS, axis=1), (SUBS, LANES)), 0.0)
    with scope('entry'):
        comm.meet()
    swap_w, swap_pos, swap_dy, swap_x, peers_qk, peers_vo = (Batch(comm) for _ in range(6))
    gain_c, gain_x, gain_y, gain_z = (Batch(comm) for _ in range(RING))
    for s, d in weight_parts(1 - core):
        swap_w.send(s, d, peer)
    gain_c.send(gtile, gbuf, peer)
    swap_pos.send(pos, pos2, peer)
    for c in loads:
        c.wait()
    with scope('wait_w'):
        swapped = wqk.at[pos_c['z'], pos_c['y'], pos_c['x']]
        swap_w.arrived(swapped)

    def land_qk(ref, s, cols):
        peers_qk.send(pick(ref, s, cols), pick(wqkp_o, s, cols), peer)

    def land_vo(ref, s, cols):
        peers_vo.send(pick(ref, s, cols), pick(wpeer, s, cols), peer)

    g1 = Gather(comm, wvo, GROUPS, land_vo)
    g2 = Gather(comm, wqk, GROUPS, land_qk)
    g1.begin(0)
    g2.begin(0)
    gain_c.arrived(gbuf)
    gx[0] = gtile[...] + gbuf[...]
    comm.ring(gain_x, gx.at[0], gx, 'x')

    swap_pos.arrived(pos2)

    @pl.loop(0, TOKENS // LANES)
    def _(i):
        want = lax.broadcasted_iota(jnp.int32, (LANES, ROWS), 0) + i * LANES
        for h, have in enumerate((pos, pos2)):
            pi[tile_at(i, LANES), h * ROWS:(h + 1) * ROWS] = jnp.where(want == have[...], 1.0, 0.0).astype(bf16)

    for i in range(RING):
        r = slice(i * PAIR, (i + 1) * PAIR)
        cos, sin = cos_t[:, r], sin_t[:, r]
        cosines[r, :] = jnp.concatenate([cos, cos], axis=0).T
        sines[r, :] = jnp.concatenate([-sin, sin], axis=0).T

    def sort(dst, src, first, last):
        with scope('sort'):
            @pl.loop(first, last)
            def _(j):
                c = tile_at(j, PAIR)
                dst[:, c] = dot(pi[...], src[:, c]).astype(bf16)

    swap_dy.send(dy, dy2.at[pl.ds(ROWS, ROWS)], peer)
    with scope('p0_end'):
        for g in (g1, g2):
            g.end()
            g.begin(1)
    swap_x.send(hidden, hid2.at[pl.ds(ROWS, ROWS)], peer)
    gain_x.arrived(gx.at[pl.ds(1, TRIO)])
    gy[pos_c['y']] = (gx[0] + gx[1]) + (gx[DUO] + gx[TRIO])
    for hop in (1, DUO, TRIO):
        gain_y.send(gy.at[pos_c['y']], gy.at[pos_c['y']], comm.far('y', hop))
    with scope('wait_dy'):
        load_x[1].wait()
        swap_dy.arrived(dy2.at[pl.ds(ROWS, ROWS)])
    sort(dys, dy2, 0, RING)
    with scope('p1a_fwd'):
        g1.forward()
    sort(dys, dy2, RING, 6)
    with scope('p1b_fwd'):
        g2.forward()
    sort(dys, dy2, 6, SUBS)
    with scope('p1a_end'):
        g1.end()
    gain_y.arrived(gy.at[pl.ds(1, TRIO)])
    for j in range(RING):
        gz[pos_c['z'], j] = gy[j]
    for hop in (1, DUO, TRIO):
        gain_z.send(gz.at[pos_c['z']], gz.at[pos_c['z']], comm.far('z', hop))
    g1.begin(DUO)
    comm.store(dys.at[:, tile_at(core, HALF)], dyc_o)
    with scope('p1b_end'):
        g2.end()
    with scope('wait_x'):
        load_x[0].wait()
        swap_x.arrived(hid2.at[pl.ds(ROWS, ROWS)])
    sort(rs, hid2, 0, SUBS)
    with scope('p2q_fwd'):
        g1.forward()
    g2a, g2b = (Gather(comm, wqk, colors, land_qk, g2.held) for colors in (QK_FIRST, QK_LAST))
    g2a.begin(DUO)
    with scope('gain'):
        gain_z.arrived(gz.at[pl.ds(1, TRIO)])
    for i in range(RING):
        for j in range(RING):
            gain[:, (i * RING + j) * LANES:(i * RING + j + 1) * LANES] = gz[i, j]
    comm.store(gain, gain_o)

    def norm(first, last):
        with scope('norm'):
            @pl.loop(first, last)
            def _(i):
                r = tile_at(i, CHIP)
                x = rs[r, :].astype(f32)
                inv = lax.rsqrt(jnp.mean(x * x, axis=-1, keepdims=True) + RMS_EPS)
                rs[r, :] = (x * inv * gain[0:1, :]).astype(bf16)

    norm(0, TOKENS // CHIP)
    with scope('r_t'):
        @pl.loop(0, DIM // PAIR)
        def _(i):
            c = tile_at(i, PAIR)

            @pl.loop(0, TOKENS // PAIR)
            def _(j):
                r = tile_at(j, PAIR)
                rt[c, r] = rs[r, c].T
    comm.store(rt, rt_o)
    with scope('p2o_end'):
        g1.end()
    w_qk, w_vo, w_peer = wqk.reshape(DIM, GROUP), wvo.reshape(DIM, GROUP), wpeer.reshape(DIM, GROUP)
    with scope('vals'):
        @pl.loop(0, DUO)
        def _(i):
            r = tile_at(i, ROWS)
            val = dot(rs[r, :], w_vo[:, :LANES]).astype(bf16)
            vv[r, :] = val
            vt[:, r] = val.T
    for src, dst in ((wvo, wvo_o), (vv, v_o), (vt, vt_o)):
        comm.store(src, dst)
    with scope('p2q_fwd'):
        g2a.forward()
    g2b.begin(DUO)
    with scope('wo_peer'):
        peers_vo.arrived(wpeer)
    comm.store(wpeer, wvop_o)
    with scope('do_t'):
        mine = tile_at(core, HALF)

        @pl.loop(0, TOKENS // PAIR)
        def _(j):
            t = tile_at(j, PAIR)
            w_rows = jnp.concatenate([w_vo[mine, LANES:], w_peer[mine, LANES:]], axis=1)
            d_rows = jnp.concatenate([dys[t, mine], dys[t, tile_at(1 - core, HALF)]], axis=1)
            dot_s[:, t] = dot_nt(w_rows, d_rows).astype(bf16)
    comm.store(dot_s, dot_o)

    def rotated(x, r):
        return (x * cosines[r, :] + pltpu.roll(x, TURN, 1) * sines[r, :]).astype(bf16)

    def queries(columns, heads):
        for i in range(DUO):
            r = slice(i * ROWS, (i + 1) * ROWS)
            x = dot(rs[r, :], columns)
            for h, head in enumerate(heads):
                qt[tile_at(head, LANES), r] = rotated(x[:, h * LANES:(h + 1) * LANES], r).T

    with scope('p2q_end'):
        g2a.end()

    with scope('last_fwd'):
        g2b.forward()
    with scope('q'):
        for t in range(TRIO):
            queries(w_qk[:, t * 384:t * 384 + PAIR], (TRIO * t, TRIO * t + 1))
    for t in range(TRIO):
        two_heads = pl.ds(t * 384, PAIR)
        comm.store(qt.at[two_heads], qt_o.at[two_heads])
    with scope('last_end'):
        g2b.end()
    comm.store(wqk, wqk_o)
    with scope('q_last'):
        last = jnp.concatenate([w_qk[:, PAIR:384], w_qk[:, 640:768], w_qk[:, HALF:]], axis=1)
        for i in range(DUO):
            r = slice(i * ROWS, (i + 1) * ROWS)
            x = dot(rs[r, :], last)
            for h, head in enumerate((DUO, 5)):
                qt[tile_at(head, LANES), r] = rotated(x[:, h * LANES:(h + 1) * LANES], r).T
            key = rotated(x[:, PAIR:], r)
            kk[r, :] = key
            kt[:, r] = key.T
    for src, dst in ((kk, k_o), (kt, kt_o)) + tuple((qt.at[tile_at(h, LANES)], qt_o.at[tile_at(h, LANES)]) for h in (DUO, 5)):
        comm.store(src, dst)
    with scope('finish'):
        peers_qk.arrived(wqk)
        for batch, whole in ((swap_w, swapped), (swap_pos, pos2), (swap_dy, dy2.at[pl.ds(ROWS, ROWS)]), (swap_x, hid2.at[pl.ds(ROWS, ROWS)]), (peers_qk, wqk), (peers_vo, wvo),
                             (gain_c, gbuf), (gain_x, gx.at[pl.ds(1, TRIO)]), (gain_y, gy.at[pl.ds(1, TRIO)]), (gain_z, gz.at[pl.ds(1, TRIO)])):
            batch.sent(whole)
        for g in (g1, g2, g2a, g2b):
            g.finish()
        for c in comm.stored:
            c.wait()


def head(hidden, dy, wq, wk, wv, wo, pos, gain, cos_t, sin_t):
    bf16, f32 = jnp.bfloat16, jnp.float32
    any_ = pl.BlockSpec(memory_space=pl.ANY)
    vmem = pl.BlockSpec(memory_space=pltpu.VMEM)
    S = lambda shape, d=bf16: jax.ShapeDtypeStruct(shape, d)
    V = lambda shape, d=bf16: pltpu.VMEM(shape, d)
    group = (RING, RING, RING, CHIP, GROUP)
    sq, tall, wide = (HALF, TOKENS), (TOKENS, LANES), (LANES, TOKENS)
    full = (TOKENS, DIM)
    return pl.pallas_call(
        head_kernel,
        out_shape=[S(sq), S(sq), S(tall), S(wide), S(tall), S(wide), S((DIM, TOKENS)), S((TOKENS, HALF)), S(group), S(group), S(group), S(group), S((SUBS, DIM), f32)],
        in_specs=[any_] * 6 + [vmem] * RING,
        out_specs=[any_] * 13,
        scratch_shapes=[V(full), V(full), V(full), V(full), V((DIM, TOKENS)), V(group), V(group), V(group), V((TOKENS, TOKENS)), V((1, ROWS), jnp.int32),
                        V(sq), V(sq), V(tall), V(wide), V(tall), V(wide), V(tall, f32), V(tall, f32), V((SUBS, DIM), f32), V((SUBS, LANES), f32), V((SUBS, LANES), f32), V((RING, SUBS, LANES), f32), V((RING, SUBS, LANES), f32), V((RING, RING, SUBS, LANES), f32)] + sem_scratch(47, 22),
        compiler_params=pltpu.CompilerParams(collective_id=0, has_side_effects=True, vmem_limit_bytes=60 * DUO**20),
        name='head',
    )(hidden, dy, wq, wk, wv, wo, pos, gain, cos_t, sin_t)


HEADS = SUBS
UNIT_K, UNIT_V = SUBS, 9
N_UNITS = 18
GAIN = N_UNITS
SLOTS = RING
LAST = 5
ABREAST = DUO
LINES = ((0, TRIO, 6, 9, 12, 15), (1, RING, 7, 10, 13, SHARE), (DUO, 5, SUBS, 11, 14, 17))
COLOR = {u: k for k, line in enumerate(LINES) for u in line}
RANK = {u: i for line in LINES for i, u in enumerate(line)}
SWAPPED = (1, TRIO, RING, SUBS, 10)
ORDER = {u: ORDERS[k] if u not in SWAPPED else (ORDERS[k][0], ORDERS[k][DUO], ORDERS[k][1]) for u, k in COLOR.items()}
BEFORE = {u: line[i - SLOTS] if i >= SLOTS else None for line in LINES for i, u in enumerate(line)}
PLACES = 12
PLACE = {u: u % PLACES for u in range(N_UNITS)}
WIRE = (2.82, 0.71, 0.36)
LATENCY = 2.4
STAGE_COST = 0.08


class Plan:
    def __init__(self):
        self.now, self.stage, self.ready, self.order, self.link = 0.0, {}, {}, [], {}
        self.mark = {}

    def _wire(self, u, phase, count):
        link = ORDER[u][phase]
        t = max(self.link.get(link, 0.0), self.now)
        first = t + WIRE[phase] + LATENCY
        self.link[link] = t + WIRE[phase] * count
        return first if phase < DUO else self.link[link] + LATENCY

    def free(self, u, phase):
        if BEFORE[u] is None:
            return True
        done = self.mark.get((BEFORE[u], (DUO, RING, 5)[phase]))
        if done is None:
            return False
        sent = ((0, 1), (DUO, TRIO), (RING,))[phase]
        return any(self.mark.get((j, s), -1) > done and (j, s + 1) in self.mark for j, order in ORDER.items() if order[phase] == ORDER[u][phase] for s in sent)

    def run(self, u):
        stage = self.stage[u]
        self.order.append((u, stage))
        self.mark[u, stage] = len(self.order)
        self.now = max(self.now, self.ready[u]) + STAGE_COST
        self.stage[u] = stage + 1
        if stage == (TRIO if u == GAIN else LAST):
            del self.stage[u]
        elif u == GAIN:
            self.ready[u] = max([self.now] + [self.link.get(a, 0.0) for a in ('', 'z', 'xy')[stage]]) + DUO * LATENCY
        elif stage % DUO:
            self.ready[u] = self._wire(u, stage // DUO, 1)
        else:
            self.ready[u] = self._wire(u, stage // DUO, DUO)

    def blocked(self, u):
        stage = self.stage[u]
        if u == GAIN:
            return False
        if stage == 0 and sum(0 < self.stage.get(j, 0) <= DUO for j in LINES[COLOR[u]]) >= ABREAST:
            return True
        if stage == DUO and BEFORE[u] is not None and (BEFORE[u], LAST) not in self.mark:
            return True
        return stage in (0, DUO, RING) and not self.free(u, stage // DUO)

    def start(self, u):
        self.stage[u], self.ready[u] = 0, self.now

    def due(self):
        first = len(self.order)
        while True:
            ripe = [(self.ready[u], u) for u in self.stage if self.ready[u] <= self.now and not self.blocked(u)]
            if not ripe:
                return self.order[first:]
            self.run(min(ripe)[1])

    def vacated(self, u):
        return (u, DUO) in self.mark

    def rush(self, done):
        first = len(self.order)
        while not done():
            self.run(min((self.ready[u], u) for u in self.stage if not self.blocked(u))[1])
        return self.order[first:]


QB = PAIR
PAIRS = HEADS // DUO
NBLK = TOKENS // QB
HALVES = (pl.ds(0, SHARE), pl.ds(SHARE, SHARE))
PLANE = tuple((dy, dx) for dy in range(RING) for dx in range(RING) if dy or dx)
CORNERS = tuple((dy, dx) for dy, dx in PLANE if dy and dx)


class Scatter:
    def __init__(self, comm, part, mid, bufs, fin, outs, send_sems, recv_sems, swap_sems):
        self.pos, self.part, self.mid, self.bufs, self.fin, self.outs = comm.pos, part, mid, bufs, fin, outs
        self.send_sems, self.recv_sems, self.swap_sems = send_sems, recv_sems, swap_sems
        self.near = {(a, hop): comm.far(a, hop) for a in AXES for hop in (1, DUO, TRIO)}
        self.hops = {(a, hop): step(comm.pos, a, hop) for a in AXES for hop in (1, DUO, TRIO)}
        self.peer, self.core = comm.peer(), comm.core
        self.keep, self.give = tile_at(comm.core, SHARE), tile_at(1 - comm.core, SHARE)
        self.drained, self.done = set(), []

    def slot(self, u):
        return COLOR[u], RANK[u] % SLOTS

    def buf(self, u, phase):
        return self.bufs[phase].at[self.slot(u)]

    def view(self, u, phase, hop, half=None):
        order = ORDER[u]
        at = {a: ALL for a in AXES}
        for a in order[1:phase]:
            at[a] = self.pos[a]
        at[order[phase]] = self.hops[order[phase], hop] if hop else self.pos[order[phase]]
        rows = pl.ds(0, CHIP) if half is None else HALVES[half]
        if phase == 0:
            return self.part.at[PLACE[u], at['z'], at['y'], at['x'], rows, :]
        return self.mid.at[self.slot(u) + tuple(at[a] for a in 'zyx' if a != order[0]) + (rows, slice(None))]

    def copy(self, src, dst, sems, device):
        return pltpu.make_async_remote_copy(src_ref=src, dst_ref=dst, send_sem=sems[0], recv_sem=sems[1], device_id=device, device_id_type=MESH)

    def sems(self, u, phase, kind=0):
        k, i = self.slot(u)
        at = (k * SLOTS + i) * TRIO + phase
        return self.send_sems.at[at], self.recv_sems.at[(k * SLOTS + i) * 5 + DUO * phase + kind]

    def send(self, u, phase, name):
        axis = ORDER[u][phase]
        if phase == DUO:
            src, to = self.view(u, DUO, name + 1), name + 1
        else:
            hop, half, to = ((DUO, 0, 1), (DUO, 1, TRIO), (1, 1, 1), (TRIO, 0, TRIO), (1, 0, 1), (TRIO, 1, TRIO))[name]
            src = self.view(u, phase, hop, half)
        self.copy(src, self.buf(u, phase).at[name], self.sems(u, phase, int(name > 1 and phase < DUO)), self.near[axis, to]).start()

    def launch(self, u, phase):
        if BEFORE[u] is not None:
            self.drain(BEFORE[u], phase)
        for name in range(RING if phase < DUO else TRIO):
            self.send(u, phase, name)

    def arrived(self, u, phase, first, count):
        whole = self.buf(u, phase).at[pl.ds(first, count)]
        self.copy(whole, whole, self.sems(u, phase, int(first > 0)), self.peer).wait_recv()

    def drain(self, u, phase):
        if (u, phase) not in self.drained:
            self.drained.add((u, phase))
            whole = self.buf(u, phase)
            self.copy(whole, whole, self.sems(u, phase), self.peer).wait_send()

    def out(self, u):
        if u < HEADS:
            out, col = self.outs[0], self.core * HALF + u * LANES
        elif u < 10:
            out, col = self.outs[u - 7], self.core * LANES
        else:
            out, col = self.outs[TRIO], self.core * HALF + (u - 10) * LANES
        return out.at[:, pl.ds(pl.multiple_of(col, LANES), LANES)]

    def kept(self, u, turn):
        return pltpu.make_async_copy(self.fin.at[u, self.keep], self.out(u), self.swap_sems.at[DUO + turn])

    def run(self, u, stage):
        if stage == 0:
            return self.launch(u, 0)
        phase = (stage - 1) // DUO
        if stage == LAST:
            self.arrived(u, DUO, 0, TRIO)
            got = self.buf(u, DUO)
            self.fin[u] = self.view(u, DUO, 0)[...] + (got[0] + got[1] + got[DUO])
            self.copy(self.fin.at[u, self.give], self.out(u), (self.swap_sems.at[0], self.swap_sems.at[1]), self.peer).start()
            turn = len(self.done) % DUO
            if len(self.done) > 1:
                self.kept(self.done[-DUO], turn).wait()
            self.kept(u, turn).start()
            self.done.append(u)
            return
        got = self.buf(u, phase)
        if stage % DUO:
            self.arrived(u, phase, 0, DUO)
            for name, hop in ((0, 1), (1, TRIO)):
                add_into(self.view(u, phase, hop, name), got.at[name])
                self.send(u, phase, name + RING)
            return
        self.arrived(u, phase, DUO, RING)
        if phase == 0 and BEFORE[u] is not None:
            self.drain(BEFORE[u], 1)
            self.drain(BEFORE[u], DUO)
        for half, names in ((0, (TRIO, RING)), (1, (DUO, 5))):
            if phase:
                add_into(self.view(u, phase, 0, half), *[got.at[name] for name in names])
            else:
                dst = self.mid.at[self.slot(u) + (ALL, ALL, HALVES[half], slice(None))]
                add_into(dst, self.view(u, 0, 0, half), *[got.at[name] for name in names], fresh=True)
        self.launch(u, phase + 1)

    def finish(self):
        for u in range(N_UNITS):
            for phase in range(TRIO):
                self.drain(u, phase)
        half = self.fin.at[:, pl.ds(0, SHARE)]
        swaps = self.copy(half, half, (self.swap_sems.at[0], self.swap_sems.at[1]), self.peer)
        swaps.wait_send()
        swaps.wait_recv()
        for turn in range(DUO):
            self.kept(self.done[turn - DUO], turn).wait()


def attend(heads, qt, do_t, k, kt, v, vt, cos, sin, o_row, ot, dq, dkt, dvt, s_scr, e_scr, p_scr, d_scr):
    f32, bf16 = jnp.float32, jnp.bfloat16
    strip = TURN
    work = [(h, j) for j in range(NBLK) for h in range(len(heads))]

    def strips(c):
        return [(i * strip, slice(c * QB + i * strip, c * QB + (i + 1) * strip)) for i in range(QB // strip)]

    def fold(x, op):
        return op(x.reshape(strip // SUBS, SUBS, QB), axis=0)

    def scores(i):
        (h, j), b = work[i], i % DUO
        q_t = qt[heads[h], j * QB:(j + 1) * QB]
        top = jnp.full((SUBS, QB), -jnp.inf, f32)
        for c in range(j + 1):
            tile = dot(k[c * QB:(c + 1) * QB, :], q_t)
            for at, rows in strips(c):
                s = tile[at:at + strip]
                if c == j:
                    seen = lax.broadcasted_iota(jnp.int32, (strip, QB), 0) + at <= lax.broadcasted_iota(jnp.int32, (strip, QB), 1)
                    s = jnp.where(seen, s, -jnp.inf)
                s_scr[b, rows, :] = s
                top = jnp.maximum(top, fold(s, jnp.max))
        return jnp.max(top, axis=0, keepdims=True)

    def rest(i, m):
        (h, j), b = work[i], i % DUO
        cols, n = slice(j * QB, (j + 1) * QB), (j + 1) * QB
        q_t, d_t = qt[heads[h], cols], do_t[heads[h], cols]
        tot = jnp.zeros((SUBS, QB), f32)
        for c in range(j + 1):
            for at, rows in strips(c):
                e = jnp.exp2((s_scr[b, rows, :] - m) * (SCALE * LOG2E))
                s_scr[b, rows, :] = e
                e_scr[b, rows, :] = e.astype(bf16)
                tot = tot + fold(e, jnp.sum)
        den = jnp.sum(tot, axis=0, keepdims=True)
        inv = 1.0 / den
        o = (dot(vt[:, :n], e_scr[b, :n, :]) / den).astype(bf16)
        ot[o_row(h), cols] = o
        delta = jnp.sum(d_t.astype(f32) * o.astype(f32), axis=0, keepdims=True)
        for c in range(j + 1):
            dp = dot(v[c * QB:(c + 1) * QB, :], d_t)
            for at, rows in strips(c):
                p = s_scr[b, rows, :] * inv
                p_scr[b, rows, :] = p.astype(bf16)
                d_scr[b, rows, :] = (p * (dp[at:at + strip] - delta)).astype(bf16)
        dvt[:, :n] += dot_nt(d_t, p_scr[b, :n, :])
        dkt[:, :n] += dot_nt(q_t, d_scr[b, :n, :])
        g = dot(kt[:, :n], d_scr[b, :n, :]) * SCALE
        co, si = cos[:, cols], sin[:, cols]
        x, y = g[:TURN], g[TURN:]
        dq[heads[h], cols] = jnp.concatenate([x * co + y * si, y * co - x * si], axis=0).astype(bf16)

    m = scores(0)
    for i in range(len(work)):
        later = scores(i + 1) if i + 1 < len(work) else None
        rest(i, m)
        m = later


def tail_kernel(qt, do_t, k, kt, v, vt, rt, dyc, wqk, wqkp, wvo, wvop, gain, hidden, dy, pos, cos, sin,
                result, grad_x, gq, gk, gv, go, gout,
                two, ks, kts, vs, vts, rts, ots, dqo, dqp, dkvo, dkvp, dkt, dvt, s_scr, e_scr, p_scr, d_scr, dycs, part, mid, buf1, buf2, buf3, fin, own, onat, dnat, xs, gacc, gpart, gpeer, gz, gx,
                send_sems, recv_sems, swap_sems, trade_send, trade_recv, local_sems):
    comm = Singles(trade_send, trade_recv, local_sems)
    comm.used = HEADS
    f32, bf16 = jnp.float32, jnp.bfloat16
    core, peer = comm.core, comm.peer()
    a1, a2 = two.at[0], two.at[1]
    sc = Scatter(comm, part, mid, (buf1, buf2, buf3), fin, (gq, gk, gv, go), send_sems, recv_sems, swap_sems)
    plan = Plan()
    some, most = pl.ds(0, PAIR), pl.ds(PAIR, HALF - PAIR)
    loads = [comm.local(s, d) for s, d in ((qt.at[some], two.at[0, some]), (k, ks), (do_t.at[some], two.at[1, some]), (vt, vts), (v, vs), (kt, kts))]
    comm.announce(CORNERS)
    dkt[...] = jnp.zeros_like(dkt)
    dvt[...] = jnp.zeros_like(dvt)
    with scope('wait_q'):
        for c in loads:
            c.wait()
    loads = [comm.local(s, d) for s, d in ((rt, rts), (qt.at[most], two.at[0, most]), (do_t.at[most], two.at[1, most]))]
    later = [comm.local(s, d) for s, d in ((dyc, dycs), (hidden, xs))]

    def emit(stages):
        for u, stage in stages:
            with scope(f'u{u}_s{stage}'):
                if u == GAIN:
                    sum_gain(stage)
                else:
                    sc.run(u, stage)

    def after(cost):
        plan.now += cost
        return plan.due()

    def head_trades(g):
        row = pl.ds(pl.multiple_of((core * HEADS + DUO * g) * LANES, PAIR), PAIR)
        mine = tile_at(g, PAIR)
        return [pltpu.make_async_remote_copy(src_ref=s, dst_ref=d, send_sem=trade_send.at[i], recv_sem=trade_recv.at[i], device_id=peer, device_id_type=MESH)
                for s, d, i in ((ots.at[row], ots.at[row], g), (dqo.at[mine], dqp.at[mine], PAIRS + g))]

    def gradient(place, count, left, right, mul):
        with scope('grad'):
            @pl.loop(0, DUO)
            def _(z):
                g = mul(left[tile_at(z, HALF), :], right())
                for i in range(count):
                    part[place + i, tile_at(z, DUO)] = g[:, i * LANES:(i + 1) * LANES].reshape(DUO, RING, RING, CHIP, LANES)

    attended, paired = [], []
    for g in range(PAIRS):
        attended.append(after(5.1))
        plan.now += 1.5
        plan.start(DUO * g)
        plan.start(DUO * g + 1)
        paired.append(plan.due())

    @pl.loop(0, PAIRS)
    def _(g):
        def at(table):
            for i in range(PAIRS):
                if table[i]:
                    pl.when(g == i)(functools.partial(emit, table[i]))

        heads = [tile_at(DUO * g + i, LANES) for i in range(DUO)]
        with scope('attend'):
            attend(heads, a1, a2, ks, kts, vs, vts, cos, sin, lambda i: tile_at(core * HEADS + DUO * g + i, LANES), ots, dqo, dkt, dvt, s_scr, e_scr, p_scr, d_scr)

        @pl.when(g == 0)
        def _():
            with scope('entry'):
                comm.meet(CORNERS)
                for c in loads:
                    c.wait()
        for c in head_trades(g):
            c.start()
        at(attended)
        gradient(DUO * g, DUO, rts, lambda: dqo[tile_at(g, PAIR), :], dot_nt)
        at(paired)

    def beat(cost, *starts):
        plan.now += cost
        for u in starts:
            plan.start(u)
        emit(plan.due())

    wkv, wkvp = e_scr.reshape(DIM, PAIR), p_scr.reshape(DIM, PAIR)
    later += [comm.local(src.at[:, pl.ds(at, LANES)], dst.at[:, pl.ds(to, LANES)]) for srcs, dst in (((wqk, wvo), wkv), ((wqkp, wvop), wkvp)) for src, at, to in ((srcs[0], HALF, 0), (srcs[1], 0, LANES))]
    wqp_loads = [comm.local(wqkp.at[tile_at(i, HALF), pl.ds(0, HALF)], two.at[i]) for i in range(DUO)]
    key = dkt[...] * SCALE
    co, si, x, y = cos[...], sin[...], key[:TURN], key[TURN:]
    dkvo[:LANES, :] = jnp.concatenate([x * co + y * si, y * co - x * si], axis=0).astype(bf16)
    dkvo[LANES:, :] = dvt[...].astype(bf16)
    comm.trade(dkvo, dkvp)
    gradient(UNIT_K, DUO, rts, lambda: dkvo[...], dot_nt)
    beat(1.8, UNIT_K, UNIT_V)
    wq_load = comm.local(wqk.at[:, pl.ds(0, HALF)], rts)
    for c in later:
        c.wait()
    with scope('trades'):
        for g in range(PAIRS):
            for c in head_trades(g):
                c.wait()

    waiting = list(range(RING))

    def output_gradients(force=False):
        while waiting:
            first = 10 + DUO * waiting[0]
            before = [u for u in range(N_UNITS) if u < first and PLACE[u] in (PLACE[first], PLACE[first + 1])]
            if force:
                emit(plan.rush(lambda: all(map(plan.vacated, before))))
            if not all(map(plan.vacated, before)):
                return
            for u in before:
                sc.drain(u, 0)
            i = waiting.pop(0)
            gradient(PLACE[first], DUO, ots, lambda: dycs[:, i * PAIR:(i + 1) * PAIR], dot)
            plan.start(first)
            plan.start(first + 1)
            beat(1.5)

    def piece(cost):
        beat(cost)
        output_gradients()

    def ticking(n, cost, body):
        tables = [after(cost) for _ in range(n)]

        @pl.loop(0, n)
        def _(i):
            body(i)
            for j, table in enumerate(tables):
                if table:
                    pl.when(i == j)(functools.partial(emit, table))
        output_gradients()

    @pl.loop(0, TOKENS // LANES)
    def _(i):
        want = lax.broadcasted_iota(jnp.int32, (LANES, ROWS), 0) + i * LANES
        own[tile_at(i, LANES), :] = jnp.where(want == pos[...], 1.0, 0.0).astype(bf16)

    def unsort(at, src_t, n):
        with scope('unsort'):
            dnat[at:at + n, :] = dot(src_t[:n, :], own[...]).astype(bf16)

    output_gradients()
    for c in comm.exchanged:
        c.wait_recv()
    unsort(0, dqo, HALF)
    dy_loads = [comm.local(dy.at[:, tile_at(i, HALF)], dqo.at[tile_at(i, ROWS)]) for i in range(DUO)]
    piece(1.2)
    unsort(HALF, dqp, HALF)
    piece(1.2)
    unsort(DUO * HALF, dkvo, PAIR)
    unsort(DUO * HALF + PAIR, dkvp, PAIR)
    piece(0.7)
    wq_load.wait()
    for c in wqp_loads + dy_loads:
        c.wait()
    gacc[...] = jnp.zeros_like(gacc)

    def dr_parts(half, r):
        return [s_scr.at[half, r(i * PAIR), :] for i in range(RING)]

    def back(block, then):
        def dr(half):
            with scope('dr'):
                c = tile_at(half, HALF)
                left = jnp.concatenate([rts[c, :], two[half], wkv[c, :], wkvp[c, :]], axis=1)
                acc = dot(left, dnat[:, block * PAIR:(block + 1) * PAIR])
                for i, ref in enumerate(dr_parts(half, lambda at: pl.ds(at, PAIR))):
                    ref[...] = acc[i * PAIR:(i + 1) * PAIR, :].T

        def norm(part):
            with scope('back'):
                @pl.loop(0, RING)
                def _(i):
                    j = part * RING + i
                    q = pl.ds(pl.multiple_of(block * PAIR + j * SHARE, SHARE), SHARE)
                    d = jnp.concatenate([ref[...] for half in range(DUO) for ref in dr_parts(half, lambda at: pl.ds(pl.multiple_of(at + j * SHARE, SHARE), SHARE))], axis=1)
                    x = xs[q, :].astype(f32)
                    inv = lax.rsqrt(jnp.mean(x * x, axis=-1, keepdims=True) + RMS_EPS)
                    unit = x * inv
                    gacc[...] += jnp.sum((d * unit).reshape(DUO, SUBS, DIM), axis=0)
                    dg = d * gain[0:1, :]
                    new = inv * (dg - unit * jnp.mean(dg * unit, axis=-1, keepdims=True))
                    for half in range(DUO):
                        r = pl.ds(pl.multiple_of(half * ROWS + block * PAIR + j * SHARE, SHARE), SHARE)
                        dqo[r, :] = (dqo[r, :].astype(f32) + new[:, half * HALF:(half + 1) * HALF]).astype(bf16)

        ticking(DUO, 1.6, dr)
        then()
        ticking(RING, 0.92, norm)

    back(0, lambda: None)
    wo_loads = []
    back(1, lambda: wo_loads.extend([comm.local(wvo.at[:, pl.ds(LANES, HALF)], rts)] + [comm.local(wvop.at[tile_at(i, HALF), pl.ds(LANES, HALF)], two.at[i]) for i in range(DUO)]))
    for i in range(DUO):
        comm.store(dqo.at[tile_at(i, ROWS)], grad_x.at[:, tile_at(i, HALF)])
    total = jnp.sum(gacc[...], axis=0, keepdims=True)
    gpart[...] = jnp.zeros_like(gpart)
    for i in range(RING):
        for j in range(RING):
            gpart[i, j:j + 1, :] = total[:, (i * RING + j) * LANES:(i * RING + j + 1) * LANES]

    gain_c, gain_z, gain_p = (Batch(comm) for _ in range(TRIO))

    def sum_gain(stage):
        if stage == 0:
            gain_c.send(gpart, gpeer, peer)
        elif stage == 1:
            gain_c.arrived(gpeer)
            for j in range(RING):
                gz[j] = gpart[j] + gpeer[j]
            for hop in (1, DUO, TRIO):
                gain_z.send(gz.at[step(comm.pos, 'z', hop)], gz.at[TRIO + hop], comm.far('z', hop))
        elif stage == DUO:
            gain_z.arrived(gz.at[pl.ds(RING, TRIO)])
            gx[0] = (gz[comm.pos['z']] + gz[RING]) + (gz[5] + gz[6])
            for dy, dx in PLANE:
                gain_p.send(gx.at[0], gx.at[dy * RING + dx], comm.aside(dy, dx))
        else:
            gain_p.arrived(gx.at[pl.ds(1, 15)])
            gpeer[0] = jnp.sum(gx[...], axis=0)
            mine = jnp.broadcast_to(gpeer[0, pl.ds(comm.pos['y'], 1), :], (SUBS, LANES))
            gout[...] = pltpu.roll(mine, LANES - (comm.pos['x'] * CHIP + core * SHARE), 1)

    plan.start(GAIN)
    beat(0.2)
    for i in range(DUO):
        with scope('unsort_o'):
            @pl.loop(0, DUO)
            def _(j):
                r = pl.ds(pl.multiple_of(i * HALF + j * ROWS, ROWS), ROWS)
                onat[:, r] = dot(ots[r, :], own[...]).astype(bf16).T
        piece(1.58)
    output_gradients(True)

    def project_out(col, weights, i):
        with scope('project'):
            @pl.loop(DUO * i, DUO * i + DUO)
            def _(j):
                c = tile_at(j, PAIR)
                dst = pl.ds(pl.multiple_of(col + j * PAIR, PAIR), PAIR)
                xs[:, dst] = (xs[:, dst].astype(f32) + dot(onat[...], weights(c))).astype(bf16)
        beat(1.48)

    def own_half(c):
        return rts[:, c]

    def other_half(c):
        return jnp.concatenate([a1[:, c], a2[:, c]], axis=0)

    for c in wo_loads:
        c.wait()
    for col, weights in ((core * HALF, own_half), ((1 - core) * HALF, other_half)):
        for i in range(DUO):
            project_out(col, weights, i)
    comm.store(xs, result)
    emit(plan.rush(lambda: not plan.stage))
    with scope('finish'):
        sc.finish()
        for batch, whole in ((gain_c, gpart), (gain_z, gz.at[pl.ds(RING, TRIO)]), (gain_p, gx.at[pl.ds(1, 15)])):
            batch.sent(whole)
        for c in comm.exchanged:
            c.wait_send()
        for c in comm.stored:
            c.wait()


def tail(qt, do_t, k, kt, v, vt, rt, dyc, wqk, wqkp, wvo, wvop, gain, hidden, dy, pos, cos, sin):
    bf16, f32 = jnp.bfloat16, jnp.float32
    any_ = pl.BlockSpec(memory_space=pl.ANY)
    vmem = pl.BlockSpec(memory_space=pltpu.VMEM)
    S = lambda shape, d=bf16: jax.ShapeDtypeStruct(shape, d)
    V = lambda shape, d=bf16: pltpu.VMEM(shape, d)
    D = lambda n: pltpu.SemaphoreType.DMA((n,))
    sq, tall, wide = (HALF, TOKENS), (TOKENS, LANES), (LANES, TOKENS)
    mine, kv = (ROWS, DIM), (PAIR, TOKENS)
    return pl.pallas_call(
        tail_kernel,
        out_shape=[S(mine), S(mine), S((SHARE, DIM), f32), S((SHARE, PAIR), f32), S((SHARE, PAIR), f32), S((SHARE, DIM), f32), S((SUBS, LANES), f32)],
        in_specs=[any_] * 12 + [vmem] + [any_] * DUO + [vmem] * TRIO,
        out_specs=[any_] * 6 + [vmem],
        scratch_shapes=[V((DUO,) + sq), V(tall), V(wide), V(tall), V(wide), V((DIM, TOKENS)), V((DIM, TOKENS)), V(sq), V(sq), V(kv), V(kv), V(wide, f32), V(wide, f32),
                        V((DUO, TOKENS, QB), f32), V((DUO, TOKENS, QB)), V((DUO, TOKENS, QB)), V((DUO, TOKENS, QB)), V(sq), V((PLACES, RING, RING, RING, CHIP, LANES), f32), V((TRIO, SLOTS, RING, RING, CHIP, LANES), f32),
                        V((TRIO, SLOTS, 6, RING, RING, SHARE, LANES), f32), V((TRIO, SLOTS, 6, RING, SHARE, LANES), f32), V((TRIO, SLOTS, TRIO, CHIP, LANES), f32), V((N_UNITS, CHIP, LANES), f32), V((TOKENS, ROWS)), V(mine), V((DUO * QKV, ROWS)), V(mine),
                        V((SUBS, DIM), f32), V((RING, SUBS, LANES), f32), V((RING, SUBS, LANES), f32), V((7, SUBS, LANES), f32), V((SHARE, SUBS, LANES), f32),
                        D(9 * SLOTS), D(15 * SLOTS), D(RING), D(HEADS + RING), D(HEADS + RING), D(26)],
        compiler_params=pltpu.CompilerParams(collective_id=1, has_side_effects=True, vmem_limit_bytes=67043328),
        name='tail',
    )(qt, do_t, k, kt, v, vt, rt, dyc, wqk, wqkp, wvo, wvop, gain, hidden, dy, pos, cos, sin)


def settle_kernel(n, *refs):
    ins, gain, outs, gain_out, bufs, sems = refs[:n], refs[n], refs[n + 1:DUO * n + 1], refs[DUO * n + 1], refs[DUO * n + DUO:-1], refs[-1]
    jobs = []
    for a, o, b in zip(ins, outs, bufs):
        size = a.shape[0] // RING if a.shape[0] == ROWS else a.shape[0]
        jobs += [tuple(r.at[pl.ds(i, size)] for r in (a, b, o)) for i in range(0, a.shape[0], size)]
    takes = [pltpu.make_async_copy(a, b, sems.at[0, i]) for i, (a, b, _) in enumerate(jobs)]
    puts = [pltpu.make_async_copy(b, o, sems.at[1, i]) for i, (_, b, o) in enumerate(jobs)]
    for c in takes:
        c.start()
    gain_out[...] = gain[0:1, :SHARE]
    for take, put in zip(takes, puts):
        take.wait()
        put.start()
    for c in puts:
        c.wait()


def settle(*arrays):
    *large, gain = arrays
    any_, vmem = pl.BlockSpec(memory_space=pl.ANY), pl.BlockSpec(memory_space=pltpu.VMEM)
    return pl.pallas_call(
        functools.partial(settle_kernel, len(large)),
        out_shape=[jax.ShapeDtypeStruct(a.shape, a.dtype) for a in large] + [jax.ShapeDtypeStruct((1, SHARE), gain.dtype)],
        in_specs=[any_] * len(large) + [vmem],
        out_specs=[any_] * len(large) + [vmem],
        scratch_shapes=[pltpu.VMEM(a.shape, a.dtype) for a in large] + [pltpu.SemaphoreType.DMA((DUO, 12))],
        name='settle',
    )(*arrays)


def rope_tables():
    j = np.arange(HEAD_DIM // DUO, dtype=np.float64) / (HEAD_DIM // DUO)
    freq = (ROPE_THETA ** -j).astype(np.float32)
    angle = freq[:, None] * np.arange(TOKENS, dtype=np.float32)[None, :]
    return np.cos(angle.astype(np.float64)).astype(np.float32), np.sin(angle.astype(np.float64)).astype(np.float32)


def solution(mesh):
    def shard_fn(hidden, tok_pos, grad_out, norm_gain, w_query, w_key, w_value, w_out):
        hidden, grad_out = hidden[0], grad_out[0]
        cos_t, sin_t = (jnp.asarray(t) for t in rope_tables())
        *parts, gain = head(hidden, grad_out, w_query, w_key, w_value, w_out, tok_pos, norm_gain.reshape(1, SHARE), cos_t, sin_t)
        parts = [p.reshape(DIM, GROUP) if p.ndim > DUO else p for p in parts]
        result, grad_hidden, gq, gk, gv, go, gout = settle(*tail(*parts, gain, hidden, grad_out, tok_pos, cos_t, sin_t))
        return result[None], grad_hidden[None], gq, gk, gv, go, gout.reshape(SHARE)

    row_spec, pos_spec = P('fsdp', 'cp', None), P('fsdp', 'cp')
    weight_spec, gain_spec = P(('fsdp', 'cp'), None), P(('fsdp', 'cp'))
    return jax.shard_map(shard_fn, mesh=mesh, in_specs=(row_spec, pos_spec, row_spec, gain_spec, weight_spec, weight_spec, weight_spec, weight_spec), out_specs=(row_spec, row_spec, weight_spec, weight_spec, weight_spec, weight_spec, gain_spec), check_vma=False)
```

```python
import functools
import jax
import jax.numpy as jnp
import numpy as np
from jax import lax
from jax.experimental import pallas as pl
from jax.experimental.pallas import tpu as pltpu
from jax.sharding import PartitionSpec as P

LANES, SUBS, RING, TRIO, DUO = 128, 8, 4, 3, 2
PAIR, ROWS, CHIP, SHARE, TURN = 256, 512, 32, 16, 64
HEAD_DIM = LANES
ROPE_THETA = 1000000.0
RMS_EPS = 1e-5
SCALE = HEAD_DIM ** -0.5
LOG2E = 1.4426950408889634

MESH = pl.DeviceIdType.MESH
AXES = ('x', 'y', 'z')
ORDERS = (('x', 'y', 'z'), ('y', 'z', 'x'), ('z', 'x', 'y'))
ALL = pl.ds(0, RING)


def torus():
    f = lax.axis_index('fsdp')
    return {'x': lax.rem(f, RING), 'y': lax.rem(lax.div(f, RING), RING), 'z': lax.div(f, SHARE)}


def step(pos, axis, hop):
    return lax.rem(pos[axis] + hop, RING)


class Batch:
    def __init__(self, comm):
        self.comm, self.index = comm, comm.used
        comm.used += 1

    def _copy(self, src, dst, device):
        send, recv, _ = self.comm.sems
        return pltpu.make_async_remote_copy(src_ref=src, dst_ref=dst, send_sem=send.at[self.index], recv_sem=recv.at[self.index], device_id=device, device_id_type=MESH)

    def send(self, src, dst, device):
        self._copy(src, dst, device).start()
        return self

    def arrived(self, whole):
        self._copy(whole, whole, self.comm.peer()).wait_recv()

    def sent(self, whole):
        self._copy(whole, whole, self.comm.peer()).wait_send()


class Comm:
    def __init__(self, send_sems, recv_sems, local_sems):
        self.pos = torus()
        self.core = lax.axis_index('cp')
        self.sems = (send_sems, recv_sems, local_sems)
        self.used = self.used_local = 0
        self.stored = []

    def far(self, axis, hop):
        p = dict(self.pos)
        p[axis] = step(self.pos, axis, hop)
        return {'fsdp': (p['z'] * RING + p['y']) * RING + p['x'], 'cp': self.core}

    def peer(self):
        return {'fsdp': lax.axis_index('fsdp'), 'cp': 1 - self.core}

    def aside(self, dy, dx):
        return {'fsdp': (self.pos['z'] * RING + step(self.pos, 'y', dy)) * RING + step(self.pos, 'x', dx), 'cp': self.core}

    def announce(self, corners=()):
        sem = pltpu.get_barrier_semaphore()
        for axis in AXES:
            for hop in (1, DUO, TRIO):
                pl.semaphore_signal(sem, inc=1, device_id=self.far(axis, hop), device_id_type=MESH)
        for dy, dx in corners:
            pl.semaphore_signal(sem, inc=1, device_id=self.aside(dy, dx), device_id_type=MESH)
        pl.semaphore_signal(sem, inc=1, device_id=self.peer(), device_id_type=MESH)

    def meet(self, corners=()):
        pl.semaphore_wait(pltpu.get_barrier_semaphore(), 10 + len(corners))

    def ring(self, batch, src, slots, axis):
        for hop in (1, DUO, TRIO):
            batch.send(src, slots.at[hop], self.far(axis, hop))

    def local(self, src, dst):
        i = self.used_local
        self.used_local += 1
        c = pltpu.make_async_copy(src, dst, self.sems[DUO].at[i])
        c.start()
        return c

    def store(self, src, dst):
        self.stored.append(self.local(src, dst))


class Singles(Comm):
    def __init__(self, *sems):
        super().__init__(*sems)
        self.sent, self.exchanged = [], []

    def _copy(self, src, dst, device):
        i = self.used
        self.used += 1
        c = pltpu.make_async_remote_copy(src_ref=src, dst_ref=dst, send_sem=self.sems[0].at[i], recv_sem=self.sems[1].at[i], device_id=device, device_id_type=MESH)
        c.start()
        return c

    def send(self, src, dst, device):
        c = self._copy(src, dst, device)
        self.sent.append(c)
        return c

    def trade(self, src, dst):
        self.exchanged.append(self._copy(src, dst, self.peer()))


def pick(ref, sel, piece):
    lo, cols, first, rows = piece
    return ref.at[sel['z'], sel['y'], sel['x'], pl.ds(first, rows), pl.ds(lo, cols)]


def sem_scratch(remote, local):
    return [pltpu.SemaphoreType.DMA((remote,)), pltpu.SemaphoreType.DMA((remote,)), pltpu.SemaphoreType.DMA((local,))]


def add_into(dst, *srcs, fresh=False):
    def add(idx):
        total, *rest = [s[idx] for s in (srcs if fresh else (dst,) + srcs)]
        for more in rest:
            total = total + more
        dst[idx] = total

    if len(dst.shape) > TRIO:
        @pl.loop(0, dst.shape[0])
        def _(i):
            add((i,))
    else:
        add(Ellipsis)


def halves(lo, n):
    return (lo, n, 0, SHARE), (lo, n, SHARE, SHARE)


GROUPS = (halves(0, 384), halves(384, 384), halves(768, 384))
QK_FIRST = (halves(0, PAIR), halves(384, PAIR), halves(768, PAIR))
QK_LAST = (halves(PAIR, LANES), halves(640, LANES), halves(1024, LANES))
TOKENS = 1024
DIM = 2048
HALF = 1024
QKV = 1280
GROUP = 1152


def scope(name):
    return jax.named_scope(name)


def dot(a, b):
    return jnp.dot(a, b, preferred_element_type=jnp.float32)


def dot_nt(a, b):
    return lax.dot_general(a, b, (((1,), (1,)), ((), ())), preferred_element_type=jnp.float32)


def tile_at(i, n):
    return pl.ds(pl.multiple_of(i * n, n), n)


class Gather:
    def __init__(self, comm, ref, colors, land, held=None):
        self.comm, self.ref, self.colors, self.land = comm, ref, colors, land
        self.held = list(held or [dict(comm.pos) for _ in colors])
        self.spent = []

    def move(self, batch, s, piece, to):
        batch.send(pick(self.ref, s, piece), pick(self.ref, s, piece), to)

    def at(self, k, hop):
        d = ORDERS[k][self.phase]
        return dict(self.held[k], **{d: step(self.comm.pos, d, hop)})

    def begin(self, phase):
        self.phase = phase
        self.rest = Batch(self.comm)
        if phase == 0:
            for hop in (DUO, 1, TRIO):
                for k, (a, _) in enumerate(self.colors):
                    self.move(self.rest, self.held[k], (a[0], a[1], 0, CHIP), self.comm.far(ORDERS[k][0], hop))
            return
        self.up, self.dn = ([Batch(self.comm) for _ in range(TRIO)] for _ in range(DUO))
        for k, (a, b) in enumerate(self.colors):
            d = ORDERS[k][phase]
            up, dn, s = self.comm.far(d, 1), self.comm.far(d, TRIO), self.held[k]
            self.move(self.up[k], s, a, up)
            self.move(self.dn[k], s, b, dn)
            self.move(self.rest, s, b, up)
            self.move(self.rest, s, a, dn)
        if phase == DUO:
            for k, pieces in enumerate(self.colors):
                for piece in pieces:
                    self.land(self.ref, self.held[k], piece)

    def forward(self):
        for k, (a, b) in enumerate(self.colors):
            d = ORDERS[k][self.phase]
            for batch, hop, piece, to in ((self.up[k], TRIO, a, 1), (self.dn[k], 1, b, TRIO)):
                s = self.at(k, hop)
                batch.arrived(pick(self.ref, s, piece))
                self.move(self.rest, s, piece, self.comm.far(d, to))
                if self.phase == DUO:
                    self.land(self.ref, s, piece)
                self.spent.append((batch, pick(self.ref, self.held[k], piece)))

    def end(self):
        axis = ORDERS[0][self.phase]
        blocks = dict(self.held[0], **{axis: pl.ds(0, DUO if self.phase else TRIO)})
        width = sum(a[1] for a, _ in self.colors)
        whole = pick(self.ref, blocks, (0, width, 0, CHIP))
        self.rest.arrived(whole)
        self.spent.append((self.rest, whole))
        for k, (a, b) in enumerate(self.colors):
            if self.phase == DUO:
                for hop, piece in ((TRIO, b), (1, a), (DUO, a), (DUO, b)):
                    self.land(self.ref, self.at(k, hop), piece)
            self.held[k] = dict(self.held[k], **{ORDERS[k][self.phase]: ALL})

    def finish(self):
        for batch, whole in self.spent:
            batch.sent(whole)


def head_kernel(hidden, dy, wq, wk, wv, wo, pos, gain_in, cos_t, sin_t,
                qt_o, dot_o, k_o, kt_o, v_o, vt_o, rt_o, dyc_o, wqk_o, wqkp_o, wvo_o, wvop_o, gain_o,
                hid2, dy2, dys, rs, rt, wqk, wvo, wpeer, pi, pos2, qt, dot_s, kk, kt, vv, vt, cosines, sines, gain, gtile, gbuf, gx, gy, gz, *sems):
    comm = Comm(*sems)
    comm.announce()
    pos_c, core = comm.pos, comm.core
    bf16, f32 = jnp.bfloat16, jnp.float32
    peer = comm.peer()
    rows = tile_at(core, SHARE)
    mine_qk = wqk.at[pos_c['z'], pos_c['y'], pos_c['x'], rows]
    mine_vo = wvo.at[pos_c['z'], pos_c['y'], pos_c['x'], rows]

    def weight_parts(c):
        return ((wq.at[:, tile_at(c, HALF)], mine_qk.at[:, pl.ds(0, HALF)]), (wk.at[:, tile_at(c, LANES)], mine_qk.at[:, pl.ds(HALF, LANES)]),
                (wv.at[:, tile_at(c, LANES)], mine_vo.at[:, pl.ds(0, LANES)]), (wo.at[:, tile_at(c, HALF)], mine_vo.at[:, pl.ds(LANES, HALF)]))

    loads = [comm.local(s, d) for s, d in weight_parts(core)]
    load_x = [comm.local(hidden, hid2.at[pl.ds(0, ROWS)]), comm.local(dy, dy2.at[pl.ds(0, ROWS)])]
    share = lax.broadcasted_iota(jnp.int32, (SUBS, LANES), 1) // SHARE
    gtile[...] = jnp.where(share == pos_c['x'] * DUO + core, jnp.broadcast_to(jnp.concatenate([gain_in[...]] * SUBS, axis=1), (SUBS, LANES)), 0.0)
    with scope('entry'):
        comm.meet()
    swap_w, swap_pos, swap_dy, swap_x, peers_qk, peers_vo = (Batch(comm) for _ in range(6))
    gain_c, gain_x, gain_y, gain_z = (Batch(comm) for _ in range(RING))
    for s, d in weight_parts(1 - core):
        swap_w.send(s, d, peer)
    gain_c.send(gtile, gbuf, peer)
    swap_pos.send(pos, pos2, peer)
    for c in loads:
        c.wait()
    with scope('wait_w'):
        swapped = wqk.at[pos_c['z'], pos_c['y'], pos_c['x']]
        swap_w.arrived(swapped)

    def land_qk(ref, s, cols):
        peers_qk.send(pick(ref, s, cols), pick(wqkp_o, s, cols), peer)

    def land_vo(ref, s, cols):
        peers_vo.send(pick(ref, s, cols), pick(wpeer, s, cols), peer)

    g1 = Gather(comm, wvo, GROUPS, land_vo)
    g2 = Gather(comm, wqk, GROUPS, land_qk)
    g1.begin(0)
    g2.begin(0)
    gain_c.arrived(gbuf)
    gx[0] = gtile[...] + gbuf[...]
    comm.ring(gain_x, gx.at[0], gx, 'x')

    swap_pos.arrived(pos2)

    @pl.loop(0, TOKENS // LANES)
    def _(i):
        want = lax.broadcasted_iota(jnp.int32, (LANES, ROWS), 0) + i * LANES
        for h, have in enumerate((pos, pos2)):
            pi[tile_at(i, LANES), h * ROWS:(h + 1) * ROWS] = jnp.where(want == have[...], 1.0, 0.0).astype(bf16)

    for i in range(RING):
        r = slice(i * PAIR, (i + 1) * PAIR)
        cos, sin = cos_t[:, r], sin_t[:, r]
        cosines[r, :] = jnp.concatenate([cos, cos], axis=0).T
        sines[r, :] = jnp.concatenate([-sin, sin], axis=0).T

    def sort(dst, src, first, last):
        with scope('sort'):
            @pl.loop(first, last)
            def _(j):
                c = tile_at(j, PAIR)
                dst[:, c] = dot(pi[...], src[:, c]).astype(bf16)

    swap_dy.send(dy, dy2.at[pl.ds(ROWS, ROWS)], peer)
    with scope('p0_end'):
        for g in (g1, g2):
            g.end()
            g.begin(1)
    swap_x.send(hidden, hid2.at[pl.ds(ROWS, ROWS)], peer)
    gain_x.arrived(gx.at[pl.ds(1, TRIO)])
    gy[pos_c['y']] = (gx[0] + gx[1]) + (gx[DUO] + gx[TRIO])
    for hop in (1, DUO, TRIO):
        gain_y.send(gy.at[pos_c['y']], gy.at[pos_c['y']], comm.far('y', hop))
    with scope('wait_dy'):
        load_x[1].wait()
        swap_dy.arrived(dy2.at[pl.ds(ROWS, ROWS)])
    sort(dys, dy2, 0, RING)
    with scope('p1a_fwd'):
        g1.forward()
    sort(dys, dy2, RING, 6)
    with scope('p1b_fwd'):
        g2.forward()
    sort(dys, dy2, 6, SUBS)
    with scope('p1a_end'):
        g1.end()
    gain_y.arrived(gy.at[pl.ds(1, TRIO)])
    for j in range(RING):
        gz[pos_c['z'], j] = gy[j]
    for hop in (1, DUO, TRIO):
        gain_z.send(gz.at[pos_c['z']], gz.at[pos_c['z']], comm.far('z', hop))
    g1.begin(DUO)
    comm.store(dys.at[:, tile_at(core, HALF)], dyc_o)
    with scope('p1b_end'):
        g2.end()
    with scope('wait_x'):
        load_x[0].wait()
        swap_x.arrived(hid2.at[pl.ds(ROWS, ROWS)])
    sort(rs, hid2, 0, SUBS)
    with scope('p2q_fwd'):
        g1.forward()
    g2a, g2b = (Gather(comm, wqk, colors, land_qk, g2.held) for colors in (QK_FIRST, QK_LAST))
    g2a.begin(DUO)
    with scope('gain'):
        gain_z.arrived(gz.at[pl.ds(1, TRIO)])
    for i in range(RING):
        for j in range(RING):
            gain[:, (i * RING + j) * LANES:(i * RING + j + 1) * LANES] = gz[i, j]
    comm.store(gain, gain_o)

    def norm(first, last):
        with scope('norm'):
            @pl.loop(first, last)
            def _(i):
                r = tile_at(i, CHIP)
                x = rs[r, :].astype(f32)
                inv = lax.rsqrt(jnp.mean(x * x, axis=-1, keepdims=True) + RMS_EPS)
                rs[r, :] = (x * inv * gain[0:1, :]).astype(bf16)

    norm(0, TOKENS // CHIP)
    with scope('r_t'):
        @pl.loop(0, DIM // PAIR)
        def _(i):
            c = tile_at(i, PAIR)

            @pl.loop(0, TOKENS // PAIR)
            def _(j):
                r = tile_at(j, PAIR)
                rt[c, r] = rs[r, c].T
    comm.store(rt, rt_o)
    with scope('p2o_end'):
        g1.end()
    w_qk, w_vo, w_peer = wqk.reshape(DIM, GROUP), wvo.reshape(DIM, GROUP), wpeer.reshape(DIM, GROUP)
    with scope('vals'):
        @pl.loop(0, DUO)
        def _(i):
            r = tile_at(i, ROWS)
            val = dot(rs[r, :], w_vo[:, :LANES]).astype(bf16)
            vv[r, :] = val
            vt[:, r] = val.T
    for src, dst in ((wvo, wvo_o), (vv, v_o), (vt, vt_o)):
        comm.store(src, dst)
    with scope('p2q_fwd'):
        g2a.forward()
    g2b.begin(DUO)
    with scope('wo_peer'):
        peers_vo.arrived(wpeer)
    comm.store(wpeer, wvop_o)
    with scope('do_t'):
        mine = tile_at(core, HALF)

        @pl.loop(0, TOKENS // PAIR)
        def _(j):
            t = tile_at(j, PAIR)
            w_rows = jnp.concatenate([w_vo[mine, LANES:], w_peer[mine, LANES:]], axis=1)
            d_rows = jnp.concatenate([dys[t, mine], dys[t, tile_at(1 - core, HALF)]], axis=1)
            dot_s[:, t] = dot_nt(w_rows, d_rows).astype(bf16)
    comm.store(dot_s, dot_o)

    def rotated(x, r):
        return (x * cosines[r, :] + pltpu.roll(x, TURN, 1) * sines[r, :]).astype(bf16)

    def queries(columns, heads):
        for i in range(DUO):
            r = slice(i * ROWS, (i + 1) * ROWS)
            x = dot(rs[r, :], columns)
            for h, head in enumerate(heads):
                qt[tile_at(head, LANES), r] = rotated(x[:, h * LANES:(h + 1) * LANES], r).T

    with scope('p2q_end'):
        g2a.end()

    with scope('last_fwd'):
        g2b.forward()
    with scope('q'):
        for t in range(TRIO):
            queries(w_qk[:, t * 384:t * 384 + PAIR], (TRIO * t, TRIO * t + 1))
    for t in range(TRIO):
        two_heads = pl.ds(t * 384, PAIR)
        comm.store(qt.at[two_heads], qt_o.at[two_heads])
    with scope('last_end'):
        g2b.end()
    comm.store(wqk, wqk_o)
    with scope('q_last'):
        last = jnp.concatenate([w_qk[:, PAIR:384], w_qk[:, 640:768], w_qk[:, HALF:]], axis=1)
        for i in range(DUO):
            r = slice(i * ROWS, (i + 1) * ROWS)
            x = dot(rs[r, :], last)
            for h, head in enumerate((DUO, 5)):
                qt[tile_at(head, LANES), r] = rotated(x[:, h * LANES:(h + 1) * LANES], r).T
            key = rotated(x[:, PAIR:], r)
            kk[r, :] = key
            kt[:, r] = key.T
    for src, dst in ((kk, k_o), (kt, kt_o)) + tuple((qt.at[tile_at(h, LANES)], qt_o.at[tile_at(h, LANES)]) for h in (DUO, 5)):
        comm.store(src, dst)
    with scope('finish'):
        peers_qk.arrived(wqk)
        for batch, whole in ((swap_w, swapped), (swap_pos, pos2), (swap_dy, dy2.at[pl.ds(ROWS, ROWS)]), (swap_x, hid2.at[pl.ds(ROWS, ROWS)]), (peers_qk, wqk), (peers_vo, wvo),
                             (gain_c, gbuf), (gain_x, gx.at[pl.ds(1, TRIO)]), (gain_y, gy.at[pl.ds(1, TRIO)]), (gain_z, gz.at[pl.ds(1, TRIO)])):
            batch.sent(whole)
        for g in (g1, g2, g2a, g2b):
            g.finish()
        for c in comm.stored:
            c.wait()


def head(hidden, dy, wq, wk, wv, wo, pos, gain, cos_t, sin_t):
    bf16, f32 = jnp.bfloat16, jnp.float32
    any_ = pl.BlockSpec(memory_space=pl.ANY)
    vmem = pl.BlockSpec(memory_space=pltpu.VMEM)
    S = lambda shape, d=bf16: jax.ShapeDtypeStruct(shape, d)
    V = lambda shape, d=bf16: pltpu.VMEM(shape, d)
    group = (RING, RING, RING, CHIP, GROUP)
    sq, tall, wide = (HALF, TOKENS), (TOKENS, LANES), (LANES, TOKENS)
    full = (TOKENS, DIM)
    return pl.pallas_call(
        head_kernel,
        out_shape=[S(sq), S(sq), S(tall), S(wide), S(tall), S(wide), S((DIM, TOKENS)), S((TOKENS, HALF)), S(group), S(group), S(group), S(group), S((SUBS, DIM), f32)],
        in_specs=[any_] * 6 + [vmem] * RING,
        out_specs=[any_] * 13,
        scratch_shapes=[V(full), V(full), V(full), V(full), V((DIM, TOKENS)), V(group), V(group), V(group), V((TOKENS, TOKENS)), V((1, ROWS), jnp.int32),
                        V(sq), V(sq), V(tall), V(wide), V(tall), V(wide), V(tall, f32), V(tall, f32), V((SUBS, DIM), f32), V((SUBS, LANES), f32), V((SUBS, LANES), f32), V((RING, SUBS, LANES), f32), V((RING, SUBS, LANES), f32), V((RING, RING, SUBS, LANES), f32)] + sem_scratch(47, 22),
        compiler_params=pltpu.CompilerParams(collective_id=0, has_side_effects=True, vmem_limit_bytes=60 * DUO**20),
        name='head',
    )(hidden, dy, wq, wk, wv, wo, pos, gain, cos_t, sin_t)


HEADS = SUBS
UNIT_K, UNIT_V = SUBS, 9
N_UNITS = 18
GAIN = N_UNITS
SLOTS = RING
LAST = 5
ABREAST = DUO
LINES = ((0, TRIO, 6, 9, 12, 15), (1, RING, 7, 10, 13, SHARE), (DUO, 5, SUBS, 11, 14, 17))
COLOR = {u: k for k, line in enumerate(LINES) for u in line}
RANK = {u: i for line in LINES for i, u in enumerate(line)}
SWAPPED = (1, TRIO, RING, SUBS, 10)
ORDER = {u: ORDERS[k] if u not in SWAPPED else (ORDERS[k][0], ORDERS[k][DUO], ORDERS[k][1]) for u, k in COLOR.items()}
BEFORE = {u: line[i - SLOTS] if i >= SLOTS else None for line in LINES for i, u in enumerate(line)}
PLACES = 12
PLACE = {u: u % PLACES for u in range(N_UNITS)}
WIRE = (2.82, 0.71, 0.36)
LATENCY = 2.4
STAGE_COST = 0.08


class Plan:
    def __init__(self):
        self.now, self.stage, self.ready, self.order, self.link = 0.0, {}, {}, [], {}
        self.mark = {}

    def _wire(self, u, phase, count):
        link = ORDER[u][phase]
        t = max(self.link.get(link, 0.0), self.now)
        first = t + WIRE[phase] + LATENCY
        self.link[link] = t + WIRE[phase] * count
        return first if phase < DUO else self.link[link] + LATENCY

    def free(self, u, phase):
        if BEFORE[u] is None:
            return True
        done = self.mark.get((BEFORE[u], (DUO, RING, 5)[phase]))
        if done is None:
            return False
        sent = ((0, 1), (DUO, TRIO), (RING,))[phase]
        return any(self.mark.get((j, s), -1) > done and (j, s + 1) in self.mark for j, order in ORDER.items() if order[phase] == ORDER[u][phase] for s in sent)

    def run(self, u):
        stage = self.stage[u]
        self.order.append((u, stage))
        self.mark[u, stage] = len(self.order)
        self.now = max(self.now, self.ready[u]) + STAGE_COST
        self.stage[u] = stage + 1
        if stage == (TRIO if u == GAIN else LAST):
            del self.stage[u]
        elif u == GAIN:
            self.ready[u] = max([self.now] + [self.link.get(a, 0.0) for a in ('', 'z', 'xy')[stage]]) + DUO * LATENCY
        elif stage % DUO:
            self.ready[u] = self._wire(u, stage // DUO, 1)
        else:
            self.ready[u] = self._wire(u, stage // DUO, DUO)

    def blocked(self, u):
        stage = self.stage[u]
        if u == GAIN:
            return False
        if stage == 0 and sum(0 < self.stage.get(j, 0) <= DUO for j in LINES[COLOR[u]]) >= ABREAST:
            return True
        if stage == DUO and BEFORE[u] is not None and (BEFORE[u], LAST) not in self.mark:
            return True
        return stage in (0, DUO, RING) and not self.free(u, stage // DUO)

    def start(self, u):
        self.stage[u], self.ready[u] = 0, self.now

    def due(self):
        first = len(self.order)
        while True:
            ripe = [(self.ready[u], u) for u in self.stage if self.ready[u] <= self.now and not self.blocked(u)]
            if not ripe:
                return self.order[first:]
            self.run(min(ripe)[1])

    def vacated(self, u):
        return (u, DUO) in self.mark

    def rush(self, done):
        first = len(self.order)
        while not done():
            self.run(min((self.ready[u], u) for u in self.stage if not self.blocked(u))[1])
        return self.order[first:]


QB = PAIR
PAIRS = HEADS // DUO
NBLK = TOKENS // QB
HALVES = (pl.ds(0, SHARE), pl.ds(SHARE, SHARE))
PLANE = tuple((dy, dx) for dy in range(RING) for dx in range(RING) if dy or dx)
CORNERS = tuple((dy, dx) for dy, dx in PLANE if dy and dx)


class Scatter:
    def __init__(self, comm, part, mid, bufs, fin, outs, send_sems, recv_sems, swap_sems):
        self.pos, self.part, self.mid, self.bufs, self.fin, self.outs = comm.pos, part, mid, bufs, fin, outs
        self.send_sems, self.recv_sems, self.swap_sems = send_sems, recv_sems, swap_sems
        self.near = {(a, hop): comm.far(a, hop) for a in AXES for hop in (1, DUO, TRIO)}
        self.hops = {(a, hop): step(comm.pos, a, hop) for a in AXES for hop in (1, DUO, TRIO)}
        self.peer, self.core = comm.peer(), comm.core
        self.keep, self.give = tile_at(comm.core, SHARE), tile_at(1 - comm.core, SHARE)
        self.drained, self.done = set(), []

    def slot(self, u):
        return COLOR[u], RANK[u] % SLOTS

    def buf(self, u, phase):
        return self.bufs[phase].at[self.slot(u)]

    def view(self, u, phase, hop, half=None):
        order = ORDER[u]
        at = {a: ALL for a in AXES}
        for a in order[1:phase]:
            at[a] = self.pos[a]
        at[order[phase]] = self.hops[order[phase], hop] if hop else self.pos[order[phase]]
        rows = pl.ds(0, CHIP) if half is None else HALVES[half]
        if phase == 0:
            return self.part.at[PLACE[u], at['z'], at['y'], at['x'], rows, :]
        return self.mid.at[self.slot(u) + tuple(at[a] for a in 'zyx' if a != order[0]) + (rows, slice(None))]

    def copy(self, src, dst, sems, device):
        return pltpu.make_async_remote_copy(src_ref=src, dst_ref=dst, send_sem=sems[0], recv_sem=sems[1], device_id=device, device_id_type=MESH)

    def sems(self, u, phase, kind=0):
        k, i = self.slot(u)
        at = (k * SLOTS + i) * TRIO + phase
        return self.send_sems.at[at], self.recv_sems.at[(k * SLOTS + i) * 5 + DUO * phase + kind]

    def send(self, u, phase, name):
        axis = ORDER[u][phase]
        if phase == DUO:
            src, to = self.view(u, DUO, name + 1), name + 1
        else:
            hop, half, to = ((DUO, 0, 1), (DUO, 1, TRIO), (1, 1, 1), (TRIO, 0, TRIO), (1, 0, 1), (TRIO, 1, TRIO))[name]
            src = self.view(u, phase, hop, half)
        self.copy(src, self.buf(u, phase).at[name], self.sems(u, phase, int(name > 1 and phase < DUO)), self.near[axis, to]).start()

    def launch(self, u, phase):
        if BEFORE[u] is not None:
            self.drain(BEFORE[u], phase)
        for name in range(RING if phase < DUO else TRIO):
            self.send(u, phase, name)

    def arrived(self, u, phase, first, count):
        whole = self.buf(u, phase).at[pl.ds(first, count)]
        self.copy(whole, whole, self.sems(u, phase, int(first > 0)), self.peer).wait_recv()

    def drain(self, u, phase):
        if (u, phase) not in self.drained:
            self.drained.add((u, phase))
            whole = self.buf(u, phase)
            self.copy(whole, whole, self.sems(u, phase), self.peer).wait_send()

    def out(self, u):
        if u < HEADS:
            out, col = self.outs[0], self.core * HALF + u * LANES
        elif u < 10:
            out, col = self.outs[u - 7], self.core * LANES
        else:
            out, col = self.outs[TRIO], self.core * HALF + (u - 10) * LANES
        return out.at[:, pl.ds(pl.multiple_of(col, LANES), LANES)]

    def kept(self, u, turn):
        return pltpu.make_async_copy(self.fin.at[u, self.keep], self.out(u), self.swap_sems.at[DUO + turn])

    def run(self, u, stage):
        if stage == 0:
            return self.launch(u, 0)
        phase = (stage - 1) // DUO
        if stage == LAST:
            self.arrived(u, DUO, 0, TRIO)
            got = self.buf(u, DUO)
            self.fin[u] = self.view(u, DUO, 0)[...] + (got[0] + got[1] + got[DUO])
            self.copy(self.fin.at[u, self.give], self.out(u), (self.swap_sems.at[0], self.swap_sems.at[1]), self.peer).start()
            turn = len(self.done) % DUO
            if len(self.done) > 1:
                self.kept(self.done[-DUO], turn).wait()
            self.kept(u, turn).start()
            self.done.append(u)
            return
        got = self.buf(u, phase)
        if stage % DUO:
            self.arrived(u, phase, 0, DUO)
            for name, hop in ((0, 1), (1, TRIO)):
                add_into(self.view(u, phase, hop, name), got.at[name])
                self.send(u, phase, name + RING)
            return
        self.arrived(u, phase, DUO, RING)
        if phase == 0 and BEFORE[u] is not None:
            self.drain(BEFORE[u], 1)
            self.drain(BEFORE[u], DUO)
        for half, names in ((0, (TRIO, RING)), (1, (DUO, 5))):
            if phase:
                add_into(self.view(u, phase, 0, half), *[got.at[name] for name in names])
            else:
                dst = self.mid.at[self.slot(u) + (ALL, ALL, HALVES[half], slice(None))]
                add_into(dst, self.view(u, 0, 0, half), *[got.at[name] for name in names], fresh=True)
        self.launch(u, phase + 1)

    def finish(self):
        for u in range(N_UNITS):
            for phase in range(TRIO):
                self.drain(u, phase)
        half = self.fin.at[:, pl.ds(0, SHARE)]
        swaps = self.copy(half, half, (self.swap_sems.at[0], self.swap_sems.at[1]), self.peer)
        swaps.wait_send()
        swaps.wait_recv()
        for turn in range(DUO):
            self.kept(self.done[turn - DUO], turn).wait()


def attend(heads, qt, do_t, k, kt, v, vt, cos, sin, o_row, ot, dq, dkt, dvt, s_scr, e_scr, p_scr, d_scr):
    f32, bf16 = jnp.float32, jnp.bfloat16
    strip = TURN
    work = [(h, j) for j in range(NBLK) for h in range(len(heads))]

    def strips(c):
        return [(i * strip, slice(c * QB + i * strip, c * QB + (i + 1) * strip)) for i in range(QB // strip)]

    def fold(x, op):
        return op(x.reshape(strip // SUBS, SUBS, QB), axis=0)

    def scores(i):
        (h, j), b = work[i], i % DUO
        q_t = qt[heads[h], j * QB:(j + 1) * QB]
        top = jnp.full((SUBS, QB), -jnp.inf, f32)
        for c in range(j + 1):
            tile = dot(k[c * QB:(c + 1) * QB, :], q_t)
            for at, rows in strips(c):
                s = tile[at:at + strip]
                if c == j:
                    seen = lax.broadcasted_iota(jnp.int32, (strip, QB), 0) + at <= lax.broadcasted_iota(jnp.int32, (strip, QB), 1)
                    s = jnp.where(seen, s, -jnp.inf)
                s_scr[b, rows, :] = s
                top = jnp.maximum(top, fold(s, jnp.max))
        return jnp.max(top, axis=0, keepdims=True)

    def rest(i, m):
        (h, j), b = work[i], i % DUO
        cols, n = slice(j * QB, (j + 1) * QB), (j + 1) * QB
        q_t, d_t = qt[heads[h], cols], do_t[heads[h], cols]
        tot = jnp.zeros((SUBS, QB), f32)
        for c in range(j + 1):
            for at, rows in strips(c):
                e = jnp.exp2((s_scr[b, rows, :] - m) * (SCALE * LOG2E))
                s_scr[b, rows, :] = e
                e_scr[b, rows, :] = e.astype(bf16)
                tot = tot + fold(e, jnp.sum)
        den = jnp.sum(tot, axis=0, keepdims=True)
        inv = 1.0 / den
        o = (dot(vt[:, :n], e_scr[b, :n, :]) / den).astype(bf16)
        ot[o_row(h), cols] = o
        delta = jnp.sum(d_t.astype(f32) * o.astype(f32), axis=0, keepdims=True)
        for c in range(j + 1):
            dp = dot(v[c * QB:(c + 1) * QB, :], d_t)
            for at, rows in strips(c):
                p = s_scr[b, rows, :] * inv
                p_scr[b, rows, :] = p.astype(bf16)
                d_scr[b, rows, :] = (p * (dp[at:at + strip] - delta)).astype(bf16)
        dvt[:, :n] += dot_nt(d_t, p_scr[b, :n, :])
        dkt[:, :n] += dot_nt(q_t, d_scr[b, :n, :])
        g = dot(kt[:, :n], d_scr[b, :n, :]) * SCALE
        co, si = cos[:, cols], sin[:, cols]
        x, y = g[:TURN], g[TURN:]
        dq[heads[h], cols] = jnp.concatenate([x * co + y * si, y * co - x * si], axis=0).astype(bf16)

    m = scores(0)
    for i in range(len(work)):
        later = scores(i + 1) if i + 1 < len(work) else None
        rest(i, m)
        m = later


def tail_kernel(qt, do_t, k, kt, v, vt, rt, dyc, wqk, wqkp, wvo, wvop, gain, hidden, dy, pos, cos, sin,
                result, grad_x, gq, gk, gv, go, gout,
                two, ks, kts, vs, vts, rts, ots, dqo, dqp, dkvo, dkvp, dkt, dvt, s_scr, e_scr, p_scr, d_scr, dycs, part, mid, buf1, buf2, buf3, fin, own, onat, dnat, xs, gacc, gpart, gpeer, gz, gx,
                send_sems, recv_sems, swap_sems, trade_send, trade_recv, local_sems):
    comm = Singles(trade_send, trade_recv, local_sems)
    comm.used = HEADS
    f32, bf16 = jnp.float32, jnp.bfloat16
    core, peer = comm.core, comm.peer()
    a1, a2 = two.at[0], two.at[1]
    sc = Scatter(comm, part, mid, (buf1, buf2, buf3), fin, (gq, gk, gv, go), send_sems, recv_sems, swap_sems)
    plan = Plan()
    some, most = pl.ds(0, PAIR), pl.ds(PAIR, HALF - PAIR)
    loads = [comm.local(s, d) for s, d in ((qt.at[some], two.at[0, some]), (k, ks), (do_t.at[some], two.at[1, some]), (vt, vts), (v, vs), (kt, kts))]
    comm.announce(CORNERS)
    dkt[...] = jnp.zeros_like(dkt)
    dvt[...] = jnp.zeros_like(dvt)
    with scope('wait_q'):
        for c in loads:
            c.wait()
    loads = [comm.local(s, d) for s, d in ((rt, rts), (qt.at[most], two.at[0, most]), (do_t.at[most], two.at[1, most]))]
    later = [comm.local(s, d) for s, d in ((dyc, dycs), (hidden, xs))]

    def emit(stages):
        for u, stage in stages:
            with scope(f'u{u}_s{stage}'):
                if u == GAIN:
                    sum_gain(stage)
                else:
                    sc.run(u, stage)

    def after(cost):
        plan.now += cost
        return plan.due()

    def head_trades(g):
        row = pl.ds(pl.multiple_of((core * HEADS + DUO * g) * LANES, PAIR), PAIR)
        mine = tile_at(g, PAIR)
        return [pltpu.make_async_remote_copy(src_ref=s, dst_ref=d, send_sem=trade_send.at[i], recv_sem=trade_recv.at[i], device_id=peer, device_id_type=MESH)
                for s, d, i in ((ots.at[row], ots.at[row], g), (dqo.at[mine], dqp.at[mine], PAIRS + g))]

    def gradient(place, count, left, right, mul, steps=DUO):
        with scope('grad'):
            @pl.loop(0, steps)
            def _(z):
                g = mul(left[tile_at(z, DIM // steps), :], right())
                for i in range(count):
                    part[place + i, tile_at(z, RING // steps)] = g[:, i * LANES:(i + 1) * LANES].reshape(RING // steps, RING, RING, CHIP, LANES)

    attended, paired = [], []
    for g in range(PAIRS):
        attended.append(after(5.1))
        plan.now += 1.5
        plan.start(DUO * g)
        plan.start(DUO * g + 1)
        paired.append(plan.due())

    @pl.loop(0, PAIRS)
    def _(g):
        def at(table):
            for i in range(PAIRS):
                if table[i]:
                    pl.when(g == i)(functools.partial(emit, table[i]))

        heads = [tile_at(DUO * g + i, LANES) for i in range(DUO)]
        with scope('attend'):
            attend(heads, a1, a2, ks, kts, vs, vts, cos, sin, lambda i: tile_at(core * HEADS + DUO * g + i, LANES), ots, dqo, dkt, dvt, s_scr, e_scr, p_scr, d_scr)

        @pl.when(g == 0)
        def _():
            with scope('entry'):
                comm.meet(CORNERS)
                for c in loads:
                    c.wait()
        for c in head_trades(g):
            c.start()
        at(attended)
        gradient(DUO * g, DUO, rts, lambda: dqo[tile_at(g, PAIR), :], dot_nt, 1)
        at(paired)

    def beat(cost, *starts):
        plan.now += cost
        for u in starts:
            plan.start(u)
        emit(plan.due())

    wkv, wkvp = e_scr.reshape(DIM, PAIR), p_scr.reshape(DIM, PAIR)
    later += [comm.local(src.at[:, pl.ds(at, LANES)], dst.at[:, pl.ds(to, LANES)]) for srcs, dst in (((wqk, wvo), wkv), ((wqkp, wvop), wkvp)) for src, at, to in ((srcs[0], HALF, 0), (srcs[1], 0, LANES))]
    wqp_loads = [comm.local(wqkp.at[tile_at(i, HALF), pl.ds(0, HALF)], two.at[i]) for i in range(DUO)]
    key = dkt[...] * SCALE
    co, si, x, y = cos[...], sin[...], key[:TURN], key[TURN:]
    dkvo[:LANES, :] = jnp.concatenate([x * co + y * si, y * co - x * si], axis=0).astype(bf16)
    dkvo[LANES:, :] = dvt[...].astype(bf16)
    comm.trade(dkvo, dkvp)
    gradient(UNIT_K, DUO, rts, lambda: dkvo[...], dot_nt)
    beat(1.8, UNIT_K, UNIT_V)
    wq_load = comm.local(wqk.at[:, pl.ds(0, HALF)], rts)
    for c in later:
        c.wait()
    with scope('trades'):
        for g in range(PAIRS):
            for c in head_trades(g):
                c.wait()

    waiting = list(range(RING))

    def output_gradients(force=False):
        while waiting:
            first = 10 + DUO * waiting[0]
            before = [u for u in range(N_UNITS) if u < first and PLACE[u] in (PLACE[first], PLACE[first + 1])]
            if force:
                emit(plan.rush(lambda: all(map(plan.vacated, before))))
            if not all(map(plan.vacated, before)):
                return
            for u in before:
                sc.drain(u, 0)
            i = waiting.pop(0)
            gradient(PLACE[first], DUO, ots, lambda: dycs[:, i * PAIR:(i + 1) * PAIR], dot)
            plan.start(first)
            plan.start(first + 1)
            beat(1.5)

    def piece(cost):
        beat(cost)
        output_gradients()

    def ticking(n, cost, body):
        tables = [after(cost) for _ in range(n)]

        @pl.loop(0, n)
        def _(i):
            body(i)
            for j, table in enumerate(tables):
                if table:
                    pl.when(i == j)(functools.partial(emit, table))
        output_gradients()

    @pl.loop(0, TOKENS // LANES)
    def _(i):
        want = lax.broadcasted_iota(jnp.int32, (LANES, ROWS), 0) + i * LANES
        own[tile_at(i, LANES), :] = jnp.where(want == pos[...], 1.0, 0.0).astype(bf16)

    def unsort(at, src_t, n):
        with scope('unsort'):
            dnat[at:at + n, :] = dot(src_t[:n, :], own[...]).astype(bf16)

    output_gradients()
    for c in comm.exchanged:
        c.wait_recv()
    unsort(0, dqo, HALF)
    dy_loads = [comm.local(dy.at[:, tile_at(i, HALF)], dqo.at[tile_at(i, ROWS)]) for i in range(DUO)]
    piece(1.2)
    unsort(HALF, dqp, HALF)
    piece(1.2)
    unsort(DUO * HALF, dkvo, PAIR)
    unsort(DUO * HALF + PAIR, dkvp, PAIR)
    piece(0.7)
    wq_load.wait()
    for c in wqp_loads + dy_loads:
        c.wait()
    gacc[...] = jnp.zeros_like(gacc)

    def dr_parts(half, r):
        return [s_scr.at[half, r(i * PAIR), :] for i in range(RING)]

    def back(block, then):
        def dr(half):
            with scope('dr'):
                c = tile_at(half, HALF)
                left = jnp.concatenate([rts[c, :], two[half], wkv[c, :], wkvp[c, :]], axis=1)
                acc = dot(left, dnat[:, block * PAIR:(block + 1) * PAIR])
                for i, ref in enumerate(dr_parts(half, lambda at: pl.ds(at, PAIR))):
                    ref[...] = acc[i * PAIR:(i + 1) * PAIR, :].T

        def norm(part):
            with scope('back'):
                @pl.loop(0, RING)
                def _(i):
                    j = part * RING + i
                    q = pl.ds(pl.multiple_of(block * PAIR + j * SHARE, SHARE), SHARE)
                    d = jnp.concatenate([ref[...] for half in range(DUO) for ref in dr_parts(half, lambda at: pl.ds(pl.multiple_of(at + j * SHARE, SHARE), SHARE))], axis=1)
                    x = xs[q, :].astype(f32)
                    inv = lax.rsqrt(jnp.mean(x * x, axis=-1, keepdims=True) + RMS_EPS)
                    unit = x * inv
                    gacc[...] += jnp.sum((d * unit).reshape(DUO, SUBS, DIM), axis=0)
                    dg = d * gain[0:1, :]
                    new = inv * (dg - unit * jnp.mean(dg * unit, axis=-1, keepdims=True))
                    for half in range(DUO):
                        r = pl.ds(pl.multiple_of(half * ROWS + block * PAIR + j * SHARE, SHARE), SHARE)
                        dqo[r, :] = (dqo[r, :].astype(f32) + new[:, half * HALF:(half + 1) * HALF]).astype(bf16)

        ticking(DUO, 1.6, dr)
        then()
        ticking(RING, 0.92, norm)

    back(0, lambda: None)
    wo_loads = []
    back(1, lambda: wo_loads.extend([comm.local(wvo.at[:, pl.ds(LANES, HALF)], rts)] + [comm.local(wvop.at[tile_at(i, HALF), pl.ds(LANES, HALF)], two.at[i]) for i in range(DUO)]))
    for i in range(DUO):
        comm.store(dqo.at[tile_at(i, ROWS)], grad_x.at[:, tile_at(i, HALF)])
    total = jnp.sum(gacc[...], axis=0, keepdims=True)
    gpart[...] = jnp.zeros_like(gpart)
    for i in range(RING):
        for j in range(RING):
            gpart[i, j:j + 1, :] = total[:, (i * RING + j) * LANES:(i * RING + j + 1) * LANES]

    gain_c, gain_z, gain_p = (Batch(comm) for _ in range(TRIO))

    def sum_gain(stage):
        if stage == 0:
            gain_c.send(gpart, gpeer, peer)
        elif stage == 1:
            gain_c.arrived(gpeer)
            for j in range(RING):
                gz[j] = gpart[j] + gpeer[j]
            for hop in (1, DUO, TRIO):
                gain_z.send(gz.at[step(comm.pos, 'z', hop)], gz.at[TRIO + hop], comm.far('z', hop))
        elif stage == DUO:
            gain_z.arrived(gz.at[pl.ds(RING, TRIO)])
            gx[0] = (gz[comm.pos['z']] + gz[RING]) + (gz[5] + gz[6])
            for dy, dx in PLANE:
                gain_p.send(gx.at[0], gx.at[dy * RING + dx], comm.aside(dy, dx))
        else:
            gain_p.arrived(gx.at[pl.ds(1, 15)])
            gpeer[0] = jnp.sum(gx[...], axis=0)
            mine = jnp.broadcast_to(gpeer[0, pl.ds(comm.pos['y'], 1), :], (SUBS, LANES))
            gout[...] = pltpu.roll(mine, LANES - (comm.pos['x'] * CHIP + core * SHARE), 1)

    plan.start(GAIN)
    beat(0.2)
    for i in range(DUO):
        with scope('unsort_o'):
            @pl.loop(0, DUO)
            def _(j):
                r = pl.ds(pl.multiple_of(i * HALF + j * ROWS, ROWS), ROWS)
                onat[:, r] = dot(ots[r, :], own[...]).astype(bf16).T
        piece(1.58)
    output_gradients(True)

    def project_out(col, weights, i):
        with scope('project'):
            @pl.loop(DUO * i, DUO * i + DUO)
            def _(j):
                c = tile_at(j, PAIR)
                dst = pl.ds(pl.multiple_of(col + j * PAIR, PAIR), PAIR)
                xs[:, dst] = (xs[:, dst].astype(f32) + dot(onat[...], weights(c))).astype(bf16)
        beat(1.48)

    def own_half(c):
        return rts[:, c]

    def other_half(c):
        return jnp.concatenate([a1[:, c], a2[:, c]], axis=0)

    for c in wo_loads:
        c.wait()
    for col, weights in ((core * HALF, own_half), ((1 - core) * HALF, other_half)):
        for i in range(DUO):
            project_out(col, weights, i)
    comm.store(xs, result)
    emit(plan.rush(lambda: not plan.stage))
    with scope('finish'):
        sc.finish()
        for batch, whole in ((gain_c, gpart), (gain_z, gz.at[pl.ds(RING, TRIO)]), (gain_p, gx.at[pl.ds(1, 15)])):
            batch.sent(whole)
        for c in comm.exchanged:
            c.wait_send()
        for c in comm.stored:
            c.wait()


def tail(qt, do_t, k, kt, v, vt, rt, dyc, wqk, wqkp, wvo, wvop, gain, hidden, dy, pos, cos, sin):
    bf16, f32 = jnp.bfloat16, jnp.float32
    any_ = pl.BlockSpec(memory_space=pl.ANY)
    vmem = pl.BlockSpec(memory_space=pltpu.VMEM)
    S = lambda shape, d=bf16: jax.ShapeDtypeStruct(shape, d)
    V = lambda shape, d=bf16: pltpu.VMEM(shape, d)
    D = lambda n: pltpu.SemaphoreType.DMA((n,))
    sq, tall, wide = (HALF, TOKENS), (TOKENS, LANES), (LANES, TOKENS)
    mine, kv = (ROWS, DIM), (PAIR, TOKENS)
    return pl.pallas_call(
        tail_kernel,
        out_shape=[S(mine), S(mine), S((SHARE, DIM), f32), S((SHARE, PAIR), f32), S((SHARE, PAIR), f32), S((SHARE, DIM), f32), S((SUBS, LANES), f32)],
        in_specs=[any_] * 12 + [vmem] + [any_] * DUO + [vmem] * TRIO,
        out_specs=[any_] * 6 + [vmem],
        scratch_shapes=[V((DUO,) + sq), V(tall), V(wide), V(tall), V(wide), V((DIM, TOKENS)), V((DIM, TOKENS)), V(sq), V(sq), V(kv), V(kv), V(wide, f32), V(wide, f32),
                        V((DUO, TOKENS, QB), f32), V((DUO, TOKENS, QB)), V((DUO, TOKENS, QB)), V((DUO, TOKENS, QB)), V(sq), V((PLACES, RING, RING, RING, CHIP, LANES), f32), V((TRIO, SLOTS, RING, RING, CHIP, LANES), f32),
                        V((TRIO, SLOTS, 6, RING, RING, SHARE, LANES), f32), V((TRIO, SLOTS, 6, RING, SHARE, LANES), f32), V((TRIO, SLOTS, TRIO, CHIP, LANES), f32), V((N_UNITS, CHIP, LANES), f32), V((TOKENS, ROWS)), V(mine), V((DUO * QKV, ROWS)), V(mine),
                        V((SUBS, DIM), f32), V((RING, SUBS, LANES), f32), V((RING, SUBS, LANES), f32), V((7, SUBS, LANES), f32), V((SHARE, SUBS, LANES), f32),
                        D(9 * SLOTS), D(15 * SLOTS), D(RING), D(HEADS + RING), D(HEADS + RING), D(26)],
        compiler_params=pltpu.CompilerParams(collective_id=1, has_side_effects=True, vmem_limit_bytes=67043328),
        name='tail',
    )(qt, do_t, k, kt, v, vt, rt, dyc, wqk, wqkp, wvo, wvop, gain, hidden, dy, pos, cos, sin)


def settle_kernel(n, *refs):
    ins, gain, outs, gain_out, bufs, sems = refs[:n], refs[n], refs[n + 1:DUO * n + 1], refs[DUO * n + 1], refs[DUO * n + DUO:-1], refs[-1]
    jobs = []
    for a, o, b in zip(ins, outs, bufs):
        size = a.shape[0] // RING if a.shape[0] == ROWS else a.shape[0]
        jobs += [tuple(r.at[pl.ds(i, size)] for r in (a, b, o)) for i in range(0, a.shape[0], size)]
    takes = [pltpu.make_async_copy(a, b, sems.at[0, i]) for i, (a, b, _) in enumerate(jobs)]
    puts = [pltpu.make_async_copy(b, o, sems.at[1, i]) for i, (_, b, o) in enumerate(jobs)]
    for c in takes:
        c.start()
    gain_out[...] = gain[0:1, :SHARE]
    for take, put in zip(takes, puts):
        take.wait()
        put.start()
    for c in puts:
        c.wait()


def settle(*arrays):
    *large, gain = arrays
    any_, vmem = pl.BlockSpec(memory_space=pl.ANY), pl.BlockSpec(memory_space=pltpu.VMEM)
    return pl.pallas_call(
        functools.partial(settle_kernel, len(large)),
        out_shape=[jax.ShapeDtypeStruct(a.shape, a.dtype) for a in large] + [jax.ShapeDtypeStruct((1, SHARE), gain.dtype)],
        in_specs=[any_] * len(large) + [vmem],
        out_specs=[any_] * len(large) + [vmem],
        scratch_shapes=[pltpu.VMEM(a.shape, a.dtype) for a in large] + [pltpu.SemaphoreType.DMA((DUO, 12))],
        name='settle',
    )(*arrays)


def rope_tables():
    j = np.arange(HEAD_DIM // DUO, dtype=np.float64) / (HEAD_DIM // DUO)
    freq = (ROPE_THETA ** -j).astype(np.float32)
    angle = freq[:, None] * np.arange(TOKENS, dtype=np.float32)[None, :]
    return np.cos(angle.astype(np.float64)).astype(np.float32), np.sin(angle.astype(np.float64)).astype(np.float32)


def solution(mesh):
    def shard_fn(hidden, tok_pos, grad_out, norm_gain, w_query, w_key, w_value, w_out):
        hidden, grad_out = hidden[0], grad_out[0]
        cos_t, sin_t = (jnp.asarray(t) for t in rope_tables())
        *parts, gain = head(hidden, grad_out, w_query, w_key, w_value, w_out, tok_pos, norm_gain.reshape(1, SHARE), cos_t, sin_t)
        parts = [p.reshape(DIM, GROUP) if p.ndim > DUO else p for p in parts]
        result, grad_hidden, gq, gk, gv, go, gout = settle(*tail(*parts, gain, hidden, grad_out, tok_pos, cos_t, sin_t))
        return result[None], grad_hidden[None], gq, gk, gv, go, gout.reshape(SHARE)

    row_spec, pos_spec = P('fsdp', 'cp', None), P('fsdp', 'cp')
    weight_spec, gain_spec = P(('fsdp', 'cp'), None), P(('fsdp', 'cp'))
    return jax.shard_map(shard_fn, mesh=mesh, in_specs=(row_spec, pos_spec, row_spec, gain_spec, weight_spec, weight_spec, weight_spec, weight_spec), out_specs=(row_spec, row_spec, weight_spec, weight_spec, weight_spec, weight_spec, gain_spec), check_vma=False)
```

```python
import functools
import jax
import jax.numpy as jnp
import numpy as np
from jax import lax
from jax.experimental import pallas as pl
from jax.experimental.pallas import tpu as pltpu
from jax.sharding import PartitionSpec as P

LANES, SUBS, RING, TRIO, DUO = 128, 8, 4, 3, 2
PAIR, ROWS, CHIP, SHARE, TURN = 256, 512, 32, 16, 64
HEAD_DIM = LANES
ROPE_THETA = 1000000.0
RMS_EPS = 1e-5
SCALE = HEAD_DIM ** -0.5
LOG2E = 1.4426950408889634

MESH = pl.DeviceIdType.MESH
AXES = ('x', 'y', 'z')
ORDERS = (('x', 'y', 'z'), ('y', 'z', 'x'), ('z', 'x', 'y'))
ALL = pl.ds(0, RING)


def torus():
    f = lax.axis_index('fsdp')
    return {'x': lax.rem(f, RING), 'y': lax.rem(lax.div(f, RING), RING), 'z': lax.div(f, SHARE)}


def step(pos, axis, hop):
    return lax.rem(pos[axis] + hop, RING)


class Batch:
    def __init__(self, comm):
        self.comm, self.index = comm, comm.used
        comm.used += 1

    def _copy(self, src, dst, device):
        send, recv, _ = self.comm.sems
        return pltpu.make_async_remote_copy(src_ref=src, dst_ref=dst, send_sem=send.at[self.index], recv_sem=recv.at[self.index], device_id=device, device_id_type=MESH)

    def send(self, src, dst, device):
        self._copy(src, dst, device).start()
        return self

    def arrived(self, whole):
        self._copy(whole, whole, self.comm.peer()).wait_recv()

    def sent(self, whole):
        self._copy(whole, whole, self.comm.peer()).wait_send()


class Comm:
    def __init__(self, send_sems, recv_sems, local_sems):
        self.pos = torus()
        self.core = lax.axis_index('cp')
        self.sems = (send_sems, recv_sems, local_sems)
        self.used = self.used_local = 0
        self.stored = []

    def far(self, axis, hop):
        p = dict(self.pos)
        p[axis] = step(self.pos, axis, hop)
        return {'fsdp': (p['z'] * RING + p['y']) * RING + p['x'], 'cp': self.core}

    def peer(self):
        return {'fsdp': lax.axis_index('fsdp'), 'cp': 1 - self.core}

    def aside(self, dy, dx):
        return {'fsdp': (self.pos['z'] * RING + step(self.pos, 'y', dy)) * RING + step(self.pos, 'x', dx), 'cp': self.core}

    def announce(self, corners=()):
        sem = pltpu.get_barrier_semaphore()
        for axis in AXES:
            for hop in (1, DUO, TRIO):
                pl.semaphore_signal(sem, inc=1, device_id=self.far(axis, hop), device_id_type=MESH)
        for dy, dx in corners:
            pl.semaphore_signal(sem, inc=1, device_id=self.aside(dy, dx), device_id_type=MESH)
        pl.semaphore_signal(sem, inc=1, device_id=self.peer(), device_id_type=MESH)

    def meet(self, corners=()):
        pl.semaphore_wait(pltpu.get_barrier_semaphore(), 10 + len(corners))

    def ring(self, batch, src, slots, axis):
        for hop in (1, DUO, TRIO):
            batch.send(src, slots.at[hop], self.far(axis, hop))

    def local(self, src, dst):
        i = self.used_local
        self.used_local += 1
        c = pltpu.make_async_copy(src, dst, self.sems[DUO].at[i])
        c.start()
        return c

    def store(self, src, dst):
        self.stored.append(self.local(src, dst))


class Singles(Comm):
    def __init__(self, *sems):
        super().__init__(*sems)
        self.sent, self.exchanged = [], []

    def _copy(self, src, dst, device):
        i = self.used
        self.used += 1
        c = pltpu.make_async_remote_copy(src_ref=src, dst_ref=dst, send_sem=self.sems[0].at[i], recv_sem=self.sems[1].at[i], device_id=device, device_id_type=MESH)
        c.start()
        return c

    def send(self, src, dst, device):
        c = self._copy(src, dst, device)
        self.sent.append(c)
        return c

    def trade(self, src, dst):
        self.exchanged.append(self._copy(src, dst, self.peer()))


def pick(ref, sel, piece):
    lo, cols, first, rows = piece
    return ref.at[sel['z'], sel['y'], sel['x'], pl.ds(first, rows), pl.ds(lo, cols)]


def sem_scratch(remote, local):
    return [pltpu.SemaphoreType.DMA((remote,)), pltpu.SemaphoreType.DMA((remote,)), pltpu.SemaphoreType.DMA((local,))]


def add_into(dst, *srcs, fresh=False):
    def add(idx):
        total, *rest = [s[idx] for s in (srcs if fresh else (dst,) + srcs)]
        for more in rest:
            total = total + more
        dst[idx] = total

    if len(dst.shape) > TRIO:
        @pl.loop(0, dst.shape[0])
        def _(i):
            add((i,))
    else:
        add(Ellipsis)


def halves(lo, n):
    return (lo, n, 0, SHARE), (lo, n, SHARE, SHARE)


GROUPS = (halves(0, 384), halves(384, 384), halves(768, 384))
QK_FIRST = (halves(0, PAIR), halves(384, PAIR), halves(768, PAIR))
QK_LAST = (halves(PAIR, LANES), halves(640, LANES), halves(1024, LANES))
TOKENS = 1024
DIM = 2048
HALF = 1024
QKV = 1280
GROUP = 1152


def scope(name):
    return jax.named_scope(name)


def dot(a, b):
    return jnp.dot(a, b, preferred_element_type=jnp.float32)


def dot_nt(a, b):
    return lax.dot_general(a, b, (((1,), (1,)), ((), ())), preferred_element_type=jnp.float32)


def tile_at(i, n):
    return pl.ds(pl.multiple_of(i * n, n), n)


class Gather:
    def __init__(self, comm, ref, colors, land, held=None):
        self.comm, self.ref, self.colors, self.land = comm, ref, colors, land
        self.held = list(held or [dict(comm.pos) for _ in colors])
        self.spent = []

    def move(self, batch, s, piece, to):
        batch.send(pick(self.ref, s, piece), pick(self.ref, s, piece), to)

    def at(self, k, hop):
        d = ORDERS[k][self.phase]
        return dict(self.held[k], **{d: step(self.comm.pos, d, hop)})

    def begin(self, phase):
        self.phase = phase
        self.rest = Batch(self.comm)
        if phase == 0:
            for hop in (DUO, 1, TRIO):
                for k, (a, _) in enumerate(self.colors):
                    self.move(self.rest, self.held[k], (a[0], a[1], 0, CHIP), self.comm.far(ORDERS[k][0], hop))
            return
        self.up, self.dn = ([Batch(self.comm) for _ in range(TRIO)] for _ in range(DUO))
        for k, (a, b) in enumerate(self.colors):
            d = ORDERS[k][phase]
            up, dn, s = self.comm.far(d, 1), self.comm.far(d, TRIO), self.held[k]
            self.move(self.up[k], s, a, up)
            self.move(self.dn[k], s, b, dn)
            self.move(self.rest, s, b, up)
            self.move(self.rest, s, a, dn)
        if phase == DUO:
            for k, pieces in enumerate(self.colors):
                for piece in pieces:
                    self.land(self.ref, self.held[k], piece)

    def forward(self):
        for k, (a, b) in enumerate(self.colors):
            d = ORDERS[k][self.phase]
            for batch, hop, piece, to in ((self.up[k], TRIO, a, 1), (self.dn[k], 1, b, TRIO)):
                s = self.at(k, hop)
                batch.arrived(pick(self.ref, s, piece))
                self.move(self.rest, s, piece, self.comm.far(d, to))
                if self.phase == DUO:
                    self.land(self.ref, s, piece)
                self.spent.append((batch, pick(self.ref, self.held[k], piece)))

    def end(self):
        axis = ORDERS[0][self.phase]
        blocks = dict(self.held[0], **{axis: pl.ds(0, DUO if self.phase else TRIO)})
        width = sum(a[1] for a, _ in self.colors)
        whole = pick(self.ref, blocks, (0, width, 0, CHIP))
        self.rest.arrived(whole)
        self.spent.append((self.rest, whole))
        for k, (a, b) in enumerate(self.colors):
            if self.phase == DUO:
                for hop, piece in ((TRIO, b), (1, a), (DUO, a), (DUO, b)):
                    self.land(self.ref, self.at(k, hop), piece)
            self.held[k] = dict(self.held[k], **{ORDERS[k][self.phase]: ALL})

    def finish(self):
        for batch, whole in self.spent:
            batch.sent(whole)


def head_kernel(hidden, dy, wq, wk, wv, wo, pos, gain_in, cos_t, sin_t,
                qt_o, dot_o, k_o, kt_o, v_o, vt_o, rt_o, dyc_o, wqk_o, wqkp_o, wvo_o, wvop_o, gain_o,
                hid2, dy2, dys, rs, rt, wqk, wvo, wpeer, pi, pos2, qt, dot_s, kk, kt, vv, vt, cosines, sines, gain, gtile, gbuf, gx, gy, gz, *sems):
    comm = Comm(*sems)
    comm.announce()
    pos_c, core = comm.pos, comm.core
    bf16, f32 = jnp.bfloat16, jnp.float32
    peer = comm.peer()
    rows = tile_at(core, SHARE)
    mine_qk = wqk.at[pos_c['z'], pos_c['y'], pos_c['x'], rows]
    mine_vo = wvo.at[pos_c['z'], pos_c['y'], pos_c['x'], rows]

    def weight_parts(c):
        return ((wq.at[:, tile_at(c, HALF)], mine_qk.at[:, pl.ds(0, HALF)]), (wk.at[:, tile_at(c, LANES)], mine_qk.at[:, pl.ds(HALF, LANES)]),
                (wv.at[:, tile_at(c, LANES)], mine_vo.at[:, pl.ds(0, LANES)]), (wo.at[:, tile_at(c, HALF)], mine_vo.at[:, pl.ds(LANES, HALF)]))

    loads = [comm.local(s, d) for s, d in weight_parts(core)]
    load_x = [comm.local(hidden, hid2.at[pl.ds(0, ROWS)]), comm.local(dy, dy2.at[pl.ds(0, ROWS)])]
    share = lax.broadcasted_iota(jnp.int32, (SUBS, LANES), 1) // SHARE
    gtile[...] = jnp.where(share == pos_c['x'] * DUO + core, jnp.broadcast_to(jnp.concatenate([gain_in[...]] * SUBS, axis=1), (SUBS, LANES)), 0.0)
    with scope('entry'):
        comm.meet()
    swap_w, swap_pos, swap_dy, swap_x, peers_qk, peers_vo = (Batch(comm) for _ in range(6))
    gain_c, gain_x, gain_y, gain_z = (Batch(comm) for _ in range(RING))
    for s, d in weight_parts(1 - core):
        swap_w.send(s, d, peer)
    gain_c.send(gtile, gbuf, peer)
    swap_pos.send(pos, pos2, peer)
    for c in loads:
        c.wait()
    with scope('wait_w'):
        swapped = wqk.at[pos_c['z'], pos_c['y'], pos_c['x']]
        swap_w.arrived(swapped)

    def land_qk(ref, s, cols):
        peers_qk.send(pick(ref, s, cols), pick(wqkp_o, s, cols), peer)

    def land_vo(ref, s, cols):
        peers_vo.send(pick(ref, s, cols), pick(wpeer, s, cols), peer)

    g1 = Gather(comm, wvo, GROUPS, land_vo)
    g2 = Gather(comm, wqk, GROUPS, land_qk)
    g1.begin(0)
    g2.begin(0)
    gain_c.arrived(gbuf)
    gx[0] = gtile[...] + gbuf[...]
    comm.ring(gain_x, gx.at[0], gx, 'x')

    swap_pos.arrived(pos2)

    @pl.loop(0, TOKENS // LANES)
    def _(i):
        want = lax.broadcasted_iota(jnp.int32, (LANES, ROWS), 0) + i * LANES
        for h, have in enumerate((pos, pos2)):
            pi[tile_at(i, LANES), h * ROWS:(h + 1) * ROWS] = jnp.where(want == have[...], 1.0, 0.0).astype(bf16)

    for i in range(RING):
        r = slice(i * PAIR, (i + 1) * PAIR)
        cos, sin = cos_t[:, r], sin_t[:, r]
        cosines[r, :] = jnp.concatenate([cos, cos], axis=0).T
        sines[r, :] = jnp.concatenate([-sin, sin], axis=0).T

    def sort(dst, src, first, last):
        with scope('sort'):
            @pl.loop(first, last)
            def _(j):
                c = tile_at(j, PAIR)
                dst[:, c] = dot(pi[...], src[:, c]).astype(bf16)

    swap_dy.send(dy, dy2.at[pl.ds(ROWS, ROWS)], peer)
    with scope('p0_end'):
        for g in (g1, g2):
            g.end()
            g.begin(1)
    swap_x.send(hidden, hid2.at[pl.ds(ROWS, ROWS)], peer)
    gain_x.arrived(gx.at[pl.ds(1, TRIO)])
    gy[pos_c['y']] = (gx[0] + gx[1]) + (gx[DUO] + gx[TRIO])
    for hop in (1, DUO, TRIO):
        gain_y.send(gy.at[pos_c['y']], gy.at[pos_c['y']], comm.far('y', hop))
    with scope('wait_dy'):
        load_x[1].wait()
        swap_dy.arrived(dy2.at[pl.ds(ROWS, ROWS)])
    sort(dys, dy2, 0, RING)
    with scope('p1a_fwd'):
        g1.forward()
    sort(dys, dy2, RING, 6)
    with scope('p1b_fwd'):
        g2.forward()
    sort(dys, dy2, 6, SUBS)
    with scope('p1a_end'):
        g1.end()
    gain_y.arrived(gy.at[pl.ds(1, TRIO)])
    for j in range(RING):
        gz[pos_c['z'], j] = gy[j]
    for hop in (1, DUO, TRIO):
        gain_z.send(gz.at[pos_c['z']], gz.at[pos_c['z']], comm.far('z', hop))
    g1.begin(DUO)
    comm.store(dys.at[:, tile_at(core, HALF)], dyc_o)
    with scope('p1b_end'):
        g2.end()
    with scope('wait_x'):
        load_x[0].wait()
        swap_x.arrived(hid2.at[pl.ds(ROWS, ROWS)])
    sort(rs, hid2, 0, SUBS)
    with scope('p2q_fwd'):
        g1.forward()
    g2a, g2b = (Gather(comm, wqk, colors, land_qk, g2.held) for colors in (QK_FIRST, QK_LAST))
    g2a.begin(DUO)
    with scope('gain'):
        gain_z.arrived(gz.at[pl.ds(1, TRIO)])
    for i in range(RING):
        for j in range(RING):
            gain[:, (i * RING + j) * LANES:(i * RING + j + 1) * LANES] = gz[i, j]
    comm.store(gain, gain_o)

    def norm(first, last):
        with scope('norm'):
            @pl.loop(first, last)
            def _(i):
                r = tile_at(i, CHIP)
                x = rs[r, :].astype(f32)
                inv = lax.rsqrt(jnp.mean(x * x, axis=-1, keepdims=True) + RMS_EPS)
                rs[r, :] = (x * inv * gain[0:1, :]).astype(bf16)

    norm(0, TOKENS // CHIP)
    with scope('r_t'):
        @pl.loop(0, DIM // PAIR)
        def _(i):
            c = tile_at(i, PAIR)

            @pl.loop(0, TOKENS // PAIR)
            def _(j):
                r = tile_at(j, PAIR)
                rt[c, r] = rs[r, c].T
    comm.store(rt, rt_o)
    with scope('p2o_end'):
        g1.end()
    w_qk, w_vo, w_peer = wqk.reshape(DIM, GROUP), wvo.reshape(DIM, GROUP), wpeer.reshape(DIM, GROUP)
    with scope('vals'):
        @pl.loop(0, DUO)
        def _(i):
            r = tile_at(i, ROWS)
            val = dot(rs[r, :], w_vo[:, :LANES]).astype(bf16)
            vv[r, :] = val
            vt[:, r] = val.T
    for src, dst in ((wvo, wvo_o), (vv, v_o), (vt, vt_o)):
        comm.store(src, dst)
    with scope('p2q_fwd'):
        g2a.forward()
    g2b.begin(DUO)
    with scope('wo_peer'):
        peers_vo.arrived(wpeer)
    comm.store(wpeer, wvop_o)
    with scope('do_t'):
        mine = tile_at(core, HALF)

        @pl.loop(0, TOKENS // PAIR)
        def _(j):
            t = tile_at(j, PAIR)
            w_rows = jnp.concatenate([w_vo[mine, LANES:], w_peer[mine, LANES:]], axis=1)
            d_rows = jnp.concatenate([dys[t, mine], dys[t, tile_at(1 - core, HALF)]], axis=1)
            dot_s[:, t] = dot_nt(w_rows, d_rows).astype(bf16)
    comm.store(dot_s, dot_o)

    def rotated(x, r):
        return (x * cosines[r, :] + pltpu.roll(x, TURN, 1) * sines[r, :]).astype(bf16)

    def queries(columns, heads):
        for i in range(DUO):
            r = slice(i * ROWS, (i + 1) * ROWS)
            x = dot(rs[r, :], columns)
            for h, head in enumerate(heads):
                qt[tile_at(head, LANES), r] = rotated(x[:, h * LANES:(h + 1) * LANES], r).T

    with scope('p2q_end'):
        g2a.end()

    with scope('last_fwd'):
        g2b.forward()
    with scope('q'):
        for t in range(TRIO):
            queries(w_qk[:, t * 384:t * 384 + PAIR], (TRIO * t, TRIO * t + 1))
    for t in range(TRIO):
        two_heads = pl.ds(t * 384, PAIR)
        comm.store(qt.at[two_heads], qt_o.at[two_heads])
    with scope('last_end'):
        g2b.end()
    comm.store(wqk, wqk_o)
    with scope('q_last'):
        last = jnp.concatenate([w_qk[:, PAIR:384], w_qk[:, 640:768], w_qk[:, HALF:]], axis=1)
        for i in range(DUO):
            r = slice(i * ROWS, (i + 1) * ROWS)
            x = dot(rs[r, :], last)
            for h, head in enumerate((DUO, 5)):
                qt[tile_at(head, LANES), r] = rotated(x[:, h * LANES:(h + 1) * LANES], r).T
            key = rotated(x[:, PAIR:], r)
            kk[r, :] = key
            kt[:, r] = key.T
    for src, dst in ((kk, k_o), (kt, kt_o)) + tuple((qt.at[tile_at(h, LANES)], qt_o.at[tile_at(h, LANES)]) for h in (DUO, 5)):
        comm.store(src, dst)
    with scope('finish'):
        peers_qk.arrived(wqk)
        for batch, whole in ((swap_w, swapped), (swap_pos, pos2), (swap_dy, dy2.at[pl.ds(ROWS, ROWS)]), (swap_x, hid2.at[pl.ds(ROWS, ROWS)]), (peers_qk, wqk), (peers_vo, wvo),
                             (gain_c, gbuf), (gain_x, gx.at[pl.ds(1, TRIO)]), (gain_y, gy.at[pl.ds(1, TRIO)]), (gain_z, gz.at[pl.ds(1, TRIO)])):
            batch.sent(whole)
        for g in (g1, g2, g2a, g2b):
            g.finish()
        for c in comm.stored:
            c.wait()


def head(hidden, dy, wq, wk, wv, wo, pos, gain, cos_t, sin_t):
    bf16, f32 = jnp.bfloat16, jnp.float32
    any_ = pl.BlockSpec(memory_space=pl.ANY)
    vmem = pl.BlockSpec(memory_space=pltpu.VMEM)
    S = lambda shape, d=bf16: jax.ShapeDtypeStruct(shape, d)
    V = lambda shape, d=bf16: pltpu.VMEM(shape, d)
    group = (RING, RING, RING, CHIP, GROUP)
    sq, tall, wide = (HALF, TOKENS), (TOKENS, LANES), (LANES, TOKENS)
    full = (TOKENS, DIM)
    return pl.pallas_call(
        head_kernel,
        out_shape=[S(sq), S(sq), S(tall), S(wide), S(tall), S(wide), S((DIM, TOKENS)), S((TOKENS, HALF)), S(group), S(group), S(group), S(group), S((SUBS, DIM), f32)],
        in_specs=[any_] * 6 + [vmem] * RING,
        out_specs=[any_] * 13,
        scratch_shapes=[V(full), V(full), V(full), V(full), V((DIM, TOKENS)), V(group), V(group), V(group), V((TOKENS, TOKENS)), V((1, ROWS), jnp.int32),
                        V(sq), V(sq), V(tall), V(wide), V(tall), V(wide), V(tall, f32), V(tall, f32), V((SUBS, DIM), f32), V((SUBS, LANES), f32), V((SUBS, LANES), f32), V((RING, SUBS, LANES), f32), V((RING, SUBS, LANES), f32), V((RING, RING, SUBS, LANES), f32)] + sem_scratch(47, 22),
        compiler_params=pltpu.CompilerParams(collective_id=0, has_side_effects=True, vmem_limit_bytes=60 * DUO**20),
        name='head',
    )(hidden, dy, wq, wk, wv, wo, pos, gain, cos_t, sin_t)


HEADS = SUBS
UNIT_K, UNIT_V = SUBS, 9
N_UNITS = 18
GAIN = N_UNITS
SLOTS = RING
LAST = 5
ABREAST = DUO
LINES = ((0, TRIO, 6, 9, 12, 15), (1, RING, 7, 10, 13, SHARE), (DUO, 5, SUBS, 11, 14, 17))
COLOR = {u: k for k, line in enumerate(LINES) for u in line}
RANK = {u: i for line in LINES for i, u in enumerate(line)}
SWAPPED = (1, TRIO, RING, SUBS, 10)
ORDER = {u: ORDERS[k] if u not in SWAPPED else (ORDERS[k][0], ORDERS[k][DUO], ORDERS[k][1]) for u, k in COLOR.items()}
BEFORE = {u: line[i - SLOTS] if i >= SLOTS else None for line in LINES for i, u in enumerate(line)}
PLACES = 12
PLACE = {u: u % PLACES for u in range(N_UNITS)}
WIRE = (2.82, 0.71, 0.36)
LATENCY = 2.4
STAGE_COST = 0.08


class Plan:
    def __init__(self):
        self.now, self.stage, self.ready, self.order, self.link = 0.0, {}, {}, [], {}
        self.mark = {}

    def _wire(self, u, phase, count):
        link = ORDER[u][phase]
        t = max(self.link.get(link, 0.0), self.now)
        first = t + WIRE[phase] + LATENCY
        self.link[link] = t + WIRE[phase] * count
        return first if phase < DUO else self.link[link] + LATENCY

    def free(self, u, phase):
        if BEFORE[u] is None:
            return True
        done = self.mark.get((BEFORE[u], (DUO, RING, 5)[phase]))
        if done is None:
            return False
        sent = ((0, 1), (DUO, TRIO), (RING,))[phase]
        return any(self.mark.get((j, s), -1) > done and (j, s + 1) in self.mark for j, order in ORDER.items() if order[phase] == ORDER[u][phase] for s in sent)

    def run(self, u):
        stage = self.stage[u]
        self.order.append((u, stage))
        self.mark[u, stage] = len(self.order)
        self.now = max(self.now, self.ready[u]) + STAGE_COST
        self.stage[u] = stage + 1
        if stage == (TRIO if u == GAIN else LAST):
            del self.stage[u]
        elif u == GAIN:
            self.ready[u] = max([self.now] + [self.link.get(a, 0.0) for a in ('', 'z', 'xy')[stage]]) + DUO * LATENCY
        elif stage % DUO:
            self.ready[u] = self._wire(u, stage // DUO, 1)
        else:
            self.ready[u] = self._wire(u, stage // DUO, DUO)

    def blocked(self, u):
        stage = self.stage[u]
        if u == GAIN:
            return False
        if stage == 0 and sum(0 < self.stage.get(j, 0) <= DUO for j in LINES[COLOR[u]]) >= ABREAST:
            return True
        if stage == DUO and BEFORE[u] is not None and (BEFORE[u], LAST) not in self.mark:
            return True
        return stage in (0, DUO, RING) and not self.free(u, stage // DUO)

    def start(self, u):
        self.stage[u], self.ready[u] = 0, self.now

    def due(self):
        first = len(self.order)
        while True:
            ripe = [(self.ready[u], u) for u in self.stage if self.ready[u] <= self.now and not self.blocked(u)]
            if not ripe:
                return self.order[first:]
            self.run(min(ripe)[1])

    def vacated(self, u):
        return (u, DUO) in self.mark

    def rush(self, done):
        first = len(self.order)
        while not done():
            self.run(min((self.ready[u], u) for u in self.stage if not self.blocked(u))[1])
        return self.order[first:]


QB = PAIR
PAIRS = HEADS // DUO
NBLK = TOKENS // QB
HALVES = (pl.ds(0, SHARE), pl.ds(SHARE, SHARE))
PLANE = tuple((dy, dx) for dy in range(RING) for dx in range(RING) if dy or dx)
CORNERS = tuple((dy, dx) for dy, dx in PLANE if dy and dx)


class Scatter:
    def __init__(self, comm, part, mid, bufs, fin, outs, send_sems, recv_sems, swap_sems):
        self.pos, self.part, self.mid, self.bufs, self.fin, self.outs = comm.pos, part, mid, bufs, fin, outs
        self.send_sems, self.recv_sems, self.swap_sems = send_sems, recv_sems, swap_sems
        self.near = {(a, hop): comm.far(a, hop) for a in AXES for hop in (1, DUO, TRIO)}
        self.hops = {(a, hop): step(comm.pos, a, hop) for a in AXES for hop in (1, DUO, TRIO)}
        self.peer, self.core = comm.peer(), comm.core
        self.keep, self.give = tile_at(comm.core, SHARE), tile_at(1 - comm.core, SHARE)
        self.drained, self.done = set(), []

    def slot(self, u):
        return COLOR[u], RANK[u] % SLOTS

    def buf(self, u, phase):
        return self.bufs[phase].at[self.slot(u)]

    def view(self, u, phase, hop, half=None):
        order = ORDER[u]
        at = {a: ALL for a in AXES}
        for a in order[1:phase]:
            at[a] = self.pos[a]
        at[order[phase]] = self.hops[order[phase], hop] if hop else self.pos[order[phase]]
        rows = pl.ds(0, CHIP) if half is None else HALVES[half]
        if phase == 0:
            return self.part.at[PLACE[u], at['z'], at['y'], at['x'], rows, :]
        return self.mid.at[self.slot(u) + tuple(at[a] for a in 'zyx' if a != order[0]) + (rows, slice(None))]

    def copy(self, src, dst, sems, device):
        return pltpu.make_async_remote_copy(src_ref=src, dst_ref=dst, send_sem=sems[0], recv_sem=sems[1], device_id=device, device_id_type=MESH)

    def sems(self, u, phase, kind=0):
        k, i = self.slot(u)
        at = (k * SLOTS + i) * TRIO + phase
        return self.send_sems.at[at], self.recv_sems.at[(k * SLOTS + i) * 5 + DUO * phase + kind]

    def send(self, u, phase, name):
        axis = ORDER[u][phase]
        if phase == DUO:
            src, to = self.view(u, DUO, name + 1), name + 1
        else:
            hop, half, to = ((DUO, 0, 1), (DUO, 1, TRIO), (1, 1, 1), (TRIO, 0, TRIO), (1, 0, 1), (TRIO, 1, TRIO))[name]
            src = self.view(u, phase, hop, half)
        self.copy(src, self.buf(u, phase).at[name], self.sems(u, phase, int(name > 1 and phase < DUO)), self.near[axis, to]).start()

    def launch(self, u, phase):
        if BEFORE[u] is not None:
            self.drain(BEFORE[u], phase)
        for name in range(RING if phase < DUO else TRIO):
            self.send(u, phase, name)

    def arrived(self, u, phase, first, count):
        whole = self.buf(u, phase).at[pl.ds(first, count)]
        self.copy(whole, whole, self.sems(u, phase, int(first > 0)), self.peer).wait_recv()

    def drain(self, u, phase):
        if (u, phase) not in self.drained:
            self.drained.add((u, phase))
            whole = self.buf(u, phase)
            self.copy(whole, whole, self.sems(u, phase), self.peer).wait_send()

    def out(self, u):
        if u < HEADS:
            out, col = self.outs[0], self.core * HALF + u * LANES
        elif u < 10:
            out, col = self.outs[u - 7], self.core * LANES
        else:
            out, col = self.outs[TRIO], self.core * HALF + (u - 10) * LANES
        return out.at[:, pl.ds(pl.multiple_of(col, LANES), LANES)]

    def kept(self, u, turn):
        return pltpu.make_async_copy(self.fin.at[u, self.keep], self.out(u), self.swap_sems.at[DUO + turn])

    def run(self, u, stage):
        if stage == 0:
            return self.launch(u, 0)
        phase = (stage - 1) // DUO
        if stage == LAST:
            self.arrived(u, DUO, 0, TRIO)
            got = self.buf(u, DUO)
            self.fin[u] = self.view(u, DUO, 0)[...] + (got[0] + got[1] + got[DUO])
            self.copy(self.fin.at[u, self.give], self.out(u), (self.swap_sems.at[0], self.swap_sems.at[1]), self.peer).start()
            turn = len(self.done) % DUO
            if len(self.done) > 1:
                self.kept(self.done[-DUO], turn).wait()
            self.kept(u, turn).start()
            self.done.append(u)
            return
        got = self.buf(u, phase)
        if stage % DUO:
            self.arrived(u, phase, 0, DUO)
            for name, hop in ((0, 1), (1, TRIO)):
                add_into(self.view(u, phase, hop, name), got.at[name])
                self.send(u, phase, name + RING)
            return
        self.arrived(u, phase, DUO, RING)
        if phase == 0 and BEFORE[u] is not None:
            self.drain(BEFORE[u], 1)
            self.drain(BEFORE[u], DUO)
        for half, names in ((0, (TRIO, RING)), (1, (DUO, 5))):
            if phase:
                add_into(self.view(u, phase, 0, half), *[got.at[name] for name in names])
            else:
                dst = self.mid.at[self.slot(u) + (ALL, ALL, HALVES[half], slice(None))]
                add_into(dst, self.view(u, 0, 0, half), *[got.at[name] for name in names], fresh=True)
        self.launch(u, phase + 1)

    def finish(self):
        for u in range(N_UNITS):
            for phase in range(TRIO):
                self.drain(u, phase)
        half = self.fin.at[:, pl.ds(0, SHARE)]
        swaps = self.copy(half, half, (self.swap_sems.at[0], self.swap_sems.at[1]), self.peer)
        swaps.wait_send()
        swaps.wait_recv()
        for turn in range(DUO):
            self.kept(self.done[turn - DUO], turn).wait()


def attend(heads, qt, do_t, k, kt, v, vt, cos, sin, o_row, ot, dq, dkt, dvt, s_scr, e_scr, p_scr, d_scr):
    f32, bf16 = jnp.float32, jnp.bfloat16
    strip = TURN
    work = [(h, j) for j in range(NBLK) for h in range(len(heads))]

    def strips(c):
        return [(i * strip, slice(c * QB + i * strip, c * QB + (i + 1) * strip)) for i in range(QB // strip)]

    def fold(x, op):
        return op(x.reshape(strip // SUBS, SUBS, QB), axis=0)

    def scores(i):
        (h, j), b = work[i], i % DUO
        q_t = qt[heads[h], j * QB:(j + 1) * QB]
        top = jnp.full((SUBS, QB), -jnp.inf, f32)
        for c in range(j + 1):
            tile = dot(k[c * QB:(c + 1) * QB, :], q_t)
            for at, rows in strips(c):
                s = tile[at:at + strip]
                if c == j:
                    seen = lax.broadcasted_iota(jnp.int32, (strip, QB), 0) + at <= lax.broadcasted_iota(jnp.int32, (strip, QB), 1)
                    s = jnp.where(seen, s, -jnp.inf)
                s_scr[b, rows, :] = s
                top = jnp.maximum(top, fold(s, jnp.max))
        return jnp.max(top, axis=0, keepdims=True)

    def rest(i, m):
        (h, j), b = work[i], i % DUO
        cols, n = slice(j * QB, (j + 1) * QB), (j + 1) * QB
        q_t, d_t = qt[heads[h], cols], do_t[heads[h], cols]
        tot = jnp.zeros((SUBS, QB), f32)
        for c in range(j + 1):
            for at, rows in strips(c):
                e = jnp.exp2((s_scr[b, rows, :] - m) * (SCALE * LOG2E))
                s_scr[b, rows, :] = e
                e_scr[b, rows, :] = e.astype(bf16)
                tot = tot + fold(e, jnp.sum)
        den = jnp.sum(tot, axis=0, keepdims=True)
        inv = 1.0 / den
        o = (dot(vt[:, :n], e_scr[b, :n, :]) / den).astype(bf16)
        ot[o_row(h), cols] = o
        delta = jnp.sum(d_t.astype(f32) * o.astype(f32), axis=0, keepdims=True)
        for c in range(j + 1):
            dp = dot(v[c * QB:(c + 1) * QB, :], d_t)
            for at, rows in strips(c):
                p = s_scr[b, rows, :] * inv
                p_scr[b, rows, :] = p.astype(bf16)
                d_scr[b, rows, :] = (p * (dp[at:at + strip] - delta)).astype(bf16)
        dvt[:, :n] += dot_nt(d_t, p_scr[b, :n, :])
        dkt[:, :n] += dot_nt(q_t, d_scr[b, :n, :])
        g = dot(kt[:, :n], d_scr[b, :n, :]) * SCALE
        co, si = cos[:, cols], sin[:, cols]
        x, y = g[:TURN], g[TURN:]
        dq[heads[h], cols] = jnp.concatenate([x * co + y * si, y * co - x * si], axis=0).astype(bf16)

    m = scores(0)
    for i in range(len(work)):
        later = scores(i + 1) if i + 1 < len(work) else None
        rest(i, m)
        m = later


def tail_kernel(qt, do_t, k, kt, v, vt, rt, dyc, wqk, wqkp, wvo, wvop, gain, hidden, dy, pos, cos, sin,
                result, grad_x, gq, gk, gv, go, gout,
                two, ks, kts, vs, vts, rts, ots, dqo, dqp, dkvo, dkvp, dkt, dvt, s_scr, e_scr, p_scr, d_scr, dycs, part, mid, buf1, buf2, buf3, fin, own, onat, dnat, xs, gacc, gpart, gpeer, gz, gx,
                send_sems, recv_sems, swap_sems, trade_send, trade_recv, local_sems):
    comm = Singles(trade_send, trade_recv, local_sems)
    comm.used = HEADS
    f32, bf16 = jnp.float32, jnp.bfloat16
    core, peer = comm.core, comm.peer()
    a1, a2 = two.at[0], two.at[1]
    sc = Scatter(comm, part, mid, (buf1, buf2, buf3), fin, (gq, gk, gv, go), send_sems, recv_sems, swap_sems)
    plan = Plan()
    some, most = pl.ds(0, PAIR), pl.ds(PAIR, HALF - PAIR)
    loads = [comm.local(s, d) for s, d in ((qt.at[some], two.at[0, some]), (k, ks), (do_t.at[some], two.at[1, some]), (vt, vts), (v, vs), (kt, kts))]
    comm.announce(CORNERS)
    dkt[...] = jnp.zeros_like(dkt)
    dvt[...] = jnp.zeros_like(dvt)
    with scope('wait_q'):
        for c in loads:
            c.wait()
    loads = [comm.local(s, d) for s, d in ((rt, rts), (qt.at[most], two.at[0, most]), (do_t.at[most], two.at[1, most]))]
    later = [comm.local(s, d) for s, d in ((dyc, dycs), (hidden, xs))]

    def emit(stages):
        for u, stage in stages:
            with scope(f'u{u}_s{stage}'):
                if u == GAIN:
                    sum_gain(stage)
                else:
                    sc.run(u, stage)

    def after(cost):
        plan.now += cost
        return plan.due()

    def head_trades(g):
        row = pl.ds(pl.multiple_of((core * HEADS + DUO * g) * LANES, PAIR), PAIR)
        mine = tile_at(g, PAIR)
        return [pltpu.make_async_remote_copy(src_ref=s, dst_ref=d, send_sem=trade_send.at[i], recv_sem=trade_recv.at[i], device_id=peer, device_id_type=MESH)
                for s, d, i in ((ots.at[row], ots.at[row], g), (dqo.at[mine], dqp.at[mine], PAIRS + g))]

    def gradient(place, count, left, right, mul, steps=DUO):
        with scope('grad'):
            @pl.loop(0, steps)
            def _(z):
                g = mul(left[tile_at(z, DIM // steps), :], right())
                for i in range(count):
                    part[place + i, tile_at(z, RING // steps)] = g[:, i * LANES:(i + 1) * LANES].reshape(RING // steps, RING, RING, CHIP, LANES)

    attended, paired = [], []
    for g in range(PAIRS):
        attended.append(after(5.15))
        plan.now += 1.4
        plan.start(DUO * g)
        plan.start(DUO * g + 1)
        paired.append(plan.due())

    @pl.loop(0, PAIRS)
    def _(g):
        def at(table):
            for i in range(PAIRS):
                if table[i]:
                    pl.when(g == i)(functools.partial(emit, table[i]))

        heads = [tile_at(DUO * g + i, LANES) for i in range(DUO)]
        with scope('attend'):
            attend(heads, a1, a2, ks, kts, vs, vts, cos, sin, lambda i: tile_at(core * HEADS + DUO * g + i, LANES), ots, dqo, dkt, dvt, s_scr, e_scr, p_scr, d_scr)

        @pl.when(g == 0)
        def _():
            with scope('entry'):
                comm.meet(CORNERS)
                for c in loads:
                    c.wait()
        for c in head_trades(g):
            c.start()
        at(attended)
        gradient(DUO * g, DUO, rts, lambda: dqo[tile_at(g, PAIR), :], dot_nt, 1)
        at(paired)

    def beat(cost, *starts):
        plan.now += cost
        for u in starts:
            plan.start(u)
        emit(plan.due())

    wkv, wkvp = e_scr.reshape(DIM, PAIR), p_scr.reshape(DIM, PAIR)
    later += [comm.local(src.at[:, pl.ds(at, LANES)], dst.at[:, pl.ds(to, LANES)]) for srcs, dst in (((wqk, wvo), wkv), ((wqkp, wvop), wkvp)) for src, at, to in ((srcs[0], HALF, 0), (srcs[1], 0, LANES))]
    wqp_loads = [comm.local(wqkp.at[tile_at(i, HALF), pl.ds(0, HALF)], two.at[i]) for i in range(DUO)]
    key = dkt[...] * SCALE
    co, si, x, y = cos[...], sin[...], key[:TURN], key[TURN:]
    dkvo[:LANES, :] = jnp.concatenate([x * co + y * si, y * co - x * si], axis=0).astype(bf16)
    dkvo[LANES:, :] = dvt[...].astype(bf16)
    comm.trade(dkvo, dkvp)
    gradient(UNIT_K, DUO, rts, lambda: dkvo[...], dot_nt)
    beat(1.8, UNIT_K, UNIT_V)
    wq_load = comm.local(wqk.at[:, pl.ds(0, HALF)], rts)
    for c in later:
        c.wait()
    with scope('trades'):
        for g in range(PAIRS):
            for c in head_trades(g):
                c.wait()

    waiting = list(range(RING))

    def output_gradients(force=False):
        while waiting:
            first = 10 + DUO * waiting[0]
            before = [u for u in range(N_UNITS) if u < first and PLACE[u] in (PLACE[first], PLACE[first + 1])]
            if force:
                emit(plan.rush(lambda: all(map(plan.vacated, before))))
            if not all(map(plan.vacated, before)):
                return
            for u in before:
                sc.drain(u, 0)
            i = waiting.pop(0)
            gradient(PLACE[first], DUO, ots, lambda: dycs[:, i * PAIR:(i + 1) * PAIR], dot)
            plan.start(first)
            plan.start(first + 1)
            beat(1.5)

    def piece(cost):
        beat(cost)
        output_gradients()

    def ticking(n, cost, body):
        tables = [after(cost) for _ in range(n)]

        @pl.loop(0, n)
        def _(i):
            body(i)
            for j, table in enumerate(tables):
                if table:
                    pl.when(i == j)(functools.partial(emit, table))
        output_gradients()

    @pl.loop(0, TOKENS // LANES)
    def _(i):
        want = lax.broadcasted_iota(jnp.int32, (LANES, ROWS), 0) + i * LANES
        own[tile_at(i, LANES), :] = jnp.where(want == pos[...], 1.0, 0.0).astype(bf16)

    def unsort(at, src_t, n):
        with scope('unsort'):
            dnat[at:at + n, :] = dot(src_t[:n, :], own[...]).astype(bf16)

    output_gradients()
    for c in comm.exchanged:
        c.wait_recv()
    unsort(0, dqo, HALF)
    dy_loads = [comm.local(dy.at[:, tile_at(i, HALF)], dqo.at[tile_at(i, ROWS)]) for i in range(DUO)]
    piece(1.2)
    unsort(HALF, dqp, HALF)
    piece(1.2)
    unsort(DUO * HALF, dkvo, PAIR)
    unsort(DUO * HALF + PAIR, dkvp, PAIR)
    piece(0.7)
    wq_load.wait()
    for c in wqp_loads + dy_loads:
        c.wait()
    gacc[...] = jnp.zeros_like(gacc)

    def dr_parts(half, r):
        return [s_scr.at[half, r(i * PAIR), :] for i in range(RING)]

    def back(block, then):
        def dr(half):
            with scope('dr'):
                c = tile_at(half, HALF)
                left = jnp.concatenate([rts[c, :], two[half], wkv[c, :], wkvp[c, :]], axis=1)
                acc = dot(left, dnat[:, block * PAIR:(block + 1) * PAIR])
                for i, ref in enumerate(dr_parts(half, lambda at: pl.ds(at, PAIR))):
                    ref[...] = acc[i * PAIR:(i + 1) * PAIR, :].T

        def norm(part):
            with scope('back'):
                @pl.loop(0, RING)
                def _(i):
                    j = part * RING + i
                    q = pl.ds(pl.multiple_of(block * PAIR + j * SHARE, SHARE), SHARE)
                    d = jnp.concatenate([ref[...] for half in range(DUO) for ref in dr_parts(half, lambda at: pl.ds(pl.multiple_of(at + j * SHARE, SHARE), SHARE))], axis=1)
                    x = xs[q, :].astype(f32)
                    inv = lax.rsqrt(jnp.mean(x * x, axis=-1, keepdims=True) + RMS_EPS)
                    unit = x * inv
                    gacc[...] += jnp.sum((d * unit).reshape(DUO, SUBS, DIM), axis=0)
                    dg = d * gain[0:1, :]
                    new = inv * (dg - unit * jnp.mean(dg * unit, axis=-1, keepdims=True))
                    for half in range(DUO):
                        r = pl.ds(pl.multiple_of(half * ROWS + block * PAIR + j * SHARE, SHARE), SHARE)
                        dqo[r, :] = (dqo[r, :].astype(f32) + new[:, half * HALF:(half + 1) * HALF]).astype(bf16)

        ticking(DUO, 1.6, dr)
        then()
        ticking(RING, 0.92, norm)

    back(0, lambda: None)
    wo_loads = []
    back(1, lambda: wo_loads.extend([comm.local(wvo.at[:, pl.ds(LANES, HALF)], rts)] + [comm.local(wvop.at[tile_at(i, HALF), pl.ds(LANES, HALF)], two.at[i]) for i in range(DUO)]))
    for i in range(DUO):
        comm.store(dqo.at[tile_at(i, ROWS)], grad_x.at[:, tile_at(i, HALF)])
    total = jnp.sum(gacc[...], axis=0, keepdims=True)
    gpart[...] = jnp.zeros_like(gpart)
    for i in range(RING):
        for j in range(RING):
            gpart[i, j:j + 1, :] = total[:, (i * RING + j) * LANES:(i * RING + j + 1) * LANES]

    gain_c, gain_z, gain_p = (Batch(comm) for _ in range(TRIO))

    def sum_gain(stage):
        if stage == 0:
            gain_c.send(gpart, gpeer, peer)
        elif stage == 1:
            gain_c.arrived(gpeer)
            for j in range(RING):
                gz[j] = gpart[j] + gpeer[j]
            for hop in (1, DUO, TRIO):
                gain_z.send(gz.at[step(comm.pos, 'z', hop)], gz.at[TRIO + hop], comm.far('z', hop))
        elif stage == DUO:
            gain_z.arrived(gz.at[pl.ds(RING, TRIO)])
            gx[0] = (gz[comm.pos['z']] + gz[RING]) + (gz[5] + gz[6])
            for dy, dx in PLANE:
                gain_p.send(gx.at[0], gx.at[dy * RING + dx], comm.aside(dy, dx))
        else:
            gain_p.arrived(gx.at[pl.ds(1, 15)])
            gpeer[0] = jnp.sum(gx[...], axis=0)
            mine = jnp.broadcast_to(gpeer[0, pl.ds(comm.pos['y'], 1), :], (SUBS, LANES))
            gout[...] = pltpu.roll(mine, LANES - (comm.pos['x'] * CHIP + core * SHARE), 1)

    plan.start(GAIN)
    beat(0.2)
    for i in range(DUO):
        with scope('unsort_o'):
            @pl.loop(0, DUO)
            def _(j):
                r = pl.ds(pl.multiple_of(i * HALF + j * ROWS, ROWS), ROWS)
                onat[:, r] = dot(ots[r, :], own[...]).astype(bf16).T
        piece(1.58)
    output_gradients(True)

    def project_out(col, weights, i):
        with scope('project'):
            @pl.loop(DUO * i, DUO * i + DUO)
            def _(j):
                c = tile_at(j, PAIR)
                dst = pl.ds(pl.multiple_of(col + j * PAIR, PAIR), PAIR)
                xs[:, dst] = (xs[:, dst].astype(f32) + dot(onat[...], weights(c))).astype(bf16)
        beat(1.48)

    def own_half(c):
        return rts[:, c]

    def other_half(c):
        return jnp.concatenate([a1[:, c], a2[:, c]], axis=0)

    for c in wo_loads:
        c.wait()
    for col, weights in ((core * HALF, own_half), ((1 - core) * HALF, other_half)):
        for i in range(DUO):
            project_out(col, weights, i)
    comm.store(xs, result)
    emit(plan.rush(lambda: not plan.stage))
    with scope('finish'):
        sc.finish()
        for batch, whole in ((gain_c, gpart), (gain_z, gz.at[pl.ds(RING, TRIO)]), (gain_p, gx.at[pl.ds(1, 15)])):
            batch.sent(whole)
        for c in comm.exchanged:
            c.wait_send()
        for c in comm.stored:
            c.wait()


def tail(qt, do_t, k, kt, v, vt, rt, dyc, wqk, wqkp, wvo, wvop, gain, hidden, dy, pos, cos, sin):
    bf16, f32 = jnp.bfloat16, jnp.float32
    any_ = pl.BlockSpec(memory_space=pl.ANY)
    vmem = pl.BlockSpec(memory_space=pltpu.VMEM)
    S = lambda shape, d=bf16: jax.ShapeDtypeStruct(shape, d)
    V = lambda shape, d=bf16: pltpu.VMEM(shape, d)
    D = lambda n: pltpu.SemaphoreType.DMA((n,))
    sq, tall, wide = (HALF, TOKENS), (TOKENS, LANES), (LANES, TOKENS)
    mine, kv = (ROWS, DIM), (PAIR, TOKENS)
    return pl.pallas_call(
        tail_kernel,
        out_shape=[S(mine), S(mine), S((SHARE, DIM), f32), S((SHARE, PAIR), f32), S((SHARE, PAIR), f32), S((SHARE, DIM), f32), S((SUBS, LANES), f32)],
        in_specs=[any_] * 12 + [vmem] + [any_] * DUO + [vmem] * TRIO,
        out_specs=[any_] * 6 + [vmem],
        scratch_shapes=[V((DUO,) + sq), V(tall), V(wide), V(tall), V(wide), V((DIM, TOKENS)), V((DIM, TOKENS)), V(sq), V(sq), V(kv), V(kv), V(wide, f32), V(wide, f32),
                        V((DUO, TOKENS, QB), f32), V((DUO, TOKENS, QB)), V((DUO, TOKENS, QB)), V((DUO, TOKENS, QB)), V(sq), V((PLACES, RING, RING, RING, CHIP, LANES), f32), V((TRIO, SLOTS, RING, RING, CHIP, LANES), f32),
                        V((TRIO, SLOTS, 6, RING, RING, SHARE, LANES), f32), V((TRIO, SLOTS, 6, RING, SHARE, LANES), f32), V((TRIO, SLOTS, TRIO, CHIP, LANES), f32), V((N_UNITS, CHIP, LANES), f32), V((TOKENS, ROWS)), V(mine), V((DUO * QKV, ROWS)), V(mine),
                        V((SUBS, DIM), f32), V((RING, SUBS, LANES), f32), V((RING, SUBS, LANES), f32), V((7, SUBS, LANES), f32), V((SHARE, SUBS, LANES), f32),
                        D(9 * SLOTS), D(15 * SLOTS), D(RING), D(HEADS + RING), D(HEADS + RING), D(26)],
        compiler_params=pltpu.CompilerParams(collective_id=1, has_side_effects=True, vmem_limit_bytes=67043328),
        name='tail',
    )(qt, do_t, k, kt, v, vt, rt, dyc, wqk, wqkp, wvo, wvop, gain, hidden, dy, pos, cos, sin)


def settle_kernel(n, *refs):
    ins, gain, outs, gain_out, bufs, sems = refs[:n], refs[n], refs[n + 1:DUO * n + 1], refs[DUO * n + 1], refs[DUO * n + DUO:-1], refs[-1]
    jobs = []
    for a, o, b in zip(ins, outs, bufs):
        size = a.shape[0] // RING if a.shape[0] == ROWS else a.shape[0]
        jobs += [tuple(r.at[pl.ds(i, size)] for r in (a, b, o)) for i in range(0, a.shape[0], size)]
    takes = [pltpu.make_async_copy(a, b, sems.at[0, i]) for i, (a, b, _) in enumerate(jobs)]
    puts = [pltpu.make_async_copy(b, o, sems.at[1, i]) for i, (_, b, o) in enumerate(jobs)]
    for c in takes:
        c.start()
    gain_out[...] = gain[0:1, :SHARE]
    for take, put in zip(takes, puts):
        take.wait()
        put.start()
    for c in puts:
        c.wait()


def settle(*arrays):
    *large, gain = arrays
    any_, vmem = pl.BlockSpec(memory_space=pl.ANY), pl.BlockSpec(memory_space=pltpu.VMEM)
    return pl.pallas_call(
        functools.partial(settle_kernel, len(large)),
        out_shape=[jax.ShapeDtypeStruct(a.shape, a.dtype) for a in large] + [jax.ShapeDtypeStruct((1, SHARE), gain.dtype)],
        in_specs=[any_] * len(large) + [vmem],
        out_specs=[any_] * len(large) + [vmem],
        scratch_shapes=[pltpu.VMEM(a.shape, a.dtype) for a in large] + [pltpu.SemaphoreType.DMA((DUO, 12))],
        name='settle',
    )(*arrays)


def rope_tables():
    j = np.arange(HEAD_DIM // DUO, dtype=np.float64) / (HEAD_DIM // DUO)
    freq = (ROPE_THETA ** -j).astype(np.float32)
    angle = freq[:, None] * np.arange(TOKENS, dtype=np.float32)[None, :]
    return np.cos(angle.astype(np.float64)).astype(np.float32), np.sin(angle.astype(np.float64)).astype(np.float32)


def solution(mesh):
    def shard_fn(hidden, tok_pos, grad_out, norm_gain, w_query, w_key, w_value, w_out):
        hidden, grad_out = hidden[0], grad_out[0]
        cos_t, sin_t = (jnp.asarray(t) for t in rope_tables())
        *parts, gain = head(hidden, grad_out, w_query, w_key, w_value, w_out, tok_pos, norm_gain.reshape(1, SHARE), cos_t, sin_t)
        parts = [p.reshape(DIM, GROUP) if p.ndim > DUO else p for p in parts]
        result, grad_hidden, gq, gk, gv, go, gout = settle(*tail(*parts, gain, hidden, grad_out, tok_pos, cos_t, sin_t))
        return result[None], grad_hidden[None], gq, gk, gv, go, gout.reshape(SHARE)

    row_spec, pos_spec = P('fsdp', 'cp', None), P('fsdp', 'cp')
    weight_spec, gain_spec = P(('fsdp', 'cp'), None), P(('fsdp', 'cp'))
    return jax.shard_map(shard_fn, mesh=mesh, in_specs=(row_spec, pos_spec, row_spec, gain_spec, weight_spec, weight_spec, weight_spec, weight_spec), out_specs=(row_spec, row_spec, weight_spec, weight_spec, weight_spec, weight_spec, gain_spec), check_vma=False)
```
